8 devices in a mesh: rep: 1 (over z), tp: 2 (over y), stage: 4 (over x, core).
Axes of the slice: x: 2, y: 2, z: 1, core: 2. Of those that a mesh axis runs over, the one named last changes fastest.
Arguments:
- inputs: bfloat16 [8, 2, 192, 1536], P('rep')
- targets: bfloat16 [8, 2, 192, 1536], P('rep')
- w_qkv: bfloat16 [4, 1536, 3, 16, 96], P(('rep', 'stage'), None, None, 'tp')
- w_out: bfloat16 [4, 16, 96, 1536], P(('rep', 'stage'), 'tp')
- w_up: bfloat16 [4, 1536, 6144], P(('rep', 'stage'), None, 'tp')
- w_down: bfloat16 [4, 6144, 1536], P(('rep', 'stage'), 'tp')
- gain_attn: bfloat16 [4, 1536], P(('rep', 'stage'))
- gain_mlp: bfloat16 [4, 1536], P(('rep', 'stage'))
Outputs:
- output 1: float32 [1], P('rep')
- output 2: bfloat16 [8, 2, 192, 1536], P('rep')
- output 3: float32 [4, 1536, 3, 16, 96], P(('rep', 'stage'), None, None, 'tp')
- output 4: float32 [4, 16, 96, 1536], P(('rep', 'stage'), 'tp')
- output 5: float32 [4, 1536, 6144], P(('rep', 'stage'), None, 'tp')
- output 6: float32 [4, 6144, 1536], P(('rep', 'stage'), 'tp')
- output 7: float32 [4, 1536], P(('rep', 'stage'))
- output 8: float32 [4, 1536], P(('rep', 'stage'))
All inputs are finite; a program needn't handle non-finite values.
Results may differ from the reference program's by a relative error of at most 0.02.
Values are sent between devices in bfloat16 or wider.
A program may use at most 1 GiB of HBM per device.

```python
import jax
import jax.numpy as jnp
from jax import lax

MICROBATCHES = 8
SEQ_PER_MICRO = 2
SEQ_LEN = 192
HIDDEN = 1536
NUM_HEADS = 16
STAGES = 4
HEAD_DIM = HIDDEN // NUM_HEADS
FFN_WIDTH = 4 * HIDDEN
NORM_EPS = 1e-5


def setup_inputs(seed: int = 0, part: int = 0) -> dict:
    base_key = jax.random.fold_in(jax.random.key(seed), part)
    sub_keys = jax.random.split(base_key, 8)
    act_shape = (MICROBATCHES, SEQ_PER_MICRO, SEQ_LEN, HIDDEN)

    def normal_draw(key_index, shape, scale):
        return (jax.random.normal(sub_keys[key_index], shape, jnp.float32) * scale).astype(jnp.bfloat16)

    return {
        'inputs': normal_draw(0, act_shape, 1.0),
        'targets': normal_draw(1, act_shape, 1.0),
        'w_qkv': normal_draw(2, (STAGES, HIDDEN, 3, NUM_HEADS, HEAD_DIM), HIDDEN ** -0.5),
        'w_out': normal_draw(3, (STAGES, NUM_HEADS, HEAD_DIM, HIDDEN), HIDDEN ** -0.5),
        'w_up': normal_draw(4, (STAGES, HIDDEN, FFN_WIDTH), HIDDEN ** -0.5),
        'w_down': normal_draw(5, (STAGES, FFN_WIDTH, HIDDEN), FFN_WIDTH ** -0.5),
        'gain_attn': (1.0 + 0.3 * jax.random.normal(sub_keys[6], (STAGES, HIDDEN), jnp.float32)).astype(jnp.bfloat16),
        'gain_mlp': (1.0 + 0.3 * jax.random.normal(sub_keys[7], (STAGES, HIDDEN), jnp.float32)).astype(jnp.bfloat16),
    }


def rms_core(x_f32, gain_f32):
    inv_rms = lax.rsqrt(jnp.mean(x_f32 * x_f32, axis=-1, keepdims=True) + NORM_EPS)
    return x_f32 * inv_rms * gain_f32


def layer_apply(act_in, params):
    w_qkv, w_out, w_up, w_down, gain_attn, gain_mlp = params
    in_f32 = act_in.astype(jnp.float32)
    normed_a = rms_core(in_f32, gain_attn).astype(jnp.bfloat16)
    proj_qkv = jnp.einsum('bsd,dkhe->kbhse', normed_a.astype(jnp.float32), w_qkv).astype(jnp.bfloat16)
    query = proj_qkv[0].astype(jnp.float32)
    key_f32 = proj_qkv[1].astype(jnp.float32)
    value = proj_qkv[2].astype(jnp.float32)
    scores = jnp.einsum('bhqe,bhke->bhqk', query, key_f32) * (HEAD_DIM ** -0.5)
    positions = jnp.arange(SEQ_LEN)
    causal = positions[None, :] <= positions[:, None]
    attn_probs = jax.nn.softmax(jnp.where(causal, scores, -1e30), axis=-1).astype(jnp.bfloat16)
    context = jnp.einsum('bhqk,bhke->bhqe', attn_probs.astype(jnp.float32), value).astype(jnp.bfloat16)
    attn_sum = jnp.einsum('bhse,hed->bsd', context.astype(jnp.float32), w_out)
    mid_f32 = (in_f32 + attn_sum).astype(jnp.bfloat16).astype(jnp.float32)
    normed_m = rms_core(mid_f32, gain_mlp).astype(jnp.bfloat16)
    up_proj = jnp.einsum('bsd,df->bsf', normed_m.astype(jnp.float32), w_up).astype(jnp.bfloat16)
    hidden_act = jax.nn.gelu(up_proj.astype(jnp.float32), approximate=True).astype(jnp.bfloat16)
    down_sum = jnp.einsum('bsf,fd->bsd', hidden_act.astype(jnp.float32), w_down)
    return (mid_f32 + down_sum).astype(jnp.bfloat16)


def reference(inputs, targets, w_qkv, w_out, w_up, w_down, gain_attn, gain_mlp):
    params = tuple(weight.astype(jnp.float32) for weight in (w_qkv, w_out, w_up, w_down, gain_attn, gain_mlp))
    norm_factor = 1.0 / (MICROBATCHES * SEQ_PER_MICRO * SEQ_LEN * HIDDEN)
    layer_saved = jax.checkpoint(layer_apply)

    def micro_loss(param_set, x_micro, y_micro):
        def body(act_carry, layer_params):
            return layer_saved(act_carry, layer_params), None
        final_act, _ = lax.scan(body, x_micro, param_set)
        error_f32 = final_act.astype(jnp.float32) - y_micro.astype(jnp.float32)
        return 0.5 * jnp.sum(error_f32 * error_f32) * norm_factor

    def step(carry, pair):
        loss_sum, grad_sums = carry
        x_micro, y_micro = pair
        loss_micro, pull_back = jax.vjp(lambda param_set, x_in: micro_loss(param_set, x_in, y_micro), params, x_micro)
        grad_params, grad_x = pull_back(jnp.ones((), jnp.float32))
        grad_sums = tuple(total + grad_part for total, grad_part in zip(grad_sums, grad_params))
        return (loss_sum + loss_micro, grad_sums), grad_x

    init_carry = (jnp.zeros((), jnp.float32), tuple(jnp.zeros_like(weight) for weight in params))
    (loss_total, grads), d_inputs = lax.scan(step, init_carry, (inputs, targets))
    return (loss_total.reshape(1), d_inputs, grads[0], grads[1], grads[2], grads[3], grads[4], grads[5])
```

```python
import jax
import jax.numpy as jnp
from jax import lax
from jax.sharding import PartitionSpec as P

NORM_EPS = 1e-5
AX = ('tp', 'stage')
BF = jnp.bfloat16
F32 = jnp.float32

FWD = [(0, 4), (1, 5), (4, 6), (5, 7), (6, 2), (7, 3)]
BWD = [(b, a) for a, b in FWD]
R_SWAP = [(1, 4), (4, 1), (2, 7), (7, 2)]
CORE_SWAP = [(0, 1), (1, 0), (2, 3), (3, 2), (4, 5), (5, 4), (6, 7), (7, 6)]
L_TO_R = [(0, 1), (5, 4), (6, 7), (3, 2)]
R_TO_L = [(1, 0), (4, 5), (7, 6), (2, 3)]
L_ACROSS = [(0, 4), (5, 1), (6, 2), (3, 7)]


def move(value, perm):
    return lax.ppermute(value, AX, perm)


def inv_rms(x_f32):
    return lax.rsqrt(jnp.mean(x_f32 * x_f32, axis=-1, keepdims=True) + NORM_EPS)


def rms_core(x_f32, gain_f32):
    return x_f32 * inv_rms(x_f32) * gain_f32


def gelu_tanh(up_f32):
    return jax.nn.gelu(up_f32, approximate=True)


def dot(eq, a, b):
    return jnp.einsum(eq, a, b, preferred_element_type=F32)


def attn_scores(query, key):
    seq_len = query.shape[-2]
    scores = dot('bhqe,bhke->bhqk', query, key) * (query.shape[-1] ** -0.5)
    q_pos = lax.broadcasted_iota(jnp.int32, (seq_len, seq_len), 0)
    k_pos = lax.broadcasted_iota(jnp.int32, (seq_len, seq_len), 1)
    return jax.nn.softmax(jnp.where(k_pos <= q_pos, scores, -1e30), axis=-1)


def attn_forward(qkv):
    probs = attn_scores(qkv[0], qkv[1])
    return probs, dot('bhqk,bhke->bhqe', probs.astype(BF), qkv[2]).astype(BF)


def attn_backward(qkv, probs, d_context):
    scale = qkv.shape[-1] ** -0.5
    d_probs = dot('bhqe,bhke->bhqk', d_context, qkv[2]).astype(BF).astype(F32)
    d_value = dot('bhqk,bhqe->bhke', probs.astype(BF), d_context).astype(BF)
    d_scores = probs * (d_probs - jnp.sum(d_probs * probs, axis=-1, keepdims=True)) * scale
    d_query = jnp.einsum('bhqk,bhke->bhqe', d_scores, qkv[1].astype(F32), precision=lax.Precision.HIGHEST).astype(BF)
    d_key = jnp.einsum('bhqk,bhqe->bhke', d_scores, qkv[0].astype(F32), precision=lax.Precision.HIGHEST).astype(BF)
    return jnp.stack([d_query, d_key, d_value])


def home_forward(act, slots, gain_attn, gain_mlp):
    in_f32 = act.astype(F32)
    normed_a = rms_core(in_f32, gain_attn).astype(BF)
    total = in_f32
    saved_qkv = []
    part = None
    for w_qkv, w_out, _, _ in slots:
        qkv = dot('bsd,dkhe->kbhse', normed_a, w_qkv).astype(BF)
        _, context = attn_forward(qkv)
        term = dot('bhse,hed->bsd', context, w_out)
        part = term if part is None else part + term
        saved_qkv.append(qkv)
    mid = (in_f32 + part).astype(BF)
    normed_m = rms_core(mid.astype(F32), gain_mlp).astype(BF)
    part = None
    saved_up = []
    for _, _, w_up, w_down in slots:
        up = dot('bsd,df->bsf', normed_m, w_up).astype(BF)
        hidden = gelu_tanh(up.astype(F32)).astype(BF)
        term = dot('bsf,fd->bsd', hidden, w_down)
        part = term if part is None else part + term
        saved_up.append(up)
    out = (mid.astype(F32) + part).astype(BF)
    return out, (act, mid, saved_qkv, saved_up)


def norm_backward(x_f32, gain, d_normed):
    _, pull = jax.vjp(rms_core, x_f32, gain)
    return pull(d_normed)


def home_backward(saved, grad_out, slots, gain_attn, gain_mlp):
    act, mid, saved_qkv, saved_up = saved
    part = None
    for (_, _, w_up, w_down), up in zip(slots, saved_up):
        d_act = dot('bsd,fd->bsf', grad_out, w_down).astype(BF)
        _, pull = jax.vjp(gelu_tanh, up.astype(F32))
        d_up = pull(d_act.astype(F32))[0].astype(BF)
        term = dot('bsf,df->bsd', d_up, w_up)
        part = term if part is None else part + term
    d_mid_norm, d_gain_mlp = norm_backward(mid.astype(F32), gain_mlp, part.astype(BF).astype(F32))
    d_mid = (grad_out.astype(F32) + d_mid_norm).astype(BF)
    part = None
    for (w_qkv, w_out, _, _), qkv in zip(slots, saved_qkv):
        d_context = dot('bsd,hed->bhse', d_mid, w_out).astype(BF)
        probs = attn_scores(qkv[0], qkv[1])
        d_qkv = attn_backward(qkv, probs, d_context)
        term = dot('kbhse,dkhe->bsd', d_qkv, w_qkv)
        part = term if part is None else part + term
    d_in_norm, d_gain_attn = norm_backward(act.astype(F32), gain_attn, part.astype(BF).astype(F32))
    d_in = (d_mid.astype(F32) + d_in_norm).astype(BF)
    return d_in, d_mid, d_gain_attn, d_gain_mlp


def owner_grads(act, mid, d_mid, grad_out, weights):
    w_qkv, w_out, w_up, w_down, gain_attn, gain_mlp = weights
    normed_a = rms_core(act.astype(F32), gain_attn).astype(BF)
    qkv = dot('bsd,dkhe->kbhse', normed_a, w_qkv).astype(BF)
    probs, context = attn_forward(qkv)
    d_w_out = dot('bhse,bsd->hed', context, d_mid)
    d_context = dot('bsd,hed->bhse', d_mid, w_out).astype(BF)
    d_qkv = attn_backward(qkv, probs, d_context)
    d_w_qkv = dot('bsd,kbhse->dkhe', normed_a, d_qkv)
    normed_m = rms_core(mid.astype(F32), gain_mlp).astype(BF)
    up_f32 = dot('bsd,df->bsf', normed_m, w_up).astype(BF).astype(F32)
    hidden = gelu_tanh(up_f32).astype(BF)
    d_w_down = dot('bsf,bsd->fd', hidden, grad_out)
    d_act = dot('bsd,fd->bsf', grad_out, w_down).astype(BF)
    _, pull = jax.vjp(gelu_tanh, up_f32)
    d_up = pull(d_act.astype(F32))[0].astype(BF)
    d_w_up = dot('bsd,bsf->df', normed_m, d_up)
    return d_w_qkv, d_w_out, d_w_up, d_w_down


def solution(mesh):
    act_spec = P('rep', None, None, None)
    weight_specs = (
        P(('rep', 'stage'), None, None, 'tp', None),
        P(('rep', 'stage'), 'tp', None, None),
        P(('rep', 'stage'), None, 'tp'),
        P(('rep', 'stage'), 'tp', None),
        P(('rep', 'stage'), None),
        P(('rep', 'stage'), None),
    )

    def device_fn(inputs, targets, w_qkv, w_out, w_up, w_down, gain_attn, gain_mlp):
        micro_count, _, seq_len, width = inputs.shape
        norm_factor = 1.0 / (inputs.size)
        stage = lax.axis_index('stage')
        tp = lax.axis_index('tp')
        x_pos, core = stage // 2, stage % 2
        home = jnp.where(x_pos == 0, tp, 3 - tp)
        is_l = stage == home
        is_first, is_last = home == 0, home == 3
        own = (w_qkv[0], w_out[0], w_up[0], w_down[0])
        own_gains = (gain_attn[0].astype(F32), gain_mlp[0].astype(F32))

        slot_x, slot_y = [], []
        for w in own:
            held = jnp.where(is_l, w, move(w, R_SWAP))
            slot_x.append(held)
            slot_y.append(move(held, CORE_SWAP))
        slots = (tuple(slot_x), tuple(slot_y))
        gains = jnp.stack(own_gains)
        gains = jnp.where(is_l, gains, move(gains, L_TO_R))
        g_attn, g_mlp = gains[0], gains[1]

        x_core = lax.dynamic_slice_in_dim(inputs, core, 1, 1)
        x_other = lax.dynamic_slice_in_dim(inputs, 1 - core, 1, 1)
        y_core = lax.dynamic_slice_in_dim(targets, core, 1, 1)

        ticks = micro_count + 6

        saved, outs, arrived = [], [], []
        for t in range(ticks):
            recv = arrived[t - 2] if t >= 2 else jnp.zeros((1, seq_len, width), BF)
            act = jnp.where(is_first, x_core[t], recv) if t < micro_count else recv
            out, keep = home_forward(act, slots, g_attn, g_mlp)
            saved.append(keep)
            outs.append(out)
            arrived.append(move(out, FWD))

        def aligned(values, m):
            result = values[m]
            for pos in (1, 2, 3):
                result = jnp.where(home == pos, values[m + 2 * pos], result)
            return result

        loss_acc = jnp.zeros((), F32)
        seeds = []
        for m in range(micro_count):
            error = outs[m + 6].astype(F32) - y_core[m].astype(F32)
            seeds.append((error * norm_factor).astype(BF))
            loss_acc = loss_acc + 0.5 * jnp.sum(error * error) * norm_factor
        loss_acc = jnp.where(is_last, loss_acc, 0.0)

        grads = [None] * ticks
        prevs = [None] * ticks
        mids = [None] * ticks
        back = [None] * ticks
        dga = jnp.zeros((width,), F32)
        dgm = jnp.zeros((width,), F32)
        for t in reversed(range(ticks)):
            recv = back[t + 2] if t + 2 < ticks else jnp.zeros((1, seq_len, width), BF)
            grad = jnp.where(is_last, seeds[t - 6], recv) if t >= 6 else recv
            prev, d_mid, dga_t, dgm_t = home_backward(saved[t], grad, slots, g_attn, g_mlp)
            valid = (t >= 2 * home) & (t < 2 * home + micro_count)
            dga = dga + jnp.where(valid, dga_t, 0.0)
            dgm = dgm + jnp.where(valid, dgm_t, 0.0)
            grads[t], prevs[t], mids[t] = grad, prev, d_mid
            back[t] = move(prev, BWD)

        acts = [s[0] for s in saved]
        hs = [s[1] for s in saved]
        is_4 = (home == 1) & jnp.logical_not(is_l)
        is_2 = (home == 3) & jnp.logical_not(is_l)
        gather_rows = {k: [] for k in ('a', 'h', 'd', 'g')}
        for m in range(micro_count):
            def both(value):
                r1 = move(value, L_ACROSS + R_TO_L)
                r2 = move(value, R_SWAP)
                return jnp.where(is_l, value, r1), jnp.where(is_l, r1, r2)
            gather_rows['h'].append(both(aligned(hs, m)))
            gather_rows['d'].append(both(aligned(mids, m)))
            a_m, o_m = aligned(acts, m), aligned(outs, m)
            r1 = move(a_m, R_TO_L + [(6, 2)])
            r2 = move(jnp.where(is_l, o_m, a_m), [(7, 2), (0, 1), (6, 7)])
            same = jnp.where(is_l, a_m, jnp.where(is_4, x_core[m], jnp.where(is_2, r1, o_m)))
            other = jnp.where(is_l, r1, jnp.where(is_4, x_other[m], r2))
            gather_rows['a'].append((same, other))
            g_m, p_m = aligned(grads, m), aligned(prevs, m)
            r1 = move(g_m, R_TO_L + [(5, 1), (3, 7)])
            r2 = move(jnp.where(is_l, p_m, g_m), [(4, 1), (2, 7), (5, 4), (3, 2)])
            same = jnp.where(is_l, g_m, jnp.where(is_4 | is_2, p_m, r1))
            other = jnp.where(is_l, r1, r2)
            gather_rows['g'].append((same, other))
        rows = {k: jnp.concatenate([p[0] for p in v] + [p[1] for p in v], 0) for k, v in gather_rows.items()}
        weight_grads = owner_grads(rows['a'], rows['h'], rows['d'], rows['g'], own + own_gains)

        layer_ids = jnp.arange(4)
        gain_sums = jnp.where((layer_ids == home)[:, None, None], jnp.stack([dga, dgm])[None], 0.0)
        gain_sums, loss = lax.psum((gain_sums, loss_acc), AX)
        mine = jnp.sum(jnp.where((layer_ids == stage)[:, None, None], gain_sums, 0.0), 0)

        dx = jnp.stack([prevs[m] for m in range(micro_count)])
        at_b = move(dx, [(0, 4), (1, 5)])
        at_d = move(dx, [(0, 2), (1, 3)])
        at_c = move(at_b, [(4, 6), (5, 7)])
        dx = jnp.where(home == 0, dx, jnp.where(home == 1, at_b, jnp.where(home == 2, at_c, at_d)))
        other = move(dx, CORE_SWAP)
        d_inputs = jnp.concatenate([jnp.where(core == 0, dx, other), jnp.where(core == 0, other, dx)], 1)
        return (loss.reshape(1), d_inputs) + tuple(g[None] for g in weight_grads) + (mine[0][None], mine[1][None])

    return jax.shard_map(device_fn, mesh=mesh, in_specs=(act_spec, act_spec) + weight_specs, out_specs=(P('rep'), act_spec) + weight_specs, check_vma=False)
```

```python
import functools

import jax
import jax.numpy as jnp
from jax import lax
from jax.experimental import pallas as pl
from jax.experimental.pallas import tpu as pltpu
from jax.sharding import PartitionSpec as P

NORM_EPS = 1e-5
AX = ('tp', 'stage')
BF = jnp.bfloat16
F32 = jnp.float32
MESH = pl.DeviceIdType.MESH
ANY = pl.ANY

R_SWAP = [(1, 4), (4, 1), (2, 7), (7, 2)]
CORE_SWAP = [(0, 1), (1, 0), (2, 3), (3, 2), (4, 5), (5, 4), (6, 7), (7, 6)]
L_TO_R = [(0, 1), (5, 4), (6, 7), (3, 2)]

GELU_A = 0.7978845608028654
GELU_B = 0.044715
CHUNK = 1024
SUB = 256
DEPTH = 3
HEAD_PAD = 128


def move(value, perm):
    return lax.ppermute(value, AX, perm)


def rms_core(x_f32, gain_f32):
    inv_rms = lax.rsqrt(jnp.mean(x_f32 * x_f32, axis=-1, keepdims=True) + NORM_EPS)
    return x_f32 * inv_rms * gain_f32


def gelu_tanh(up_f32):
    return jax.nn.gelu(up_f32, approximate=True)


def dot(eq, a, b):
    return jnp.einsum(eq, a, b, preferred_element_type=F32)


def mm(a, b):
    return lax.dot_general(a, b, (((1,), (0,)), ((), ())), preferred_element_type=F32)


def mm_nt(a, b):
    return lax.dot_general(a, b, (((1,), (1,)), ((), ())), preferred_element_type=F32)


def mm_tn(a, b):
    return lax.dot_general(a, b, (((0,), (0,)), ((), ())), preferred_element_type=F32)


class Place:
    def __init__(self):
        self.tp = lax.axis_index('tp')
        self.stage = lax.axis_index('stage')
        self.core = self.stage % 2
        self.x_pos = self.stage // 2
        self.home = self.x_pos * (3 - 2 * self.tp) + self.tp
        self.is_l = self.stage == self.home
        self.sib = self.stage + 1 - 2 * self.core

    def at(self, tp, stage):
        return {'tp': tp, 'stage': stage}

    @property
    def sibling(self):
        return self.at(self.tp, self.sib)

    @property
    def across(self):
        return self.at(1 - self.tp, self.stage)

    @property
    def across_other(self):
        return self.at(1 - self.tp, self.sib)

    def chain(self, delta):
        there = self.home + delta
        x_pos = there // 2
        tp = there % 2 + x_pos * (1 - 2 * (there % 2))
        return self.at(tp, 2 * x_pos + self.core)


def entry_barrier(place):
    barrier = pltpu.get_barrier_semaphore()
    for d_tp in (0, 1):
        for d_stage in range(4):
            if d_tp or d_stage:
                tp = place.tp + d_tp - 2 * d_tp * place.tp
                stage = (place.stage + d_stage) % 4
                pl.semaphore_signal(barrier, inc=1, device_id=place.at(tp, stage), device_id_type=MESH)
    pl.semaphore_wait(barrier, 7)


def remote(src, dst, send_sem, recv_sem, device_id):
    return pltpu.make_async_remote_copy(src_ref=src, dst_ref=dst, send_sem=send_sem, recv_sem=recv_sem, device_id=device_id, device_id_type=MESH)


class Stream:
    def __init__(self, buf, sem, parts, total):
        self.buf, self.sem, self.parts, self.total = buf, sem, parts, total
        self.per_tick = sum(p[1] for p in parts)

    def view(self, ref, axis, index):
        where = pl.ds(pl.multiple_of(index * CHUNK, CHUNK), CHUNK)
        return ref.at[where, :] if axis == 0 else ref.at[:, where]

    def start(self, seq):
        @pl.when(seq < self.total)
        def _():
            j = seq % self.per_tick
            slot = seq % DEPTH
            base = 0
            for ref, chunks, axis in self.parts:
                low = base

                @pl.when((j >= low) & (j < low + chunks))
                def _(ref=ref, low=low, axis=axis):
                    pltpu.make_async_copy(self.view(ref, axis, j - low), self.buf.at[slot], self.sem.at[slot]).start()
                base += chunks

    def prime(self):
        for seq in range(DEPTH):
            self.start(jnp.int32(seq))

    def wait(self, seq):
        ref, _, axis = self.parts[0]
        slot = seq % DEPTH
        pltpu.make_async_copy(self.view(ref, axis, 0), self.buf.at[slot], self.sem.at[slot]).wait()
        return self.buf.at[slot]


def rows_loop(total, step, body):
    def run(i, carry):
        body(pl.ds(pl.multiple_of(i * step, step), step))
        return carry
    lax.fori_loop(0, total // step, run, 0)


def norm_rows(src, gain_row, dst, total):
    def body(rows):
        v = src[rows, :].astype(F32)
        inv = lax.rsqrt(jnp.mean(v * v, axis=-1, keepdims=True) + NORM_EPS)
        dst[rows, :] = (v * inv * gain_row).astype(BF)
    rows_loop(total, 32, body)


def gelu_gate(u):
    u2 = u * u
    t = jnp.tanh(u * (GELU_A + (GELU_A * GELU_B) * u2))
    return 0.5 * t + 0.5, u2


def causal_probs(q, k, scale):
    s = mm_nt(q, k) * scale
    q_pos = lax.broadcasted_iota(jnp.int32, s.shape, 0)
    k_pos = lax.broadcasted_iota(jnp.int32, s.shape, 1)
    s = jnp.where(k_pos <= q_pos, s, -1e30)
    e = jnp.exp(s - jnp.max(s, axis=-1, keepdims=True))
    return e * (1.0 / jnp.sum(e, axis=-1, keepdims=True))


def lanes(offset, size):
    return pl.ds(pl.multiple_of(offset, 128), size)


def forward_kernel(dims, x_ref, wqx, wqy, wox, woy, wux, wuy, wdx, wdy, gains,
                   a_s, h_s, out_s, qkv_s, u_s, oh_same, oh_other, oa_same, oa_other,
                   abuf, hbuf, obuf, nbuf, qkvbuf, ubuf, zbuf, ctxbuf, acc, wn, wk,
                   act_sem, hop_send, save_sem, stream_n, stream_k, os_sem, oo_sem, as_sem, ao_sem, send_sems, big_sem):
    micro, seq, width, heads, head_dim, ffn = dims
    place = Place()
    is_first, is_last = place.home == 0, place.home == 3
    home02 = (place.home == 0) | (place.home == 2)
    is_r = jnp.logical_not(place.is_l)
    half = heads // 2 * HEAD_PAD
    qkv_cols = 6 * half
    entry_barrier(place)
    sn = Stream(wn, stream_n, [(wqx, 3, 1), (wqy, 3, 1), (wux, 3, 1), (wuy, 3, 1)], micro * 12)
    sk = Stream(wk, stream_k, [(wox, 1, 0), (woy, 1, 0), (wdx, 3, 0), (wdy, 3, 0)], micro * 8)

    @pl.when(is_first)
    def _():
        for m in range(micro):
            pltpu.make_async_copy(x_ref.at[m], abuf.at[m], act_sem.at[m]).start()
    sn.prime()
    sk.prime()

    def big_copies(m):
        return (pltpu.make_async_copy(qkvbuf, qkv_s.at[m], big_sem.at[0]), pltpu.make_async_copy(ubuf, u_s.at[m], big_sem.at[1]))

    def tick(m, carry):
        act, mid, out = abuf.at[m], hbuf.at[m], obuf.at[m]
        pltpu.make_async_copy(x_ref.at[m], act, act_sem.at[m]).wait()
        pltpu.make_async_copy(act, a_s.at[m], save_sem.at[0]).start()

        @pl.when(place.is_l)
        def _():
            pltpu.make_async_copy(act, oa_same.at[m], as_sem).start()

        @pl.when(is_r)
        def _():
            remote(act, oa_other.at[m], send_sems.at[0], ao_sem, place.sibling).start()

        @pl.when((place.home == 2) & place.is_l)
        def _():
            remote(act, oa_same.at[m], send_sems.at[1], as_sem, place.across).start()

        @pl.when((place.home == 2) & is_r)
        def _():
            remote(act, oa_other.at[m], send_sems.at[1], ao_sem, place.across_other).start()

        norm_rows(act, gains[0:1, :], nbuf, seq)

        @pl.when(m > 0)
        def _():
            big_copies(m)[0].wait()

        def qkv_step(j, c):
            w = sn.wait(m * 12 + j)
            for n in range(0, CHUNK, SUB):
                qkvbuf[:, lanes(j * CHUNK + n, SUB)] = mm(nbuf[...], w[:, n:n + SUB]).astype(BF)
            sn.start(m * 12 + j + DEPTH)
            return c
        lax.fori_loop(0, 6, qkv_step, 0)
        big_copies(m)[0].start()

        def head_step(i, c):
            for r in range(4):
                base = (i // 2) * (3 * half) + ((i % 2) * 4 + r) * HEAD_PAD
                q = qkvbuf[:, lanes(base, HEAD_PAD)]
                k = qkvbuf[:, lanes(base + half, HEAD_PAD)]
                v = qkvbuf[:, lanes(base + 2 * half, HEAD_PAD)]
                probs = causal_probs(q, k, head_dim ** -0.5).astype(BF)
                ctxbuf[:, lanes((i * 4 + r) * HEAD_PAD, HEAD_PAD)] = mm(probs, v).astype(BF)
            return c
        lax.fori_loop(0, heads // 4, head_step, 0)

        w0, w1 = sk.wait(m * 8), sk.wait(m * 8 + 1)
        for n in range(0, width, SUB):
            total = mm(ctxbuf[:, 0:half], w0[:, n:n + SUB]) + mm(ctxbuf[:, half:2 * half], w1[:, n:n + SUB])
            mid[:, n:n + SUB] = (act[:, n:n + SUB].astype(F32) + total).astype(BF)
        sk.start(m * 8 + DEPTH)
        sk.start(m * 8 + 1 + DEPTH)
        pltpu.make_async_copy(mid, h_s.at[m], save_sem.at[1]).start()

        norm_rows(mid, gains[1:2, :], nbuf, seq)

        @pl.when(place.is_l)
        def _():
            pltpu.make_async_copy(mid, oh_same.at[m], os_sem).start()
            remote(mid, oh_same.at[m], send_sems.at[2], os_sem, place.across).start()

        @pl.when(is_r)
        def _():
            remote(mid, oh_other.at[m], send_sems.at[2], oo_sem, place.sibling).start()
            remote(mid, oh_other.at[m], send_sems.at[3], oo_sem, place.across_other).start()

        @pl.when(m > 0)
        def _():
            big_copies(m)[1].wait()

        acc[...] = jnp.zeros_like(acc)

        def mlp_step(j, c):
            w = sn.wait(m * 12 + 6 + j)
            for n in range(0, CHUNK, SUB):
                u = mm(nbuf[...], w[:, n:n + SUB]).astype(BF)
                ubuf[:, lanes(j * CHUNK + n, SUB)] = u
                uf = u.astype(F32)
                zbuf[:, n:n + SUB] = (uf * gelu_gate(uf)[0]).astype(BF)
            sn.start(m * 12 + 6 + j + DEPTH)
            w2 = sk.wait(m * 8 + 2 + j)
            for n in range(0, width, SUB):
                acc[:, n:n + SUB] += mm(zbuf[...], w2[:, n:n + SUB])
            sk.start(m * 8 + 2 + j + DEPTH)
            return c
        lax.fori_loop(0, 6, mlp_step, 0)
        big_copies(m)[1].start()

        def finish(rows):
            out[rows, :] = (mid[rows, :].astype(F32) + acc[rows, :]).astype(BF)
        rows_loop(seq, 32, finish)

        @pl.when(jnp.logical_not(is_last))
        def _():
            remote(out, abuf.at[m], hop_send, act_sem.at[m], place.chain(1)).start()
        pltpu.make_async_copy(out, out_s.at[m], save_sem.at[2]).start()

        @pl.when(home02 & place.is_l)
        def _():
            remote(out, oa_other.at[m], send_sems.at[4], ao_sem, place.sibling).start()

        @pl.when(home02 & is_r)
        def _():
            pltpu.make_async_copy(out, oa_same.at[m], as_sem).start()
        return carry

    lax.fori_loop(0, micro, tick, 0)

    for copy in big_copies(micro - 1):
        copy.wait()
    for buf, dst, index in ((abuf, a_s, 0), (hbuf, h_s, 1), (obuf, out_s, 2)):
        pltpu.make_async_copy(buf, dst, save_sem.at[index]).wait()

    def sent(buf, sem):
        remote(buf, a_s, sem, act_sem.at[0], place.sibling).wait_send()

    def got(dst, sem):
        pltpu.make_async_copy(dst, dst, sem).wait()

    sent(hbuf, send_sems.at[2])

    @pl.when(is_r)
    def _():
        sent(abuf, send_sems.at[0])
        sent(hbuf, send_sems.at[3])

    @pl.when(place.home == 2)
    def _():
        sent(abuf, send_sems.at[1])

    @pl.when(home02 & place.is_l)
    def _():
        sent(obuf, send_sems.at[4])

    @pl.when(jnp.logical_not(is_last))
    def _():
        sent(obuf, hop_send)
    got(oh_same, os_sem)
    got(oh_other, oo_sem)

    @pl.when(place.is_l | (place.home != 1))
    def _():
        got(oa_same, as_sem)
        got(oa_other, ao_sem)


def backward_kernel(dims, seed_ref, a_ref, h_ref, qkv_ref, u_ref, wdx, wdy, wox, woy, wux, wuy, wqx, wqy, gains,
                    dx_s, od_same, od_other, og_same, og_other, dgain,
                    gbuf, dbuf, pbuf, accg, qkvbuf, ubuf, habuf, dupbuf, dctxbuf, dqkvbuf, acc, wn, wk,
                    act_sem, hop_send, save_sem, stream_n, stream_k, load_sem, os_sem, oo_sem, gs_sem, go_sem, send_sems):
    micro, seq, width, heads, head_dim, ffn = dims
    place = Place()
    is_first, is_last = place.home == 0, place.home == 3
    home13 = (place.home == 1) | (place.home == 3)
    is_r = jnp.logical_not(place.is_l)
    half = heads // 2 * HEAD_PAD
    scale = head_dim ** -0.5
    entry_barrier(place)
    sn = Stream(wn, stream_n, [(wdx, 3, 1), (wdy, 3, 1), (wox, 1, 1), (woy, 1, 1)], micro * 8)
    sk = Stream(wk, stream_k, [(wux, 3, 0), (wuy, 3, 0), (wqx, 3, 0), (wqy, 3, 0)], micro * 12)

    @pl.when(is_last)
    def _():
        for m in range(micro):
            pltpu.make_async_copy(seed_ref.at[m], gbuf.at[m], act_sem.at[m]).start()

    def loads(i):
        m = micro - 1 - i
        slot = i % 2
        return (pltpu.make_async_copy(u_ref.at[m], ubuf.at[slot], load_sem.at[0, slot]),
                pltpu.make_async_copy(qkv_ref.at[m], qkvbuf.at[slot], load_sem.at[1, slot]),
                pltpu.make_async_copy(h_ref.at[m], habuf.at[slot, 0], load_sem.at[2, slot]),
                pltpu.make_async_copy(a_ref.at[m], habuf.at[slot, 1], load_sem.at[3, slot]))

    sn.prime()
    sk.prime()
    for copy in loads(0):
        copy.start()
    accg[...] = jnp.zeros_like(accg)

    def norm_back(index, x, dn, base, dst, gain_row):
        def body(rows):
            xf = x[rows, :].astype(F32)
            dy = dn[rows, :].astype(BF).astype(F32)
            inv = lax.rsqrt(jnp.mean(xf * xf, axis=-1, keepdims=True) + NORM_EPS)
            xn = xf * inv
            accg[index] += jnp.sum((dy * xn).reshape(4, 8, width), axis=0)
            dyg = dy * gain_row
            dx = inv * (dyg - xn * jnp.mean(dyg * xn, axis=-1, keepdims=True))
            dst[rows, :] = (base[rows, :].astype(F32) + dx).astype(BF)
        rows_loop(seq, 32, body)

    def tick(i, carry):
        m = micro - 1 - i
        slot = i % 2
        grad, dmid, prev = gbuf.at[m], dbuf.at[m], pbuf.at[m]
        u_now, qkv_now, h_now, a_now = ubuf.at[slot], qkvbuf.at[slot], habuf.at[slot, 0], habuf.at[slot, 1]

        @pl.when(i + 1 < micro)
        def _():
            for copy in loads(i + 1):
                copy.start()
        pltpu.make_async_copy(seed_ref.at[m], grad, act_sem.at[m]).wait()

        @pl.when(place.is_l)
        def _():
            pltpu.make_async_copy(grad, og_same.at[m], gs_sem).start()

        @pl.when(is_r)
        def _():
            remote(grad, og_other.at[m], send_sems.at[0], go_sem, place.sibling).start()

        @pl.when(home13 & place.is_l)
        def _():
            remote(grad, og_same.at[m], send_sems.at[1], gs_sem, place.across).start()

        @pl.when(home13 & is_r)
        def _():
            remote(grad, og_other.at[m], send_sems.at[1], go_sem, place.across_other).start()

        for copy in loads(i)[:1]:
            copy.wait()
        acc[...] = jnp.zeros_like(acc)

        def mlp_step(j, c):
            w = sn.wait(i * 8 + j)
            for n in range(0, CHUNK, SUB):
                dz = mm(grad[...], w[:, n:n + SUB]).astype(BF).astype(F32)
                u = u_now[:, lanes(j * CHUNK + n, SUB)].astype(F32)
                gate, u2 = gelu_gate(u)
                slope = gate + u * gate * (1.0 - gate) * (2.0 * GELU_A + (6.0 * GELU_A * GELU_B) * u2)
                dupbuf[:, n:n + SUB] = (dz * slope).astype(BF)
            sn.start(i * 8 + j + DEPTH)
            w2 = sk.wait(i * 12 + j)
            for n in range(0, width, SUB):
                acc[:, n:n + SUB] += mm(dupbuf[...], w2[:, n:n + SUB])
            sk.start(i * 12 + j + DEPTH)
            return c
        lax.fori_loop(0, 6, mlp_step, 0)

        for copy in loads(i)[1:]:
            copy.wait()
        norm_back(1, h_now, acc, grad, dmid, gains[1:2, :])

        for c in range(2):
            w = sn.wait(i * 8 + 6 + c)
            for n in range(0, CHUNK, SUB):
                dctxbuf[:, c * CHUNK + n:c * CHUNK + n + SUB] = mm(dmid[...], w[:, n:n + SUB]).astype(BF)
            sn.start(i * 8 + 6 + c + DEPTH)

        @pl.when(place.is_l)
        def _():
            pltpu.make_async_copy(dmid, od_same.at[m], os_sem).start()
            remote(dmid, od_same.at[m], send_sems.at[2], os_sem, place.across).start()

        @pl.when(is_r)
        def _():
            remote(dmid, od_other.at[m], send_sems.at[2], oo_sem, place.sibling).start()
            remote(dmid, od_other.at[m], send_sems.at[3], oo_sem, place.across_other).start()

        def head_step(t, c):
            for r in range(2):
                base = (t // 4) * (3 * half) + ((t % 4) * 2 + r) * HEAD_PAD
                q = qkv_now[:, lanes(base, HEAD_PAD)]
                k = qkv_now[:, lanes(base + half, HEAD_PAD)]
                v = qkv_now[:, lanes(base + 2 * half, HEAD_PAD)]
                dc = dctxbuf[:, lanes((t * 2 + r) * HEAD_PAD, HEAD_PAD)]
                probs = causal_probs(q, k, scale)
                dp = mm_nt(dc, v).astype(BF).astype(F32)
                ds = probs * (dp - jnp.sum(dp * probs, axis=-1, keepdims=True)) * scale
                dv = mm_tn(probs.astype(BF), dc)
                hi = ds.astype(BF)
                rest = ds - hi.astype(F32)
                lo = rest.astype(BF)
                tail = (rest - lo.astype(F32)).astype(BF)
                dq = mm(hi, k) + (mm(lo, k) + mm(tail, k))
                dk = mm_tn(hi, q) + (mm_tn(lo, q) + mm_tn(tail, q))
                dqkvbuf[:, lanes(base, HEAD_PAD)] = dq.astype(BF)
                dqkvbuf[:, lanes(base + half, HEAD_PAD)] = dk.astype(BF)
                dqkvbuf[:, lanes(base + 2 * half, HEAD_PAD)] = dv.astype(BF)
            return c
        lax.fori_loop(0, heads // 2, head_step, 0)

        acc[...] = jnp.zeros_like(acc)

        def qkv_step(j, c):
            w2 = sk.wait(i * 12 + 6 + j)
            for n in range(0, width, SUB):
                acc[:, n:n + SUB] += mm(dqkvbuf[:, lanes(j * CHUNK, CHUNK)], w2[:, n:n + SUB])
            sk.start(i * 12 + 6 + j + DEPTH)
            return c
        lax.fori_loop(0, 6, qkv_step, 0)
        norm_back(0, a_now, acc, dmid, prev, gains[0:1, :])

        @pl.when(jnp.logical_not(is_first))
        def _():
            remote(prev, gbuf.at[m], hop_send, act_sem.at[m], place.chain(-1)).start()
        pltpu.make_async_copy(prev, dx_s.at[m], save_sem).start()

        @pl.when(home13 & place.is_l)
        def _():
            remote(prev, og_other.at[m], send_sems.at[4], go_sem, place.sibling).start()

        @pl.when(home13 & is_r)
        def _():
            pltpu.make_async_copy(prev, og_same.at[m], gs_sem).start()
        return carry

    lax.fori_loop(0, micro, tick, 0)
    dgain[...] = accg[...]
    pltpu.make_async_copy(pbuf, dx_s, save_sem).wait()

    def sent(buf, sem):
        remote(buf, dx_s, sem, act_sem.at[0], place.sibling).wait_send()

    def got(dst, sem):
        pltpu.make_async_copy(dst, dst, sem).wait()

    sent(dbuf, send_sems.at[2])

    @pl.when(is_r)
    def _():
        sent(gbuf, send_sems.at[0])
        sent(dbuf, send_sems.at[3])

    @pl.when(home13)
    def _():
        sent(gbuf, send_sems.at[1])

    @pl.when(home13 & place.is_l)
    def _():
        sent(pbuf, send_sems.at[4])

    @pl.when(jnp.logical_not(is_first))
    def _():
        sent(pbuf, hop_send)
    got(od_same, os_sem)
    got(od_other, oo_sem)
    got(og_same, gs_sem)
    got(og_other, go_sem)


def bf(*shape):
    return jax.ShapeDtypeStruct(shape, BF)


def forward_phase(dims, x, weights, gains):
    micro, seq, width, heads, head_dim, ffn = dims
    half = heads // 2 * HEAD_PAD
    act = bf(micro, seq, width)
    vmem, dma = pltpu.VMEM, pltpu.SemaphoreType.DMA
    return pl.pallas_call(
        functools.partial(forward_kernel, dims),
        out_shape=(act, act, act, bf(micro, seq, 6 * half), bf(micro, seq, ffn), act, act, act, act),
        in_specs=[pl.BlockSpec(memory_space=ANY)] * 9 + [pl.BlockSpec(memory_space=vmem)],
        out_specs=(pl.BlockSpec(memory_space=ANY),) * 9,
        scratch_shapes=[
            vmem((micro, seq, width), BF), vmem((micro, seq, width), BF), vmem((micro, seq, width), BF),
            vmem((seq, width), BF), vmem((seq, 6 * half), BF), vmem((seq, ffn), BF), vmem((seq, CHUNK), BF), vmem((seq, 2 * half), BF),
            vmem((seq, width), F32), vmem((DEPTH, width, CHUNK), BF), vmem((DEPTH, CHUNK, width), BF),
            dma((micro,)), dma(()), dma((3,)), dma((DEPTH,)), dma((DEPTH,)), dma(()), dma(()), dma(()), dma(()), dma((5,)), dma((2,)),
        ],
        compiler_params=pltpu.CompilerParams(collective_id=0, has_side_effects=True, vmem_limit_bytes=60 * 1024 * 1024),
        name='forward_phase',
    )(x, *weights, gains)


def backward_phase(dims, seeds, acts, mids, qkv, ups, weights, gains):
    micro, seq, width, heads, head_dim, ffn = dims
    half = heads // 2 * HEAD_PAD
    act = bf(micro, seq, width)
    vmem, dma = pltpu.VMEM, pltpu.SemaphoreType.DMA
    return pl.pallas_call(
        functools.partial(backward_kernel, dims),
        out_shape=(act, act, act, act, act, jax.ShapeDtypeStruct((2, 8, width), F32)),
        in_specs=[pl.BlockSpec(memory_space=ANY)] * 13 + [pl.BlockSpec(memory_space=vmem)],
        out_specs=(pl.BlockSpec(memory_space=ANY),) * 5 + (pl.BlockSpec(memory_space=vmem),),
        scratch_shapes=[
            vmem((micro, seq, width), BF), vmem((micro, seq, width), BF), vmem((micro, seq, width), BF),
            vmem((2, 8, width), F32), vmem((2, seq, 6 * half), BF), vmem((2, seq, ffn), BF), vmem((2, 2, seq, width), BF),
            vmem((seq, CHUNK), BF), vmem((seq, 2 * half), BF), vmem((seq, 6 * half), BF), vmem((seq, width), F32),
            vmem((DEPTH, width, CHUNK), BF), vmem((DEPTH, CHUNK, width), BF),
            dma((micro,)), dma(()), dma(()), dma((DEPTH,)), dma((DEPTH,)), dma((4, 2)), dma(()), dma(()), dma(()), dma(()), dma((5,)),
        ],
        compiler_params=pltpu.CompilerParams(collective_id=1, has_side_effects=True, vmem_limit_bytes=62 * 1024 * 1024),
        name='backward_phase',
    )(seeds, acts, mids, qkv, ups, *weights, gains)


def attn_scores(query, key):
    seq_len = query.shape[-2]
    scores = dot('bhqe,bhke->bhqk', query, key) * (query.shape[-1] ** -0.5)
    q_pos = lax.broadcasted_iota(jnp.int32, (seq_len, seq_len), 0)
    k_pos = lax.broadcasted_iota(jnp.int32, (seq_len, seq_len), 1)
    return jax.nn.softmax(jnp.where(k_pos <= q_pos, scores, -1e30), axis=-1)


def attn_backward(qkv, probs, d_context):
    scale = qkv.shape[-1] ** -0.5
    d_probs = dot('bhqe,bhke->bhqk', d_context, qkv[2]).astype(BF).astype(F32)
    d_value = dot('bhqk,bhqe->bhke', probs.astype(BF), d_context).astype(BF)
    d_scores = probs * (d_probs - jnp.sum(d_probs * probs, axis=-1, keepdims=True)) * scale
    d_query = jnp.einsum('bhqk,bhke->bhqe', d_scores, qkv[1].astype(F32), precision=lax.Precision.HIGHEST).astype(BF)
    d_key = jnp.einsum('bhqk,bhqe->bhke', d_scores, qkv[0].astype(F32), precision=lax.Precision.HIGHEST).astype(BF)
    return jnp.stack([d_query, d_key, d_value])


def owner_grads(act, mid, d_mid, grad_out, weights):
    w_qkv, w_out, w_up, w_down, gain_attn, gain_mlp = weights
    normed_a = rms_core(act.astype(F32), gain_attn).astype(BF)
    qkv = dot('bsd,dkhe->kbhse', normed_a, w_qkv).astype(BF)
    probs = attn_scores(qkv[0], qkv[1])
    context = dot('bhqk,bhke->bhqe', probs.astype(BF), qkv[2]).astype(BF)
    d_w_out = dot('bhse,bsd->hed', context, d_mid)
    d_context = dot('bsd,hed->bhse', d_mid, w_out).astype(BF)
    d_qkv = attn_backward(qkv, probs, d_context)
    d_w_qkv = dot('bsd,kbhse->dkhe', normed_a, d_qkv)
    normed_m = rms_core(mid.astype(F32), gain_mlp).astype(BF)
    up_f32 = dot('bsd,df->bsf', normed_m, w_up).astype(BF).astype(F32)
    hidden = gelu_tanh(up_f32).astype(BF)
    d_w_down = dot('bsf,bsd->fd', hidden, grad_out)
    d_act = dot('bsd,fd->bsf', grad_out, w_down).astype(BF)
    _, pull = jax.vjp(gelu_tanh, up_f32)
    d_up = pull(d_act.astype(F32))[0].astype(BF)
    d_w_up = dot('bsd,bsf->df', normed_m, d_up)
    return d_w_qkv, d_w_out, d_w_up, d_w_down


def pad_qkv(w):
    pad = HEAD_PAD - w.shape[-1]
    return jnp.pad(w, ((0, 0), (0, 0), (0, 0), (0, pad))).reshape(w.shape[0], -1)


def pad_out(w):
    pad = HEAD_PAD - w.shape[1]
    return jnp.pad(w, ((0, 0), (0, pad), (0, 0))).reshape(-1, w.shape[2])


def solution(mesh):
    act_spec = P('rep', None, None, None)
    weight_specs = (
        P(('rep', 'stage'), None, None, 'tp', None),
        P(('rep', 'stage'), 'tp', None, None),
        P(('rep', 'stage'), None, 'tp'),
        P(('rep', 'stage'), 'tp', None),
        P(('rep', 'stage'), None),
        P(('rep', 'stage'), None),
    )

    def device_fn(inputs, targets, w_qkv, w_out, w_up, w_down, gain_attn, gain_mlp):
        micro_count, _, seq_len, width = inputs.shape
        dims = (micro_count, seq_len, width, 2 * w_out.shape[1], w_out.shape[2], 2 * w_up.shape[2])
        norm_factor = 1.0 / (inputs.size)
        stage = lax.axis_index('stage')
        tp = lax.axis_index('tp')
        x_pos, core = stage // 2, stage % 2
        home = jnp.where(x_pos == 0, tp, 3 - tp)
        is_l = stage == home
        is_last = home == 3
        own = (w_qkv[0], w_out[0], w_up[0], w_down[0])
        own_gains = (gain_attn[0].astype(F32), gain_mlp[0].astype(F32))

        slots = []
        for w in own:
            held = jnp.where(is_l, w, move(w, R_SWAP))
            slots.append((held, move(held, CORE_SWAP)))
        gains = jnp.stack(own_gains)
        gains = jnp.where(is_l, gains, move(gains, L_TO_R))
        wq = [pad_qkv(w) for w in slots[0]]
        wo = [pad_out(w) for w in slots[1]]
        wu, wd = slots[2], slots[3]

        x_core = lax.dynamic_index_in_dim(inputs, core, 1, keepdims=False)
        x_other = lax.dynamic_index_in_dim(inputs, 1 - core, 1, keepdims=False)
        y_core = lax.dynamic_index_in_dim(targets, core, 1, keepdims=False)

        acts, mids, outs, qkv, ups, oh_same, oh_other, oa_same, oa_other = forward_phase(dims, x_core, (*wq, *wo, *wu, *wd), gains)
        error = outs.astype(F32) - y_core.astype(F32)
        seeds = (error * norm_factor).astype(BF)
        loss = jnp.where(is_last, 0.5 * jnp.sum(error * error) * norm_factor, 0.0)

        turned = [w.T for w in (*wd, *wo, *wu, *wq)]
        dx, od_same, od_other, og_same, og_other, gain_sum = backward_phase(dims, seeds, acts, mids, qkv, ups, turned, gains)

        is_4 = (home == 1) & jnp.logical_not(is_l)
        both = lambda same, other: jnp.concatenate([same, other], 0)
        rows_a = both(jnp.where(is_4, x_core, oa_same), jnp.where(is_4, x_other, oa_other))
        weight_grads = owner_grads(rows_a, both(oh_same, oh_other), both(od_same, od_other), both(og_same, og_other), own + own_gains)

        layer_ids = jnp.arange(4)
        gain_sums = jnp.where((layer_ids == home)[:, None, None], jnp.sum(gain_sum, 1)[None], 0.0)
        gain_sums, loss = lax.psum((gain_sums, loss), AX)
        mine = jnp.sum(jnp.where((layer_ids == stage)[:, None, None], gain_sums, 0.0), 0)

        dx = dx[:, None]
        at_b = move(dx, [(0, 4), (1, 5)])
        at_d = move(dx, [(0, 2), (1, 3)])
        at_c = move(at_b, [(4, 6), (5, 7)])
        dx = jnp.where(home == 0, dx, jnp.where(home == 1, at_b, jnp.where(home == 2, at_c, at_d)))
        other = move(dx, CORE_SWAP)
        d_inputs = jnp.concatenate([jnp.where(core == 0, dx, other), jnp.where(core == 0, other, dx)], 1)
        return (loss.reshape(1), d_inputs) + tuple(g[None] for g in weight_grads) + (mine[0][None], mine[1][None])

    return jax.shard_map(device_fn, mesh=mesh, in_specs=(act_spec, act_spec) + weight_specs, out_specs=(P('rep'), act_spec) + weight_specs, check_vma=False)
```

```python
import functools

import jax
import jax.numpy as jnp
from jax import lax
from jax.experimental import pallas as pl
from jax.experimental.pallas import tpu as pltpu
from jax.sharding import PartitionSpec as P

NORM_EPS = 1e-5
AX = ('tp', 'stage')
BF = jnp.bfloat16
F32 = jnp.float32
MESH = pl.DeviceIdType.MESH
ANY = pl.ANY

R_SWAP = [(1, 4), (4, 1), (2, 7), (7, 2)]
CORE_SWAP = [(0, 1), (1, 0), (2, 3), (3, 2), (4, 5), (5, 4), (6, 7), (7, 6)]
L_TO_R = [(0, 1), (5, 4), (6, 7), (3, 2)]

GELU_A = 0.7978845608028654
GELU_B = 0.044715
CHUNK = 1024
SUB = 256
DEPTH = 3
KDEPTH = 2
HEAD_PAD = 128


def move(value, perm):
    return lax.ppermute(value, AX, perm)


def rms_core(x_f32, gain_f32):
    inv_rms = lax.rsqrt(jnp.mean(x_f32 * x_f32, axis=-1, keepdims=True) + NORM_EPS)
    return x_f32 * inv_rms * gain_f32


def gelu_tanh(up_f32):
    return jax.nn.gelu(up_f32, approximate=True)


def dot(eq, a, b):
    return jnp.einsum(eq, a, b, preferred_element_type=F32)


def mm(a, b):
    return lax.dot_general(a, b, (((1,), (0,)), ((), ())), preferred_element_type=F32)


def mm_nt(a, b):
    return lax.dot_general(a, b, (((1,), (1,)), ((), ())), preferred_element_type=F32)


def mm_tn(a, b):
    return lax.dot_general(a, b, (((0,), (0,)), ((), ())), preferred_element_type=F32)


class Place:
    def __init__(self):
        self.tp = lax.axis_index('tp')
        self.stage = lax.axis_index('stage')
        self.core = self.stage % 2
        self.x_pos = self.stage // 2
        self.home = self.x_pos * (3 - 2 * self.tp) + self.tp
        self.is_l = self.stage == self.home
        self.sib = self.stage + 1 - 2 * self.core

    def at(self, tp, stage):
        return {'tp': tp, 'stage': stage}

    @property
    def sibling(self):
        return self.at(self.tp, self.sib)

    @property
    def across(self):
        return self.at(1 - self.tp, self.stage)

    @property
    def across_other(self):
        return self.at(1 - self.tp, self.sib)

    def others(self, src, dst, send_sems, recv_sem):
        copies = []
        for d_tp in (0, 1):
            for d_stage in range(4):
                if d_tp or d_stage:
                    there = self.at(self.tp + d_tp - 2 * d_tp * self.tp, (self.stage + d_stage) % 4)
                    copies.append(remote(src, dst, send_sems.at[len(copies)], recv_sem, there))
        return copies

    def chain(self, delta):
        there = self.home + delta
        x_pos = there // 2
        tp = there % 2 + x_pos * (1 - 2 * (there % 2))
        return self.at(tp, 2 * x_pos + self.core)


def entry_barrier(place):
    barrier = pltpu.get_barrier_semaphore()
    for d_tp in (0, 1):
        for d_stage in range(4):
            if d_tp or d_stage:
                tp = place.tp + d_tp - 2 * d_tp * place.tp
                stage = (place.stage + d_stage) % 4
                pl.semaphore_signal(barrier, inc=1, device_id=place.at(tp, stage), device_id_type=MESH)
    pl.semaphore_wait(barrier, 7)


def remote(src, dst, send_sem, recv_sem, device_id):
    return pltpu.make_async_remote_copy(src_ref=src, dst_ref=dst, send_sem=send_sem, recv_sem=recv_sem, device_id=device_id, device_id_type=MESH)


def rows_loop(total, step, body):
    def run(i, carry):
        body(pl.ds(pl.multiple_of(i * step, step), step))
        return carry
    lax.fori_loop(0, total // step, run, 0)


def norm_rows(src, gain_row, dst, total):
    def body(rows):
        v = src[rows, :].astype(F32)
        inv = lax.rsqrt(jnp.mean(v * v, axis=-1, keepdims=True) + NORM_EPS)
        dst[rows, :] = (v * inv * gain_row).astype(BF)
    rows_loop(total, 32, body)


def gelu_gate(u):
    u2 = u * u
    t = jnp.tanh(u * (GELU_A + (GELU_A * GELU_B) * u2))
    return 0.5 * t + 0.5, u2


def causal_probs(q, k, scale):
    s = mm_nt(q, k) * scale
    q_pos = lax.broadcasted_iota(jnp.int32, s.shape, 0)
    k_pos = lax.broadcasted_iota(jnp.int32, s.shape, 1)
    s = jnp.where(k_pos <= q_pos, s, -1e30)
    e = jnp.exp(s - jnp.max(s, axis=-1, keepdims=True))
    return e * (1.0 / jnp.sum(e, axis=-1, keepdims=True))


def lanes(offset, size):
    return pl.ds(pl.multiple_of(offset, 128), size)


class Stream:
    def __init__(self, buf, sem, depth, parts, total, by_heads):
        self.buf, self.sem, self.depth, self.parts, self.total, self.by_heads = buf, sem, depth, parts, total, by_heads
        self.per_tick = sum(p[1] for p in parts)

    def copy_in(self, ref, index, slot):
        if not self.by_heads:
            where = pl.ds(pl.multiple_of(index * CHUNK, CHUNK), CHUNK)
            pltpu.make_async_copy(ref.at[:, where], self.buf.at[slot], self.sem.at[slot]).start()
            return
        for r in range(8):
            rows = pl.ds(pl.multiple_of(index * 768 + r * 96, 96), 96)
            pltpu.make_async_copy(ref.at[rows, :], self.buf.at[slot, r * 128:r * 128 + 96, :], self.sem.at[slot]).start()

    def start(self, seq):
        @pl.when(seq < self.total)
        def _():
            j = seq % self.per_tick
            slot = seq % self.depth
            base = 0
            for choices, chunks in self.parts:
                for condition, ref in choices:
                    here = (j >= base) & (j < base + chunks)
                    here = here if condition is None else here & condition

                    @pl.when(here)
                    def _(ref=ref, low=base):
                        self.copy_in(ref, j - low, slot)
                base += chunks

    def prime(self):
        for seq in range(self.depth):
            self.start(jnp.int32(seq))

    def wait(self, seq):
        slot = seq % self.depth
        ref = self.parts[0][0][0][1]
        if self.by_heads:
            pltpu.make_async_copy(ref.at[0:768, :], self.buf.at[slot, 0:768, :], self.sem.at[slot]).wait()
        else:
            pltpu.make_async_copy(ref.at[:, 0:CHUNK], self.buf.at[slot], self.sem.at[slot]).wait()
        return self.buf.at[slot]


PIECES = [(0, 0, 0), (0, 0, 1), (0, 0, 2), (1, 0, 0), (2, 1, 0), (2, 1, 1), (2, 1, 2), (2, 1, 3), (3, 0, 0), (3, 0, 1), (3, 0, 2), (3, 0, 3)]


def piece(ref, axis, index):
    return ref.at[index * 768:(index + 1) * 768, :] if axis == 0 else ref.at[:, index * 768:(index + 1) * 768]


def weight_phase(place, is_r, own, near, far, turned, wn, wk, send_sem, y_send, d_send, near_sem, far_sem, load_sem, store_sem):
    wk[...] = jnp.zeros_like(wk)

    @pl.when(place.is_l)
    def _():
        for i in range(4):
            remote(own[i], near[i], send_sem.at[i], near_sem.at[i], place.sibling).start()

    @pl.when(is_r)
    def _():
        for c, (i, axis, index) in enumerate(PIECES):
            remote(piece(own[i], axis, index), piece(far[i], axis, index), y_send.at[i], far_sem.at[c], place.across_other).start()

    def load(i, refs, t, slot):
        for condition, ref in refs:
            def go(ref=ref):
                if i < 2:
                    for r in range(2):
                        rows = pl.ds(pl.multiple_of(t * 192 + r * 96, 96), 96)
                        pltpu.make_async_copy(ref.at[rows, :], wk.at[0, pl.ds(slot * 256 + r * 128, 96), :], load_sem.at[slot]).start()
                elif i == 2:
                    pltpu.make_async_copy(ref.at[:, lanes(t * 256, 256)], wn.at[slot, :, 0:256], load_sem.at[slot]).start()
                else:
                    rows = pl.ds(pl.multiple_of(t * 256, 256), 256)
                    pltpu.make_async_copy(ref.at[rows, :], wk.at[0, pl.ds(512 + slot * 256, 256), :], load_sem.at[slot]).start()
            if condition is None:
                go()
            else:
                pl.when(condition)(go)

    def loaded(i, refs, slot):
        ref = refs[0][1]
        if i < 2:
            pltpu.make_async_copy(ref.at[0:192, :], wk.at[0, 0:192, :], load_sem.at[slot]).wait()
        elif i == 2:
            pltpu.make_async_copy(ref.at[:, 0:256], wn.at[slot, :, 0:256], load_sem.at[slot]).wait()
        else:
            pltpu.make_async_copy(ref.at[0:256, :], wk.at[0, 512:768, :], load_sem.at[slot]).wait()

    def store(i, dst, t, slot):
        if i == 2:
            rows = pl.ds(pl.multiple_of(t * 256, 256), 256)
            return pltpu.make_async_copy(wk.at[1, pl.ds(slot * 256, 256), :], dst.at[rows, :], store_sem.at[slot])
        return pltpu.make_async_copy(wn.at[slot, :, 256:512], dst.at[:, lanes(t * 256, 256)], store_sem.at[slot])

    def turn(i, refs, dst, first, count):
        load(i, refs, first, 0)

        def step(n, c):
            slot = n % 2

            @pl.when(n + 1 < count)
            def _():
                load(i, refs, first + n + 1, 1 - slot)
            loaded(i, refs, slot)

            @pl.when(n >= 2)
            def _():
                store(i, dst, first + n - 2, slot).wait()
            for b in range(6):
                cut = slice(b * 256, b * 256 + 256)
                if i == 2:
                    wk[1, pl.ds(pl.multiple_of(slot * 256, 256), 256), cut] = wn[slot, cut, 0:256].T
                else:
                    base = 0 if i < 2 else 512
                    wn[slot, cut, 256:512] = wk[0, pl.ds(pl.multiple_of(base + slot * 256, 256), 256), cut].T
            store(i, dst, first + n, slot).start()
            return c
        lax.fori_loop(0, count, step, 0)
        for n in (count - 2, count - 1):
            store(i, dst, first + n, n % 2).wait()

    counts = (12, 4, 12, 12)
    for i in range(4):
        @pl.when(is_r)
        def _(i=i):
            remote(near[i], near[i], send_sem.at[i], near_sem.at[i], place.sibling).wait_recv()
        turn(i, [(place.is_l, own[i]), (is_r, near[i])], turned[i][0], 0, counts[i])
    done = [0, 0, 0, 0]
    for c, (i, axis, index) in enumerate(PIECES):
        view = piece(far[i], axis, index)
        remote(view, view, d_send.at[i], far_sem.at[c], place.sibling).wait_recv()

        @pl.when(is_r)
        def _(i=i, c=c, view=view):
            remote(view, view, d_send.at[i], far_sem.at[c], place.sibling).start()
        count = 4 if i < 2 else 3
        turn(i, [(None, far[i])], turned[i][1], done[i], count)
        done[i] += count

    @pl.when(place.is_l)
    def _():
        for i in range(4):
            remote(own[i], near[i], send_sem.at[i], near_sem.at[i], place.sibling).wait_send()

    @pl.when(is_r)
    def _():
        for i in range(4):
            remote(own[i], far[i], y_send.at[i], far_sem.at[0], place.across_other).wait_send()
            remote(far[i], far[i], d_send.at[i], far_sem.at[0], place.sibling).wait_send()


def step_kernel(dims, x_ref, y_ref, wq, wo, wu, wd, own_gains,
                a_s, h_s, m_s, qkv_s, u_s, dx_s, oh_same, oh_other, oa_same, oa_other, od_same, od_other, og_same, og_other,
                dg_same, dg_other, loss_all, nq, no, nu, nd, fq, fo, fu, fd, tq0, to0, tu0, td0, tq1, to1, tu1, td1,
                abuf, gbuf, hbuf, obuf, nbuf, ybuf, qkvbuf, ubuf, habuf, zbuf, ctxbuf, dqkvbuf, acc, accg, lossbuf, losstile, gains, wres, wn, wk,
                send_sem, y_send, d_send, near_sem, far_sem, t_load, t_store,
                act_sem, grad_sem, hop_f, hop_b, keep_sem, back_sem, save_sem, stream_n, stream_k, res_sem, big_sem, load_sem, y_sem,
                os_sem, oo_sem, as_sem, ao_sem, ds_sem, do_sem, gs_sem, go_sem, bulk, gain_sem, tiny, loss_send):
    micro, seq, width, heads, head_dim, ffn = dims
    place = Place()
    is_first, is_last = place.home == 0, place.home == 3
    home02 = (place.home == 0) | (place.home == 2)
    home13 = jnp.logical_not(home02)
    is_r = jnp.logical_not(place.is_l)
    half = heads // 2 * HEAD_PAD
    scale = head_dim ** -0.5
    norm_factor = 1.0 / (micro * 2 * seq * width)
    own, near, far = (wq, wo, wu, wd), (nq, no, nu, nd), (fq, fo, fu, fd)
    turned = ((tq0, tq1), (to0, to1), (tu0, tu1), (td0, td1))
    entry_barrier(place)

    @pl.when(place.is_l)
    def _():
        pltpu.make_async_copy(own_gains, gains, gain_sem.at[0]).start()
        remote(own_gains, gains, gain_sem.at[1], gain_sem.at[0], place.sibling).start()

    @pl.when(is_first)
    def _():
        for m in range(micro):
            pltpu.make_async_copy(x_ref.at[m, place.core], abuf.at[m], act_sem.at[m]).start()
    weight_phase(place, is_r, own, near, far, turned, wn, wk, send_sem, y_send, d_send, near_sem, far_sem, t_load, t_store)
    pltpu.make_async_copy(own_gains, gains, gain_sem.at[0]).wait()

    @pl.when(place.is_l)
    def _():
        remote(own_gains, gains, gain_sem.at[1], gain_sem.at[0], place.sibling).wait_send()

    def near_of(i):
        return [(place.is_l, own[i]), (is_r, near[i])]

    def resident(choices_of_half, start):
        for c in range(6):
            for condition, ref in choices_of_half[c // 3]:
                copy = pltpu.make_async_copy(ref.at[(c % 3) * CHUNK:(c % 3 + 1) * CHUNK, :], wres.at[c], res_sem.at[c])
                if condition is None:
                    copy.start()
                else:
                    pl.when(condition)(copy.start)

    def resident_ready(j):
        pltpu.make_async_copy(wd.at[0:CHUNK, :], wres.at[j], res_sem.at[j]).wait()

    def saved(dst, index):
        return pltpu.make_async_copy(hbuf, dst, save_sem.at[index])

    sn = Stream(wn, stream_n, DEPTH, [([(None, tq0)], 3), ([(None, tq1)], 3), (near_of(2), 3), ([(None, fu)], 3)], micro * 12, False)
    sk = Stream(wk, stream_k, KDEPTH, [(near_of(1), 1), ([(None, fo)], 1)], micro * 2, True)
    sn.prime()
    sk.prime()
    resident((near_of(3), [(None, fd)]), True)
    lossbuf[...] = jnp.zeros_like(lossbuf)

    def qkv_out(m):
        return pltpu.make_async_copy(qkvbuf.at[0], qkv_s.at[m], big_sem.at[0])

    def up_out(m):
        return pltpu.make_async_copy(ubuf.at[0], u_s.at[m], big_sem.at[1])

    def act_out(m):
        return pltpu.make_async_copy(abuf.at[m], a_s.at[m], save_sem.at[2])

    def hop_forward(m):
        return remote(obuf.at[m % 2], abuf.at[m], hop_f.at[m % 2], act_sem.at[m], place.chain(1))

    def near_hand(src, dst_far, dst_own, sem, recv_sem):
        return (lambda: remote(src, dst_far, sem, recv_sem, place.sibling)), (lambda: pltpu.make_async_copy(src, dst_own, sem))

    def hand_out(m):
        return near_hand(obuf.at[m % 2], oa_other.at[m], oa_same.at[m], keep_sem.at[m % 2], ao_sem)

    def both_kinds(condition, copies, start):
        far_copy, own_copy = copies

        @pl.when(condition & place.is_l)
        def _():
            far_copy().start() if start else far_copy().wait_send()

        @pl.when(condition & is_r)
        def _():
            own_copy().start() if start else own_copy().wait()

    def forward_tick(m, carry):
        act, mid, out = abuf.at[m], hbuf, obuf.at[m % 2]
        pltpu.make_async_copy(x_ref.at[m, place.core], act, act_sem.at[m]).wait()
        act_out(m).start()

        @pl.when(place.is_l)
        def _():
            pltpu.make_async_copy(act, oa_same.at[m], as_sem).start()

        @pl.when(is_last)
        def _():
            pltpu.make_async_copy(y_ref.at[m, place.core], ybuf, y_sem).start()
        norm_rows(act, gains[0:1, :], nbuf, seq)

        @pl.when(m > 0)
        def _():
            qkv_out(m).wait()

        def qkv_step(j, c):
            w = sn.wait(m * 12 + j)
            for n in range(0, CHUNK, SUB):
                qkvbuf[0, :, lanes(j * CHUNK + n, SUB)] = mm(nbuf[...], w[:, n:n + SUB]).astype(BF)
            sn.start(m * 12 + j + DEPTH)
            return c
        lax.fori_loop(0, 6, qkv_step, 0)
        qkv_out(m).start()
        act_out(m).wait()

        @pl.when(is_r)
        def _():
            remote(a_s.at[m], oa_other.at[m], bulk.at[0], ao_sem, place.sibling).start()

        def head_step(i, c):
            for r in range(4):
                base = (i // 2) * (3 * half) + ((i % 2) * 4 + r) * HEAD_PAD
                q = qkvbuf[0, :, lanes(base, HEAD_PAD)]
                k = qkvbuf[0, :, lanes(base + half, HEAD_PAD)]
                v = qkvbuf[0, :, lanes(base + 2 * half, HEAD_PAD)]
                probs = causal_probs(q, k, scale).astype(BF)
                ctxbuf[:, lanes((i * 4 + r) * HEAD_PAD, HEAD_PAD)] = mm(probs, v).astype(BF)
            return c
        lax.fori_loop(0, heads // 4, head_step, 0)

        w0, w1 = sk.wait(m * 2), sk.wait(m * 2 + 1)
        for n in range(0, width, SUB):
            total = mm(ctxbuf[:, 0:half], w0[:, n:n + SUB]) + mm(ctxbuf[:, half:2 * half], w1[:, n:n + SUB])
            mid[:, n:n + SUB] = (act[:, n:n + SUB].astype(F32) + total).astype(BF)
        sk.start(m * 2 + KDEPTH)
        sk.start(m * 2 + 1 + KDEPTH)
        saved(h_s.at[m], 0).start()

        @pl.when(place.is_l)
        def _():
            saved(oh_same.at[m], 1).start()
        norm_rows(mid, gains[1:2, :], nbuf, seq)

        @pl.when(m > 0)
        def _():
            up_out(m).wait()
        acc[...] = jnp.zeros_like(acc)

        def mlp_step(j, c):
            w = sn.wait(m * 12 + 6 + j)
            for n in range(0, CHUNK, SUB):
                u = mm(nbuf[...], w[:, n:n + SUB]).astype(BF)
                ubuf[0, :, lanes(j * CHUNK + n, SUB)] = u
                uf = u.astype(F32)
                zbuf[:, n:n + SUB] = (uf * gelu_gate(uf)[0]).astype(BF)
            sn.start(m * 12 + 6 + j + DEPTH)

            @pl.when(m == 0)
            def _():
                resident_ready(j)
            for n in range(0, width, SUB):
                acc[:, n:n + SUB] += mm(zbuf[...], wres[j, :, n:n + SUB])
            return c
        lax.fori_loop(0, 6, mlp_step, 0)
        up_out(m).start()

        @pl.when((m > 1) & jnp.logical_not(is_last))
        def _():
            hop_forward(m).wait_send()

        both_kinds((m > 1) & home02, hand_out(m), False)

        def finish(rows):
            out[rows, :] = (mid[rows, :].astype(F32) + acc[rows, :]).astype(BF)
        rows_loop(seq, 32, finish)

        @pl.when(jnp.logical_not(is_last))
        def _():
            hop_forward(m).start()

        both_kinds(home02, hand_out(m), True)

        @pl.when(is_last)
        def _():
            pltpu.make_async_copy(y_ref.at[m, place.core], ybuf, y_sem).wait()

            def seed(rows):
                error = out[rows, :].astype(F32) - ybuf[rows, :].astype(F32)
                gbuf[m, rows, :] = (error * norm_factor).astype(BF)
                lossbuf[...] += jnp.sum((error * error).reshape(4, 8, width), axis=0)
            rows_loop(seq, 32, seed)

        saved(h_s.at[m], 0).wait()

        @pl.when(place.is_l)
        def _():
            saved(oh_same.at[m], 1).wait()
            remote(h_s.at[m], oh_same.at[m], bulk.at[2], os_sem, place.across).start()

        @pl.when(is_r)
        def _():
            remote(h_s.at[m], oh_other.at[m], bulk.at[2], oo_sem, place.sibling).start()
            remote(h_s.at[m], oh_other.at[m], bulk.at[3], oo_sem, place.across_other).start()

        @pl.when(is_last & place.is_l)
        def _():
            remote(gbuf.at[m], og_same.at[m], bulk.at[4], gs_sem, place.across).start()

        @pl.when(is_last & is_r)
        def _():
            remote(gbuf.at[m], og_other.at[m], bulk.at[4], go_sem, place.across_other).start()
        return carry

    lax.fori_loop(0, micro, forward_tick, 0)

    @pl.when(is_last)
    def _():
        total = lossbuf[:, 0:128]
        for n in range(128, width, 128):
            total = total + lossbuf[:, n:n + 128]
        losstile[...] = total
        pltpu.make_async_copy(losstile, loss_all.at[place.core], tiny.at[5]).start()
        for index, copy in enumerate(place.others(losstile, loss_all.at[place.core], loss_send, tiny.at[5])):
            copy.start()
    for copy in (qkv_out(micro - 1), up_out(micro - 1)):
        copy.wait()

    @pl.when(jnp.logical_not(is_last))
    def _():
        for m in (micro - 2, micro - 1):
            hop_forward(m).wait_send()
    for m in (micro - 2, micro - 1):
        both_kinds(home02, hand_out(m), False)

    bn = Stream(wn, stream_n, DEPTH, [([(None, td0)], 3), ([(None, td1)], 3), ([(None, to0)], 1), ([(None, to1)], 1)], micro * 8, False)
    bk = Stream(wk, stream_k, KDEPTH, [(near_of(0), 3), ([(None, fq)], 3)], micro * 6, True)
    bn.prime()
    bk.prime()
    resident(([(None, tu0)], [(None, tu1)]), True)

    def loads(i):
        m = micro - 1 - i
        slot = i % 2
        return (pltpu.make_async_copy(u_s.at[m], ubuf.at[slot], load_sem.at[0, slot]),
                pltpu.make_async_copy(qkv_s.at[m], qkvbuf.at[slot], load_sem.at[1, slot]),
                pltpu.make_async_copy(h_s.at[m], habuf.at[slot, 0], load_sem.at[2, slot]),
                pltpu.make_async_copy(a_s.at[m], habuf.at[slot, 1], load_sem.at[3, slot]))

    for copy in loads(0):
        copy.start()
    accg[...] = jnp.zeros_like(accg)

    def norm_back(index, x, base, dst, gain_row):
        def body(rows):
            xf = x[rows, :].astype(F32)
            dy = acc[rows, :].astype(BF).astype(F32)
            inv = lax.rsqrt(jnp.mean(xf * xf, axis=-1, keepdims=True) + NORM_EPS)
            xn = xf * inv
            accg[index] += jnp.sum((dy * xn).reshape(4, 8, width), axis=0)
            dyg = dy * gain_row
            dx = inv * (dyg - xn * jnp.mean(dyg * xn, axis=-1, keepdims=True))
            dst[rows, :] = (base[rows, :].astype(F32) + dx).astype(BF)
        rows_loop(seq, 32, body)

    def hop_back(i):
        m = micro - 1 - i
        return remote(obuf.at[i % 2], gbuf.at[m], hop_b.at[i % 2], grad_sem.at[m], place.chain(-1))

    def hand_back(i):
        m = micro - 1 - i
        return near_hand(obuf.at[i % 2], og_other.at[m], og_same.at[m], back_sem.at[i % 2], go_sem)

    def keep_dx(i):
        return pltpu.make_async_copy(obuf.at[i % 2], dx_s.at[micro - 1 - i], back_sem.at[i % 2])

    def back_ready(i):
        both_kinds((i > 1) & home13, hand_back(i), False)

        @pl.when((i > 1) & is_first)
        def _():
            keep_dx(i).wait()

        @pl.when((i > 1) & jnp.logical_not(is_first))
        def _():
            hop_back(i).wait_send()

    def backward_tick(i, carry):
        m = micro - 1 - i
        slot = i % 2
        grad, dmid, prev = gbuf.at[m], hbuf, obuf.at[slot]
        u_now, qkv_now, h_now, a_now = ubuf.at[slot], qkvbuf.at[slot], habuf.at[slot, 0], habuf.at[slot, 1]

        @pl.when(i + 1 < micro)
        def _():
            for copy in loads(i + 1):
                copy.start()

        @pl.when(jnp.logical_not(is_last))
        def _():
            remote(grad, grad, hop_b.at[slot], grad_sem.at[m], place.sibling).wait_recv()

        @pl.when(place.is_l)
        def _():
            pltpu.make_async_copy(grad, og_same.at[m], gs_sem).start()

        @pl.when(is_r)
        def _():
            remote(grad, og_other.at[m], bulk.at[5], go_sem, place.sibling).start()
        load_u, load_qkv, load_h, load_a = loads(i)
        load_u.wait()
        acc[...] = jnp.zeros_like(acc)

        def mlp_step(j, c):
            w = bn.wait(i * 8 + j)
            for n in range(0, CHUNK, SUB):
                dz = mm(grad[...], w[:, n:n + SUB]).astype(BF).astype(F32)
                u = u_now[:, lanes(j * CHUNK + n, SUB)].astype(F32)
                gate, u2 = gelu_gate(u)
                slope = gate + u * gate * (1.0 - gate) * (2.0 * GELU_A + (6.0 * GELU_A * GELU_B) * u2)
                zbuf[:, n:n + SUB] = (dz * slope).astype(BF)
            bn.start(i * 8 + j + DEPTH)

            @pl.when(i == 0)
            def _():
                resident_ready(j)
            for n in range(0, width, SUB):
                acc[:, n:n + SUB] += mm(zbuf[...], wres[j, :, n:n + SUB])
            return c
        lax.fori_loop(0, 6, mlp_step, 0)
        load_h.wait()
        norm_back(1, h_now, grad, dmid, gains[1:2, :])

        @pl.when(place.is_l)
        def _():
            saved(od_same.at[m], 0).start()

        @pl.when(is_r)
        def _():
            saved(m_s.at[m], 0).start()
        for c in range(2):
            w = bn.wait(i * 8 + 6 + c)
            for n in range(0, CHUNK, SUB):
                ctxbuf[:, c * CHUNK + n:c * CHUNK + n + SUB] = mm(dmid[...], w[:, n:n + SUB]).astype(BF)
            bn.start(i * 8 + 6 + c + DEPTH)
        load_qkv.wait()

        def head_step(t, c):
            for r in range(2):
                base = (t // 4) * (3 * half) + ((t % 4) * 2 + r) * HEAD_PAD
                q = qkv_now[:, lanes(base, HEAD_PAD)]
                k = qkv_now[:, lanes(base + half, HEAD_PAD)]
                v = qkv_now[:, lanes(base + 2 * half, HEAD_PAD)]
                dc = ctxbuf[:, lanes((t * 2 + r) * HEAD_PAD, HEAD_PAD)]
                probs = causal_probs(q, k, scale)
                dp = mm_nt(dc, v).astype(BF).astype(F32)
                ds = probs * (dp - jnp.sum(dp * probs, axis=-1, keepdims=True)) * scale
                dv = mm_tn(probs.astype(BF), dc)
                hi = ds.astype(BF)
                rest = ds - hi.astype(F32)
                lo = rest.astype(BF)
                tail = (rest - lo.astype(F32)).astype(BF)
                dq = mm(hi, k) + (mm(lo, k) + mm(tail, k))
                dk = mm_tn(hi, q) + (mm_tn(lo, q) + mm_tn(tail, q))
                dqkvbuf[:, lanes(base, HEAD_PAD)] = dq.astype(BF)
                dqkvbuf[:, lanes(base + half, HEAD_PAD)] = dk.astype(BF)
                dqkvbuf[:, lanes(base + 2 * half, HEAD_PAD)] = dv.astype(BF)
            return c
        lax.fori_loop(0, heads // 2, head_step, 0)
        acc[...] = jnp.zeros_like(acc)

        def qkv_step(j, c):
            w = bk.wait(i * 6 + j)
            for n in range(0, width, SUB):
                acc[:, n:n + SUB] += mm(dqkvbuf[:, lanes(j * CHUNK, CHUNK)], w[:, n:n + SUB])
            bk.start(i * 6 + j + KDEPTH)
            return c
        lax.fori_loop(0, 6, qkv_step, 0)
        load_a.wait()
        back_ready(i)
        norm_back(0, a_now, dmid, prev, gains[0:1, :])

        @pl.when(jnp.logical_not(is_first))
        def _():
            hop_back(i).start()

        @pl.when(is_first)
        def _():
            keep_dx(i).start()
        both_kinds(home13, hand_back(i), True)

        @pl.when(place.is_l)
        def _():
            saved(od_same.at[m], 0).wait()
            remote(od_same.at[m], od_same.at[m], bulk.at[6], ds_sem, place.across).start()

        @pl.when(is_r)
        def _():
            saved(m_s.at[m], 0).wait()
            remote(m_s.at[m], od_other.at[m], bulk.at[6], do_sem, place.sibling).start()
            remote(m_s.at[m], od_other.at[m], bulk.at[7], do_sem, place.across_other).start()

        @pl.when((place.home == 2) & place.is_l)
        def _():
            remote(a_s.at[m], oa_same.at[m], bulk.at[8], as_sem, place.across).start()

        @pl.when((place.home == 2) & is_r)
        def _():
            remote(a_s.at[m], oa_other.at[m], bulk.at[8], ao_sem, place.across_other).start()
        return carry

    lax.fori_loop(0, micro, backward_tick, 0)

    @pl.when((place.home == 1) & place.is_l)
    def _():
        for m in reversed(range(micro)):
            remote(gbuf.at[m], og_same.at[m], bulk.at[4], gs_sem, place.across).start()

    @pl.when((place.home == 1) & is_r)
    def _():
        for m in reversed(range(micro)):
            remote(gbuf.at[m], og_other.at[m], bulk.at[4], go_sem, place.across_other).start()

    @pl.when(place.is_l)
    def _():
        pltpu.make_async_copy(accg, dg_same, tiny.at[0]).start()
        remote(accg, dg_same, tiny.at[1], tiny.at[0], place.across).start()

    @pl.when(is_r)
    def _():
        remote(accg, dg_other, tiny.at[1], tiny.at[4], place.sibling).start()
        remote(accg, dg_other, tiny.at[2], tiny.at[4], place.across_other).start()

    for i in (micro - 2, micro - 1):
        back_ready(jnp.int32(i))

    def sent(buf, sem):
        remote(buf, a_s, sem, ao_sem, place.sibling).wait_send()

    def got(dst, sem):
        pltpu.make_async_copy(dst, dst, sem).wait()

    sent(h_s, bulk.at[2])
    sent(m_s, bulk.at[6])

    @pl.when(is_r)
    def _():
        sent(a_s, bulk.at[0])
        sent(h_s, bulk.at[3])
        sent(gbuf, bulk.at[5])
        sent(m_s, bulk.at[7])
        remote(accg, dg_other, tiny.at[2], tiny.at[4], place.sibling).wait_send()

    @pl.when(home13)
    def _():
        sent(gbuf, bulk.at[4])

    @pl.when(place.home == 2)
    def _():
        sent(a_s, bulk.at[8])

    @pl.when(is_last)
    def _():
        for copy in place.others(losstile, loss_all.at[place.core], loss_send, tiny.at[5]):
            copy.wait_send()
    remote(accg, dg_other, tiny.at[1], tiny.at[4], place.sibling).wait_send()
    got(oh_other, oo_sem)
    got(od_other, do_sem)
    got(og_other, go_sem)
    got(dg_same, tiny.at[0])
    got(dg_other, tiny.at[4])
    got(loss_all, tiny.at[5])

    @pl.when(is_r)
    def _():
        got(oh_same, os_sem)
        got(od_same, ds_sem)

    @pl.when(place.is_l | home02)
    def _():
        got(og_same, gs_sem)

    @pl.when(place.is_l | (place.home == 3))
    def _():
        got(oa_same, as_sem)

    @pl.when(place.is_l | (place.home != 1))
    def _():
        got(oa_other, ao_sem)


def step_phase(dims, x, y, own, own_gains):
    micro, seq, width, heads, head_dim, ffn = dims
    half = heads // 2 * HEAD_PAD
    act = (micro, seq, width)
    raw = [(heads // 2 * 3 * head_dim, width), (heads // 2 * head_dim, width), (width, ffn // 2), (ffn // 2, width)]
    turned = [(width, 3 * half), (width, half), (ffn // 2, width), (width, ffn // 2)]
    outs = [act, act, act, (micro, seq, 6 * half), (micro, seq, ffn), act] + [act] * 8
    out_shape = [jax.ShapeDtypeStruct(s, BF) for s in outs]
    out_shape += [jax.ShapeDtypeStruct(s, F32) for s in ((2, 8, width), (2, 8, width), (2, 8, 128))]
    out_shape += [jax.ShapeDtypeStruct(s, BF) for s in raw + raw + turned + turned]
    any_spec = pl.BlockSpec(memory_space=ANY)
    vmem, dma = pltpu.VMEM, pltpu.SemaphoreType.DMA
    scratch = [
        vmem(act, BF), vmem(act, BF), vmem((seq, width), BF), vmem((2, seq, width), BF), vmem((seq, width), BF), vmem((seq, width), BF),
        vmem((2, seq, 6 * half), BF), vmem((2, seq, ffn), BF), vmem((2, 2, seq, width), BF), vmem((seq, CHUNK), BF), vmem((seq, 2 * half), BF),
        vmem((seq, 6 * half), BF), vmem((seq, width), F32), vmem((2, 8, width), F32), vmem((8, width), F32), vmem((8, 128), F32),
        vmem((2, width), F32), vmem((6, CHUNK, width), BF), vmem((DEPTH, width, CHUNK), BF), vmem((KDEPTH, CHUNK, width), BF),
        dma((4,)), dma((4,)), dma((4,)), dma((4,)), dma((12,)), dma((2,)), dma((2,)),
        dma((micro,)), dma((micro,)), dma((2,)), dma((2,)), dma((2,)), dma((2,)), dma((3,)), dma((DEPTH,)), dma((KDEPTH,)), dma((6,)), dma((2,)),
        dma((4, 2)), dma(()),
        dma(()), dma(()), dma(()), dma(()), dma(()), dma(()), dma(()), dma(()), dma((9,)), dma((2,)), dma((6,)), dma((7,)),
    ]
    return pl.pallas_call(
        functools.partial(step_kernel, dims),
        out_shape=tuple(out_shape),
        in_specs=[any_spec] * 6 + [pl.BlockSpec(memory_space=vmem)],
        out_specs=(any_spec,) * len(out_shape),
        scratch_shapes=scratch,
        compiler_params=pltpu.CompilerParams(collective_id=0, has_side_effects=True, vmem_limit_bytes=67043328),
        name='step_phase',
    )(x, y, *own, own_gains)


def attn_scores(query, key):
    seq_len = query.shape[-2]
    scores = dot('bhqe,bhke->bhqk', query, key) * (query.shape[-1] ** -0.5)
    q_pos = lax.broadcasted_iota(jnp.int32, (seq_len, seq_len), 0)
    k_pos = lax.broadcasted_iota(jnp.int32, (seq_len, seq_len), 1)
    return jax.nn.softmax(jnp.where(k_pos <= q_pos, scores, -1e30), axis=-1)


def attn_backward(qkv, probs, d_context):
    scale = qkv.shape[-1] ** -0.5
    d_probs = dot('bhqe,bhke->bhqk', d_context, qkv[2]).astype(BF).astype(F32)
    d_value = dot('bhqk,bhqe->bhke', probs.astype(BF), d_context).astype(BF)
    d_scores = probs * (d_probs - jnp.sum(d_probs * probs, axis=-1, keepdims=True)) * scale
    d_query = jnp.einsum('bhqk,bhke->bhqe', d_scores, qkv[1].astype(F32), precision=lax.Precision.HIGHEST).astype(BF)
    d_key = jnp.einsum('bhqk,bhqe->bhke', d_scores, qkv[0].astype(F32), precision=lax.Precision.HIGHEST).astype(BF)
    return jnp.stack([d_query, d_key, d_value])


def owner_grads(act, mid, d_mid, grad_out, weights):
    w_qkv, w_out, w_up, w_down, gain_attn, gain_mlp = weights
    normed_a = rms_core(act.astype(F32), gain_attn).astype(BF)
    qkv = dot('bsd,dkhe->kbhse', normed_a, w_qkv).astype(BF)
    probs = attn_scores(qkv[0], qkv[1])
    context = dot('bhqk,bhke->bhqe', probs.astype(BF), qkv[2]).astype(BF)
    d_w_out = dot('bhse,bsd->hed', context, d_mid)
    d_context = dot('bsd,hed->bhse', d_mid, w_out).astype(BF)
    d_qkv = attn_backward(qkv, probs, d_context)
    d_w_qkv = dot('bsd,kbhse->dkhe', normed_a, d_qkv)
    normed_m = rms_core(mid.astype(F32), gain_mlp).astype(BF)
    up_f32 = dot('bsd,df->bsf', normed_m, w_up).astype(BF).astype(F32)
    hidden = gelu_tanh(up_f32).astype(BF)
    d_w_down = dot('bsf,bsd->fd', hidden, grad_out)
    d_act = dot('bsd,fd->bsf', grad_out, w_down).astype(BF)
    _, pull = jax.vjp(gelu_tanh, up_f32)
    d_up = pull(d_act.astype(F32))[0].astype(BF)
    d_w_up = dot('bsd,bsf->df', normed_m, d_up)
    return d_w_qkv, d_w_out, d_w_up, d_w_down


def solution(mesh):
    act_spec = P('rep', None, None, None)
    weight_specs = (
        P(('rep', 'stage'), None, None, 'tp', None),
        P(('rep', 'stage'), 'tp', None, None),
        P(('rep', 'stage'), None, 'tp'),
        P(('rep', 'stage'), 'tp', None),
        P(('rep', 'stage'), None),
        P(('rep', 'stage'), None),
    )

    def device_fn(inputs, targets, w_qkv, w_out, w_up, w_down, gain_attn, gain_mlp):
        micro_count, _, seq_len, width = inputs.shape
        dims = (micro_count, seq_len, width, 2 * w_out.shape[1], w_out.shape[2], 2 * w_up.shape[2])
        norm_factor = 1.0 / (inputs.size)
        stage = lax.axis_index('stage')
        tp = lax.axis_index('tp')
        x_pos, core = stage // 2, stage % 2
        home = jnp.where(x_pos == 0, tp, 3 - tp)
        is_l = stage == home
        own = (w_qkv[0], w_out[0], w_up[0], w_down[0])
        own_gains = (gain_attn[0].astype(F32), gain_mlp[0].astype(F32))
        rows_of = (own[0].transpose(1, 2, 3, 0).reshape(-1, width), own[1].reshape(-1, width), own[2], own[3])

        results = step_phase(dims, inputs, targets, rows_of, jnp.stack(own_gains))
        dx, oh_same, oh_other, oa_same, oa_other, od_same, od_other, og_same, og_other, dg_same, dg_other, loss_all = results[5:17]

        x_core = lax.dynamic_index_in_dim(inputs, core, 1, keepdims=False)
        x_other = lax.dynamic_index_in_dim(inputs, 1 - core, 1, keepdims=False)
        is_4 = (home == 1) & jnp.logical_not(is_l)
        both = lambda same, other: jnp.concatenate([same, other], 0)
        rows_a = both(jnp.where(is_4, x_core, oa_same), jnp.where(is_4, x_other, oa_other))
        weight_grads = owner_grads(rows_a, both(oh_same, oh_other), both(od_same, od_other), both(og_same, og_other), own + own_gains)
        mine = jnp.sum(dg_same + dg_other, 1)
        loss = jnp.sum(loss_all) * (0.5 * norm_factor)

        dx = dx[:, None]
        at_b = move(dx, [(0, 4), (1, 5)])
        at_d = move(dx, [(0, 2), (1, 3)])
        at_c = move(at_b, [(4, 6), (5, 7)])
        dx = jnp.where(home == 0, dx, jnp.where(home == 1, at_b, jnp.where(home == 2, at_c, at_d)))
        other = move(dx, CORE_SWAP)
        d_inputs = jnp.concatenate([jnp.where(core == 0, dx, other), jnp.where(core == 0, other, dx)], 1)
        return (loss.reshape(1), d_inputs) + tuple(g[None] for g in weight_grads) + (mine[0][None], mine[1][None])

    return jax.shard_map(device_fn, mesh=mesh, in_specs=(act_spec, act_spec) + weight_specs, out_specs=(P('rep'), act_spec) + weight_specs, check_vma=False)
```

```python
import functools

import jax
import jax.numpy as jnp
from jax import lax
from jax.experimental import pallas as pl
from jax.experimental.pallas import tpu as pltpu
from jax.sharding import PartitionSpec as P

NORM_EPS = 1e-5
AX = ('tp', 'stage')
BF = jnp.bfloat16
F32 = jnp.float32
MESH = pl.DeviceIdType.MESH
ANY = pl.ANY

R_SWAP = [(1, 4), (4, 1), (2, 7), (7, 2)]
CORE_SWAP = [(0, 1), (1, 0), (2, 3), (3, 2), (4, 5), (5, 4), (6, 7), (7, 6)]
L_TO_R = [(0, 1), (5, 4), (6, 7), (3, 2)]

GELU_A = 0.7978845608028654
GELU_B = 0.044715
I0, I1, I2, I3, I4, I6, I8 = 0, 1, 2, 3, 4, 6, 8
CHUNK = 1024
SUB = 256
DEPTH = 3
KDEPTH = 2
HEAD_PAD = 128
VMEM_LIMIT = 67043328


def move(value, perm):
    return lax.ppermute(value, AX, perm)


def mm(a, b):
    return lax.dot_general(a, b, (((I1,), (I0,)), ((), ())), preferred_element_type=F32)


def mm_nt(a, b):
    return lax.dot_general(a, b, (((I1,), (I1,)), ((), ())), preferred_element_type=F32)


def mm_tn(a, b):
    return lax.dot_general(a, b, (((I0,), (I0,)), ((), ())), preferred_element_type=F32)


class Place:
    def __init__(self):
        self.tp = lax.axis_index('tp')
        self.stage = lax.axis_index('stage')
        self.core = self.stage % I2
        self.x_pos = self.stage // I2
        self.home = self.x_pos * (I3 - I2 * self.tp) + self.tp
        self.is_l = self.stage == self.home
        self.sib = self.stage + I1 - I2 * self.core

    def at(self, tp, stage):
        return {'tp': tp, 'stage': stage}

    @property
    def sibling(self):
        return self.at(self.tp, self.sib)

    @property
    def across(self):
        return self.at(I1 - self.tp, self.stage)

    @property
    def across_other(self):
        return self.at(I1 - self.tp, self.sib)

    def others(self, src, dst, send_sems, recv_sem):
        copies = []
        for d_tp in (I0, I1):
            for d_stage in range(I4):
                if d_tp or d_stage:
                    there = self.at(self.tp + d_tp - I2 * d_tp * self.tp, (self.stage + d_stage) % I4)
                    copies.append(remote(src, dst, send_sems.at[len(copies)], recv_sem, there))
        return copies

    def chain(self, delta):
        there = self.home + delta
        x_pos = there // I2
        tp = there % I2 + x_pos * (I1 - I2 * (there % I2))
        return self.at(tp, I2 * x_pos + self.core)


def entry_barrier(place):
    barrier = pltpu.get_barrier_semaphore()
    for d_tp in (I0, I1):
        for d_stage in range(I4):
            if d_tp or d_stage:
                tp = place.tp + d_tp - I2 * d_tp * place.tp
                stage = (place.stage + d_stage) % I4
                pl.semaphore_signal(barrier, inc=I1, device_id=place.at(tp, stage), device_id_type=MESH)
    pl.semaphore_wait(barrier, 7)


def remote(src, dst, send_sem, recv_sem, device_id):
    return pltpu.make_async_remote_copy(src_ref=src, dst_ref=dst, send_sem=send_sem, recv_sem=recv_sem, device_id=device_id, device_id_type=MESH)


def rows_loop(total, step, body):
    def run(i, carry):
        body(pl.ds(pl.multiple_of(i * step, step), step))
        return carry
    lax.fori_loop(I0, total // step, run, I0)


def norm_rows(src, gain_row, dst, total):
    def body(rows):
        v = src[rows, :].astype(F32)
        inv = lax.rsqrt(jnp.mean(v * v, axis=-I1, keepdims=True) + NORM_EPS)
        dst[rows, :] = (v * inv * gain_row).astype(BF)
    rows_loop(total, 32, body)


def gelu_gate(u):
    u2 = u * u
    t = jnp.tanh(u * (GELU_A + (GELU_A * GELU_B) * u2))
    return 0.5 * t + 0.5, u2


def gelu_slope(hidden, gate, u2):
    return gate + hidden * (1.0 - gate) * (2.0 * GELU_A + (6.0 * GELU_A * GELU_B) * u2)


def causal_probs(q, k, scale):
    s = mm_nt(q, k) * scale
    q_pos = lax.broadcasted_iota(jnp.int32, s.shape, I0)
    k_pos = lax.broadcasted_iota(jnp.int32, s.shape, I1)
    s = jnp.where(k_pos <= q_pos, s, -1e30)
    e = jnp.exp(s - jnp.max(s, axis=-I1, keepdims=True))
    return e * (1.0 / jnp.sum(e, axis=-I1, keepdims=True))


def attention_backward(q, k, v, d_ctx, scale):
    probs = causal_probs(q, k, scale)
    probs_bf = probs.astype(BF)
    dp = mm_nt(d_ctx, v).astype(BF).astype(F32)
    ds = probs * (dp - jnp.sum(dp * probs, axis=-I1, keepdims=True)) * scale
    dv = mm_tn(probs_bf, d_ctx)
    hi = ds.astype(BF)
    rest = ds - hi.astype(F32)
    lo = rest.astype(BF)
    tail = (rest - lo.astype(F32)).astype(BF)
    dq = mm(hi, k) + (mm(lo, k) + mm(tail, k))
    dk = mm_tn(hi, q) + (mm_tn(lo, q) + mm_tn(tail, q))
    return probs_bf, dq.astype(BF), dk.astype(BF), dv.astype(BF)


def lanes(offset, size):
    return pl.ds(pl.multiple_of(offset, 128), size)


class Stream:
    def __init__(self, buf, sem, depth, parts, total, by_heads):
        self.buf, self.sem, self.depth, self.parts, self.total, self.by_heads = buf, sem, depth, parts, total, by_heads
        self.per_tick = sum(p[I1] for p in parts)

    def copy_in(self, ref, index, slot):
        if not self.by_heads:
            where = pl.ds(pl.multiple_of(index * CHUNK, CHUNK), CHUNK)
            pltpu.make_async_copy(ref.at[:, where], self.buf.at[slot], self.sem.at[slot]).start()
            return
        for r in range(I8):
            rows = pl.ds(pl.multiple_of(index * 768 + r * 96, 96), 96)
            pltpu.make_async_copy(ref.at[rows, :], self.buf.at[slot, r * 128:r * 128 + 96, :], self.sem.at[slot]).start()

    def start(self, seq):
        @pl.when(seq < self.total)
        def _():
            j = seq % self.per_tick
            slot = seq % self.depth
            base = I0
            for choices, chunks in self.parts:
                for condition, ref in choices:
                    here = (j >= base) & (j < base + chunks)
                    here = here if condition is None else here & condition

                    @pl.when(here)
                    def _(ref=ref, low=base):
                        self.copy_in(ref, j - low, slot)
                base += chunks

    def prime(self):
        for seq in range(self.depth):
            self.start(jnp.int32(seq))

    def wait(self, seq):
        slot = seq % self.depth
        ref = self.parts[I0][I0][I0][I1]
        if self.by_heads:
            pltpu.make_async_copy(ref.at[I0:768, :], self.buf.at[slot, I0:768, :], self.sem.at[slot]).wait()
        else:
            pltpu.make_async_copy(ref.at[:, I0:CHUNK], self.buf.at[slot], self.sem.at[slot]).wait()
        return self.buf.at[slot]


PIECES = [(0, 0, 0), (0, 0, 1), (0, 0, 2), (1, 0, 0), (2, 1, 0), (2, 1, 1), (2, 1, 2), (2, 1, 3), (3, 0, 0), (3, 0, 1), (3, 0, 2), (3, 0, 3)]


def piece(ref, axis, index):
    return ref.at[index * 768:(index + I1) * 768, :] if axis == I0 else ref.at[:, index * 768:(index + I1) * 768]


def weight_phase(place, is_r, own, near, far, turned, wn, wk, send_sem, y_send, d_send, near_sem, far_sem, load_sem, store_sem):
    wk[...] = jnp.zeros_like(wk)

    @pl.when(place.is_l)
    def _():
        for i in range(I4):
            remote(own[i], near[i], send_sem.at[i], near_sem.at[i], place.sibling).start()

    @pl.when(is_r)
    def _():
        for c, (i, axis, index) in enumerate(PIECES):
            remote(piece(own[i], axis, index), piece(far[i], axis, index), y_send.at[i], far_sem.at[c], place.across_other).start()

    def load(i, refs, t, slot):
        for condition, ref in refs:
            def go(ref=ref):
                if i < I2:
                    for r in range(I2):
                        rows = pl.ds(pl.multiple_of(t * 192 + r * 96, 96), 96)
                        pltpu.make_async_copy(ref.at[rows, :], wk.at[I0, pl.ds(slot * SUB + r * 128, 96), :], load_sem.at[slot]).start()
                elif i == I2:
                    pltpu.make_async_copy(ref.at[:, lanes(t * SUB, SUB)], wn.at[slot, :, I0:SUB], load_sem.at[slot]).start()
                else:
                    rows = pl.ds(pl.multiple_of(t * SUB, SUB), SUB)
                    pltpu.make_async_copy(ref.at[rows, :], wk.at[I0, pl.ds(512 + slot * SUB, SUB), :], load_sem.at[slot]).start()
            if condition is None:
                go()
            else:
                pl.when(condition)(go)

    def loaded(i, refs, slot):
        ref = refs[I0][I1]
        if i < I2:
            pltpu.make_async_copy(ref.at[I0:192, :], wk.at[I0, I0:192, :], load_sem.at[slot]).wait()
        elif i == I2:
            pltpu.make_async_copy(ref.at[:, I0:SUB], wn.at[slot, :, I0:SUB], load_sem.at[slot]).wait()
        else:
            pltpu.make_async_copy(ref.at[I0:SUB, :], wk.at[I0, 512:768, :], load_sem.at[slot]).wait()

    def store(i, dst, t, slot):
        if i == I2:
            rows = pl.ds(pl.multiple_of(t * SUB, SUB), SUB)
            return pltpu.make_async_copy(wk.at[I1, pl.ds(slot * SUB, SUB), :], dst.at[rows, :], store_sem.at[slot])
        return pltpu.make_async_copy(wn.at[slot, :, SUB:512], dst.at[:, lanes(t * SUB, SUB)], store_sem.at[slot])

    def turn(i, refs, dst, first, count):
        load(i, refs, first, I0)

        def step(n, c):
            slot = n % I2

            @pl.when(n + I1 < count)
            def _():
                load(i, refs, first + n + I1, I1 - slot)
            loaded(i, refs, slot)

            @pl.when(n >= I2)
            def _():
                store(i, dst, first + n - I2, slot).wait()
            for b in range(I6):
                cut = slice(b * SUB, b * SUB + SUB)
                if i == I2:
                    wk[I1, pl.ds(pl.multiple_of(slot * SUB, SUB), SUB), cut] = wn[slot, cut, I0:SUB].T
                else:
                    base = I0 if i < I2 else 512
                    wn[slot, cut, SUB:512] = wk[I0, pl.ds(pl.multiple_of(base + slot * SUB, SUB), SUB), cut].T
            store(i, dst, first + n, slot).start()
            return c
        lax.fori_loop(I0, count, step, I0)
        for n in (count - I2, count - I1):
            store(i, dst, first + n, n % I2).wait()

    counts = (12, I4, 12, 12)
    for i in range(I4):
        @pl.when(is_r)
        def _(i=i):
            remote(near[i], near[i], send_sem.at[i], near_sem.at[i], place.sibling).wait_recv()
        turn(i, [(place.is_l, own[i]), (is_r, near[i])], turned[i][I0], I0, counts[i])
    done = [I0, I0, I0, I0]
    for c, (i, axis, index) in enumerate(PIECES):
        view = piece(far[i], axis, index)
        remote(view, view, d_send.at[i], far_sem.at[c], place.sibling).wait_recv()

        @pl.when(is_r)
        def _(i=i, c=c, view=view):
            remote(view, view, d_send.at[i], far_sem.at[c], place.sibling).start()
        count = I4 if i < I2 else I3
        turn(i, [(None, far[i])], turned[i][I1], done[i], count)
        done[i] += count

    @pl.when(place.is_l)
    def _():
        for i in range(I4):
            remote(own[i], near[i], send_sem.at[i], near_sem.at[i], place.sibling).wait_send()

    @pl.when(is_r)
    def _():
        for i in range(I4):
            remote(own[i], far[i], y_send.at[i], far_sem.at[I0], place.across_other).wait_send()
            remote(far[i], far[i], d_send.at[i], far_sem.at[I0], place.sibling).wait_send()


def step_kernel(dims, x_ref, y_ref, wq, wo, wu, wd, own_gains,
                a_s, h_s, m_s, qkv_s, u_s, dx_s, oh_same, oh_other, oa_same, oa_other, od_same, od_other, og_same, og_other,
                dg_same, dg_other, loss_all, nq, no, nu, nd, fq, fo, fu, fd, tq0, to0, tu0, td0, tq1, to1, tu1, td1,
                abuf, gbuf, hbuf, obuf, nbuf, ybuf, qkvbuf, ubuf, habuf, zbuf, ctxbuf, dqkvbuf, acc, accg, lossbuf, losstile, gains, wres, wn, wk,
                send_sem, y_send, d_send, near_sem, far_sem, t_load, t_store,
                act_sem, grad_sem, hop_f, hop_b, keep_sem, back_sem, save_sem, stream_n, stream_k, res_sem, big_sem, load_sem, y_sem,
                os_sem, oo_sem, as_sem, ao_sem, ds_sem, do_sem, gs_sem, go_sem, bulk, gain_sem, tiny, loss_send):
    micro, seq, width, heads, head_dim, ffn = dims
    place = Place()
    is_first, is_last = place.home == I0, place.home == I3
    home02 = (place.home == I0) | (place.home == I2)
    home13 = jnp.logical_not(home02)
    is_r = jnp.logical_not(place.is_l)
    half = heads // I2 * HEAD_PAD
    scale = head_dim ** -0.5
    norm_factor = 1.0 / (micro * I2 * seq * width)
    own, near, far = (wq, wo, wu, wd), (nq, no, nu, nd), (fq, fo, fu, fd)
    turned = ((tq0, tq1), (to0, to1), (tu0, tu1), (td0, td1))
    entry_barrier(place)

    @pl.when(place.is_l)
    def _():
        pltpu.make_async_copy(own_gains, gains, gain_sem.at[I0]).start()
        remote(own_gains, gains, gain_sem.at[I1], gain_sem.at[I0], place.sibling).start()

    @pl.when(is_first)
    def _():
        for m in range(micro):
            pltpu.make_async_copy(x_ref.at[m, place.core], abuf.at[m], act_sem.at[m]).start()
    weight_phase(place, is_r, own, near, far, turned, wn, wk, send_sem, y_send, d_send, near_sem, far_sem, t_load, t_store)
    pltpu.make_async_copy(own_gains, gains, gain_sem.at[I0]).wait()

    @pl.when(place.is_l)
    def _():
        remote(own_gains, gains, gain_sem.at[I1], gain_sem.at[I0], place.sibling).wait_send()

    def near_of(i):
        return [(place.is_l, own[i]), (is_r, near[i])]

    def resident(choices_of_half, start):
        for c in range(I6):
            for condition, ref in choices_of_half[c // I3]:
                copy = pltpu.make_async_copy(ref.at[(c % I3) * CHUNK:(c % I3 + I1) * CHUNK, :], wres.at[c], res_sem.at[c])
                if condition is None:
                    copy.start()
                else:
                    pl.when(condition)(copy.start)

    def resident_ready(j):
        pltpu.make_async_copy(wd.at[I0:CHUNK, :], wres.at[j], res_sem.at[j]).wait()

    def saved(dst, index):
        return pltpu.make_async_copy(hbuf, dst, save_sem.at[index])

    sn = Stream(wn, stream_n, DEPTH, [([(None, tq0)], I3), ([(None, tq1)], I3), (near_of(I2), I3), ([(None, fu)], I3)], micro * 12, False)
    sk = Stream(wk, stream_k, KDEPTH, [(near_of(I1), I1), ([(None, fo)], I1)], micro * I2, True)
    sn.prime()
    sk.prime()
    resident((near_of(I3), [(None, fd)]), True)
    lossbuf[...] = jnp.zeros_like(lossbuf)

    def qkv_out(m):
        return pltpu.make_async_copy(qkvbuf.at[I0], qkv_s.at[m], big_sem.at[I0])

    def up_out(m):
        return pltpu.make_async_copy(ubuf.at[I0], u_s.at[m], big_sem.at[I1])

    def act_out(m):
        return pltpu.make_async_copy(abuf.at[m], a_s.at[m], save_sem.at[I2])

    def hop_forward(m):
        return remote(obuf.at[m % I2], abuf.at[m], hop_f.at[m % I2], act_sem.at[m], place.chain(I1))

    def near_hand(src, dst_far, dst_own, sem, recv_sem):
        return (lambda: remote(src, dst_far, sem, recv_sem, place.sibling)), (lambda: pltpu.make_async_copy(src, dst_own, sem))

    def hand_out(m):
        return near_hand(obuf.at[m % I2], oa_other.at[m], oa_same.at[m], keep_sem.at[m % I2], ao_sem)

    def both_kinds(condition, copies, start):
        far_copy, own_copy = copies

        @pl.when(condition & place.is_l)
        def _():
            far_copy().start() if start else far_copy().wait_send()

        @pl.when(condition & is_r)
        def _():
            own_copy().start() if start else own_copy().wait()

    def forward_tick(m, carry):
        act, mid, out = abuf.at[m], hbuf, obuf.at[m % I2]
        pltpu.make_async_copy(x_ref.at[m, place.core], act, act_sem.at[m]).wait()
        act_out(m).start()

        @pl.when(place.is_l)
        def _():
            pltpu.make_async_copy(act, oa_same.at[m], as_sem).start()

        @pl.when(is_last)
        def _():
            pltpu.make_async_copy(y_ref.at[m, place.core], ybuf, y_sem).start()
        norm_rows(act, gains[I0:I1, :], nbuf, seq)

        @pl.when(m > I0)
        def _():
            qkv_out(m).wait()

        def qkv_step(j, c):
            w = sn.wait(m * 12 + j)
            for n in range(I0, CHUNK, SUB):
                qkvbuf[I0, :, lanes(j * CHUNK + n, SUB)] = mm(nbuf[...], w[:, n:n + SUB]).astype(BF)
            sn.start(m * 12 + j + DEPTH)
            return c
        lax.fori_loop(I0, I6, qkv_step, I0)
        qkv_out(m).start()
        act_out(m).wait()

        @pl.when(is_r)
        def _():
            remote(a_s.at[m], oa_other.at[m], bulk.at[I0], ao_sem, place.sibling).start()

        def head_step(i, c):
            for r in range(I4):
                base = (i // I2) * (I3 * half) + ((i % I2) * I4 + r) * HEAD_PAD
                q = qkvbuf[I0, :, lanes(base, HEAD_PAD)]
                k = qkvbuf[I0, :, lanes(base + half, HEAD_PAD)]
                v = qkvbuf[I0, :, lanes(base + I2 * half, HEAD_PAD)]
                probs = causal_probs(q, k, scale).astype(BF)
                ctxbuf[:, lanes((i * I4 + r) * HEAD_PAD, HEAD_PAD)] = mm(probs, v).astype(BF)
            return c
        lax.fori_loop(I0, heads // I4, head_step, I0)

        w0, w1 = sk.wait(m * I2), sk.wait(m * I2 + I1)
        for n in range(I0, width, SUB):
            total = mm(ctxbuf[:, I0:half], w0[:, n:n + SUB]) + mm(ctxbuf[:, half:I2 * half], w1[:, n:n + SUB])
            mid[:, n:n + SUB] = (act[:, n:n + SUB].astype(F32) + total).astype(BF)
        sk.start(m * I2 + KDEPTH)
        sk.start(m * I2 + I1 + KDEPTH)
        saved(h_s.at[m], I0).start()

        @pl.when(place.is_l)
        def _():
            saved(oh_same.at[m], I1).start()
        norm_rows(mid, gains[I1:I2, :], nbuf, seq)

        @pl.when(m > I0)
        def _():
            up_out(m).wait()
        acc[...] = jnp.zeros_like(acc)

        def mlp_step(j, c):
            w = sn.wait(m * 12 + I6 + j)
            for n in range(I0, CHUNK, SUB):
                u = mm(nbuf[...], w[:, n:n + SUB]).astype(BF)
                ubuf[I0, :, lanes(j * CHUNK + n, SUB)] = u
                uf = u.astype(F32)
                zbuf[:, n:n + SUB] = (uf * gelu_gate(uf)[I0]).astype(BF)
            sn.start(m * 12 + I6 + j + DEPTH)

            @pl.when(m == I0)
            def _():
                resident_ready(j)
            for n in range(I0, width, SUB):
                acc[:, n:n + SUB] += mm(zbuf[...], wres[j, :, n:n + SUB])
            return c
        lax.fori_loop(I0, I6, mlp_step, I0)
        up_out(m).start()

        @pl.when((m > I1) & jnp.logical_not(is_last))
        def _():
            hop_forward(m).wait_send()

        both_kinds((m > I1) & home02, hand_out(m), False)

        def finish(rows):
            out[rows, :] = (mid[rows, :].astype(F32) + acc[rows, :]).astype(BF)
        rows_loop(seq, 32, finish)

        @pl.when(jnp.logical_not(is_last))
        def _():
            hop_forward(m).start()

        both_kinds(home02, hand_out(m), True)

        @pl.when(is_last)
        def _():
            pltpu.make_async_copy(y_ref.at[m, place.core], ybuf, y_sem).wait()

            def seed(rows):
                error = out[rows, :].astype(F32) - ybuf[rows, :].astype(F32)
                gbuf[m, rows, :] = (error * norm_factor).astype(BF)
                lossbuf[...] += jnp.sum((error * error).reshape(I4, I8, width), axis=I0)
            rows_loop(seq, 32, seed)

        saved(h_s.at[m], I0).wait()

        @pl.when(place.is_l)
        def _():
            saved(oh_same.at[m], I1).wait()
            remote(h_s.at[m], oh_same.at[m], bulk.at[I2], os_sem, place.across).start()

        @pl.when(is_r)
        def _():
            remote(h_s.at[m], oh_other.at[m], bulk.at[I2], oo_sem, place.sibling).start()
            remote(h_s.at[m], oh_other.at[m], bulk.at[I3], oo_sem, place.across_other).start()

        @pl.when(is_last & place.is_l)
        def _():
            remote(gbuf.at[m], og_same.at[m], bulk.at[I4], gs_sem, place.across).start()

        @pl.when(is_last & is_r)
        def _():
            remote(gbuf.at[m], og_other.at[m], bulk.at[I4], go_sem, place.across_other).start()
        return carry

    lax.fori_loop(I0, micro, forward_tick, I0)

    @pl.when(is_last)
    def _():
        total = lossbuf[:, I0:128]
        for n in range(128, width, 128):
            total = total + lossbuf[:, n:n + 128]
        losstile[...] = total
        pltpu.make_async_copy(losstile, loss_all.at[place.core], tiny.at[5]).start()
        for index, copy in enumerate(place.others(losstile, loss_all.at[place.core], loss_send, tiny.at[5])):
            copy.start()
    for copy in (qkv_out(micro - I1), up_out(micro - I1)):
        copy.wait()

    @pl.when(jnp.logical_not(is_last))
    def _():
        for m in (micro - I2, micro - I1):
            hop_forward(m).wait_send()
    for m in (micro - I2, micro - I1):
        both_kinds(home02, hand_out(m), False)

    bn = Stream(wn, stream_n, DEPTH, [([(None, td0)], I3), ([(None, td1)], I3), ([(None, to0)], I1), ([(None, to1)], I1)], micro * I8, False)
    bk = Stream(wk, stream_k, KDEPTH, [(near_of(I0), I3), ([(None, fq)], I3)], micro * I6, True)
    bn.prime()
    bk.prime()
    resident(([(None, tu0)], [(None, tu1)]), True)

    def loads(i):
        m = micro - I1 - i
        slot = i % I2
        return (pltpu.make_async_copy(u_s.at[m], ubuf.at[slot], load_sem.at[I0, slot]),
                pltpu.make_async_copy(qkv_s.at[m], qkvbuf.at[slot], load_sem.at[I1, slot]),
                pltpu.make_async_copy(h_s.at[m], habuf.at[slot, I0], load_sem.at[I2, slot]),
                pltpu.make_async_copy(a_s.at[m], habuf.at[slot, I1], load_sem.at[I3, slot]))

    for copy in loads(I0):
        copy.start()
    accg[...] = jnp.zeros_like(accg)

    def norm_back(index, x, base, dst, gain_row):
        def body(rows):
            xf = x[rows, :].astype(F32)
            dy = acc[rows, :].astype(BF).astype(F32)
            inv = lax.rsqrt(jnp.mean(xf * xf, axis=-I1, keepdims=True) + NORM_EPS)
            xn = xf * inv
            accg[index] += jnp.sum((dy * xn).reshape(I4, I8, width), axis=I0)
            dyg = dy * gain_row
            dx = inv * (dyg - xn * jnp.mean(dyg * xn, axis=-I1, keepdims=True))
            dst[rows, :] = (base[rows, :].astype(F32) + dx).astype(BF)
        rows_loop(seq, 32, body)

    def hop_back(i):
        m = micro - I1 - i
        return remote(obuf.at[i % I2], gbuf.at[m], hop_b.at[i % I2], grad_sem.at[m], place.chain(-I1))

    def hand_back(i):
        m = micro - I1 - i
        return near_hand(obuf.at[i % I2], og_other.at[m], og_same.at[m], back_sem.at[i % I2], go_sem)

    def keep_dx(i):
        return pltpu.make_async_copy(obuf.at[i % I2], dx_s.at[micro - I1 - i], back_sem.at[i % I2])

    def back_ready(i):
        both_kinds((i > I1) & home13, hand_back(i), False)

        @pl.when((i > I1) & is_first)
        def _():
            keep_dx(i).wait()

        @pl.when((i > I1) & jnp.logical_not(is_first))
        def _():
            hop_back(i).wait_send()

    def backward_tick(i, carry):
        m = micro - I1 - i
        slot = i % I2
        grad, dmid, prev = gbuf.at[m], hbuf, obuf.at[slot]
        u_now, qkv_now, h_now, a_now = ubuf.at[slot], qkvbuf.at[slot], habuf.at[slot, I0], habuf.at[slot, I1]

        @pl.when(i + I1 < micro)
        def _():
            for copy in loads(i + I1):
                copy.start()

        @pl.when(jnp.logical_not(is_last))
        def _():
            remote(grad, grad, hop_b.at[slot], grad_sem.at[m], place.sibling).wait_recv()

        @pl.when(place.is_l)
        def _():
            pltpu.make_async_copy(grad, og_same.at[m], gs_sem).start()

        @pl.when(is_r)
        def _():
            remote(grad, og_other.at[m], bulk.at[5], go_sem, place.sibling).start()
        load_u, load_qkv, load_h, load_a = loads(i)
        load_u.wait()
        acc[...] = jnp.zeros_like(acc)

        def mlp_step(j, c):
            w = bn.wait(i * I8 + j)
            for n in range(I0, CHUNK, SUB):
                dz = mm(grad[...], w[:, n:n + SUB]).astype(BF).astype(F32)
                u = u_now[:, lanes(j * CHUNK + n, SUB)].astype(F32)
                gate, u2 = gelu_gate(u)
                zbuf[:, n:n + SUB] = (dz * gelu_slope(u * gate, gate, u2)).astype(BF)
            bn.start(i * I8 + j + DEPTH)

            @pl.when(i == I0)
            def _():
                resident_ready(j)
            for n in range(I0, width, SUB):
                acc[:, n:n + SUB] += mm(zbuf[...], wres[j, :, n:n + SUB])
            return c
        lax.fori_loop(I0, I6, mlp_step, I0)
        load_h.wait()
        norm_back(I1, h_now, grad, dmid, gains[I1:I2, :])

        @pl.when(place.is_l)
        def _():
            saved(od_same.at[m], I0).start()

        @pl.when(is_r)
        def _():
            saved(m_s.at[m], I0).start()
        for c in range(I2):
            w = bn.wait(i * I8 + I6 + c)
            for n in range(I0, CHUNK, SUB):
                ctxbuf[:, c * CHUNK + n:c * CHUNK + n + SUB] = mm(dmid[...], w[:, n:n + SUB]).astype(BF)
            bn.start(i * I8 + I6 + c + DEPTH)
        load_qkv.wait()

        def head_step(t, c):
            for r in range(I2):
                base = (t // I4) * (I3 * half) + ((t % I4) * I2 + r) * HEAD_PAD
                q = qkv_now[:, lanes(base, HEAD_PAD)]
                k = qkv_now[:, lanes(base + half, HEAD_PAD)]
                v = qkv_now[:, lanes(base + I2 * half, HEAD_PAD)]
                dc = ctxbuf[:, lanes((t * I2 + r) * HEAD_PAD, HEAD_PAD)]
                _, dq, dk, dv = attention_backward(q, k, v, dc, scale)
                dqkvbuf[:, lanes(base, HEAD_PAD)] = dq
                dqkvbuf[:, lanes(base + half, HEAD_PAD)] = dk
                dqkvbuf[:, lanes(base + I2 * half, HEAD_PAD)] = dv
            return c
        lax.fori_loop(I0, heads // I2, head_step, I0)
        acc[...] = jnp.zeros_like(acc)

        def qkv_step(j, c):
            w = bk.wait(i * I6 + j)
            for n in range(I0, width, SUB):
                acc[:, n:n + SUB] += mm(dqkvbuf[:, lanes(j * CHUNK, CHUNK)], w[:, n:n + SUB])
            bk.start(i * I6 + j + KDEPTH)
            return c
        lax.fori_loop(I0, I6, qkv_step, I0)
        load_a.wait()
        back_ready(i)
        norm_back(I0, a_now, dmid, prev, gains[I0:I1, :])

        @pl.when(jnp.logical_not(is_first))
        def _():
            hop_back(i).start()

        @pl.when(is_first)
        def _():
            keep_dx(i).start()
        both_kinds(home13, hand_back(i), True)

        @pl.when(place.is_l)
        def _():
            saved(od_same.at[m], I0).wait()
            remote(od_same.at[m], od_same.at[m], bulk.at[I6], ds_sem, place.across).start()

        @pl.when(is_r)
        def _():
            saved(m_s.at[m], I0).wait()
            remote(m_s.at[m], od_other.at[m], bulk.at[I6], do_sem, place.sibling).start()
            remote(m_s.at[m], od_other.at[m], bulk.at[7], do_sem, place.across_other).start()

        @pl.when((place.home == I2) & place.is_l)
        def _():
            remote(a_s.at[m], oa_same.at[m], bulk.at[I8], as_sem, place.across).start()

        @pl.when((place.home == I2) & is_r)
        def _():
            remote(a_s.at[m], oa_other.at[m], bulk.at[I8], ao_sem, place.across_other).start()
        return carry

    lax.fori_loop(I0, micro, backward_tick, I0)

    @pl.when((place.home == I1) & place.is_l)
    def _():
        for m in reversed(range(micro)):
            remote(gbuf.at[m], og_same.at[m], bulk.at[I4], gs_sem, place.across).start()

    @pl.when((place.home == I1) & is_r)
    def _():
        for m in reversed(range(micro)):
            remote(gbuf.at[m], og_other.at[m], bulk.at[I4], go_sem, place.across_other).start()

    @pl.when(place.is_l)
    def _():
        pltpu.make_async_copy(accg, dg_same, tiny.at[I0]).start()
        remote(accg, dg_same, tiny.at[I1], tiny.at[I0], place.across).start()

    @pl.when(is_r)
    def _():
        remote(accg, dg_other, tiny.at[I1], tiny.at[I4], place.sibling).start()
        remote(accg, dg_other, tiny.at[I2], tiny.at[I4], place.across_other).start()

    for i in (micro - I2, micro - I1):
        back_ready(jnp.int32(i))

    def sent(buf, sem):
        remote(buf, a_s, sem, ao_sem, place.sibling).wait_send()

    def got(dst, sem):
        pltpu.make_async_copy(dst, dst, sem).wait()

    sent(h_s, bulk.at[I2])
    sent(m_s, bulk.at[I6])

    @pl.when(is_r)
    def _():
        sent(a_s, bulk.at[I0])
        sent(h_s, bulk.at[I3])
        sent(gbuf, bulk.at[5])
        sent(m_s, bulk.at[7])
        remote(accg, dg_other, tiny.at[I2], tiny.at[I4], place.sibling).wait_send()

    @pl.when(home13)
    def _():
        sent(gbuf, bulk.at[I4])

    @pl.when(place.home == I2)
    def _():
        sent(a_s, bulk.at[I8])

    @pl.when(is_last)
    def _():
        for copy in place.others(losstile, loss_all.at[place.core], loss_send, tiny.at[5]):
            copy.wait_send()
    remote(accg, dg_other, tiny.at[I1], tiny.at[I4], place.sibling).wait_send()
    got(oh_other, oo_sem)
    got(od_other, do_sem)
    got(og_other, go_sem)
    got(dg_same, tiny.at[I0])
    got(dg_other, tiny.at[I4])
    got(loss_all, tiny.at[5])

    @pl.when(is_r)
    def _():
        got(oh_same, os_sem)
        got(od_same, ds_sem)

    @pl.when(place.is_l | home02)
    def _():
        got(og_same, gs_sem)

    @pl.when(place.is_l | (place.home == I3))
    def _():
        got(oa_same, as_sem)

    @pl.when(place.is_l | (place.home != I1))
    def _():
        got(oa_other, ao_sem)


def step_phase(dims, x, y, own, own_gains):
    micro, seq, width, heads, head_dim, ffn = dims
    half = heads // I2 * HEAD_PAD
    act = (micro, seq, width)
    raw = [(heads // I2 * I3 * head_dim, width), (heads // I2 * head_dim, width), (width, ffn // I2), (ffn // I2, width)]
    turned = [(width, I3 * half), (width, half), (ffn // I2, width), (width, ffn // I2)]
    outs = [act, act, act, (micro, seq, I6 * half), (micro, seq, ffn), act] + [act] * I8
    out_shape = [jax.ShapeDtypeStruct(s, BF) for s in outs]
    out_shape += [jax.ShapeDtypeStruct(s, F32) for s in ((I2, I8, width), (I2, I8, width), (I2, I8, 128))]
    out_shape += [jax.ShapeDtypeStruct(s, BF) for s in raw + raw + turned + turned]
    any_spec = pl.BlockSpec(memory_space=ANY)
    vmem, dma = pltpu.VMEM, pltpu.SemaphoreType.DMA
    scratch = [
        vmem(act, BF), vmem(act, BF), vmem((seq, width), BF), vmem((I2, seq, width), BF), vmem((seq, width), BF), vmem((seq, width), BF),
        vmem((I2, seq, I6 * half), BF), vmem((I2, seq, ffn), BF), vmem((I2, I2, seq, width), BF), vmem((seq, CHUNK), BF), vmem((seq, I2 * half), BF),
        vmem((seq, I6 * half), BF), vmem((seq, width), F32), vmem((I2, I8, width), F32), vmem((I8, width), F32), vmem((I8, 128), F32),
        vmem((I2, width), F32), vmem((I6, CHUNK, width), BF), vmem((DEPTH, width, CHUNK), BF), vmem((KDEPTH, CHUNK, width), BF),
        dma((I4,)), dma((I4,)), dma((I4,)), dma((I4,)), dma((12,)), dma((I2,)), dma((I2,)),
        dma((micro,)), dma((micro,)), dma((I2,)), dma((I2,)), dma((I2,)), dma((I2,)), dma((I3,)), dma((DEPTH,)), dma((KDEPTH,)), dma((I6,)), dma((I2,)),
        dma((I4, I2)), dma(()),
        dma(()), dma(()), dma(()), dma(()), dma(()), dma(()), dma(()), dma(()), dma((9,)), dma((I2,)), dma((I6,)), dma((7,)),
    ]
    return pl.pallas_call(
        functools.partial(step_kernel, dims),
        out_shape=tuple(out_shape),
        in_specs=[any_spec] * I6 + [pl.BlockSpec(memory_space=vmem)],
        out_specs=(any_spec,) * len(out_shape),
        scratch_shapes=scratch,
        compiler_params=pltpu.CompilerParams(collective_id=I0, has_side_effects=True, vmem_limit_bytes=VMEM_LIMIT),
        name='step_phase',
    )(x, y, *own, own_gains)


TOKENS = 512


def bring(pairs, sem):
    copies = [pltpu.make_async_copy(src, dst, sem.at[i]) for i, (src, dst) in enumerate(pairs)]
    for copy in copies:
        copy.start()
    return copies


def turn_into(dst, src, rows, cols):
    for r in range(I0, rows, SUB):
        for c in range(I0, cols, SUB):
            high, wide = min(SUB, rows - r), min(SUB, cols - c)
            dst[c:c + wide, r:r + high] = src[r:r + high, c:c + wide].T


def owner_mlp_kernel(hs, ho, gs, go, gain, wu, wd, dwu, dwd, n2, n2t, grad, wdt, z, zt, dup, sem):
    tokens, width = n2.shape
    part = tokens // I2

    @pl.when(pl.program_id(I0) == I0)
    def _():
        low, high = pl.ds(I0, part), pl.ds(part, part)
        for copy in bring([(hs, n2.at[low]), (ho, n2.at[high]), (gs, grad.at[low]), (go, grad.at[high])], sem):
            copy.wait()

        def prepare(rows):
            norm_rows(n2.at[rows], gain[...], n2.at[rows], SUB)
            for c in range(I0, width, SUB):
                n2t[c:c + SUB, rows] = n2[rows, c:c + SUB].T
        rows_loop(tokens, SUB, prepare)
    turn_into(wdt, wd, SUB, width)

    def front(rows):
        u = mm(n2[rows, :], wu[...]).astype(BF).astype(F32)
        dz = mm(grad[rows, :], wdt[...]).astype(BF).astype(F32)
        gate, u2 = gelu_gate(u)
        hidden = u * gate
        z[rows, :] = hidden.astype(BF)
        dup[rows, :] = (dz * gelu_slope(hidden, gate, u2)).astype(BF)
    rows_loop(tokens, TOKENS, front)
    turn_into(zt, z, tokens, SUB)
    for c in range(I0, width, TOKENS):
        dwu[c:c + TOKENS, :] = mm(n2t[c:c + TOKENS, :], dup[...])
    for c in range(I0, width, SUB):
        dwd[:, c:c + SUB] = mm(zt[...], grad[:, c:c + SUB])


def owner_mlp(h_rows, g_rows, gain, w_up, w_down):
    width, ffn = w_up.shape
    part = h_rows[I0].shape[I0]
    vmem = pltpu.VMEM
    any_spec = pl.BlockSpec(memory_space=ANY)
    up_spec = pl.BlockSpec((width, SUB), lambda i: (I0, i))
    down_spec = pl.BlockSpec((SUB, width), lambda i: (i, I0))
    rows = lambda n: vmem((I2 * part, n), BF)
    return pl.pallas_call(
        owner_mlp_kernel,
        grid=(ffn // SUB,),
        out_shape=(jax.ShapeDtypeStruct(w_up.shape, F32), jax.ShapeDtypeStruct(w_down.shape, F32)),
        in_specs=[any_spec] * I4 + [pl.BlockSpec(memory_space=vmem), up_spec, down_spec],
        out_specs=(up_spec, down_spec),
        scratch_shapes=[rows(width), vmem((width, I2 * part), BF), rows(width), vmem((width, SUB), BF), rows(SUB), vmem((SUB, I2 * part), BF), rows(SUB), pltpu.SemaphoreType.DMA((I4,))],
        compiler_params=pltpu.CompilerParams(vmem_limit_bytes=VMEM_LIMIT),
        cost_estimate=pl.CostEstimate(flops=16 * part * width * ffn, bytes_accessed=12 * width * ffn, transcendentals=I2 * part * ffn),
        name='owner_mlp',
    )(*h_rows, *g_rows, gain, w_up, w_down)


def owner_attn_kernel(seq, x_ref, rs, ro, ds, do, gain, wq, wo, dwq, dwo, n1, dmid, wpad, wqt, wot, qkv, dctx, dqkv, ctx, dqkvt, ctxt, sem):
    tokens, width = n1.shape
    part = tokens // I2
    head_dim = wo.shape[I1]
    scale = head_dim ** -0.5
    pair = I2 * HEAD_PAD

    @pl.when(pl.program_id(I0) == I0)
    def _():
        place = Place()
        from_x = (place.home == I1) & jnp.logical_not(place.is_l)
        low, high = pl.ds(I0, part), pl.ds(part, part)
        d_copies = bring([(ds, dmid.at[low]), (do, dmid.at[high])], sem)
        a_pairs = [(rs, n1.at[low]), (ro, n1.at[high])]
        a_sem = sem.at[I2:I4]

        @pl.when(from_x)
        def _():
            for m in range(part // seq):
                for first, core in ((I0, place.core), (part, I1 - place.core)):
                    pltpu.make_async_copy(x_ref.at[m, core], n1.at[pl.ds(first + m * seq, seq)], a_sem.at[min(first, I1)]).start()

        @pl.when(jnp.logical_not(from_x))
        def _():
            bring(a_pairs, a_sem)
        wpad[...] = jnp.zeros_like(wpad)
        for i, (src, dst) in enumerate(a_pairs):
            pltpu.make_async_copy(src, dst, a_sem.at[i]).wait()
        norm_rows(n1, gain[...], n1, tokens)
        for copy in d_copies:
            copy.wait()
    for r in range(I2):
        for t in range(I3):
            wpad[I0:head_dim, :] = wq[t, r]
            at = t * pair + r * HEAD_PAD
            turn_into(wqt.at[:, at:at + HEAD_PAD], wpad, HEAD_PAD, width)
        wpad[I0:head_dim, :] = wo[r]
        turn_into(wot.at[:, r * HEAD_PAD:(r + I1) * HEAD_PAD], wpad, HEAD_PAD, width)

    def front(rows):
        for n in range(I0, I3 * pair, pair):
            qkv[rows, n:n + pair] = mm(n1[rows, :], wqt[:, n:n + pair]).astype(BF)
        dctx[rows, :] = mm(dmid[rows, :], wot[...]).astype(BF)
    rows_loop(tokens, TOKENS, front)

    def sequence(rows):
        for r in range(I2):
            q_at, k_at, v_at = [slice(t * pair + r * HEAD_PAD, t * pair + (r + I1) * HEAD_PAD) for t in range(I3)]
            v, dc = qkv[rows, v_at], dctx[rows, q_at]
            probs, dq, dk, dv = attention_backward(qkv[rows, q_at], qkv[rows, k_at], v, dc, scale)
            ctx[rows, q_at] = mm(probs, v).astype(BF)
            dqkv[rows, q_at], dqkv[rows, k_at], dqkv[rows, v_at] = dq, dk, dv
    rows_loop(tokens, seq, sequence)

    def turn(rows):
        for t in range(I6):
            dqkvt[t * head_dim:(t + I1) * head_dim, rows] = dqkv[rows, t * HEAD_PAD:(t + I1) * HEAD_PAD].T[I0:head_dim]
        for t in range(I2):
            ctxt[t * head_dim:(t + I1) * head_dim, rows] = ctx[rows, t * HEAD_PAD:(t + I1) * HEAD_PAD].T[I0:head_dim]
    rows_loop(tokens, SUB, turn)
    for c in range(I0, width, SUB):
        cut = slice(c, c + SUB)
        dwq[:, :, :, cut] = mm(dqkvt[...], n1[:, cut]).reshape(I3, I2, head_dim, SUB)
        dwo[:, :, cut] = mm(ctxt[...], dmid[:, cut]).reshape(I2, head_dim, SUB)


def owner_attn(seq, x, a_rows, d_rows, gain, w_qkv, w_out):
    heads, head_dim, width = w_out.shape
    part = a_rows[I0].shape[I0]
    vmem = pltpu.VMEM
    any_spec = pl.BlockSpec(memory_space=ANY)
    q_spec = pl.BlockSpec((I3, I2, head_dim, width), lambda i: (I0, i, I0, I0))
    o_spec = pl.BlockSpec((I2, head_dim, width), lambda i: (i, I0, I0))
    rows = lambda n: vmem((I2 * part, n), BF)
    pair = I2 * HEAD_PAD
    return pl.pallas_call(
        functools.partial(owner_attn_kernel, seq),
        grid=(heads // I2,),
        out_shape=(jax.ShapeDtypeStruct(w_qkv.shape, F32), jax.ShapeDtypeStruct(w_out.shape, F32)),
        in_specs=[any_spec] * 5 + [pl.BlockSpec(memory_space=vmem), q_spec, o_spec],
        out_specs=(q_spec, o_spec),
        scratch_shapes=[
            rows(width), rows(width), vmem((HEAD_PAD, width), BF), vmem((width, I3 * pair), BF), vmem((width, pair), BF),
            rows(I3 * pair), rows(pair), rows(I3 * pair), rows(pair), vmem((I6 * head_dim, I2 * part), BF), vmem((I2 * head_dim, I2 * part), BF),
            pltpu.SemaphoreType.DMA((I4,)),
        ],
        compiler_params=pltpu.CompilerParams(vmem_limit_bytes=VMEM_LIMIT),
        cost_estimate=pl.CostEstimate(flops=36 * part * width * heads * head_dim, bytes_accessed=16 * width * width, transcendentals=part * heads * seq),
        name='owner_attn',
    )(x, *a_rows, *d_rows, gain, w_qkv, w_out)


def solution(mesh):
    act_spec = P('rep', None, None, None)
    weight_specs = (
        P(('rep', 'stage'), None, None, 'tp', None),
        P(('rep', 'stage'), 'tp', None, None),
        P(('rep', 'stage'), None, 'tp'),
        P(('rep', 'stage'), 'tp', None),
        P(('rep', 'stage'), None),
        P(('rep', 'stage'), None),
    )

    def device_fn(inputs, targets, w_qkv, w_out, w_up, w_down, gain_attn, gain_mlp):
        micro_count, _, seq_len, width = inputs.shape
        dims = (micro_count, seq_len, width, I2 * w_out.shape[I1], w_out.shape[I2], I2 * w_up.shape[I2])
        norm_factor = 1.0 / (inputs.size)
        stage = lax.axis_index('stage')
        tp = lax.axis_index('tp')
        x_pos, core = stage // I2, stage % I2
        home = jnp.where(x_pos == I0, tp, I3 - tp)
        is_l = stage == home
        own = (w_qkv[I0], w_out[I0], w_up[I0], w_down[I0])
        own_gains = jnp.concatenate([gain_attn, gain_mlp]).astype(F32)
        rows_of = (own[I0].transpose(I1, I2, I3, I0).reshape(-I1, width), own[I1].reshape(-I1, width), own[I2], own[I3])

        results = step_phase(dims, inputs, targets, rows_of, own_gains)
        dx, oh_same, oh_other, oa_same, oa_other, od_same, od_other, og_same, og_other, dg_same, dg_other, loss_all = results[5:17]

        flat = lambda *rows: [r.reshape(-I1, width) for r in rows]
        d_up, d_down = owner_mlp(flat(oh_same, oh_other), flat(og_same, og_other), own_gains[I1:], own[I2], own[I3])
        w_rows = own[I0].transpose(I1, I2, I3, I0)
        d_qkv, d_out = owner_attn(seq_len, inputs, flat(oa_same, oa_other), flat(od_same, od_other), own_gains[:I1], w_rows, own[I1])
        weight_grads = (d_qkv.transpose(I3, I0, I1, I2), d_out, d_up, d_down)
        mine = jnp.sum(dg_same + dg_other, I1)
        loss = jnp.sum(loss_all) * (0.5 * norm_factor)

        dx = dx[:, None]
        at_b = move(dx, [(I0, I4), (I1, 5)])
        at_d = move(dx, [(I0, I2), (I1, I3)])
        at_c = move(at_b, [(I4, I6), (5, 7)])
        dx = jnp.where(home == I0, dx, jnp.where(home == I1, at_b, jnp.where(home == I2, at_c, at_d)))
        other = move(dx, CORE_SWAP)
        d_inputs = jnp.concatenate([jnp.where(core == I0, dx, other), jnp.where(core == I0, other, dx)], I1)
        return (loss.reshape(I1), d_inputs) + tuple(g[None] for g in weight_grads) + (mine[I0][None], mine[I1][None])

    return jax.shard_map(device_fn, mesh=mesh, in_specs=(act_spec, act_spec) + weight_specs, out_specs=(P('rep'), act_spec) + weight_specs, check_vma=False)
```

```python
import functools

import jax
import jax.numpy as jnp
from jax import lax
from jax.experimental import pallas as pl
from jax.experimental.pallas import tpu as pltpu
from jax.sharding import PartitionSpec as P

NORM_EPS = 1e-5
BF = jnp.bfloat16
F32 = jnp.float32
MESH = pl.DeviceIdType.MESH
ANY = pl.ANY


GELU_A = 0.7978845608028654
GELU_B = 0.044715
I0, I1, I2, I3, I4, I6, I8 = 0, 1, 2, 3, 4, 6, 8
CHUNK = 1024
SUB = 256
DEPTH = 3
KDEPTH = 2
HEAD_PAD = 128
VMEM_LIMIT = 67043328


def mm(a, b):
    return lax.dot_general(a, b, (((I1,), (I0,)), ((), ())), preferred_element_type=F32)


def mm_nt(a, b):
    return lax.dot_general(a, b, (((I1,), (I1,)), ((), ())), preferred_element_type=F32)


def mm_tn(a, b):
    return lax.dot_general(a, b, (((I0,), (I0,)), ((), ())), preferred_element_type=F32)


class Place:
    def __init__(self):
        self.tp = lax.axis_index('tp')
        self.stage = lax.axis_index('stage')
        self.core = self.stage % I2
        self.x_pos = self.stage // I2
        self.home = self.x_pos * (I3 - I2 * self.tp) + self.tp
        self.is_l = self.stage == self.home
        self.sib = self.stage + I1 - I2 * self.core

    def at(self, tp, stage):
        return {'tp': tp, 'stage': stage}

    @property
    def sibling(self):
        return self.at(self.tp, self.sib)

    @property
    def across(self):
        return self.at(I1 - self.tp, self.stage)

    @property
    def across_other(self):
        return self.at(I1 - self.tp, self.sib)

    def others(self, src, dst, send_sems, recv_sem):
        copies = []
        for d_tp in (I0, I1):
            for d_stage in range(I4):
                if d_tp or d_stage:
                    there = self.at(self.tp + d_tp - I2 * d_tp * self.tp, (self.stage + d_stage) % I4)
                    copies.append(remote(src, dst, send_sems.at[len(copies)], recv_sem, there))
        return copies

    def chain(self, delta):
        there = self.home + delta
        x_pos = there // I2
        tp = there % I2 + x_pos * (I1 - I2 * (there % I2))
        return self.at(tp, I2 * x_pos + self.core)


def entry_barrier(place):
    barrier = pltpu.get_barrier_semaphore()
    for d_tp in (I0, I1):
        for d_stage in range(I4):
            if d_tp or d_stage:
                tp = place.tp + d_tp - I2 * d_tp * place.tp
                stage = (place.stage + d_stage) % I4
                pl.semaphore_signal(barrier, inc=I1, device_id=place.at(tp, stage), device_id_type=MESH)
    pl.semaphore_wait(barrier, 7)


def remote(src, dst, send_sem, recv_sem, device_id):
    return pltpu.make_async_remote_copy(src_ref=src, dst_ref=dst, send_sem=send_sem, recv_sem=recv_sem, device_id=device_id, device_id_type=MESH)


def rows_loop(total, step, body):
    def run(i, carry):
        body(pl.ds(pl.multiple_of(i * step, step), step))
        return carry
    lax.fori_loop(I0, total // step, run, I0)


def norm_rows(src, gain_row, dst, total):
    def body(rows):
        v = src[rows, :].astype(F32)
        inv = lax.rsqrt(jnp.mean(v * v, axis=-I1, keepdims=True) + NORM_EPS)
        dst[rows, :] = (v * inv * gain_row).astype(BF)
    rows_loop(total, 32, body)


def gelu_gate(u):
    u2 = u * u
    t = jnp.tanh(u * (GELU_A + (GELU_A * GELU_B) * u2))
    return 0.5 * t + 0.5, u2


def gelu_slope(hidden, gate, u2):
    return gate + hidden * (1.0 - gate) * (2.0 * GELU_A + (6.0 * GELU_A * GELU_B) * u2)


def causal_probs(q, k, scale):
    s = mm_nt(q, k) * scale
    q_pos = lax.broadcasted_iota(jnp.int32, s.shape, I0)
    k_pos = lax.broadcasted_iota(jnp.int32, s.shape, I1)
    s = jnp.where(k_pos <= q_pos, s, -1e30)
    e = jnp.exp(s - jnp.max(s, axis=-I1, keepdims=True))
    return e * (1.0 / jnp.sum(e, axis=-I1, keepdims=True))


def attention_backward(q, k, v, d_ctx, scale):
    probs = causal_probs(q, k, scale)
    probs_bf = probs.astype(BF)
    dp = mm_nt(d_ctx, v).astype(BF).astype(F32)
    ds = probs * (dp - jnp.sum(dp * probs, axis=-I1, keepdims=True)) * scale
    dv = mm_tn(probs_bf, d_ctx)
    hi = ds.astype(BF)
    rest = ds - hi.astype(F32)
    lo = rest.astype(BF)
    tail = (rest - lo.astype(F32)).astype(BF)
    dq = mm(hi, k) + (mm(lo, k) + mm(tail, k))
    dk = mm_tn(hi, q) + (mm_tn(lo, q) + mm_tn(tail, q))
    return probs_bf, dq.astype(BF), dk.astype(BF), dv.astype(BF)


def lanes(offset, size):
    return pl.ds(pl.multiple_of(offset, 128), size)


class Stream:
    def __init__(self, buf, sem, depth, parts, total, by_heads):
        self.buf, self.sem, self.depth, self.parts, self.total, self.by_heads = buf, sem, depth, parts, total, by_heads
        self.per_tick = sum(p[I1] for p in parts)

    def copy_in(self, ref, index, slot):
        if not self.by_heads:
            where = pl.ds(pl.multiple_of(index * CHUNK, CHUNK), CHUNK)
            pltpu.make_async_copy(ref.at[:, where], self.buf.at[slot], self.sem.at[slot]).start()
            return
        for r in range(I8):
            rows = pl.ds(pl.multiple_of(index * 768 + r * 96, 96), 96)
            pltpu.make_async_copy(ref.at[rows, :], self.buf.at[slot, r * 128:r * 128 + 96, :], self.sem.at[slot]).start()

    def start(self, seq):
        @pl.when(seq < self.total)
        def _():
            j = seq % self.per_tick
            slot = seq % self.depth
            base = I0
            for choices, chunks in self.parts:
                for condition, ref in choices:
                    here = (j >= base) & (j < base + chunks)
                    here = here if condition is None else here & condition

                    @pl.when(here)
                    def _(ref=ref, low=base):
                        self.copy_in(ref, j - low, slot)
                base += chunks

    def prime(self):
        for seq in range(self.depth):
            self.start(jnp.int32(seq))

    def wait(self, seq):
        slot = seq % self.depth
        ref = self.parts[I0][I0][I0][I1]
        if self.by_heads:
            pltpu.make_async_copy(ref.at[I0:768, :], self.buf.at[slot, I0:768, :], self.sem.at[slot]).wait()
        else:
            pltpu.make_async_copy(ref.at[:, I0:CHUNK], self.buf.at[slot], self.sem.at[slot]).wait()
        return self.buf.at[slot]


PIECES = [(0, 0, 0), (0, 0, 1), (0, 0, 2), (1, 0, 0), (2, 1, 0), (2, 1, 1), (2, 1, 2), (2, 1, 3), (3, 0, 0), (3, 0, 1), (3, 0, 2), (3, 0, 3)]


def piece(ref, axis, index):
    return ref.at[index * 768:(index + I1) * 768, :] if axis == I0 else ref.at[:, index * 768:(index + I1) * 768]


def weight_phase(place, is_r, own, near, far, turned, wn, wk, send_sem, y_send, d_send, near_sem, far_sem, load_sem, store_sem):
    wk[...] = jnp.zeros_like(wk)

    @pl.when(place.is_l)
    def _():
        for i in range(I4):
            remote(own[i], near[i], send_sem.at[i], near_sem.at[i], place.sibling).start()

    @pl.when(is_r)
    def _():
        for c, (i, axis, index) in enumerate(PIECES):
            remote(piece(own[i], axis, index), piece(far[i], axis, index), y_send.at[i], far_sem.at[c], place.across_other).start()

    def load(i, refs, t, slot):
        for condition, ref in refs:
            def go(ref=ref):
                if i < I2:
                    for r in range(I2):
                        rows = pl.ds(pl.multiple_of(t * 192 + r * 96, 96), 96)
                        pltpu.make_async_copy(ref.at[rows, :], wk.at[I0, pl.ds(slot * SUB + r * 128, 96), :], load_sem.at[slot]).start()
                elif i == I2:
                    pltpu.make_async_copy(ref.at[:, lanes(t * SUB, SUB)], wn.at[slot, :, I0:SUB], load_sem.at[slot]).start()
                else:
                    rows = pl.ds(pl.multiple_of(t * SUB, SUB), SUB)
                    pltpu.make_async_copy(ref.at[rows, :], wk.at[I0, pl.ds(512 + slot * SUB, SUB), :], load_sem.at[slot]).start()
            if condition is None:
                go()
            else:
                pl.when(condition)(go)

    def loaded(i, refs, slot):
        ref = refs[I0][I1]
        if i < I2:
            pltpu.make_async_copy(ref.at[I0:192, :], wk.at[I0, I0:192, :], load_sem.at[slot]).wait()
        elif i == I2:
            pltpu.make_async_copy(ref.at[:, I0:SUB], wn.at[slot, :, I0:SUB], load_sem.at[slot]).wait()
        else:
            pltpu.make_async_copy(ref.at[I0:SUB, :], wk.at[I0, 512:768, :], load_sem.at[slot]).wait()

    def store(i, dst, t, slot):
        if i == I2:
            rows = pl.ds(pl.multiple_of(t * SUB, SUB), SUB)
            return pltpu.make_async_copy(wk.at[I1, pl.ds(slot * SUB, SUB), :], dst.at[rows, :], store_sem.at[slot])
        return pltpu.make_async_copy(wn.at[slot, :, SUB:512], dst.at[:, lanes(t * SUB, SUB)], store_sem.at[slot])

    def turn(i, refs, dst, first, count):
        load(i, refs, first, I0)

        def step(n, c):
            slot = n % I2

            @pl.when(n + I1 < count)
            def _():
                load(i, refs, first + n + I1, I1 - slot)
            loaded(i, refs, slot)

            @pl.when(n >= I2)
            def _():
                store(i, dst, first + n - I2, slot).wait()
            for b in range(I6):
                cut = slice(b * SUB, b * SUB + SUB)
                if i == I2:
                    wk[I1, pl.ds(pl.multiple_of(slot * SUB, SUB), SUB), cut] = wn[slot, cut, I0:SUB].T
                else:
                    base = I0 if i < I2 else 512
                    wn[slot, cut, SUB:512] = wk[I0, pl.ds(pl.multiple_of(base + slot * SUB, SUB), SUB), cut].T
            store(i, dst, first + n, slot).start()
            return c
        lax.fori_loop(I0, count, step, I0)
        for n in (count - I2, count - I1):
            store(i, dst, first + n, n % I2).wait()

    counts = (12, I4, 12, 12)
    for i in range(I4):
        @pl.when(is_r)
        def _(i=i):
            remote(near[i], near[i], send_sem.at[i], near_sem.at[i], place.sibling).wait_recv()
        turn(i, [(place.is_l, own[i]), (is_r, near[i])], turned[i][I0], I0, counts[i])
    done = [I0, I0, I0, I0]
    for c, (i, axis, index) in enumerate(PIECES):
        view = piece(far[i], axis, index)
        remote(view, view, d_send.at[i], far_sem.at[c], place.sibling).wait_recv()

        @pl.when(is_r)
        def _(i=i, c=c, view=view):
            remote(view, view, d_send.at[i], far_sem.at[c], place.sibling).start()
        count = I4 if i < I2 else I3
        turn(i, [(None, far[i])], turned[i][I1], done[i], count)
        done[i] += count

    @pl.when(place.is_l)
    def _():
        for i in range(I4):
            remote(own[i], near[i], send_sem.at[i], near_sem.at[i], place.sibling).wait_send()

    @pl.when(is_r)
    def _():
        for i in range(I4):
            remote(own[i], far[i], y_send.at[i], far_sem.at[I0], place.across_other).wait_send()
            remote(far[i], far[i], d_send.at[i], far_sem.at[I0], place.sibling).wait_send()


def step_kernel(dims, x_ref, y_ref, wq, wo, wu, wd, own_gains,
                a_s, h_s, m_s, qkv_s, u_s, dx_s, oh_same, oh_other, oa_same, oa_other, od_same, od_other, og_same, og_other,
                dg_same, dg_other, loss_all, nq, no, nu, nd, fq, fo, fu, fd, tq0, to0, tu0, td0, tq1, to1, tu1, td1,
                abuf, gbuf, hbuf, obuf, nbuf, ybuf, qkvbuf, ubuf, habuf, zbuf, ctxbuf, dqkvbuf, acc, accg, lossbuf, losstile, gains, wres, wn, wk,
                send_sem, y_send, d_send, near_sem, far_sem, t_load, t_store,
                act_sem, grad_sem, hop_f, hop_b, keep_sem, back_sem, save_sem, stream_n, stream_k, res_sem, big_sem, load_sem, y_sem,
                os_sem, oo_sem, as_sem, ao_sem, ds_sem, do_sem, gs_sem, go_sem, bulk, gain_sem, tiny, loss_send):
    micro, seq, width, heads, head_dim, ffn = dims
    place = Place()
    is_first, is_last = place.home == I0, place.home == I3
    home02 = (place.home == I0) | (place.home == I2)
    home13 = jnp.logical_not(home02)
    is_r = jnp.logical_not(place.is_l)
    half = heads // I2 * HEAD_PAD
    scale = head_dim ** -0.5
    norm_factor = 1.0 / (micro * I2 * seq * width)
    own, near, far = (wq, wo, wu, wd), (nq, no, nu, nd), (fq, fo, fu, fd)
    turned = ((tq0, tq1), (to0, to1), (tu0, tu1), (td0, td1))
    entry_barrier(place)

    @pl.when(place.is_l)
    def _():
        pltpu.make_async_copy(own_gains, gains, gain_sem.at[I0]).start()
        remote(own_gains, gains, gain_sem.at[I1], gain_sem.at[I0], place.sibling).start()

    @pl.when(is_first)
    def _():
        for m in range(micro):
            pltpu.make_async_copy(x_ref.at[m, place.core], abuf.at[m], act_sem.at[m]).start()
    weight_phase(place, is_r, own, near, far, turned, wn, wk, send_sem, y_send, d_send, near_sem, far_sem, t_load, t_store)
    pltpu.make_async_copy(own_gains, gains, gain_sem.at[I0]).wait()

    @pl.when(place.is_l)
    def _():
        remote(own_gains, gains, gain_sem.at[I1], gain_sem.at[I0], place.sibling).wait_send()

    def near_of(i):
        return [(place.is_l, own[i]), (is_r, near[i])]

    def resident(choices_of_half, start):
        for c in range(I6):
            for condition, ref in choices_of_half[c // I3]:
                copy = pltpu.make_async_copy(ref.at[(c % I3) * CHUNK:(c % I3 + I1) * CHUNK, :], wres.at[c], res_sem.at[c])
                if condition is None:
                    copy.start()
                else:
                    pl.when(condition)(copy.start)

    def resident_ready(j):
        pltpu.make_async_copy(wd.at[I0:CHUNK, :], wres.at[j], res_sem.at[j]).wait()

    def saved(dst, index):
        return pltpu.make_async_copy(hbuf, dst, save_sem.at[index])

    sn = Stream(wn, stream_n, DEPTH, [([(None, tq0)], I3), ([(None, tq1)], I3), (near_of(I2), I3), ([(None, fu)], I3)], micro * 12, False)
    sk = Stream(wk, stream_k, KDEPTH, [(near_of(I1), I1), ([(None, fo)], I1)], micro * I2, True)
    sn.prime()
    sk.prime()
    resident((near_of(I3), [(None, fd)]), True)
    lossbuf[...] = jnp.zeros_like(lossbuf)

    def qkv_out(m):
        return pltpu.make_async_copy(qkvbuf.at[I0], qkv_s.at[m], big_sem.at[I0])

    def up_out(m):
        return pltpu.make_async_copy(ubuf.at[I0], u_s.at[m], big_sem.at[I1])

    def act_out(m):
        return pltpu.make_async_copy(abuf.at[m], a_s.at[m], save_sem.at[I2])

    def hop_forward(m):
        return remote(obuf.at[m % I2], abuf.at[m], hop_f.at[m % I2], act_sem.at[m], place.chain(I1))

    def near_hand(src, dst_far, dst_own, sem, recv_sem):
        return (lambda: remote(src, dst_far, sem, recv_sem, place.sibling)), (lambda: pltpu.make_async_copy(src, dst_own, sem))

    def hand_out(m):
        return near_hand(obuf.at[m % I2], oa_other.at[m], oa_same.at[m], keep_sem.at[m % I2], ao_sem)

    def both_kinds(condition, copies, start):
        far_copy, own_copy = copies

        @pl.when(condition & place.is_l)
        def _():
            far_copy().start() if start else far_copy().wait_send()

        @pl.when(condition & is_r)
        def _():
            own_copy().start() if start else own_copy().wait()

    def forward_tick(m, carry):
        act, mid, out = abuf.at[m], hbuf, obuf.at[m % I2]
        pltpu.make_async_copy(x_ref.at[m, place.core], act, act_sem.at[m]).wait()
        act_out(m).start()

        @pl.when(place.is_l)
        def _():
            pltpu.make_async_copy(act, oa_same.at[m], as_sem).start()

        @pl.when(is_last)
        def _():
            pltpu.make_async_copy(y_ref.at[m, place.core], ybuf, y_sem).start()
        norm_rows(act, gains[I0:I1, :], nbuf, seq)

        @pl.when(m > I0)
        def _():
            qkv_out(m).wait()

        def qkv_step(j, c):
            w = sn.wait(m * 12 + j)
            for n in range(I0, CHUNK, SUB):
                qkvbuf[I0, :, lanes(j * CHUNK + n, SUB)] = mm(nbuf[...], w[:, n:n + SUB]).astype(BF)
            sn.start(m * 12 + j + DEPTH)
            return c
        lax.fori_loop(I0, I6, qkv_step, I0)
        qkv_out(m).start()
        act_out(m).wait()

        @pl.when(is_r)
        def _():
            remote(a_s.at[m], oa_other.at[m], bulk.at[I0], ao_sem, place.sibling).start()

        def head_step(i, c):
            for r in range(I4):
                base = (i // I2) * (I3 * half) + ((i % I2) * I4 + r) * HEAD_PAD
                q = qkvbuf[I0, :, lanes(base, HEAD_PAD)]
                k = qkvbuf[I0, :, lanes(base + half, HEAD_PAD)]
                v = qkvbuf[I0, :, lanes(base + I2 * half, HEAD_PAD)]
                probs = causal_probs(q, k, scale).astype(BF)
                ctxbuf[:, lanes((i * I4 + r) * HEAD_PAD, HEAD_PAD)] = mm(probs, v).astype(BF)
            return c
        lax.fori_loop(I0, heads // I4, head_step, I0)

        w0, w1 = sk.wait(m * I2), sk.wait(m * I2 + I1)
        for n in range(I0, width, SUB):
            total = mm(ctxbuf[:, I0:half], w0[:, n:n + SUB]) + mm(ctxbuf[:, half:I2 * half], w1[:, n:n + SUB])
            mid[:, n:n + SUB] = (act[:, n:n + SUB].astype(F32) + total).astype(BF)
        sk.start(m * I2 + KDEPTH)
        sk.start(m * I2 + I1 + KDEPTH)
        saved(h_s.at[m], I0).start()

        @pl.when(place.is_l)
        def _():
            saved(oh_same.at[m], I1).start()
        norm_rows(mid, gains[I1:I2, :], nbuf, seq)

        @pl.when(m > I0)
        def _():
            up_out(m).wait()
        acc[...] = jnp.zeros_like(acc)

        def mlp_step(j, c):
            w = sn.wait(m * 12 + I6 + j)
            for n in range(I0, CHUNK, SUB):
                u = mm(nbuf[...], w[:, n:n + SUB]).astype(BF)
                ubuf[I0, :, lanes(j * CHUNK + n, SUB)] = u
                uf = u.astype(F32)
                zbuf[:, n:n + SUB] = (uf * gelu_gate(uf)[I0]).astype(BF)
            sn.start(m * 12 + I6 + j + DEPTH)

            @pl.when(m == I0)
            def _():
                resident_ready(j)
            for n in range(I0, width, SUB):
                acc[:, n:n + SUB] += mm(zbuf[...], wres[j, :, n:n + SUB])
            return c
        lax.fori_loop(I0, I6, mlp_step, I0)
        up_out(m).start()

        @pl.when((m > I1) & jnp.logical_not(is_last))
        def _():
            hop_forward(m).wait_send()

        both_kinds((m > I1) & home02, hand_out(m), False)

        def finish(rows):
            out[rows, :] = (mid[rows, :].astype(F32) + acc[rows, :]).astype(BF)
        rows_loop(seq, 32, finish)

        @pl.when(jnp.logical_not(is_last))
        def _():
            hop_forward(m).start()

        both_kinds(home02, hand_out(m), True)

        @pl.when(is_last)
        def _():
            pltpu.make_async_copy(y_ref.at[m, place.core], ybuf, y_sem).wait()

            def seed(rows):
                error = out[rows, :].astype(F32) - ybuf[rows, :].astype(F32)
                gbuf[m, rows, :] = (error * norm_factor).astype(BF)
                lossbuf[...] += jnp.sum((error * error).reshape(I4, I8, width), axis=I0)
            rows_loop(seq, 32, seed)

        saved(h_s.at[m], I0).wait()

        @pl.when(place.is_l)
        def _():
            saved(oh_same.at[m], I1).wait()
            remote(h_s.at[m], oh_same.at[m], bulk.at[I2], os_sem, place.across).start()

        @pl.when(is_r)
        def _():
            remote(h_s.at[m], oh_other.at[m], bulk.at[I2], oo_sem, place.sibling).start()
            remote(h_s.at[m], oh_other.at[m], bulk.at[I3], oo_sem, place.across_other).start()

        @pl.when(is_last & place.is_l)
        def _():
            remote(gbuf.at[m], og_same.at[m], bulk.at[I4], gs_sem, place.across).start()

        @pl.when(is_last & is_r)
        def _():
            remote(gbuf.at[m], og_other.at[m], bulk.at[I4], go_sem, place.across_other).start()
        return carry

    lax.fori_loop(I0, micro, forward_tick, I0)

    @pl.when(is_last)
    def _():
        total = lossbuf[:, I0:128]
        for n in range(128, width, 128):
            total = total + lossbuf[:, n:n + 128]
        losstile[...] = total
        pltpu.make_async_copy(losstile, loss_all.at[place.core], tiny.at[5]).start()
        for index, copy in enumerate(place.others(losstile, loss_all.at[place.core], loss_send, tiny.at[5])):
            copy.start()
    for copy in (qkv_out(micro - I1), up_out(micro - I1)):
        copy.wait()

    @pl.when(jnp.logical_not(is_last))
    def _():
        for m in (micro - I2, micro - I1):
            hop_forward(m).wait_send()
    for m in (micro - I2, micro - I1):
        both_kinds(home02, hand_out(m), False)

    bn = Stream(wn, stream_n, DEPTH, [([(None, td0)], I3), ([(None, td1)], I3), ([(None, to0)], I1), ([(None, to1)], I1)], micro * I8, False)
    bk = Stream(wk, stream_k, KDEPTH, [(near_of(I0), I3), ([(None, fq)], I3)], micro * I6, True)
    bn.prime()
    bk.prime()
    resident(([(None, tu0)], [(None, tu1)]), True)

    def loads(i):
        m = micro - I1 - i
        slot = i % I2
        return (pltpu.make_async_copy(u_s.at[m], ubuf.at[slot], load_sem.at[I0, slot]),
                pltpu.make_async_copy(qkv_s.at[m], qkvbuf.at[slot], load_sem.at[I1, slot]),
                pltpu.make_async_copy(h_s.at[m], habuf.at[slot, I0], load_sem.at[I2, slot]),
                pltpu.make_async_copy(a_s.at[m], habuf.at[slot, I1], load_sem.at[I3, slot]))

    for copy in loads(I0):
        copy.start()
    accg[...] = jnp.zeros_like(accg)

    def norm_back(index, x, base, dst, gain_row):
        def body(rows):
            xf = x[rows, :].astype(F32)
            dy = acc[rows, :].astype(BF).astype(F32)
            inv = lax.rsqrt(jnp.mean(xf * xf, axis=-I1, keepdims=True) + NORM_EPS)
            xn = xf * inv
            accg[index] += jnp.sum((dy * xn).reshape(I4, I8, width), axis=I0)
            dyg = dy * gain_row
            dx = inv * (dyg - xn * jnp.mean(dyg * xn, axis=-I1, keepdims=True))
            dst[rows, :] = (base[rows, :].astype(F32) + dx).astype(BF)
        rows_loop(seq, 32, body)

    def hop_back(i):
        m = micro - I1 - i
        return remote(obuf.at[i % I2], gbuf.at[m], hop_b.at[i % I2], grad_sem.at[m], place.chain(-I1))

    def hand_back(i):
        m = micro - I1 - i
        return near_hand(obuf.at[i % I2], og_other.at[m], og_same.at[m], back_sem.at[i % I2], go_sem)

    def keep_dx(i):
        return pltpu.make_async_copy(obuf.at[i % I2], dx_s.at[micro - I1 - i], back_sem.at[i % I2])

    def back_ready(i):
        both_kinds((i > I1) & home13, hand_back(i), False)

        @pl.when((i > I1) & is_first)
        def _():
            keep_dx(i).wait()

        @pl.when((i > I1) & jnp.logical_not(is_first))
        def _():
            hop_back(i).wait_send()

    def backward_tick(i, carry):
        m = micro - I1 - i
        slot = i % I2
        grad, dmid, prev = gbuf.at[m], hbuf, obuf.at[slot]
        u_now, qkv_now, h_now, a_now = ubuf.at[slot], qkvbuf.at[slot], habuf.at[slot, I0], habuf.at[slot, I1]

        @pl.when(i + I1 < micro)
        def _():
            for copy in loads(i + I1):
                copy.start()

        @pl.when(jnp.logical_not(is_last))
        def _():
            remote(grad, grad, hop_b.at[slot], grad_sem.at[m], place.sibling).wait_recv()

        @pl.when(place.is_l)
        def _():
            pltpu.make_async_copy(grad, og_same.at[m], gs_sem).start()

        @pl.when(is_r)
        def _():
            remote(grad, og_other.at[m], bulk.at[5], go_sem, place.sibling).start()
        load_u, load_qkv, load_h, load_a = loads(i)
        load_u.wait()
        acc[...] = jnp.zeros_like(acc)

        def mlp_step(j, c):
            w = bn.wait(i * I8 + j)
            for n in range(I0, CHUNK, SUB):
                dz = mm(grad[...], w[:, n:n + SUB]).astype(BF).astype(F32)
                u = u_now[:, lanes(j * CHUNK + n, SUB)].astype(F32)
                gate, u2 = gelu_gate(u)
                zbuf[:, n:n + SUB] = (dz * gelu_slope(u * gate, gate, u2)).astype(BF)
            bn.start(i * I8 + j + DEPTH)

            @pl.when(i == I0)
            def _():
                resident_ready(j)
            for n in range(I0, width, SUB):
                acc[:, n:n + SUB] += mm(zbuf[...], wres[j, :, n:n + SUB])
            return c
        lax.fori_loop(I0, I6, mlp_step, I0)
        load_h.wait()
        norm_back(I1, h_now, grad, dmid, gains[I1:I2, :])

        @pl.when(place.is_l)
        def _():
            saved(od_same.at[m], I0).start()

        @pl.when(is_r)
        def _():
            saved(m_s.at[m], I0).start()
        for c in range(I2):
            w = bn.wait(i * I8 + I6 + c)
            for n in range(I0, CHUNK, SUB):
                ctxbuf[:, c * CHUNK + n:c * CHUNK + n + SUB] = mm(dmid[...], w[:, n:n + SUB]).astype(BF)
            bn.start(i * I8 + I6 + c + DEPTH)
        load_qkv.wait()

        def head_step(t, c):
            for r in range(I2):
                base = (t // I4) * (I3 * half) + ((t % I4) * I2 + r) * HEAD_PAD
                q = qkv_now[:, lanes(base, HEAD_PAD)]
                k = qkv_now[:, lanes(base + half, HEAD_PAD)]
                v = qkv_now[:, lanes(base + I2 * half, HEAD_PAD)]
                dc = ctxbuf[:, lanes((t * I2 + r) * HEAD_PAD, HEAD_PAD)]
                _, dq, dk, dv = attention_backward(q, k, v, dc, scale)
                dqkvbuf[:, lanes(base, HEAD_PAD)] = dq
                dqkvbuf[:, lanes(base + half, HEAD_PAD)] = dk
                dqkvbuf[:, lanes(base + I2 * half, HEAD_PAD)] = dv
            return c
        lax.fori_loop(I0, heads // I2, head_step, I0)
        acc[...] = jnp.zeros_like(acc)

        def qkv_step(j, c):
            w = bk.wait(i * I6 + j)
            for n in range(I0, width, SUB):
                acc[:, n:n + SUB] += mm(dqkvbuf[:, lanes(j * CHUNK, CHUNK)], w[:, n:n + SUB])
            bk.start(i * I6 + j + KDEPTH)
            return c
        lax.fori_loop(I0, I6, qkv_step, I0)
        load_a.wait()
        back_ready(i)
        norm_back(I0, a_now, dmid, prev, gains[I0:I1, :])

        @pl.when(jnp.logical_not(is_first))
        def _():
            hop_back(i).start()

        @pl.when(is_first)
        def _():
            keep_dx(i).start()
        both_kinds(home13, hand_back(i), True)

        @pl.when(place.is_l)
        def _():
            saved(od_same.at[m], I0).wait()
            remote(od_same.at[m], od_same.at[m], bulk.at[I6], ds_sem, place.across).start()

        @pl.when(is_r)
        def _():
            saved(m_s.at[m], I0).wait()
            remote(m_s.at[m], od_other.at[m], bulk.at[I6], do_sem, place.sibling).start()
            remote(m_s.at[m], od_other.at[m], bulk.at[7], do_sem, place.across_other).start()

        @pl.when((place.home == I2) & place.is_l)
        def _():
            remote(a_s.at[m], oa_same.at[m], bulk.at[I8], as_sem, place.across).start()

        @pl.when((place.home == I2) & is_r)
        def _():
            remote(a_s.at[m], oa_other.at[m], bulk.at[I8], ao_sem, place.across_other).start()
        far_grad(m, (place.home == I1) & (i % I2 == I0))
        return carry

    def far_grad(m, condition):
        @pl.when(condition & place.is_l)
        def _():
            remote(gbuf.at[m], og_same.at[m], bulk.at[I4], gs_sem, place.across).start()

        @pl.when(condition & is_r)
        def _():
            remote(gbuf.at[m], og_other.at[m], bulk.at[I4], go_sem, place.across_other).start()

    lax.fori_loop(I0, micro, backward_tick, I0)
    for i in range(I1, micro, I2):
        far_grad(micro - I1 - i, place.home == I1)

    @pl.when(place.is_l)
    def _():
        pltpu.make_async_copy(accg, dg_same, tiny.at[I0]).start()
        remote(accg, dg_same, tiny.at[I1], tiny.at[I0], place.across).start()

    @pl.when(is_r)
    def _():
        remote(accg, dg_other, tiny.at[I1], tiny.at[I4], place.sibling).start()
        remote(accg, dg_other, tiny.at[I2], tiny.at[I4], place.across_other).start()

    for i in (micro - I2, micro - I1):
        back_ready(jnp.int32(i))

    def sent(buf, sem):
        remote(buf, a_s, sem, ao_sem, place.sibling).wait_send()

    def got(dst, sem):
        pltpu.make_async_copy(dst, dst, sem).wait()

    sent(h_s, bulk.at[I2])
    sent(m_s, bulk.at[I6])

    @pl.when(is_r)
    def _():
        sent(a_s, bulk.at[I0])
        sent(h_s, bulk.at[I3])
        sent(gbuf, bulk.at[5])
        sent(m_s, bulk.at[7])
        remote(accg, dg_other, tiny.at[I2], tiny.at[I4], place.sibling).wait_send()

    @pl.when(home13)
    def _():
        sent(gbuf, bulk.at[I4])

    @pl.when(place.home == I2)
    def _():
        sent(a_s, bulk.at[I8])

    @pl.when(is_last)
    def _():
        for copy in place.others(losstile, loss_all.at[place.core], loss_send, tiny.at[5]):
            copy.wait_send()
    remote(accg, dg_other, tiny.at[I1], tiny.at[I4], place.sibling).wait_send()
    got(oh_other, oo_sem)
    got(od_other, do_sem)
    got(og_other, go_sem)
    got(dg_same, tiny.at[I0])
    got(dg_other, tiny.at[I4])
    got(loss_all, tiny.at[5])

    @pl.when(is_r)
    def _():
        got(oh_same, os_sem)
        got(od_same, ds_sem)

    @pl.when(place.is_l | home02)
    def _():
        got(og_same, gs_sem)

    @pl.when(place.is_l | (place.home == I3))
    def _():
        got(oa_same, as_sem)

    @pl.when(place.is_l | (place.home != I1))
    def _():
        got(oa_other, ao_sem)


def step_phase(dims, x, y, own, own_gains):
    micro, seq, width, heads, head_dim, ffn = dims
    half = heads // I2 * HEAD_PAD
    act = (micro, seq, width)
    raw = [(heads // I2 * I3 * head_dim, width), (heads // I2 * head_dim, width), (width, ffn // I2), (ffn // I2, width)]
    turned = [(width, I3 * half), (width, half), (ffn // I2, width), (width, ffn // I2)]
    outs = [act, act, act, (micro, seq, I6 * half), (micro, seq, ffn), act] + [act] * I8
    out_shape = [jax.ShapeDtypeStruct(s, BF) for s in outs]
    out_shape += [jax.ShapeDtypeStruct(s, F32) for s in ((I2, I8, width), (I2, I8, width), (I2, I8, 128))]
    out_shape += [jax.ShapeDtypeStruct(s, BF) for s in raw + raw + turned + turned]
    any_spec = pl.BlockSpec(memory_space=ANY)
    vmem, dma = pltpu.VMEM, pltpu.SemaphoreType.DMA
    scratch = [
        vmem(act, BF), vmem(act, BF), vmem((seq, width), BF), vmem((I2, seq, width), BF), vmem((seq, width), BF), vmem((seq, width), BF),
        vmem((I2, seq, I6 * half), BF), vmem((I2, seq, ffn), BF), vmem((I2, I2, seq, width), BF), vmem((seq, CHUNK), BF), vmem((seq, I2 * half), BF),
        vmem((seq, I6 * half), BF), vmem((seq, width), F32), vmem((I2, I8, width), F32), vmem((I8, width), F32), vmem((I8, 128), F32),
        vmem((I2, width), F32), vmem((I6, CHUNK, width), BF), vmem((DEPTH, width, CHUNK), BF), vmem((KDEPTH, CHUNK, width), BF),
        dma((I4,)), dma((I4,)), dma((I4,)), dma((I4,)), dma((12,)), dma((I2,)), dma((I2,)),
        dma((micro,)), dma((micro,)), dma((I2,)), dma((I2,)), dma((I2,)), dma((I2,)), dma((I3,)), dma((DEPTH,)), dma((KDEPTH,)), dma((I6,)), dma((I2,)),
        dma((I4, I2)), dma(()),
        dma(()), dma(()), dma(()), dma(()), dma(()), dma(()), dma(()), dma(()), dma((9,)), dma((I2,)), dma((I6,)), dma((7,)),
    ]
    return pl.pallas_call(
        functools.partial(step_kernel, dims),
        out_shape=tuple(out_shape),
        in_specs=[any_spec] * I6 + [pl.BlockSpec(memory_space=vmem)],
        out_specs=(any_spec,) * len(out_shape),
        scratch_shapes=scratch,
        compiler_params=pltpu.CompilerParams(collective_id=I0, has_side_effects=True, vmem_limit_bytes=VMEM_LIMIT),
        name='step_phase',
    )(x, y, *own, own_gains)


TOKENS = 512


def bring(pairs, sem):
    copies = [pltpu.make_async_copy(src, dst, sem.at[i]) for i, (src, dst) in enumerate(pairs)]
    for copy in copies:
        copy.start()
    return copies


def turn_into(dst, src, rows, cols):
    for r in range(I0, rows, SUB):
        for c in range(I0, cols, SUB):
            high, wide = min(SUB, rows - r), min(SUB, cols - c)
            dst[c:c + wide, r:r + high] = src[r:r + high, c:c + wide].T


def spread_dx(step, last, dx, d_in, here_sem, parent_sem, sib_sem, send_sems):
    place = Place()
    micro = dx.shape[I0]
    below = place.at(place.tp, (place.stage + I2) % I4)
    barrier = pltpu.get_barrier_semaphore()
    is_a, is_b = place.home == I0, place.home == I1
    is_leaf = place.home > I1

    def block(m):
        return d_in.at[m, place.core]

    def hand(m, src, index, there):
        remote(src, block(m), send_sems.at[index], sib_sem if index == I0 else parent_sem.at[m], there).start()

    def arrived(m):
        remote(block(m), block(m), send_sems.at[I0], parent_sem.at[m], place.sibling).wait_recv()

    @pl.when(step == I0)
    def _():
        def tell(there):
            pl.semaphore_signal(barrier, inc=I1, device_id=there, device_id_type=MESH)
        tell(place.sibling)

        @pl.when(is_b)
        def _():
            tell(place.across)

        @pl.when(is_leaf)
        def _():
            tell(below)

    @pl.when((step == I1) & is_a)
    def _():
        pl.semaphore_wait(barrier, I3)
        for m in reversed(range(micro)):
            hand(m, dx.at[m], I1, place.across)
            hand(m, dx.at[m], I2, below)
            hand(m, dx.at[m], I0, place.sibling)
            pltpu.make_async_copy(dx.at[m], block(m), here_sem).start()

    @pl.when((step == I2) & is_b)
    def _():
        pl.semaphore_wait(barrier, I2)

    @pl.when((step > I2) & (step < I3 + micro) & is_b)
    def _():
        m = micro + I2 - step
        arrived(m)
        hand(m, block(m), I2, below)
        hand(m, block(m), I0, place.sibling)

    @pl.when((step == last) & is_leaf)
    def _():
        pl.semaphore_wait(barrier, I1)
        for m in reversed(range(micro)):
            arrived(m)
            hand(m, block(m), I0, place.sibling)

    @pl.when(step == last)
    def _():
        def sent(index):
            remote(dx, dx, send_sems.at[index], sib_sem, place.sibling).wait_send()
        sent(I0)

        @pl.when(is_a)
        def _():
            sent(I1)
            pltpu.make_async_copy(dx, dx, here_sem).wait()

        @pl.when(jnp.logical_not(is_leaf))
        def _():
            sent(I2)
        remote(dx, dx, send_sems.at[I0], sib_sem, place.sibling).wait_recv()


def owner_mlp_kernel(dx, hs, ho, gs, go, gain, wu, wd, dwu, dwd, d_in, n2, n2t, grad, wdt, z, zt, dup, sem, here_sem, parent_sem, sib_sem, send_sems):
    tokens, width = n2.shape
    part = tokens // I2
    spread_dx(pl.program_id(I0), pl.num_programs(I0) - I1, dx, d_in, here_sem, parent_sem, sib_sem, send_sems)

    @pl.when(pl.program_id(I0) == I0)
    def _():
        low, high = pl.ds(I0, part), pl.ds(part, part)
        for copy in bring([(hs, n2.at[low]), (ho, n2.at[high]), (gs, grad.at[low]), (go, grad.at[high])], sem):
            copy.wait()

        def prepare(rows):
            norm_rows(n2.at[rows], gain[...], n2.at[rows], SUB)
            for c in range(I0, width, SUB):
                n2t[c:c + SUB, rows] = n2[rows, c:c + SUB].T
        rows_loop(tokens, SUB, prepare)
    turn_into(wdt, wd, SUB, width)

    def front(rows):
        u = mm(n2[rows, :], wu[...]).astype(BF).astype(F32)
        dz = mm(grad[rows, :], wdt[...]).astype(BF).astype(F32)
        gate, u2 = gelu_gate(u)
        hidden = u * gate
        z[rows, :] = hidden.astype(BF)
        dup[rows, :] = (dz * gelu_slope(hidden, gate, u2)).astype(BF)
    rows_loop(tokens, TOKENS, front)
    turn_into(zt, z, tokens, SUB)
    for c in range(I0, width, TOKENS):
        dwu[c:c + TOKENS, :] = mm(n2t[c:c + TOKENS, :], dup[...])
    for c in range(I0, width, SUB):
        dwd[:, c:c + SUB] = mm(zt[...], grad[:, c:c + SUB])


def owner_mlp(dx, h_rows, g_rows, gain, w_up, w_down):
    width, ffn = w_up.shape
    part, micro = h_rows[I0].shape[I0], dx.shape[I0]
    vmem, dma = pltpu.VMEM, pltpu.SemaphoreType.DMA
    any_spec = pl.BlockSpec(memory_space=ANY)
    up_spec = pl.BlockSpec((width, SUB), lambda i: (I0, i))
    down_spec = pl.BlockSpec((SUB, width), lambda i: (i, I0))
    rows = lambda n: vmem((I2 * part, n), BF)
    return pl.pallas_call(
        owner_mlp_kernel,
        grid=(ffn // SUB,),
        out_shape=(jax.ShapeDtypeStruct(w_up.shape, F32), jax.ShapeDtypeStruct(w_down.shape, F32), jax.ShapeDtypeStruct((micro, I2) + dx.shape[I1:], BF)),
        in_specs=[any_spec] * 5 + [pl.BlockSpec(memory_space=vmem), up_spec, down_spec],
        out_specs=(up_spec, down_spec, any_spec),
        scratch_shapes=[rows(width), vmem((width, I2 * part), BF), rows(width), vmem((width, SUB), BF), rows(SUB), vmem((SUB, I2 * part), BF), rows(SUB), dma((I4,)), dma(()), dma((micro,)), dma(()), dma((I3,))],
        compiler_params=pltpu.CompilerParams(collective_id=I1, has_side_effects=True, vmem_limit_bytes=VMEM_LIMIT),
        cost_estimate=pl.CostEstimate(flops=16 * part * width * ffn, bytes_accessed=12 * width * ffn, transcendentals=I2 * part * ffn),
        name='owner_mlp',
    )(dx, *h_rows, *g_rows, gain, w_up, w_down)


def owner_attn_kernel(seq, x_ref, rs, ro, ds, do, gain, wq, wo, dwq, dwo, n1, dmid, wpad, wqt, wot, qkv, dctx, dqkv, ctx, dqkvt, ctxt, sem):
    tokens, width = n1.shape
    part = tokens // I2
    head_dim = wo.shape[I1]
    scale = head_dim ** -0.5
    pair = I2 * HEAD_PAD

    @pl.when(pl.program_id(I0) == I0)
    def _():
        place = Place()
        from_x = (place.home == I1) & jnp.logical_not(place.is_l)
        low, high = pl.ds(I0, part), pl.ds(part, part)
        d_copies = bring([(ds, dmid.at[low]), (do, dmid.at[high])], sem)
        a_pairs = [(rs, n1.at[low]), (ro, n1.at[high])]
        a_sem = sem.at[I2:I4]

        @pl.when(from_x)
        def _():
            for m in range(part // seq):
                for first, core in ((I0, place.core), (part, I1 - place.core)):
                    pltpu.make_async_copy(x_ref.at[m, core], n1.at[pl.ds(first + m * seq, seq)], a_sem.at[min(first, I1)]).start()

        @pl.when(jnp.logical_not(from_x))
        def _():
            bring(a_pairs, a_sem)
        wpad[...] = jnp.zeros_like(wpad)
        for i, (src, dst) in enumerate(a_pairs):
            pltpu.make_async_copy(src, dst, a_sem.at[i]).wait()
        norm_rows(n1, gain[...], n1, tokens)
        for copy in d_copies:
            copy.wait()
    for r in range(I2):
        for t in range(I3):
            wpad[I0:head_dim, :] = wq[t, r]
            at = t * pair + r * HEAD_PAD
            turn_into(wqt.at[:, at:at + HEAD_PAD], wpad, HEAD_PAD, width)
        wpad[I0:head_dim, :] = wo[r]
        turn_into(wot.at[:, r * HEAD_PAD:(r + I1) * HEAD_PAD], wpad, HEAD_PAD, width)

    def front(rows):
        for n in range(I0, I3 * pair, pair):
            qkv[rows, n:n + pair] = mm(n1[rows, :], wqt[:, n:n + pair]).astype(BF)
        dctx[rows, :] = mm(dmid[rows, :], wot[...]).astype(BF)
    rows_loop(tokens, TOKENS, front)

    def sequence(rows):
        for r in range(I2):
            q_at, k_at, v_at = [slice(t * pair + r * HEAD_PAD, t * pair + (r + I1) * HEAD_PAD) for t in range(I3)]
            v, dc = qkv[rows, v_at], dctx[rows, q_at]
            probs, dq, dk, dv = attention_backward(qkv[rows, q_at], qkv[rows, k_at], v, dc, scale)
            ctx[rows, q_at] = mm(probs, v).astype(BF)
            dqkv[rows, q_at], dqkv[rows, k_at], dqkv[rows, v_at] = dq, dk, dv
    rows_loop(tokens, seq, sequence)

    def turn(rows):
        for t in range(I6):
            dqkvt[t * head_dim:(t + I1) * head_dim, rows] = dqkv[rows, t * HEAD_PAD:(t + I1) * HEAD_PAD].T[I0:head_dim]
        for t in range(I2):
            ctxt[t * head_dim:(t + I1) * head_dim, rows] = ctx[rows, t * HEAD_PAD:(t + I1) * HEAD_PAD].T[I0:head_dim]
    rows_loop(tokens, SUB, turn)
    for c in range(I0, width, SUB):
        cut = slice(c, c + SUB)
        dwq[:, :, :, cut] = mm(dqkvt[...], n1[:, cut]).reshape(I3, I2, head_dim, SUB)
        dwo[:, :, cut] = mm(ctxt[...], dmid[:, cut]).reshape(I2, head_dim, SUB)


def owner_attn(seq, x, a_rows, d_rows, gain, w_qkv, w_out):
    heads, head_dim, width = w_out.shape
    part = a_rows[I0].shape[I0]
    vmem = pltpu.VMEM
    any_spec = pl.BlockSpec(memory_space=ANY)
    q_spec = pl.BlockSpec((I3, I2, head_dim, width), lambda i: (I0, i, I0, I0))
    o_spec = pl.BlockSpec((I2, head_dim, width), lambda i: (i, I0, I0))
    rows = lambda n: vmem((I2 * part, n), BF)
    pair = I2 * HEAD_PAD
    return pl.pallas_call(
        functools.partial(owner_attn_kernel, seq),
        grid=(heads // I2,),
        out_shape=(jax.ShapeDtypeStruct(w_qkv.shape, F32), jax.ShapeDtypeStruct(w_out.shape, F32)),
        in_specs=[any_spec] * 5 + [pl.BlockSpec(memory_space=vmem), q_spec, o_spec],
        out_specs=(q_spec, o_spec),
        scratch_shapes=[
            rows(width), rows(width), vmem((HEAD_PAD, width), BF), vmem((width, I3 * pair), BF), vmem((width, pair), BF),
            rows(I3 * pair), rows(pair), rows(I3 * pair), rows(pair), vmem((I6 * head_dim, I2 * part), BF), vmem((I2 * head_dim, I2 * part), BF),
            pltpu.SemaphoreType.DMA((I4,)),
        ],
        compiler_params=pltpu.CompilerParams(vmem_limit_bytes=VMEM_LIMIT),
        cost_estimate=pl.CostEstimate(flops=36 * part * width * heads * head_dim, bytes_accessed=16 * width * width, transcendentals=part * heads * seq),
        name='owner_attn',
    )(x, *a_rows, *d_rows, gain, w_qkv, w_out)


def solution(mesh):
    act_spec = P('rep', None, None, None)
    weight_specs = (
        P(('rep', 'stage'), None, None, 'tp', None),
        P(('rep', 'stage'), 'tp', None, None),
        P(('rep', 'stage'), None, 'tp'),
        P(('rep', 'stage'), 'tp', None),
        P(('rep', 'stage'), None),
        P(('rep', 'stage'), None),
    )

    def device_fn(inputs, targets, w_qkv, w_out, w_up, w_down, gain_attn, gain_mlp):
        micro_count, _, seq_len, width = inputs.shape
        dims = (micro_count, seq_len, width, I2 * w_out.shape[I1], w_out.shape[I2], I2 * w_up.shape[I2])
        norm_factor = 1.0 / (inputs.size)
        own = (w_qkv[I0], w_out[I0], w_up[I0], w_down[I0])
        own_gains = jnp.concatenate([gain_attn, gain_mlp]).astype(F32)
        rows_of = (own[I0].transpose(I1, I2, I3, I0).reshape(-I1, width), own[I1].reshape(-I1, width), own[I2], own[I3])

        results = step_phase(dims, inputs, targets, rows_of, own_gains)
        dx, oh_same, oh_other, oa_same, oa_other, od_same, od_other, og_same, og_other, dg_same, dg_other, loss_all = results[5:17]

        flat = lambda *rows: [r.reshape(-I1, width) for r in rows]
        w_rows = own[I0].transpose(I1, I2, I3, I0)
        d_qkv, d_out = owner_attn(seq_len, inputs, flat(oa_same, oa_other), flat(od_same, od_other), own_gains[:I1], w_rows, own[I1])
        d_up, d_down, d_inputs = owner_mlp(dx, flat(oh_same, oh_other), flat(og_same, og_other), own_gains[I1:], own[I2], own[I3])
        weight_grads = (d_qkv.transpose(I3, I0, I1, I2), d_out, d_up, d_down)
        mine = jnp.sum(dg_same + dg_other, I1)
        loss = jnp.sum(loss_all) * (0.5 * norm_factor)

        return (loss.reshape(I1), d_inputs) + tuple(g[None] for g in weight_grads) + (mine[I0][None], mine[I1][None])

    return jax.shard_map(device_fn, mesh=mesh, in_specs=(act_spec, act_spec) + weight_specs, out_specs=(P('rep'), act_spec) + weight_specs, check_vma=False)
```

```python
import functools

import jax
import jax.numpy as jnp
from jax import lax
from jax.experimental import pallas as pl
from jax.experimental.pallas import tpu as pltpu
from jax.sharding import PartitionSpec as P

NORM_EPS = 1e-5
BF = jnp.bfloat16
F32 = jnp.float32
MESH = pl.DeviceIdType.MESH
ANY = pl.ANY


GELU_A = 0.7978845608028654
GELU_B = 0.044715
I0, I1, I2, I3, I4, I6, I8 = 0, 1, 2, 3, 4, 6, 8
CHUNK = 1024
BLOCK = 384
SUB = 256
DEPTH = 6
BACK_DEPTH = 4
KDEPTH = 2
HEAD_PAD = 128
VMEM_LIMIT = 67043328


def mm(a, b):
    return lax.dot_general(a, b, (((I1,), (I0,)), ((), ())), preferred_element_type=F32)


def mm_nt(a, b):
    return lax.dot_general(a, b, (((I1,), (I1,)), ((), ())), preferred_element_type=F32)


def mm_tn(a, b):
    return lax.dot_general(a, b, (((I0,), (I0,)), ((), ())), preferred_element_type=F32)


class Place:
    def __init__(self):
        self.tp = lax.axis_index('tp')
        self.stage = lax.axis_index('stage')
        self.core = self.stage % I2
        self.x_pos = self.stage // I2
        self.home = self.x_pos * (I3 - I2 * self.tp) + self.tp
        self.is_l = self.stage == self.home
        self.sib = self.stage + I1 - I2 * self.core

    def at(self, tp, stage):
        return {'tp': tp, 'stage': stage}

    @property
    def sibling(self):
        return self.at(self.tp, self.sib)

    @property
    def across(self):
        return self.at(I1 - self.tp, self.stage)

    @property
    def across_other(self):
        return self.at(I1 - self.tp, self.sib)

    def others(self, src, dst, send_sems, recv_sem):
        copies = []
        for d_tp in (I0, I1):
            for d_stage in range(I4):
                if d_tp or d_stage:
                    there = self.at(self.tp + d_tp - I2 * d_tp * self.tp, (self.stage + d_stage) % I4)
                    copies.append(remote(src, dst, send_sems.at[len(copies)], recv_sem, there))
        return copies

    def chain(self, delta):
        there = self.home + delta
        x_pos = there // I2
        tp = there % I2 + x_pos * (I1 - I2 * (there % I2))
        return self.at(tp, I2 * x_pos + self.core)


def entry_barrier(place):
    barrier = pltpu.get_barrier_semaphore()
    for d_tp in (I0, I1):
        for d_stage in range(I4):
            if d_tp or d_stage:
                tp = place.tp + d_tp - I2 * d_tp * place.tp
                stage = (place.stage + d_stage) % I4
                pl.semaphore_signal(barrier, inc=I1, device_id=place.at(tp, stage), device_id_type=MESH)
    pl.semaphore_wait(barrier, 7)


def remote(src, dst, send_sem, recv_sem, device_id):
    return pltpu.make_async_remote_copy(src_ref=src, dst_ref=dst, send_sem=send_sem, recv_sem=recv_sem, device_id=device_id, device_id_type=MESH)


def rows_loop(total, step, body):
    def run(i, carry):
        body(pl.ds(pl.multiple_of(i * step, step), step))
        return carry
    lax.fori_loop(I0, total // step, run, I0)


def norm_rows(src, gain_row, dst, total):
    def body(rows):
        v = src[rows, :].astype(F32)
        inv = lax.rsqrt(jnp.mean(v * v, axis=-I1, keepdims=True) + NORM_EPS)
        dst[rows, :] = (v * inv * gain_row).astype(BF)
    rows_loop(total, 32, body)


def gelu_gate(u):
    u2 = u * u
    t = jnp.tanh(u * (GELU_A + (GELU_A * GELU_B) * u2))
    return 0.5 * t + 0.5, u2


def gelu_slope(hidden, gate, u2):
    return gate + hidden * (1.0 - gate) * (2.0 * GELU_A + (6.0 * GELU_A * GELU_B) * u2)


def row_parts(heads, cut=128):
    return [(*(x[low:high] for x in queries), *(x[:high] for x in keys), low)
            for queries, keys in heads for low, high in ((I0, cut), (cut, queries[I0].shape[I0]))]


def softmax_parts(scores, starts):
    masked = []
    for s, start in zip(scores, starts):
        q_pos = lax.broadcasted_iota(jnp.int32, s.shape, I0) + start
        k_pos = lax.broadcasted_iota(jnp.int32, s.shape, I1)
        masked.append(jnp.where(k_pos <= q_pos, s, -1e30))
    tops = [jnp.max(s, axis=-I1, keepdims=True) for s in masked]
    powers = [jnp.exp(s - top) for s, top in zip(masked, tops)]
    scales = [1.0 / jnp.sum(e, axis=-I1, keepdims=True) for e in powers]
    return [e * r for e, r in zip(powers, scales)]


def join_keys(top, low, cut=128):
    return jnp.concatenate([top + low[:cut], low[cut:]], I0).astype(BF)


def attention_forward(heads, scale):
    units = row_parts([((q,), (k, v)) for q, k, v in heads])
    probs = softmax_parts([mm_nt(q, k) * scale for q, k, _, _ in units], [u[-I1] for u in units])
    parts = [mm(p.astype(BF), u[I2]) for p, u in zip(probs, units)]
    return [jnp.concatenate([a, b], I0).astype(BF) for a, b in zip(parts[I0::I2], parts[I1::I2])]


def attention_backward(heads, scale):
    units = row_parts([((q, dc), (k, v)) for q, k, v, dc in heads])
    scores = [mm_nt(q, k) * scale for q, _, k, _, _ in units]
    dps = [mm_nt(dc, v) for _, dc, _, v, _ in units]
    probs = softmax_parts(scores, [u[-I1] for u in units])
    dps = [dp.astype(BF).astype(F32) for dp in dps]
    deltas = [jnp.sum(dp * p, axis=-I1, keepdims=True) for dp, p in zip(dps, probs)]
    dvs = [mm_tn(p.astype(BF), u[I1]) for p, u in zip(probs, units)]
    dss = [p * (dp - delta) * scale for p, dp, delta in zip(probs, dps, deltas)]
    terms = []
    for ds in dss:
        hi = ds.astype(BF)
        rest = ds - hi.astype(F32)
        lo = rest.astype(BF)
        terms.append((hi, lo, (rest - lo.astype(F32)).astype(BF)))
    dqs = [mm(hi, u[I2]) + (mm(lo, u[I2]) + mm(tail, u[I2])) for (hi, lo, tail), u in zip(terms, units)]
    dks = [mm_tn(hi, u[I0]) + (mm_tn(lo, u[I0]) + mm_tn(tail, u[I0])) for (hi, lo, tail), u in zip(terms, units)]
    return [(jnp.concatenate([dqs[i], dqs[i + I1]], I0).astype(BF), join_keys(dks[i], dks[i + I1]), join_keys(dvs[i], dvs[i + I1]))
            for i in range(I0, len(units), I2)]


def lanes(offset, size):
    return pl.ds(pl.multiple_of(offset, 128), size)


def load_resident(buf, sem, halves):
    for c in range(I6):
        for condition, ref in halves[c // I3]:
            copy = pltpu.make_async_copy(ref.at[(c % I3) * CHUNK:(c % I3 + I1) * CHUNK, :], buf.at[c], sem.at[c])
            if condition is None:
                copy.start()
            else:
                pl.when(condition)(copy.start)


def load_heads(ref, index, dst, sem):
    for r in range(I8):
        rows = pl.ds(pl.multiple_of(index * 768 + r * 96, 96), 96)
        pltpu.make_async_copy(ref.at[rows, :], dst.at[r * 128:r * 128 + 96, :], sem).start()


class Stream:
    def __init__(self, buf, sem, depth, parts, total, by_heads):
        self.buf, self.sem, self.depth, self.parts, self.total, self.by_heads = buf, sem, depth, parts, total, by_heads
        self.per_tick = sum(p[I1] for p in parts)

    def copy_in(self, ref, index, slot):
        if not self.by_heads:
            where = pl.ds(pl.multiple_of(index * CHUNK, CHUNK), CHUNK)
            pltpu.make_async_copy(ref.at[:, where], self.buf.at[slot], self.sem.at[slot]).start()
            return
        load_heads(ref, index, self.buf.at[slot], self.sem.at[slot])

    def start(self, seq):
        @pl.when(seq < self.total)
        def _():
            j = seq % self.per_tick
            slot = seq % self.depth
            base = I0
            for choices, chunks in self.parts:
                for condition, ref in choices:
                    here = (j >= base) & (j < base + chunks)
                    here = here if condition is None else here & condition

                    @pl.when(here)
                    def _(ref=ref, low=base):
                        self.copy_in(ref, j - low, slot)
                base += chunks

    def prime(self):
        for seq in range(self.depth):
            self.start(jnp.int32(seq))

    def wait(self, seq):
        slot = seq % self.depth
        ref = self.parts[I0][I0][I0][I1]
        if self.by_heads:
            pltpu.make_async_copy(ref.at[I0:768, :], self.buf.at[slot, I0:768, :], self.sem.at[slot]).wait()
        else:
            pltpu.make_async_copy(ref.at[:, I0:CHUNK], self.buf.at[slot], self.sem.at[slot]).wait()
        return self.buf.at[slot]


PIECES = [(0, 0, 0), (0, 0, 1), (0, 0, 2), (1, 0, 0), (2, 1, 0), (2, 1, 1), (2, 1, 2), (2, 1, 3), (3, 0, 0), (3, 0, 1), (3, 0, 2), (3, 0, 3)]


def piece(ref, axis, index):
    return ref.at[index * 768:(index + I1) * 768, :] if axis == I0 else ref.at[:, index * 768:(index + I1) * 768]


def weight_phase(place, is_r, own, near, far, turned, wn, wk, send_sem, y_send, d_send, near_sem, far_sem, load_sem, store_sem):
    wk[...] = jnp.zeros_like(wk)

    @pl.when(place.is_l)
    def _():
        for i in range(I4):
            remote(own[i], near[i], send_sem.at[i], near_sem.at[i], place.sibling).start()

    @pl.when(is_r)
    def _():
        for c, (i, axis, index) in enumerate(PIECES):
            remote(piece(own[i], axis, index), piece(far[i], axis, index), y_send.at[i], far_sem.at[c], place.across_other).start()

    def load(i, refs, t, slot):
        for condition, ref in refs:
            def go(ref=ref):
                if i < I2:
                    for r in range(I2):
                        rows = pl.ds(pl.multiple_of(t * 192 + r * 96, 96), 96)
                        pltpu.make_async_copy(ref.at[rows, :], wk.at[I0, pl.ds(slot * SUB + r * 128, 96), :], load_sem.at[slot]).start()
                elif i == I2:
                    pltpu.make_async_copy(ref.at[:, lanes(t * SUB, SUB)], wn.at[slot, :, I0:SUB], load_sem.at[slot]).start()
                else:
                    rows = pl.ds(pl.multiple_of(t * SUB, SUB), SUB)
                    pltpu.make_async_copy(ref.at[rows, :], wk.at[I0, pl.ds(512 + slot * SUB, SUB), :], load_sem.at[slot]).start()
            if condition is None:
                go()
            else:
                pl.when(condition)(go)

    def loaded(i, refs, slot):
        ref = refs[I0][I1]
        if i < I2:
            pltpu.make_async_copy(ref.at[I0:192, :], wk.at[I0, I0:192, :], load_sem.at[slot]).wait()
        elif i == I2:
            pltpu.make_async_copy(ref.at[:, I0:SUB], wn.at[slot, :, I0:SUB], load_sem.at[slot]).wait()
        else:
            pltpu.make_async_copy(ref.at[I0:SUB, :], wk.at[I0, 512:768, :], load_sem.at[slot]).wait()

    def store(i, dst, t, slot):
        if i == I2:
            rows = pl.ds(pl.multiple_of(t * SUB, SUB), SUB)
            return pltpu.make_async_copy(wk.at[I1, pl.ds(slot * SUB, SUB), :], dst.at[rows, :], store_sem.at[slot])
        return pltpu.make_async_copy(wn.at[slot, :, SUB:512], dst.at[:, lanes(t * SUB, SUB)], store_sem.at[slot])

    def turn(i, refs, dst, first, count):
        load(i, refs, first, I0)

        def step(n, c):
            slot = n % I2

            @pl.when(n + I1 < count)
            def _():
                load(i, refs, first + n + I1, I1 - slot)
            loaded(i, refs, slot)

            @pl.when(n >= I2)
            def _():
                store(i, dst, first + n - I2, slot).wait()
            for b in range(I6):
                cut = slice(b * SUB, b * SUB + SUB)
                if i == I2:
                    wk[I1, pl.ds(pl.multiple_of(slot * SUB, SUB), SUB), cut] = wn[slot, cut, I0:SUB].T
                else:
                    base = I0 if i < I2 else 512
                    wn[slot, cut, SUB:512] = wk[I0, pl.ds(pl.multiple_of(base + slot * SUB, SUB), SUB), cut].T
            store(i, dst, first + n, slot).start()
            return c
        lax.fori_loop(I0, count, step, I0)
        for n in (count - I2, count - I1):
            store(i, dst, first + n, n % I2).wait()

    counts = (12, I4, 12, 12)
    for i in range(I4):
        @pl.when(is_r)
        def _(i=i):
            remote(near[i], near[i], send_sem.at[i], near_sem.at[i], place.sibling).wait_recv()
        turn(i, [(place.is_l, own[i]), (is_r, near[i])], turned[i][I0], I0, counts[i])
    done = [I0, I0, I0, I0]
    for c, (i, axis, index) in enumerate(PIECES):
        view = piece(far[i], axis, index)
        remote(view, view, d_send.at[i], far_sem.at[c], place.sibling).wait_recv()

        @pl.when(is_r)
        def _(i=i, c=c, view=view):
            remote(view, view, d_send.at[i], far_sem.at[c], place.sibling).start()
        count = I4 if i < I2 else I3
        turn(i, [(None, far[i])], turned[i][I1], done[i], count)
        done[i] += count

    @pl.when(place.is_l)
    def _():
        for i in range(I4):
            remote(own[i], near[i], send_sem.at[i], near_sem.at[i], place.sibling).wait_send()

    @pl.when(is_r)
    def _():
        for i in range(I4):
            remote(own[i], far[i], y_send.at[i], far_sem.at[I0], place.across_other).wait_send()
            remote(far[i], far[i], d_send.at[i], far_sem.at[I0], place.sibling).wait_send()


def near_choices(place, own, near):
    return [(place.is_l, own), (jnp.logical_not(place.is_l), near)]


def forward_kernel(dims, x_ref, y_ref, wq, wo, wu, wd, own_gains,
                   a_s, h_s, qkv_s, u_s, g_s, oh_same, oh_other, oa_same, oa_other, loss_all, home_gains,
                   nq, no, nu, nd, fq, fo, fu, fd, tq0, to0, tu0, td0, tq1, to1, tu1, td1,
                   abuf, hbuf, obuf, nbuf, ybuf, sbuf, qkvbuf, ubuf, zbuf, ctxbuf, acc, lossbuf, losstile, gains, wres, wores, wn,
                   send_sem, y_send, d_send, near_sem, far_sem, t_load, t_store,
                   act_sem, hop_f, keep_sem, save_sem, stream_n, res_sem, out_sem, big_sem, y_sem, s_sem,
                   os_sem, oo_sem, as_sem, ao_sem, bulk, gain_sem, tiny, loss_send):
    micro, seq, width, heads, head_dim, ffn = dims
    place = Place()
    is_first, is_last = place.home == I0, place.home == I3
    home02 = (place.home == I0) | (place.home == I2)
    is_r = jnp.logical_not(place.is_l)
    takes_x = (place.home == I1) & is_r
    half = heads // I2 * HEAD_PAD
    scale = head_dim ** -0.5
    norm_factor = 1.0 / (micro * I2 * seq * width)
    own, near, far = (wq, wo, wu, wd), (nq, no, nu, nd), (fq, fo, fu, fd)
    turned = ((tq0, tq1), (to0, to1), (tu0, tu1), (td0, td1))
    entry_barrier(place)

    @pl.when(place.is_l)
    def _():
        pltpu.make_async_copy(own_gains, gains, gain_sem.at[I0]).start()
        remote(own_gains, gains, gain_sem.at[I1], gain_sem.at[I0], place.sibling).start()

    @pl.when(is_first)
    def _():
        for m in range(micro):
            pltpu.make_async_copy(x_ref.at[m, place.core], abuf.at[m], act_sem.at[m]).start()
    weight_phase(place, is_r, own, near, far, turned, wn, wores, send_sem, y_send, d_send, near_sem, far_sem, t_load, t_store)
    pltpu.make_async_copy(own_gains, gains, gain_sem.at[I0]).wait()
    pltpu.make_async_copy(gains, home_gains, gain_sem.at[I0]).start()

    @pl.when(place.is_l)
    def _():
        remote(own_gains, gains, gain_sem.at[I1], gain_sem.at[I0], place.sibling).wait_send()

    def near_of(i):
        return near_choices(place, own[i], near[i])

    def saved(dst, index):
        return pltpu.make_async_copy(hbuf, dst, save_sem.at[index])

    sn = Stream(wn, stream_n, DEPTH, [([(None, tq0)], I3), ([(None, tq1)], I3), (near_of(I2), I3), ([(None, fu)], I3)], micro * 12, False)
    for c, choices in enumerate((near_of(I1), [(None, fo)])):
        for condition, ref in choices:
            def go(ref=ref, c=c):
                load_heads(ref, I0, wores.at[c], out_sem.at[c])
            go() if condition is None else pl.when(condition)(go)
    sn.prime()
    load_resident(wres, res_sem, (near_of(I3), [(None, fd)]))
    lossbuf[...] = jnp.zeros_like(lossbuf)

    def qkv_out(m):
        return pltpu.make_async_copy(qkvbuf, qkv_s.at[m], big_sem.at[I0])

    def up_out(m):
        return pltpu.make_async_copy(ubuf, u_s.at[m], big_sem.at[I1])

    def act_out(m):
        return pltpu.make_async_copy(abuf.at[m], a_s.at[m], save_sem.at[I2])

    def hop_forward(m):
        return remote(obuf.at[m % I2], abuf.at[m], hop_f.at[m % I2], act_sem.at[m], place.chain(I1))

    def near_hand(src, dst_far, dst_own, sem, recv_sem):
        return (lambda: remote(src, dst_far, sem, recv_sem, place.sibling)), (lambda: pltpu.make_async_copy(src, dst_own, sem))

    def hand_out(m):
        return near_hand(obuf.at[m % I2], oa_other.at[m], oa_same.at[m], keep_sem.at[m % I2], ao_sem)

    def both_kinds(condition, copies, start):
        far_copy, own_copy = copies

        @pl.when(condition & place.is_l)
        def _():
            far_copy().start() if start else far_copy().wait_send()

        @pl.when(condition & is_r)
        def _():
            own_copy().start() if start else own_copy().wait()

    def x_out(m):
        return pltpu.make_async_copy(ybuf, oa_same.at[m], y_sem), pltpu.make_async_copy(sbuf, oa_other.at[m], s_sem)

    def seed_out(m):
        return pltpu.make_async_copy(sbuf, g_s.at[m], s_sem)

    def forward_tick(m, carry):
        act, mid, out = abuf.at[m], hbuf, obuf.at[m % I2]
        pltpu.make_async_copy(x_ref.at[m, place.core], act, act_sem.at[m]).wait()
        act_out(m).start()

        @pl.when(place.is_l)
        def _():
            pltpu.make_async_copy(act, oa_same.at[m], as_sem).start()

        @pl.when(is_last)
        def _():
            pltpu.make_async_copy(y_ref.at[m, place.core], ybuf, y_sem).start()

        @pl.when(takes_x)
        def _():
            @pl.when(m > I0)
            def _():
                for copy in x_out(m):
                    copy.wait()
            for core, buf, sem in ((place.core, ybuf, y_sem), (I1 - place.core, sbuf, s_sem)):
                pltpu.make_async_copy(x_ref.at[m, core], buf, sem).start()
        norm_rows(act, gains[I0:I1, :], nbuf, seq)

        @pl.when(m > I0)
        def _():
            qkv_out(m).wait()

        def qkv_step(j, c):
            w = sn.wait(m * 12 + j)
            for n in range(I0, CHUNK, SUB):
                qkvbuf[:, lanes(j * CHUNK + n, SUB)] = mm(nbuf[...], w[:, n:n + SUB]).astype(BF)
            sn.start(m * 12 + j + DEPTH)
            return c
        lax.fori_loop(I0, I6, qkv_step, I0)
        qkv_out(m).start()
        act_out(m).wait()

        @pl.when(is_r)
        def _():
            remote(a_s.at[m], oa_other.at[m], bulk.at[I0], ao_sem, place.sibling).start()

        def head_step(i, c):
            base = i * (I3 * half)
            views = [[qkvbuf[:, lanes(base + t * half + r * HEAD_PAD, HEAD_PAD)] for t in range(I3)] for r in range(I8)]
            for r, context in enumerate(attention_forward(views, scale)):
                ctxbuf[:, lanes(i * half + r * HEAD_PAD, HEAD_PAD)] = context
            return c
        lax.fori_loop(I0, I2, head_step, I0)

        @pl.when(m == I0)
        def _():
            for c in range(I2):
                pltpu.make_async_copy(wo, wores.at[c, I0:768, :], out_sem.at[c]).wait()
        for n in range(I0, width, SUB):
            total = mm(ctxbuf[:, I0:half], wores[I0, :, n:n + SUB]) + mm(ctxbuf[:, half:I2 * half], wores[I1, :, n:n + SUB])
            mid[:, n:n + SUB] = (act[:, n:n + SUB].astype(F32) + total).astype(BF)
        saved(h_s.at[m], I0).start()

        @pl.when(place.is_l)
        def _():
            saved(oh_same.at[m], I1).start()
        norm_rows(mid, gains[I1:I2, :], nbuf, seq)

        @pl.when(m > I0)
        def _():
            up_out(m).wait()
        acc[...] = jnp.zeros_like(acc)

        def mlp_step(j, c):
            w = sn.wait(m * 12 + I6 + j)
            for n in range(I0, CHUNK, SUB):
                u = mm(nbuf[...], w[:, n:n + SUB]).astype(BF)
                ubuf[:, lanes(j * CHUNK + n, SUB)] = u
                uf = u.astype(F32)
                zbuf[:, n:n + SUB] = (uf * gelu_gate(uf)[I0]).astype(BF)
            sn.start(m * 12 + I6 + j + DEPTH)

            @pl.when(m == I0)
            def _():
                pltpu.make_async_copy(wd.at[I0:CHUNK, :], wres.at[j], res_sem.at[j]).wait()
            for n in range(I0, width, SUB):
                acc[:, n:n + SUB] += mm(zbuf[...], wres[j, :, n:n + SUB])
            return c
        lax.fori_loop(I0, I6, mlp_step, I0)
        up_out(m).start()

        @pl.when((m > I1) & jnp.logical_not(is_last))
        def _():
            hop_forward(m).wait_send()

        both_kinds((m > I1) & home02, hand_out(m), False)

        def finish(rows):
            out[rows, :] = (mid[rows, :].astype(F32) + acc[rows, :]).astype(BF)
        rows_loop(seq, 32, finish)

        @pl.when(jnp.logical_not(is_last))
        def _():
            hop_forward(m).start()

        both_kinds(home02, hand_out(m), True)

        @pl.when(is_last)
        def _():
            pltpu.make_async_copy(y_ref.at[m, place.core], ybuf, y_sem).wait()

            @pl.when(m > I0)
            def _():
                seed_out(m).wait()

            def seed(rows):
                error = out[rows, :].astype(F32) - ybuf[rows, :].astype(F32)
                sbuf[rows, :] = (error * norm_factor).astype(BF)
                lossbuf[...] += jnp.sum((error * error).reshape(I4, I8, width), axis=I0)
            rows_loop(seq, 32, seed)
            seed_out(m).start()

        @pl.when(takes_x)
        def _():
            for core, buf, sem in ((place.core, ybuf, y_sem), (I1 - place.core, sbuf, s_sem)):
                pltpu.make_async_copy(x_ref.at[m, core], buf, sem).wait()
            for copy in x_out(m):
                copy.start()

        saved(h_s.at[m], I0).wait()

        @pl.when(place.is_l)
        def _():
            saved(oh_same.at[m], I1).wait()
            remote(h_s.at[m], oh_same.at[m], bulk.at[I2], os_sem, place.across).start()

        @pl.when(is_r)
        def _():
            remote(h_s.at[m], oh_other.at[m], bulk.at[I2], oo_sem, place.sibling).start()
            remote(h_s.at[m], oh_other.at[m], bulk.at[I3], oo_sem, place.across_other).start()
        return carry

    lax.fori_loop(I0, micro, forward_tick, I0)

    @pl.when(is_last)
    def _():
        total = lossbuf[:, I0:128]
        for n in range(128, width, 128):
            total = total + lossbuf[:, n:n + 128]
        losstile[...] = total
        pltpu.make_async_copy(losstile, loss_all.at[place.core], tiny).start()
        for index, copy in enumerate(place.others(losstile, loss_all.at[place.core], loss_send, tiny)):
            copy.start()
    for copy in (qkv_out(micro - I1), up_out(micro - I1)):
        copy.wait()

    @pl.when(jnp.logical_not(is_last))
    def _():
        for m in (micro - I2, micro - I1):
            hop_forward(m).wait_send()
    for m in (micro - I2, micro - I1):
        both_kinds(home02, hand_out(m), False)

    @pl.when(is_last)
    def _():
        seed_out(micro - I1).wait()
        for copy in place.others(losstile, loss_all.at[place.core], loss_send, tiny):
            copy.wait_send()

    @pl.when(takes_x)
    def _():
        for copy in x_out(micro - I1):
            copy.wait()
    pltpu.make_async_copy(gains, home_gains, gain_sem.at[I0]).wait()
    sent, got = drain(place)
    sent(h_s, bulk.at[I2])
    got(oh_other, oo_sem)
    got(loss_all, tiny)

    @pl.when(is_r)
    def _():
        sent(a_s, bulk.at[I0])
        sent(h_s, bulk.at[I3])
        got(oh_same, os_sem)

    @pl.when(place.is_l)
    def _():
        got(oa_same, as_sem)

    @pl.when(place.is_l | home02)
    def _():
        got(oa_other, ao_sem)


def drain(place):
    def sent(buf, sem):
        remote(buf, buf, sem, sem, place.sibling).wait_send()

    def got(dst, sem):
        pltpu.make_async_copy(dst, dst, sem).wait()
    return sent, got


def backward_kernel(dims, a_s, h_s, qkv_s, u_s, g_s, wq, nq, fq, td0, td1, to0, to1, tu0, tu1, gains, after, oa_in_same, oa_in_other,
                    dx_s, m_s, od_same, od_other, og_same, og_other, oa_same, oa_other, dg_same, dg_other,
                    gbuf, hbuf, obuf, qkvbuf, ubuf, habuf, zbuf, ctxbuf, dqkvbuf, acc, accg, wres, wn, wk,
                    grad_sem, hop_b, back_sem, save_sem, stream_n, stream_k, res_sem, load_sem,
                    ds_sem, do_sem, gs_sem, go_sem, as_sem, ao_sem, bulk, tiny):
    micro, seq, width, heads, head_dim, ffn = dims
    place = Place()
    is_first, is_last = place.home == I0, place.home == I3
    home13 = (place.home == I1) | is_last
    is_r = jnp.logical_not(place.is_l)
    half = heads // I2 * HEAD_PAD
    scale = head_dim ** -0.5

    barrier = pltpu.get_barrier_semaphore()
    along_x = (place.home == I1) | (place.home == I2)
    for there in (place.sibling, place.across, place.across_other):
        pl.semaphore_signal(barrier, inc=I1, device_id=there, device_id_type=MESH)

    @pl.when(along_x)
    def _():
        pl.semaphore_signal(barrier, inc=I1, device_id=place.at(place.tp, (place.stage + I2) % I4), device_id_type=MESH)

    @pl.when(is_last)
    def _():
        for m in range(micro):
            pltpu.make_async_copy(g_s.at[m], gbuf.at[m], grad_sem.at[m]).start()
    wk[...] = jnp.zeros_like(wk)
    bn = Stream(wn, stream_n, BACK_DEPTH, [([(None, td0)], I3), ([(None, td1)], I3), ([(None, to0)], I1), ([(None, to1)], I1)], micro * I8, False)
    bk = Stream(wk, stream_k, KDEPTH, [(near_choices(place, wq, nq), I3), ([(None, fq)], I3)], micro * I6, True)
    bn.prime()
    bk.prime()
    load_resident(wres, res_sem, ([(None, tu0)], [(None, tu1)]))

    def saved(dst, index):
        return pltpu.make_async_copy(hbuf, dst, save_sem)

    def both_kinds(condition, copies, start):
        far_copy, own_copy = copies

        @pl.when(condition & place.is_l)
        def _():
            far_copy().start() if start else far_copy().wait_send()

        @pl.when(condition & is_r)
        def _():
            own_copy().start() if start else own_copy().wait()

    def near_hand(src, dst_far, dst_own, sem, recv_sem):
        return (lambda: remote(src, dst_far, sem, recv_sem, place.sibling)), (lambda: pltpu.make_async_copy(src, dst_own, sem))

    def loads(i):
        m = micro - I1 - i
        slot = i % I2
        return (pltpu.make_async_copy(u_s.at[m], ubuf.at[slot], load_sem.at[I0, slot]),
                pltpu.make_async_copy(qkv_s.at[m], qkvbuf.at[slot], load_sem.at[I1, slot]),
                pltpu.make_async_copy(h_s.at[m], habuf.at[slot, I0], load_sem.at[I2, slot]),
                pltpu.make_async_copy(a_s.at[m], habuf.at[slot, I1], load_sem.at[I3, slot]))

    for copy in loads(I0):
        copy.start()
    accg[...] = jnp.zeros_like(accg)

    def norm_back(index, x, base, dst, gain_row):
        def body(rows):
            xf = x[rows, :].astype(F32)
            dy = acc[rows, :].astype(BF).astype(F32)
            inv = lax.rsqrt(jnp.mean(xf * xf, axis=-I1, keepdims=True) + NORM_EPS)
            xn = xf * inv
            accg[index] += jnp.sum((dy * xn).reshape(I4, I8, width), axis=I0)
            dyg = dy * gain_row
            dx = inv * (dyg - xn * jnp.mean(dyg * xn, axis=-I1, keepdims=True))
            dst[rows, :] = (base[rows, :].astype(F32) + dx).astype(BF)
        rows_loop(seq, 32, body)

    def hop_back(i):
        m = micro - I1 - i
        return remote(obuf.at[i % I2], gbuf.at[m], hop_b.at[i % I2], grad_sem.at[m], place.chain(-I1))

    def hand_back(i):
        m = micro - I1 - i
        return near_hand(obuf.at[i % I2], og_other.at[m], og_same.at[m], back_sem.at[i % I2], go_sem)

    def keep_dx(i):
        return pltpu.make_async_copy(obuf.at[i % I2], dx_s.at[micro - I1 - i], back_sem.at[i % I2])

    def back_ready(i):
        both_kinds((i > I1) & home13, hand_back(i), False)

        @pl.when((i > I1) & is_first)
        def _():
            keep_dx(i).wait()

        @pl.when((i > I1) & jnp.logical_not(is_first))
        def _():
            hop_back(i).wait_send()

    def backward_tick(i, carry):
        m = micro - I1 - i
        slot = i % I2
        grad, dmid, prev = gbuf.at[m], hbuf, obuf.at[slot]
        u_now, qkv_now, h_now, a_now = ubuf.at[slot], qkvbuf.at[slot], habuf.at[slot, I0], habuf.at[slot, I1]

        @pl.when(i + I1 < micro)
        def _():
            for copy in loads(i + I1):
                copy.start()

        pltpu.make_async_copy(g_s.at[m], grad, grad_sem.at[m]).wait()

        @pl.when(place.is_l)
        def _():
            pltpu.make_async_copy(grad, og_same.at[m], gs_sem).start()
        load_u, load_qkv, load_h, load_a = loads(i)
        load_u.wait()
        acc[...] = jnp.zeros_like(acc)

        def mlp_step(j, c):
            w = bn.wait(i * I8 + j)
            for n in range(I0, CHUNK, SUB):
                dz = mm(grad[...], w[:, n:n + SUB]).astype(BF).astype(F32)
                u = u_now[:, lanes(j * CHUNK + n, SUB)].astype(F32)
                gate, u2 = gelu_gate(u)
                zbuf[:, n:n + SUB] = (dz * gelu_slope(u * gate, gate, u2)).astype(BF)
            bn.start(i * I8 + j + BACK_DEPTH)

            @pl.when(i == I0)
            def _():
                pltpu.make_async_copy(tu0.at[I0:CHUNK, :], wres.at[j], res_sem.at[j]).wait()
            for n in range(I0, width, SUB):
                acc[:, n:n + SUB] += mm(zbuf[...], wres[j, :, n:n + SUB])
            return c
        lax.fori_loop(I0, I6, mlp_step, I0)
        load_h.wait()
        norm_back(I1, h_now, grad, dmid, gains[I1:I2, :])

        @pl.when(place.is_l)
        def _():
            saved(od_same.at[m], I0).start()

        @pl.when(is_r)
        def _():
            saved(m_s.at[m], I0).start()
        for c in range(I2):
            w = bn.wait(i * I8 + I6 + c)
            for n in range(I0, CHUNK, SUB):
                ctxbuf[:, c * CHUNK + n:c * CHUNK + n + SUB] = mm(dmid[...], w[:, n:n + SUB]).astype(BF)
            bn.start(i * I8 + I6 + c + BACK_DEPTH)
        load_qkv.wait()

        def head_step(t, c):
            base = (t // I2) * (I3 * half) + (t % I2) * (I4 * HEAD_PAD)
            at = [[lanes(base + part * half + r * HEAD_PAD, HEAD_PAD) for part in range(I3)] for r in range(I4)]
            group = [(*(qkv_now[:, p] for p in at[r]), ctxbuf[:, lanes((t * I4 + r) * HEAD_PAD, HEAD_PAD)]) for r in range(I4)]
            for r, grads in enumerate(attention_backward(group, scale)):
                for p, value in zip(at[r], grads):
                    dqkvbuf[:, p] = value
            return c
        lax.fori_loop(I0, heads // I4, head_step, I0)
        acc[...] = jnp.zeros_like(acc)

        def qkv_step(j, c):
            w = bk.wait(i * I6 + j)
            for n in range(I0, width, SUB):
                acc[:, n:n + SUB] += mm(dqkvbuf[:, lanes(j * CHUNK, CHUNK)], w[:, n:n + SUB])
            bk.start(i * I6 + j + KDEPTH)
            return c
        lax.fori_loop(I0, I6, qkv_step, I0)
        load_a.wait()
        back_ready(i)
        norm_back(I0, a_now, dmid, prev, gains[I0:I1, :])

        @pl.when(i == I0)
        def _():
            pl.semaphore_wait(barrier, I3 + (place.home + I1) // I2 % I2)

        @pl.when(jnp.logical_not(is_first))
        def _():
            hop_back(i).start()

        @pl.when(is_first)
        def _():
            keep_dx(i).start()
        both_kinds(home13, hand_back(i), True)

        @pl.when(place.is_l)
        def _():
            saved(od_same.at[m], I0).wait()
            remote(od_same.at[m], od_same.at[m], bulk.at[I6], ds_sem, place.across).start()

        @pl.when(is_r)
        def _():
            remote(grad, og_other.at[m], bulk.at[5], go_sem, place.sibling).start()
            saved(m_s.at[m], I0).wait()
            remote(m_s.at[m], od_other.at[m], bulk.at[I6], do_sem, place.sibling).start()
            remote(m_s.at[m], od_other.at[m], bulk.at[7], do_sem, place.across_other).start()

        @pl.when((place.home == I2) & place.is_l)
        def _():
            remote(a_s.at[m], oa_same.at[m], bulk.at[I8], as_sem, place.across).start()

        @pl.when((place.home == I2) & is_r)
        def _():
            remote(a_s.at[m], oa_other.at[m], bulk.at[I8], ao_sem, place.across_other).start()
        far_grad(m, (place.home == I1) & (i % I2 == I0))
        return carry

    def far_grad(m, condition):
        @pl.when(condition & place.is_l)
        def _():
            remote(gbuf.at[m], og_same.at[m], bulk.at[I4], gs_sem, place.across).start()

        @pl.when(condition & is_r)
        def _():
            remote(gbuf.at[m], og_other.at[m], bulk.at[I4], go_sem, place.across_other).start()

    lax.fori_loop(I0, micro, backward_tick, I0)
    for i in range(micro):
        far_grad(micro - I1 - i, is_last | (place.home == I1) if i % I2 else is_last)

    @pl.when(place.is_l)
    def _():
        pltpu.make_async_copy(accg, dg_same, tiny.at[I0]).start()
        remote(accg, dg_same, tiny.at[I1], tiny.at[I0], place.across).start()

    @pl.when(is_r)
    def _():
        remote(accg, dg_other, tiny.at[I1], tiny.at[I4], place.sibling).start()
        remote(accg, dg_other, tiny.at[I2], tiny.at[I4], place.across_other).start()

    for i in (micro - I2, micro - I1):
        back_ready(jnp.int32(i))

    sent, got = drain(place)
    sent(m_s, bulk.at[I6])

    @pl.when(is_r)
    def _():
        sent(gbuf, bulk.at[5])
        sent(m_s, bulk.at[7])
        remote(accg, dg_other, tiny.at[I2], tiny.at[I4], place.sibling).wait_send()

    @pl.when(home13)
    def _():
        sent(gbuf, bulk.at[I4])

    @pl.when(place.home == I2)
    def _():
        sent(a_s, bulk.at[I8])

    remote(accg, dg_other, tiny.at[I1], tiny.at[I4], place.sibling).wait_send()
    got(od_other, do_sem)
    got(og_other, go_sem)
    got(dg_same, tiny.at[I0])
    got(dg_other, tiny.at[I4])

    @pl.when(is_r)
    def _():
        got(od_same, ds_sem)

    @pl.when(place.is_l | jnp.logical_not(home13))
    def _():
        got(og_same, gs_sem)

    @pl.when(is_last & is_r)
    def _():
        got(oa_same, as_sem)
        got(oa_other, ao_sem)


def shapes(*dims_list):
    return [jax.ShapeDtypeStruct(d, BF) for d in dims_list]


def forward_phase(dims, x, y, own, own_gains):
    micro, seq, width, heads, head_dim, ffn = dims
    half = heads // I2 * HEAD_PAD
    act = (micro, seq, width)
    raw = [w.shape for w in own]
    turned = [(width, I3 * half), (width, half), (ffn // I2, width), (width, ffn // I2)]
    out_shape = shapes(act, act, (micro, seq, I6 * half), (micro, seq, ffn), *[act] * 5)
    out_shape += [jax.ShapeDtypeStruct(s, F32) for s in ((I2, I8, 128), own_gains.shape)]
    out_shape += shapes(*raw, *raw, *turned, *turned)
    any_spec = pl.BlockSpec(memory_space=ANY)
    vmem, dma = pltpu.VMEM, pltpu.SemaphoreType.DMA
    row = vmem((seq, width), BF)
    scratch = [
        vmem(act, BF), row, vmem((I2, seq, width), BF), row, row, row, vmem((seq, I6 * half), BF), vmem((seq, ffn), BF), vmem((seq, CHUNK), BF),
        vmem((seq, I2 * half), BF), vmem((seq, width), F32), vmem((I8, width), F32), vmem((I8, 128), F32), vmem((I2, width), F32),
        vmem((I6, CHUNK, width), BF), vmem((I2, CHUNK, width), BF), vmem((DEPTH, width, CHUNK), BF),
        dma((I4,)), dma((I4,)), dma((I4,)), dma((I4,)), dma((12,)), dma((I2,)), dma((I2,)),
        dma((micro,)), dma((I2,)), dma((I2,)), dma((I3,)), dma((DEPTH,)), dma((I6,)), dma((I2,)), dma((I2,)), dma(()), dma(()),
        dma(()), dma(()), dma(()), dma(()), dma((I4,)), dma((I2,)), dma(()), dma((7,)),
    ]
    return pl.pallas_call(
        functools.partial(forward_kernel, dims),
        out_shape=tuple(out_shape),
        in_specs=[any_spec] * I6 + [pl.BlockSpec(memory_space=vmem)],
        out_specs=(any_spec,) * len(out_shape),
        scratch_shapes=scratch,
        compiler_params=pltpu.CompilerParams(collective_id=I0, has_side_effects=True, vmem_limit_bytes=VMEM_LIMIT),
        name='forward_phase',
    )(x, y, *own, own_gains)


def backward_phase(dims, saved, weights, gains, after, oa_rows):
    micro, seq, width, heads, head_dim, ffn = dims
    half = heads // I2 * HEAD_PAD
    act = (micro, seq, width)
    out_shape = shapes(*[act] * I8) + [jax.ShapeDtypeStruct((I2, I8, width), F32)] * I2
    any_spec = pl.BlockSpec(memory_space=ANY)
    vmem, dma = pltpu.VMEM, pltpu.SemaphoreType.DMA
    scratch = [
        vmem(act, BF), vmem((seq, width), BF), vmem((I2, seq, width), BF), vmem((I2, seq, I6 * half), BF), vmem((I2, seq, ffn), BF),
        vmem((I2, I2, seq, width), BF), vmem((seq, CHUNK), BF), vmem((seq, I2 * half), BF), vmem((seq, I6 * half), BF), vmem((seq, width), F32),
        vmem((I2, I8, width), F32), vmem((I6, CHUNK, width), BF), vmem((BACK_DEPTH, width, CHUNK), BF), vmem((KDEPTH, CHUNK, width), BF),
        dma((micro,)), dma((I2,)), dma((I2,)), dma(()), dma((BACK_DEPTH,)), dma((KDEPTH,)), dma((I6,)), dma((I4, I2)),
        dma(()), dma(()), dma(()), dma(()), dma(()), dma(()), dma((9,)), dma((5,)),
    ]
    return pl.pallas_call(
        functools.partial(backward_kernel, dims),
        out_shape=tuple(out_shape),
        in_specs=[any_spec] * 14 + [pl.BlockSpec(memory_space=vmem)] + [any_spec] * I3,
        out_specs=(any_spec,) * len(out_shape),
        scratch_shapes=scratch,
        input_output_aliases={16: I6, 17: 7},
        compiler_params=pltpu.CompilerParams(collective_id=I1, has_side_effects=True, vmem_limit_bytes=VMEM_LIMIT),
        name='backward_phase',
    )(*saved, *weights, gains, after, *oa_rows)


def recompute_kernel(dims, early, h_same, h_other, a_same, a_other, gains, wq, wu, *refs):
    (done, u_o, qkv_o, ctx_o, n1_o, n2_o), (wqbuf, wubuf, count, sem) = refs[-10:-I4], refs[-I4:]
    micro, seq, width, heads, head_dim, ffn = dims
    place = Place()
    scale = head_dim ** -0.5
    half = heads // I2 * HEAD_PAD
    steps = I2 * micro * seq // BLOCK

    def body(hs, ho, rs, ro, u, qkv, ctx, n1, n2):
        step = count[I0]
        count[I0] = step + I1
        for low, high, gain, dst in ((hs, ho, gains[I1:I2, :], n2), (rs, ro, gains[I0:I1, :], n1)):
            @pl.when(step < steps // I2)
            def _(low=low, gain=gain, dst=dst):
                norm_rows(low, gain, dst, BLOCK)

            @pl.when(step >= steps // I2)
            def _(high=high, gain=gain, dst=dst):
                norm_rows(high, gain, dst, BLOCK)

        def qkv_step(j, c):
            rows = pl.ds(pl.multiple_of(j * SUB, SUB), SUB)
            qkv[:, lanes(j * SUB, SUB)] = mm_nt(n1[...], wqbuf[rows, :]).astype(BF)
            u[:, lanes(j * SUB, SUB)] = mm(n2[...], wubuf[:, lanes(j * SUB, SUB)]).astype(BF)
            return c
        lax.fori_loop(I0, I3 * half // SUB, qkv_step, I0)

        def head_step(j, c):
            at = [(pl.ds(s, seq), r * HEAD_PAD) for s in range(I0, BLOCK, seq) for r in range(I4)]
            base = j * (I4 * HEAD_PAD)
            views = [[qkv[rows, lanes(base + t * half + col, HEAD_PAD)] for t in range(I3)] for rows, col in at]
            for (rows, col), context in zip(at, attention_forward(views, scale)):
                ctx[rows, lanes(base + col, HEAD_PAD)] = context
            return c
        lax.fori_loop(I0, I2, head_step, I0)

    @pl.when(place.home < I2 if early else place.home > I1)
    def _():
        wqbuf[...] = jnp.zeros_like(wqbuf)
        for t in range(I3):
            load_heads(wq, t, wqbuf.at[pl.ds(t * CHUNK, CHUNK)], sem.at[I0])
        up = pltpu.make_async_copy(wu, wubuf, sem.at[I1])
        up.start()
        up.wait()
        pltpu.make_async_copy(wq, wqbuf.at[I0:wq.shape[I0]], sem.at[I0]).wait()
        count[I0] = I0
        low = pl.BlockSpec((BLOCK, width), lambda i: (jnp.minimum(i, steps // I2 - I1), I0))
        high = pl.BlockSpec((BLOCK, width), lambda i: (jnp.maximum(i - steps // I2, I0), I0))
        block = lambda n: pl.BlockSpec((BLOCK, n), lambda i: (i, I0))
        pltpu.emit_pipeline(body, grid=(steps,), in_specs=[low, high, low, high],
                            out_specs=[block(ffn // I2), block(I3 * half), block(half), block(width), block(width)])(
            h_same, h_other, a_same, a_other, u_o, qkv_o, ctx_o, n1_o, n2_o)


def owner_recompute(dims, early, again, h_rows, a_rows, gains, own):
    micro, seq, width, heads, head_dim, ffn = dims
    half = heads // I2 * HEAD_PAD
    tokens = I2 * micro * seq
    any_spec = pl.BlockSpec(memory_space=ANY)
    vmem = pltpu.VMEM
    earlier = () if early else tuple(again)
    return pl.pallas_call(
        functools.partial(recompute_kernel, dims, early),
        out_shape=(jax.ShapeDtypeStruct((I8, 128), F32), *shapes((tokens, ffn // I2), (tokens, I3 * half), (tokens, half), (tokens, width), (tokens, width))),
        in_specs=[any_spec] * I4 + [pl.BlockSpec(memory_space=vmem)] + [any_spec] * (I2 + len(earlier)),
        out_specs=(any_spec,) * I6,
        scratch_shapes=[vmem((I3 * half, width), BF), vmem((width, ffn // I2), BF), pltpu.SMEM((I1,), jnp.int32), pltpu.SemaphoreType.DMA((I2,))],
        input_output_aliases={7 + i: I1 + i for i in range(len(earlier))},
        compiler_params=pltpu.CompilerParams(has_side_effects=True, vmem_limit_bytes=VMEM_LIMIT),
        name='owner_recompute',
    )(*h_rows, *a_rows, gains, own[I0], own[I2], *earlier)


def spread_dx(step, last, dx, d_in, bounce, here_sem, parent_sem, sib_sem, send_sems):
    place = Place()
    micro = dx.shape[I0]
    below = place.at(place.tp, (place.stage + I2) % I4)
    barrier = pltpu.get_barrier_semaphore()
    is_a, is_b = place.home == I0, place.home == I1
    is_leaf = place.home > I1

    def block(m):
        return d_in.at[m, place.core]

    def hand(m, src, index, there):
        remote(src, block(m), send_sems.at[index], sib_sem if index == I0 else parent_sem.at[m], there).start()

    def arrived(m):
        remote(block(m), block(m), send_sems.at[I0], parent_sem.at[m], place.sibling).wait_recv()

    @pl.when(step == I0)
    def _():
        def tell(there):
            pl.semaphore_signal(barrier, inc=I1, device_id=there, device_id_type=MESH)
        tell(place.sibling)

        @pl.when(is_b)
        def _():
            tell(place.across)

        @pl.when(is_leaf)
        def _():
            tell(below)

    @pl.when((step == I1) & is_a)
    def _():
        pl.semaphore_wait(barrier, I3)
        for m in reversed(range(micro)):
            hand(m, dx.at[m], I1, place.across)
            hand(m, dx.at[m], I2, below)
            hand(m, dx.at[m], I0, place.sibling)
        pltpu.make_async_copy(dx, bounce, here_sem).start()

    @pl.when((step == I2) & is_a)
    def _():
        pltpu.make_async_copy(dx, bounce, here_sem).wait()
        for m in range(micro):
            pltpu.make_async_copy(bounce.at[m], block(m), here_sem).start()

    @pl.when((step == I2) & is_b)
    def _():
        pl.semaphore_wait(barrier, I2)

    @pl.when((step > I2) & (step < I3 + micro // I2) & is_b)
    def _():
        for r in (I1, I2):
            m = micro + I6 - I2 * step - r
            arrived(m)
            hand(m, block(m), I2, below)
            hand(m, block(m), I0, place.sibling)

    @pl.when((step == last) & is_leaf)
    def _():
        pl.semaphore_wait(barrier, I1)
        for m in reversed(range(micro)):
            arrived(m)
            hand(m, block(m), I0, place.sibling)

    @pl.when(step == last)
    def _():
        def sent(index):
            remote(dx, dx, send_sems.at[index], sib_sem, place.sibling).wait_send()
        sent(I0)

        @pl.when(is_a)
        def _():
            sent(I1)
            pltpu.make_async_copy(dx, dx, here_sem).wait()

        @pl.when(jnp.logical_not(is_leaf))
        def _():
            sent(I2)
        remote(dx, dx, send_sems.at[I0], sib_sem, place.sibling).wait_recv()


def owner_backward_kernel(dims, dx, ds, do, gs, go, u, qkv, wo, wd, dqkv, dup, z, d_in,
                          dmid, grad, dctx, wobuf, bounce, sem, here_sem, parent_sem, sib_sem, send_sems):
    micro, seq, width, heads, head_dim, ffn = dims
    half = heads // I2 * HEAD_PAD
    scale = head_dim ** -0.5
    step, steps = pl.program_id(I0), pl.num_programs(I0)
    spread_dx(step, steps - I1, dx, d_in, bounce, here_sem, parent_sem, sib_sem, send_sems)

    @pl.when(step == I0)
    def _():
        wobuf[...] = jnp.zeros_like(wobuf)
        load_heads(wo, I0, wobuf, sem)
        pltpu.make_async_copy(wo, wobuf.at[I0:wo.shape[I0]], sem).wait()
    for near, far, dst in ((ds, do, dmid), (gs, go, grad)):
        @pl.when(step < steps // I2)
        def _(near=near, dst=dst):
            dst[...] = near[...]

        @pl.when(step >= steps // I2)
        def _(far=far, dst=dst):
            dst[...] = far[...]

    def ctx_step(j, c):
        rows = pl.ds(pl.multiple_of(j * SUB, SUB), SUB)
        dctx[:, lanes(j * SUB, SUB)] = mm_nt(dmid[...], wobuf[rows, :]).astype(BF)
        return c
    lax.fori_loop(I0, half // SUB, ctx_step, I0)

    def mlp_step(j, c):
        rows = pl.ds(pl.multiple_of(j * SUB, SUB), SUB)
        cols = lanes(j * SUB, SUB)
        dz = mm_nt(grad[...], wd[rows, :]).astype(BF).astype(F32)
        up = u[:, cols].astype(F32)
        gate, up2 = gelu_gate(up)
        hidden = up * gate
        z[:, cols] = hidden.astype(BF)
        dup[:, cols] = (dz * gelu_slope(hidden, gate, up2)).astype(BF)
        return c
    lax.fori_loop(I0, ffn // I2 // SUB, mlp_step, I0)

    def head_step(j, c):
        base = j * (I2 * HEAD_PAD)
        at = [(pl.ds(s, seq), base + r * HEAD_PAD) for s in range(I0, BLOCK, seq) for r in range(I2)]
        group = [(*(qkv[rows, lanes(t * half + col, HEAD_PAD)] for t in range(I3)), dctx[rows, lanes(col, HEAD_PAD)]) for rows, col in at]
        for (rows, col), grads in zip(at, attention_backward(group, scale)):
            for t, value in enumerate(grads):
                dqkv[rows, lanes(t * half + col, HEAD_PAD)] = value
        return c
    lax.fori_loop(I0, heads // I4, head_step, I0)


def owner_backward(dims, dx, d_rows, g_rows, ups, qkv, own):
    micro, seq, width, heads, head_dim, ffn = dims
    half = heads // I2 * HEAD_PAD
    tokens = I2 * micro * seq
    steps = tokens // BLOCK
    vmem, dma = pltpu.VMEM, pltpu.SemaphoreType.DMA
    any_spec = pl.BlockSpec(memory_space=ANY)
    low = pl.BlockSpec((BLOCK, width), lambda i: (jnp.minimum(i, steps // I2 - I1), I0))
    high = pl.BlockSpec((BLOCK, width), lambda i: (jnp.maximum(i - steps // I2, I0), I0))
    block = lambda n: pl.BlockSpec((BLOCK, n), lambda i: (i, I0))
    return pl.pallas_call(
        functools.partial(owner_backward_kernel, dims),
        grid=(steps,),
        out_shape=tuple(shapes((tokens, I3 * half), (tokens, ffn // I2), (tokens, ffn // I2), (micro, I2, seq, width))),
        in_specs=[any_spec, low, high, low, high, block(ffn // I2), block(I3 * half), any_spec, pl.BlockSpec((ffn // I2, width), lambda i: (I0, I0))],
        out_specs=(block(I3 * half), block(ffn // I2), block(ffn // I2), any_spec),
        scratch_shapes=[vmem((BLOCK, width), BF), vmem((BLOCK, width), BF), vmem((BLOCK, half), BF), vmem((half, width), BF), vmem((micro, seq, width), BF),
                        dma(()), dma(()), dma((micro,)), dma(()), dma((I3,))],
        compiler_params=pltpu.CompilerParams(collective_id=I2, has_side_effects=True, vmem_limit_bytes=VMEM_LIMIT),
        name='owner_backward',
    )(dx, *d_rows, *g_rows, ups, qkv, own[I1], own[I3])


def bring(pairs, sem):
    copies = [pltpu.make_async_copy(src, dst, sem.at[i]) for i, (src, dst) in enumerate(pairs)]
    for copy in copies:
        copy.start()
    for copy in copies:
        copy.wait()


def attn_products_kernel(dq, dk, dv, ctx, n1_o, ds, do, dwq, dwo, n1, dmid, dqkvt, ctxt, sem):
    tokens, width = n1.shape
    part = tokens // I2
    head_dim = dwo.shape[I1]

    @pl.when(pl.program_id(I0) == I0)
    def _():
        bring([(n1_o, n1), (ds, dmid.at[pl.ds(I0, part)]), (do, dmid.at[pl.ds(part, part)])], sem)

    def turn(rows):
        for t, block in enumerate((dq, dk, dv)):
            for r in range(I2):
                at = (I2 * t + r) * head_dim
                dqkvt[at:at + head_dim, rows] = block[rows, r * HEAD_PAD:(r + I1) * HEAD_PAD].T[I0:head_dim]
        for r in range(I2):
            ctxt[r * head_dim:(r + I1) * head_dim, rows] = ctx[rows, r * HEAD_PAD:(r + I1) * HEAD_PAD].T[I0:head_dim]
    rows_loop(tokens, SUB, turn)
    for c in range(I0, width, SUB):
        cut = slice(c, c + SUB)
        dwq[:, :, :, cut] = mm(dqkvt[...], n1[:, cut]).reshape(I3, I2, head_dim, SUB)
        dwo[:, :, cut] = mm(ctxt[...], dmid[:, cut]).reshape(I2, head_dim, SUB)


def attn_products(dqkv, ctx, n1, d_rows, out_dims):
    heads, head_dim, width = out_dims
    tokens = n1.shape[I0]
    vmem = pltpu.VMEM
    any_spec = pl.BlockSpec(memory_space=ANY)
    pairs = heads // I2
    cols = lambda t: pl.BlockSpec((tokens, I2 * HEAD_PAD), lambda i: (I0, t * pairs + i))
    return pl.pallas_call(
        attn_products_kernel,
        grid=(pairs,),
        out_shape=(jax.ShapeDtypeStruct((I3,) + out_dims, F32), jax.ShapeDtypeStruct(out_dims, F32)),
        in_specs=[cols(I0), cols(I1), cols(I2), cols(I0), any_spec, any_spec, any_spec],
        out_specs=(pl.BlockSpec((I3, I2, head_dim, width), lambda i: (I0, i, I0, I0)), pl.BlockSpec((I2, head_dim, width), lambda i: (i, I0, I0))),
        scratch_shapes=[vmem((tokens, width), BF), vmem((tokens, width), BF), vmem((I6 * head_dim, tokens), BF), vmem((I2 * head_dim, tokens), BF),
                        pltpu.SemaphoreType.DMA((I3,))],
        compiler_params=pltpu.CompilerParams(vmem_limit_bytes=VMEM_LIMIT),
        name='attn_products',
    )(dqkv, dqkv, dqkv, ctx, n1, *d_rows)


def mlp_products_kernel(dup, z, n2_o, gs, go, dwu, dwd, n2t, grad, zt, stage, sem):
    width, tokens = n2t.shape
    part = tokens // I2

    @pl.when(pl.program_id(I0) == I0)
    def _():
        bring([(n2_o, stage), (gs, grad.at[pl.ds(I0, part)]), (go, grad.at[pl.ds(part, part)])], sem)

        def turn(rows):
            for c in range(I0, width, SUB):
                n2t[c:c + SUB, rows] = stage[rows, c:c + SUB].T
        rows_loop(tokens, SUB, turn)

    def turn_z(rows):
        for c in range(I0, z.shape[I1], SUB):
            zt[c:c + SUB, rows] = z[rows, c:c + SUB].T
    rows_loop(tokens, SUB, turn_z)
    for c in range(I0, width, I2 * SUB):
        dwu[c:c + I2 * SUB, :] = mm(n2t[c:c + I2 * SUB, :], dup[...])
    for c in range(I0, width, SUB):
        dwd[:, c:c + SUB] = mm(zt[...], grad[:, c:c + SUB])


def mlp_products(dup, hidden, n2, g_rows):
    tokens, width = n2.shape
    cols = dup.shape[I1]
    vmem = pltpu.VMEM
    any_spec = pl.BlockSpec(memory_space=ANY)
    block = pl.BlockSpec((tokens, SUB), lambda i: (I0, i))
    return pl.pallas_call(
        mlp_products_kernel,
        grid=(cols // SUB,),
        out_shape=(jax.ShapeDtypeStruct((width, cols), F32), jax.ShapeDtypeStruct((cols, width), F32)),
        in_specs=[block, block, any_spec, any_spec, any_spec],
        out_specs=(pl.BlockSpec((width, SUB), lambda i: (I0, i)), pl.BlockSpec((SUB, width), lambda i: (i, I0))),
        scratch_shapes=[vmem((width, tokens), BF), vmem((tokens, width), BF), vmem((SUB, tokens), BF), vmem((tokens, width), BF), pltpu.SemaphoreType.DMA((I3,))],
        compiler_params=pltpu.CompilerParams(vmem_limit_bytes=VMEM_LIMIT),
        name='mlp_products',
    )(dup, hidden, n2, *g_rows)


def solution(mesh):
    act_spec = P('rep', None, None, None)
    weight_specs = (
        P(('rep', 'stage'), None, None, 'tp', None),
        P(('rep', 'stage'), 'tp', None, None),
        P(('rep', 'stage'), None, 'tp'),
        P(('rep', 'stage'), 'tp', None),
        P(('rep', 'stage'), None),
        P(('rep', 'stage'), None),
    )

    def device_fn(inputs, targets, w_qkv, w_out, w_up, w_down, gain_attn, gain_mlp):
        micro_count, _, seq_len, width = inputs.shape
        dims = (micro_count, seq_len, width, I2 * w_out.shape[I1], w_out.shape[I2], I2 * w_up.shape[I2])
        norm_factor = 1.0 / (inputs.size)
        own = (w_qkv[I0], w_out[I0], w_up[I0], w_down[I0])
        own_gains = jnp.concatenate([gain_attn, gain_mlp]).astype(F32)
        rows_of = (own[I0].transpose(I1, I2, I3, I0).reshape(-I1, width), own[I1].reshape(-I1, width), own[I2], own[I3])

        (acts, mids, qkv, ups, seeds, oh_same, oh_other, oa_same, oa_other, loss_all, home_gains, *weights) = forward_phase(dims, inputs, targets, rows_of, own_gains)
        (nq, no, nu, nd), (fq, fo, fu, fd) = weights[I0:I4], weights[I4:I8]
        (tq0, to0, tu0, td0), (tq1, to1, tu1, td1) = weights[I8:12], weights[12:16]

        flat = lambda *rows: [r.reshape(-I1, width) for r in rows]
        h_rows = flat(oh_same, oh_other)
        done, *again = owner_recompute(dims, True, None, h_rows, flat(oa_same, oa_other), own_gains, rows_of)
        dx, _, od_same, od_other, og_same, og_other, oa_same, oa_other, dg_same, dg_other = backward_phase(
            dims, (acts, mids, qkv, ups, seeds), (rows_of[I0], nq, fq, td0, td1, to0, to1, tu0, tu1), home_gains, done, (oa_same, oa_other))
        _, *again = owner_recompute(dims, False, again, h_rows, flat(oa_same, oa_other), own_gains, rows_of)
        ups_own, qkv_own, ctx_own, n1, n2 = again
        d_rows, g_rows = flat(od_same, od_other), flat(og_same, og_other)
        d_qkv_rows, d_up_rows, hidden, d_inputs = owner_backward(dims, dx, d_rows, g_rows, ups_own, qkv_own, rows_of)
        d_qkv, d_out = attn_products(d_qkv_rows, ctx_own, n1, d_rows, w_out.shape[I1:])
        d_up, d_down = mlp_products(d_up_rows, hidden, n2, g_rows)
        weight_grads = (d_qkv.transpose(I3, I0, I1, I2), d_out, d_up, d_down)
        mine = jnp.sum(dg_same + dg_other, I1)
        loss = jnp.sum(loss_all) * (0.5 * norm_factor)

        return (loss.reshape(I1), d_inputs) + tuple(g[None] for g in weight_grads) + (mine[I0][None], mine[I1][None])

    return jax.shard_map(device_fn, mesh=mesh, in_specs=(act_spec, act_spec) + weight_specs, out_specs=(P('rep'), act_spec) + weight_specs, check_vma=False)
```

```python
import functools

import jax
import jax.numpy as jnp
from jax import lax
from jax.experimental import pallas as pl
from jax.experimental.pallas import tpu as pltpu
from jax.sharding import PartitionSpec as P

NORM_EPS = 1e-5
BF = jnp.bfloat16
F32 = jnp.float32
MESH = pl.DeviceIdType.MESH
ANY = pl.ANY


GELU_A = 0.7978845608028654
GELU_B = 0.044715
I0, I1, I2, I3, I4, I6, I8 = 0, 1, 2, 3, 4, 6, 8
CHUNK = 1024
BLOCK = 384
SUB = 256
DEPTH = 6
BACK_DEPTH = 6
KDEPTH = 3
HEAD_PAD = 128
VMEM_LIMIT = 67043328


def mm(a, b):
    return lax.dot_general(a, b, (((I1,), (I0,)), ((), ())), preferred_element_type=F32)


def mm_nt(a, b):
    return lax.dot_general(a, b, (((I1,), (I1,)), ((), ())), preferred_element_type=F32)


def mm_tn(a, b):
    return lax.dot_general(a, b, (((I0,), (I0,)), ((), ())), preferred_element_type=F32)


class Place:
    def __init__(self):
        self.tp = lax.axis_index('tp')
        self.stage = lax.axis_index('stage')
        self.core = self.stage % I2
        self.x_pos = self.stage // I2
        self.home = self.x_pos * (I3 - I2 * self.tp) + self.tp
        self.is_l = self.stage == self.home
        self.sib = self.stage + I1 - I2 * self.core

    def at(self, tp, stage):
        return {'tp': tp, 'stage': stage}

    @property
    def sibling(self):
        return self.at(self.tp, self.sib)

    @property
    def across(self):
        return self.at(I1 - self.tp, self.stage)

    @property
    def across_other(self):
        return self.at(I1 - self.tp, self.sib)

    def chain(self, delta):
        there = self.home + delta
        x_pos = there // I2
        tp = there % I2 + x_pos * (I1 - I2 * (there % I2))
        return self.at(tp, I2 * x_pos + self.core)


def entry_barrier(place):
    barrier = pltpu.get_barrier_semaphore()
    for d_tp in (I0, I1):
        for d_stage in range(I4):
            if d_tp or d_stage:
                tp = place.tp + d_tp - I2 * d_tp * place.tp
                stage = (place.stage + d_stage) % I4
                pl.semaphore_signal(barrier, inc=I1, device_id=place.at(tp, stage), device_id_type=MESH)
    pl.semaphore_wait(barrier, 7)


def remote(src, dst, send_sem, recv_sem, device_id):
    return pltpu.make_async_remote_copy(src_ref=src, dst_ref=dst, send_sem=send_sem, recv_sem=recv_sem, device_id=device_id, device_id_type=MESH)


def rows_loop(total, step, body):
    def run(i, carry):
        body(pl.ds(pl.multiple_of(i * step, step), step))
        return carry
    lax.fori_loop(I0, total // step, run, I0)


def norm_rows(src, gain_row, dst, total):
    def body(rows):
        v = src[rows, :].astype(F32)
        inv = lax.rsqrt(jnp.mean(v * v, axis=-I1, keepdims=True) + NORM_EPS)
        dst[rows, :] = (v * inv * gain_row).astype(BF)
    rows_loop(total, 32, body)


def gelu_gate(u):
    u2 = u * u
    t = jnp.tanh(u * (GELU_A + (GELU_A * GELU_B) * u2))
    return 0.5 * t + 0.5, u2


def gelu_slope(hidden, gate, u2):
    return gate + hidden * (1.0 - gate) * (2.0 * GELU_A + (6.0 * GELU_A * GELU_B) * u2)


def row_parts(heads, cut=128):
    return [(*(x[low:high] for x in queries), *(x[:high] for x in keys), low)
            for queries, keys in heads for low, high in ((I0, cut), (cut, queries[I0].shape[I0]))]


def softmax_parts(scores, starts):
    masked = []
    for s, start in zip(scores, starts):
        q_pos = lax.broadcasted_iota(jnp.int32, s.shape, I0) + start
        k_pos = lax.broadcasted_iota(jnp.int32, s.shape, I1)
        masked.append(jnp.where(k_pos <= q_pos, s, -1e30))
    tops = [jnp.max(s, axis=-I1, keepdims=True) for s in masked]
    powers = [jnp.exp(s - top) for s, top in zip(masked, tops)]
    scales = [1.0 / jnp.sum(e, axis=-I1, keepdims=True) for e in powers]
    return [e * r for e, r in zip(powers, scales)]


def join_keys(top, low, cut=128):
    return jnp.concatenate([top + low[:cut], low[cut:]], I0).astype(BF)


def attention_forward(heads, scale):
    units = row_parts([((q,), (k, v)) for q, k, v in heads])
    probs = softmax_parts([mm_nt(q, k) * scale for q, k, _, _ in units], [u[-I1] for u in units])
    parts = [mm(p.astype(BF), u[I2]) for p, u in zip(probs, units)]
    return [jnp.concatenate([a, b], I0).astype(BF) for a, b in zip(parts[I0::I2], parts[I1::I2])]


def attention_backward(heads, scale):
    units = row_parts([((q, dc), (k, v)) for q, k, v, dc in heads])
    scores = [mm_nt(q, k) * scale for q, _, k, _, _ in units]
    dps = [mm_nt(dc, v) for _, dc, _, v, _ in units]
    probs = softmax_parts(scores, [u[-I1] for u in units])
    dps = [dp.astype(BF).astype(F32) for dp in dps]
    deltas = [jnp.sum(dp * p, axis=-I1, keepdims=True) for dp, p in zip(dps, probs)]
    dvs = [mm_tn(p.astype(BF), u[I1]) for p, u in zip(probs, units)]
    dss = [p * (dp - delta) * scale for p, dp, delta in zip(probs, dps, deltas)]
    terms = []
    for ds in dss:
        hi = ds.astype(BF)
        rest = ds - hi.astype(F32)
        lo = rest.astype(BF)
        terms.append((hi, lo, (rest - lo.astype(F32)).astype(BF)))
    dqs = [mm(hi, u[I2]) + (mm(lo, u[I2]) + mm(tail, u[I2])) for (hi, lo, tail), u in zip(terms, units)]
    dks = [mm_tn(hi, u[I0]) + (mm_tn(lo, u[I0]) + mm_tn(tail, u[I0])) for (hi, lo, tail), u in zip(terms, units)]
    return [(jnp.concatenate([dqs[i], dqs[i + I1]], I0).astype(BF), join_keys(dks[i], dks[i + I1]), join_keys(dvs[i], dvs[i + I1]))
            for i in range(I0, len(units), I2)]


def lanes(offset, size):
    return pl.ds(pl.multiple_of(offset, 128), size)


def load_resident(buf, sem, halves):
    for c in range(I6):
        for condition, ref in halves[c // I3]:
            copy = pltpu.make_async_copy(ref.at[(c % I3) * CHUNK:(c % I3 + I1) * CHUNK, :], buf.at[c], sem.at[c])
            if condition is None:
                copy.start()
            else:
                pl.when(condition)(copy.start)


def load_heads(ref, index, dst, sem):
    for r in range(I8):
        rows = pl.ds(pl.multiple_of(index * 768 + r * 96, 96), 96)
        pltpu.make_async_copy(ref.at[rows, :], dst.at[r * 128:r * 128 + 96, :], sem).start()


class Stream:
    def __init__(self, buf, sem, depth, parts, total, by_heads):
        self.buf, self.sem, self.depth, self.parts, self.total, self.by_heads = buf, sem, depth, parts, total, by_heads
        self.per_tick = sum(p[I1] for p in parts)

    def copy_in(self, ref, index, slot):
        if not self.by_heads:
            pltpu.make_async_copy(ref.at[index], self.buf.at[slot], self.sem.at[slot]).start()
            return
        load_heads(ref, index, self.buf.at[slot], self.sem.at[slot])

    def start(self, seq):
        @pl.when(seq < self.total)
        def _():
            j = seq % self.per_tick
            slot = seq % self.depth
            base = I0
            for choices, chunks in self.parts:
                for condition, ref in choices:
                    here = (j >= base) & (j < base + chunks)
                    here = here if condition is None else here & condition

                    @pl.when(here)
                    def _(ref=ref, low=base):
                        self.copy_in(ref, j - low, slot)
                base += chunks

    def prime(self):
        for seq in range(self.depth):
            self.start(jnp.int32(seq))

    def wait(self, seq):
        slot = seq % self.depth
        ref = self.parts[I0][I0][I0][I1]
        if self.by_heads:
            pltpu.make_async_copy(ref.at[I0:768, :], self.buf.at[slot, I0:768, :], self.sem.at[slot]).wait()
        else:
            pltpu.make_async_copy(ref.at[I0], self.buf.at[slot], self.sem.at[slot]).wait()
        return self.buf.at[slot]


PIECES = [(0, 0, 0), (0, 0, 1), (0, 0, 2), (1, 0, 0), (2, 1, 0), (2, 1, 1), (2, 1, 2), (2, 1, 3), (3, 0, 0), (3, 0, 1), (3, 0, 2), (3, 0, 3)]


def piece(ref, axis, index):
    return ref.at[index * 768:(index + I1) * 768, :] if axis == I0 else ref.at[:, index * 768:(index + I1) * 768]


def weight_phase(place, is_r, own, near, far, turned, up_chunks, wn, wk, send_sem, y_send, d_send, near_sem, far_sem, load_sem, store_sem, chunk_sem):
    wk[...] = jnp.zeros_like(wk)

    @pl.when(place.is_l)
    def _():
        for i in range(I4):
            remote(own[i], near[i], send_sem.at[i], near_sem.at[i], place.sibling).start()

    @pl.when(is_r)
    def _():
        for c, (i, axis, index) in enumerate(PIECES):
            remote(piece(own[i], axis, index), piece(far[i], axis, index), y_send.at[i], far_sem.at[c], place.across_other).start()

    def load(i, refs, t, slot):
        for condition, ref in refs:
            def go(ref=ref):
                if i < I2:
                    for r in range(I2):
                        rows = pl.ds(pl.multiple_of(t * 192 + r * 96, 96), 96)
                        pltpu.make_async_copy(ref.at[rows, :], wk.at[I0, pl.ds(slot * SUB + r * 128, 96), :], load_sem.at[slot]).start()
                elif i == I2:
                    pltpu.make_async_copy(ref.at[:, lanes(t * SUB, SUB)], wn.at[slot, :, I0:SUB], load_sem.at[slot]).start()
                else:
                    rows = pl.ds(pl.multiple_of(t * SUB, SUB), SUB)
                    pltpu.make_async_copy(ref.at[rows, :], wk.at[I0, pl.ds(512 + slot * SUB, SUB), :], load_sem.at[slot]).start()
            if condition is None:
                go()
            else:
                pl.when(condition)(go)

    def loaded(i, refs, slot):
        ref = refs[I0][I1]
        if i < I2:
            pltpu.make_async_copy(ref.at[I0:192, :], wk.at[I0, I0:192, :], load_sem.at[slot]).wait()
        elif i == I2:
            pltpu.make_async_copy(ref.at[:, I0:SUB], wn.at[slot, :, I0:SUB], load_sem.at[slot]).wait()
        else:
            pltpu.make_async_copy(ref.at[I0:SUB, :], wk.at[I0, 512:768, :], load_sem.at[slot]).wait()

    def store(i, dst, t, slot):
        if i == I2:
            rows = pl.ds(pl.multiple_of(t * SUB, SUB), SUB)
            return pltpu.make_async_copy(wk.at[I1, pl.ds(slot * SUB, SUB), :], dst.at[rows, :], store_sem.at[slot])
        return pltpu.make_async_copy(wn.at[slot, :, SUB:512], dst.at[t // I4, :, lanes(t % I4 * SUB, SUB)], store_sem.at[slot])

    def keep(which, t, slot):
        return pltpu.make_async_copy(wn.at[slot, :, I0:SUB], up_chunks[which].at[t // I4, :, lanes(t % I4 * SUB, SUB)], chunk_sem.at[slot])

    def turn(i, refs, which, first, count):
        dst = turned[i][which]
        load(i, refs, first, I0)

        def step(n, c):
            slot = n % I2

            if i == I2:
                @pl.when(n > I0)
                def _():
                    keep(which, first + n - I1, I1 - slot).wait()

            @pl.when(n + I1 < count)
            def _():
                load(i, refs, first + n + I1, I1 - slot)
            loaded(i, refs, slot)
            if i == I2:
                keep(which, first + n, slot).start()

            @pl.when(n >= I2)
            def _():
                store(i, dst, first + n - I2, slot).wait()
            for b in range(I6):
                cut = slice(b * SUB, b * SUB + SUB)
                if i == I2:
                    wk[I1, pl.ds(pl.multiple_of(slot * SUB, SUB), SUB), cut] = wn[slot, cut, I0:SUB].T
                else:
                    base = I0 if i < I2 else 512
                    wn[slot, cut, SUB:512] = wk[I0, pl.ds(pl.multiple_of(base + slot * SUB, SUB), SUB), cut].T
            store(i, dst, first + n, slot).start()
            return c
        lax.fori_loop(I0, count, step, I0)
        for n in (count - I2, count - I1):
            store(i, dst, first + n, n % I2).wait()
        if i == I2:
            keep(which, first + count - I1, (count - I1) % I2).wait()

    counts = (12, I4, 12, 12)
    for i in range(I4):
        @pl.when(is_r)
        def _(i=i):
            remote(near[i], near[i], send_sem.at[i], near_sem.at[i], place.sibling).wait_recv()
        turn(i, [(place.is_l, own[i]), (is_r, near[i])], I0, I0, counts[i])
    done = [I0, I0, I0, I0]
    for c, (i, axis, index) in enumerate(PIECES):
        view = piece(far[i], axis, index)
        remote(view, view, d_send.at[i], far_sem.at[c], place.sibling).wait_recv()

        @pl.when(is_r)
        def _(i=i, c=c, view=view):
            remote(view, view, d_send.at[i], far_sem.at[c], place.sibling).start()
        count = I4 if i < I2 else I3
        turn(i, [(None, far[i])], I1, done[i], count)
        done[i] += count

    @pl.when(place.is_l)
    def _():
        for i in range(I4):
            remote(own[i], near[i], send_sem.at[i], near_sem.at[i], place.sibling).wait_send()

    @pl.when(is_r)
    def _():
        for i in range(I4):
            remote(own[i], far[i], y_send.at[i], far_sem.at[I0], place.across_other).wait_send()
            remote(far[i], far[i], d_send.at[i], far_sem.at[I0], place.sibling).wait_send()


def near_choices(place, own, near):
    return [(place.is_l, own), (jnp.logical_not(place.is_l), near)]


def forward_kernel(dims, x_ref, y_ref, wq, wo, wu, wd, own_gains,
                   a_s, h_s, qkv_s, u_s, g_s, oh_same, oh_other, oa_same, oa_other, og_same, og_other, loss_s, home_gains,
                   nq, no, nu, nd, fq, fo, fu, fd, tq0, to0, tu0, td0, tq1, to1, tu1, td1, uc0, uc1,
                   abuf, hbuf, obuf, nbuf, ybuf, sbuf, qkvbuf, ubuf, zbuf, ctxbuf, acc, lossbuf, losstile, gains, wres, wores, wn,
                   send_sem, y_send, d_send, near_sem, far_sem, t_load, t_store, t_keep,
                   act_sem, hop_f, keep_sem, save_sem, stream_n, res_sem, out_sem, big_sem, y_sem, s_sem,
                   os_sem, oo_sem, as_sem, ao_sem, gs_sem, go_sem, bulk, gain_sem, tiny):
    micro, seq, width, heads, head_dim, ffn = dims
    place = Place()
    is_first, is_last = place.home == I0, place.home == I3
    home02 = (place.home == I0) | (place.home == I2)
    is_r = jnp.logical_not(place.is_l)
    takes_x = (place.home == I1) & is_r
    half = heads // I2 * HEAD_PAD
    scale = head_dim ** -0.5
    norm_factor = 1.0 / (micro * I2 * seq * width)
    own, near, far = (wq, wo, wu, wd), (nq, no, nu, nd), (fq, fo, fu, fd)
    turned = ((tq0, tq1), (to0, to1), (tu0, tu1), (td0, td1))
    entry_barrier(place)

    @pl.when(place.is_l)
    def _():
        pltpu.make_async_copy(own_gains, gains, gain_sem.at[I0]).start()
        remote(own_gains, gains, gain_sem.at[I1], gain_sem.at[I0], place.sibling).start()

    @pl.when(is_first)
    def _():
        for m in range(micro):
            pltpu.make_async_copy(x_ref.at[m, place.core], abuf.at[m], act_sem.at[m]).start()
    weight_phase(place, is_r, own, near, far, turned, (uc0, uc1), wn, wores, send_sem, y_send, d_send, near_sem, far_sem, t_load, t_store, t_keep)
    pltpu.make_async_copy(own_gains, gains, gain_sem.at[I0]).wait()
    pltpu.make_async_copy(gains, home_gains, gain_sem.at[I0]).start()

    @pl.when(place.is_l)
    def _():
        remote(own_gains, gains, gain_sem.at[I1], gain_sem.at[I0], place.sibling).wait_send()

    def near_of(i):
        return near_choices(place, own[i], near[i])

    def saved(dst, index):
        return pltpu.make_async_copy(hbuf, dst, save_sem.at[index])

    sn = Stream(wn, stream_n, DEPTH, [([(None, tq0)], I3), ([(None, tq1)], I3), ([(None, uc0)], I3), ([(None, uc1)], I3)], micro * 12, False)
    for c, choices in enumerate((near_of(I1), [(None, fo)])):
        for condition, ref in choices:
            def go(ref=ref, c=c):
                load_heads(ref, I0, wores.at[c], out_sem.at[c])
            go() if condition is None else pl.when(condition)(go)
    sn.prime()
    load_resident(wres, res_sem, (near_of(I3), [(None, fd)]))
    lossbuf[...] = jnp.zeros_like(lossbuf)

    def qkv_out(m):
        return pltpu.make_async_copy(qkvbuf, qkv_s.at[m], big_sem.at[I0])

    def up_out(m):
        return pltpu.make_async_copy(ubuf, u_s.at[m], big_sem.at[I1])

    def act_out(m):
        return pltpu.make_async_copy(abuf.at[m], a_s.at[m], save_sem.at[I2])

    def hop_forward(m):
        return remote(obuf.at[m % I2], abuf.at[m], hop_f.at[m % I2], act_sem.at[m], place.chain(I1))

    def near_hand(src, dst_far, dst_own, sem, recv_sem):
        return (lambda: remote(src, dst_far, sem, recv_sem, place.sibling)), (lambda: pltpu.make_async_copy(src, dst_own, sem))

    def hand_out(m):
        return near_hand(obuf.at[m % I2], oa_other.at[m], oa_same.at[m], keep_sem.at[m % I2], ao_sem)

    def both_kinds(condition, copies, start):
        far_copy, own_copy = copies

        @pl.when(condition & place.is_l)
        def _():
            far_copy().start() if start else far_copy().wait_send()

        @pl.when(condition & is_r)
        def _():
            own_copy().start() if start else own_copy().wait()

    def x_out(m):
        return pltpu.make_async_copy(ybuf, oa_same.at[m], y_sem), pltpu.make_async_copy(sbuf, oa_other.at[m], s_sem)

    def seed_out(m):
        return pltpu.make_async_copy(sbuf, g_s.at[m], s_sem)

    def send_seed(m):
        seed_out(m).wait()

        @pl.when(place.is_l)
        def _():
            remote(g_s.at[m], og_same.at[m], bulk.at[I1], gs_sem, place.across).start()

        @pl.when(is_r)
        def _():
            remote(g_s.at[m], og_other.at[m], bulk.at[I1], go_sem, place.across_other).start()

    def forward_tick(m, carry):
        act, mid, out = abuf.at[m], hbuf, obuf.at[m % I2]
        pltpu.make_async_copy(x_ref.at[m, place.core], act, act_sem.at[m]).wait()
        act_out(m).start()

        @pl.when(place.is_l)
        def _():
            pltpu.make_async_copy(act, oa_same.at[m], as_sem).start()

        @pl.when(is_last)
        def _():
            pltpu.make_async_copy(y_ref.at[m, place.core], ybuf, y_sem).start()

        @pl.when(takes_x)
        def _():
            @pl.when(m > I0)
            def _():
                for copy in x_out(m):
                    copy.wait()
            for core, buf, sem in ((place.core, ybuf, y_sem), (I1 - place.core, sbuf, s_sem)):
                pltpu.make_async_copy(x_ref.at[m, core], buf, sem).start()
        norm_rows(act, gains[I0:I1, :], nbuf, seq)

        @pl.when(m > I0)
        def _():
            qkv_out(m).wait()

        def qkv_step(j, c):
            w = sn.wait(m * 12 + j)
            for n in range(I0, CHUNK, SUB):
                qkvbuf[:, lanes(j * CHUNK + n, SUB)] = mm(nbuf[...], w[:, n:n + SUB]).astype(BF)
            sn.start(m * 12 + j + DEPTH)
            return c
        lax.fori_loop(I0, I6, qkv_step, I0)
        qkv_out(m).start()
        act_out(m).wait()

        @pl.when(is_r)
        def _():
            remote(a_s.at[m], oa_other.at[m], bulk.at[I0], ao_sem, place.sibling).start()

        def head_step(i, c):
            base = i * (I3 * half)
            views = [[qkvbuf[:, lanes(base + t * half + r * HEAD_PAD, HEAD_PAD)] for t in range(I3)] for r in range(I8)]
            for r, context in enumerate(attention_forward(views, scale)):
                ctxbuf[:, lanes(i * half + r * HEAD_PAD, HEAD_PAD)] = context
            return c
        lax.fori_loop(I0, I2, head_step, I0)

        @pl.when(m == I0)
        def _():
            for c in range(I2):
                pltpu.make_async_copy(wo, wores.at[c, I0:768, :], out_sem.at[c]).wait()
        for n in range(I0, width, SUB):
            total = mm(ctxbuf[:, I0:half], wores[I0, :, n:n + SUB]) + mm(ctxbuf[:, half:I2 * half], wores[I1, :, n:n + SUB])
            mid[:, n:n + SUB] = (act[:, n:n + SUB].astype(F32) + total).astype(BF)
        saved(h_s.at[m], I0).start()

        @pl.when(place.is_l)
        def _():
            saved(oh_same.at[m], I1).start()
        norm_rows(mid, gains[I1:I2, :], nbuf, seq)

        @pl.when(m > I0)
        def _():
            up_out(m).wait()
        acc[...] = jnp.zeros_like(acc)

        def mlp_step(j, c):
            w = sn.wait(m * 12 + I6 + j)
            for n in range(I0, CHUNK, SUB):
                u = mm(nbuf[...], w[:, n:n + SUB]).astype(BF)
                ubuf[:, lanes(j * CHUNK + n, SUB)] = u
                uf = u.astype(F32)
                zbuf[:, n:n + SUB] = (uf * gelu_gate(uf)[I0]).astype(BF)
            sn.start(m * 12 + I6 + j + DEPTH)

            @pl.when(m == I0)
            def _():
                pltpu.make_async_copy(wd.at[I0:CHUNK, :], wres.at[j], res_sem.at[j]).wait()
            for n in range(I0, width, SUB):
                acc[:, n:n + SUB] += mm(zbuf[...], wres[j, :, n:n + SUB])
            return c
        lax.fori_loop(I0, I6, mlp_step, I0)
        up_out(m).start()

        @pl.when((m > I1) & jnp.logical_not(is_last))
        def _():
            hop_forward(m).wait_send()

        both_kinds((m > I1) & home02, hand_out(m), False)

        def finish(rows):
            out[rows, :] = (mid[rows, :].astype(F32) + acc[rows, :]).astype(BF)
        rows_loop(seq, 32, finish)

        @pl.when(jnp.logical_not(is_last))
        def _():
            hop_forward(m).start()

        both_kinds(home02, hand_out(m), True)

        @pl.when(is_last)
        def _():
            pltpu.make_async_copy(y_ref.at[m, place.core], ybuf, y_sem).wait()

            @pl.when(m > I0)
            def _():
                send_seed(m - I1)

            def seed(rows):
                error = out[rows, :].astype(F32) - ybuf[rows, :].astype(F32)
                sbuf[rows, :] = (error * norm_factor).astype(BF)
                lossbuf[...] += jnp.sum((error * error).reshape(I4, I8, width), axis=I0)
            rows_loop(seq, 32, seed)
            seed_out(m).start()

        @pl.when(takes_x)
        def _():
            for core, buf, sem in ((place.core, ybuf, y_sem), (I1 - place.core, sbuf, s_sem)):
                pltpu.make_async_copy(x_ref.at[m, core], buf, sem).wait()
            for copy in x_out(m):
                copy.start()

        saved(h_s.at[m], I0).wait()

        @pl.when(place.is_l)
        def _():
            saved(oh_same.at[m], I1).wait()
            remote(h_s.at[m], oh_same.at[m], bulk.at[I2], os_sem, place.across).start()

        @pl.when(is_r)
        def _():
            remote(h_s.at[m], oh_other.at[m], bulk.at[I2], oo_sem, place.sibling).start()
            remote(h_s.at[m], oh_other.at[m], bulk.at[I3], oo_sem, place.across_other).start()
        return carry

    lax.fori_loop(I0, micro, forward_tick, I0)

    @pl.when(is_last)
    def _():
        total = lossbuf[:, I0:128]
        for n in range(128, width, 128):
            total = total + lossbuf[:, n:n + 128]
        losstile[...] = total
        pltpu.make_async_copy(losstile, loss_s, tiny).start()
    for copy in (qkv_out(micro - I1), up_out(micro - I1)):
        copy.wait()

    @pl.when(jnp.logical_not(is_last))
    def _():
        for m in (micro - I2, micro - I1):
            hop_forward(m).wait_send()
    for m in (micro - I2, micro - I1):
        both_kinds(home02, hand_out(m), False)

    @pl.when(is_last)
    def _():
        send_seed(micro - I1)
        pltpu.make_async_copy(losstile, loss_s, tiny).wait()

    @pl.when(takes_x)
    def _():
        for copy in x_out(micro - I1):
            copy.wait()
    pltpu.make_async_copy(gains, home_gains, gain_sem.at[I0]).wait()
    sent, got = drain(place)
    sent(h_s, bulk.at[I2])
    got(oh_other, oo_sem)

    @pl.when(is_last)
    def _():
        sent(g_s, bulk.at[I1])

    @pl.when((place.home == I2) & is_r)
    def _():
        got(og_same, gs_sem)
        got(og_other, go_sem)

    @pl.when(is_r)
    def _():
        sent(a_s, bulk.at[I0])
        sent(h_s, bulk.at[I3])
        got(oh_same, os_sem)

    @pl.when(place.is_l)
    def _():
        got(oa_same, as_sem)

    @pl.when(place.is_l | home02)
    def _():
        got(oa_other, ao_sem)


def drain(place):
    def sent(buf, sem):
        remote(buf, buf, sem, sem, place.sibling).wait_send()

    def got(dst, sem):
        pltpu.make_async_copy(dst, dst, sem).wait()
    return sent, got


def backward_kernel(dims, a_s, h_s, qkv_s, u_s, g_s, wq, nq, fq, td0, td1, to0, to1, tu0, tu1, gains, loss_s, after, *refs):
    (dx_s, m_s, od_same, od_other, og_same, og_other, oa_same, oa_other, dg_same, dg_other, loss_all,
     gbuf, hbuf, obuf, qkvbuf, ubuf, habuf, zbuf, ctxbuf, dqkvbuf, acc, accg, wres, wn, wk,
     grad_sem, hop_b, back_sem, dx_sem, dx_send, save_sem, stream_n, stream_k, res_sem, load_sem,
     ds_sem, do_sem, gs_sem, go_sem, as_sem, ao_sem, bulk, tiny, loss_sem) = refs[I4:]
    micro, seq, width, heads, head_dim, ffn = dims
    place = Place()
    is_first, is_last = place.home == I0, place.home == I3
    home13 = (place.home == I1) | is_last
    is_r = jnp.logical_not(place.is_l)
    half = heads // I2 * HEAD_PAD
    scale = head_dim ** -0.5

    barrier = pltpu.get_barrier_semaphore()
    along_x = (place.home == I1) | (place.home == I2)
    for there in (place.sibling, place.across, place.across_other):
        pl.semaphore_signal(barrier, inc=I1, device_id=there, device_id_type=MESH)

    @pl.when(along_x)
    def _():
        pl.semaphore_signal(barrier, inc=I1, device_id=place.at(place.tp, (place.stage + I2) % I4), device_id_type=MESH)

    @pl.when(is_last)
    def _():
        for m in range(micro):
            pltpu.make_async_copy(g_s.at[m], gbuf.at[m], grad_sem.at[m]).start()
    wk[...] = jnp.zeros_like(wk)
    bn = Stream(wn, stream_n, BACK_DEPTH, [([(None, td0)], I3), ([(None, td1)], I3), ([(None, to0)], I1), ([(None, to1)], I1)], micro * I8, False)
    bk = Stream(wk, stream_k, KDEPTH, [(near_choices(place, wq, nq), I3), ([(None, fq)], I3)], micro * I6, True)
    bn.prime()
    bk.prime()
    load_resident(wres, res_sem, ([(None, tu0)], [(None, tu1)]))

    def saved(dst, index):
        return pltpu.make_async_copy(hbuf, dst, save_sem)

    def both_kinds(condition, copies, start):
        far_copy, own_copy = copies

        @pl.when(condition & place.is_l)
        def _():
            far_copy().start() if start else far_copy().wait_send()

        @pl.when(condition & is_r)
        def _():
            own_copy().start() if start else own_copy().wait()

    def near_hand(src, dst_far, dst_own, sem, recv_sem):
        return (lambda: remote(src, dst_far, sem, recv_sem, place.sibling)), (lambda: pltpu.make_async_copy(src, dst_own, sem))

    def loads(i):
        m = micro - I1 - i
        return [pltpu.make_async_copy(src.at[m], dst, load_sem.at[k])
                for k, (src, dst) in enumerate(((u_s, ubuf), (qkv_s, qkvbuf), (h_s, habuf.at[I0]), (a_s, habuf.at[I1])))]

    def load_next(i, k):
        @pl.when(i + I1 < micro)
        def _():
            loads(i + I1)[k].start()

    for copy in loads(I0):
        copy.start()
    accg[...] = jnp.zeros_like(accg)

    def norm_back(index, x, base, dst, gain_row):
        def body(rows):
            xf = x[rows, :].astype(F32)
            dy = acc[rows, :].astype(BF).astype(F32)
            inv = lax.rsqrt(jnp.mean(xf * xf, axis=-I1, keepdims=True) + NORM_EPS)
            xn = xf * inv
            accg[index] += jnp.sum((dy * xn).reshape(I4, I8, width), axis=I0)
            dyg = dy * gain_row
            dx = inv * (dyg - xn * jnp.mean(dyg * xn, axis=-I1, keepdims=True))
            dst[rows, :] = (base[rows, :].astype(F32) + dx).astype(BF)
        rows_loop(seq, 32, body)

    def hop_back(i):
        m = micro - I1 - i
        return remote(obuf.at[i % I2], gbuf.at[m], hop_b.at[i % I2], grad_sem.at[m], place.chain(-I1))

    def hand_back(i):
        m = micro - I1 - i
        return near_hand(obuf.at[i % I2], og_other.at[m], og_same.at[m], back_sem.at[i % I2], go_sem)

    def keep_dx(i):
        return pltpu.make_async_copy(obuf.at[i % I2], dx_s.at[micro - I1 - i], back_sem.at[i % I2])

    def back_ready(i):
        both_kinds((i > I1) & home13, hand_back(i), False)

        @pl.when((i > I1) & is_first)
        def _():
            keep_dx(i).wait()
            dx_to_b(i).wait_send()

        @pl.when((i > I1) & jnp.logical_not(is_first))
        def _():
            hop_back(i).wait_send()

    def pass_loss(tile):
        @pl.when(jnp.logical_not(is_first))
        def _():
            remote(tile, loss_all.at[place.core], loss_sem.at[I0], loss_sem.at[I1], place.chain(-I1)).start()
        remote(tile, loss_all.at[place.core], loss_sem.at[I2], loss_sem.at[I3], place.sibling).start()

    def dx_to_b(i):
        return remote(obuf.at[i % I2], dx_s.at[micro - I1 - i], dx_send.at[i % I2], dx_sem, place.across)

    def backward_tick(i, carry):
        m = micro - I1 - i
        slot = i % I2
        grad, dmid, prev = gbuf.at[m], hbuf, obuf.at[slot]
        u_now, qkv_now, h_now, a_now = ubuf, qkvbuf, habuf.at[I0], habuf.at[I1]

        pltpu.make_async_copy(g_s.at[m], grad, grad_sem.at[m]).wait()

        @pl.when(place.is_l)
        def _():
            pltpu.make_async_copy(grad, og_same.at[m], gs_sem).start()
        load_u, load_qkv, load_h, load_a = loads(i)
        load_u.wait()
        acc[...] = jnp.zeros_like(acc)

        def mlp_step(j, c):
            w = bn.wait(i * I8 + j)
            for n in range(I0, CHUNK, SUB):
                dz = mm(grad[...], w[:, n:n + SUB]).astype(BF).astype(F32)
                u = u_now[:, lanes(j * CHUNK + n, SUB)].astype(F32)
                gate, u2 = gelu_gate(u)
                zbuf[:, n:n + SUB] = (dz * gelu_slope(u * gate, gate, u2)).astype(BF)
            bn.start(i * I8 + j + BACK_DEPTH)

            @pl.when(i == I0)
            def _():
                pltpu.make_async_copy(tu0.at[I0:CHUNK, :], wres.at[j], res_sem.at[j]).wait()
            for n in range(I0, width, SUB):
                acc[:, n:n + SUB] += mm(zbuf[...], wres[j, :, n:n + SUB])
            return c
        lax.fori_loop(I0, I6, mlp_step, I0)
        load_next(i, I0)
        load_h.wait()
        norm_back(I1, h_now, grad, dmid, gains[I1:I2, :])
        load_next(i, I2)

        @pl.when(place.is_l)
        def _():
            saved(od_same.at[m], I0).start()

        @pl.when(is_r)
        def _():
            saved(m_s.at[m], I0).start()
        for c in range(I2):
            w = bn.wait(i * I8 + I6 + c)
            for n in range(I0, CHUNK, SUB):
                ctxbuf[:, c * CHUNK + n:c * CHUNK + n + SUB] = mm(dmid[...], w[:, n:n + SUB]).astype(BF)
            bn.start(i * I8 + I6 + c + BACK_DEPTH)
        load_qkv.wait()

        def head_step(t, c):
            base = (t // I2) * (I3 * half) + (t % I2) * (I4 * HEAD_PAD)
            at = [[lanes(base + part * half + r * HEAD_PAD, HEAD_PAD) for part in range(I3)] for r in range(I4)]
            group = [(*(qkv_now[:, p] for p in at[r]), ctxbuf[:, lanes((t * I4 + r) * HEAD_PAD, HEAD_PAD)]) for r in range(I4)]
            for r, grads in enumerate(attention_backward(group, scale)):
                for p, value in zip(at[r], grads):
                    dqkvbuf[:, p] = value
            return c
        lax.fori_loop(I0, heads // I4, head_step, I0)
        load_next(i, I1)
        acc[...] = jnp.zeros_like(acc)

        def qkv_step(j, c):
            w = bk.wait(i * I6 + j)
            for n in range(I0, width, SUB):
                acc[:, n:n + SUB] += mm(dqkvbuf[:, lanes(j * CHUNK, CHUNK)], w[:, n:n + SUB])
            bk.start(i * I6 + j + KDEPTH)
            return c
        lax.fori_loop(I0, I6, qkv_step, I0)
        load_a.wait()
        back_ready(i)
        norm_back(I0, a_now, dmid, prev, gains[I0:I1, :])
        load_next(i, I3)

        @pl.when(i == I0)
        def _():
            pl.semaphore_wait(barrier, I3 + (place.home + I1) // I2 % I2)

            @pl.when(is_last)
            def _():
                pass_loss(loss_s)

            @pl.when((place.home == I2) & place.is_l)
            def _():
                for t in range(micro):
                    remote(a_s.at[t], oa_same.at[t], bulk.at[I8], as_sem, place.across).start()

            @pl.when((place.home == I2) & is_r)
            def _():
                for t in range(micro):
                    remote(a_s.at[t], oa_other.at[t], bulk.at[I8], ao_sem, place.across_other).start()

        @pl.when(jnp.logical_not(is_first))
        def _():
            hop_back(i).start()

        @pl.when(is_first)
        def _():
            keep_dx(i).start()
            dx_to_b(i).start()
        both_kinds(home13, hand_back(i), True)

        @pl.when(place.is_l)
        def _():
            saved(od_same.at[m], I0).wait()
            remote(od_same.at[m], od_same.at[m], bulk.at[I6], ds_sem, place.across).start()

        @pl.when(is_r)
        def _():
            remote(grad, og_other.at[m], bulk.at[5], go_sem, place.sibling).start()
            saved(m_s.at[m], I0).wait()
            remote(m_s.at[m], od_other.at[m], bulk.at[I6], do_sem, place.sibling).start()
            remote(m_s.at[m], od_other.at[m], bulk.at[7], do_sem, place.across_other).start()

        far_grad(m, (place.home == I1) & (i % I2 == I0))
        return carry

    def far_grad(m, condition):
        @pl.when(condition & place.is_l)
        def _():
            remote(gbuf.at[m], og_same.at[m], bulk.at[I4], gs_sem, place.across).start()

        @pl.when(condition & is_r)
        def _():
            remote(gbuf.at[m], og_other.at[m], bulk.at[I4], go_sem, place.across_other).start()

    lax.fori_loop(I0, micro, backward_tick, I0)
    for i in range(I1, micro, I2):
        far_grad(micro - I1 - i, place.home == I1)
    loss_mine = loss_all.at[place.core]

    @pl.when(is_last)
    def _():
        own_loss = pltpu.make_async_copy(loss_s, loss_mine, loss_sem.at[I1])
        own_loss.start()
        own_loss.wait()

    @pl.when(jnp.logical_not(is_last))
    def _():
        remote(loss_mine, loss_mine, loss_sem.at[I0], loss_sem.at[I1], place.sibling).wait_recv()
        pass_loss(loss_mine)

    @pl.when(place.is_l)
    def _():
        pltpu.make_async_copy(accg, dg_same, tiny.at[I0]).start()
        remote(accg, dg_same, tiny.at[I1], tiny.at[I0], place.across).start()

    @pl.when(is_r)
    def _():
        remote(accg, dg_other, tiny.at[I1], tiny.at[I4], place.sibling).start()
        remote(accg, dg_other, tiny.at[I2], tiny.at[I4], place.across_other).start()

    for i in (micro - I2, micro - I1):
        back_ready(jnp.int32(i))

    sent, got = drain(place)
    sent(m_s, bulk.at[I6])

    @pl.when(is_r)
    def _():
        sent(gbuf, bulk.at[5])
        sent(m_s, bulk.at[7])
        remote(accg, dg_other, tiny.at[I2], tiny.at[I4], place.sibling).wait_send()

    @pl.when(place.home == I1)
    def _():
        sent(gbuf, bulk.at[I4])
        got(dx_s, dx_sem)

    @pl.when(jnp.logical_not(is_first))
    def _():
        remote(loss_mine, loss_mine, loss_sem.at[I0], loss_sem.at[I1], place.sibling).wait_send()
    remote(loss_mine, loss_mine, loss_sem.at[I2], loss_sem.at[I3], place.sibling).wait_send()
    remote(loss_mine, loss_mine, loss_sem.at[I2], loss_sem.at[I3], place.sibling).wait_recv()

    @pl.when(place.home == I2)
    def _():
        sent(a_s, bulk.at[I8])

    remote(accg, dg_other, tiny.at[I1], tiny.at[I4], place.sibling).wait_send()
    got(od_other, do_sem)

    @pl.when(place.is_l | (place.home != I2))
    def _():
        got(og_other, go_sem)
    got(dg_same, tiny.at[I0])
    got(dg_other, tiny.at[I4])

    @pl.when(is_r)
    def _():
        got(od_same, ds_sem)

    @pl.when(place.is_l | is_first)
    def _():
        got(og_same, gs_sem)

    @pl.when(is_last & is_r)
    def _():
        got(oa_same, as_sem)
        got(oa_other, ao_sem)


def shapes(*dims_list):
    return [jax.ShapeDtypeStruct(d, BF) for d in dims_list]


def forward_phase(dims, x, y, own, own_gains):
    micro, seq, width, heads, head_dim, ffn = dims
    half = heads // I2 * HEAD_PAD
    act = (micro, seq, width)
    raw = [w.shape for w in own]
    turned = [(I3, width, CHUNK), (I1, width, CHUNK), (ffn // I2, width), (I3, width, CHUNK)]
    out_shape = shapes(act, act, (micro, seq, I6 * half), (micro, seq, ffn), *[act] * 7)
    out_shape += [jax.ShapeDtypeStruct(s, F32) for s in ((I8, 128), own_gains.shape)]
    out_shape += shapes(*raw, *raw, *turned, *turned, turned[I0], turned[I0])
    any_spec = pl.BlockSpec(memory_space=ANY)
    vmem, dma = pltpu.VMEM, pltpu.SemaphoreType.DMA
    row = vmem((seq, width), BF)
    scratch = [
        vmem(act, BF), row, vmem((I2, seq, width), BF), row, row, row, vmem((seq, I6 * half), BF), vmem((seq, ffn), BF), vmem((seq, CHUNK), BF),
        vmem((seq, I2 * half), BF), vmem((seq, width), F32), vmem((I8, width), F32), vmem((I8, 128), F32), vmem((I2, width), F32),
        vmem((I6, CHUNK, width), BF), vmem((I2, CHUNK, width), BF), vmem((DEPTH, width, CHUNK), BF),
        dma((I4,)), dma((I4,)), dma((I4,)), dma((I4,)), dma((12,)), dma((I2,)), dma((I2,)), dma((I2,)),
        dma((micro,)), dma((I2,)), dma((I2,)), dma((I3,)), dma((DEPTH,)), dma((I6,)), dma((I2,)), dma((I2,)), dma(()), dma(()),
        dma(()), dma(()), dma(()), dma(()), dma(()), dma(()), dma((I4,)), dma((I2,)), dma(()),
    ]
    return pl.pallas_call(
        functools.partial(forward_kernel, dims),
        out_shape=tuple(out_shape),
        in_specs=[any_spec] * I6 + [pl.BlockSpec(memory_space=vmem)],
        out_specs=(any_spec,) * len(out_shape),
        scratch_shapes=scratch,
        compiler_params=pltpu.CompilerParams(collective_id=I0, has_side_effects=True, vmem_limit_bytes=VMEM_LIMIT),
        name='forward_phase',
    )(x, y, *own, own_gains)


def backward_phase(dims, saved, weights, gains, loss, after, placed):
    micro, seq, width, heads, head_dim, ffn = dims
    half = heads // I2 * HEAD_PAD
    act = (micro, seq, width)
    out_shape = shapes(*[act] * I8) + [jax.ShapeDtypeStruct((I2, I8, width), F32)] * I2 + [jax.ShapeDtypeStruct((I2, I8, 128), F32)]
    any_spec = pl.BlockSpec(memory_space=ANY)
    vmem, dma = pltpu.VMEM, pltpu.SemaphoreType.DMA
    scratch = [
        vmem(act, BF), vmem((seq, width), BF), vmem((I2, seq, width), BF), vmem((seq, I6 * half), BF), vmem((seq, ffn), BF),
        vmem((I2, seq, width), BF), vmem((seq, CHUNK), BF), vmem((seq, I2 * half), BF), vmem((seq, I6 * half), BF), vmem((seq, width), F32),
        vmem((I2, I8, width), F32), vmem((I6, CHUNK, width), BF), vmem((BACK_DEPTH, width, CHUNK), BF), vmem((KDEPTH, CHUNK, width), BF),
        dma((micro,)), dma((I2,)), dma((I2,)), dma(()), dma((I2,)), dma(()), dma((BACK_DEPTH,)), dma((KDEPTH,)), dma((I6,)), dma((I4,)),
        dma(()), dma(()), dma(()), dma(()), dma(()), dma(()), dma((9,)), dma((5,)), dma((I4,)),
    ]
    return pl.pallas_call(
        functools.partial(backward_kernel, dims),
        out_shape=tuple(out_shape),
        in_specs=[any_spec] * 14 + [pl.BlockSpec(memory_space=vmem)] * I2 + [any_spec] * 5,
        out_specs=(any_spec,) * len(out_shape),
        scratch_shapes=scratch,
        input_output_aliases={17: I4, 18: 5, 19: I6, 20: 7},
        compiler_params=pltpu.CompilerParams(collective_id=I1, has_side_effects=True, vmem_limit_bytes=VMEM_LIMIT),
        name='backward_phase',
    )(*saved, *weights, gains, loss, after, *placed)


def recompute_kernel(dims, early, h_same, h_other, a_same, a_other, gains, wq, wu, *refs):
    (done, u_o, qkv_o, ctx_o, n1_o, n2_o), (wqbuf, wubuf, count, sem) = refs[-10:-I4], refs[-I4:]
    micro, seq, width, heads, head_dim, ffn = dims
    place = Place()
    scale = head_dim ** -0.5
    half = heads // I2 * HEAD_PAD
    steps = I2 * micro * seq // BLOCK

    def body(hs, ho, rs, ro, u, qkv, ctx, n1, n2):
        step = count[I0]
        count[I0] = step + I1
        for low, high, gain, dst in ((hs, ho, gains[I1:I2, :], n2), (rs, ro, gains[I0:I1, :], n1)):
            @pl.when(step < steps // I2)
            def _(low=low, gain=gain, dst=dst):
                norm_rows(low, gain, dst, BLOCK)

            @pl.when(step >= steps // I2)
            def _(high=high, gain=gain, dst=dst):
                norm_rows(high, gain, dst, BLOCK)

        def qkv_step(j, c):
            rows = pl.ds(pl.multiple_of(j * SUB, SUB), SUB)
            qkv[:, lanes(j * SUB, SUB)] = mm_nt(n1[...], wqbuf[rows, :]).astype(BF)
            u[:, lanes(j * SUB, SUB)] = mm(n2[...], wubuf[:, lanes(j * SUB, SUB)]).astype(BF)
            return c
        lax.fori_loop(I0, I3 * half // SUB, qkv_step, I0)

        def head_step(j, c):
            at = [(pl.ds(s, seq), r * HEAD_PAD) for s in range(I0, BLOCK, seq) for r in range(I4)]
            base = j * (I4 * HEAD_PAD)
            views = [[qkv[rows, lanes(base + t * half + col, HEAD_PAD)] for t in range(I3)] for rows, col in at]
            for (rows, col), context in zip(at, attention_forward(views, scale)):
                ctx[rows, lanes(base + col, HEAD_PAD)] = context
            return c
        lax.fori_loop(I0, I2, head_step, I0)

    @pl.when(place.home < I2 if early else place.home > I1)
    def _():
        wqbuf[...] = jnp.zeros_like(wqbuf)
        for t in range(I3):
            load_heads(wq, t, wqbuf.at[pl.ds(t * CHUNK, CHUNK)], sem.at[I0])
        up = pltpu.make_async_copy(wu, wubuf, sem.at[I1])
        up.start()
        up.wait()
        pltpu.make_async_copy(wq, wqbuf.at[I0:wq.shape[I0]], sem.at[I0]).wait()
        count[I0] = I0
        low = pl.BlockSpec((BLOCK, width), lambda i: (jnp.minimum(i, steps // I2 - I1), I0))
        high = pl.BlockSpec((BLOCK, width), lambda i: (jnp.maximum(i - steps // I2, I0), I0))
        block = lambda n: pl.BlockSpec((BLOCK, n), lambda i: (i, I0))
        pltpu.emit_pipeline(body, grid=(steps,), in_specs=[low, high, low, high],
                            out_specs=[block(ffn // I2), block(I3 * half), block(half), block(width), block(width)])(
            h_same, h_other, a_same, a_other, u_o, qkv_o, ctx_o, n1_o, n2_o)


def owner_recompute(dims, early, again, h_rows, a_rows, gains, own):
    micro, seq, width, heads, head_dim, ffn = dims
    half = heads // I2 * HEAD_PAD
    tokens = I2 * micro * seq
    any_spec = pl.BlockSpec(memory_space=ANY)
    vmem = pltpu.VMEM
    earlier = () if early else tuple(again)
    return pl.pallas_call(
        functools.partial(recompute_kernel, dims, early),
        out_shape=(jax.ShapeDtypeStruct((I8, 128), F32), *shapes((tokens, ffn // I2), (tokens, I3 * half), (tokens, half), (tokens, width), (tokens, width))),
        in_specs=[any_spec] * I4 + [pl.BlockSpec(memory_space=vmem)] + [any_spec] * (I2 + len(earlier)),
        out_specs=(any_spec,) * I6,
        scratch_shapes=[vmem((I3 * half, width), BF), vmem((width, ffn // I2), BF), pltpu.SMEM((I1,), jnp.int32), pltpu.SemaphoreType.DMA((I2,))],
        input_output_aliases={7 + i: I1 + i for i in range(len(earlier))},
        compiler_params=pltpu.CompilerParams(has_side_effects=True, vmem_limit_bytes=VMEM_LIMIT),
        name='owner_recompute',
    )(*h_rows, *a_rows, gains, own[I0], own[I2], *earlier)


def spread_dx(step, last, dx, d_in, bounce, here_sem, parent_sem, sib_sem, send_sems):
    place = Place()
    micro = dx.shape[I0]
    along_x = place.at(place.tp, (place.stage + I2) % I4)
    barrier = pltpu.get_barrier_semaphore()
    is_leaf = place.home > I1

    def block(m):
        return d_in.at[m, place.core]

    def to_sibling(m, src):
        remote(src, block(m), send_sems.at[I0], sib_sem, place.sibling).start()

    @pl.when(step == I0)
    def _():
        pl.semaphore_signal(barrier, inc=I1, device_id=place.sibling, device_id_type=MESH)

        @pl.when(is_leaf)
        def _():
            pl.semaphore_signal(barrier, inc=I1, device_id=along_x, device_id_type=MESH)

    @pl.when((step == I1) & jnp.logical_not(is_leaf))
    def _():
        pl.semaphore_wait(barrier, I2)
        for m in reversed(range(micro)):
            remote(dx.at[m], block(m), send_sems.at[I1], parent_sem.at[m], along_x).start()
            to_sibling(m, dx.at[m])
        pltpu.make_async_copy(dx, bounce, here_sem).start()

    @pl.when((step == I2) & jnp.logical_not(is_leaf))
    def _():
        pltpu.make_async_copy(dx, bounce, here_sem).wait()
        for m in range(micro):
            pltpu.make_async_copy(bounce.at[m], block(m), here_sem).start()

    @pl.when((step == last) & is_leaf)
    def _():
        pl.semaphore_wait(barrier, I1)
        for m in reversed(range(micro)):
            remote(block(m), block(m), send_sems.at[I0], parent_sem.at[m], place.sibling).wait_recv()
            to_sibling(m, block(m))

    @pl.when(step == last)
    def _():
        remote(dx, dx, send_sems.at[I0], sib_sem, place.sibling).wait_send()

        @pl.when(jnp.logical_not(is_leaf))
        def _():
            remote(dx, dx, send_sems.at[I1], sib_sem, place.sibling).wait_send()
            pltpu.make_async_copy(dx, dx, here_sem).wait()
        remote(dx, dx, send_sems.at[I0], sib_sem, place.sibling).wait_recv()


def owner_backward_kernel(dims, dx, ds, do, gs, go, u, qkv, wo, wd, dqkv, dup, z, d_in,
                          dmid, grad, dctx, wobuf, bounce, sem, here_sem, parent_sem, sib_sem, send_sems):
    micro, seq, width, heads, head_dim, ffn = dims
    half = heads // I2 * HEAD_PAD
    scale = head_dim ** -0.5
    step, steps = pl.program_id(I0), pl.num_programs(I0)
    spread_dx(step, steps - I1, dx, d_in, bounce, here_sem, parent_sem, sib_sem, send_sems)

    @pl.when(step == I0)
    def _():
        wobuf[...] = jnp.zeros_like(wobuf)
        load_heads(wo, I0, wobuf, sem)
        pltpu.make_async_copy(wo, wobuf.at[I0:wo.shape[I0]], sem).wait()
    for near, far, dst in ((ds, do, dmid), (gs, go, grad)):
        @pl.when(step < steps // I2)
        def _(near=near, dst=dst):
            dst[...] = near[...]

        @pl.when(step >= steps // I2)
        def _(far=far, dst=dst):
            dst[...] = far[...]

    def ctx_step(j, c):
        rows = pl.ds(pl.multiple_of(j * SUB, SUB), SUB)
        dctx[:, lanes(j * SUB, SUB)] = mm_nt(dmid[...], wobuf[rows, :]).astype(BF)
        return c
    lax.fori_loop(I0, half // SUB, ctx_step, I0)

    def mlp_step(j, c):
        rows = pl.ds(pl.multiple_of(j * SUB, SUB), SUB)
        cols = lanes(j * SUB, SUB)
        dz = mm_nt(grad[...], wd[rows, :]).astype(BF).astype(F32)
        up = u[:, cols].astype(F32)
        gate, up2 = gelu_gate(up)
        hidden = up * gate
        z[:, cols] = hidden.astype(BF)
        dup[:, cols] = (dz * gelu_slope(hidden, gate, up2)).astype(BF)
        return c
    lax.fori_loop(I0, ffn // I2 // SUB, mlp_step, I0)

    def head_step(j, c):
        base = j * (I2 * HEAD_PAD)
        at = [(pl.ds(s, seq), base + r * HEAD_PAD) for s in range(I0, BLOCK, seq) for r in range(I2)]
        group = [(*(qkv[rows, lanes(t * half + col, HEAD_PAD)] for t in range(I3)), dctx[rows, lanes(col, HEAD_PAD)]) for rows, col in at]
        for (rows, col), grads in zip(at, attention_backward(group, scale)):
            for t, value in enumerate(grads):
                dqkv[rows, lanes(t * half + col, HEAD_PAD)] = value
        return c
    lax.fori_loop(I0, heads // I4, head_step, I0)


def owner_backward(dims, dx, d_rows, g_rows, ups, qkv, own):
    micro, seq, width, heads, head_dim, ffn = dims
    half = heads // I2 * HEAD_PAD
    tokens = I2 * micro * seq
    steps = tokens // BLOCK
    vmem, dma = pltpu.VMEM, pltpu.SemaphoreType.DMA
    any_spec = pl.BlockSpec(memory_space=ANY)
    low = pl.BlockSpec((BLOCK, width), lambda i: (jnp.minimum(i, steps // I2 - I1), I0))
    high = pl.BlockSpec((BLOCK, width), lambda i: (jnp.maximum(i - steps // I2, I0), I0))
    block = lambda n: pl.BlockSpec((BLOCK, n), lambda i: (i, I0))
    return pl.pallas_call(
        functools.partial(owner_backward_kernel, dims),
        grid=(steps,),
        out_shape=tuple(shapes((tokens, I3 * half), (tokens, ffn // I2), (tokens, ffn // I2), (micro, I2, seq, width))),
        in_specs=[any_spec, low, high, low, high, block(ffn // I2), block(I3 * half), any_spec, pl.BlockSpec((ffn // I2, width), lambda i: (I0, I0))],
        out_specs=(block(I3 * half), block(ffn // I2), block(ffn // I2), any_spec),
        scratch_shapes=[vmem((BLOCK, width), BF), vmem((BLOCK, width), BF), vmem((BLOCK, half), BF), vmem((half, width), BF), vmem((micro, seq, width), BF),
                        dma(()), dma(()), dma((micro,)), dma(()), dma((I2,))],
        compiler_params=pltpu.CompilerParams(collective_id=I2, has_side_effects=True, vmem_limit_bytes=VMEM_LIMIT),
        name='owner_backward',
    )(dx, *d_rows, *g_rows, ups, qkv, own[I1], own[I3])


def bring(pairs, sem):
    copies = [pltpu.make_async_copy(src, dst, sem.at[i]) for i, (src, dst) in enumerate(pairs)]
    for copy in copies:
        copy.start()
    for copy in copies:
        copy.wait()


def attn_products_kernel(dq, dk, dv, ctx, n1_o, ds, do, dwq, dwo, n1, dmid, dqkvt, ctxt, sem):
    tokens, width = n1.shape
    part = tokens // I2
    head_dim = dwo.shape[I1]

    @pl.when(pl.program_id(I0) == I0)
    def _():
        bring([(n1_o, n1), (ds, dmid.at[pl.ds(I0, part)]), (do, dmid.at[pl.ds(part, part)])], sem)

    def turn(rows):
        for t, block in enumerate((dq, dk, dv)):
            for r in range(I2):
                at = (I2 * t + r) * head_dim
                dqkvt[at:at + head_dim, rows] = block[rows, r * HEAD_PAD:(r + I1) * HEAD_PAD].T[I0:head_dim]
        for r in range(I2):
            ctxt[r * head_dim:(r + I1) * head_dim, rows] = ctx[rows, r * HEAD_PAD:(r + I1) * HEAD_PAD].T[I0:head_dim]
    rows_loop(tokens, SUB, turn)
    for c in range(I0, width, SUB):
        cut = slice(c, c + SUB)
        dwq[:, :, :, cut] = mm(dqkvt[...], n1[:, cut]).reshape(I3, I2, head_dim, SUB)
        dwo[:, :, cut] = mm(ctxt[...], dmid[:, cut]).reshape(I2, head_dim, SUB)


def attn_products(dqkv, ctx, n1, d_rows, out_dims):
    heads, head_dim, width = out_dims
    tokens = n1.shape[I0]
    vmem = pltpu.VMEM
    any_spec = pl.BlockSpec(memory_space=ANY)
    pairs = heads // I2
    cols = lambda t: pl.BlockSpec((tokens, I2 * HEAD_PAD), lambda i: (I0, t * pairs + i))
    return pl.pallas_call(
        attn_products_kernel,
        grid=(pairs,),
        out_shape=(jax.ShapeDtypeStruct((I3,) + out_dims, F32), jax.ShapeDtypeStruct(out_dims, F32)),
        in_specs=[cols(I0), cols(I1), cols(I2), cols(I0), any_spec, any_spec, any_spec],
        out_specs=(pl.BlockSpec((I3, I2, head_dim, width), lambda i: (I0, i, I0, I0)), pl.BlockSpec((I2, head_dim, width), lambda i: (i, I0, I0))),
        scratch_shapes=[vmem((tokens, width), BF), vmem((tokens, width), BF), vmem((I6 * head_dim, tokens), BF), vmem((I2 * head_dim, tokens), BF),
                        pltpu.SemaphoreType.DMA((I3,))],
        compiler_params=pltpu.CompilerParams(vmem_limit_bytes=VMEM_LIMIT),
        name='attn_products',
    )(dqkv, dqkv, dqkv, ctx, n1, *d_rows)


def mlp_products_kernel(dup, z, n2_o, gs, go, dwu, dwd, n2t, grad, zt, stage, sem):
    width, tokens = n2t.shape
    part = tokens // I2

    @pl.when(pl.program_id(I0) == I0)
    def _():
        bring([(n2_o, stage), (gs, grad.at[pl.ds(I0, part)]), (go, grad.at[pl.ds(part, part)])], sem)

        def turn(rows):
            for c in range(I0, width, SUB):
                n2t[c:c + SUB, rows] = stage[rows, c:c + SUB].T
        rows_loop(tokens, SUB, turn)

    def turn_z(rows):
        for c in range(I0, z.shape[I1], SUB):
            zt[c:c + SUB, rows] = z[rows, c:c + SUB].T
    rows_loop(tokens, SUB, turn_z)
    for c in range(I0, width, I2 * SUB):
        dwu[c:c + I2 * SUB, :] = mm(n2t[c:c + I2 * SUB, :], dup[...])
    for c in range(I0, width, SUB):
        dwd[:, c:c + SUB] = mm(zt[...], grad[:, c:c + SUB])


def mlp_products(dup, hidden, n2, g_rows):
    tokens, width = n2.shape
    cols = dup.shape[I1]
    vmem = pltpu.VMEM
    any_spec = pl.BlockSpec(memory_space=ANY)
    block = pl.BlockSpec((tokens, SUB), lambda i: (I0, i))
    return pl.pallas_call(
        mlp_products_kernel,
        grid=(cols // SUB,),
        out_shape=(jax.ShapeDtypeStruct((width, cols), F32), jax.ShapeDtypeStruct((cols, width), F32)),
        in_specs=[block, block, any_spec, any_spec, any_spec],
        out_specs=(pl.BlockSpec((width, SUB), lambda i: (I0, i)), pl.BlockSpec((SUB, width), lambda i: (i, I0))),
        scratch_shapes=[vmem((width, tokens), BF), vmem((tokens, width), BF), vmem((SUB, tokens), BF), vmem((tokens, width), BF), pltpu.SemaphoreType.DMA((I3,))],
        compiler_params=pltpu.CompilerParams(vmem_limit_bytes=VMEM_LIMIT),
        name='mlp_products',
    )(dup, hidden, n2, *g_rows)


def solution(mesh):
    act_spec = P('rep', None, None, None)
    weight_specs = (
        P(('rep', 'stage'), None, None, 'tp', None),
        P(('rep', 'stage'), 'tp', None, None),
        P(('rep', 'stage'), None, 'tp'),
        P(('rep', 'stage'), 'tp', None),
        P(('rep', 'stage'), None),
        P(('rep', 'stage'), None),
    )

    def device_fn(inputs, targets, w_qkv, w_out, w_up, w_down, gain_attn, gain_mlp):
        micro_count, _, seq_len, width = inputs.shape
        dims = (micro_count, seq_len, width, I2 * w_out.shape[I1], w_out.shape[I2], I2 * w_up.shape[I2])
        norm_factor = 1.0 / (inputs.size)
        own = (w_qkv[I0], w_out[I0], w_up[I0], w_down[I0])
        own_gains = jnp.concatenate([gain_attn, gain_mlp]).astype(F32)
        rows_of = (own[I0].transpose(I1, I2, I3, I0).reshape(-I1, width), own[I1].reshape(-I1, width), own[I2], own[I3])

        (acts, mids, qkv, ups, seeds, oh_same, oh_other, oa_same, oa_other, og_same, og_other, loss_tile, home_gains, *weights) = forward_phase(dims, inputs, targets, rows_of, own_gains)
        (nq, no, nu, nd), (fq, fo, fu, fd) = weights[I0:I4], weights[I4:I8]
        (tq0, to0, tu0, td0), (tq1, to1, tu1, td1) = weights[I8:12], weights[12:16]

        flat = lambda *rows: [r.reshape(-I1, width) for r in rows]
        h_rows = flat(oh_same, oh_other)
        done, *again = owner_recompute(dims, True, None, h_rows, flat(oa_same, oa_other), own_gains, rows_of)
        dx, _, od_same, od_other, og_same, og_other, oa_same, oa_other, dg_same, dg_other, loss_all = backward_phase(
            dims, (acts, mids, qkv, ups, seeds), (rows_of[I0], nq, fq, td0, td1, to0, to1, tu0, tu1), home_gains, loss_tile, done, (og_same, og_other, oa_same, oa_other))
        _, *again = owner_recompute(dims, False, again, h_rows, flat(oa_same, oa_other), own_gains, rows_of)
        ups_own, qkv_own, ctx_own, n1, n2 = again
        d_rows, g_rows = flat(od_same, od_other), flat(og_same, og_other)
        d_qkv_rows, d_up_rows, hidden, d_inputs = owner_backward(dims, dx, d_rows, g_rows, ups_own, qkv_own, rows_of)
        d_qkv, d_out = attn_products(d_qkv_rows, ctx_own, n1, d_rows, w_out.shape[I1:])
        d_up, d_down = mlp_products(d_up_rows, hidden, n2, g_rows)
        weight_grads = (d_qkv.transpose(I3, I0, I1, I2), d_out, d_up, d_down)
        mine = jnp.sum(dg_same + dg_other, I1)
        loss = jnp.sum(loss_all) * (0.5 * norm_factor)

        return (loss.reshape(I1), d_inputs) + tuple(g[None] for g in weight_grads) + (mine[I0][None], mine[I1][None])

    return jax.shard_map(device_fn, mesh=mesh, in_specs=(act_spec, act_spec) + weight_specs, out_specs=(P('rep'), act_spec) + weight_specs, check_vma=False)
```

```python
import functools

import jax
import jax.numpy as jnp
from jax import lax
from jax.experimental import pallas as pl
from jax.experimental.pallas import tpu as pltpu
from jax.sharding import PartitionSpec as P

NORM_EPS = 1e-5
BF = jnp.bfloat16
F32 = jnp.float32
MESH = pl.DeviceIdType.MESH
ANY = pl.ANY


GELU_A = 0.7978845608028654
GELU_B = 0.044715
I0, I1, I2, I3, I4, I6, I8 = 0, 1, 2, 3, 4, 6, 8
CHUNK = 1024
BLOCK = 384
SUB = 256
DEPTH = 6
BACK_DEPTH = 6
KDEPTH = 3
EARLY_G = 3
HEAD_PAD = 128
VMEM_LIMIT = 67043328


def mm(a, b):
    return lax.dot_general(a, b, (((I1,), (I0,)), ((), ())), preferred_element_type=F32)


def mm_nt(a, b):
    return lax.dot_general(a, b, (((I1,), (I1,)), ((), ())), preferred_element_type=F32)


def mm_tn(a, b):
    return lax.dot_general(a, b, (((I0,), (I0,)), ((), ())), preferred_element_type=F32)


class Place:
    def __init__(self):
        self.tp = lax.axis_index('tp')
        self.stage = lax.axis_index('stage')
        self.core = self.stage % I2
        self.x_pos = self.stage // I2
        self.home = self.x_pos * (I3 - I2 * self.tp) + self.tp
        self.is_l = self.stage == self.home
        self.sib = self.stage + I1 - I2 * self.core

    def at(self, tp, stage):
        return {'tp': tp, 'stage': stage}

    @property
    def sibling(self):
        return self.at(self.tp, self.sib)

    @property
    def across(self):
        return self.at(I1 - self.tp, self.stage)

    @property
    def across_other(self):
        return self.at(I1 - self.tp, self.sib)

    def chain(self, delta):
        there = self.home + delta
        x_pos = there // I2
        tp = there % I2 + x_pos * (I1 - I2 * (there % I2))
        return self.at(tp, I2 * x_pos + self.core)


def entry_barrier(place):
    barrier = pltpu.get_barrier_semaphore()
    for d_tp in (I0, I1):
        for d_stage in range(I4):
            if d_tp or d_stage:
                tp = place.tp + d_tp - I2 * d_tp * place.tp
                stage = (place.stage + d_stage) % I4
                pl.semaphore_signal(barrier, inc=I1, device_id=place.at(tp, stage), device_id_type=MESH)
    pl.semaphore_wait(barrier, 7)


def remote(src, dst, send_sem, recv_sem, device_id):
    return pltpu.make_async_remote_copy(src_ref=src, dst_ref=dst, send_sem=send_sem, recv_sem=recv_sem, device_id=device_id, device_id_type=MESH)


def rows_loop(total, step, body):
    def run(i, carry):
        body(pl.ds(pl.multiple_of(i * step, step), step))
        return carry
    lax.fori_loop(I0, total // step, run, I0)


def norm_rows(src, gain_row, dst, total):
    def body(rows):
        v = src[rows, :].astype(F32)
        inv = lax.rsqrt(jnp.mean(v * v, axis=-I1, keepdims=True) + NORM_EPS)
        dst[rows, :] = (v * inv * gain_row).astype(BF)
    rows_loop(total, 32, body)


def gelu_gate(u):
    u2 = u * u
    t = jnp.tanh(u * (GELU_A + (GELU_A * GELU_B) * u2))
    return 0.5 * t + 0.5, u2


def gelu_slope(hidden, gate, u2):
    return gate + hidden * (1.0 - gate) * (2.0 * GELU_A + (6.0 * GELU_A * GELU_B) * u2)


def row_parts(heads, cut=128):
    return [(*(x[low:high] for x in queries), *(x[:high] for x in keys), low)
            for queries, keys in heads for low, high in ((I0, cut), (cut, queries[I0].shape[I0]))]


def softmax_parts(scores, starts):
    masked = []
    for s, start in zip(scores, starts):
        q_pos = lax.broadcasted_iota(jnp.int32, s.shape, I0) + start
        k_pos = lax.broadcasted_iota(jnp.int32, s.shape, I1)
        masked.append(jnp.where(k_pos <= q_pos, s, -1e30))
    tops = [jnp.max(s, axis=-I1, keepdims=True) for s in masked]
    powers = [jnp.exp(s - top) for s, top in zip(masked, tops)]
    scales = [1.0 / jnp.sum(e, axis=-I1, keepdims=True) for e in powers]
    return [e * r for e, r in zip(powers, scales)]


def join_keys(top, low, cut=128):
    return jnp.concatenate([top + low[:cut], low[cut:]], I0).astype(BF)


def attention_forward(heads, scale):
    units = row_parts([((q,), (k, v)) for q, k, v in heads])
    probs = softmax_parts([mm_nt(q, k) * scale for q, k, _, _ in units], [u[-I1] for u in units])
    parts = [mm(p.astype(BF), u[I2]) for p, u in zip(probs, units)]
    return [jnp.concatenate([a, b], I0).astype(BF) for a, b in zip(parts[I0::I2], parts[I1::I2])]


def attention_backward(heads, scale):
    units = row_parts([((q, dc), (k, v)) for q, k, v, dc in heads])
    scores = [mm_nt(q, k) * scale for q, _, k, _, _ in units]
    dps = [mm_nt(dc, v) for _, dc, _, v, _ in units]
    probs = softmax_parts(scores, [u[-I1] for u in units])
    dps = [dp.astype(BF).astype(F32) for dp in dps]
    deltas = [jnp.sum(dp * p, axis=-I1, keepdims=True) for dp, p in zip(dps, probs)]
    dvs = [mm_tn(p.astype(BF), u[I1]) for p, u in zip(probs, units)]
    dss = [p * (dp - delta) * scale for p, dp, delta in zip(probs, dps, deltas)]
    terms = []
    for ds in dss:
        hi = ds.astype(BF)
        rest = ds - hi.astype(F32)
        lo = rest.astype(BF)
        terms.append((hi, lo, (rest - lo.astype(F32)).astype(BF)))
    dqs = [mm(hi, u[I2]) + (mm(lo, u[I2]) + mm(tail, u[I2])) for (hi, lo, tail), u in zip(terms, units)]
    dks = [mm_tn(hi, u[I0]) + (mm_tn(lo, u[I0]) + mm_tn(tail, u[I0])) for (hi, lo, tail), u in zip(terms, units)]
    return [(jnp.concatenate([dqs[i], dqs[i + I1]], I0).astype(BF), join_keys(dks[i], dks[i + I1]), join_keys(dvs[i], dvs[i + I1]))
            for i in range(I0, len(units), I2)]


def lanes(offset, size):
    return pl.ds(pl.multiple_of(offset, 128), size)


def load_resident(buf, sem, halves):
    for c in range(I6):
        for condition, ref in halves[c // I3]:
            copy = pltpu.make_async_copy(ref.at[(c % I3) * CHUNK:(c % I3 + I1) * CHUNK, :], buf.at[c], sem.at[c])
            if condition is None:
                copy.start()
            else:
                pl.when(condition)(copy.start)


def load_heads(ref, index, dst, sem):
    for r in range(I8):
        rows = pl.ds(pl.multiple_of(index * 768 + r * 96, 96), 96)
        pltpu.make_async_copy(ref.at[rows, :], dst.at[r * 128:r * 128 + 96, :], sem).start()


class Stream:
    def __init__(self, buf, sem, depth, parts, total, by_heads):
        self.buf, self.sem, self.depth, self.parts, self.total, self.by_heads = buf, sem, depth, parts, total, by_heads
        self.per_tick = sum(p[I1] for p in parts)

    def copy_in(self, ref, index, slot):
        if not self.by_heads:
            pltpu.make_async_copy(ref.at[index], self.buf.at[slot], self.sem.at[slot]).start()
            return
        load_heads(ref, index, self.buf.at[slot], self.sem.at[slot])

    def start(self, seq):
        @pl.when(seq < self.total)
        def _():
            j = seq % self.per_tick
            slot = seq % self.depth
            base = I0
            for choices, chunks in self.parts:
                for condition, ref in choices:
                    here = (j >= base) & (j < base + chunks)
                    here = here if condition is None else here & condition

                    @pl.when(here)
                    def _(ref=ref, low=base):
                        self.copy_in(ref, j - low, slot)
                base += chunks

    def prime(self):
        for seq in range(self.depth):
            self.start(jnp.int32(seq))

    def wait(self, seq):
        slot = seq % self.depth
        ref = self.parts[I0][I0][I0][I1]
        if self.by_heads:
            pltpu.make_async_copy(ref.at[I0:768, :], self.buf.at[slot, I0:768, :], self.sem.at[slot]).wait()
        else:
            pltpu.make_async_copy(ref.at[I0], self.buf.at[slot], self.sem.at[slot]).wait()
        return self.buf.at[slot]


PIECES = [(0, 0, 0), (0, 0, 1), (0, 0, 2), (1, 0, 0), (2, 1, 0), (2, 1, 1), (2, 1, 2), (2, 1, 3), (3, 0, 0), (3, 0, 1), (3, 0, 2), (3, 0, 3)]


def piece(ref, axis, index):
    return ref.at[index * 768:(index + I1) * 768, :] if axis == I0 else ref.at[:, index * 768:(index + I1) * 768]


def weight_phase(place, is_r, own, near, far, turned, up_chunks, wn, wk, send_sem, y_send, d_send, near_sem, far_sem, load_sem, store_sem, chunk_sem):
    wk[...] = jnp.zeros_like(wk)

    @pl.when(place.is_l)
    def _():
        for i in range(I4):
            remote(own[i], near[i], send_sem.at[i], near_sem.at[i], place.sibling).start()

    @pl.when(is_r)
    def _():
        for c, (i, axis, index) in enumerate(PIECES):
            remote(piece(own[i], axis, index), piece(far[i], axis, index), y_send.at[i], far_sem.at[c], place.across_other).start()

    def load(i, refs, t, slot):
        for condition, ref in refs:
            def go(ref=ref):
                if i < I2:
                    for r in range(I2):
                        rows = pl.ds(pl.multiple_of(t * 192 + r * 96, 96), 96)
                        pltpu.make_async_copy(ref.at[rows, :], wk.at[I0, pl.ds(slot * SUB + r * 128, 96), :], load_sem.at[slot]).start()
                elif i == I2:
                    pltpu.make_async_copy(ref.at[:, lanes(t * SUB, SUB)], wn.at[slot, :, I0:SUB], load_sem.at[slot]).start()
                else:
                    rows = pl.ds(pl.multiple_of(t * SUB, SUB), SUB)
                    pltpu.make_async_copy(ref.at[rows, :], wk.at[I0, pl.ds(512 + slot * SUB, SUB), :], load_sem.at[slot]).start()
            if condition is None:
                go()
            else:
                pl.when(condition)(go)

    def loaded(i, refs, slot):
        ref = refs[I0][I1]
        if i < I2:
            pltpu.make_async_copy(ref.at[I0:192, :], wk.at[I0, I0:192, :], load_sem.at[slot]).wait()
        elif i == I2:
            pltpu.make_async_copy(ref.at[:, I0:SUB], wn.at[slot, :, I0:SUB], load_sem.at[slot]).wait()
        else:
            pltpu.make_async_copy(ref.at[I0:SUB, :], wk.at[I0, 512:768, :], load_sem.at[slot]).wait()

    def store(i, dst, t, slot):
        if i == I2:
            rows = pl.ds(pl.multiple_of(t * SUB, SUB), SUB)
            return pltpu.make_async_copy(wk.at[I1, pl.ds(slot * SUB, SUB), :], dst.at[rows, :], store_sem.at[slot])
        return pltpu.make_async_copy(wn.at[slot, :, SUB:512], dst.at[t // I4, :, lanes(t % I4 * SUB, SUB)], store_sem.at[slot])

    def keep(which, t, slot):
        return pltpu.make_async_copy(wn.at[slot, :, I0:SUB], up_chunks[which].at[t // I4, :, lanes(t % I4 * SUB, SUB)], chunk_sem.at[slot])

    def turn(i, refs, which, first, count):
        dst = turned[i][which]
        load(i, refs, first, I0)

        def step(n, c):
            slot = n % I2

            if i == I2:
                @pl.when(n > I0)
                def _():
                    keep(which, first + n - I1, I1 - slot).wait()

            @pl.when(n + I1 < count)
            def _():
                load(i, refs, first + n + I1, I1 - slot)
            loaded(i, refs, slot)
            if i == I2:
                keep(which, first + n, slot).start()

            @pl.when(n >= I2)
            def _():
                store(i, dst, first + n - I2, slot).wait()
            for b in range(I6):
                cut = slice(b * SUB, b * SUB + SUB)
                if i == I2:
                    wk[I1, pl.ds(pl.multiple_of(slot * SUB, SUB), SUB), cut] = wn[slot, cut, I0:SUB].T
                else:
                    base = I0 if i < I2 else 512
                    wn[slot, cut, SUB:512] = wk[I0, pl.ds(pl.multiple_of(base + slot * SUB, SUB), SUB), cut].T
            store(i, dst, first + n, slot).start()
            return c
        lax.fori_loop(I0, count, step, I0)
        for n in (count - I2, count - I1):
            store(i, dst, first + n, n % I2).wait()
        if i == I2:
            keep(which, first + count - I1, (count - I1) % I2).wait()

    counts = (12, I4, 12, 12)
    for i in range(I4):
        @pl.when(is_r)
        def _(i=i):
            remote(near[i], near[i], send_sem.at[i], near_sem.at[i], place.sibling).wait_recv()
        turn(i, [(place.is_l, own[i]), (is_r, near[i])], I0, I0, counts[i])
    done = [I0, I0, I0, I0]
    for c, (i, axis, index) in enumerate(PIECES):
        view = piece(far[i], axis, index)
        remote(view, view, d_send.at[i], far_sem.at[c], place.sibling).wait_recv()

        @pl.when(is_r)
        def _(i=i, c=c, view=view):
            remote(view, view, d_send.at[i], far_sem.at[c], place.sibling).start()
        count = I4 if i < I2 else I3
        turn(i, [(None, far[i])], I1, done[i], count)
        done[i] += count

    @pl.when(place.is_l)
    def _():
        for i in range(I4):
            remote(own[i], near[i], send_sem.at[i], near_sem.at[i], place.sibling).wait_send()

    @pl.when(is_r)
    def _():
        for i in range(I4):
            remote(own[i], far[i], y_send.at[i], far_sem.at[I0], place.across_other).wait_send()
            remote(far[i], far[i], d_send.at[i], far_sem.at[I0], place.sibling).wait_send()


def near_choices(place, own, near):
    return [(place.is_l, own), (jnp.logical_not(place.is_l), near)]


def forward_kernel(dims, x_ref, y_ref, wq, wo, wu, wd, own_gains,
                   a_s, h_s, qkv_s, u_s, g_s, oh_same, oh_other, oa_same, oa_other, og_same, og_other, loss_s, home_gains,
                   nq, no, nu, nd, fq, fo, fu, fd, tq0, to0, tu0, td0, tq1, to1, tu1, td1, uc0, uc1,
                   abuf, hbuf, obuf, nbuf, ybuf, sbuf, qkvbuf, ubuf, zbuf, ctxbuf, acc, lossbuf, losstile, gains, wres, wores, wn,
                   send_sem, y_send, d_send, near_sem, far_sem, t_load, t_store, t_keep,
                   act_sem, hop_f, keep_sem, save_sem, stream_n, res_sem, out_sem, big_sem, y_sem, s_sem,
                   os_sem, oo_sem, as_sem, ao_sem, gs_sem, go_sem, bulk, gain_sem, tiny):
    micro, seq, width, heads, head_dim, ffn = dims
    place = Place()
    is_first, is_last = place.home == I0, place.home == I3
    home02 = (place.home == I0) | (place.home == I2)
    home13 = jnp.logical_not(home02)
    is_r = jnp.logical_not(place.is_l)
    takes_x = (place.home == I1) & is_r
    half = heads // I2 * HEAD_PAD
    scale = head_dim ** -0.5
    norm_factor = 1.0 / (micro * I2 * seq * width)
    own, near, far = (wq, wo, wu, wd), (nq, no, nu, nd), (fq, fo, fu, fd)
    turned = ((tq0, tq1), (to0, to1), (tu0, tu1), (td0, td1))
    entry_barrier(place)

    @pl.when(place.is_l)
    def _():
        pltpu.make_async_copy(own_gains, gains, gain_sem.at[I0]).start()
        remote(own_gains, gains, gain_sem.at[I1], gain_sem.at[I0], place.sibling).start()

    @pl.when(is_first)
    def _():
        for m in range(micro):
            pltpu.make_async_copy(x_ref.at[m, place.core], abuf.at[m], act_sem.at[m]).start()
    weight_phase(place, is_r, own, near, far, turned, (uc0, uc1), wn, wores, send_sem, y_send, d_send, near_sem, far_sem, t_load, t_store, t_keep)
    pltpu.make_async_copy(own_gains, gains, gain_sem.at[I0]).wait()
    pltpu.make_async_copy(gains, home_gains, gain_sem.at[I0]).start()

    @pl.when(place.is_l)
    def _():
        remote(own_gains, gains, gain_sem.at[I1], gain_sem.at[I0], place.sibling).wait_send()

    def near_of(i):
        return near_choices(place, own[i], near[i])

    def saved(dst, index):
        return pltpu.make_async_copy(hbuf, dst, save_sem.at[index])

    sn = Stream(wn, stream_n, DEPTH, [([(None, tq0)], I3), ([(None, tq1)], I3), ([(None, uc0)], I3), ([(None, uc1)], I3)], micro * 12, False)
    for c, choices in enumerate((near_of(I1), [(None, fo)])):
        for condition, ref in choices:
            def go(ref=ref, c=c):
                load_heads(ref, I0, wores.at[c], out_sem.at[c])
            go() if condition is None else pl.when(condition)(go)
    sn.prime()
    load_resident(wres, res_sem, (near_of(I3), [(None, fd)]))
    lossbuf[...] = jnp.zeros_like(lossbuf)

    def qkv_out(m):
        return pltpu.make_async_copy(qkvbuf, qkv_s.at[m], big_sem.at[I0])

    def up_out(m):
        return pltpu.make_async_copy(ubuf, u_s.at[m], big_sem.at[I1])

    def act_out(m):
        return pltpu.make_async_copy(abuf.at[m], a_s.at[m], save_sem.at[I2])

    def hop_forward(m):
        return remote(obuf.at[m % I2], abuf.at[m], hop_f.at[m % I2], act_sem.at[m], place.chain(I1))

    def near_hand(src, dst_far, dst_own, sem, recv_sem):
        return (lambda: remote(src, dst_far, sem, recv_sem, place.sibling)), (lambda: pltpu.make_async_copy(src, dst_own, sem))

    def hand_out(m):
        return near_hand(obuf.at[m % I2], oa_other.at[m], oa_same.at[m], keep_sem.at[m % I2], ao_sem)

    def both_kinds(condition, copies, start):
        far_copy, own_copy = copies

        @pl.when(condition & place.is_l)
        def _():
            far_copy().start() if start else far_copy().wait_send()

        @pl.when(condition & is_r)
        def _():
            own_copy().start() if start else own_copy().wait()

    def x_out(m):
        return pltpu.make_async_copy(ybuf, oa_same.at[m], y_sem), pltpu.make_async_copy(sbuf, oa_other.at[m], s_sem)

    def seed_out(m):
        return pltpu.make_async_copy(sbuf, g_s.at[m], s_sem)

    def far_mid(m, condition):
        @pl.when(condition & place.is_l)
        def _():
            remote(h_s.at[m], oh_same.at[m], bulk.at[I2], os_sem, place.across).start()

        @pl.when(condition & is_r)
        def _():
            remote(h_s.at[m], oh_other.at[m], bulk.at[I2], oo_sem, place.across_other).start()

    def send_seed(m):
        seed_out(m).wait()

        @pl.when(place.is_l)
        def _():
            remote(g_s.at[m], og_same.at[m], bulk.at[I1], gs_sem, place.across).start()

        @pl.when(is_r)
        def _():
            remote(g_s.at[m], og_other.at[m], bulk.at[I1], go_sem, place.across_other).start()

    def forward_tick(m, carry):
        act, mid, out = abuf.at[m], hbuf, obuf.at[m % I2]
        pltpu.make_async_copy(x_ref.at[m, place.core], act, act_sem.at[m]).wait()
        act_out(m).start()

        @pl.when(place.is_l)
        def _():
            pltpu.make_async_copy(act, oa_same.at[m], as_sem).start()

        @pl.when(is_last)
        def _():
            pltpu.make_async_copy(y_ref.at[m, place.core], ybuf, y_sem).start()

        @pl.when(takes_x)
        def _():
            @pl.when(m > I0)
            def _():
                for copy in x_out(m):
                    copy.wait()
            for core, buf, sem in ((place.core, ybuf, y_sem), (I1 - place.core, sbuf, s_sem)):
                pltpu.make_async_copy(x_ref.at[m, core], buf, sem).start()
        norm_rows(act, gains[I0:I1, :], nbuf, seq)

        @pl.when(m > I0)
        def _():
            qkv_out(m).wait()

        def qkv_step(j, c):
            w = sn.wait(m * 12 + j)
            for n in range(I0, CHUNK, SUB):
                qkvbuf[:, lanes(j * CHUNK + n, SUB)] = mm(nbuf[...], w[:, n:n + SUB]).astype(BF)
            sn.start(m * 12 + j + DEPTH)
            return c
        lax.fori_loop(I0, I6, qkv_step, I0)
        qkv_out(m).start()
        act_out(m).wait()

        @pl.when(is_r)
        def _():
            remote(a_s.at[m], oa_other.at[m], bulk.at[I0], ao_sem, place.sibling).start()

        def head_step(i, c):
            base = i * (I3 * half)
            views = [[qkvbuf[:, lanes(base + t * half + r * HEAD_PAD, HEAD_PAD)] for t in range(I3)] for r in range(I8)]
            for r, context in enumerate(attention_forward(views, scale)):
                ctxbuf[:, lanes(i * half + r * HEAD_PAD, HEAD_PAD)] = context
            return c
        lax.fori_loop(I0, I2, head_step, I0)

        @pl.when(m == I0)
        def _():
            for c in range(I2):
                pltpu.make_async_copy(wo, wores.at[c, I0:768, :], out_sem.at[c]).wait()
        for n in range(I0, width, SUB):
            total = mm(ctxbuf[:, I0:half], wores[I0, :, n:n + SUB]) + mm(ctxbuf[:, half:I2 * half], wores[I1, :, n:n + SUB])
            mid[:, n:n + SUB] = (act[:, n:n + SUB].astype(F32) + total).astype(BF)
        saved(h_s.at[m], I0).start()

        @pl.when(place.is_l)
        def _():
            saved(oh_same.at[m], I1).start()
        norm_rows(mid, gains[I1:I2, :], nbuf, seq)

        @pl.when(m > I0)
        def _():
            up_out(m).wait()
        acc[...] = jnp.zeros_like(acc)

        def mlp_step(j, c):
            w = sn.wait(m * 12 + I6 + j)
            for n in range(I0, CHUNK, SUB):
                u = mm(nbuf[...], w[:, n:n + SUB]).astype(BF)
                ubuf[:, lanes(j * CHUNK + n, SUB)] = u
                uf = u.astype(F32)
                zbuf[:, n:n + SUB] = (uf * gelu_gate(uf)[I0]).astype(BF)
            sn.start(m * 12 + I6 + j + DEPTH)

            @pl.when(m == I0)
            def _():
                pltpu.make_async_copy(wd.at[I0:CHUNK, :], wres.at[j], res_sem.at[j]).wait()
            for n in range(I0, width, SUB):
                acc[:, n:n + SUB] += mm(zbuf[...], wres[j, :, n:n + SUB])
            return c
        lax.fori_loop(I0, I6, mlp_step, I0)
        up_out(m).start()

        @pl.when((m > I1) & jnp.logical_not(is_last))
        def _():
            hop_forward(m).wait_send()

        both_kinds((m > I1) & home02, hand_out(m), False)

        def finish(rows):
            out[rows, :] = (mid[rows, :].astype(F32) + acc[rows, :]).astype(BF)
        rows_loop(seq, 32, finish)

        @pl.when(jnp.logical_not(is_last))
        def _():
            hop_forward(m).start()

        both_kinds(home02, hand_out(m), True)

        @pl.when(is_last)
        def _():
            pltpu.make_async_copy(y_ref.at[m, place.core], ybuf, y_sem).wait()

            @pl.when(m > I0)
            def _():
                send_seed(m - I1)

            def seed(rows):
                error = out[rows, :].astype(F32) - ybuf[rows, :].astype(F32)
                sbuf[rows, :] = (error * norm_factor).astype(BF)
                lossbuf[...] += jnp.sum((error * error).reshape(I4, I8, width), axis=I0)
            rows_loop(seq, 32, seed)
            seed_out(m).start()

        @pl.when(takes_x)
        def _():
            for core, buf, sem in ((place.core, ybuf, y_sem), (I1 - place.core, sbuf, s_sem)):
                pltpu.make_async_copy(x_ref.at[m, core], buf, sem).wait()
            for copy in x_out(m):
                copy.start()

        saved(h_s.at[m], I0).wait()

        @pl.when(place.is_l)
        def _():
            saved(oh_same.at[m], I1).wait()

        @pl.when(is_r)
        def _():
            remote(h_s.at[m], oh_other.at[m], bulk.at[I3], oo_sem, place.sibling).start()

        far_mid(m, home13 | (m % I2 == I1))
        return carry

    lax.fori_loop(I0, micro, forward_tick, I0)
    for m in range(I0, micro, I2):
        far_mid(m, home02)

    @pl.when(is_last)
    def _():
        total = lossbuf[:, I0:128]
        for n in range(128, width, 128):
            total = total + lossbuf[:, n:n + 128]
        losstile[...] = total
        pltpu.make_async_copy(losstile, loss_s, tiny).start()
    for copy in (qkv_out(micro - I1), up_out(micro - I1)):
        copy.wait()

    @pl.when(jnp.logical_not(is_last))
    def _():
        for m in (micro - I2, micro - I1):
            hop_forward(m).wait_send()
    for m in (micro - I2, micro - I1):
        both_kinds(home02, hand_out(m), False)

    @pl.when(is_last)
    def _():
        send_seed(micro - I1)
        pltpu.make_async_copy(losstile, loss_s, tiny).wait()

    @pl.when(takes_x)
    def _():
        for copy in x_out(micro - I1):
            copy.wait()
    pltpu.make_async_copy(gains, home_gains, gain_sem.at[I0]).wait()
    sent, got = drain(place)
    sent(h_s, bulk.at[I2])
    got(oh_other, oo_sem)

    @pl.when(is_last)
    def _():
        sent(g_s, bulk.at[I1])

    @pl.when((place.home == I2) & is_r)
    def _():
        got(og_same, gs_sem)
        got(og_other, go_sem)

    @pl.when(is_r)
    def _():
        sent(a_s, bulk.at[I0])
        sent(h_s, bulk.at[I3])
        got(oh_same, os_sem)

    @pl.when(place.is_l)
    def _():
        got(oa_same, as_sem)

    @pl.when(place.is_l | home02)
    def _():
        got(oa_other, ao_sem)


def drain(place):
    def sent(buf, sem):
        remote(buf, buf, sem, sem, place.sibling).wait_send()

    def got(dst, sem):
        pltpu.make_async_copy(dst, dst, sem).wait()
    return sent, got


def backward_kernel(dims, a_s, h_s, qkv_s, u_s, g_s, wq, nq, fq, td0, td1, to0, to1, tu0, tu1, gains, loss_s, after, *refs):
    (dx_s, m_s, od_same, od_other, og_same, og_other, oa_same, oa_other, dg_same, dg_other, loss_all,
     gbuf, hbuf, obuf, qkvbuf, ubuf, habuf, zbuf, ctxbuf, dqkvbuf, acc, accg, wres, wn, wk,
     grad_sem, hop_b, back_sem, dx_sem, dx_send, save_sem, stream_n, stream_k, res_sem, load_sem,
     ds_sem, do_sem, gs_sem, go_sem, as_sem, ao_sem, bulk, tiny, loss_sem) = refs[I4:]
    micro, seq, width, heads, head_dim, ffn = dims
    place = Place()
    is_first, is_last = place.home == I0, place.home == I3
    home13 = (place.home == I1) | is_last
    is_r = jnp.logical_not(place.is_l)
    half = heads // I2 * HEAD_PAD
    scale = head_dim ** -0.5

    barrier = pltpu.get_barrier_semaphore()
    along_x = (place.home == I1) | (place.home == I2)
    for there in (place.sibling, place.across, place.across_other):
        pl.semaphore_signal(barrier, inc=I1, device_id=there, device_id_type=MESH)

    @pl.when(along_x)
    def _():
        pl.semaphore_signal(barrier, inc=I1, device_id=place.at(place.tp, (place.stage + I2) % I4), device_id_type=MESH)

    @pl.when(is_last)
    def _():
        for m in range(micro):
            pltpu.make_async_copy(g_s.at[m], gbuf.at[m], grad_sem.at[m]).start()
    wk[...] = jnp.zeros_like(wk)
    bn = Stream(wn, stream_n, BACK_DEPTH, [([(None, td0)], I3), ([(None, td1)], I3), ([(None, to0)], I1), ([(None, to1)], I1)], micro * I8, False)
    bk = Stream(wk, stream_k, KDEPTH, [(near_choices(place, wq, nq), I3), ([(None, fq)], I3)], micro * I6, True)
    bn.prime()
    bk.prime()
    load_resident(wres, res_sem, ([(None, tu0)], [(None, tu1)]))

    def saved(dst, index):
        return pltpu.make_async_copy(hbuf, dst, save_sem)

    def both_kinds(condition, copies, start):
        far_copy, own_copy = copies

        @pl.when(condition & place.is_l)
        def _():
            far_copy().start() if start else far_copy().wait_send()

        @pl.when(condition & is_r)
        def _():
            own_copy().start() if start else own_copy().wait()

    def near_hand(src, dst_far, dst_own, sem, recv_sem):
        return (lambda: remote(src, dst_far, sem, recv_sem, place.sibling)), (lambda: pltpu.make_async_copy(src, dst_own, sem))

    def loads(i):
        m = micro - I1 - i
        return [pltpu.make_async_copy(src.at[m], dst, load_sem.at[k])
                for k, (src, dst) in enumerate(((u_s, ubuf), (qkv_s, qkvbuf), (h_s, habuf.at[I0]), (a_s, habuf.at[I1])))]

    def load_next(i, k):
        @pl.when(i + I1 < micro)
        def _():
            loads(i + I1)[k].start()

    for copy in loads(I0):
        copy.start()
    accg[...] = jnp.zeros_like(accg)

    def norm_back(index, x, base, dst, gain_row):
        def body(rows):
            xf = x[rows, :].astype(F32)
            dy = acc[rows, :].astype(BF).astype(F32)
            inv = lax.rsqrt(jnp.mean(xf * xf, axis=-I1, keepdims=True) + NORM_EPS)
            xn = xf * inv
            accg[index] += jnp.sum((dy * xn).reshape(I4, I8, width), axis=I0)
            dyg = dy * gain_row
            dx = inv * (dyg - xn * jnp.mean(dyg * xn, axis=-I1, keepdims=True))
            dst[rows, :] = (base[rows, :].astype(F32) + dx).astype(BF)
        rows_loop(seq, 32, body)

    def hop_back(i):
        m = micro - I1 - i
        return remote(obuf.at[i % I2], gbuf.at[m], hop_b.at[i % I2], grad_sem.at[m], place.chain(-I1))

    def hand_back(i):
        m = micro - I1 - i
        return near_hand(obuf.at[i % I2], og_other.at[m], og_same.at[m], back_sem.at[i % I2], go_sem)

    def keep_dx(i):
        return pltpu.make_async_copy(obuf.at[i % I2], dx_s.at[micro - I1 - i], back_sem.at[i % I2])

    def back_ready(i):
        both_kinds((i > I1) & home13, hand_back(i), False)

        @pl.when((i > I1) & is_first)
        def _():
            keep_dx(i).wait()
            dx_to_b(i).wait_send()

        @pl.when((i > I1) & jnp.logical_not(is_first))
        def _():
            hop_back(i).wait_send()

    def pass_loss(tile):
        @pl.when(jnp.logical_not(is_first))
        def _():
            remote(tile, loss_all.at[place.core], loss_sem.at[I0], loss_sem.at[I1], place.chain(-I1)).start()
        remote(tile, loss_all.at[place.core], loss_sem.at[I2], loss_sem.at[I3], place.sibling).start()

    def dx_to_b(i):
        return remote(obuf.at[i % I2], dx_s.at[micro - I1 - i], dx_send.at[i % I2], dx_sem, place.across)

    def backward_tick(i, carry):
        m = micro - I1 - i
        slot = i % I2
        grad, dmid, prev = gbuf.at[m], hbuf, obuf.at[slot]
        u_now, qkv_now, h_now, a_now = ubuf, qkvbuf, habuf.at[I0], habuf.at[I1]

        pltpu.make_async_copy(g_s.at[m], grad, grad_sem.at[m]).wait()

        @pl.when(place.is_l)
        def _():
            pltpu.make_async_copy(grad, og_same.at[m], gs_sem).start()
        load_u, load_qkv, load_h, load_a = loads(i)
        load_u.wait()
        acc[...] = jnp.zeros_like(acc)

        def mlp_step(j, c):
            w = bn.wait(i * I8 + j)
            for n in range(I0, CHUNK, SUB):
                dz = mm(grad[...], w[:, n:n + SUB]).astype(BF).astype(F32)
                u = u_now[:, lanes(j * CHUNK + n, SUB)].astype(F32)
                gate, u2 = gelu_gate(u)
                zbuf[:, n:n + SUB] = (dz * gelu_slope(u * gate, gate, u2)).astype(BF)
            bn.start(i * I8 + j + BACK_DEPTH)

            @pl.when(i == I0)
            def _():
                pltpu.make_async_copy(tu0.at[I0:CHUNK, :], wres.at[j], res_sem.at[j]).wait()
            for n in range(I0, width, SUB):
                acc[:, n:n + SUB] += mm(zbuf[...], wres[j, :, n:n + SUB])
            return c
        lax.fori_loop(I0, I6, mlp_step, I0)
        load_next(i, I0)
        load_h.wait()
        norm_back(I1, h_now, grad, dmid, gains[I1:I2, :])
        load_next(i, I2)

        @pl.when(place.is_l)
        def _():
            saved(od_same.at[m], I0).start()

        @pl.when(is_r)
        def _():
            saved(m_s.at[m], I0).start()
        for c in range(I2):
            w = bn.wait(i * I8 + I6 + c)
            for n in range(I0, CHUNK, SUB):
                ctxbuf[:, c * CHUNK + n:c * CHUNK + n + SUB] = mm(dmid[...], w[:, n:n + SUB]).astype(BF)
            bn.start(i * I8 + I6 + c + BACK_DEPTH)
        load_qkv.wait()

        def head_step(t, c):
            base = (t // I2) * (I3 * half) + (t % I2) * (I4 * HEAD_PAD)
            at = [[lanes(base + part * half + r * HEAD_PAD, HEAD_PAD) for part in range(I3)] for r in range(I4)]
            group = [(*(qkv_now[:, p] for p in at[r]), ctxbuf[:, lanes((t * I4 + r) * HEAD_PAD, HEAD_PAD)]) for r in range(I4)]
            for r, grads in enumerate(attention_backward(group, scale)):
                for p, value in zip(at[r], grads):
                    dqkvbuf[:, p] = value
            return c
        lax.fori_loop(I0, heads // I4, head_step, I0)
        load_next(i, I1)
        acc[...] = jnp.zeros_like(acc)

        def qkv_step(j, c):
            w = bk.wait(i * I6 + j)
            for n in range(I0, width, SUB):
                acc[:, n:n + SUB] += mm(dqkvbuf[:, lanes(j * CHUNK, CHUNK)], w[:, n:n + SUB])
            bk.start(i * I6 + j + KDEPTH)
            return c
        lax.fori_loop(I0, I6, qkv_step, I0)
        load_a.wait()
        back_ready(i)
        norm_back(I0, a_now, dmid, prev, gains[I0:I1, :])
        load_next(i, I3)

        @pl.when(i == I0)
        def _():
            pl.semaphore_wait(barrier, I3 + (place.home + I1) // I2 % I2)

            @pl.when(is_last)
            def _():
                pass_loss(loss_s)

            @pl.when((place.home == I2) & place.is_l)
            def _():
                for t in range(micro):
                    remote(a_s.at[t], oa_same.at[t], bulk.at[I8], as_sem, place.across).start()

            @pl.when((place.home == I2) & is_r)
            def _():
                for t in range(micro):
                    remote(a_s.at[t], oa_other.at[t], bulk.at[I8], ao_sem, place.across_other).start()

        @pl.when(jnp.logical_not(is_first))
        def _():
            hop_back(i).start()

        @pl.when(is_first)
        def _():
            keep_dx(i).start()
            dx_to_b(i).start()
        both_kinds(home13, hand_back(i), True)

        @pl.when(place.is_l)
        def _():
            saved(od_same.at[m], I0).wait()
            remote(od_same.at[m], od_same.at[m], bulk.at[I6], ds_sem, place.across).start()

        @pl.when(is_r)
        def _():
            remote(grad, og_other.at[m], bulk.at[5], go_sem, place.sibling).start()
            saved(m_s.at[m], I0).wait()
            remote(m_s.at[m], od_other.at[m], bulk.at[I6], do_sem, place.sibling).start()
            remote(m_s.at[m], od_other.at[m], bulk.at[7], do_sem, place.across_other).start()

        far_grad(m, (place.home == I1) & (i % I2 == I1) & (i < I2 * EARLY_G))
        return carry

    def far_grad(m, condition):
        @pl.when(condition & place.is_l)
        def _():
            remote(gbuf.at[m], og_same.at[m], bulk.at[I4], gs_sem, place.across).start()

        @pl.when(condition & is_r)
        def _():
            remote(gbuf.at[m], og_other.at[m], bulk.at[I4], go_sem, place.across_other).start()

    lax.fori_loop(I0, micro, backward_tick, I0)
    loss_mine = loss_all.at[place.core]

    @pl.when(is_last)
    def _():
        own_loss = pltpu.make_async_copy(loss_s, loss_mine, loss_sem.at[I1])
        own_loss.start()
        own_loss.wait()

    @pl.when(jnp.logical_not(is_last))
    def _():
        remote(loss_mine, loss_mine, loss_sem.at[I0], loss_sem.at[I1], place.sibling).wait_recv()
        pass_loss(loss_mine)

    @pl.when(place.is_l)
    def _():
        pltpu.make_async_copy(accg, dg_same, tiny.at[I0]).start()
        remote(accg, dg_same, tiny.at[I1], tiny.at[I0], place.across).start()

    @pl.when(is_r)
    def _():
        remote(accg, dg_other, tiny.at[I1], tiny.at[I4], place.sibling).start()
        remote(accg, dg_other, tiny.at[I2], tiny.at[I4], place.across_other).start()

    for i in (micro - I2, micro - I1):
        back_ready(jnp.int32(i))

    sent, got = drain(place)
    sent(m_s, bulk.at[I6])

    @pl.when(is_r)
    def _():
        sent(gbuf, bulk.at[5])
        sent(m_s, bulk.at[7])
        remote(accg, dg_other, tiny.at[I2], tiny.at[I4], place.sibling).wait_send()

    @pl.when(place.home == I1)
    def _():
        sent(gbuf.at[I0:EARLY_G], bulk.at[I4])
        got(dx_s, dx_sem)

    @pl.when(jnp.logical_not(is_first))
    def _():
        remote(loss_mine, loss_mine, loss_sem.at[I0], loss_sem.at[I1], place.sibling).wait_send()
    remote(loss_mine, loss_mine, loss_sem.at[I2], loss_sem.at[I3], place.sibling).wait_send()
    remote(loss_mine, loss_mine, loss_sem.at[I2], loss_sem.at[I3], place.sibling).wait_recv()

    @pl.when(place.home == I2)
    def _():
        sent(a_s, bulk.at[I8])

    remote(accg, dg_other, tiny.at[I1], tiny.at[I4], place.sibling).wait_send()
    got(od_other, do_sem)

    @pl.when(place.is_l | home13)
    def _():
        got(og_other, go_sem)

    @pl.when(is_first & is_r)
    def _():
        got(og_same.at[I0:EARLY_G], gs_sem)
        got(og_other.at[I0:EARLY_G], go_sem)
    got(dg_same, tiny.at[I0])
    got(dg_other, tiny.at[I4])

    @pl.when(is_r)
    def _():
        got(od_same, ds_sem)

    @pl.when(place.is_l)
    def _():
        got(og_same, gs_sem)

    @pl.when(is_last & is_r)
    def _():
        got(oa_same, as_sem)
        got(oa_other, ao_sem)


def shapes(*dims_list):
    return [jax.ShapeDtypeStruct(d, BF) for d in dims_list]


def forward_phase(dims, x, y, own, own_gains):
    micro, seq, width, heads, head_dim, ffn = dims
    half = heads // I2 * HEAD_PAD
    act = (micro, seq, width)
    raw = [w.shape for w in own]
    turned = [(I3, width, CHUNK), (I1, width, CHUNK), (ffn // I2, width), (I3, width, CHUNK)]
    out_shape = shapes(act, act, (micro, seq, I6 * half), (micro, seq, ffn), *[act] * 7)
    out_shape += [jax.ShapeDtypeStruct(s, F32) for s in ((I8, 128), own_gains.shape)]
    out_shape += shapes(*raw, *raw, *turned, *turned, turned[I0], turned[I0])
    any_spec = pl.BlockSpec(memory_space=ANY)
    vmem, dma = pltpu.VMEM, pltpu.SemaphoreType.DMA
    row = vmem((seq, width), BF)
    scratch = [
        vmem(act, BF), row, vmem((I2, seq, width), BF), row, row, row, vmem((seq, I6 * half), BF), vmem((seq, ffn), BF), vmem((seq, CHUNK), BF),
        vmem((seq, I2 * half), BF), vmem((seq, width), F32), vmem((I8, width), F32), vmem((I8, 128), F32), vmem((I2, width), F32),
        vmem((I6, CHUNK, width), BF), vmem((I2, CHUNK, width), BF), vmem((DEPTH, width, CHUNK), BF),
        dma((I4,)), dma((I4,)), dma((I4,)), dma((I4,)), dma((12,)), dma((I2,)), dma((I2,)), dma((I2,)),
        dma((micro,)), dma((I2,)), dma((I2,)), dma((I3,)), dma((DEPTH,)), dma((I6,)), dma((I2,)), dma((I2,)), dma(()), dma(()),
        dma(()), dma(()), dma(()), dma(()), dma(()), dma(()), dma((I4,)), dma((I2,)), dma(()),
    ]
    return pl.pallas_call(
        functools.partial(forward_kernel, dims),
        out_shape=tuple(out_shape),
        in_specs=[any_spec] * I6 + [pl.BlockSpec(memory_space=vmem)],
        out_specs=(any_spec,) * len(out_shape),
        scratch_shapes=scratch,
        compiler_params=pltpu.CompilerParams(collective_id=I0, has_side_effects=True, vmem_limit_bytes=VMEM_LIMIT),
        name='forward_phase',
    )(x, y, *own, own_gains)


def backward_phase(dims, saved, weights, gains, loss, after, placed):
    micro, seq, width, heads, head_dim, ffn = dims
    half = heads // I2 * HEAD_PAD
    act = (micro, seq, width)
    out_shape = shapes(*[act] * I8) + [jax.ShapeDtypeStruct((I2, I8, width), F32)] * I2 + [jax.ShapeDtypeStruct((I2, I8, 128), F32)]
    any_spec = pl.BlockSpec(memory_space=ANY)
    vmem, dma = pltpu.VMEM, pltpu.SemaphoreType.DMA
    scratch = [
        vmem(act, BF), vmem((seq, width), BF), vmem((I2, seq, width), BF), vmem((seq, I6 * half), BF), vmem((seq, ffn), BF),
        vmem((I2, seq, width), BF), vmem((seq, CHUNK), BF), vmem((seq, I2 * half), BF), vmem((seq, I6 * half), BF), vmem((seq, width), F32),
        vmem((I2, I8, width), F32), vmem((I6, CHUNK, width), BF), vmem((BACK_DEPTH, width, CHUNK), BF), vmem((KDEPTH, CHUNK, width), BF),
        dma((micro,)), dma((I2,)), dma((I2,)), dma(()), dma((I2,)), dma(()), dma((BACK_DEPTH,)), dma((KDEPTH,)), dma((I6,)), dma((I4,)),
        dma(()), dma(()), dma(()), dma(()), dma(()), dma(()), dma((9,)), dma((5,)), dma((I4,)),
    ]
    return pl.pallas_call(
        functools.partial(backward_kernel, dims),
        out_shape=tuple(out_shape),
        in_specs=[any_spec] * 14 + [pl.BlockSpec(memory_space=vmem)] * I2 + [any_spec] * 5,
        out_specs=(any_spec,) * len(out_shape),
        scratch_shapes=scratch,
        input_output_aliases={17: I4, 18: 5, 19: I6, 20: 7},
        compiler_params=pltpu.CompilerParams(collective_id=I1, has_side_effects=True, vmem_limit_bytes=VMEM_LIMIT),
        name='backward_phase',
    )(*saved, *weights, gains, loss, after, *placed)


def recompute_kernel(dims, early, h_same, h_other, a_same, a_other, gains, wq, wu, *refs):
    (done, u_o, qkv_o, ctx_o, n1_o, n2_o), (wqbuf, wubuf, count, sem) = refs[-10:-I4], refs[-I4:]
    micro, seq, width, heads, head_dim, ffn = dims
    place = Place()
    scale = head_dim ** -0.5
    half = heads // I2 * HEAD_PAD
    steps = I2 * micro * seq // BLOCK

    def body(hs, ho, rs, ro, u, qkv, ctx, n1, n2):
        step = count[I0]
        count[I0] = step + I1
        for low, high, gain, dst in ((hs, ho, gains[I1:I2, :], n2), (rs, ro, gains[I0:I1, :], n1)):
            @pl.when(step < steps // I2)
            def _(low=low, gain=gain, dst=dst):
                norm_rows(low, gain, dst, BLOCK)

            @pl.when(step >= steps // I2)
            def _(high=high, gain=gain, dst=dst):
                norm_rows(high, gain, dst, BLOCK)

        def qkv_step(j, c):
            rows = pl.ds(pl.multiple_of(j * SUB, SUB), SUB)
            qkv[:, lanes(j * SUB, SUB)] = mm_nt(n1[...], wqbuf[rows, :]).astype(BF)
            u[:, lanes(j * SUB, SUB)] = mm(n2[...], wubuf[:, lanes(j * SUB, SUB)]).astype(BF)
            return c
        lax.fori_loop(I0, I3 * half // SUB, qkv_step, I0)

        def head_step(j, c):
            at = [(pl.ds(s, seq), r * HEAD_PAD) for s in range(I0, BLOCK, seq) for r in range(I4)]
            base = j * (I4 * HEAD_PAD)
            views = [[qkv[rows, lanes(base + t * half + col, HEAD_PAD)] for t in range(I3)] for rows, col in at]
            for (rows, col), context in zip(at, attention_forward(views, scale)):
                ctx[rows, lanes(base + col, HEAD_PAD)] = context
            return c
        lax.fori_loop(I0, I2, head_step, I0)

    @pl.when(place.home < I2 if early else place.home > I1)
    def _():
        wqbuf[...] = jnp.zeros_like(wqbuf)
        for t in range(I3):
            load_heads(wq, t, wqbuf.at[pl.ds(t * CHUNK, CHUNK)], sem.at[I0])
        up = pltpu.make_async_copy(wu, wubuf, sem.at[I1])
        up.start()
        up.wait()
        pltpu.make_async_copy(wq, wqbuf.at[I0:wq.shape[I0]], sem.at[I0]).wait()
        count[I0] = I0
        low = pl.BlockSpec((BLOCK, width), lambda i: (jnp.minimum(i, steps // I2 - I1), I0))
        high = pl.BlockSpec((BLOCK, width), lambda i: (jnp.maximum(i - steps // I2, I0), I0))
        block = lambda n: pl.BlockSpec((BLOCK, n), lambda i: (i, I0))
        pltpu.emit_pipeline(body, grid=(steps,), in_specs=[low, high, low, high],
                            out_specs=[block(ffn // I2), block(I3 * half), block(half), block(width), block(width)])(
            h_same, h_other, a_same, a_other, u_o, qkv_o, ctx_o, n1_o, n2_o)


def owner_recompute(dims, early, again, h_rows, a_rows, gains, own):
    micro, seq, width, heads, head_dim, ffn = dims
    half = heads // I2 * HEAD_PAD
    tokens = I2 * micro * seq
    any_spec = pl.BlockSpec(memory_space=ANY)
    vmem = pltpu.VMEM
    earlier = () if early else tuple(again)
    return pl.pallas_call(
        functools.partial(recompute_kernel, dims, early),
        out_shape=(jax.ShapeDtypeStruct((I8, 128), F32), *shapes((tokens, ffn // I2), (tokens, I3 * half), (tokens, half), (tokens, width), (tokens, width))),
        in_specs=[any_spec] * I4 + [pl.BlockSpec(memory_space=vmem)] + [any_spec] * (I2 + len(earlier)),
        out_specs=(any_spec,) * I6,
        scratch_shapes=[vmem((I3 * half, width), BF), vmem((width, ffn // I2), BF), pltpu.SMEM((I1,), jnp.int32), pltpu.SemaphoreType.DMA((I2,))],
        input_output_aliases={7 + i: I1 + i for i in range(len(earlier))},
        compiler_params=pltpu.CompilerParams(has_side_effects=True, vmem_limit_bytes=VMEM_LIMIT),
        name='owner_recompute',
    )(*h_rows, *a_rows, gains, own[I0], own[I2], *earlier)


def spread_dx(step, last, dx, d_in, og_same, og_other, bounce, here_sem, parent_sem, sib_sem, send_sems, og_sems):
    place = Place()
    micro = dx.shape[I0]
    along_x = place.at(place.tp, (place.stage + I2) % I4)
    barrier = pltpu.get_barrier_semaphore()
    is_leaf = place.home > I1
    gives_g = (place.home == I1) & place.is_l
    takes_g = (place.home == I0) & jnp.logical_not(place.is_l)
    late = [micro - I1 - i for i in range(micro) if i % I2 == I0 or i > I2 * EARLY_G]

    def block(m):
        return d_in.at[m, place.core]

    def to_sibling(m, src):
        remote(src, block(m), send_sems.at[I0], sib_sem, place.sibling).start()

    def tell(there):
        pl.semaphore_signal(barrier, inc=I1, device_id=there, device_id_type=MESH)

    @pl.when(step == I0)
    def _():
        tell(place.sibling)

        @pl.when(is_leaf)
        def _():
            tell(along_x)

        @pl.when(takes_g)
        def _():
            tell(place.across)

    @pl.when((step == I1) & jnp.logical_not(is_leaf))
    def _():
        pl.semaphore_wait(barrier, I2 + gives_g.astype(jnp.int32))

        @pl.when(gives_g)
        def _():
            for t, og in enumerate((og_same, og_other)):
                for m in late:
                    remote(og.at[m], og.at[m], og_sems.at[t], og_sems.at[I2 + t], place.across).start()
        for m in reversed(range(micro)):
            remote(dx.at[m], block(m), send_sems.at[I1], parent_sem.at[m], along_x).start()
            to_sibling(m, dx.at[m])
        pltpu.make_async_copy(dx, bounce, here_sem).start()

    @pl.when((step == I2) & jnp.logical_not(is_leaf))
    def _():
        pltpu.make_async_copy(dx, bounce, here_sem).wait()
        for m in range(micro):
            pltpu.make_async_copy(bounce.at[m], block(m), here_sem).start()

    @pl.when((step == (last + I1) // I2) & takes_g)
    def _():
        for t, og in enumerate((og_same, og_other)):
            part = og.at[I0:len(late)]
            remote(part, part, og_sems.at[t], og_sems.at[I2 + t], place.across).wait_recv()

    @pl.when((step == last) & is_leaf)
    def _():
        pl.semaphore_wait(barrier, I1)
        for m in reversed(range(micro)):
            remote(block(m), block(m), send_sems.at[I0], parent_sem.at[m], place.sibling).wait_recv()
            to_sibling(m, block(m))

    @pl.when(step == last)
    def _():
        remote(dx, dx, send_sems.at[I0], sib_sem, place.sibling).wait_send()

        @pl.when(jnp.logical_not(is_leaf))
        def _():
            remote(dx, dx, send_sems.at[I1], sib_sem, place.sibling).wait_send()
            pltpu.make_async_copy(dx, dx, here_sem).wait()

        @pl.when(gives_g)
        def _():
            for t, og in enumerate((og_same, og_other)):
                part = og.at[I0:len(late)]
                remote(part, part, og_sems.at[t], og_sems.at[I2 + t], place.across).wait_send()
        remote(dx, dx, send_sems.at[I0], sib_sem, place.sibling).wait_recv()


def owner_backward_kernel(dims, dx, ds, do, u, qkv, wo, wd, gs_in, go_in, dqkv, dup, z, d_in, og_same, og_other,
                          dmid, gbuf, dctx, wobuf, bounce, sem, g_sem, here_sem, parent_sem, sib_sem, send_sems, og_sems):
    micro, seq, width, heads, head_dim, ffn = dims
    half = heads // I2 * HEAD_PAD
    scale = head_dim ** -0.5
    step, steps = pl.program_id(I0), pl.num_programs(I0)
    blocks = steps // I2
    spread_dx(step, steps - I1, dx, d_in, og_same, og_other, bounce, here_sem, parent_sem, sib_sem, send_sems, og_sems)

    @pl.when(step == I0)
    def _():
        wobuf[...] = jnp.zeros_like(wobuf)
        load_heads(wo, I0, wobuf, sem)
        pltpu.make_async_copy(wo, wobuf.at[I0:wo.shape[I0]], sem).wait()

    def g_load(n, start):
        rows = BLOCK // seq
        for og, low in ((og_same, I0), (og_other, blocks // I2)):
            @pl.when((n >= low) & (n < low + blocks // I2))
            def _(og=og, low=low):
                copy = pltpu.make_async_copy(og.at[pl.ds((n - low) * rows, rows)], gbuf.at[n % I2], g_sem.at[n % I2])
                copy.start() if start else copy.wait()

    @pl.when(step < blocks)
    def _():
        @pl.when(step < blocks // I2)
        def _():
            dmid[...] = ds[...]

        @pl.when(step >= blocks // I2)
        def _():
            dmid[...] = do[...]

        def ctx_step(j, c):
            rows = pl.ds(pl.multiple_of(j * SUB, SUB), SUB)
            dctx[:, lanes(j * SUB, SUB)] = mm_nt(dmid[...], wobuf[rows, :]).astype(BF)
            return c
        lax.fori_loop(I0, half // SUB, ctx_step, I0)

        def head_step(j, c):
            base = j * (I2 * HEAD_PAD)
            at = [(pl.ds(s, seq), base + r * HEAD_PAD) for s in range(I0, BLOCK, seq) for r in range(I2)]
            group = [(*(qkv[rows, lanes(t * half + col, HEAD_PAD)] for t in range(I3)), dctx[rows, lanes(col, HEAD_PAD)]) for rows, col in at]
            for (rows, col), grads in zip(at, attention_backward(group, scale)):
                for t, value in enumerate(grads):
                    dqkv[rows, lanes(t * half + col, HEAD_PAD)] = value
            return c
        lax.fori_loop(I0, heads // I4, head_step, I0)

    @pl.when(step == blocks)
    def _():
        g_load(step - blocks, True)

    @pl.when(step >= blocks)
    def _():
        n = step - blocks
        g_load(n + I1, True)
        g_load(n, False)
        grad = gbuf.at[n % I2]

        def mlp_step(j, c):
            rows = pl.ds(pl.multiple_of(j * SUB, SUB), SUB)
            cols = lanes(j * SUB, SUB)
            dz = mm_nt(grad[...].reshape(BLOCK, width), wd[rows, :]).astype(BF).astype(F32)
            up = u[:, cols].astype(F32)
            gate, up2 = gelu_gate(up)
            hidden = up * gate
            z[:, cols] = hidden.astype(BF)
            dup[:, cols] = (dz * gelu_slope(hidden, gate, up2)).astype(BF)
            return c
        lax.fori_loop(I0, ffn // I2 // SUB, mlp_step, I0)


def owner_backward(dims, dx, d_rows, og, ups, qkv, own):
    micro, seq, width, heads, head_dim, ffn = dims
    half = heads // I2 * HEAD_PAD
    tokens = I2 * micro * seq
    blocks = tokens // BLOCK
    vmem, dma = pltpu.VMEM, pltpu.SemaphoreType.DMA
    any_spec = pl.BlockSpec(memory_space=ANY)
    first = lambda i: jnp.minimum(i, blocks - I1)
    second = lambda i: jnp.maximum(i - blocks, I0)
    low = pl.BlockSpec((BLOCK, width), lambda i: (jnp.minimum(i, blocks // I2 - I1), I0))
    high = pl.BlockSpec((BLOCK, width), lambda i: (jnp.maximum(first(i) - blocks // I2, I0), I0))
    attn_block = pl.BlockSpec((BLOCK, I3 * half), lambda i: (first(i), I0))
    mlp_block = pl.BlockSpec((BLOCK, ffn // I2), lambda i: (second(i), I0))
    act = (micro, seq, width)
    return pl.pallas_call(
        functools.partial(owner_backward_kernel, dims),
        grid=(I2 * blocks,),
        out_shape=tuple(shapes((tokens, I3 * half), (tokens, ffn // I2), (tokens, ffn // I2), (micro, I2, seq, width), act, act)),
        in_specs=[any_spec, low, high, mlp_block, attn_block, any_spec, pl.BlockSpec((ffn // I2, width), lambda i: (I0, I0)), any_spec, any_spec],
        out_specs=(attn_block, mlp_block, mlp_block, any_spec, any_spec, any_spec),
        scratch_shapes=[vmem((BLOCK, width), BF), vmem((I2, BLOCK // seq, seq, width), BF), vmem((BLOCK, half), BF), vmem((half, width), BF), vmem(act, BF),
                        dma(()), dma((I2,)), dma(()), dma((micro,)), dma(()), dma((I2,)), dma((I4,))],
        input_output_aliases={7: I4, I8: 5},
        compiler_params=pltpu.CompilerParams(collective_id=I2, has_side_effects=True, vmem_limit_bytes=VMEM_LIMIT),
        name='owner_backward',
    )(dx, *d_rows, ups, qkv, own[I1], own[I3], *og)


def bring(pairs, sem):
    copies = [pltpu.make_async_copy(src, dst, sem.at[i]) for i, (src, dst) in enumerate(pairs)]
    for copy in copies:
        copy.start()
    for copy in copies:
        copy.wait()


def attn_products_kernel(dq, dk, dv, ctx, n1_o, ds, do, dx_in, dwq, dwo, dx_out, n1, dmid, dqkvt, ctxt, bounce, sem, dx_sem):
    tokens, width = n1.shape
    part = tokens // I2
    head_dim = dwo.shape[I1]
    step, last = pl.program_id(I0), pl.num_programs(I0) - I1
    into, out_of = pltpu.make_async_copy(dx_in, bounce, dx_sem), pltpu.make_async_copy(bounce, dx_out, dx_sem)

    @pl.when(step == I1)
    def _():
        into.start()

    @pl.when(step == I2)
    def _():
        into.wait()
        out_of.start()

    @pl.when(step == last)
    def _():
        out_of.wait()

    @pl.when(step == I0)
    def _():
        bring([(n1_o, n1), (ds, dmid.at[pl.ds(I0, part)]), (do, dmid.at[pl.ds(part, part)])], sem)

    def turn(rows):
        for t, block in enumerate((dq, dk, dv)):
            for r in range(I2):
                at = (I2 * t + r) * head_dim
                dqkvt[at:at + head_dim, rows] = block[rows, r * HEAD_PAD:(r + I1) * HEAD_PAD].T[I0:head_dim]
        for r in range(I2):
            ctxt[r * head_dim:(r + I1) * head_dim, rows] = ctx[rows, r * HEAD_PAD:(r + I1) * HEAD_PAD].T[I0:head_dim]
    rows_loop(tokens, SUB, turn)
    for c in range(I0, width, SUB):
        cut = slice(c, c + SUB)
        dwq[:, :, :, cut] = mm(dqkvt[...], n1[:, cut]).reshape(I3, I2, head_dim, SUB)
        dwo[:, :, cut] = mm(ctxt[...], dmid[:, cut]).reshape(I2, head_dim, SUB)


def attn_products(dqkv, ctx, n1, d_rows, dx, out_dims):
    heads, head_dim, width = out_dims
    tokens = n1.shape[I0]
    vmem = pltpu.VMEM
    any_spec = pl.BlockSpec(memory_space=ANY)
    pairs = heads // I2
    cols = lambda t: pl.BlockSpec((tokens, I2 * HEAD_PAD), lambda i: (I0, t * pairs + i))
    return pl.pallas_call(
        attn_products_kernel,
        grid=(pairs,),
        out_shape=(jax.ShapeDtypeStruct((I3,) + out_dims, F32), jax.ShapeDtypeStruct(out_dims, F32), jax.ShapeDtypeStruct(dx.shape, BF)),
        in_specs=[cols(I0), cols(I1), cols(I2), cols(I0), any_spec, any_spec, any_spec, any_spec],
        out_specs=(pl.BlockSpec((I3, I2, head_dim, width), lambda i: (I0, i, I0, I0)), pl.BlockSpec((I2, head_dim, width), lambda i: (i, I0, I0)), any_spec),
        scratch_shapes=[vmem((tokens, width), BF), vmem((tokens, width), BF), vmem((I6 * head_dim, tokens), BF), vmem((I2 * head_dim, tokens), BF),
                        vmem(dx.shape, BF), pltpu.SemaphoreType.DMA((I3,)), pltpu.SemaphoreType.DMA(())],
        compiler_params=pltpu.CompilerParams(vmem_limit_bytes=VMEM_LIMIT),
        name='attn_products',
    )(dqkv, dqkv, dqkv, ctx, n1, *d_rows, dx)


def mlp_products_kernel(dup, z, n2_o, gs, go, dwu, dwd, n2t, grad, zt, stage, sem):
    width, tokens = n2t.shape
    part = tokens // I2

    @pl.when(pl.program_id(I0) == I0)
    def _():
        bring([(n2_o, stage), (gs, grad.at[pl.ds(I0, part)]), (go, grad.at[pl.ds(part, part)])], sem)

        def turn(rows):
            for c in range(I0, width, SUB):
                n2t[c:c + SUB, rows] = stage[rows, c:c + SUB].T
        rows_loop(tokens, SUB, turn)

    def turn_z(rows):
        for c in range(I0, z.shape[I1], SUB):
            zt[c:c + SUB, rows] = z[rows, c:c + SUB].T
    rows_loop(tokens, SUB, turn_z)
    for c in range(I0, width, I2 * SUB):
        dwu[c:c + I2 * SUB, :] = mm(n2t[c:c + I2 * SUB, :], dup[...])
    for c in range(I0, width, SUB):
        dwd[:, c:c + SUB] = mm(zt[...], grad[:, c:c + SUB])


def mlp_products(dup, hidden, n2, g_rows):
    tokens, width = n2.shape
    cols = dup.shape[I1]
    vmem = pltpu.VMEM
    any_spec = pl.BlockSpec(memory_space=ANY)
    block = pl.BlockSpec((tokens, SUB), lambda i: (I0, i))
    return pl.pallas_call(
        mlp_products_kernel,
        grid=(cols // SUB,),
        out_shape=(jax.ShapeDtypeStruct((width, cols), F32), jax.ShapeDtypeStruct((cols, width), F32)),
        in_specs=[block, block, any_spec, any_spec, any_spec],
        out_specs=(pl.BlockSpec((width, SUB), lambda i: (I0, i)), pl.BlockSpec((SUB, width), lambda i: (i, I0))),
        scratch_shapes=[vmem((width, tokens), BF), vmem((tokens, width), BF), vmem((SUB, tokens), BF), vmem((tokens, width), BF), pltpu.SemaphoreType.DMA((I3,))],
        compiler_params=pltpu.CompilerParams(vmem_limit_bytes=VMEM_LIMIT),
        name='mlp_products',
    )(dup, hidden, n2, *g_rows)


def solution(mesh):
    act_spec = P('rep', None, None, None)
    weight_specs = (
        P(('rep', 'stage'), None, None, 'tp', None),
        P(('rep', 'stage'), 'tp', None, None),
        P(('rep', 'stage'), None, 'tp'),
        P(('rep', 'stage'), 'tp', None),
        P(('rep', 'stage'), None),
        P(('rep', 'stage'), None),
    )

    def device_fn(inputs, targets, w_qkv, w_out, w_up, w_down, gain_attn, gain_mlp):
        micro_count, _, seq_len, width = inputs.shape
        dims = (micro_count, seq_len, width, I2 * w_out.shape[I1], w_out.shape[I2], I2 * w_up.shape[I2])
        norm_factor = 1.0 / (inputs.size)
        own = (w_qkv[I0], w_out[I0], w_up[I0], w_down[I0])
        own_gains = jnp.concatenate([gain_attn, gain_mlp]).astype(F32)
        rows_of = (own[I0].transpose(I1, I2, I3, I0).reshape(-I1, width), own[I1].reshape(-I1, width), own[I2], own[I3])

        (acts, mids, qkv, ups, seeds, oh_same, oh_other, oa_same, oa_other, og_same, og_other, loss_tile, home_gains, *weights) = forward_phase(dims, inputs, targets, rows_of, own_gains)
        (nq, no, nu, nd), (fq, fo, fu, fd) = weights[I0:I4], weights[I4:I8]
        (tq0, to0, tu0, td0), (tq1, to1, tu1, td1) = weights[I8:12], weights[12:16]

        flat = lambda *rows: [r.reshape(-I1, width) for r in rows]
        h_rows = flat(oh_same, oh_other)
        done, *again = owner_recompute(dims, True, None, h_rows, flat(oa_same, oa_other), own_gains, rows_of)
        dx, _, od_same, od_other, og_same, og_other, oa_same, oa_other, dg_same, dg_other, loss_all = backward_phase(
            dims, (acts, mids, qkv, ups, seeds), (rows_of[I0], nq, fq, td0, td1, to0, to1, tu0, tu1), home_gains, loss_tile, done, (og_same, og_other, oa_same, oa_other))
        _, *again = owner_recompute(dims, False, again, h_rows, flat(oa_same, oa_other), own_gains, rows_of)
        ups_own, qkv_own, ctx_own, n1, n2 = again
        d_rows = flat(od_same, od_other)
        d_qkv_rows, d_up_rows, hidden, dx_all, og_same, og_other = owner_backward(dims, dx, d_rows, (og_same, og_other), ups_own, qkv_own, rows_of)
        d_qkv, d_out, d_inputs = attn_products(d_qkv_rows, ctx_own, n1, d_rows, dx_all, w_out.shape[I1:])
        d_up, d_down = mlp_products(d_up_rows, hidden, n2, flat(og_same, og_other))
        weight_grads = (d_qkv.transpose(I3, I0, I1, I2), d_out, d_up, d_down)
        mine = jnp.sum(dg_same + dg_other, I1)
        loss = jnp.sum(loss_all) * (0.5 * norm_factor)

        return (loss.reshape(I1), d_inputs) + tuple(g[None] for g in weight_grads) + (mine[I0][None], mine[I1][None])

    return jax.shard_map(device_fn, mesh=mesh, in_specs=(act_spec, act_spec) + weight_specs, out_specs=(P('rep'), act_spec) + weight_specs, check_vma=False)
```

```python
import functools

import jax
import jax.numpy as jnp
from jax import lax
from jax.experimental import pallas as pl
from jax.experimental.pallas import tpu as pltpu
from jax.sharding import PartitionSpec as P

NORM_EPS = 1e-5
BF = jnp.bfloat16
F32 = jnp.float32
MESH = pl.DeviceIdType.MESH
ANY = pl.ANY


GELU_A = 0.7978845608028654
GELU_B = 0.044715
I0, I1, I2, I3, I4, I6, I8 = 0, 1, 2, 3, 4, 6, 8
CHUNK = 1024
BLOCK = 384
SUB = 256
DEPTH = 6
BACK_DEPTH = 6
KDEPTH = 3
EARLY_G = 3
STAGGER_NS = 6000
EARLY_SEEDS = 5
HEAD_PAD = 128
VMEM_LIMIT = 67043328


def mm(a, b):
    return lax.dot_general(a, b, (((I1,), (I0,)), ((), ())), preferred_element_type=F32)


def mm_nt(a, b):
    return lax.dot_general(a, b, (((I1,), (I1,)), ((), ())), preferred_element_type=F32)


def mm_tn(a, b):
    return lax.dot_general(a, b, (((I0,), (I0,)), ((), ())), preferred_element_type=F32)


class Place:
    def __init__(self):
        self.tp = lax.axis_index('tp')
        self.stage = lax.axis_index('stage')
        self.core = self.stage % I2
        self.x_pos = self.stage // I2
        self.home = self.x_pos * (I3 - I2 * self.tp) + self.tp
        self.is_l = self.stage == self.home
        self.sib = self.stage + I1 - I2 * self.core

    def at(self, tp, stage):
        return {'tp': tp, 'stage': stage}

    @property
    def sibling(self):
        return self.at(self.tp, self.sib)

    @property
    def along_x(self):
        return self.at(self.tp, (self.stage + I2) % I4)

    @property
    def across(self):
        return self.at(I1 - self.tp, self.stage)

    @property
    def across_other(self):
        return self.at(I1 - self.tp, self.sib)

    def chain(self, delta):
        there = self.home + delta
        x_pos = there // I2
        tp = there % I2 + x_pos * (I1 - I2 * (there % I2))
        return self.at(tp, I2 * x_pos + self.core)


def entry_barrier(place):
    barrier = pltpu.get_barrier_semaphore()
    for d_tp in (I0, I1):
        for d_stage in range(I4):
            if d_tp or d_stage:
                tp = place.tp + d_tp - I2 * d_tp * place.tp
                stage = (place.stage + d_stage) % I4
                pl.semaphore_signal(barrier, inc=I1, device_id=place.at(tp, stage), device_id_type=MESH)
    pl.semaphore_wait(barrier, 7)


def remote(src, dst, send_sem, recv_sem, device_id):
    return pltpu.make_async_remote_copy(src_ref=src, dst_ref=dst, send_sem=send_sem, recv_sem=recv_sem, device_id=device_id, device_id_type=MESH)


def rows_loop(total, step, body):
    def run(i, carry):
        body(pl.ds(pl.multiple_of(i * step, step), step))
        return carry
    lax.fori_loop(I0, total // step, run, I0)


def norm_rows(src, gain_row, dst, total):
    def body(rows):
        v = src[rows, :].astype(F32)
        inv = lax.rsqrt(jnp.mean(v * v, axis=-I1, keepdims=True) + NORM_EPS)
        dst[rows, :] = (v * inv * gain_row).astype(BF)
    rows_loop(total, 32, body)


def gelu_gate(u):
    u2 = u * u
    t = jnp.tanh(u * (GELU_A + (GELU_A * GELU_B) * u2))
    return 0.5 * t + 0.5, u2


def gelu_slope(hidden, gate, u2):
    return gate + hidden * (1.0 - gate) * (2.0 * GELU_A + (6.0 * GELU_A * GELU_B) * u2)


def row_parts(heads, cut=128):
    return [(*(x[low:high] for x in queries), *(x[:high] for x in keys), low)
            for queries, keys in heads for low, high in ((I0, cut), (cut, queries[I0].shape[I0]))]


def softmax_parts(scores, starts):
    masked = []
    for s, start in zip(scores, starts):
        q_pos = lax.broadcasted_iota(jnp.int32, s.shape, I0) + start
        k_pos = lax.broadcasted_iota(jnp.int32, s.shape, I1)
        masked.append(jnp.where(k_pos <= q_pos, s, -1e30))
    tops = [jnp.max(s, axis=-I1, keepdims=True) for s in masked]
    powers = [jnp.exp(s - top) for s, top in zip(masked, tops)]
    scales = [1.0 / jnp.sum(e, axis=-I1, keepdims=True) for e in powers]
    return [e * r for e, r in zip(powers, scales)]


def join_keys(top, low, cut=128):
    return jnp.concatenate([top + low[:cut], low[cut:]], I0).astype(BF)


def attention_forward(heads, scale):
    units = row_parts([((q,), (k, v)) for q, k, v in heads])
    probs = softmax_parts([mm_nt(q, k) * scale for q, k, _, _ in units], [u[-I1] for u in units])
    parts = [mm(p.astype(BF), u[I2]) for p, u in zip(probs, units)]
    return [jnp.concatenate([a, b], I0).astype(BF) for a, b in zip(parts[I0::I2], parts[I1::I2])]


def attention_backward(heads, scale):
    units = row_parts([((q, dc), (k, v)) for q, k, v, dc in heads])
    scores = [mm_nt(q, k) * scale for q, _, k, _, _ in units]
    dps = [mm_nt(dc, v) for _, dc, _, v, _ in units]
    probs = softmax_parts(scores, [u[-I1] for u in units])
    dps = [dp.astype(BF).astype(F32) for dp in dps]
    deltas = [jnp.sum(dp * p, axis=-I1, keepdims=True) for dp, p in zip(dps, probs)]
    dvs = [mm_tn(p.astype(BF), u[I1]) for p, u in zip(probs, units)]
    dss = [p * (dp - delta) * scale for p, dp, delta in zip(probs, dps, deltas)]
    terms = []
    for ds in dss:
        hi = ds.astype(BF)
        rest = ds - hi.astype(F32)
        lo = rest.astype(BF)
        terms.append((hi, lo, (rest - lo.astype(F32)).astype(BF)))
    dqs = [mm(hi, u[I2]) + (mm(lo, u[I2]) + mm(tail, u[I2])) for (hi, lo, tail), u in zip(terms, units)]
    dks = [mm_tn(hi, u[I0]) + (mm_tn(lo, u[I0]) + mm_tn(tail, u[I0])) for (hi, lo, tail), u in zip(terms, units)]
    return [(jnp.concatenate([dqs[i], dqs[i + I1]], I0).astype(BF), join_keys(dks[i], dks[i + I1]), join_keys(dvs[i], dvs[i + I1]))
            for i in range(I0, len(units), I2)]


def lanes(offset, size):
    return pl.ds(pl.multiple_of(offset, 128), size)


def load_resident(buf, sem, halves):
    for c in range(I6):
        for condition, ref in halves[c // I3]:
            copy = pltpu.make_async_copy(ref.at[(c % I3) * CHUNK:(c % I3 + I1) * CHUNK, :], buf.at[c], sem.at[c])
            if condition is None:
                copy.start()
            else:
                pl.when(condition)(copy.start)


def load_heads(ref, index, dst, sem):
    for r in range(I8):
        rows = pl.ds(pl.multiple_of(index * 768 + r * 96, 96), 96)
        pltpu.make_async_copy(ref.at[rows, :], dst.at[r * 128:r * 128 + 96, :], sem).start()


class Stream:
    def __init__(self, buf, sem, depth, parts, total, by_heads):
        self.buf, self.sem, self.depth, self.parts, self.total, self.by_heads = buf, sem, depth, parts, total, by_heads
        self.per_tick = sum(p[I1] for p in parts)

    def copy_in(self, ref, index, slot):
        if not self.by_heads:
            pltpu.make_async_copy(ref.at[index], self.buf.at[slot], self.sem.at[slot]).start()
            return
        load_heads(ref, index, self.buf.at[slot], self.sem.at[slot])

    def start(self, seq):
        @pl.when(seq < self.total)
        def _():
            j = seq % self.per_tick
            slot = seq % self.depth
            base = I0
            for choices, chunks in self.parts:
                for condition, ref in choices:
                    here = (j >= base) & (j < base + chunks)
                    here = here if condition is None else here & condition

                    @pl.when(here)
                    def _(ref=ref, low=base):
                        self.copy_in(ref, j - low, slot)
                base += chunks

    def prime(self):
        for seq in range(self.depth):
            self.start(jnp.int32(seq))

    def wait(self, seq):
        slot = seq % self.depth
        ref = self.parts[I0][I0][I0][I1]
        if self.by_heads:
            pltpu.make_async_copy(ref.at[I0:768, :], self.buf.at[slot, I0:768, :], self.sem.at[slot]).wait()
        else:
            pltpu.make_async_copy(ref.at[I0], self.buf.at[slot], self.sem.at[slot]).wait()
        return self.buf.at[slot]


PIECES = [(0, 0, 0), (0, 0, 1), (0, 0, 2), (1, 0, 0), (2, 1, 0), (2, 1, 1), (2, 1, 2), (2, 1, 3), (3, 0, 0), (3, 0, 1), (3, 0, 2), (3, 0, 3)]


ROUND = (10, 11)
ROUND_STEPS = (6, 8)


def piece(ref, axis, index):
    return ref.at[index * 768:(index + I1) * 768, :] if axis == I0 else ref.at[:, index * 768:(index + I1) * 768]


def weight_phase(place, is_r, own, near, far, turned, up_chunks, wn, wk, send_sem, y_send, d_send, near_sem, far_sem, load_sem, store_sem, chunk_sem,
                 round_a, round_b, ra_sem, rb_sem, x_send, xd_send, rs_send):
    wk[...] = jnp.zeros_like(wk)
    early = place.home < I2

    def piece_of(arrays, c):
        i, axis, index = PIECES[c]
        return piece(arrays[i], axis, index)

    @pl.when(place.is_l)
    def _():
        for i in range(I4):
            remote(own[i], near[i], send_sem.at[i], near_sem.at[i], place.sibling).start()

    @pl.when(is_r)
    def _():
        for k, c in enumerate(ROUND):
            @pl.when(early)
            def _(k=k, c=c):
                remote(piece_of(own, c), round_a.at[k], x_send.at[k], ra_sem.at[k], place.along_x).start()
        for c, (i, axis, index) in enumerate(PIECES):
            if c not in ROUND:
                remote(piece_of(own, c), piece_of(far, c), y_send.at[i], far_sem.at[c], place.across_other).start()
        for k, c in enumerate(ROUND):
            @pl.when(jnp.logical_not(early))
            def _(k=k, c=c):
                remote(piece_of(own, c), piece_of(far, c), x_send.at[k], far_sem.at[c], place.across_other).start()

    def load(i, refs, t, slot):
        for condition, ref in refs:
            def go(ref=ref):
                if i < I2:
                    for r in range(I2):
                        rows = pl.ds(pl.multiple_of(t * 192 + r * 96, 96), 96)
                        pltpu.make_async_copy(ref.at[rows, :], wk.at[I0, pl.ds(slot * SUB + r * 128, 96), :], load_sem.at[slot]).start()
                elif i == I2:
                    pltpu.make_async_copy(ref.at[:, lanes(t * SUB, SUB)], wn.at[slot, :, I0:SUB], load_sem.at[slot]).start()
                else:
                    rows = pl.ds(pl.multiple_of(t * SUB, SUB), SUB)
                    pltpu.make_async_copy(ref.at[rows, :], wk.at[I0, pl.ds(512 + slot * SUB, SUB), :], load_sem.at[slot]).start()
            if condition is None:
                go()
            else:
                pl.when(condition)(go)

    def loaded(i, refs, slot):
        ref = refs[I0][I1]
        if i < I2:
            pltpu.make_async_copy(ref.at[I0:192, :], wk.at[I0, I0:192, :], load_sem.at[slot]).wait()
        elif i == I2:
            pltpu.make_async_copy(ref.at[:, I0:SUB], wn.at[slot, :, I0:SUB], load_sem.at[slot]).wait()
        else:
            pltpu.make_async_copy(ref.at[I0:SUB, :], wk.at[I0, 512:768, :], load_sem.at[slot]).wait()

    def store(i, dst, t, slot):
        if i == I2:
            rows = pl.ds(pl.multiple_of(t * SUB, SUB), SUB)
            return pltpu.make_async_copy(wk.at[I1, pl.ds(slot * SUB, SUB), :], dst.at[rows, :], store_sem.at[slot])
        return pltpu.make_async_copy(wn.at[slot, :, SUB:512], dst.at[t // I4, :, lanes(t % I4 * SUB, SUB)], store_sem.at[slot])

    def keep(which, t, slot):
        return pltpu.make_async_copy(wn.at[slot, :, I0:SUB], up_chunks[which].at[t // I4, :, lanes(t % I4 * SUB, SUB)], chunk_sem.at[slot])

    def turn(i, refs, which, first, count):
        dst = turned[i][which]
        load(i, refs, first, I0)

        def step(n, c):
            slot = n % I2

            if i == I2:
                @pl.when(n > I0)
                def _():
                    keep(which, first + n - I1, I1 - slot).wait()

            @pl.when(n + I1 < count)
            def _():
                load(i, refs, first + n + I1, I1 - slot)
            loaded(i, refs, slot)
            if i == I2:
                keep(which, first + n, slot).start()

            @pl.when(n >= I2)
            def _():
                store(i, dst, first + n - I2, slot).wait()
            for b in range(I6):
                cut = slice(b * SUB, b * SUB + SUB)
                if i == I2:
                    wk[I1, pl.ds(pl.multiple_of(slot * SUB, SUB), SUB), cut] = wn[slot, cut, I0:SUB].T
                else:
                    base = I0 if i < I2 else 512
                    wn[slot, cut, SUB:512] = wk[I0, pl.ds(pl.multiple_of(base + slot * SUB, SUB), SUB), cut].T
            store(i, dst, first + n, slot).start()
            return c
        lax.fori_loop(I0, count, step, I0)
        for n in (count - I2, count - I1):
            store(i, dst, first + n, n % I2).wait()
        if i == I2:
            keep(which, first + count - I1, (count - I1) % I2).wait()

    counts = (12, I4, 12, 12)
    for i in range(I4):
        @pl.when(is_r)
        def _(i=i):
            remote(near[i], near[i], send_sem.at[i], near_sem.at[i], place.sibling).wait_recv()
        turn(i, [(place.is_l, own[i]), (is_r, near[i])], I0, I0, counts[i])
    done = [I0, I0, I0, I0]

    @pl.when(place.is_l & jnp.logical_not(early))
    def _():
        for k in range(len(ROUND)):
            remote(round_a.at[k], round_a.at[k], rs_send.at[k], ra_sem.at[k], place.sibling).wait_recv()
            remote(round_a.at[k], round_b.at[k], rs_send.at[k], rb_sem.at[k], place.across).start()
    for c, (i, axis, index) in enumerate(PIECES):
        view = piece_of(far, c)
        for k, step in enumerate(ROUND_STEPS):
            if c == step:
                @pl.when(is_r & jnp.logical_not(early))
                def _(k=k):
                    remote(round_b.at[k], round_b.at[k], rs_send.at[k], rb_sem.at[k], place.sibling).wait_recv()
                    remote(round_b.at[k], piece_of(far, ROUND[k]), rs_send.at[k], far_sem.at[ROUND[k]], place.along_x).start()
        remote(view, view, d_send.at[i], far_sem.at[c], place.sibling).wait_recv()
        gives = is_r
        sem = d_send.at[i]
        if c in ROUND:
            gives = (early & place.is_l) | (jnp.logical_not(early) & is_r)
            sem = xd_send.at[ROUND.index(c)]

        @pl.when(gives)
        def _(c=c, view=view, sem=sem):
            remote(view, view, sem, far_sem.at[c], place.sibling).start()
        count = I4 if i < I2 else I3
        turn(i, [(None, far[i])], I1, done[i], count)
        done[i] += count

    @pl.when(place.is_l)
    def _():
        for i in range(I4):
            remote(own[i], near[i], send_sem.at[i], near_sem.at[i], place.sibling).wait_send()

    @pl.when(is_r)
    def _():
        for i in range(I4):
            part = own[i] if i < I3 else own[i].at[I0:I2 * 768, :]
            remote(part, part, y_send.at[i], far_sem.at[I0], place.across_other).wait_send()
            remote(part, part, d_send.at[i], far_sem.at[I0], place.sibling).wait_send()
        for k in range(len(ROUND)):
            remote(round_a.at[k], round_a.at[k], x_send.at[k], far_sem.at[I0], place.sibling).wait_send()

    @pl.when((early & place.is_l) | (jnp.logical_not(early) & is_r))
    def _():
        for k in range(len(ROUND)):
            remote(round_a.at[k], round_a.at[k], xd_send.at[k], far_sem.at[I0], place.sibling).wait_send()

    @pl.when(jnp.logical_not(early))
    def _():
        for k in range(len(ROUND)):
            remote(round_a.at[k], round_a.at[k], rs_send.at[k], far_sem.at[I0], place.sibling).wait_send()


def near_choices(place, own, near):
    return [(place.is_l, own), (jnp.logical_not(place.is_l), near)]


def forward_kernel(dims, x_ref, y_ref, wq, wo, wu, wd, own_gains,
                   a_s, h_s, qkv_s, u_s, g_s, oh_same, oh_other, oa_same, oa_other, og_same, og_other, loss_s, home_gains,
                   nq, no, nu, nd, fq, fo, fu, fd, tq0, to0, tu0, td0, tq1, to1, tu1, td1, uc0, uc1, round_a, round_b,
                   abuf, hbuf, obuf, nbuf, ybuf, sbuf, qkvbuf, ubuf, zbuf, ctxbuf, acc, lossbuf, losstile, gains, wres, wores, wn,
                   send_sem, y_send, d_send, near_sem, far_sem, t_load, t_store, t_keep, ra_sem, rb_sem, x_send, xd_send, rs_send,
                   act_sem, hop_f, keep_sem, save_sem, stream_n, res_sem, out_sem, big_sem, y_sem, s_sem,
                   os_sem, oo_sem, as_sem, ao_sem, gs_sem, go_sem, bulk, gain_sem, tiny):
    micro, seq, width, heads, head_dim, ffn = dims
    place = Place()
    is_first, is_last = place.home == I0, place.home == I3
    home02 = (place.home == I0) | (place.home == I2)
    home13 = jnp.logical_not(home02)
    is_r = jnp.logical_not(place.is_l)
    takes_x = (place.home == I1) & is_r
    half = heads // I2 * HEAD_PAD
    scale = head_dim ** -0.5
    norm_factor = 1.0 / (micro * I2 * seq * width)
    own, near, far = (wq, wo, wu, wd), (nq, no, nu, nd), (fq, fo, fu, fd)
    turned = ((tq0, tq1), (to0, to1), (tu0, tu1), (td0, td1))
    entry_barrier(place)

    @pl.when(place.is_l)
    def _():
        pltpu.make_async_copy(own_gains, gains, gain_sem.at[I0]).start()
        remote(own_gains, gains, gain_sem.at[I1], gain_sem.at[I0], place.sibling).start()

    @pl.when(is_first)
    def _():
        for m in range(micro):
            pltpu.make_async_copy(x_ref.at[m, place.core], abuf.at[m], act_sem.at[m]).start()
    weight_phase(place, is_r, own, near, far, turned, (uc0, uc1), wn, wores, send_sem, y_send, d_send, near_sem, far_sem, t_load, t_store, t_keep,
                 round_a, round_b, ra_sem, rb_sem, x_send, xd_send, rs_send)
    pltpu.make_async_copy(own_gains, gains, gain_sem.at[I0]).wait()
    pltpu.make_async_copy(gains, home_gains, gain_sem.at[I0]).start()

    @pl.when(place.is_l)
    def _():
        remote(own_gains, gains, gain_sem.at[I1], gain_sem.at[I0], place.sibling).wait_send()

    def near_of(i):
        return near_choices(place, own[i], near[i])

    def saved(dst, index):
        return pltpu.make_async_copy(hbuf, dst, save_sem.at[index])

    sn = Stream(wn, stream_n, DEPTH, [([(None, tq0)], I3), ([(None, tq1)], I3), ([(None, uc0)], I3), ([(None, uc1)], I3)], micro * 12, False)
    for c, choices in enumerate((near_of(I1), [(None, fo)])):
        for condition, ref in choices:
            def go(ref=ref, c=c):
                load_heads(ref, I0, wores.at[c], out_sem.at[c])
            go() if condition is None else pl.when(condition)(go)
    sn.prime()
    load_resident(wres, res_sem, (near_of(I3), [(None, fd)]))
    lossbuf[...] = jnp.zeros_like(lossbuf)

    def qkv_out(m):
        return pltpu.make_async_copy(qkvbuf, qkv_s.at[m], big_sem.at[I0])

    def up_out(m):
        return pltpu.make_async_copy(ubuf, u_s.at[m], big_sem.at[I1])

    def act_out(m):
        return pltpu.make_async_copy(abuf.at[m], a_s.at[m], save_sem.at[I2])

    def hop_forward(m):
        return remote(obuf.at[m % I2], abuf.at[m], hop_f.at[m % I2], act_sem.at[m], place.chain(I1))

    def near_hand(src, dst_far, dst_own, sem, recv_sem):
        return (lambda: remote(src, dst_far, sem, recv_sem, place.sibling)), (lambda: pltpu.make_async_copy(src, dst_own, sem))

    def hand_out(m):
        return near_hand(obuf.at[m % I2], oa_other.at[m], oa_same.at[m], keep_sem.at[m % I2], ao_sem)

    def both_kinds(condition, copies, start):
        far_copy, own_copy = copies

        @pl.when(condition & place.is_l)
        def _():
            far_copy().start() if start else far_copy().wait_send()

        @pl.when(condition & is_r)
        def _():
            own_copy().start() if start else own_copy().wait()

    def x_out(m):
        return pltpu.make_async_copy(ybuf, oa_same.at[m], y_sem), pltpu.make_async_copy(sbuf, oa_other.at[m], s_sem)

    def seed_out(m):
        return pltpu.make_async_copy(sbuf, g_s.at[m], s_sem)

    def far_mid(m, condition):
        @pl.when(condition & place.is_l)
        def _():
            remote(h_s.at[m], oh_same.at[m], bulk.at[I2], os_sem, place.across).start()

        @pl.when(condition & is_r)
        def _():
            remote(h_s.at[m], oh_other.at[m], bulk.at[I2], oo_sem, place.across_other).start()

    def send_seed(m):
        seed_out(m).wait()

        @pl.when(place.is_l & (m < EARLY_SEEDS))
        def _():
            remote(g_s.at[m], og_same.at[m], bulk.at[I1], gs_sem, place.across).start()

        @pl.when(is_r & (m < EARLY_SEEDS))
        def _():
            remote(g_s.at[m], og_other.at[m], bulk.at[I1], go_sem, place.across_other).start()

    def forward_tick(m, carry):
        act, mid, out = abuf.at[m], hbuf, obuf.at[m % I2]
        pltpu.make_async_copy(x_ref.at[m, place.core], act, act_sem.at[m]).wait()
        act_out(m).start()

        @pl.when(place.is_l)
        def _():
            pltpu.make_async_copy(act, oa_same.at[m], as_sem).start()

        @pl.when(is_last)
        def _():
            pltpu.make_async_copy(y_ref.at[m, place.core], ybuf, y_sem).start()

        @pl.when(takes_x)
        def _():
            @pl.when(m > I0)
            def _():
                for copy in x_out(m):
                    copy.wait()
            for core, buf, sem in ((place.core, ybuf, y_sem), (I1 - place.core, sbuf, s_sem)):
                pltpu.make_async_copy(x_ref.at[m, core], buf, sem).start()
        norm_rows(act, gains[I0:I1, :], nbuf, seq)

        @pl.when(m > I0)
        def _():
            qkv_out(m).wait()

        def qkv_step(j, c):
            w = sn.wait(m * 12 + j)
            for n in range(I0, CHUNK, SUB):
                qkvbuf[:, lanes(j * CHUNK + n, SUB)] = mm(nbuf[...], w[:, n:n + SUB]).astype(BF)
            sn.start(m * 12 + j + DEPTH)
            return c
        lax.fori_loop(I0, I6, qkv_step, I0)
        qkv_out(m).start()
        act_out(m).wait()

        @pl.when(is_r)
        def _():
            remote(a_s.at[m], oa_other.at[m], bulk.at[I0], ao_sem, place.sibling).start()

        def head_step(i, c):
            base = i * (I3 * half)
            views = [[qkvbuf[:, lanes(base + t * half + r * HEAD_PAD, HEAD_PAD)] for t in range(I3)] for r in range(I8)]
            for r, context in enumerate(attention_forward(views, scale)):
                ctxbuf[:, lanes(i * half + r * HEAD_PAD, HEAD_PAD)] = context
            return c
        lax.fori_loop(I0, I2, head_step, I0)

        @pl.when(m == I0)
        def _():
            for c in range(I2):
                pltpu.make_async_copy(wo, wores.at[c, I0:768, :], out_sem.at[c]).wait()
        for n in range(I0, width, SUB):
            total = mm(ctxbuf[:, I0:half], wores[I0, :, n:n + SUB]) + mm(ctxbuf[:, half:I2 * half], wores[I1, :, n:n + SUB])
            mid[:, n:n + SUB] = (act[:, n:n + SUB].astype(F32) + total).astype(BF)
        saved(h_s.at[m], I0).start()

        @pl.when(place.is_l)
        def _():
            saved(oh_same.at[m], I1).start()
        norm_rows(mid, gains[I1:I2, :], nbuf, seq)

        @pl.when(m > I0)
        def _():
            up_out(m).wait()
        acc[...] = jnp.zeros_like(acc)

        def mlp_step(j, c):
            w = sn.wait(m * 12 + I6 + j)
            for n in range(I0, CHUNK, SUB):
                u = mm(nbuf[...], w[:, n:n + SUB]).astype(BF)
                ubuf[:, lanes(j * CHUNK + n, SUB)] = u
                uf = u.astype(F32)
                zbuf[:, n:n + SUB] = (uf * gelu_gate(uf)[I0]).astype(BF)
            sn.start(m * 12 + I6 + j + DEPTH)

            @pl.when(m == I0)
            def _():
                pltpu.make_async_copy(wd.at[I0:CHUNK, :], wres.at[j], res_sem.at[j]).wait()
            for n in range(I0, width, SUB):
                acc[:, n:n + SUB] += mm(zbuf[...], wres[j, :, n:n + SUB])
            return c
        lax.fori_loop(I0, I6, mlp_step, I0)
        up_out(m).start()

        @pl.when((m > I1) & jnp.logical_not(is_last))
        def _():
            hop_forward(m).wait_send()

        both_kinds((m > I1) & home02, hand_out(m), False)

        def finish(rows):
            out[rows, :] = (mid[rows, :].astype(F32) + acc[rows, :]).astype(BF)
        rows_loop(seq, 32, finish)

        @pl.when(jnp.logical_not(is_last))
        def _():
            hop_forward(m).start()

        both_kinds(home02, hand_out(m), True)

        @pl.when(is_last)
        def _():
            pltpu.make_async_copy(y_ref.at[m, place.core], ybuf, y_sem).wait()

            @pl.when(m > I0)
            def _():
                send_seed(m - I1)

            def seed(rows):
                error = out[rows, :].astype(F32) - ybuf[rows, :].astype(F32)
                sbuf[rows, :] = (error * norm_factor).astype(BF)
                lossbuf[...] += jnp.sum((error * error).reshape(I4, I8, width), axis=I0)
            rows_loop(seq, 32, seed)
            seed_out(m).start()

        @pl.when(takes_x)
        def _():
            for core, buf, sem in ((place.core, ybuf, y_sem), (I1 - place.core, sbuf, s_sem)):
                pltpu.make_async_copy(x_ref.at[m, core], buf, sem).wait()
            for copy in x_out(m):
                copy.start()

        saved(h_s.at[m], I0).wait()

        @pl.when(place.is_l)
        def _():
            saved(oh_same.at[m], I1).wait()

        @pl.when(is_r)
        def _():
            remote(h_s.at[m], oh_other.at[m], bulk.at[I3], oo_sem, place.sibling).start()

        far_mid(m, home13 | (m % I2 == I1))
        return carry

    @pl.when(is_first & (place.core == I0))
    def _():
        pl.delay(STAGGER_NS)
    lax.fori_loop(I0, micro, forward_tick, I0)
    for m in range(I0, micro, I2):
        far_mid(m, home02)

    @pl.when(is_last)
    def _():
        total = lossbuf[:, I0:128]
        for n in range(128, width, 128):
            total = total + lossbuf[:, n:n + 128]
        losstile[...] = total
        pltpu.make_async_copy(losstile, loss_s, tiny).start()
    for copy in (qkv_out(micro - I1), up_out(micro - I1)):
        copy.wait()

    @pl.when(jnp.logical_not(is_last))
    def _():
        for m in (micro - I2, micro - I1):
            hop_forward(m).wait_send()
    for m in (micro - I2, micro - I1):
        both_kinds(home02, hand_out(m), False)

    @pl.when(is_last)
    def _():
        seed_out(micro - I1).wait()
        pltpu.make_async_copy(losstile, loss_s, tiny).wait()

    @pl.when(takes_x)
    def _():
        for copy in x_out(micro - I1):
            copy.wait()
    pltpu.make_async_copy(gains, home_gains, gain_sem.at[I0]).wait()
    sent, got = drain(place)
    sent(h_s, bulk.at[I2])
    got(oh_other, oo_sem)

    @pl.when(is_last)
    def _():
        sent(g_s.at[I0:EARLY_SEEDS], bulk.at[I1])

    @pl.when((place.home == I2) & is_r)
    def _():
        got(og_same.at[I0:EARLY_SEEDS], gs_sem)
        got(og_other.at[I0:EARLY_SEEDS], go_sem)

    @pl.when(is_r)
    def _():
        sent(a_s, bulk.at[I0])
        sent(h_s, bulk.at[I3])
        got(oh_same, os_sem)

    @pl.when(place.is_l)
    def _():
        got(oa_same, as_sem)

    @pl.when(place.is_l | home02)
    def _():
        got(oa_other, ao_sem)


def drain(place):
    def sent(buf, sem):
        remote(buf, buf, sem, sem, place.sibling).wait_send()

    def got(dst, sem):
        pltpu.make_async_copy(dst, dst, sem).wait()
    return sent, got


def backward_kernel(dims, a_s, h_s, qkv_s, u_s, g_s, wq, nq, fq, td0, td1, to0, to1, tu0, tu1, gains, loss_s, after, *refs):
    (dx_s, m_s, od_same, od_other, og_same, og_other, oa_same, oa_other, dg_same, dg_other, loss_all,
     gbuf, hbuf, obuf, qkvbuf, ubuf, habuf, zbuf, ctxbuf, dqkvbuf, acc, accg, wres, wn, wk,
     grad_sem, hop_b, back_sem, dx_sem, dx_send, save_sem, stream_n, stream_k, res_sem, load_sem,
     ds_sem, do_sem, gs_sem, go_sem, as_sem, ao_sem, bulk, tiny, loss_sem) = refs[I4:]
    micro, seq, width, heads, head_dim, ffn = dims
    place = Place()
    is_first, is_last = place.home == I0, place.home == I3
    home13 = (place.home == I1) | is_last
    is_r = jnp.logical_not(place.is_l)
    half = heads // I2 * HEAD_PAD
    scale = head_dim ** -0.5

    barrier = pltpu.get_barrier_semaphore()
    along_x = (place.home == I1) | (place.home == I2)
    for there in (place.sibling, place.across, place.across_other):
        pl.semaphore_signal(barrier, inc=I1, device_id=there, device_id_type=MESH)

    @pl.when(along_x)
    def _():
        pl.semaphore_signal(barrier, inc=I1, device_id=place.at(place.tp, (place.stage + I2) % I4), device_id_type=MESH)

    @pl.when(is_last)
    def _():
        for m in range(micro):
            pltpu.make_async_copy(g_s.at[m], gbuf.at[m], grad_sem.at[m]).start()
    wk[...] = jnp.zeros_like(wk)
    bn = Stream(wn, stream_n, BACK_DEPTH, [([(None, td0)], I3), ([(None, td1)], I3), ([(None, to0)], I1), ([(None, to1)], I1)], micro * I8, False)
    bk = Stream(wk, stream_k, KDEPTH, [(near_choices(place, wq, nq), I3), ([(None, fq)], I3)], micro * I6, True)
    bn.prime()
    bk.prime()
    load_resident(wres, res_sem, ([(None, tu0)], [(None, tu1)]))

    def saved(dst, index):
        return pltpu.make_async_copy(hbuf, dst, save_sem)

    def both_kinds(condition, copies, start):
        far_copy, own_copy = copies

        @pl.when(condition & place.is_l)
        def _():
            far_copy().start() if start else far_copy().wait_send()

        @pl.when(condition & is_r)
        def _():
            own_copy().start() if start else own_copy().wait()

    def near_hand(src, dst_far, dst_own, sem, recv_sem):
        return (lambda: remote(src, dst_far, sem, recv_sem, place.sibling)), (lambda: pltpu.make_async_copy(src, dst_own, sem))

    def loads(i):
        m = micro - I1 - i
        return [pltpu.make_async_copy(src.at[m], dst, load_sem.at[k])
                for k, (src, dst) in enumerate(((u_s, ubuf), (qkv_s, qkvbuf), (h_s, habuf.at[I0]), (a_s, habuf.at[I1])))]

    def load_next(i, k):
        @pl.when(i + I1 < micro)
        def _():
            loads(i + I1)[k].start()

    for copy in loads(I0):
        copy.start()
    accg[...] = jnp.zeros_like(accg)

    def norm_back(index, x, base, dst, gain_row):
        def body(rows):
            xf = x[rows, :].astype(F32)
            dy = acc[rows, :].astype(BF).astype(F32)
            inv = lax.rsqrt(jnp.mean(xf * xf, axis=-I1, keepdims=True) + NORM_EPS)
            xn = xf * inv
            accg[index] += jnp.sum((dy * xn).reshape(I4, I8, width), axis=I0)
            dyg = dy * gain_row
            dx = inv * (dyg - xn * jnp.mean(dyg * xn, axis=-I1, keepdims=True))
            dst[rows, :] = (base[rows, :].astype(F32) + dx).astype(BF)
        rows_loop(seq, 32, body)

    def hop_back(i):
        m = micro - I1 - i
        return remote(obuf.at[i % I2], gbuf.at[m], hop_b.at[i % I2], grad_sem.at[m], place.chain(-I1))

    def hand_back(i):
        m = micro - I1 - i
        return near_hand(obuf.at[i % I2], og_other.at[m], og_same.at[m], back_sem.at[i % I2], go_sem)

    def keep_dx(i):
        return pltpu.make_async_copy(obuf.at[i % I2], dx_s.at[micro - I1 - i], back_sem.at[i % I2])

    def back_ready(i):
        both_kinds((i > I1) & home13, hand_back(i), False)

        @pl.when((i > I1) & is_first)
        def _():
            keep_dx(i).wait()
            dx_to_b(i).wait_send()

        @pl.when((i > I1) & jnp.logical_not(is_first))
        def _():
            hop_back(i).wait_send()

    def pass_loss(tile):
        @pl.when(jnp.logical_not(is_first))
        def _():
            remote(tile, loss_all.at[place.core], loss_sem.at[I0], loss_sem.at[I1], place.chain(-I1)).start()
        remote(tile, loss_all.at[place.core], loss_sem.at[I2], loss_sem.at[I3], place.sibling).start()

    def dx_to_b(i):
        return remote(obuf.at[i % I2], dx_s.at[micro - I1 - i], dx_send.at[i % I2], dx_sem, place.across)

    def backward_tick(i, carry):
        m = micro - I1 - i
        slot = i % I2
        grad, dmid, prev = gbuf.at[m], hbuf, obuf.at[slot]
        u_now, qkv_now, h_now, a_now = ubuf, qkvbuf, habuf.at[I0], habuf.at[I1]

        pltpu.make_async_copy(g_s.at[m], grad, grad_sem.at[m]).wait()

        @pl.when(place.is_l)
        def _():
            pltpu.make_async_copy(grad, og_same.at[m], gs_sem).start()
        load_u, load_qkv, load_h, load_a = loads(i)
        load_u.wait()
        acc[...] = jnp.zeros_like(acc)

        def mlp_step(j, c):
            w = bn.wait(i * I8 + j)
            for n in range(I0, CHUNK, SUB):
                dz = mm(grad[...], w[:, n:n + SUB]).astype(BF).astype(F32)
                u = u_now[:, lanes(j * CHUNK + n, SUB)].astype(F32)
                gate, u2 = gelu_gate(u)
                zbuf[:, n:n + SUB] = (dz * gelu_slope(u * gate, gate, u2)).astype(BF)
            bn.start(i * I8 + j + BACK_DEPTH)

            @pl.when(i == I0)
            def _():
                pltpu.make_async_copy(tu0.at[I0:CHUNK, :], wres.at[j], res_sem.at[j]).wait()
            for n in range(I0, width, SUB):
                acc[:, n:n + SUB] += mm(zbuf[...], wres[j, :, n:n + SUB])
            return c
        lax.fori_loop(I0, I6, mlp_step, I0)
        load_next(i, I0)
        load_h.wait()
        norm_back(I1, h_now, grad, dmid, gains[I1:I2, :])
        load_next(i, I2)

        @pl.when(place.is_l)
        def _():
            saved(od_same.at[m], I0).start()

        @pl.when(is_r)
        def _():
            saved(m_s.at[m], I0).start()
        for c in range(I2):
            w = bn.wait(i * I8 + I6 + c)
            for n in range(I0, CHUNK, SUB):
                ctxbuf[:, c * CHUNK + n:c * CHUNK + n + SUB] = mm(dmid[...], w[:, n:n + SUB]).astype(BF)
            bn.start(i * I8 + I6 + c + BACK_DEPTH)
        load_qkv.wait()

        def head_step(t, c):
            base = (t // I2) * (I3 * half) + (t % I2) * (I4 * HEAD_PAD)
            at = [[lanes(base + part * half + r * HEAD_PAD, HEAD_PAD) for part in range(I3)] for r in range(I4)]
            group = [(*(qkv_now[:, p] for p in at[r]), ctxbuf[:, lanes((t * I4 + r) * HEAD_PAD, HEAD_PAD)]) for r in range(I4)]
            for r, grads in enumerate(attention_backward(group, scale)):
                for p, value in zip(at[r], grads):
                    dqkvbuf[:, p] = value
            return c
        lax.fori_loop(I0, heads // I4, head_step, I0)
        load_next(i, I1)
        acc[...] = jnp.zeros_like(acc)

        def qkv_step(j, c):
            w = bk.wait(i * I6 + j)
            for n in range(I0, width, SUB):
                acc[:, n:n + SUB] += mm(dqkvbuf[:, lanes(j * CHUNK, CHUNK)], w[:, n:n + SUB])
            bk.start(i * I6 + j + KDEPTH)
            return c
        lax.fori_loop(I0, I6, qkv_step, I0)
        load_a.wait()
        back_ready(i)
        norm_back(I0, a_now, dmid, prev, gains[I0:I1, :])
        load_next(i, I3)

        @pl.when(i == I0)
        def _():
            pl.semaphore_wait(barrier, I3 + (place.home + I1) // I2 % I2)

            @pl.when(is_last)
            def _():
                pass_loss(loss_s)

            @pl.when((place.home == I2) & place.is_l)
            def _():
                for t in range(micro):
                    remote(a_s.at[t], oa_same.at[t], bulk.at[I8], as_sem, place.across).start()

            @pl.when((place.home == I2) & is_r)
            def _():
                for t in range(micro):
                    remote(a_s.at[t], oa_other.at[t], bulk.at[I8], ao_sem, place.across_other).start()

        @pl.when(jnp.logical_not(is_first))
        def _():
            hop_back(i).start()

        @pl.when(is_first)
        def _():
            keep_dx(i).start()
            dx_to_b(i).start()
        both_kinds(home13, hand_back(i), True)

        @pl.when(place.is_l)
        def _():
            saved(od_same.at[m], I0).wait()
            remote(od_same.at[m], od_same.at[m], bulk.at[I6], ds_sem, place.across).start()

        @pl.when(is_r)
        def _():
            remote(grad, og_other.at[m], bulk.at[5], go_sem, place.sibling).start()
            saved(m_s.at[m], I0).wait()
            remote(m_s.at[m], od_other.at[m], bulk.at[I6], do_sem, place.sibling).start()
            remote(m_s.at[m], od_other.at[m], bulk.at[7], do_sem, place.across_other).start()

        now = (i % I2 == I1) & (i < I2 * EARLY_G)
        far_grad(m, (place.home == I1) & now)
        far_grad(micro - I1 - i // I2, is_last & now)
        return carry

    def far_grad(m, condition):
        @pl.when(condition & place.is_l)
        def _():
            remote(gbuf.at[m], og_same.at[m], bulk.at[I4], gs_sem, place.across).start()

        @pl.when(condition & is_r)
        def _():
            remote(gbuf.at[m], og_other.at[m], bulk.at[I4], go_sem, place.across_other).start()

    lax.fori_loop(I0, micro, backward_tick, I0)
    loss_mine = loss_all.at[place.core]

    @pl.when(is_last)
    def _():
        own_loss = pltpu.make_async_copy(loss_s, loss_mine, loss_sem.at[I1])
        own_loss.start()
        own_loss.wait()

    @pl.when(jnp.logical_not(is_last))
    def _():
        remote(loss_mine, loss_mine, loss_sem.at[I0], loss_sem.at[I1], place.sibling).wait_recv()
        pass_loss(loss_mine)

    @pl.when(place.is_l)
    def _():
        pltpu.make_async_copy(accg, dg_same, tiny.at[I0]).start()
        remote(accg, dg_same, tiny.at[I1], tiny.at[I0], place.across).start()

    @pl.when(is_r)
    def _():
        remote(accg, dg_other, tiny.at[I1], tiny.at[I4], place.sibling).start()
        remote(accg, dg_other, tiny.at[I2], tiny.at[I4], place.across_other).start()

    for i in (micro - I2, micro - I1):
        back_ready(jnp.int32(i))

    sent, got = drain(place)
    sent(m_s, bulk.at[I6])

    @pl.when(is_r)
    def _():
        sent(gbuf, bulk.at[5])
        sent(m_s, bulk.at[7])
        remote(accg, dg_other, tiny.at[I2], tiny.at[I4], place.sibling).wait_send()

    @pl.when(home13)
    def _():
        sent(gbuf.at[I0:EARLY_G], bulk.at[I4])

    @pl.when(place.home == I1)
    def _():
        got(dx_s, dx_sem)

    @pl.when(jnp.logical_not(is_first))
    def _():
        remote(loss_mine, loss_mine, loss_sem.at[I0], loss_sem.at[I1], place.sibling).wait_send()
    remote(loss_mine, loss_mine, loss_sem.at[I2], loss_sem.at[I3], place.sibling).wait_send()
    remote(loss_mine, loss_mine, loss_sem.at[I2], loss_sem.at[I3], place.sibling).wait_recv()

    @pl.when(place.home == I2)
    def _():
        sent(a_s, bulk.at[I8])

    remote(accg, dg_other, tiny.at[I1], tiny.at[I4], place.sibling).wait_send()
    got(od_other, do_sem)

    @pl.when(place.is_l | home13)
    def _():
        got(og_other, go_sem)

    @pl.when(jnp.logical_not(home13) & is_r)
    def _():
        got(og_same.at[I0:EARLY_G], gs_sem)
        got(og_other.at[I0:EARLY_G], go_sem)
    got(dg_same, tiny.at[I0])
    got(dg_other, tiny.at[I4])

    @pl.when(is_r)
    def _():
        got(od_same, ds_sem)

    @pl.when(place.is_l)
    def _():
        got(og_same, gs_sem)

    @pl.when(is_last & is_r)
    def _():
        got(oa_same, as_sem)
        got(oa_other, ao_sem)


def shapes(*dims_list):
    return [jax.ShapeDtypeStruct(d, BF) for d in dims_list]


def forward_phase(dims, x, y, own, own_gains):
    micro, seq, width, heads, head_dim, ffn = dims
    half = heads // I2 * HEAD_PAD
    act = (micro, seq, width)
    raw = [w.shape for w in own]
    turned = [(I3, width, CHUNK), (I1, width, CHUNK), (ffn // I2, width), (I3, width, CHUNK)]
    out_shape = shapes(act, act, (micro, seq, I6 * half), (micro, seq, ffn), *[act] * 7)
    out_shape += [jax.ShapeDtypeStruct(s, F32) for s in ((I8, 128), own_gains.shape)]
    out_shape += shapes(*raw, *raw, *turned, *turned, turned[I0], turned[I0], *[(len(ROUND), 768, width)] * I2)
    any_spec = pl.BlockSpec(memory_space=ANY)
    vmem, dma = pltpu.VMEM, pltpu.SemaphoreType.DMA
    row = vmem((seq, width), BF)
    scratch = [
        vmem(act, BF), row, vmem((I2, seq, width), BF), row, row, row, vmem((seq, I6 * half), BF), vmem((seq, ffn), BF), vmem((seq, CHUNK), BF),
        vmem((seq, I2 * half), BF), vmem((seq, width), F32), vmem((I8, width), F32), vmem((I8, 128), F32), vmem((I2, width), F32),
        vmem((I6, CHUNK, width), BF), vmem((I2, CHUNK, width), BF), vmem((DEPTH, width, CHUNK), BF),
        dma((I4,)), dma((I4,)), dma((I4,)), dma((I4,)), dma((12,)), dma((I2,)), dma((I2,)), dma((I2,)), *[dma((len(ROUND),))] * 5,
        dma((micro,)), dma((I2,)), dma((I2,)), dma((I3,)), dma((DEPTH,)), dma((I6,)), dma((I2,)), dma((I2,)), dma(()), dma(()),
        dma(()), dma(()), dma(()), dma(()), dma(()), dma(()), dma((I4,)), dma((I2,)), dma(()),
    ]
    return pl.pallas_call(
        functools.partial(forward_kernel, dims),
        out_shape=tuple(out_shape),
        in_specs=[any_spec] * I6 + [pl.BlockSpec(memory_space=vmem)],
        out_specs=(any_spec,) * len(out_shape),
        scratch_shapes=scratch,
        compiler_params=pltpu.CompilerParams(collective_id=I0, has_side_effects=True, vmem_limit_bytes=VMEM_LIMIT),
        name='forward_phase',
    )(x, y, *own, own_gains)


def backward_phase(dims, saved, weights, gains, loss, after, placed):
    micro, seq, width, heads, head_dim, ffn = dims
    half = heads // I2 * HEAD_PAD
    act = (micro, seq, width)
    out_shape = shapes(*[act] * I8) + [jax.ShapeDtypeStruct((I2, I8, width), F32)] * I2 + [jax.ShapeDtypeStruct((I2, I8, 128), F32)]
    any_spec = pl.BlockSpec(memory_space=ANY)
    vmem, dma = pltpu.VMEM, pltpu.SemaphoreType.DMA
    scratch = [
        vmem(act, BF), vmem((seq, width), BF), vmem((I2, seq, width), BF), vmem((seq, I6 * half), BF), vmem((seq, ffn), BF),
        vmem((I2, seq, width), BF), vmem((seq, CHUNK), BF), vmem((seq, I2 * half), BF), vmem((seq, I6 * half), BF), vmem((seq, width), F32),
        vmem((I2, I8, width), F32), vmem((I6, CHUNK, width), BF), vmem((BACK_DEPTH, width, CHUNK), BF), vmem((KDEPTH, CHUNK, width), BF),
        dma((micro,)), dma((I2,)), dma((I2,)), dma(()), dma((I2,)), dma(()), dma((BACK_DEPTH,)), dma((KDEPTH,)), dma((I6,)), dma((I4,)),
        dma(()), dma(()), dma(()), dma(()), dma(()), dma(()), dma((9,)), dma((5,)), dma((I4,)),
    ]
    return pl.pallas_call(
        functools.partial(backward_kernel, dims),
        out_shape=tuple(out_shape),
        in_specs=[any_spec] * 14 + [pl.BlockSpec(memory_space=vmem)] * I2 + [any_spec] * 5,
        out_specs=(any_spec,) * len(out_shape),
        scratch_shapes=scratch,
        input_output_aliases={17: I4, 18: 5, 19: I6, 20: 7},
        compiler_params=pltpu.CompilerParams(collective_id=I1, has_side_effects=True, vmem_limit_bytes=VMEM_LIMIT),
        name='backward_phase',
    )(*saved, *weights, gains, loss, after, *placed)


def recompute_kernel(dims, early, h_same, h_other, a_same, a_other, gains, wq, wu, *refs):
    (done, u_o, qkv_o, ctx_o, n1_o, n2_o), (wqbuf, wubuf, count, sem) = refs[-10:-I4], refs[-I4:]
    micro, seq, width, heads, head_dim, ffn = dims
    place = Place()
    scale = head_dim ** -0.5
    half = heads // I2 * HEAD_PAD
    steps = I2 * micro * seq // BLOCK

    def body(hs, ho, rs, ro, u, qkv, ctx, n1, n2):
        step = count[I0]
        count[I0] = step + I1
        for low, high, gain, dst in ((hs, ho, gains[I1:I2, :], n2), (rs, ro, gains[I0:I1, :], n1)):
            @pl.when(step < steps // I2)
            def _(low=low, gain=gain, dst=dst):
                norm_rows(low, gain, dst, BLOCK)

            @pl.when(step >= steps // I2)
            def _(high=high, gain=gain, dst=dst):
                norm_rows(high, gain, dst, BLOCK)

        def qkv_step(j, c):
            rows = pl.ds(pl.multiple_of(j * SUB, SUB), SUB)
            qkv[:, lanes(j * SUB, SUB)] = mm_nt(n1[...], wqbuf[rows, :]).astype(BF)
            u[:, lanes(j * SUB, SUB)] = mm(n2[...], wubuf[:, lanes(j * SUB, SUB)]).astype(BF)
            return c
        lax.fori_loop(I0, I3 * half // SUB, qkv_step, I0)

        def head_step(j, c):
            at = [(pl.ds(s, seq), r * HEAD_PAD) for s in range(I0, BLOCK, seq) for r in range(I4)]
            base = j * (I4 * HEAD_PAD)
            views = [[qkv[rows, lanes(base + t * half + col, HEAD_PAD)] for t in range(I3)] for rows, col in at]
            for (rows, col), context in zip(at, attention_forward(views, scale)):
                ctx[rows, lanes(base + col, HEAD_PAD)] = context
            return c
        lax.fori_loop(I0, I2, head_step, I0)

    @pl.when(place.home < I2 if early else place.home > I1)
    def _():
        wqbuf[...] = jnp.zeros_like(wqbuf)
        for t in range(I3):
            load_heads(wq, t, wqbuf.at[pl.ds(t * CHUNK, CHUNK)], sem.at[I0])
        up = pltpu.make_async_copy(wu, wubuf, sem.at[I1])
        up.start()
        up.wait()
        pltpu.make_async_copy(wq, wqbuf.at[I0:wq.shape[I0]], sem.at[I0]).wait()
        count[I0] = I0
        low = pl.BlockSpec((BLOCK, width), lambda i: (jnp.minimum(i, steps // I2 - I1), I0))
        high = pl.BlockSpec((BLOCK, width), lambda i: (jnp.maximum(i - steps // I2, I0), I0))
        block = lambda n: pl.BlockSpec((BLOCK, n), lambda i: (i, I0))
        pltpu.emit_pipeline(body, grid=(steps,), in_specs=[low, high, low, high],
                            out_specs=[block(ffn // I2), block(I3 * half), block(half), block(width), block(width)])(
            h_same, h_other, a_same, a_other, u_o, qkv_o, ctx_o, n1_o, n2_o)


def owner_recompute(dims, early, again, h_rows, a_rows, gains, own):
    micro, seq, width, heads, head_dim, ffn = dims
    half = heads // I2 * HEAD_PAD
    tokens = I2 * micro * seq
    any_spec = pl.BlockSpec(memory_space=ANY)
    vmem = pltpu.VMEM
    earlier = () if early else tuple(again)
    return pl.pallas_call(
        functools.partial(recompute_kernel, dims, early),
        out_shape=(jax.ShapeDtypeStruct((I8, 128), F32), *shapes((tokens, ffn // I2), (tokens, I3 * half), (tokens, half), (tokens, width), (tokens, width))),
        in_specs=[any_spec] * I4 + [pl.BlockSpec(memory_space=vmem)] + [any_spec] * (I2 + len(earlier)),
        out_specs=(any_spec,) * I6,
        scratch_shapes=[vmem((I3 * half, width), BF), vmem((width, ffn // I2), BF), pltpu.SMEM((I1,), jnp.int32), pltpu.SemaphoreType.DMA((I2,))],
        input_output_aliases={7 + i: I1 + i for i in range(len(earlier))},
        compiler_params=pltpu.CompilerParams(has_side_effects=True, vmem_limit_bytes=VMEM_LIMIT),
        name='owner_recompute',
    )(*h_rows, *a_rows, gains, own[I0], own[I2], *earlier)


def spread_dx(step, last, dx, d_in, og_same, og_other, bounce, here_sem, parent_sem, sib_sem, send_sems, og_sems):
    place = Place()
    micro = dx.shape[I0]
    along_x = place.at(place.tp, (place.stage + I2) % I4)
    barrier = pltpu.get_barrier_semaphore()
    is_leaf = place.home > I1
    gives_g = (place.home == I1) & place.is_l
    takes_g = (place.home == I0) & jnp.logical_not(place.is_l)
    late = [micro - I1 - i for i in range(micro) if i % I2 == I0 or i > I2 * EARLY_G]

    def block(m):
        return d_in.at[m, place.core]

    def to_sibling(m, src):
        remote(src, block(m), send_sems.at[I0], sib_sem, place.sibling).start()

    def tell(there):
        pl.semaphore_signal(barrier, inc=I1, device_id=there, device_id_type=MESH)

    @pl.when(step == I0)
    def _():
        tell(place.sibling)

        @pl.when(is_leaf)
        def _():
            tell(along_x)

        @pl.when(takes_g)
        def _():
            tell(place.across)

    @pl.when((step == I1) & jnp.logical_not(is_leaf))
    def _():
        pl.semaphore_wait(barrier, I2 + gives_g.astype(jnp.int32))

        @pl.when(gives_g)
        def _():
            for t, og in enumerate((og_same, og_other)):
                for m in late:
                    remote(og.at[m], og.at[m], og_sems.at[t], og_sems.at[I2 + t], place.across).start()
        for m in reversed(range(micro)):
            remote(dx.at[m], block(m), send_sems.at[I1], parent_sem.at[m], along_x).start()
            to_sibling(m, dx.at[m])
        pltpu.make_async_copy(dx, bounce, here_sem).start()

    @pl.when((step == I2) & jnp.logical_not(is_leaf))
    def _():
        pltpu.make_async_copy(dx, bounce, here_sem).wait()
        for m in range(micro):
            pltpu.make_async_copy(bounce.at[m], block(m), here_sem).start()

    @pl.when((step == (last + I1) // I2) & takes_g)
    def _():
        for t, og in enumerate((og_same, og_other)):
            part = og.at[I0:len(late)]
            remote(part, part, og_sems.at[t], og_sems.at[I2 + t], place.across).wait_recv()

    @pl.when((step == last) & is_leaf)
    def _():
        pl.semaphore_wait(barrier, I1)
        for m in reversed(range(micro)):
            remote(block(m), block(m), send_sems.at[I0], parent_sem.at[m], place.sibling).wait_recv()
            to_sibling(m, block(m))

    @pl.when(step == last)
    def _():
        remote(dx, dx, send_sems.at[I0], sib_sem, place.sibling).wait_send()

        @pl.when(jnp.logical_not(is_leaf))
        def _():
            remote(dx, dx, send_sems.at[I1], sib_sem, place.sibling).wait_send()
            pltpu.make_async_copy(dx, dx, here_sem).wait()

        @pl.when(gives_g)
        def _():
            for t, og in enumerate((og_same, og_other)):
                part = og.at[I0:len(late)]
                remote(part, part, og_sems.at[t], og_sems.at[I2 + t], place.across).wait_send()
        remote(dx, dx, send_sems.at[I0], sib_sem, place.sibling).wait_recv()


def owner_backward_kernel(dims, dx, ds, do, u, qkv, wo, wd, gs_in, go_in, dqkv, dup, z, d_in, og_same, og_other,
                          dmid, gbuf, dctx, wobuf, bounce, sem, g_sem, here_sem, parent_sem, sib_sem, send_sems, og_sems):
    micro, seq, width, heads, head_dim, ffn = dims
    half = heads // I2 * HEAD_PAD
    scale = head_dim ** -0.5
    step, steps = pl.program_id(I0), pl.num_programs(I0)
    blocks = steps // I2
    spread_dx(step, steps - I1, dx, d_in, og_same, og_other, bounce, here_sem, parent_sem, sib_sem, send_sems, og_sems)

    @pl.when(step == I0)
    def _():
        wobuf[...] = jnp.zeros_like(wobuf)
        load_heads(wo, I0, wobuf, sem)
        pltpu.make_async_copy(wo, wobuf.at[I0:wo.shape[I0]], sem).wait()

    def g_load(n, start):
        rows = BLOCK // seq
        for og, low in ((og_same, I0), (og_other, blocks // I2)):
            @pl.when((n >= low) & (n < low + blocks // I2))
            def _(og=og, low=low):
                copy = pltpu.make_async_copy(og.at[pl.ds((n - low) * rows, rows)], gbuf.at[n % I2], g_sem.at[n % I2])
                copy.start() if start else copy.wait()

    @pl.when(step < blocks)
    def _():
        @pl.when(step < blocks // I2)
        def _():
            dmid[...] = ds[...]

        @pl.when(step >= blocks // I2)
        def _():
            dmid[...] = do[...]

        def ctx_step(j, c):
            rows = pl.ds(pl.multiple_of(j * SUB, SUB), SUB)
            dctx[:, lanes(j * SUB, SUB)] = mm_nt(dmid[...], wobuf[rows, :]).astype(BF)
            return c
        lax.fori_loop(I0, half // SUB, ctx_step, I0)

        def head_step(j, c):
            base = j * (I2 * HEAD_PAD)
            at = [(pl.ds(s, seq), base + r * HEAD_PAD) for s in range(I0, BLOCK, seq) for r in range(I2)]
            group = [(*(qkv[rows, lanes(t * half + col, HEAD_PAD)] for t in range(I3)), dctx[rows, lanes(col, HEAD_PAD)]) for rows, col in at]
            for (rows, col), grads in zip(at, attention_backward(group, scale)):
                for t, value in enumerate(grads):
                    dqkv[rows, lanes(t * half + col, HEAD_PAD)] = value
            return c
        lax.fori_loop(I0, heads // I4, head_step, I0)

    @pl.when(step == blocks)
    def _():
        g_load(step - blocks, True)

    @pl.when(step >= blocks)
    def _():
        n = step - blocks
        g_load(n + I1, True)
        g_load(n, False)
        grad = gbuf.at[n % I2]

        def mlp_step(j, c):
            rows = pl.ds(pl.multiple_of(j * SUB, SUB), SUB)
            cols = lanes(j * SUB, SUB)
            dz = mm_nt(grad[...].reshape(BLOCK, width), wd[rows, :]).astype(BF).astype(F32)
            up = u[:, cols].astype(F32)
            gate, up2 = gelu_gate(up)
            hidden = up * gate
            z[:, cols] = hidden.astype(BF)
            dup[:, cols] = (dz * gelu_slope(hidden, gate, up2)).astype(BF)
            return c
        lax.fori_loop(I0, ffn // I2 // SUB, mlp_step, I0)


def owner_backward(dims, dx, d_rows, og, ups, qkv, own):
    micro, seq, width, heads, head_dim, ffn = dims
    half = heads // I2 * HEAD_PAD
    tokens = I2 * micro * seq
    blocks = tokens // BLOCK
    vmem, dma = pltpu.VMEM, pltpu.SemaphoreType.DMA
    any_spec = pl.BlockSpec(memory_space=ANY)
    first = lambda i: jnp.minimum(i, blocks - I1)
    second = lambda i: jnp.maximum(i - blocks, I0)
    low = pl.BlockSpec((BLOCK, width), lambda i: (jnp.minimum(i, blocks // I2 - I1), I0))
    high = pl.BlockSpec((BLOCK, width), lambda i: (jnp.maximum(first(i) - blocks // I2, I0), I0))
    attn_block = pl.BlockSpec((BLOCK, I3 * half), lambda i: (first(i), I0))
    mlp_block = pl.BlockSpec((BLOCK, ffn // I2), lambda i: (second(i), I0))
    act = (micro, seq, width)
    return pl.pallas_call(
        functools.partial(owner_backward_kernel, dims),
        grid=(I2 * blocks,),
        out_shape=tuple(shapes((tokens, I3 * half), (tokens, ffn // I2), (tokens, ffn // I2), (micro, I2, seq, width), act, act)),
        in_specs=[any_spec, low, high, mlp_block, attn_block, any_spec, pl.BlockSpec((ffn // I2, width), lambda i: (I0, I0)), any_spec, any_spec],
        out_specs=(attn_block, mlp_block, mlp_block, any_spec, any_spec, any_spec),
        scratch_shapes=[vmem((BLOCK, width), BF), vmem((I2, BLOCK // seq, seq, width), BF), vmem((BLOCK, half), BF), vmem((half, width), BF), vmem(act, BF),
                        dma(()), dma((I2,)), dma(()), dma((micro,)), dma(()), dma((I2,)), dma((I4,))],
        input_output_aliases={7: I4, I8: 5},
        compiler_params=pltpu.CompilerParams(collective_id=I2, has_side_effects=True, vmem_limit_bytes=VMEM_LIMIT),
        name='owner_backward',
    )(dx, *d_rows, ups, qkv, own[I1], own[I3], *og)


def bring(pairs, sem):
    copies = [pltpu.make_async_copy(src, dst, sem.at[i]) for i, (src, dst) in enumerate(pairs)]
    for copy in copies:
        copy.start()
    for copy in copies:
        copy.wait()


def attn_products_kernel(dq, dk, dv, ctx, n1_o, ds, do, dx_in, dwq, dwo, dx_out, n1, dmid, dqkvt, ctxt, bounce, sem, dx_sem):
    tokens, width = n1.shape
    part = tokens // I2
    head_dim = dwo.shape[I1]
    step, last = pl.program_id(I0), pl.num_programs(I0) - I1
    into, out_of = pltpu.make_async_copy(dx_in, bounce, dx_sem), pltpu.make_async_copy(bounce, dx_out, dx_sem)

    @pl.when(step == I1)
    def _():
        into.start()

    @pl.when(step == I2)
    def _():
        into.wait()
        out_of.start()

    @pl.when(step == last)
    def _():
        out_of.wait()

    @pl.when(step == I0)
    def _():
        bring([(n1_o, n1), (ds, dmid.at[pl.ds(I0, part)]), (do, dmid.at[pl.ds(part, part)])], sem)

    def turn(rows):
        for t, block in enumerate((dq, dk, dv)):
            for r in range(I2):
                at = (I2 * t + r) * head_dim
                dqkvt[at:at + head_dim, rows] = block[rows, r * HEAD_PAD:(r + I1) * HEAD_PAD].T[I0:head_dim]
        for r in range(I2):
            ctxt[r * head_dim:(r + I1) * head_dim, rows] = ctx[rows, r * HEAD_PAD:(r + I1) * HEAD_PAD].T[I0:head_dim]
    rows_loop(tokens, SUB, turn)
    for c in range(I0, width, SUB):
        cut = slice(c, c + SUB)
        dwq[:, :, :, cut] = mm(dqkvt[...], n1[:, cut]).reshape(I3, I2, head_dim, SUB)
        dwo[:, :, cut] = mm(ctxt[...], dmid[:, cut]).reshape(I2, head_dim, SUB)


def attn_products(dqkv, ctx, n1, d_rows, dx, out_dims):
    heads, head_dim, width = out_dims
    tokens = n1.shape[I0]
    vmem = pltpu.VMEM
    any_spec = pl.BlockSpec(memory_space=ANY)
    pairs = heads // I2
    cols = lambda t: pl.BlockSpec((tokens, I2 * HEAD_PAD), lambda i: (I0, t * pairs + i))
    return pl.pallas_call(
        attn_products_kernel,
        grid=(pairs,),
        out_shape=(jax.ShapeDtypeStruct((I3,) + out_dims, F32), jax.ShapeDtypeStruct(out_dims, F32), jax.ShapeDtypeStruct(dx.shape, BF)),
        in_specs=[cols(I0), cols(I1), cols(I2), cols(I0), any_spec, any_spec, any_spec, any_spec],
        out_specs=(pl.BlockSpec((I3, I2, head_dim, width), lambda i: (I0, i, I0, I0)), pl.BlockSpec((I2, head_dim, width), lambda i: (i, I0, I0)), any_spec),
        scratch_shapes=[vmem((tokens, width), BF), vmem((tokens, width), BF), vmem((I6 * head_dim, tokens), BF), vmem((I2 * head_dim, tokens), BF),
                        vmem(dx.shape, BF), pltpu.SemaphoreType.DMA((I3,)), pltpu.SemaphoreType.DMA(())],
        compiler_params=pltpu.CompilerParams(vmem_limit_bytes=VMEM_LIMIT),
        name='attn_products',
    )(dqkv, dqkv, dqkv, ctx, n1, *d_rows, dx)


def mlp_products_kernel(dup, z, n2_o, gs, go, dwu, dwd, n2t, grad, zt, stage, sem):
    width, tokens = n2t.shape
    part = tokens // I2

    @pl.when(pl.program_id(I0) == I0)
    def _():
        bring([(n2_o, stage), (gs, grad.at[pl.ds(I0, part)]), (go, grad.at[pl.ds(part, part)])], sem)

        def turn(rows):
            for c in range(I0, width, SUB):
                n2t[c:c + SUB, rows] = stage[rows, c:c + SUB].T
        rows_loop(tokens, SUB, turn)

    def turn_z(rows):
        for c in range(I0, z.shape[I1], SUB):
            zt[c:c + SUB, rows] = z[rows, c:c + SUB].T
    rows_loop(tokens, SUB, turn_z)
    for c in range(I0, width, I2 * SUB):
        dwu[c:c + I2 * SUB, :] = mm(n2t[c:c + I2 * SUB, :], dup[...])
    for c in range(I0, width, SUB):
        dwd[:, c:c + SUB] = mm(zt[...], grad[:, c:c + SUB])


def mlp_products(dup, hidden, n2, g_rows):
    tokens, width = n2.shape
    cols = dup.shape[I1]
    vmem = pltpu.VMEM
    any_spec = pl.BlockSpec(memory_space=ANY)
    block = pl.BlockSpec((tokens, SUB), lambda i: (I0, i))
    return pl.pallas_call(
        mlp_products_kernel,
        grid=(cols // SUB,),
        out_shape=(jax.ShapeDtypeStruct((width, cols), F32), jax.ShapeDtypeStruct((cols, width), F32)),
        in_specs=[block, block, any_spec, any_spec, any_spec],
        out_specs=(pl.BlockSpec((width, SUB), lambda i: (I0, i)), pl.BlockSpec((SUB, width), lambda i: (i, I0))),
        scratch_shapes=[vmem((width, tokens), BF), vmem((tokens, width), BF), vmem((SUB, tokens), BF), vmem((tokens, width), BF), pltpu.SemaphoreType.DMA((I3,))],
        compiler_params=pltpu.CompilerParams(vmem_limit_bytes=VMEM_LIMIT),
        name='mlp_products',
    )(dup, hidden, n2, *g_rows)


def solution(mesh):
    act_spec = P('rep', None, None, None)
    weight_specs = (
        P(('rep', 'stage'), None, None, 'tp', None),
        P(('rep', 'stage'), 'tp', None, None),
        P(('rep', 'stage'), None, 'tp'),
        P(('rep', 'stage'), 'tp', None),
        P(('rep', 'stage'), None),
        P(('rep', 'stage'), None),
    )

    def device_fn(inputs, targets, w_qkv, w_out, w_up, w_down, gain_attn, gain_mlp):
        micro_count, _, seq_len, width = inputs.shape
        dims = (micro_count, seq_len, width, I2 * w_out.shape[I1], w_out.shape[I2], I2 * w_up.shape[I2])
        norm_factor = 1.0 / (inputs.size)
        own = (w_qkv[I0], w_out[I0], w_up[I0], w_down[I0])
        own_gains = jnp.concatenate([gain_attn, gain_mlp]).astype(F32)
        rows_of = (own[I0].transpose(I1, I2, I3, I0).reshape(-I1, width), own[I1].reshape(-I1, width), own[I2], own[I3])

        (acts, mids, qkv, ups, seeds, oh_same, oh_other, oa_same, oa_other, og_same, og_other, loss_tile, home_gains, *weights) = forward_phase(dims, inputs, targets, rows_of, own_gains)
        (nq, no, nu, nd), (fq, fo, fu, fd) = weights[I0:I4], weights[I4:I8]
        (tq0, to0, tu0, td0), (tq1, to1, tu1, td1) = weights[I8:12], weights[12:16]

        flat = lambda *rows: [r.reshape(-I1, width) for r in rows]
        h_rows = flat(oh_same, oh_other)
        done, *again = owner_recompute(dims, True, None, h_rows, flat(oa_same, oa_other), own_gains, rows_of)
        dx, _, od_same, od_other, og_same, og_other, oa_same, oa_other, dg_same, dg_other, loss_all = backward_phase(
            dims, (acts, mids, qkv, ups, seeds), (rows_of[I0], nq, fq, td0, td1, to0, to1, tu0, tu1), home_gains, loss_tile, done, (og_same, og_other, oa_same, oa_other))
        _, *again = owner_recompute(dims, False, again, h_rows, flat(oa_same, oa_other), own_gains, rows_of)
        ups_own, qkv_own, ctx_own, n1, n2 = again
        d_rows = flat(od_same, od_other)
        d_qkv_rows, d_up_rows, hidden, dx_all, og_same, og_other = owner_backward(dims, dx, d_rows, (og_same, og_other), ups_own, qkv_own, rows_of)
        d_qkv, d_out, d_inputs = attn_products(d_qkv_rows, ctx_own, n1, d_rows, dx_all, w_out.shape[I1:])
        d_up, d_down = mlp_products(d_up_rows, hidden, n2, flat(og_same, og_other))
        weight_grads = (d_qkv.transpose(I3, I0, I1, I2), d_out, d_up, d_down)
        mine = jnp.sum(dg_same + dg_other, I1)
        loss = jnp.sum(loss_all) * (0.5 * norm_factor)

        return (loss.reshape(I1), d_inputs) + tuple(g[None] for g in weight_grads) + (mine[I0][None], mine[I1][None])

    return jax.shard_map(device_fn, mesh=mesh, in_specs=(act_spec, act_spec) + weight_specs, out_specs=(P('rep'), act_spec) + weight_specs, check_vma=False)
```

```python
import functools

import jax
import jax.numpy as jnp
from jax import lax
from jax.experimental import pallas as pl
from jax.experimental.pallas import tpu as pltpu
from jax.sharding import PartitionSpec as P

NORM_EPS = 1e-5
BF = jnp.bfloat16
F32 = jnp.float32
MESH = pl.DeviceIdType.MESH
ANY = pl.ANY


GELU_A = 0.7978845608028654
GELU_B = 0.044715
I0, I1, I2, I3, I4, I6, I8 = 0, 1, 2, 3, 4, 6, 8
CHUNK = 1024
BLOCK = 384
SUB = 256
DEPTH = 6
BACK_DEPTH = 6
KDEPTH = 3
EARLY_G = 3
STAGGER_NS = 6000
EARLY_SEEDS = 5
HEAD_PAD = 128
VMEM_LIMIT = 67043328


def mm(a, b):
    return lax.dot_general(a, b, (((I1,), (I0,)), ((), ())), preferred_element_type=F32)


def mm_nt(a, b):
    return lax.dot_general(a, b, (((I1,), (I1,)), ((), ())), preferred_element_type=F32)


def mm_tn(a, b):
    return lax.dot_general(a, b, (((I0,), (I0,)), ((), ())), preferred_element_type=F32)


class Place:
    def __init__(self):
        self.tp = lax.axis_index('tp')
        self.stage = lax.axis_index('stage')
        self.core = self.stage % I2
        self.x_pos = self.stage // I2
        self.home = self.x_pos * (I3 - I2 * self.tp) + self.tp
        self.is_l = self.stage == self.home
        self.sib = self.stage + I1 - I2 * self.core

    def at(self, tp, stage):
        return {'tp': tp, 'stage': stage}

    @property
    def sibling(self):
        return self.at(self.tp, self.sib)

    @property
    def along_x(self):
        return self.at(self.tp, (self.stage + I2) % I4)

    @property
    def across(self):
        return self.at(I1 - self.tp, self.stage)

    @property
    def across_other(self):
        return self.at(I1 - self.tp, self.sib)

    def chain(self, delta):
        there = self.home + delta
        x_pos = there // I2
        tp = there % I2 + x_pos * (I1 - I2 * (there % I2))
        return self.at(tp, I2 * x_pos + self.core)


def entry_barrier(place):
    barrier = pltpu.get_barrier_semaphore()
    for d_tp in (I0, I1):
        for d_stage in range(I4):
            if d_tp or d_stage:
                tp = place.tp + d_tp - I2 * d_tp * place.tp
                stage = (place.stage + d_stage) % I4
                pl.semaphore_signal(barrier, inc=I1, device_id=place.at(tp, stage), device_id_type=MESH)
    pl.semaphore_wait(barrier, 7)


def remote(src, dst, send_sem, recv_sem, device_id):
    return pltpu.make_async_remote_copy(src_ref=src, dst_ref=dst, send_sem=send_sem, recv_sem=recv_sem, device_id=device_id, device_id_type=MESH)


def rows_loop(total, step, body):
    def run(i, carry):
        body(pl.ds(pl.multiple_of(i * step, step), step))
        return carry
    lax.fori_loop(I0, total // step, run, I0)


def norm_rows(src, gain_row, dst, total):
    def body(rows):
        v = src[rows, :].astype(F32)
        inv = lax.rsqrt(jnp.mean(v * v, axis=-I1, keepdims=True) + NORM_EPS)
        dst[rows, :] = (v * inv * gain_row).astype(BF)
    rows_loop(total, 32, body)


def gelu_gate(u):
    u2 = u * u
    t = jnp.tanh(u * (GELU_A + (GELU_A * GELU_B) * u2))
    return 0.5 * t + 0.5, u2


def gelu_slope(hidden, gate, u2):
    return gate + hidden * (1.0 - gate) * (2.0 * GELU_A + (6.0 * GELU_A * GELU_B) * u2)


def row_parts(heads, cut=128):
    return [(*(x[low:high] for x in queries), *(x[:high] for x in keys), low)
            for queries, keys in heads for low, high in ((I0, cut), (cut, queries[I0].shape[I0]))]


def softmax_parts(scores, starts, keys_axis):
    masked = []
    for s, start in zip(scores, starts):
        k_pos = lax.broadcasted_iota(jnp.int32, s.shape, keys_axis)
        q_pos = lax.broadcasted_iota(jnp.int32, s.shape, I1 - keys_axis) + start
        masked.append(jnp.where(k_pos <= q_pos, s, -1e30))
    tops = [jnp.max(s, axis=keys_axis, keepdims=True) for s in masked]
    powers = [jnp.exp(s - top) for s, top in zip(masked, tops)]
    scales = [1.0 / jnp.sum(e, axis=keys_axis, keepdims=True) for e in powers]
    return [e * r for e, r in zip(powers, scales)]


def join_keys(top, low, cut=128):
    return jnp.concatenate([top + low[:cut], low[cut:]], I0).astype(BF)


def attention_forward(heads, scale):
    units = row_parts([((q,), (k, v)) for q, k, v in heads])
    probs = softmax_parts([mm_nt(q, k) * scale for q, k, _, _ in units], [u[-I1] for u in units], I1)
    parts = [mm(p.astype(BF), u[I2]) for p, u in zip(probs, units)]
    return [jnp.concatenate([a, b], I0).astype(BF) for a, b in zip(parts[I0::I2], parts[I1::I2])]


def attention_backward(heads, scale):
    units = row_parts([((q, dc), (k, v)) for q, k, v, dc in heads])
    scores = [mm_nt(k, q) * scale for q, _, k, _, _ in units]
    dps = [mm_nt(v, dc) for _, dc, _, v, _ in units]
    probs = softmax_parts(scores, [u[-I1] for u in units], I0)
    dps = [dp.astype(BF).astype(F32) for dp in dps]
    deltas = [jnp.sum(dp * p, axis=I0, keepdims=True) for dp, p in zip(dps, probs)]
    dss = [p * (dp - delta) * scale for p, dp, delta in zip(probs, dps, deltas)]
    terms = []
    for ds in dss:
        hi = ds.astype(BF)
        rest = ds - hi.astype(F32)
        lo = rest.astype(BF)
        terms.append((hi, lo, (rest - lo.astype(F32)).astype(BF)))
    dvs = [mm(p.astype(BF), u[I1]) for p, u in zip(probs, units)]
    dks = [mm(hi, u[I0]) + (mm(lo, u[I0]) + mm(tail, u[I0])) for (hi, lo, tail), u in zip(terms, units)]
    k_turned = [u[I2].T for u in units]
    dqs = [(mm(kt, hi) + (mm(kt, lo) + mm(kt, tail))).astype(BF) for (hi, lo, tail), kt in zip(terms, k_turned)]
    return [(jnp.concatenate([dqs[i].T, dqs[i + I1].T], I0), join_keys(dks[i], dks[i + I1]), join_keys(dvs[i], dvs[i + I1]))
            for i in range(I0, len(units), I2)]


def lanes(offset, size):
    return pl.ds(pl.multiple_of(offset, 128), size)


def load_resident(buf, sem, halves):
    for c in range(I6):
        for condition, ref in halves[c // I3]:
            copy = pltpu.make_async_copy(ref.at[(c % I3) * CHUNK:(c % I3 + I1) * CHUNK, :], buf.at[c], sem.at[c])
            if condition is None:
                copy.start()
            else:
                pl.when(condition)(copy.start)


def load_heads(ref, index, dst, sem):
    for r in range(I8):
        rows = pl.ds(pl.multiple_of(index * 768 + r * 96, 96), 96)
        pltpu.make_async_copy(ref.at[rows, :], dst.at[r * 128:r * 128 + 96, :], sem).start()


class Stream:
    def __init__(self, buf, sem, depth, parts, total, by_heads):
        self.buf, self.sem, self.depth, self.parts, self.total, self.by_heads = buf, sem, depth, parts, total, by_heads
        self.per_tick = sum(p[I1] for p in parts)

    def copy_in(self, ref, index, slot):
        if not self.by_heads:
            pltpu.make_async_copy(ref.at[index], self.buf.at[slot], self.sem.at[slot]).start()
            return
        load_heads(ref, index, self.buf.at[slot], self.sem.at[slot])

    def start(self, seq):
        @pl.when(seq < self.total)
        def _():
            j = seq % self.per_tick
            slot = seq % self.depth
            base = I0
            for choices, chunks in self.parts:
                for condition, ref in choices:
                    here = (j >= base) & (j < base + chunks)
                    here = here if condition is None else here & condition

                    @pl.when(here)
                    def _(ref=ref, low=base):
                        self.copy_in(ref, j - low, slot)
                base += chunks

    def prime(self):
        for seq in range(self.depth):
            self.start(jnp.int32(seq))

    def wait(self, seq):
        slot = seq % self.depth
        ref = self.parts[I0][I0][I0][I1]
        if self.by_heads:
            pltpu.make_async_copy(ref.at[I0:768, :], self.buf.at[slot, I0:768, :], self.sem.at[slot]).wait()
        else:
            pltpu.make_async_copy(ref.at[I0], self.buf.at[slot], self.sem.at[slot]).wait()
        return self.buf.at[slot]


PIECES = [(0, 0, 0), (0, 0, 1), (0, 0, 2), (1, 0, 0), (2, 1, 0), (2, 1, 1), (2, 1, 2), (2, 1, 3), (3, 0, 0), (3, 0, 1), (3, 0, 2), (3, 0, 3)]


ROUND = (10, 11)
ROUND_STEPS = (6, 8)


def piece(ref, axis, index):
    return ref.at[index * 768:(index + I1) * 768, :] if axis == I0 else ref.at[:, index * 768:(index + I1) * 768]


def weight_phase(place, is_r, own, near, far, turned, up_chunks, wn, wk, send_sem, y_send, d_send, near_sem, far_sem, load_sem, store_sem, chunk_sem,
                 round_a, round_b, ra_sem, rb_sem, x_send, xd_send, rs_send):
    wk[...] = jnp.zeros_like(wk)
    early = place.home < I2

    def piece_of(arrays, c):
        i, axis, index = PIECES[c]
        return piece(arrays[i], axis, index)

    @pl.when(place.is_l)
    def _():
        for i in range(I4):
            remote(own[i], near[i], send_sem.at[i], near_sem.at[i], place.sibling).start()

    @pl.when(is_r)
    def _():
        for k, c in enumerate(ROUND):
            @pl.when(early)
            def _(k=k, c=c):
                remote(piece_of(own, c), round_a.at[k], x_send.at[k], ra_sem.at[k], place.along_x).start()
        for c, (i, axis, index) in enumerate(PIECES):
            if c not in ROUND:
                remote(piece_of(own, c), piece_of(far, c), y_send.at[i], far_sem.at[c], place.across_other).start()
        for k, c in enumerate(ROUND):
            @pl.when(jnp.logical_not(early))
            def _(k=k, c=c):
                remote(piece_of(own, c), piece_of(far, c), x_send.at[k], far_sem.at[c], place.across_other).start()

    def load(i, refs, t, slot):
        for condition, ref in refs:
            def go(ref=ref):
                if i < I2:
                    for r in range(I2):
                        rows = pl.ds(pl.multiple_of(t * 192 + r * 96, 96), 96)
                        pltpu.make_async_copy(ref.at[rows, :], wk.at[I0, pl.ds(slot * SUB + r * 128, 96), :], load_sem.at[slot]).start()
                elif i == I2:
                    pltpu.make_async_copy(ref.at[:, lanes(t * SUB, SUB)], wn.at[slot, :, I0:SUB], load_sem.at[slot]).start()
                else:
                    rows = pl.ds(pl.multiple_of(t * SUB, SUB), SUB)
                    pltpu.make_async_copy(ref.at[rows, :], wk.at[I0, pl.ds(512 + slot * SUB, SUB), :], load_sem.at[slot]).start()
            if condition is None:
                go()
            else:
                pl.when(condition)(go)

    def loaded(i, refs, slot):
        ref = refs[I0][I1]
        if i < I2:
            pltpu.make_async_copy(ref.at[I0:192, :], wk.at[I0, I0:192, :], load_sem.at[slot]).wait()
        elif i == I2:
            pltpu.make_async_copy(ref.at[:, I0:SUB], wn.at[slot, :, I0:SUB], load_sem.at[slot]).wait()
        else:
            pltpu.make_async_copy(ref.at[I0:SUB, :], wk.at[I0, 512:768, :], load_sem.at[slot]).wait()

    def store(i, dst, t, slot):
        if i == I2:
            rows = pl.ds(pl.multiple_of(t * SUB, SUB), SUB)
            return pltpu.make_async_copy(wk.at[I1, pl.ds(slot * SUB, SUB), :], dst.at[rows, :], store_sem.at[slot])
        return pltpu.make_async_copy(wn.at[slot, :, SUB:512], dst.at[t // I4, :, lanes(t % I4 * SUB, SUB)], store_sem.at[slot])

    def keep(which, t, slot):
        return pltpu.make_async_copy(wn.at[slot, :, I0:SUB], up_chunks[which].at[t // I4, :, lanes(t % I4 * SUB, SUB)], chunk_sem.at[slot])

    def turn(i, refs, which, first, count):
        dst = turned[i][which]
        load(i, refs, first, I0)

        def step(n, c):
            slot = n % I2

            if i == I2:
                @pl.when(n > I0)
                def _():
                    keep(which, first + n - I1, I1 - slot).wait()

            @pl.when(n + I1 < count)
            def _():
                load(i, refs, first + n + I1, I1 - slot)
            loaded(i, refs, slot)
            if i == I2:
                keep(which, first + n, slot).start()

            @pl.when(n >= I2)
            def _():
                store(i, dst, first + n - I2, slot).wait()
            for b in range(I6):
                cut = slice(b * SUB, b * SUB + SUB)
                if i == I2:
                    wk[I1, pl.ds(pl.multiple_of(slot * SUB, SUB), SUB), cut] = wn[slot, cut, I0:SUB].T
                else:
                    base = I0 if i < I2 else 512
                    wn[slot, cut, SUB:512] = wk[I0, pl.ds(pl.multiple_of(base + slot * SUB, SUB), SUB), cut].T
            store(i, dst, first + n, slot).start()
            return c
        lax.fori_loop(I0, count, step, I0)
        for n in (count - I2, count - I1):
            store(i, dst, first + n, n % I2).wait()
        if i == I2:
            keep(which, first + count - I1, (count - I1) % I2).wait()

    counts = (12, I4, 12, 12)
    for i in range(I4):
        @pl.when(is_r)
        def _(i=i):
            remote(near[i], near[i], send_sem.at[i], near_sem.at[i], place.sibling).wait_recv()
        turn(i, [(place.is_l, own[i]), (is_r, near[i])], I0, I0, counts[i])
    done = [I0, I0, I0, I0]

    @pl.when(place.is_l & jnp.logical_not(early))
    def _():
        for k in range(len(ROUND)):
            remote(round_a.at[k], round_a.at[k], rs_send.at[k], ra_sem.at[k], place.sibling).wait_recv()
            remote(round_a.at[k], round_b.at[k], rs_send.at[k], rb_sem.at[k], place.across).start()
    for c, (i, axis, index) in enumerate(PIECES):
        view = piece_of(far, c)
        for k, step in enumerate(ROUND_STEPS):
            if c == step:
                @pl.when(is_r & jnp.logical_not(early))
                def _(k=k):
                    remote(round_b.at[k], round_b.at[k], rs_send.at[k], rb_sem.at[k], place.sibling).wait_recv()
                    remote(round_b.at[k], piece_of(far, ROUND[k]), rs_send.at[k], far_sem.at[ROUND[k]], place.along_x).start()
        remote(view, view, d_send.at[i], far_sem.at[c], place.sibling).wait_recv()
        gives = is_r
        sem = d_send.at[i]
        if c in ROUND:
            gives = (early & place.is_l) | (jnp.logical_not(early) & is_r)
            sem = xd_send.at[ROUND.index(c)]

        @pl.when(gives)
        def _(c=c, view=view, sem=sem):
            remote(view, view, sem, far_sem.at[c], place.sibling).start()
        count = I4 if i < I2 else I3
        turn(i, [(None, far[i])], I1, done[i], count)
        done[i] += count

    @pl.when(place.is_l)
    def _():
        for i in range(I4):
            remote(own[i], near[i], send_sem.at[i], near_sem.at[i], place.sibling).wait_send()

    @pl.when(is_r)
    def _():
        for i in range(I4):
            part = own[i] if i < I3 else own[i].at[I0:I2 * 768, :]
            remote(part, part, y_send.at[i], far_sem.at[I0], place.across_other).wait_send()
            remote(part, part, d_send.at[i], far_sem.at[I0], place.sibling).wait_send()
        for k in range(len(ROUND)):
            remote(round_a.at[k], round_a.at[k], x_send.at[k], far_sem.at[I0], place.sibling).wait_send()

    @pl.when((early & place.is_l) | (jnp.logical_not(early) & is_r))
    def _():
        for k in range(len(ROUND)):
            remote(round_a.at[k], round_a.at[k], xd_send.at[k], far_sem.at[I0], place.sibling).wait_send()

    @pl.when(jnp.logical_not(early))
    def _():
        for k in range(len(ROUND)):
            remote(round_a.at[k], round_a.at[k], rs_send.at[k], far_sem.at[I0], place.sibling).wait_send()


def near_choices(place, own, near):
    return [(place.is_l, own), (jnp.logical_not(place.is_l), near)]


def forward_kernel(dims, x_ref, y_ref, wq, wo, wu, wd, own_gains,
                   a_s, h_s, qkv_s, u_s, g_s, oh_same, oh_other, oa_same, oa_other, og_same, og_other, loss_s, home_gains,
                   nq, no, nu, nd, fq, fo, fu, fd, tq0, to0, tu0, td0, tq1, to1, tu1, td1, uc0, uc1, round_a, round_b,
                   abuf, hbuf, obuf, nbuf, ybuf, sbuf, qkvbuf, ubuf, zbuf, ctxbuf, acc, lossbuf, losstile, gains, wres, wores, wn,
                   send_sem, y_send, d_send, near_sem, far_sem, t_load, t_store, t_keep, ra_sem, rb_sem, x_send, xd_send, rs_send,
                   act_sem, hop_f, keep_sem, save_sem, stream_n, res_sem, out_sem, big_sem, y_sem, s_sem,
                   os_sem, oo_sem, as_sem, ao_sem, gs_sem, go_sem, bulk, gain_sem, tiny):
    micro, seq, width, heads, head_dim, ffn = dims
    place = Place()
    is_first, is_last = place.home == I0, place.home == I3
    home02 = (place.home == I0) | (place.home == I2)
    home13 = jnp.logical_not(home02)
    is_r = jnp.logical_not(place.is_l)
    takes_x = (place.home == I1) & is_r
    half = heads // I2 * HEAD_PAD
    scale = head_dim ** -0.5
    norm_factor = 1.0 / (micro * I2 * seq * width)
    own, near, far = (wq, wo, wu, wd), (nq, no, nu, nd), (fq, fo, fu, fd)
    turned = ((tq0, tq1), (to0, to1), (tu0, tu1), (td0, td1))
    entry_barrier(place)

    @pl.when(place.is_l)
    def _():
        pltpu.make_async_copy(own_gains, gains, gain_sem.at[I0]).start()
        remote(own_gains, gains, gain_sem.at[I1], gain_sem.at[I0], place.sibling).start()

    @pl.when(is_first)
    def _():
        for m in range(micro):
            pltpu.make_async_copy(x_ref.at[m, place.core], abuf.at[m], act_sem.at[m]).start()
    weight_phase(place, is_r, own, near, far, turned, (uc0, uc1), wn, wores, send_sem, y_send, d_send, near_sem, far_sem, t_load, t_store, t_keep,
                 round_a, round_b, ra_sem, rb_sem, x_send, xd_send, rs_send)
    pltpu.make_async_copy(own_gains, gains, gain_sem.at[I0]).wait()
    pltpu.make_async_copy(gains, home_gains, gain_sem.at[I0]).start()

    @pl.when(place.is_l)
    def _():
        remote(own_gains, gains, gain_sem.at[I1], gain_sem.at[I0], place.sibling).wait_send()

    def near_of(i):
        return near_choices(place, own[i], near[i])

    def saved(dst, index):
        return pltpu.make_async_copy(hbuf, dst, save_sem.at[index])

    sn = Stream(wn, stream_n, DEPTH, [([(None, tq0)], I3), ([(None, tq1)], I3), ([(None, uc0)], I3), ([(None, uc1)], I3)], micro * 12, False)
    for c, choices in enumerate((near_of(I1), [(None, fo)])):
        for condition, ref in choices:
            def go(ref=ref, c=c):
                load_heads(ref, I0, wores.at[c], out_sem.at[c])
            go() if condition is None else pl.when(condition)(go)
    sn.prime()
    load_resident(wres, res_sem, (near_of(I3), [(None, fd)]))
    lossbuf[...] = jnp.zeros_like(lossbuf)

    def qkv_out(m):
        return pltpu.make_async_copy(qkvbuf, qkv_s.at[m], big_sem.at[I0])

    def up_out(m):
        return pltpu.make_async_copy(ubuf, u_s.at[m], big_sem.at[I1])

    def act_out(m):
        return pltpu.make_async_copy(abuf.at[m], a_s.at[m], save_sem.at[I2])

    def hop_forward(m):
        return remote(obuf.at[m % I2], abuf.at[m], hop_f.at[m % I2], act_sem.at[m], place.chain(I1))

    def near_hand(src, dst_far, dst_own, sem, recv_sem):
        return (lambda: remote(src, dst_far, sem, recv_sem, place.sibling)), (lambda: pltpu.make_async_copy(src, dst_own, sem))

    def hand_out(m):
        return near_hand(obuf.at[m % I2], oa_other.at[m], oa_same.at[m], keep_sem.at[m % I2], ao_sem)

    def both_kinds(condition, copies, start):
        far_copy, own_copy = copies

        @pl.when(condition & place.is_l)
        def _():
            far_copy().start() if start else far_copy().wait_send()

        @pl.when(condition & is_r)
        def _():
            own_copy().start() if start else own_copy().wait()

    def x_out(m):
        return pltpu.make_async_copy(ybuf, oa_same.at[m], y_sem), pltpu.make_async_copy(sbuf, oa_other.at[m], s_sem)

    def seed_out(m):
        return pltpu.make_async_copy(sbuf, g_s.at[m], s_sem)

    def far_mid(m, condition):
        @pl.when(condition & place.is_l)
        def _():
            remote(h_s.at[m], oh_same.at[m], bulk.at[I2], os_sem, place.across).start()

        @pl.when(condition & is_r)
        def _():
            remote(h_s.at[m], oh_other.at[m], bulk.at[I2], oo_sem, place.across_other).start()

    def send_seed(m):
        seed_out(m).wait()

        @pl.when(place.is_l & (m < EARLY_SEEDS))
        def _():
            remote(g_s.at[m], og_same.at[m], bulk.at[I1], gs_sem, place.across).start()

        @pl.when(is_r & (m < EARLY_SEEDS))
        def _():
            remote(g_s.at[m], og_other.at[m], bulk.at[I1], go_sem, place.across_other).start()

    def forward_tick(m, carry):
        act, mid, out = abuf.at[m], hbuf, obuf.at[m % I2]
        pltpu.make_async_copy(x_ref.at[m, place.core], act, act_sem.at[m]).wait()
        act_out(m).start()

        @pl.when(place.is_l)
        def _():
            pltpu.make_async_copy(act, oa_same.at[m], as_sem).start()

        @pl.when(is_last)
        def _():
            pltpu.make_async_copy(y_ref.at[m, place.core], ybuf, y_sem).start()

        @pl.when(takes_x)
        def _():
            @pl.when(m > I0)
            def _():
                for copy in x_out(m):
                    copy.wait()
            for core, buf, sem in ((place.core, ybuf, y_sem), (I1 - place.core, sbuf, s_sem)):
                pltpu.make_async_copy(x_ref.at[m, core], buf, sem).start()
        norm_rows(act, gains[I0:I1, :], nbuf, seq)

        @pl.when(m > I0)
        def _():
            qkv_out(m).wait()

        def qkv_step(j, c):
            w = sn.wait(m * 12 + j)
            for n in range(I0, CHUNK, SUB):
                qkvbuf[:, lanes(j * CHUNK + n, SUB)] = mm(nbuf[...], w[:, n:n + SUB]).astype(BF)
            sn.start(m * 12 + j + DEPTH)
            return c
        lax.fori_loop(I0, I6, qkv_step, I0)
        qkv_out(m).start()
        act_out(m).wait()

        @pl.when(is_r)
        def _():
            remote(a_s.at[m], oa_other.at[m], bulk.at[I0], ao_sem, place.sibling).start()

        def head_step(i, c):
            base = i * (I3 * half)
            views = [[qkvbuf[:, lanes(base + t * half + r * HEAD_PAD, HEAD_PAD)] for t in range(I3)] for r in range(I8)]
            for r, context in enumerate(attention_forward(views, scale)):
                ctxbuf[:, lanes(i * half + r * HEAD_PAD, HEAD_PAD)] = context
            return c
        lax.fori_loop(I0, I2, head_step, I0)

        @pl.when(m == I0)
        def _():
            for c in range(I2):
                pltpu.make_async_copy(wo, wores.at[c, I0:768, :], out_sem.at[c]).wait()
        for n in range(I0, width, SUB):
            total = mm(ctxbuf[:, I0:half], wores[I0, :, n:n + SUB]) + mm(ctxbuf[:, half:I2 * half], wores[I1, :, n:n + SUB])
            mid[:, n:n + SUB] = (act[:, n:n + SUB].astype(F32) + total).astype(BF)
        saved(h_s.at[m], I0).start()

        @pl.when(place.is_l)
        def _():
            saved(oh_same.at[m], I1).start()
        norm_rows(mid, gains[I1:I2, :], nbuf, seq)

        @pl.when(m > I0)
        def _():
            up_out(m).wait()
        acc[...] = jnp.zeros_like(acc)

        def mlp_step(j, c):
            w = sn.wait(m * 12 + I6 + j)
            for n in range(I0, CHUNK, SUB):
                u = mm(nbuf[...], w[:, n:n + SUB]).astype(BF)
                ubuf[:, lanes(j * CHUNK + n, SUB)] = u
                uf = u.astype(F32)
                zbuf[:, n:n + SUB] = (uf * gelu_gate(uf)[I0]).astype(BF)
            sn.start(m * 12 + I6 + j + DEPTH)

            @pl.when(m == I0)
            def _():
                pltpu.make_async_copy(wd.at[I0:CHUNK, :], wres.at[j], res_sem.at[j]).wait()
            for n in range(I0, width, SUB):
                acc[:, n:n + SUB] += mm(zbuf[...], wres[j, :, n:n + SUB])
            return c
        lax.fori_loop(I0, I6, mlp_step, I0)
        up_out(m).start()

        @pl.when((m > I1) & jnp.logical_not(is_last))
        def _():
            hop_forward(m).wait_send()

        both_kinds((m > I1) & home02, hand_out(m), False)

        def finish(rows):
            out[rows, :] = (mid[rows, :].astype(F32) + acc[rows, :]).astype(BF)
        rows_loop(seq, 32, finish)

        @pl.when(jnp.logical_not(is_last))
        def _():
            hop_forward(m).start()

        both_kinds(home02, hand_out(m), True)

        @pl.when(is_last)
        def _():
            pltpu.make_async_copy(y_ref.at[m, place.core], ybuf, y_sem).wait()

            @pl.when(m > I0)
            def _():
                send_seed(m - I1)

            def seed(rows):
                error = out[rows, :].astype(F32) - ybuf[rows, :].astype(F32)
                sbuf[rows, :] = (error * norm_factor).astype(BF)
                lossbuf[...] += jnp.sum((error * error).reshape(I4, I8, width), axis=I0)
            rows_loop(seq, 32, seed)
            seed_out(m).start()

        @pl.when(takes_x)
        def _():
            for core, buf, sem in ((place.core, ybuf, y_sem), (I1 - place.core, sbuf, s_sem)):
                pltpu.make_async_copy(x_ref.at[m, core], buf, sem).wait()
            for copy in x_out(m):
                copy.start()

        saved(h_s.at[m], I0).wait()

        @pl.when(place.is_l)
        def _():
            saved(oh_same.at[m], I1).wait()

        @pl.when(is_r)
        def _():
            remote(h_s.at[m], oh_other.at[m], bulk.at[I3], oo_sem, place.sibling).start()

        far_mid(m, home13 | (m % I2 == I1))
        return carry

    @pl.when(is_first & (place.core == I0))
    def _():
        pl.delay(STAGGER_NS)
    lax.fori_loop(I0, micro, forward_tick, I0)
    for m in range(I0, micro, I2):
        far_mid(m, is_first)

    @pl.when(is_last)
    def _():
        total = lossbuf[:, I0:128]
        for n in range(128, width, 128):
            total = total + lossbuf[:, n:n + 128]
        losstile[...] = total
        pltpu.make_async_copy(losstile, loss_s, tiny).start()
    for copy in (qkv_out(micro - I1), up_out(micro - I1)):
        copy.wait()

    @pl.when(jnp.logical_not(is_last))
    def _():
        for m in (micro - I2, micro - I1):
            hop_forward(m).wait_send()
    for m in (micro - I2, micro - I1):
        both_kinds(home02, hand_out(m), False)

    @pl.when(is_last)
    def _():
        seed_out(micro - I1).wait()
        pltpu.make_async_copy(losstile, loss_s, tiny).wait()

    @pl.when(takes_x)
    def _():
        for copy in x_out(micro - I1):
            copy.wait()
    pltpu.make_async_copy(gains, home_gains, gain_sem.at[I0]).wait()
    sent, got = drain(place)

    @pl.when(place.home != I2)
    def _():
        sent(h_s, bulk.at[I2])

    @pl.when(place.home == I2)
    def _():
        sent(h_s.at[I0:micro // I2], bulk.at[I2])

    @pl.when(place.is_l | jnp.logical_not(is_last))
    def _():
        got(oh_other, oo_sem)

    @pl.when(is_r & is_last)
    def _():
        got(oh_other.at[I0:micro // I2], oo_sem)

    @pl.when(is_last)
    def _():
        sent(g_s.at[I0:EARLY_SEEDS], bulk.at[I1])

    @pl.when((place.home == I2) & is_r)
    def _():
        got(og_same.at[I0:EARLY_SEEDS], gs_sem)
        got(og_other.at[I0:EARLY_SEEDS], go_sem)

    @pl.when(is_r)
    def _():
        sent(a_s, bulk.at[I0])
        sent(h_s, bulk.at[I3])

    @pl.when(is_r & jnp.logical_not(is_last))
    def _():
        got(oh_same, os_sem)

    @pl.when(is_r & is_last)
    def _():
        got(oh_same.at[I0:micro // I2], os_sem)

    @pl.when(place.is_l)
    def _():
        got(oa_same, as_sem)

    @pl.when(place.is_l | home02)
    def _():
        got(oa_other, ao_sem)


def drain(place):
    def sent(buf, sem):
        remote(buf, buf, sem, sem, place.sibling).wait_send()

    def got(dst, sem):
        pltpu.make_async_copy(dst, dst, sem).wait()
    return sent, got


def backward_kernel(dims, a_s, h_s, qkv_s, u_s, g_s, wq, nq, fq, td0, td1, to0, to1, tu0, tu1, gains, loss_s, after, *refs):
    (dx_s, m_s, od_same, od_other, og_same, og_other, oa_same, oa_other, oh_same, oh_other, dg_same, dg_other, loss_all,
     gbuf, hbuf, obuf, qkvbuf, ubuf, habuf, zbuf, ctxbuf, dqkvbuf, acc, accg, wres, wn, wk,
     grad_sem, hop_b, back_sem, dx_sem, dx_send, save_sem, stream_n, stream_k, res_sem, load_sem,
     ds_sem, do_sem, gs_sem, go_sem, as_sem, ao_sem, os_sem, oo_sem, bulk, tiny, loss_sem) = refs[I6:]
    micro, seq, width, heads, head_dim, ffn = dims
    place = Place()
    is_first, is_last = place.home == I0, place.home == I3
    home13 = (place.home == I1) | is_last
    is_r = jnp.logical_not(place.is_l)
    half = heads // I2 * HEAD_PAD
    scale = head_dim ** -0.5

    barrier = pltpu.get_barrier_semaphore()
    along_x = (place.home == I1) | (place.home == I2)
    for there in (place.sibling, place.across, place.across_other):
        pl.semaphore_signal(barrier, inc=I1, device_id=there, device_id_type=MESH)

    @pl.when(along_x)
    def _():
        pl.semaphore_signal(barrier, inc=I1, device_id=place.at(place.tp, (place.stage + I2) % I4), device_id_type=MESH)

    @pl.when(is_last)
    def _():
        for m in range(micro):
            pltpu.make_async_copy(g_s.at[m], gbuf.at[m], grad_sem.at[m]).start()
    wk[...] = jnp.zeros_like(wk)
    bn = Stream(wn, stream_n, BACK_DEPTH, [([(None, td0)], I3), ([(None, td1)], I3), ([(None, to0)], I1), ([(None, to1)], I1)], micro * I8, False)
    bk = Stream(wk, stream_k, KDEPTH, [(near_choices(place, wq, nq), I3), ([(None, fq)], I3)], micro * I6, True)
    bn.prime()
    bk.prime()
    load_resident(wres, res_sem, ([(None, tu0)], [(None, tu1)]))

    def saved(dst, index):
        return pltpu.make_async_copy(hbuf, dst, save_sem)

    def both_kinds(condition, copies, start):
        far_copy, own_copy = copies

        @pl.when(condition & place.is_l)
        def _():
            far_copy().start() if start else far_copy().wait_send()

        @pl.when(condition & is_r)
        def _():
            own_copy().start() if start else own_copy().wait()

    def near_hand(src, dst_far, dst_own, sem, recv_sem):
        return (lambda: remote(src, dst_far, sem, recv_sem, place.sibling)), (lambda: pltpu.make_async_copy(src, dst_own, sem))

    def loads(i):
        m = micro - I1 - i
        return [pltpu.make_async_copy(src.at[m], dst, load_sem.at[k])
                for k, (src, dst) in enumerate(((u_s, ubuf), (qkv_s, qkvbuf), (h_s, habuf.at[I0]), (a_s, habuf.at[I1])))]

    def load_next(i, k):
        @pl.when(i + I1 < micro)
        def _():
            loads(i + I1)[k].start()

    for copy in loads(I0):
        copy.start()
    accg[...] = jnp.zeros_like(accg)

    def norm_back(index, x, base, dst, gain_row):
        def body(rows):
            xf = x[rows, :].astype(F32)
            dy = acc[rows, :].astype(BF).astype(F32)
            inv = lax.rsqrt(jnp.mean(xf * xf, axis=-I1, keepdims=True) + NORM_EPS)
            xn = xf * inv
            accg[index] += jnp.sum((dy * xn).reshape(I4, I8, width), axis=I0)
            dyg = dy * gain_row
            dx = inv * (dyg - xn * jnp.mean(dyg * xn, axis=-I1, keepdims=True))
            dst[rows, :] = (base[rows, :].astype(F32) + dx).astype(BF)
        rows_loop(seq, 32, body)

    def hop_back(i):
        m = micro - I1 - i
        return remote(obuf.at[i % I2], gbuf.at[m], hop_b.at[i % I2], grad_sem.at[m], place.chain(-I1))

    def hand_back(i):
        m = micro - I1 - i
        return near_hand(obuf.at[i % I2], og_other.at[m], og_same.at[m], back_sem.at[i % I2], go_sem)

    def keep_dx(i):
        return pltpu.make_async_copy(obuf.at[i % I2], dx_s.at[micro - I1 - i], back_sem.at[i % I2])

    def back_ready(i):
        both_kinds((i > I1) & home13, hand_back(i), False)

        @pl.when((i > I1) & is_first)
        def _():
            keep_dx(i).wait()
            dx_to_b(i).wait_send()

        @pl.when((i > I1) & jnp.logical_not(is_first))
        def _():
            hop_back(i).wait_send()

    def pass_loss(tile):
        @pl.when(jnp.logical_not(is_first))
        def _():
            remote(tile, loss_all.at[place.core], loss_sem.at[I0], loss_sem.at[I1], place.chain(-I1)).start()
        remote(tile, loss_all.at[place.core], loss_sem.at[I2], loss_sem.at[I3], place.sibling).start()

    def dx_to_b(i):
        return remote(obuf.at[i % I2], dx_s.at[micro - I1 - i], dx_send.at[i % I2], dx_sem, place.across)

    def backward_tick(i, carry):
        m = micro - I1 - i
        slot = i % I2
        grad, dmid, prev = gbuf.at[m], hbuf, obuf.at[slot]
        u_now, qkv_now, h_now, a_now = ubuf, qkvbuf, habuf.at[I0], habuf.at[I1]

        pltpu.make_async_copy(g_s.at[m], grad, grad_sem.at[m]).wait()

        @pl.when(place.is_l)
        def _():
            pltpu.make_async_copy(grad, og_same.at[m], gs_sem).start()
        load_u, load_qkv, load_h, load_a = loads(i)
        load_u.wait()
        acc[...] = jnp.zeros_like(acc)

        def mlp_step(j, c):
            w = bn.wait(i * I8 + j)
            for n in range(I0, CHUNK, SUB):
                dz = mm(grad[...], w[:, n:n + SUB]).astype(BF).astype(F32)
                u = u_now[:, lanes(j * CHUNK + n, SUB)].astype(F32)
                gate, u2 = gelu_gate(u)
                zbuf[:, n:n + SUB] = (dz * gelu_slope(u * gate, gate, u2)).astype(BF)
            bn.start(i * I8 + j + BACK_DEPTH)

            @pl.when(i == I0)
            def _():
                pltpu.make_async_copy(tu0.at[I0:CHUNK, :], wres.at[j], res_sem.at[j]).wait()
            for n in range(I0, width, SUB):
                acc[:, n:n + SUB] += mm(zbuf[...], wres[j, :, n:n + SUB])
            return c
        lax.fori_loop(I0, I6, mlp_step, I0)
        load_next(i, I0)
        load_h.wait()
        norm_back(I1, h_now, grad, dmid, gains[I1:I2, :])
        load_next(i, I2)

        @pl.when(place.is_l)
        def _():
            saved(od_same.at[m], I0).start()

        @pl.when(is_r)
        def _():
            saved(m_s.at[m], I0).start()
        for c in range(I2):
            w = bn.wait(i * I8 + I6 + c)
            for n in range(I0, CHUNK, SUB):
                ctxbuf[:, c * CHUNK + n:c * CHUNK + n + SUB] = mm(dmid[...], w[:, n:n + SUB]).astype(BF)
            bn.start(i * I8 + I6 + c + BACK_DEPTH)
        load_qkv.wait()

        def head_step(t, c):
            base = (t // I2) * (I3 * half) + (t % I2) * (I4 * HEAD_PAD)
            at = [[lanes(base + part * half + r * HEAD_PAD, HEAD_PAD) for part in range(I3)] for r in range(I4)]
            group = [(*(qkv_now[:, p] for p in at[r]), ctxbuf[:, lanes((t * I4 + r) * HEAD_PAD, HEAD_PAD)]) for r in range(I4)]
            for r, grads in enumerate(attention_backward(group, scale)):
                for p, value in zip(at[r], grads):
                    dqkvbuf[:, p] = value
            return c
        lax.fori_loop(I0, heads // I4, head_step, I0)
        load_next(i, I1)
        acc[...] = jnp.zeros_like(acc)

        def qkv_step(j, c):
            w = bk.wait(i * I6 + j)
            for n in range(I0, width, SUB):
                acc[:, n:n + SUB] += mm(dqkvbuf[:, lanes(j * CHUNK, CHUNK)], w[:, n:n + SUB])
            bk.start(i * I6 + j + KDEPTH)
            return c
        lax.fori_loop(I0, I6, qkv_step, I0)
        load_a.wait()
        back_ready(i)
        norm_back(I0, a_now, dmid, prev, gains[I0:I1, :])
        load_next(i, I3)

        @pl.when(i == I0)
        def _():
            pl.semaphore_wait(barrier, I3 + (place.home + I1) // I2 % I2)

            @pl.when(is_last)
            def _():
                pass_loss(loss_s)

            @pl.when((place.home == I2) & place.is_l)
            def _():
                for t in range(micro):
                    remote(a_s.at[t], oa_same.at[t], bulk.at[I8], as_sem, place.across).start()
                for t in range(I0, micro, I2):
                    remote(h_s.at[t], oh_same.at[t], bulk.at[9], os_sem, place.across).start()

            @pl.when((place.home == I2) & is_r)
            def _():
                for t in range(micro):
                    remote(a_s.at[t], oa_other.at[t], bulk.at[I8], ao_sem, place.across_other).start()
                for t in range(I0, micro, I2):
                    remote(h_s.at[t], oh_other.at[t], bulk.at[9], oo_sem, place.across_other).start()

        @pl.when(jnp.logical_not(is_first))
        def _():
            hop_back(i).start()

        @pl.when(is_first)
        def _():
            keep_dx(i).start()
            dx_to_b(i).start()
        both_kinds(home13, hand_back(i), True)

        @pl.when(place.is_l)
        def _():
            saved(od_same.at[m], I0).wait()
            remote(od_same.at[m], od_same.at[m], bulk.at[I6], ds_sem, place.across).start()

        @pl.when(is_r)
        def _():
            remote(grad, og_other.at[m], bulk.at[5], go_sem, place.sibling).start()
            saved(m_s.at[m], I0).wait()
            remote(m_s.at[m], od_other.at[m], bulk.at[I6], do_sem, place.sibling).start()
            remote(m_s.at[m], od_other.at[m], bulk.at[7], do_sem, place.across_other).start()

        now = (i % I2 == I1) & (i < I2 * EARLY_G)
        far_grad(m, (place.home == I1) & now)
        far_grad(micro - I1 - i // I2, is_last & now)
        return carry

    def far_grad(m, condition):
        @pl.when(condition & place.is_l)
        def _():
            remote(gbuf.at[m], og_same.at[m], bulk.at[I4], gs_sem, place.across).start()

        @pl.when(condition & is_r)
        def _():
            remote(gbuf.at[m], og_other.at[m], bulk.at[I4], go_sem, place.across_other).start()

    lax.fori_loop(I0, micro, backward_tick, I0)
    loss_mine = loss_all.at[place.core]

    @pl.when(is_last)
    def _():
        own_loss = pltpu.make_async_copy(loss_s, loss_mine, loss_sem.at[I1])
        own_loss.start()
        own_loss.wait()

    @pl.when(jnp.logical_not(is_last))
    def _():
        remote(loss_mine, loss_mine, loss_sem.at[I0], loss_sem.at[I1], place.sibling).wait_recv()
        pass_loss(loss_mine)

    @pl.when(place.is_l)
    def _():
        pltpu.make_async_copy(accg, dg_same, tiny.at[I0]).start()
        remote(accg, dg_same, tiny.at[I1], tiny.at[I0], place.across).start()

    @pl.when(is_r)
    def _():
        remote(accg, dg_other, tiny.at[I1], tiny.at[I4], place.sibling).start()
        remote(accg, dg_other, tiny.at[I2], tiny.at[I4], place.across_other).start()

    for i in (micro - I2, micro - I1):
        back_ready(jnp.int32(i))

    sent, got = drain(place)
    sent(m_s, bulk.at[I6])

    @pl.when(is_r)
    def _():
        sent(gbuf, bulk.at[5])
        sent(m_s, bulk.at[7])
        remote(accg, dg_other, tiny.at[I2], tiny.at[I4], place.sibling).wait_send()

    @pl.when(home13)
    def _():
        sent(gbuf.at[I0:EARLY_G], bulk.at[I4])

    @pl.when(place.home == I1)
    def _():
        got(dx_s, dx_sem)

    @pl.when(jnp.logical_not(is_first))
    def _():
        remote(loss_mine, loss_mine, loss_sem.at[I0], loss_sem.at[I1], place.sibling).wait_send()
    remote(loss_mine, loss_mine, loss_sem.at[I2], loss_sem.at[I3], place.sibling).wait_send()
    remote(loss_mine, loss_mine, loss_sem.at[I2], loss_sem.at[I3], place.sibling).wait_recv()

    @pl.when(place.home == I2)
    def _():
        sent(a_s, bulk.at[I8])
        sent(h_s.at[I0:micro // I2], bulk.at[9])

    remote(accg, dg_other, tiny.at[I1], tiny.at[I4], place.sibling).wait_send()
    got(od_other, do_sem)

    @pl.when(place.is_l | home13)
    def _():
        got(og_other, go_sem)

    @pl.when(jnp.logical_not(home13) & is_r)
    def _():
        got(og_same.at[I0:EARLY_G], gs_sem)
        got(og_other.at[I0:EARLY_G], go_sem)
    got(dg_same, tiny.at[I0])
    got(dg_other, tiny.at[I4])

    @pl.when(is_r)
    def _():
        got(od_same, ds_sem)

    @pl.when(place.is_l)
    def _():
        got(og_same, gs_sem)

    @pl.when(is_last & is_r)
    def _():
        got(oa_same, as_sem)
        got(oa_other, ao_sem)
        got(oh_same.at[I0:micro // I2], os_sem)
        got(oh_other.at[I0:micro // I2], oo_sem)


def shapes(*dims_list):
    return [jax.ShapeDtypeStruct(d, BF) for d in dims_list]


def forward_phase(dims, x, y, own, own_gains):
    micro, seq, width, heads, head_dim, ffn = dims
    half = heads // I2 * HEAD_PAD
    act = (micro, seq, width)
    raw = [w.shape for w in own]
    turned = [(I3, width, CHUNK), (I1, width, CHUNK), (ffn // I2, width), (I3, width, CHUNK)]
    out_shape = shapes(act, act, (micro, seq, I6 * half), (micro, seq, ffn), *[act] * 7)
    out_shape += [jax.ShapeDtypeStruct(s, F32) for s in ((I8, 128), own_gains.shape)]
    out_shape += shapes(*raw, *raw, *turned, *turned, turned[I0], turned[I0], *[(len(ROUND), 768, width)] * I2)
    any_spec = pl.BlockSpec(memory_space=ANY)
    vmem, dma = pltpu.VMEM, pltpu.SemaphoreType.DMA
    row = vmem((seq, width), BF)
    scratch = [
        vmem(act, BF), row, vmem((I2, seq, width), BF), row, row, row, vmem((seq, I6 * half), BF), vmem((seq, ffn), BF), vmem((seq, CHUNK), BF),
        vmem((seq, I2 * half), BF), vmem((seq, width), F32), vmem((I8, width), F32), vmem((I8, 128), F32), vmem((I2, width), F32),
        vmem((I6, CHUNK, width), BF), vmem((I2, CHUNK, width), BF), vmem((DEPTH, width, CHUNK), BF),
        dma((I4,)), dma((I4,)), dma((I4,)), dma((I4,)), dma((12,)), dma((I2,)), dma((I2,)), dma((I2,)), *[dma((len(ROUND),))] * 5,
        dma((micro,)), dma((I2,)), dma((I2,)), dma((I3,)), dma((DEPTH,)), dma((I6,)), dma((I2,)), dma((I2,)), dma(()), dma(()),
        dma(()), dma(()), dma(()), dma(()), dma(()), dma(()), dma((I4,)), dma((I2,)), dma(()),
    ]
    return pl.pallas_call(
        functools.partial(forward_kernel, dims),
        out_shape=tuple(out_shape),
        in_specs=[any_spec] * I6 + [pl.BlockSpec(memory_space=vmem)],
        out_specs=(any_spec,) * len(out_shape),
        scratch_shapes=scratch,
        compiler_params=pltpu.CompilerParams(collective_id=I0, has_side_effects=True, vmem_limit_bytes=VMEM_LIMIT),
        name='forward_phase',
    )(x, y, *own, own_gains)


def backward_phase(dims, saved, weights, gains, loss, after, placed):
    micro, seq, width, heads, head_dim, ffn = dims
    half = heads // I2 * HEAD_PAD
    act = (micro, seq, width)
    out_shape = shapes(*[act] * 10) + [jax.ShapeDtypeStruct((I2, I8, width), F32)] * I2 + [jax.ShapeDtypeStruct((I2, I8, 128), F32)]
    any_spec = pl.BlockSpec(memory_space=ANY)
    vmem, dma = pltpu.VMEM, pltpu.SemaphoreType.DMA
    scratch = [
        vmem(act, BF), vmem((seq, width), BF), vmem((I2, seq, width), BF), vmem((seq, I6 * half), BF), vmem((seq, ffn), BF),
        vmem((I2, seq, width), BF), vmem((seq, CHUNK), BF), vmem((seq, I2 * half), BF), vmem((seq, I6 * half), BF), vmem((seq, width), F32),
        vmem((I2, I8, width), F32), vmem((I6, CHUNK, width), BF), vmem((BACK_DEPTH, width, CHUNK), BF), vmem((KDEPTH, CHUNK, width), BF),
        dma((micro,)), dma((I2,)), dma((I2,)), dma(()), dma((I2,)), dma(()), dma((BACK_DEPTH,)), dma((KDEPTH,)), dma((I6,)), dma((I4,)),
        *[dma(())] * I8, dma((10,)), dma((5,)), dma((I4,)),
    ]
    return pl.pallas_call(
        functools.partial(backward_kernel, dims),
        out_shape=tuple(out_shape),
        in_specs=[any_spec] * 14 + [pl.BlockSpec(memory_space=vmem)] * I2 + [any_spec] * 7,
        out_specs=(any_spec,) * len(out_shape),
        scratch_shapes=scratch,
        input_output_aliases={17 + i: I4 + i for i in range(I6)},
        compiler_params=pltpu.CompilerParams(collective_id=I1, has_side_effects=True, vmem_limit_bytes=VMEM_LIMIT),
        name='backward_phase',
    )(*saved, *weights, gains, loss, after, *placed)


def recompute_kernel(dims, early, h_same, h_other, a_same, a_other, gains, wq, wu, *refs):
    (done, u_o, qkv_o, ctx_o, n1_o, n2_o), (wqbuf, wubuf, count, sem) = refs[-10:-I4], refs[-I4:]
    micro, seq, width, heads, head_dim, ffn = dims
    place = Place()
    scale = head_dim ** -0.5
    half = heads // I2 * HEAD_PAD
    steps = I2 * micro * seq // BLOCK

    def body(hs, ho, rs, ro, u, qkv, ctx, n1, n2):
        step = count[I0]
        count[I0] = step + I1
        for low, high, gain, dst in ((hs, ho, gains[I1:I2, :], n2), (rs, ro, gains[I0:I1, :], n1)):
            @pl.when(step < steps // I2)
            def _(low=low, gain=gain, dst=dst):
                norm_rows(low, gain, dst, BLOCK)

            @pl.when(step >= steps // I2)
            def _(high=high, gain=gain, dst=dst):
                norm_rows(high, gain, dst, BLOCK)

        def qkv_step(j, c):
            rows = pl.ds(pl.multiple_of(j * SUB, SUB), SUB)
            qkv[:, lanes(j * SUB, SUB)] = mm_nt(n1[...], wqbuf[rows, :]).astype(BF)
            u[:, lanes(j * SUB, SUB)] = mm(n2[...], wubuf[:, lanes(j * SUB, SUB)]).astype(BF)
            return c
        lax.fori_loop(I0, I3 * half // SUB, qkv_step, I0)

        def head_step(j, c):
            at = [(pl.ds(s, seq), r * HEAD_PAD) for s in range(I0, BLOCK, seq) for r in range(I4)]
            base = j * (I4 * HEAD_PAD)
            views = [[qkv[rows, lanes(base + t * half + col, HEAD_PAD)] for t in range(I3)] for rows, col in at]
            for (rows, col), context in zip(at, attention_forward(views, scale)):
                ctx[rows, lanes(base + col, HEAD_PAD)] = context
            return c
        lax.fori_loop(I0, I2, head_step, I0)

    @pl.when(place.home < I2 if early else place.home > I1)
    def _():
        wqbuf[...] = jnp.zeros_like(wqbuf)
        for t in range(I3):
            load_heads(wq, t, wqbuf.at[pl.ds(t * CHUNK, CHUNK)], sem.at[I0])
        up = pltpu.make_async_copy(wu, wubuf, sem.at[I1])
        up.start()
        up.wait()
        pltpu.make_async_copy(wq, wqbuf.at[I0:wq.shape[I0]], sem.at[I0]).wait()
        count[I0] = I0
        low = pl.BlockSpec((BLOCK, width), lambda i: (jnp.minimum(i, steps // I2 - I1), I0))
        high = pl.BlockSpec((BLOCK, width), lambda i: (jnp.maximum(i - steps // I2, I0), I0))
        block = lambda n: pl.BlockSpec((BLOCK, n), lambda i: (i, I0))
        pltpu.emit_pipeline(body, grid=(steps,), in_specs=[low, high, low, high],
                            out_specs=[block(ffn // I2), block(I3 * half), block(half), block(width), block(width)])(
            h_same, h_other, a_same, a_other, u_o, qkv_o, ctx_o, n1_o, n2_o)


def owner_recompute(dims, early, again, h_rows, a_rows, gains, own):
    micro, seq, width, heads, head_dim, ffn = dims
    half = heads // I2 * HEAD_PAD
    tokens = I2 * micro * seq
    any_spec = pl.BlockSpec(memory_space=ANY)
    vmem = pltpu.VMEM
    earlier = () if early else tuple(again)
    return pl.pallas_call(
        functools.partial(recompute_kernel, dims, early),
        out_shape=(jax.ShapeDtypeStruct((I8, 128), F32), *shapes((tokens, ffn // I2), (tokens, I3 * half), (tokens, half), (tokens, width), (tokens, width))),
        in_specs=[any_spec] * I4 + [pl.BlockSpec(memory_space=vmem)] + [any_spec] * (I2 + len(earlier)),
        out_specs=(any_spec,) * I6,
        scratch_shapes=[vmem((I3 * half, width), BF), vmem((width, ffn // I2), BF), pltpu.SMEM((I1,), jnp.int32), pltpu.SemaphoreType.DMA((I2,))],
        input_output_aliases={7 + i: I1 + i for i in range(len(earlier))},
        compiler_params=pltpu.CompilerParams(has_side_effects=True, vmem_limit_bytes=VMEM_LIMIT),
        name='owner_recompute',
    )(*h_rows, *a_rows, gains, own[I0], own[I2], *earlier)


def spread_dx(step, last, dx, d_in, og_same, og_other, bounce, here_sem, parent_sem, sib_sem, send_sems, og_sems):
    place = Place()
    micro = dx.shape[I0]
    along_x = place.at(place.tp, (place.stage + I2) % I4)
    barrier = pltpu.get_barrier_semaphore()
    is_leaf = place.home > I1
    gives_g = (place.home == I1) & place.is_l
    takes_g = (place.home == I0) & jnp.logical_not(place.is_l)
    late = [micro - I1 - i for i in range(micro) if i % I2 == I0 or i > I2 * EARLY_G]

    def block(m):
        return d_in.at[m, place.core]

    def to_sibling(m, src):
        remote(src, block(m), send_sems.at[I0], sib_sem, place.sibling).start()

    def tell(there):
        pl.semaphore_signal(barrier, inc=I1, device_id=there, device_id_type=MESH)

    @pl.when(step == I0)
    def _():
        tell(place.sibling)

        @pl.when(is_leaf)
        def _():
            tell(along_x)

        @pl.when(takes_g)
        def _():
            tell(place.across)

    @pl.when((step == I1) & jnp.logical_not(is_leaf))
    def _():
        pl.semaphore_wait(barrier, I2 + gives_g.astype(jnp.int32))

        @pl.when(gives_g)
        def _():
            for t, og in enumerate((og_same, og_other)):
                for m in late:
                    remote(og.at[m], og.at[m], og_sems.at[t], og_sems.at[I2 + t], place.across).start()
        for m in reversed(range(micro)):
            remote(dx.at[m], block(m), send_sems.at[I1], parent_sem.at[m], along_x).start()
            to_sibling(m, dx.at[m])
        pltpu.make_async_copy(dx, bounce, here_sem).start()

    @pl.when((step == I2) & jnp.logical_not(is_leaf))
    def _():
        pltpu.make_async_copy(dx, bounce, here_sem).wait()
        for m in range(micro):
            pltpu.make_async_copy(bounce.at[m], block(m), here_sem).start()

    @pl.when((step == (last + I1) // I2) & takes_g)
    def _():
        for t, og in enumerate((og_same, og_other)):
            part = og.at[I0:len(late)]
            remote(part, part, og_sems.at[t], og_sems.at[I2 + t], place.across).wait_recv()

    @pl.when((step == last) & is_leaf)
    def _():
        pl.semaphore_wait(barrier, I1)
        for m in reversed(range(micro)):
            remote(block(m), block(m), send_sems.at[I0], parent_sem.at[m], place.sibling).wait_recv()
            to_sibling(m, block(m))

    @pl.when(step == last)
    def _():
        remote(dx, dx, send_sems.at[I0], sib_sem, place.sibling).wait_send()

        @pl.when(jnp.logical_not(is_leaf))
        def _():
            remote(dx, dx, send_sems.at[I1], sib_sem, place.sibling).wait_send()
            pltpu.make_async_copy(dx, dx, here_sem).wait()

        @pl.when(gives_g)
        def _():
            for t, og in enumerate((og_same, og_other)):
                part = og.at[I0:len(late)]
                remote(part, part, og_sems.at[t], og_sems.at[I2 + t], place.across).wait_send()
        remote(dx, dx, send_sems.at[I0], sib_sem, place.sibling).wait_recv()


def owner_backward_kernel(dims, dx, ds, do, u, qkv, wo, wd, gs_in, go_in, dqkv, dup, z, d_in, og_same, og_other,
                          dmid, gbuf, dctx, wobuf, bounce, sem, g_sem, here_sem, parent_sem, sib_sem, send_sems, og_sems):
    micro, seq, width, heads, head_dim, ffn = dims
    half = heads // I2 * HEAD_PAD
    scale = head_dim ** -0.5
    step, steps = pl.program_id(I0), pl.num_programs(I0)
    blocks = steps // I2
    spread_dx(step, steps - I1, dx, d_in, og_same, og_other, bounce, here_sem, parent_sem, sib_sem, send_sems, og_sems)

    @pl.when(step == I0)
    def _():
        wobuf[...] = jnp.zeros_like(wobuf)
        load_heads(wo, I0, wobuf, sem)
        pltpu.make_async_copy(wo, wobuf.at[I0:wo.shape[I0]], sem).wait()

    def g_load(n, start):
        rows = BLOCK // seq
        for og, low in ((og_same, I0), (og_other, blocks // I2)):
            @pl.when((n >= low) & (n < low + blocks // I2))
            def _(og=og, low=low):
                copy = pltpu.make_async_copy(og.at[pl.ds((n - low) * rows, rows)], gbuf.at[n % I2], g_sem.at[n % I2])
                copy.start() if start else copy.wait()

    @pl.when(step < blocks)
    def _():
        @pl.when(step < blocks // I2)
        def _():
            dmid[...] = ds[...]

        @pl.when(step >= blocks // I2)
        def _():
            dmid[...] = do[...]

        def ctx_step(j, c):
            rows = pl.ds(pl.multiple_of(j * SUB, SUB), SUB)
            dctx[:, lanes(j * SUB, SUB)] = mm_nt(dmid[...], wobuf[rows, :]).astype(BF)
            return c
        lax.fori_loop(I0, half // SUB, ctx_step, I0)

        def head_step(j, c):
            base = j * (I2 * HEAD_PAD)
            at = [(pl.ds(s, seq), base + r * HEAD_PAD) for s in range(I0, BLOCK, seq) for r in range(I2)]
            group = [(*(qkv[rows, lanes(t * half + col, HEAD_PAD)] for t in range(I3)), dctx[rows, lanes(col, HEAD_PAD)]) for rows, col in at]
            for (rows, col), grads in zip(at, attention_backward(group, scale)):
                for t, value in enumerate(grads):
                    dqkv[rows, lanes(t * half + col, HEAD_PAD)] = value
            return c
        lax.fori_loop(I0, heads // I4, head_step, I0)

    @pl.when(step == blocks)
    def _():
        g_load(step - blocks, True)

    @pl.when(step >= blocks)
    def _():
        n = step - blocks
        g_load(n + I1, True)
        g_load(n, False)
        grad = gbuf.at[n % I2]

        def mlp_step(j, c):
            rows = pl.ds(pl.multiple_of(j * SUB, SUB), SUB)
            cols = lanes(j * SUB, SUB)
            dz = mm_nt(grad[...].reshape(BLOCK, width), wd[rows, :]).astype(BF).astype(F32)
            up = u[:, cols].astype(F32)
            gate, up2 = gelu_gate(up)
            hidden = up * gate
            z[:, cols] = hidden.astype(BF)
            dup[:, cols] = (dz * gelu_slope(hidden, gate, up2)).astype(BF)
            return c
        lax.fori_loop(I0, ffn // I2 // SUB, mlp_step, I0)


def owner_backward(dims, dx, d_rows, og, ups, qkv, own):
    micro, seq, width, heads, head_dim, ffn = dims
    half = heads // I2 * HEAD_PAD
    tokens = I2 * micro * seq
    blocks = tokens // BLOCK
    vmem, dma = pltpu.VMEM, pltpu.SemaphoreType.DMA
    any_spec = pl.BlockSpec(memory_space=ANY)
    first = lambda i: jnp.minimum(i, blocks - I1)
    second = lambda i: jnp.maximum(i - blocks, I0)
    low = pl.BlockSpec((BLOCK, width), lambda i: (jnp.minimum(i, blocks // I2 - I1), I0))
    high = pl.BlockSpec((BLOCK, width), lambda i: (jnp.maximum(first(i) - blocks // I2, I0), I0))
    attn_block = pl.BlockSpec((BLOCK, I3 * half), lambda i: (first(i), I0))
    mlp_block = pl.BlockSpec((BLOCK, ffn // I2), lambda i: (second(i), I0))
    act = (micro, seq, width)
    return pl.pallas_call(
        functools.partial(owner_backward_kernel, dims),
        grid=(I2 * blocks,),
        out_shape=tuple(shapes((tokens, I3 * half), (tokens, ffn // I2), (tokens, ffn // I2), (micro, I2, seq, width), act, act)),
        in_specs=[any_spec, low, high, mlp_block, attn_block, any_spec, pl.BlockSpec((ffn // I2, width), lambda i: (I0, I0)), any_spec, any_spec],
        out_specs=(attn_block, mlp_block, mlp_block, any_spec, any_spec, any_spec),
        scratch_shapes=[vmem((BLOCK, width), BF), vmem((I2, BLOCK // seq, seq, width), BF), vmem((BLOCK, half), BF), vmem((half, width), BF), vmem(act, BF),
                        dma(()), dma((I2,)), dma(()), dma((micro,)), dma(()), dma((I2,)), dma((I4,))],
        input_output_aliases={7: I4, I8: 5},
        compiler_params=pltpu.CompilerParams(collective_id=I2, has_side_effects=True, vmem_limit_bytes=VMEM_LIMIT),
        name='owner_backward',
    )(dx, *d_rows, ups, qkv, own[I1], own[I3], *og)


def bring(pairs, sem):
    copies = [pltpu.make_async_copy(src, dst, sem.at[i]) for i, (src, dst) in enumerate(pairs)]
    for copy in copies:
        copy.start()
    for copy in copies:
        copy.wait()


def attn_products_kernel(dq, dk, dv, ctx, n1_o, ds, do, dx_in, dwq, dwo, dx_out, n1, dmid, dqkvt, ctxt, bounce, sem, dx_sem):
    tokens, width = n1.shape
    part = tokens // I2
    head_dim = dwo.shape[I1]
    step, last = pl.program_id(I0), pl.num_programs(I0) - I1
    into, out_of = pltpu.make_async_copy(dx_in, bounce, dx_sem), pltpu.make_async_copy(bounce, dx_out, dx_sem)

    @pl.when(step == I1)
    def _():
        into.start()

    @pl.when(step == I2)
    def _():
        into.wait()
        out_of.start()

    @pl.when(step == last)
    def _():
        out_of.wait()

    @pl.when(step == I0)
    def _():
        bring([(n1_o, n1), (ds, dmid.at[pl.ds(I0, part)]), (do, dmid.at[pl.ds(part, part)])], sem)

    def turn(rows):
        for t, block in enumerate((dq, dk, dv)):
            for r in range(I2):
                at = (I2 * t + r) * head_dim
                dqkvt[at:at + head_dim, rows] = block[rows, r * HEAD_PAD:(r + I1) * HEAD_PAD].T[I0:head_dim]
        for r in range(I2):
            ctxt[r * head_dim:(r + I1) * head_dim, rows] = ctx[rows, r * HEAD_PAD:(r + I1) * HEAD_PAD].T[I0:head_dim]
    rows_loop(tokens, SUB, turn)
    for c in range(I0, width, SUB):
        cut = slice(c, c + SUB)
        dwq[:, :, :, cut] = mm(dqkvt[...], n1[:, cut]).reshape(I3, I2, head_dim, SUB)
        dwo[:, :, cut] = mm(ctxt[...], dmid[:, cut]).reshape(I2, head_dim, SUB)


def attn_products(dqkv, ctx, n1, d_rows, dx, out_dims):
    heads, head_dim, width = out_dims
    tokens = n1.shape[I0]
    vmem = pltpu.VMEM
    any_spec = pl.BlockSpec(memory_space=ANY)
    pairs = heads // I2
    cols = lambda t: pl.BlockSpec((tokens, I2 * HEAD_PAD), lambda i: (I0, t * pairs + i))
    return pl.pallas_call(
        attn_products_kernel,
        grid=(pairs,),
        out_shape=(jax.ShapeDtypeStruct((I3,) + out_dims, F32), jax.ShapeDtypeStruct(out_dims, F32), jax.ShapeDtypeStruct(dx.shape, BF)),
        in_specs=[cols(I0), cols(I1), cols(I2), cols(I0), any_spec, any_spec, any_spec, any_spec],
        out_specs=(pl.BlockSpec((I3, I2, head_dim, width), lambda i: (I0, i, I0, I0)), pl.BlockSpec((I2, head_dim, width), lambda i: (i, I0, I0)), any_spec),
        scratch_shapes=[vmem((tokens, width), BF), vmem((tokens, width), BF), vmem((I6 * head_dim, tokens), BF), vmem((I2 * head_dim, tokens), BF),
                        vmem(dx.shape, BF), pltpu.SemaphoreType.DMA((I3,)), pltpu.SemaphoreType.DMA(())],
        compiler_params=pltpu.CompilerParams(vmem_limit_bytes=VMEM_LIMIT),
        name='attn_products',
    )(dqkv, dqkv, dqkv, ctx, n1, *d_rows, dx)


def mlp_products_kernel(dup, z, n2_o, gs, go, dwu, dwd, n2t, grad, zt, stage, sem):
    width, tokens = n2t.shape
    part = tokens // I2

    @pl.when(pl.program_id(I0) == I0)
    def _():
        bring([(n2_o, stage), (gs, grad.at[pl.ds(I0, part)]), (go, grad.at[pl.ds(part, part)])], sem)

        def turn(rows):
            for c in range(I0, width, SUB):
                n2t[c:c + SUB, rows] = stage[rows, c:c + SUB].T
        rows_loop(tokens, SUB, turn)

    def turn_z(rows):
        for c in range(I0, z.shape[I1], SUB):
            zt[c:c + SUB, rows] = z[rows, c:c + SUB].T
    rows_loop(tokens, SUB, turn_z)
    for c in range(I0, width, I2 * SUB):
        dwu[c:c + I2 * SUB, :] = mm(n2t[c:c + I2 * SUB, :], dup[...])
    for c in range(I0, width, SUB):
        dwd[:, c:c + SUB] = mm(zt[...], grad[:, c:c + SUB])


def mlp_products(dup, hidden, n2, g_rows):
    tokens, width = n2.shape
    cols = dup.shape[I1]
    vmem = pltpu.VMEM
    any_spec = pl.BlockSpec(memory_space=ANY)
    block = pl.BlockSpec((tokens, SUB), lambda i: (I0, i))
    return pl.pallas_call(
        mlp_products_kernel,
        grid=(cols // SUB,),
        out_shape=(jax.ShapeDtypeStruct((width, cols), F32), jax.ShapeDtypeStruct((cols, width), F32)),
        in_specs=[block, block, any_spec, any_spec, any_spec],
        out_specs=(pl.BlockSpec((width, SUB), lambda i: (I0, i)), pl.BlockSpec((SUB, width), lambda i: (i, I0))),
        scratch_shapes=[vmem((width, tokens), BF), vmem((tokens, width), BF), vmem((SUB, tokens), BF), vmem((tokens, width), BF), pltpu.SemaphoreType.DMA((I3,))],
        compiler_params=pltpu.CompilerParams(vmem_limit_bytes=VMEM_LIMIT),
        name='mlp_products',
    )(dup, hidden, n2, *g_rows)


def solution(mesh):
    act_spec = P('rep', None, None, None)
    weight_specs = (
        P(('rep', 'stage'), None, None, 'tp', None),
        P(('rep', 'stage'), 'tp', None, None),
        P(('rep', 'stage'), None, 'tp'),
        P(('rep', 'stage'), 'tp', None),
        P(('rep', 'stage'), None),
        P(('rep', 'stage'), None),
    )

    def device_fn(inputs, targets, w_qkv, w_out, w_up, w_down, gain_attn, gain_mlp):
        micro_count, _, seq_len, width = inputs.shape
        dims = (micro_count, seq_len, width, I2 * w_out.shape[I1], w_out.shape[I2], I2 * w_up.shape[I2])
        norm_factor = 1.0 / (inputs.size)
        own = (w_qkv[I0], w_out[I0], w_up[I0], w_down[I0])
        own_gains = jnp.concatenate([gain_attn, gain_mlp]).astype(F32)
        rows_of = (own[I0].transpose(I1, I2, I3, I0).reshape(-I1, width), own[I1].reshape(-I1, width), own[I2], own[I3])

        (acts, mids, qkv, ups, seeds, oh_same, oh_other, oa_same, oa_other, og_same, og_other, loss_tile, home_gains, *weights) = forward_phase(dims, inputs, targets, rows_of, own_gains)
        (nq, no, nu, nd), (fq, fo, fu, fd) = weights[I0:I4], weights[I4:I8]
        (tq0, to0, tu0, td0), (tq1, to1, tu1, td1) = weights[I8:12], weights[12:16]

        flat = lambda *rows: [r.reshape(-I1, width) for r in rows]
        done, *again = owner_recompute(dims, True, None, flat(oh_same, oh_other), flat(oa_same, oa_other), own_gains, rows_of)
        dx, _, od_same, od_other, og_same, og_other, oa_same, oa_other, oh_same, oh_other, dg_same, dg_other, loss_all = backward_phase(
            dims, (acts, mids, qkv, ups, seeds), (rows_of[I0], nq, fq, td0, td1, to0, to1, tu0, tu1), home_gains, loss_tile, done,
            (og_same, og_other, oa_same, oa_other, oh_same, oh_other))
        _, *again = owner_recompute(dims, False, again, flat(oh_same, oh_other), flat(oa_same, oa_other), own_gains, rows_of)
        ups_own, qkv_own, ctx_own, n1, n2 = again
        d_rows = flat(od_same, od_other)
        d_qkv_rows, d_up_rows, hidden, dx_all, og_same, og_other = owner_backward(dims, dx, d_rows, (og_same, og_other), ups_own, qkv_own, rows_of)
        d_qkv, d_out, d_inputs = attn_products(d_qkv_rows, ctx_own, n1, d_rows, dx_all, w_out.shape[I1:])
        d_up, d_down = mlp_products(d_up_rows, hidden, n2, flat(og_same, og_other))
        weight_grads = (d_qkv.transpose(I3, I0, I1, I2), d_out, d_up, d_down)
        mine = jnp.sum(dg_same + dg_other, I1)
        loss = jnp.sum(loss_all) * (0.5 * norm_factor)

        return (loss.reshape(I1), d_inputs) + tuple(g[None] for g in weight_grads) + (mine[I0][None], mine[I1][None])

    return jax.shard_map(device_fn, mesh=mesh, in_specs=(act_spec, act_spec) + weight_specs, out_specs=(P('rep'), act_spec) + weight_specs, check_vma=False)
```

```python
import functools

import jax
import jax.numpy as jnp
from jax import lax
from jax.experimental import pallas as pl
from jax.experimental.pallas import tpu as pltpu
from jax.sharding import PartitionSpec as P

NORM_EPS = 1e-5
BF = jnp.bfloat16
F32 = jnp.float32
MESH = pl.DeviceIdType.MESH
ANY = pl.ANY


GELU_A = 0.7978845608028654
GELU_B = 0.044715
I0, I1, I2, I3, I4, I6, I8 = 0, 1, 2, 3, 4, 6, 8
CHUNK = 1024
BLOCK = 384
SUB = 256
DEPTH = 6
BACK_DEPTH = 5
KDEPTH = 3
EARLY_G = 3
STAGGER_NS = 6000
EARLY_SEEDS = 5
HEAD_PAD = 128
VMEM_LIMIT = 67043328


def mm(a, b):
    return lax.dot_general(a, b, (((I1,), (I0,)), ((), ())), preferred_element_type=F32)


def mm_nt(a, b):
    return lax.dot_general(a, b, (((I1,), (I1,)), ((), ())), preferred_element_type=F32)


def mm_tn(a, b):
    return lax.dot_general(a, b, (((I0,), (I0,)), ((), ())), preferred_element_type=F32)


class Place:
    def __init__(self):
        self.tp = lax.axis_index('tp')
        self.stage = lax.axis_index('stage')
        self.core = self.stage % I2
        self.x_pos = self.stage // I2
        self.home = self.x_pos * (I3 - I2 * self.tp) + self.tp
        self.is_l = self.stage == self.home
        self.sib = self.stage + I1 - I2 * self.core

    def at(self, tp, stage):
        return {'tp': tp, 'stage': stage}

    @property
    def sibling(self):
        return self.at(self.tp, self.sib)

    @property
    def along_x(self):
        return self.at(self.tp, (self.stage + I2) % I4)

    @property
    def across(self):
        return self.at(I1 - self.tp, self.stage)

    @property
    def across_other(self):
        return self.at(I1 - self.tp, self.sib)

    def chain(self, delta):
        there = self.home + delta
        x_pos = there // I2
        tp = there % I2 + x_pos * (I1 - I2 * (there % I2))
        return self.at(tp, I2 * x_pos + self.core)


def entry_barrier(place):
    barrier = pltpu.get_barrier_semaphore()
    for d_tp in (I0, I1):
        for d_stage in range(I4):
            if d_tp or d_stage:
                tp = place.tp + d_tp - I2 * d_tp * place.tp
                stage = (place.stage + d_stage) % I4
                pl.semaphore_signal(barrier, inc=I1, device_id=place.at(tp, stage), device_id_type=MESH)
    pl.semaphore_wait(barrier, 7)


def remote(src, dst, send_sem, recv_sem, device_id):
    return pltpu.make_async_remote_copy(src_ref=src, dst_ref=dst, send_sem=send_sem, recv_sem=recv_sem, device_id=device_id, device_id_type=MESH)


def rows_loop(total, step, body):
    def run(i, carry):
        body(pl.ds(pl.multiple_of(i * step, step), step))
        return carry
    lax.fori_loop(I0, total // step, run, I0)


def norm_rows(src, gain_row, dst, total):
    def body(rows):
        v = src[rows, :].astype(F32)
        inv = lax.rsqrt(jnp.mean(v * v, axis=-I1, keepdims=True) + NORM_EPS)
        dst[rows, :] = (v * inv * gain_row).astype(BF)
    rows_loop(total, 32, body)


def gelu_gate(u):
    u2 = u * u
    t = jnp.tanh(u * (GELU_A + (GELU_A * GELU_B) * u2))
    return 0.5 * t + 0.5, u2


def gelu_slope(hidden, gate, u2):
    return gate + hidden * (1.0 - gate) * (2.0 * GELU_A + (6.0 * GELU_A * GELU_B) * u2)


def row_parts(heads, cut=128):
    return [(*(x[low:high] for x in queries), *(x[:high] for x in keys), low)
            for queries, keys in heads for low, high in ((I0, cut), (cut, queries[I0].shape[I0]))]


def softmax_parts(scores, starts, keys_axis):
    masked = []
    for s, start in zip(scores, starts):
        k_pos = lax.broadcasted_iota(jnp.int32, s.shape, keys_axis)
        q_pos = lax.broadcasted_iota(jnp.int32, s.shape, I1 - keys_axis) + start
        masked.append(jnp.where(k_pos <= q_pos, s, -1e30))
    tops = [jnp.max(s, axis=keys_axis, keepdims=True) for s in masked]
    powers = [jnp.exp(s - top) for s, top in zip(masked, tops)]
    scales = [1.0 / jnp.sum(e, axis=keys_axis, keepdims=True) for e in powers]
    return [e * r for e, r in zip(powers, scales)]


def join_keys(top, low, cut=128):
    return jnp.concatenate([top + low[:cut], low[cut:]], I0).astype(BF)


def attention_forward(heads, scale):
    units = row_parts([((q,), (k, v)) for q, k, v in heads])
    probs = softmax_parts([mm_nt(q, k) * scale for q, k, _, _ in units], [u[-I1] for u in units], I1)
    parts = [mm(p.astype(BF), u[I2]) for p, u in zip(probs, units)]
    return [jnp.concatenate([a, b], I0).astype(BF) for a, b in zip(parts[I0::I2], parts[I1::I2])]


def attention_backward(heads, scale):
    units = row_parts([((q, dc), (k, v)) for q, k, v, dc in heads])
    scores = [mm_nt(k, q) * scale for q, _, k, _, _ in units]
    dps = [mm_nt(v, dc) for _, dc, _, v, _ in units]
    probs = softmax_parts(scores, [u[-I1] for u in units], I0)
    dps = [dp.astype(BF).astype(F32) for dp in dps]
    deltas = [jnp.sum(dp * p, axis=I0, keepdims=True) for dp, p in zip(dps, probs)]
    dss = [p * (dp - delta) * scale for p, dp, delta in zip(probs, dps, deltas)]
    terms = []
    for ds in dss:
        hi = ds.astype(BF)
        rest = ds - hi.astype(F32)
        lo = rest.astype(BF)
        terms.append((hi, lo, (rest - lo.astype(F32)).astype(BF)))
    dvs = [mm(p.astype(BF), u[I1]) for p, u in zip(probs, units)]
    dks = [mm(hi, u[I0]) + (mm(lo, u[I0]) + mm(tail, u[I0])) for (hi, lo, tail), u in zip(terms, units)]
    k_turned = [u[I2].T for u in units]
    dqs = [(mm(kt, hi) + (mm(kt, lo) + mm(kt, tail))).astype(BF) for (hi, lo, tail), kt in zip(terms, k_turned)]
    return [(jnp.concatenate([dqs[i].T, dqs[i + I1].T], I0), join_keys(dks[i], dks[i + I1]), join_keys(dvs[i], dvs[i + I1]))
            for i in range(I0, len(units), I2)]


def blocked(rows, stack, cols):
    total = mm(rows[:, I0:CHUNK], stack[I0, :, cols])
    for j in range(I1, stack.shape[I0]):
        total = total + mm(rows[:, j * CHUNK:(j + I1) * CHUNK], stack[j, :, cols])
    return total


def lanes(offset, size):
    return pl.ds(pl.multiple_of(offset, 128), size)


def load_resident(buf, sem, halves):
    for c in range(I6):
        for condition, ref in halves[c // I3]:
            copy = pltpu.make_async_copy(ref.at[(c % I3) * CHUNK:(c % I3 + I1) * CHUNK, :], buf.at[c], sem.at[c])
            if condition is None:
                copy.start()
            else:
                pl.when(condition)(copy.start)


def load_heads(ref, index, dst, sem):
    for r in range(I8):
        rows = pl.ds(pl.multiple_of(index * 768 + r * 96, 96), 96)
        pltpu.make_async_copy(ref.at[rows, :], dst.at[r * 128:r * 128 + 96, :], sem).start()


class Stream:
    def __init__(self, buf, sem, depth, parts, total, by_heads):
        self.buf, self.sem, self.depth, self.parts, self.total, self.by_heads = buf, sem, depth, parts, total, by_heads
        self.per_tick = sum(p[I1] for p in parts)

    def copy_in(self, ref, index, slot):
        if not self.by_heads:
            pltpu.make_async_copy(ref.at[index], self.buf.at[slot], self.sem.at[slot]).start()
            return
        load_heads(ref, index, self.buf.at[slot], self.sem.at[slot])

    def start(self, seq):
        @pl.when(seq < self.total)
        def _():
            j = seq % self.per_tick
            slot = seq % self.depth
            base = I0
            for choices, chunks in self.parts:
                for condition, ref in choices:
                    here = (j >= base) & (j < base + chunks)
                    here = here if condition is None else here & condition

                    @pl.when(here)
                    def _(ref=ref, low=base):
                        self.copy_in(ref, j - low, slot)
                base += chunks

    def prime(self):
        for seq in range(self.depth):
            self.start(jnp.int32(seq))

    def wait(self, seq):
        slot = seq % self.depth
        ref = self.parts[I0][I0][I0][I1]
        if self.by_heads:
            pltpu.make_async_copy(ref.at[I0:768, :], self.buf.at[slot, I0:768, :], self.sem.at[slot]).wait()
        else:
            pltpu.make_async_copy(ref.at[I0], self.buf.at[slot], self.sem.at[slot]).wait()
        return self.buf.at[slot]


PIECES = [(0, 0, 0), (0, 0, 1), (0, 0, 2), (1, 0, 0), (2, 1, 0), (2, 1, 1), (2, 1, 2), (2, 1, 3), (3, 0, 0), (3, 0, 1), (3, 0, 2), (3, 0, 3)]


ROUND = (10, 11)
ROUND_STEPS = (1, 3)


def piece(ref, axis, index):
    return ref.at[index * 768:(index + I1) * 768, :] if axis == I0 else ref.at[:, index * 768:(index + I1) * 768]


def weight_phase(place, is_r, own, near, far, turned, up_chunks, wn, wk, send_sem, y_send, d_send, near_sem, far_sem, load_sem, store_sem, chunk_sem,
                 round_a, round_b, ra_sem, rb_sem, x_send, xd_send, rs_send):
    wk[...] = jnp.zeros_like(wk)
    early = place.home < I2

    def piece_of(arrays, c):
        i, axis, index = PIECES[c]
        return piece(arrays[i], axis, index)

    @pl.when(place.is_l)
    def _():
        for i in range(I4):
            remote(own[i], near[i], send_sem.at[i], near_sem.at[i], place.sibling).start()

    @pl.when(is_r)
    def _():
        for k, c in enumerate(ROUND):
            @pl.when(early)
            def _(k=k, c=c):
                remote(piece_of(own, c), round_a.at[k], x_send.at[k], ra_sem.at[k], place.along_x).start()
        for c, (i, axis, index) in enumerate(PIECES):
            if c not in ROUND:
                remote(piece_of(own, c), piece_of(far, c), y_send.at[i], far_sem.at[c], place.across_other).start()
        for k, c in enumerate(ROUND):
            @pl.when(jnp.logical_not(early))
            def _(k=k, c=c):
                remote(piece_of(own, c), piece_of(far, c), x_send.at[k], far_sem.at[c], place.across_other).start()

    def load(i, refs, t, slot):
        for condition, ref in refs:
            def go(ref=ref):
                if i < I2:
                    for r in range(I2):
                        rows = pl.ds(pl.multiple_of(t * 192 + r * 96, 96), 96)
                        pltpu.make_async_copy(ref.at[rows, :], wk.at[I0, pl.ds(slot * SUB + r * 128, 96), :], load_sem.at[slot]).start()
                elif i == I2:
                    pltpu.make_async_copy(ref.at[:, lanes(t * SUB, SUB)], wn.at[slot, :, I0:SUB], load_sem.at[slot]).start()
                else:
                    rows = pl.ds(pl.multiple_of(t * SUB, SUB), SUB)
                    pltpu.make_async_copy(ref.at[rows, :], wk.at[I0, pl.ds(512 + slot * SUB, SUB), :], load_sem.at[slot]).start()
            if condition is None:
                go()
            else:
                pl.when(condition)(go)

    def loaded(i, refs, slot):
        ref = refs[I0][I1]
        if i < I2:
            pltpu.make_async_copy(ref.at[I0:192, :], wk.at[I0, I0:192, :], load_sem.at[slot]).wait()
        elif i == I2:
            pltpu.make_async_copy(ref.at[:, I0:SUB], wn.at[slot, :, I0:SUB], load_sem.at[slot]).wait()
        else:
            pltpu.make_async_copy(ref.at[I0:SUB, :], wk.at[I0, 512:768, :], load_sem.at[slot]).wait()

    def store(i, dst, t, slot):
        if i == I2:
            rows = pl.ds(pl.multiple_of(t * SUB, SUB), SUB)
            return pltpu.make_async_copy(wk.at[I1, pl.ds(slot * SUB, SUB), :], dst.at[rows, :], store_sem.at[slot])
        return pltpu.make_async_copy(wn.at[slot, :, SUB:512], dst.at[t // I4, :, lanes(t % I4 * SUB, SUB)], store_sem.at[slot])

    def keep(which, t, slot):
        return pltpu.make_async_copy(wn.at[slot, :, I0:SUB], up_chunks[which].at[t // I4, :, lanes(t % I4 * SUB, SUB)], chunk_sem.at[slot])

    def turn(i, refs, which, first, count):
        dst = turned[i][which]
        load(i, refs, first, I0)

        def step(n, c):
            slot = n % I2

            if i == I2:
                @pl.when(n > I0)
                def _():
                    keep(which, first + n - I1, I1 - slot).wait()

            @pl.when(n + I1 < count)
            def _():
                load(i, refs, first + n + I1, I1 - slot)
            loaded(i, refs, slot)
            if i == I2:
                keep(which, first + n, slot).start()

            @pl.when(n >= I2)
            def _():
                store(i, dst, first + n - I2, slot).wait()
            for b in range(I6):
                cut = slice(b * SUB, b * SUB + SUB)
                if i == I2:
                    wk[I1, pl.ds(pl.multiple_of(slot * SUB, SUB), SUB), cut] = wn[slot, cut, I0:SUB].T
                else:
                    base = I0 if i < I2 else 512
                    wn[slot, cut, SUB:512] = wk[I0, pl.ds(pl.multiple_of(base + slot * SUB, SUB), SUB), cut].T
            store(i, dst, first + n, slot).start()
            return c
        lax.fori_loop(I0, count, step, I0)
        for n in (count - I2, count - I1):
            store(i, dst, first + n, n % I2).wait()
        if i == I2:
            keep(which, first + count - I1, (count - I1) % I2).wait()

    counts = (12, I4, 12, 12)
    for i in range(I4):
        @pl.when(is_r)
        def _(i=i):
            remote(near[i], near[i], send_sem.at[i], near_sem.at[i], place.sibling).wait_recv()
        turn(i, [(place.is_l, own[i]), (is_r, near[i])], I0, I0, counts[i])
        if i < len(ROUND):
            @pl.when(place.is_l & jnp.logical_not(early))
            def _(k=i):
                remote(round_a.at[k], round_a.at[k], rs_send.at[k], ra_sem.at[k], place.sibling).wait_recv()
                remote(round_a.at[k], round_b.at[k], rs_send.at[k], rb_sem.at[k], place.across).start()
    done = [I0, I0, I0, I0]

    for c, (i, axis, index) in enumerate(PIECES):
        view = piece_of(far, c)
        for k, step in enumerate(ROUND_STEPS):
            if c == step:
                @pl.when(is_r & jnp.logical_not(early))
                def _(k=k):
                    remote(round_b.at[k], round_b.at[k], rs_send.at[k], rb_sem.at[k], place.sibling).wait_recv()
                    remote(round_b.at[k], piece_of(far, ROUND[k]), rs_send.at[k], far_sem.at[ROUND[k]], place.along_x).start()
        remote(view, view, d_send.at[i], far_sem.at[c], place.sibling).wait_recv()
        gives = is_r
        sem = d_send.at[i]
        if c in ROUND:
            gives = (early & place.is_l) | (jnp.logical_not(early) & is_r)
            sem = xd_send.at[ROUND.index(c)]

        @pl.when(gives)
        def _(c=c, view=view, sem=sem):
            remote(view, view, sem, far_sem.at[c], place.sibling).start()
        count = I4 if i < I2 else I3
        turn(i, [(None, far[i])], I1, done[i], count)
        done[i] += count

    @pl.when(place.is_l)
    def _():
        for i in range(I4):
            remote(own[i], near[i], send_sem.at[i], near_sem.at[i], place.sibling).wait_send()

    @pl.when(is_r)
    def _():
        for i in range(I4):
            part = own[i] if i < I3 else own[i].at[I0:I2 * 768, :]
            remote(part, part, y_send.at[i], far_sem.at[I0], place.across_other).wait_send()
            remote(part, part, d_send.at[i], far_sem.at[I0], place.sibling).wait_send()
        for k in range(len(ROUND)):
            remote(round_a.at[k], round_a.at[k], x_send.at[k], far_sem.at[I0], place.sibling).wait_send()

    @pl.when((early & place.is_l) | (jnp.logical_not(early) & is_r))
    def _():
        for k in range(len(ROUND)):
            remote(round_a.at[k], round_a.at[k], xd_send.at[k], far_sem.at[I0], place.sibling).wait_send()

    @pl.when(jnp.logical_not(early))
    def _():
        for k in range(len(ROUND)):
            remote(round_a.at[k], round_a.at[k], rs_send.at[k], far_sem.at[I0], place.sibling).wait_send()


def near_choices(place, own, near):
    return [(place.is_l, own), (jnp.logical_not(place.is_l), near)]


def forward_kernel(dims, x_ref, y_ref, wq, wo, wu, wd, own_gains,
                   a_s, h_s, qkv_s, u_s, g_s, oh_same, oh_other, oa_same, oa_other, og_same, og_other, loss_s, home_gains,
                   nq, no, nu, nd, fq, fo, fu, fd, tq0, to0, tu0, td0, tq1, to1, tu1, td1, uc0, uc1, round_a, round_b,
                   abuf, hbuf, obuf, nbuf, ybuf, sbuf, qkvbuf, ubuf, zbuf, ctxbuf, lossbuf, losstile, gains, wres, wores, wn,
                   send_sem, y_send, d_send, near_sem, far_sem, t_load, t_store, t_keep, ra_sem, rb_sem, x_send, xd_send, rs_send,
                   act_sem, hop_f, keep_sem, save_sem, stream_n, res_sem, out_sem, big_sem, y_sem, s_sem,
                   os_sem, oo_sem, as_sem, ao_sem, gs_sem, go_sem, bulk, gain_sem, tiny):
    micro, seq, width, heads, head_dim, ffn = dims
    place = Place()
    is_first, is_last = place.home == I0, place.home == I3
    home02 = (place.home == I0) | (place.home == I2)
    home13 = jnp.logical_not(home02)
    is_r = jnp.logical_not(place.is_l)
    takes_x = (place.home == I1) & is_r
    half = heads // I2 * HEAD_PAD
    scale = head_dim ** -0.5
    norm_factor = 1.0 / (micro * I2 * seq * width)
    own, near, far = (wq, wo, wu, wd), (nq, no, nu, nd), (fq, fo, fu, fd)
    turned = ((tq0, tq1), (to0, to1), (tu0, tu1), (td0, td1))
    entry_barrier(place)

    @pl.when(place.is_l)
    def _():
        pltpu.make_async_copy(own_gains, gains, gain_sem.at[I0]).start()
        remote(own_gains, gains, gain_sem.at[I1], gain_sem.at[I0], place.sibling).start()

    @pl.when(is_first)
    def _():
        for m in range(micro):
            pltpu.make_async_copy(x_ref.at[m, place.core], abuf.at[m], act_sem.at[m]).start()
    weight_phase(place, is_r, own, near, far, turned, (uc0, uc1), wn, wores, send_sem, y_send, d_send, near_sem, far_sem, t_load, t_store, t_keep,
                 round_a, round_b, ra_sem, rb_sem, x_send, xd_send, rs_send)
    pltpu.make_async_copy(own_gains, gains, gain_sem.at[I0]).wait()
    pltpu.make_async_copy(gains, home_gains, gain_sem.at[I0]).start()

    @pl.when(place.is_l)
    def _():
        remote(own_gains, gains, gain_sem.at[I1], gain_sem.at[I0], place.sibling).wait_send()

    def near_of(i):
        return near_choices(place, own[i], near[i])

    def saved(dst, index):
        return pltpu.make_async_copy(hbuf, dst, save_sem.at[index])

    sn = Stream(wn, stream_n, DEPTH, [([(None, tq0)], I3), ([(None, tq1)], I3), ([(None, uc0)], I3), ([(None, uc1)], I3)], micro * 12, False)
    for c, choices in enumerate((near_of(I1), [(None, fo)])):
        for condition, ref in choices:
            def go(ref=ref, c=c):
                load_heads(ref, I0, wores.at[c], out_sem.at[c])
            go() if condition is None else pl.when(condition)(go)
    sn.prime()
    load_resident(wres, res_sem, (near_of(I3), [(None, fd)]))
    lossbuf[...] = jnp.zeros_like(lossbuf)

    def qkv_out(m):
        return pltpu.make_async_copy(qkvbuf, qkv_s.at[m], big_sem.at[I0])

    def up_out(m):
        return pltpu.make_async_copy(ubuf, u_s.at[m], big_sem.at[I1])

    def act_out(m):
        return pltpu.make_async_copy(abuf.at[m], a_s.at[m], save_sem.at[I2])

    def hop_block(m, n):
        cols = lanes(n * SUB, SUB)
        return remote(obuf.at[m % I2, :, cols], abuf.at[m, :, cols], hop_f.at[m % I2], act_sem.at[m], place.chain(I1))

    def hop_forward(m):
        return remote(obuf.at[m % I2], abuf.at[m], hop_f.at[m % I2], act_sem.at[m], place.chain(I1))

    def near_hand(src, dst_far, dst_own, sem, recv_sem):
        return (lambda: remote(src, dst_far, sem, recv_sem, place.sibling)), (lambda: pltpu.make_async_copy(src, dst_own, sem))

    def hand_out(m):
        return near_hand(obuf.at[m % I2], oa_other.at[m], oa_same.at[m], keep_sem.at[m % I2], ao_sem)

    def both_kinds(condition, copies, start):
        far_copy, own_copy = copies

        @pl.when(condition & place.is_l)
        def _():
            far_copy().start() if start else far_copy().wait_send()

        @pl.when(condition & is_r)
        def _():
            own_copy().start() if start else own_copy().wait()

    def x_out(m):
        return pltpu.make_async_copy(ybuf, oa_same.at[m], y_sem), pltpu.make_async_copy(sbuf, oa_other.at[m], s_sem)

    def seed_out(m):
        return pltpu.make_async_copy(sbuf, g_s.at[m], s_sem)

    def far_mid(m, condition):
        @pl.when(condition & place.is_l)
        def _():
            remote(h_s.at[m], oh_same.at[m], bulk.at[I2], os_sem, place.across).start()

        @pl.when(condition & is_r)
        def _():
            remote(h_s.at[m], oh_other.at[m], bulk.at[I2], oo_sem, place.across_other).start()

    def send_seed(m):
        seed_out(m).wait()

        @pl.when(place.is_l & (m < EARLY_SEEDS))
        def _():
            remote(g_s.at[m], og_same.at[m], bulk.at[I1], gs_sem, place.across).start()

        @pl.when(is_r & (m < EARLY_SEEDS))
        def _():
            remote(g_s.at[m], og_other.at[m], bulk.at[I1], go_sem, place.across_other).start()

    def forward_tick(m, carry):
        act, mid, out = abuf.at[m], hbuf, obuf.at[m % I2]
        pltpu.make_async_copy(x_ref.at[m, place.core], act, act_sem.at[m]).wait()
        act_out(m).start()

        @pl.when(place.is_l)
        def _():
            pltpu.make_async_copy(act, oa_same.at[m], as_sem).start()

        @pl.when(is_last)
        def _():
            pltpu.make_async_copy(y_ref.at[m, place.core], ybuf, y_sem).start()

        @pl.when(takes_x)
        def _():
            @pl.when(m > I0)
            def _():
                for copy in x_out(m):
                    copy.wait()
            for core, buf, sem in ((place.core, ybuf, y_sem), (I1 - place.core, sbuf, s_sem)):
                pltpu.make_async_copy(x_ref.at[m, core], buf, sem).start()
        norm_rows(act, gains[I0:I1, :], nbuf, seq)

        @pl.when(m > I0)
        def _():
            qkv_out(m).wait()

        def qkv_step(j, c):
            w = sn.wait(m * 12 + j)
            for n in range(I0, CHUNK, SUB):
                qkvbuf[:, lanes(j * CHUNK + n, SUB)] = mm(nbuf[...], w[:, n:n + SUB]).astype(BF)
            sn.start(m * 12 + j + DEPTH)
            return c
        lax.fori_loop(I0, I6, qkv_step, I0)
        qkv_out(m).start()
        act_out(m).wait()

        @pl.when(is_r)
        def _():
            remote(a_s.at[m], oa_other.at[m], bulk.at[I0], ao_sem, place.sibling).start()

        def head_step(i, c):
            base = i * (I3 * half)
            views = [[qkvbuf[:, lanes(base + t * half + r * HEAD_PAD, HEAD_PAD)] for t in range(I3)] for r in range(I8)]
            for r, context in enumerate(attention_forward(views, scale)):
                ctxbuf[:, lanes(i * half + r * HEAD_PAD, HEAD_PAD)] = context
            return c
        lax.fori_loop(I0, I2, head_step, I0)

        @pl.when(m == I0)
        def _():
            for c in range(I2):
                pltpu.make_async_copy(wo, wores.at[c, I0:768, :], out_sem.at[c]).wait()
        for n in range(I0, width, SUB):
            total = mm(ctxbuf[:, I0:half], wores[I0, :, n:n + SUB]) + mm(ctxbuf[:, half:I2 * half], wores[I1, :, n:n + SUB])
            mid[:, n:n + SUB] = (act[:, n:n + SUB].astype(F32) + total).astype(BF)
        saved(h_s.at[m], I0).start()

        @pl.when(place.is_l)
        def _():
            saved(oh_same.at[m], I1).start()
        norm_rows(mid, gains[I1:I2, :], nbuf, seq)

        @pl.when(m > I0)
        def _():
            up_out(m).wait()

        def up_step(j, c):
            w = sn.wait(m * 12 + I6 + j)
            for n in range(I0, CHUNK, SUB):
                u = mm(nbuf[...], w[:, n:n + SUB]).astype(BF)
                at = lanes(j * CHUNK + n, SUB)
                ubuf[:, at] = u
                uf = u.astype(F32)
                zbuf[:, at] = (uf * gelu_gate(uf)[I0]).astype(BF)
            sn.start(m * 12 + I6 + j + DEPTH)
            return c
        lax.fori_loop(I0, I6, up_step, I0)
        up_out(m).start()

        @pl.when((m > I1) & jnp.logical_not(is_last))
        def _():
            hop_forward(m).wait_send()

        both_kinds((m > I1) & home02, hand_out(m), False)

        @pl.when(m == I0)
        def _():
            for j in range(I6):
                pltpu.make_async_copy(wd.at[I0:CHUNK, :], wres.at[j], res_sem.at[j]).wait()

        def down_step(n, c):
            cols = lanes(n * SUB, SUB)
            out[:, cols] = (mid[:, cols].astype(F32) + blocked(zbuf, wres, cols)).astype(BF)

            @pl.when((n > I0) & jnp.logical_not(is_last))
            def _():
                hop_block(m, n - I1).start()
            return c
        lax.fori_loop(I0, width // SUB, down_step, I0)

        @pl.when(jnp.logical_not(is_last))
        def _():
            hop_block(m, width // SUB - I1).start()

        both_kinds(home02, hand_out(m), True)

        @pl.when(is_last)
        def _():
            pltpu.make_async_copy(y_ref.at[m, place.core], ybuf, y_sem).wait()

            @pl.when(m > I0)
            def _():
                send_seed(m - I1)

            def seed(rows):
                error = out[rows, :].astype(F32) - ybuf[rows, :].astype(F32)
                sbuf[rows, :] = (error * norm_factor).astype(BF)
                lossbuf[...] += jnp.sum((error * error).reshape(I4, I8, width), axis=I0)
            rows_loop(seq, 32, seed)
            seed_out(m).start()

        @pl.when(takes_x)
        def _():
            for core, buf, sem in ((place.core, ybuf, y_sem), (I1 - place.core, sbuf, s_sem)):
                pltpu.make_async_copy(x_ref.at[m, core], buf, sem).wait()
            for copy in x_out(m):
                copy.start()

        saved(h_s.at[m], I0).wait()

        @pl.when(place.is_l)
        def _():
            saved(oh_same.at[m], I1).wait()

        @pl.when(is_r)
        def _():
            remote(h_s.at[m], oh_other.at[m], bulk.at[I3], oo_sem, place.sibling).start()

        far_mid(m, home13 | (m % I2 == I1))
        return carry

    @pl.when(is_first & (place.core == I0))
    def _():
        pl.delay(STAGGER_NS)
    lax.fori_loop(I0, micro, forward_tick, I0)
    for m in range(I0, micro, I2):
        far_mid(m, is_first)

    @pl.when(is_last)
    def _():
        total = lossbuf[:, I0:128]
        for n in range(128, width, 128):
            total = total + lossbuf[:, n:n + 128]
        losstile[...] = total
        pltpu.make_async_copy(losstile, loss_s, tiny).start()
    for copy in (qkv_out(micro - I1), up_out(micro - I1)):
        copy.wait()

    @pl.when(jnp.logical_not(is_last))
    def _():
        for m in (micro - I2, micro - I1):
            hop_forward(m).wait_send()
    for m in (micro - I2, micro - I1):
        both_kinds(home02, hand_out(m), False)

    @pl.when(is_last)
    def _():
        seed_out(micro - I1).wait()
        pltpu.make_async_copy(losstile, loss_s, tiny).wait()

    @pl.when(takes_x)
    def _():
        for copy in x_out(micro - I1):
            copy.wait()
    pltpu.make_async_copy(gains, home_gains, gain_sem.at[I0]).wait()
    sent, got = drain(place)

    @pl.when(place.home != I2)
    def _():
        sent(h_s, bulk.at[I2])

    @pl.when(place.home == I2)
    def _():
        sent(h_s.at[I0:micro // I2], bulk.at[I2])

    @pl.when(place.is_l | jnp.logical_not(is_last))
    def _():
        got(oh_other, oo_sem)

    @pl.when(is_r & is_last)
    def _():
        got(oh_other.at[I0:micro // I2], oo_sem)

    @pl.when(is_last)
    def _():
        sent(g_s.at[I0:EARLY_SEEDS], bulk.at[I1])

    @pl.when((place.home == I2) & is_r)
    def _():
        got(og_same.at[I0:EARLY_SEEDS], gs_sem)
        got(og_other.at[I0:EARLY_SEEDS], go_sem)

    @pl.when(is_r)
    def _():
        sent(a_s, bulk.at[I0])
        sent(h_s, bulk.at[I3])

    @pl.when(is_r & jnp.logical_not(is_last))
    def _():
        got(oh_same, os_sem)

    @pl.when(is_r & is_last)
    def _():
        got(oh_same.at[I0:micro // I2], os_sem)

    @pl.when(place.is_l)
    def _():
        got(oa_same, as_sem)

    @pl.when(place.is_l | home02)
    def _():
        got(oa_other, ao_sem)


def drain(place):
    def sent(buf, sem):
        remote(buf, buf, sem, sem, place.sibling).wait_send()

    def got(dst, sem):
        pltpu.make_async_copy(dst, dst, sem).wait()
    return sent, got


def backward_kernel(dims, a_s, h_s, qkv_s, u_s, g_s, wq, nq, fq, td0, td1, to0, to1, tu0, tu1, gains, loss_s, after, *refs):
    (dx_s, m_s, od_same, od_other, og_same, og_other, oa_same, oa_other, oh_same, oh_other, dg_same, dg_other, loss_all,
     gbuf, hbuf, obuf, qkvbuf, ubuf, habuf, zbuf, ctxbuf, dqkvbuf, acc, accg, wres, wn, wk,
     grad_sem, hop_b, back_sem, dx_sem, dx_send, save_sem, stream_n, stream_k, res_sem, load_sem,
     ds_sem, do_sem, gs_sem, go_sem, as_sem, ao_sem, os_sem, oo_sem, bulk, tiny, loss_sem, ready) = refs[I6:]
    micro, seq, width, heads, head_dim, ffn = dims
    place = Place()
    is_first, is_last = place.home == I0, place.home == I3
    home13 = (place.home == I1) | is_last
    is_r = jnp.logical_not(place.is_l)
    half = heads // I2 * HEAD_PAD
    scale = head_dim ** -0.5

    barrier = pltpu.get_barrier_semaphore()
    is_b, is_c = place.home == I1, place.home == I2
    for there in (place.sibling, place.across, place.across_other):
        pl.semaphore_signal(barrier, inc=I1, device_id=there, device_id_type=MESH)

    @pl.when(is_c)
    def _():
        pl.semaphore_signal(barrier, inc=I1, device_id=place.along_x, device_id_type=MESH)

    @pl.when(is_last)
    def _():
        for m in range(micro):
            pltpu.make_async_copy(g_s.at[m], gbuf.at[m], grad_sem.at[m]).start()
    wk[...] = jnp.zeros_like(wk)
    bn = Stream(wn, stream_n, BACK_DEPTH, [([(None, td0)], I3), ([(None, td1)], I3), ([(None, to0)], I1), ([(None, to1)], I1)], micro * I8, False)
    bk = Stream(wk, stream_k, KDEPTH, [(near_choices(place, wq, nq), I3), ([(None, fq)], I3)], micro * I6, True)
    bn.prime()
    bk.prime()
    load_resident(wres, res_sem, ([(None, tu0)], [(None, tu1)]))

    def saved(dst, index):
        return pltpu.make_async_copy(hbuf, dst, save_sem)

    def both_kinds(condition, copies, start):
        far_copy, own_copy = copies

        @pl.when(condition & place.is_l)
        def _():
            far_copy().start() if start else far_copy().wait_send()

        @pl.when(condition & is_r)
        def _():
            own_copy().start() if start else own_copy().wait()

    def near_hand(src, dst_far, dst_own, sem, recv_sem):
        return (lambda: remote(src, dst_far, sem, recv_sem, place.sibling)), (lambda: pltpu.make_async_copy(src, dst_own, sem))

    def loads(i):
        m = micro - I1 - i
        return [pltpu.make_async_copy(src.at[m], dst, load_sem.at[k])
                for k, (src, dst) in enumerate(((u_s, ubuf), (qkv_s, qkvbuf), (h_s, habuf.at[I0]), (a_s, habuf.at[I1])))]

    def load_next(i, k):
        @pl.when(i + I1 < micro)
        def _():
            loads(i + I1)[k].start()

    for copy in loads(I0):
        copy.start()
    accg[...] = jnp.zeros_like(accg)

    def norm_back(index, x, base, dst, gain_row):
        def body(rows):
            xf = x[rows, :].astype(F32)
            dy = acc[rows, :].astype(BF).astype(F32)
            inv = lax.rsqrt(jnp.mean(xf * xf, axis=-I1, keepdims=True) + NORM_EPS)
            xn = xf * inv
            accg[index] += jnp.sum((dy * xn).reshape(I4, I8, width), axis=I0)
            dyg = dy * gain_row
            dx = inv * (dyg - xn * jnp.mean(dyg * xn, axis=-I1, keepdims=True))
            dst[rows, :] = (base[rows, :].astype(F32) + dx).astype(BF)
        rows_loop(seq, 32, body)

    def hop_back(i):
        m = micro - I1 - i
        return remote(obuf.at[i % I2], gbuf.at[m], hop_b.at[i % I2], grad_sem.at[m], place.chain(-I1))

    def hand_back(i):
        m = micro - I1 - i
        return near_hand(obuf.at[i % I2], og_other.at[m], og_same.at[m], back_sem.at[i % I2], go_sem)

    def keep_dx(i):
        return pltpu.make_async_copy(obuf.at[i % I2], dx_s.at[micro - I1 - i], back_sem.at[i % I2])

    def back_ready(i):
        both_kinds((i > I1) & home13, hand_back(i), False)

        @pl.when((i > I1) & is_first)
        def _():
            keep_dx(i).wait()
            dx_to_b(i).wait_send()

        @pl.when((i > I1) & jnp.logical_not(is_first))
        def _():
            hop_back(i).wait_send()

    def pass_loss(tile):
        @pl.when(jnp.logical_not(is_first))
        def _():
            remote(tile, loss_all.at[place.core], loss_sem.at[I0], loss_sem.at[I1], place.chain(-I1)).start()
        remote(tile, loss_all.at[place.core], loss_sem.at[I2], loss_sem.at[I3], place.sibling).start()

    def dx_to_b(i):
        return remote(obuf.at[i % I2], dx_s.at[micro - I1 - i], dx_send.at[i % I2], dx_sem, place.across)

    def backward_tick(i, carry):
        m = micro - I1 - i
        slot = i % I2
        grad, dmid, prev = gbuf.at[m], hbuf, obuf.at[slot]
        u_now, qkv_now, h_now, a_now = ubuf, qkvbuf, habuf.at[I0], habuf.at[I1]

        pltpu.make_async_copy(g_s.at[m], grad, grad_sem.at[m]).wait()

        @pl.when(place.is_l)
        def _():
            pltpu.make_async_copy(grad, og_same.at[m], gs_sem).start()
        load_u, load_qkv, load_h, load_a = loads(i)
        load_u.wait()

        def mlp_step(j, c):
            w = bn.wait(i * I8 + j)
            for n in range(I0, CHUNK, SUB):
                at = lanes(j * CHUNK + n, SUB)
                dz = mm(grad[...], w[:, n:n + SUB]).astype(BF).astype(F32)
                u = u_now[:, at].astype(F32)
                gate, u2 = gelu_gate(u)
                zbuf[:, at] = (dz * gelu_slope(u * gate, gate, u2)).astype(BF)
            bn.start(i * I8 + j + BACK_DEPTH)
            return c
        lax.fori_loop(I0, I6, mlp_step, I0)

        @pl.when(i == I0)
        def _():
            for j in range(I6):
                pltpu.make_async_copy(tu0.at[I0:CHUNK, :], wres.at[j], res_sem.at[j]).wait()

        def turn_back(n, c):
            cols = lanes(n * SUB, SUB)
            acc[:, cols] = blocked(zbuf, wres, cols)
            return c
        lax.fori_loop(I0, width // SUB, turn_back, I0)
        load_next(i, I0)
        load_h.wait()
        norm_back(I1, h_now, grad, dmid, gains[I1:I2, :])
        load_next(i, I2)

        @pl.when(place.is_l)
        def _():
            saved(od_same.at[m], I0).start()

        @pl.when(is_r)
        def _():
            saved(m_s.at[m], I0).start()
        for c in range(I2):
            w = bn.wait(i * I8 + I6 + c)
            for n in range(I0, CHUNK, SUB):
                ctxbuf[:, c * CHUNK + n:c * CHUNK + n + SUB] = mm(dmid[...], w[:, n:n + SUB]).astype(BF)
            bn.start(i * I8 + I6 + c + BACK_DEPTH)
        load_qkv.wait()

        def head_step(t, c):
            base = (t // I2) * (I3 * half) + (t % I2) * (I4 * HEAD_PAD)
            at = [[lanes(base + part * half + r * HEAD_PAD, HEAD_PAD) for part in range(I3)] for r in range(I4)]
            group = [(*(qkv_now[:, p] for p in at[r]), ctxbuf[:, lanes((t * I4 + r) * HEAD_PAD, HEAD_PAD)]) for r in range(I4)]
            for r, grads in enumerate(attention_backward(group, scale)):
                for p, value in zip(at[r], grads):
                    dqkvbuf[:, p] = value
            return c
        lax.fori_loop(I0, heads // I4, head_step, I0)
        load_next(i, I1)
        acc[...] = jnp.zeros_like(acc)

        def qkv_step(j, c):
            w = bk.wait(i * I6 + j)
            for n in range(I0, width, SUB):
                acc[:, n:n + SUB] += mm(dqkvbuf[:, lanes(j * CHUNK, CHUNK)], w[:, n:n + SUB])
            bk.start(i * I6 + j + KDEPTH)
            return c
        lax.fori_loop(I0, I6, qkv_step, I0)
        load_a.wait()
        back_ready(i)
        norm_back(I0, a_now, dmid, prev, gains[I0:I1, :])
        load_next(i, I3)

        @pl.when(i == I0)
        def _():
            @pl.when(is_first | is_last)
            def _():
                pl.semaphore_wait(barrier, I3)

            @pl.when(is_c)
            def _():
                pl.semaphore_wait(ready, I1)

            @pl.when(is_last)
            def _():
                pass_loss(loss_s)

        @pl.when(jnp.logical_not(is_first))
        def _():
            hop_back(i).start()

        @pl.when(is_first)
        def _():
            keep_dx(i).start()
            dx_to_b(i).start()
        both_kinds(home13, hand_back(i), True)

        @pl.when(place.is_l)
        def _():
            saved(od_same.at[m], I0).wait()
            remote(od_same.at[m], od_same.at[m], bulk.at[I6], ds_sem, place.across).start()

        @pl.when(is_r)
        def _():
            remote(grad, og_other.at[m], bulk.at[5], go_sem, place.sibling).start()
            saved(m_s.at[m], I0).wait()
            remote(m_s.at[m], od_other.at[m], bulk.at[I6], do_sem, place.sibling).start()
            remote(m_s.at[m], od_other.at[m], bulk.at[7], do_sem, place.across_other).start()

        now = (i % I2 == I1) & (i < I2 * EARLY_G)
        far_grad(m, (place.home == I1) & now)
        far_grad(micro - I1 - i // I2, is_last & now)
        return carry

    def far_grad(m, condition):
        @pl.when(condition & place.is_l)
        def _():
            remote(gbuf.at[m], og_same.at[m], bulk.at[I4], gs_sem, place.across).start()

        @pl.when(condition & is_r)
        def _():
            remote(gbuf.at[m], og_other.at[m], bulk.at[I4], go_sem, place.across_other).start()

    @pl.when(is_b | is_c)
    def _():
        pl.semaphore_wait(barrier, 5 - place.home)

    @pl.when(is_b)
    def _():
        pl.semaphore_signal(ready, inc=I1, device_id=place.along_x, device_id_type=MESH)

    @pl.when(is_c & place.is_l)
    def _():
        for t in range(micro):
            remote(a_s.at[t], oa_same.at[t], bulk.at[I8], as_sem, place.across).start()
        for t in range(I0, micro, I2):
            remote(h_s.at[t], oh_same.at[t], bulk.at[9], os_sem, place.across).start()

    @pl.when(is_c & is_r)
    def _():
        for t in range(micro):
            remote(a_s.at[t], oa_other.at[t], bulk.at[I8], ao_sem, place.across_other).start()
        for t in range(I0, micro, I2):
            remote(h_s.at[t], oh_other.at[t], bulk.at[9], oo_sem, place.across_other).start()
    lax.fori_loop(I0, micro, backward_tick, I0)
    loss_mine = loss_all.at[place.core]

    @pl.when(is_last)
    def _():
        own_loss = pltpu.make_async_copy(loss_s, loss_mine, loss_sem.at[I1])
        own_loss.start()
        own_loss.wait()

    @pl.when(jnp.logical_not(is_last))
    def _():
        remote(loss_mine, loss_mine, loss_sem.at[I0], loss_sem.at[I1], place.sibling).wait_recv()
        pass_loss(loss_mine)

    @pl.when(place.is_l)
    def _():
        pltpu.make_async_copy(accg, dg_same, tiny.at[I0]).start()
        remote(accg, dg_same, tiny.at[I1], tiny.at[I0], place.across).start()

    @pl.when(is_r)
    def _():
        remote(accg, dg_other, tiny.at[I1], tiny.at[I4], place.sibling).start()
        remote(accg, dg_other, tiny.at[I2], tiny.at[I4], place.across_other).start()

    for i in (micro - I2, micro - I1):
        back_ready(jnp.int32(i))

    sent, got = drain(place)
    sent(m_s, bulk.at[I6])

    @pl.when(is_r)
    def _():
        sent(gbuf, bulk.at[5])
        sent(m_s, bulk.at[7])
        remote(accg, dg_other, tiny.at[I2], tiny.at[I4], place.sibling).wait_send()

    @pl.when(home13)
    def _():
        sent(gbuf.at[I0:EARLY_G], bulk.at[I4])

    @pl.when(place.home == I1)
    def _():
        got(dx_s, dx_sem)

    @pl.when(jnp.logical_not(is_first))
    def _():
        remote(loss_mine, loss_mine, loss_sem.at[I0], loss_sem.at[I1], place.sibling).wait_send()
    remote(loss_mine, loss_mine, loss_sem.at[I2], loss_sem.at[I3], place.sibling).wait_send()
    remote(loss_mine, loss_mine, loss_sem.at[I2], loss_sem.at[I3], place.sibling).wait_recv()

    @pl.when(place.home == I2)
    def _():
        sent(a_s, bulk.at[I8])
        sent(h_s.at[I0:micro // I2], bulk.at[9])

    remote(accg, dg_other, tiny.at[I1], tiny.at[I4], place.sibling).wait_send()
    got(od_other, do_sem)

    @pl.when(place.is_l | home13)
    def _():
        got(og_other, go_sem)

    @pl.when(jnp.logical_not(home13) & is_r)
    def _():
        got(og_same.at[I0:EARLY_G], gs_sem)
        got(og_other.at[I0:EARLY_G], go_sem)
    got(dg_same, tiny.at[I0])
    got(dg_other, tiny.at[I4])

    @pl.when(is_r)
    def _():
        got(od_same, ds_sem)

    @pl.when(place.is_l)
    def _():
        got(og_same, gs_sem)

    @pl.when(is_last & is_r)
    def _():
        got(oa_same, as_sem)
        got(oa_other, ao_sem)
        got(oh_same.at[I0:micro // I2], os_sem)
        got(oh_other.at[I0:micro // I2], oo_sem)


def shapes(*dims_list):
    return [jax.ShapeDtypeStruct(d, BF) for d in dims_list]


def forward_phase(dims, x, y, own, own_gains):
    micro, seq, width, heads, head_dim, ffn = dims
    half = heads // I2 * HEAD_PAD
    act = (micro, seq, width)
    raw = [w.shape for w in own]
    turned = [(I3, width, CHUNK), (I1, width, CHUNK), (ffn // I2, width), (I3, width, CHUNK)]
    out_shape = shapes(act, act, (micro, seq, I6 * half), (micro, seq, ffn), *[act] * 7)
    out_shape += [jax.ShapeDtypeStruct(s, F32) for s in ((I8, 128), own_gains.shape)]
    out_shape += shapes(*raw, *raw, *turned, *turned, turned[I0], turned[I0], *[(len(ROUND), 768, width)] * I2)
    any_spec = pl.BlockSpec(memory_space=ANY)
    vmem, dma = pltpu.VMEM, pltpu.SemaphoreType.DMA
    row = vmem((seq, width), BF)
    scratch = [
        vmem(act, BF), row, vmem((I2, seq, width), BF), row, row, row, vmem((seq, I6 * half), BF), vmem((seq, ffn), BF), vmem((seq, ffn), BF),
        vmem((seq, I2 * half), BF), vmem((I8, width), F32), vmem((I8, 128), F32), vmem((I2, width), F32),
        vmem((I6, CHUNK, width), BF), vmem((I2, CHUNK, width), BF), vmem((DEPTH, width, CHUNK), BF),
        dma((I4,)), dma((I4,)), dma((I4,)), dma((I4,)), dma((12,)), dma((I2,)), dma((I2,)), dma((I2,)), *[dma((len(ROUND),))] * 5,
        dma((micro,)), dma((I2,)), dma((I2,)), dma((I3,)), dma((DEPTH,)), dma((I6,)), dma((I2,)), dma((I2,)), dma(()), dma(()),
        dma(()), dma(()), dma(()), dma(()), dma(()), dma(()), dma((I4,)), dma((I2,)), dma(()),
    ]
    return pl.pallas_call(
        functools.partial(forward_kernel, dims),
        out_shape=tuple(out_shape),
        in_specs=[any_spec] * I6 + [pl.BlockSpec(memory_space=vmem)],
        out_specs=(any_spec,) * len(out_shape),
        scratch_shapes=scratch,
        compiler_params=pltpu.CompilerParams(collective_id=I0, has_side_effects=True, vmem_limit_bytes=VMEM_LIMIT),
        name='forward_phase',
    )(x, y, *own, own_gains)


def backward_phase(dims, saved, weights, gains, loss, after, placed):
    micro, seq, width, heads, head_dim, ffn = dims
    half = heads // I2 * HEAD_PAD
    act = (micro, seq, width)
    out_shape = shapes(*[act] * 10) + [jax.ShapeDtypeStruct((I2, I8, width), F32)] * I2 + [jax.ShapeDtypeStruct((I2, I8, 128), F32)]
    any_spec = pl.BlockSpec(memory_space=ANY)
    vmem, dma = pltpu.VMEM, pltpu.SemaphoreType.DMA
    scratch = [
        vmem(act, BF), vmem((seq, width), BF), vmem((I2, seq, width), BF), vmem((seq, I6 * half), BF), vmem((seq, ffn), BF),
        vmem((I2, seq, width), BF), vmem((seq, ffn), BF), vmem((seq, I2 * half), BF), vmem((seq, I6 * half), BF), vmem((seq, width), F32),
        vmem((I2, I8, width), F32), vmem((I6, CHUNK, width), BF), vmem((BACK_DEPTH, width, CHUNK), BF), vmem((KDEPTH, CHUNK, width), BF),
        dma((micro,)), dma((I2,)), dma((I2,)), dma(()), dma((I2,)), dma(()), dma((BACK_DEPTH,)), dma((KDEPTH,)), dma((I6,)), dma((I4,)),
        *[dma(())] * I8, dma((10,)), dma((5,)), dma((I4,)), pltpu.SemaphoreType.REGULAR,
    ]
    return pl.pallas_call(
        functools.partial(backward_kernel, dims),
        out_shape=tuple(out_shape),
        in_specs=[any_spec] * 14 + [pl.BlockSpec(memory_space=vmem)] * I2 + [any_spec] * 7,
        out_specs=(any_spec,) * len(out_shape),
        scratch_shapes=scratch,
        input_output_aliases={17 + i: I4 + i for i in range(I6)},
        compiler_params=pltpu.CompilerParams(collective_id=I1, has_side_effects=True, vmem_limit_bytes=VMEM_LIMIT),
        name='backward_phase',
    )(*saved, *weights, gains, loss, after, *placed)


def recompute_kernel(dims, early, h_same, h_other, a_same, a_other, gains, wq, wu, *refs):
    (done, u_o, qkv_o, ctx_o, n1_o, n2_o), (wqbuf, wubuf, count, sem) = refs[-10:-I4], refs[-I4:]
    micro, seq, width, heads, head_dim, ffn = dims
    place = Place()
    scale = head_dim ** -0.5
    half = heads // I2 * HEAD_PAD
    steps = I2 * micro * seq // BLOCK

    def body(hs, ho, rs, ro, u, qkv, ctx, n1, n2):
        step = count[I0]
        count[I0] = step + I1
        for low, high, gain, dst in ((hs, ho, gains[I1:I2, :], n2), (rs, ro, gains[I0:I1, :], n1)):
            @pl.when(step < steps // I2)
            def _(low=low, gain=gain, dst=dst):
                norm_rows(low, gain, dst, BLOCK)

            @pl.when(step >= steps // I2)
            def _(high=high, gain=gain, dst=dst):
                norm_rows(high, gain, dst, BLOCK)

        def qkv_step(j, c):
            rows = pl.ds(pl.multiple_of(j * SUB, SUB), SUB)
            qkv[:, lanes(j * SUB, SUB)] = mm_nt(n1[...], wqbuf[rows, :]).astype(BF)
            u[:, lanes(j * SUB, SUB)] = mm(n2[...], wubuf[:, lanes(j * SUB, SUB)]).astype(BF)
            return c
        lax.fori_loop(I0, I3 * half // SUB, qkv_step, I0)

        def head_step(j, c):
            at = [(pl.ds(s, seq), r * HEAD_PAD) for s in range(I0, BLOCK, seq) for r in range(I4)]
            base = j * (I4 * HEAD_PAD)
            views = [[qkv[rows, lanes(base + t * half + col, HEAD_PAD)] for t in range(I3)] for rows, col in at]
            for (rows, col), context in zip(at, attention_forward(views, scale)):
                ctx[rows, lanes(base + col, HEAD_PAD)] = context
            return c
        lax.fori_loop(I0, I2, head_step, I0)

    @pl.when(place.home < I2 if early else place.home > I1)
    def _():
        wqbuf[...] = jnp.zeros_like(wqbuf)
        for t in range(I3):
            load_heads(wq, t, wqbuf.at[pl.ds(t * CHUNK, CHUNK)], sem.at[I0])
        up = pltpu.make_async_copy(wu, wubuf, sem.at[I1])
        up.start()
        up.wait()
        pltpu.make_async_copy(wq, wqbuf.at[I0:wq.shape[I0]], sem.at[I0]).wait()
        count[I0] = I0
        low = pl.BlockSpec((BLOCK, width), lambda i: (jnp.minimum(i, steps // I2 - I1), I0))
        high = pl.BlockSpec((BLOCK, width), lambda i: (jnp.maximum(i - steps // I2, I0), I0))
        block = lambda n: pl.BlockSpec((BLOCK, n), lambda i: (i, I0))
        pltpu.emit_pipeline(body, grid=(steps,), in_specs=[low, high, low, high],
                            out_specs=[block(ffn // I2), block(I3 * half), block(half), block(width), block(width)])(
            h_same, h_other, a_same, a_other, u_o, qkv_o, ctx_o, n1_o, n2_o)


def owner_recompute(dims, early, again, h_rows, a_rows, gains, own):
    micro, seq, width, heads, head_dim, ffn = dims
    half = heads // I2 * HEAD_PAD
    tokens = I2 * micro * seq
    any_spec = pl.BlockSpec(memory_space=ANY)
    vmem = pltpu.VMEM
    earlier = () if early else tuple(again)
    return pl.pallas_call(
        functools.partial(recompute_kernel, dims, early),
        out_shape=(jax.ShapeDtypeStruct((I8, 128), F32), *shapes((tokens, ffn // I2), (tokens, I3 * half), (tokens, half), (tokens, width), (tokens, width))),
        in_specs=[any_spec] * I4 + [pl.BlockSpec(memory_space=vmem)] + [any_spec] * (I2 + len(earlier)),
        out_specs=(any_spec,) * I6,
        scratch_shapes=[vmem((I3 * half, width), BF), vmem((width, ffn // I2), BF), pltpu.SMEM((I1,), jnp.int32), pltpu.SemaphoreType.DMA((I2,))],
        input_output_aliases={7 + i: I1 + i for i in range(len(earlier))},
        compiler_params=pltpu.CompilerParams(has_side_effects=True, vmem_limit_bytes=VMEM_LIMIT),
        name='owner_recompute',
    )(*h_rows, *a_rows, gains, own[I0], own[I2], *earlier)


def spread_dx(step, last, dx, d_in, og_same, og_other, bounce, here_sem, parent_sem, sib_sem, send_sems, og_sems):
    place = Place()
    micro = dx.shape[I0]
    along_x = place.at(place.tp, (place.stage + I2) % I4)
    barrier = pltpu.get_barrier_semaphore()
    is_leaf = place.home > I1
    gives_g = (place.home == I1) & place.is_l
    takes_g = (place.home == I0) & jnp.logical_not(place.is_l)
    late = [micro - I1 - i for i in range(micro) if i % I2 == I0 or i > I2 * EARLY_G]

    def block(m):
        return d_in.at[m, place.core]

    def to_sibling(m, src):
        remote(src, block(m), send_sems.at[I0], sib_sem, place.sibling).start()

    def tell(there):
        pl.semaphore_signal(barrier, inc=I1, device_id=there, device_id_type=MESH)

    @pl.when(step == I0)
    def _():
        tell(place.sibling)

        @pl.when(is_leaf)
        def _():
            tell(along_x)

        @pl.when(takes_g)
        def _():
            tell(place.across)

    @pl.when((step == I1) & jnp.logical_not(is_leaf))
    def _():
        pl.semaphore_wait(barrier, I2 + gives_g.astype(jnp.int32))

        @pl.when(gives_g)
        def _():
            for t, og in enumerate((og_same, og_other)):
                for m in late:
                    remote(og.at[m], og.at[m], og_sems.at[t], og_sems.at[I2 + t], place.across).start()
        for m in reversed(range(micro)):
            remote(dx.at[m], block(m), send_sems.at[I1], parent_sem.at[m], along_x).start()
            to_sibling(m, dx.at[m])
        pltpu.make_async_copy(dx, bounce, here_sem).start()

    @pl.when((step == I2) & jnp.logical_not(is_leaf))
    def _():
        pltpu.make_async_copy(dx, bounce, here_sem).wait()
        for m in range(micro):
            pltpu.make_async_copy(bounce.at[m], block(m), here_sem).start()

    @pl.when((step == (last + I1) // I2) & takes_g)
    def _():
        for t, og in enumerate((og_same, og_other)):
            part = og.at[I0:len(late)]
            remote(part, part, og_sems.at[t], og_sems.at[I2 + t], place.across).wait_recv()

    @pl.when((step == last) & is_leaf)
    def _():
        pl.semaphore_wait(barrier, I1)
        for m in reversed(range(micro)):
            remote(block(m), block(m), send_sems.at[I0], parent_sem.at[m], place.sibling).wait_recv()
            to_sibling(m, block(m))

    @pl.when(step == last)
    def _():
        remote(dx, dx, send_sems.at[I0], sib_sem, place.sibling).wait_send()

        @pl.when(jnp.logical_not(is_leaf))
        def _():
            remote(dx, dx, send_sems.at[I1], sib_sem, place.sibling).wait_send()
            pltpu.make_async_copy(dx, dx, here_sem).wait()

        @pl.when(gives_g)
        def _():
            for t, og in enumerate((og_same, og_other)):
                part = og.at[I0:len(late)]
                remote(part, part, og_sems.at[t], og_sems.at[I2 + t], place.across).wait_send()
        remote(dx, dx, send_sems.at[I0], sib_sem, place.sibling).wait_recv()


def owner_backward_kernel(dims, dx, ds, do, u, qkv, wo, wd, gs_in, go_in, dqkv, dup, z, d_in, og_same, og_other,
                          dmid, gbuf, dctx, wobuf, bounce, sem, g_sem, here_sem, parent_sem, sib_sem, send_sems, og_sems):
    micro, seq, width, heads, head_dim, ffn = dims
    half = heads // I2 * HEAD_PAD
    scale = head_dim ** -0.5
    step, steps = pl.program_id(I0), pl.num_programs(I0)
    blocks = steps // I2
    spread_dx(step, steps - I1, dx, d_in, og_same, og_other, bounce, here_sem, parent_sem, sib_sem, send_sems, og_sems)

    @pl.when(step == I0)
    def _():
        wobuf[...] = jnp.zeros_like(wobuf)
        load_heads(wo, I0, wobuf, sem)
        pltpu.make_async_copy(wo, wobuf.at[I0:wo.shape[I0]], sem).wait()

    def g_load(n, start):
        rows = BLOCK // seq
        for og, low in ((og_same, I0), (og_other, blocks // I2)):
            @pl.when((n >= low) & (n < low + blocks // I2))
            def _(og=og, low=low):
                copy = pltpu.make_async_copy(og.at[pl.ds((n - low) * rows, rows)], gbuf.at[n % I2], g_sem.at[n % I2])
                copy.start() if start else copy.wait()

    @pl.when(step < blocks)
    def _():
        @pl.when(step < blocks // I2)
        def _():
            dmid[...] = ds[...]

        @pl.when(step >= blocks // I2)
        def _():
            dmid[...] = do[...]

        def ctx_step(j, c):
            rows = pl.ds(pl.multiple_of(j * SUB, SUB), SUB)
            dctx[:, lanes(j * SUB, SUB)] = mm_nt(dmid[...], wobuf[rows, :]).astype(BF)
            return c
        lax.fori_loop(I0, half // SUB, ctx_step, I0)

        def head_step(j, c):
            base = j * (I2 * HEAD_PAD)
            at = [(pl.ds(s, seq), base + r * HEAD_PAD) for s in range(I0, BLOCK, seq) for r in range(I2)]
            group = [(*(qkv[rows, lanes(t * half + col, HEAD_PAD)] for t in range(I3)), dctx[rows, lanes(col, HEAD_PAD)]) for rows, col in at]
            for (rows, col), grads in zip(at, attention_backward(group, scale)):
                for t, value in enumerate(grads):
                    dqkv[rows, lanes(t * half + col, HEAD_PAD)] = value
            return c
        lax.fori_loop(I0, heads // I4, head_step, I0)

    @pl.when(step == blocks)
    def _():
        g_load(step - blocks, True)

    @pl.when(step >= blocks)
    def _():
        n = step - blocks
        g_load(n + I1, True)
        g_load(n, False)
        grad = gbuf.at[n % I2]

        def mlp_step(j, c):
            rows = pl.ds(pl.multiple_of(j * SUB, SUB), SUB)
            cols = lanes(j * SUB, SUB)
            dz = mm_nt(grad[...].reshape(BLOCK, width), wd[rows, :]).astype(BF).astype(F32)
            up = u[:, cols].astype(F32)
            gate, up2 = gelu_gate(up)
            hidden = up * gate
            z[:, cols] = hidden.astype(BF)
            dup[:, cols] = (dz * gelu_slope(hidden, gate, up2)).astype(BF)
            return c
        lax.fori_loop(I0, ffn // I2 // SUB, mlp_step, I0)


def owner_backward(dims, dx, d_rows, og, ups, qkv, own):
    micro, seq, width, heads, head_dim, ffn = dims
    half = heads // I2 * HEAD_PAD
    tokens = I2 * micro * seq
    blocks = tokens // BLOCK
    vmem, dma = pltpu.VMEM, pltpu.SemaphoreType.DMA
    any_spec = pl.BlockSpec(memory_space=ANY)
    first = lambda i: jnp.minimum(i, blocks - I1)
    second = lambda i: jnp.maximum(i - blocks, I0)
    low = pl.BlockSpec((BLOCK, width), lambda i: (jnp.minimum(i, blocks // I2 - I1), I0))
    high = pl.BlockSpec((BLOCK, width), lambda i: (jnp.maximum(first(i) - blocks // I2, I0), I0))
    attn_block = pl.BlockSpec((BLOCK, I3 * half), lambda i: (first(i), I0))
    mlp_block = pl.BlockSpec((BLOCK, ffn // I2), lambda i: (second(i), I0))
    act = (micro, seq, width)
    return pl.pallas_call(
        functools.partial(owner_backward_kernel, dims),
        grid=(I2 * blocks,),
        out_shape=tuple(shapes((tokens, I3 * half), (tokens, ffn // I2), (tokens, ffn // I2), (micro, I2, seq, width), act, act)),
        in_specs=[any_spec, low, high, mlp_block, attn_block, any_spec, pl.BlockSpec((ffn // I2, width), lambda i: (I0, I0)), any_spec, any_spec],
        out_specs=(attn_block, mlp_block, mlp_block, any_spec, any_spec, any_spec),
        scratch_shapes=[vmem((BLOCK, width), BF), vmem((I2, BLOCK // seq, seq, width), BF), vmem((BLOCK, half), BF), vmem((half, width), BF), vmem(act, BF),
                        dma(()), dma((I2,)), dma(()), dma((micro,)), dma(()), dma((I2,)), dma((I4,))],
        input_output_aliases={7: I4, I8: 5},
        compiler_params=pltpu.CompilerParams(collective_id=I2, has_side_effects=True, vmem_limit_bytes=VMEM_LIMIT),
        name='owner_backward',
    )(dx, *d_rows, ups, qkv, own[I1], own[I3], *og)


def bring(pairs, sem):
    copies = [pltpu.make_async_copy(src, dst, sem.at[i]) for i, (src, dst) in enumerate(pairs)]
    for copy in copies:
        copy.start()
    for copy in copies:
        copy.wait()


def attn_products_kernel(dq, dk, dv, ctx, n1_o, ds, do, dx_in, dwq, dwo, dx_out, n1, dmid, dqkvt, ctxt, bounce, sem, dx_sem):
    tokens, width = n1.shape
    part = tokens // I2
    head_dim = dwo.shape[I1]
    step, last = pl.program_id(I0), pl.num_programs(I0) - I1
    into, out_of = pltpu.make_async_copy(dx_in, bounce, dx_sem), pltpu.make_async_copy(bounce, dx_out, dx_sem)

    @pl.when(step == I1)
    def _():
        into.start()

    @pl.when(step == I2)
    def _():
        into.wait()
        out_of.start()

    @pl.when(step == last)
    def _():
        out_of.wait()

    @pl.when(step == I0)
    def _():
        bring([(n1_o, n1), (ds, dmid.at[pl.ds(I0, part)]), (do, dmid.at[pl.ds(part, part)])], sem)

    def turn(rows):
        for t, block in enumerate((dq, dk, dv)):
            for r in range(I2):
                at = (I2 * t + r) * head_dim
                dqkvt[at:at + head_dim, rows] = block[rows, r * HEAD_PAD:(r + I1) * HEAD_PAD].T[I0:head_dim]
        for r in range(I2):
            ctxt[r * head_dim:(r + I1) * head_dim, rows] = ctx[rows, r * HEAD_PAD:(r + I1) * HEAD_PAD].T[I0:head_dim]
    rows_loop(tokens, SUB, turn)
    for c in range(I0, width, SUB):
        cut = slice(c, c + SUB)
        dwq[:, :, :, cut] = mm(dqkvt[...], n1[:, cut]).reshape(I3, I2, head_dim, SUB)
        dwo[:, :, cut] = mm(ctxt[...], dmid[:, cut]).reshape(I2, head_dim, SUB)


def attn_products(dqkv, ctx, n1, d_rows, dx, out_dims):
    heads, head_dim, width = out_dims
    tokens = n1.shape[I0]
    vmem = pltpu.VMEM
    any_spec = pl.BlockSpec(memory_space=ANY)
    pairs = heads // I2
    cols = lambda t: pl.BlockSpec((tokens, I2 * HEAD_PAD), lambda i: (I0, t * pairs + i))
    return pl.pallas_call(
        attn_products_kernel,
        grid=(pairs,),
        out_shape=(jax.ShapeDtypeStruct((I3,) + out_dims, F32), jax.ShapeDtypeStruct(out_dims, F32), jax.ShapeDtypeStruct(dx.shape, BF)),
        in_specs=[cols(I0), cols(I1), cols(I2), cols(I0), any_spec, any_spec, any_spec, any_spec],
        out_specs=(pl.BlockSpec((I3, I2, head_dim, width), lambda i: (I0, i, I0, I0)), pl.BlockSpec((I2, head_dim, width), lambda i: (i, I0, I0)), any_spec),
        scratch_shapes=[vmem((tokens, width), BF), vmem((tokens, width), BF), vmem((I6 * head_dim, tokens), BF), vmem((I2 * head_dim, tokens), BF),
                        vmem(dx.shape, BF), pltpu.SemaphoreType.DMA((I3,)), pltpu.SemaphoreType.DMA(())],
        compiler_params=pltpu.CompilerParams(vmem_limit_bytes=VMEM_LIMIT),
        name='attn_products',
    )(dqkv, dqkv, dqkv, ctx, n1, *d_rows, dx)


def mlp_products_kernel(dup, z, n2_o, gs, go, dwu, dwd, n2t, grad, zt, stage, sem):
    width, tokens = n2t.shape
    part = tokens // I2

    @pl.when(pl.program_id(I0) == I0)
    def _():
        bring([(n2_o, stage), (gs, grad.at[pl.ds(I0, part)]), (go, grad.at[pl.ds(part, part)])], sem)

        def turn(rows):
            for c in range(I0, width, SUB):
                n2t[c:c + SUB, rows] = stage[rows, c:c + SUB].T
        rows_loop(tokens, SUB, turn)

    def turn_z(rows):
        for c in range(I0, z.shape[I1], SUB):
            zt[c:c + SUB, rows] = z[rows, c:c + SUB].T
    rows_loop(tokens, SUB, turn_z)
    for c in range(I0, width, I2 * SUB):
        dwu[c:c + I2 * SUB, :] = mm(n2t[c:c + I2 * SUB, :], dup[...])
    for c in range(I0, width, SUB):
        dwd[:, c:c + SUB] = mm(zt[...], grad[:, c:c + SUB])


def mlp_products(dup, hidden, n2, g_rows):
    tokens, width = n2.shape
    cols = dup.shape[I1]
    vmem = pltpu.VMEM
    any_spec = pl.BlockSpec(memory_space=ANY)
    block = pl.BlockSpec((tokens, SUB), lambda i: (I0, i))
    return pl.pallas_call(
        mlp_products_kernel,
        grid=(cols // SUB,),
        out_shape=(jax.ShapeDtypeStruct((width, cols), F32), jax.ShapeDtypeStruct((cols, width), F32)),
        in_specs=[block, block, any_spec, any_spec, any_spec],
        out_specs=(pl.BlockSpec((width, SUB), lambda i: (I0, i)), pl.BlockSpec((SUB, width), lambda i: (i, I0))),
        scratch_shapes=[vmem((width, tokens), BF), vmem((tokens, width), BF), vmem((SUB, tokens), BF), vmem((tokens, width), BF), pltpu.SemaphoreType.DMA((I3,))],
        compiler_params=pltpu.CompilerParams(vmem_limit_bytes=VMEM_LIMIT),
        name='mlp_products',
    )(dup, hidden, n2, *g_rows)


def solution(mesh):
    act_spec = P('rep', None, None, None)
    weight_specs = (
        P(('rep', 'stage'), None, None, 'tp', None),
        P(('rep', 'stage'), 'tp', None, None),
        P(('rep', 'stage'), None, 'tp'),
        P(('rep', 'stage'), 'tp', None),
        P(('rep', 'stage'), None),
        P(('rep', 'stage'), None),
    )

    def device_fn(inputs, targets, w_qkv, w_out, w_up, w_down, gain_attn, gain_mlp):
        micro_count, _, seq_len, width = inputs.shape
        dims = (micro_count, seq_len, width, I2 * w_out.shape[I1], w_out.shape[I2], I2 * w_up.shape[I2])
        norm_factor = 1.0 / (inputs.size)
        own = (w_qkv[I0], w_out[I0], w_up[I0], w_down[I0])
        own_gains = jnp.concatenate([gain_attn, gain_mlp]).astype(F32)
        rows_of = (own[I0].transpose(I1, I2, I3, I0).reshape(-I1, width), own[I1].reshape(-I1, width), own[I2], own[I3])

        (acts, mids, qkv, ups, seeds, oh_same, oh_other, oa_same, oa_other, og_same, og_other, loss_tile, home_gains, *weights) = forward_phase(dims, inputs, targets, rows_of, own_gains)
        (nq, no, nu, nd), (fq, fo, fu, fd) = weights[I0:I4], weights[I4:I8]
        (tq0, to0, tu0, td0), (tq1, to1, tu1, td1) = weights[I8:12], weights[12:16]

        flat = lambda *rows: [r.reshape(-I1, width) for r in rows]
        done, *again = owner_recompute(dims, True, None, flat(oh_same, oh_other), flat(oa_same, oa_other), own_gains, rows_of)
        dx, _, od_same, od_other, og_same, og_other, oa_same, oa_other, oh_same, oh_other, dg_same, dg_other, loss_all = backward_phase(
            dims, (acts, mids, qkv, ups, seeds), (rows_of[I0], nq, fq, td0, td1, to0, to1, tu0, tu1), home_gains, loss_tile, done,
            (og_same, og_other, oa_same, oa_other, oh_same, oh_other))
        _, *again = owner_recompute(dims, False, again, flat(oh_same, oh_other), flat(oa_same, oa_other), own_gains, rows_of)
        ups_own, qkv_own, ctx_own, n1, n2 = again
        d_rows = flat(od_same, od_other)
        d_qkv_rows, d_up_rows, hidden, dx_all, og_same, og_other = owner_backward(dims, dx, d_rows, (og_same, og_other), ups_own, qkv_own, rows_of)
        d_qkv, d_out, d_inputs = attn_products(d_qkv_rows, ctx_own, n1, d_rows, dx_all, w_out.shape[I1:])
        d_up, d_down = mlp_products(d_up_rows, hidden, n2, flat(og_same, og_other))
        weight_grads = (d_qkv.transpose(I3, I0, I1, I2), d_out, d_up, d_down)
        mine = jnp.sum(dg_same + dg_other, I1)
        loss = jnp.sum(loss_all) * (0.5 * norm_factor)

        return (loss.reshape(I1), d_inputs) + tuple(g[None] for g in weight_grads) + (mine[I0][None], mine[I1][None])

    return jax.shard_map(device_fn, mesh=mesh, in_specs=(act_spec, act_spec) + weight_specs, out_specs=(P('rep'), act_spec) + weight_specs, check_vma=False)
```

```python
import functools

import jax
import jax.numpy as jnp
from jax import lax
from jax.experimental import pallas as pl
from jax.experimental.pallas import tpu as pltpu
from jax.sharding import PartitionSpec as P

NORM_EPS = 1e-5
BF = jnp.bfloat16
F32 = jnp.float32
MESH = pl.DeviceIdType.MESH
ANY = pl.ANY


GELU_A = 0.7978845608028654
GELU_B = 0.044715
I0, I1, I2, I3, I4, I6, I8 = 0, 1, 2, 3, 4, 6, 8
CHUNK = 1024
BLOCK = 384
SUB = 256
DEPTH = 6
BACK_DEPTH = 5
KDEPTH = 3
EARLY_G = 3
STAGGER_NS = 6000
EARLY_SEEDS = 5
HEAD_PAD = 128
VMEM_LIMIT = 67043328


def mm(a, b):
    return lax.dot_general(a, b, (((I1,), (I0,)), ((), ())), preferred_element_type=F32)


def mm_nt(a, b):
    return lax.dot_general(a, b, (((I1,), (I1,)), ((), ())), preferred_element_type=F32)


def mm_tn(a, b):
    return lax.dot_general(a, b, (((I0,), (I0,)), ((), ())), preferred_element_type=F32)


class Place:
    def __init__(self):
        self.tp = lax.axis_index('tp')
        self.stage = lax.axis_index('stage')
        self.core = self.stage % I2
        self.x_pos = self.stage // I2
        self.home = self.x_pos * (I3 - I2 * self.tp) + self.tp
        self.is_l = self.stage == self.home
        self.sib = self.stage + I1 - I2 * self.core

    def at(self, tp, stage):
        return {'tp': tp, 'stage': stage}

    @property
    def sibling(self):
        return self.at(self.tp, self.sib)

    @property
    def along_x(self):
        return self.at(self.tp, (self.stage + I2) % I4)

    @property
    def across(self):
        return self.at(I1 - self.tp, self.stage)

    @property
    def across_other(self):
        return self.at(I1 - self.tp, self.sib)

    def chain(self, delta):
        there = self.home + delta
        x_pos = there // I2
        tp = there % I2 + x_pos * (I1 - I2 * (there % I2))
        return self.at(tp, I2 * x_pos + self.core)


def entry_barrier(place):
    barrier = pltpu.get_barrier_semaphore()
    for d_tp in (I0, I1):
        for d_stage in range(I4):
            if d_tp or d_stage:
                tp = place.tp + d_tp - I2 * d_tp * place.tp
                stage = (place.stage + d_stage) % I4
                pl.semaphore_signal(barrier, inc=I1, device_id=place.at(tp, stage), device_id_type=MESH)
    pl.semaphore_wait(barrier, 7)


def remote(src, dst, send_sem, recv_sem, device_id):
    return pltpu.make_async_remote_copy(src_ref=src, dst_ref=dst, send_sem=send_sem, recv_sem=recv_sem, device_id=device_id, device_id_type=MESH)


def rows_loop(total, step, body):
    def run(i, carry):
        body(pl.ds(pl.multiple_of(i * step, step), step))
        return carry
    lax.fori_loop(I0, total // step, run, I0)


def norm_rows(src, gain_row, dst, total):
    def body(rows):
        v = src[rows, :].astype(F32)
        inv = lax.rsqrt(jnp.mean(v * v, axis=-I1, keepdims=True) + NORM_EPS)
        dst[rows, :] = (v * inv * gain_row).astype(BF)
    rows_loop(total, 32, body)


def gelu_gate(u):
    u2 = u * u
    t = jnp.tanh(u * (GELU_A + (GELU_A * GELU_B) * u2))
    return 0.5 * t + 0.5, u2


def gelu_slope(hidden, gate, u2):
    return gate + hidden * (1.0 - gate) * (2.0 * GELU_A + (6.0 * GELU_A * GELU_B) * u2)


def row_parts(heads, cut=128):
    return [(*(x[low:high] for x in queries), *(x[:high] for x in keys), low)
            for queries, keys in heads for low, high in ((I0, cut), (cut, queries[I0].shape[I0]))]


def softmax_parts(scores, starts, keys_axis):
    masked = []
    for s, start in zip(scores, starts):
        k_pos = lax.broadcasted_iota(jnp.int32, s.shape, keys_axis)
        q_pos = lax.broadcasted_iota(jnp.int32, s.shape, I1 - keys_axis) + start
        masked.append(jnp.where(k_pos <= q_pos, s, -1e30))
    tops = [jnp.max(s, axis=keys_axis, keepdims=True) for s in masked]
    powers = [jnp.exp(s - top) for s, top in zip(masked, tops)]
    scales = [1.0 / jnp.sum(e, axis=keys_axis, keepdims=True) for e in powers]
    return [e * r for e, r in zip(powers, scales)]


def join_keys(top, low, cut=128):
    return jnp.concatenate([top + low[:cut], low[cut:]], I0).astype(BF)


def attention_forward(heads, scale):
    units = row_parts([((q,), (k, v)) for q, k, v in heads])
    probs = softmax_parts([mm_nt(q, k) * scale for q, k, _, _ in units], [u[-I1] for u in units], I1)
    parts = [mm(p.astype(BF), u[I2]) for p, u in zip(probs, units)]
    return [jnp.concatenate([a, b], I0).astype(BF) for a, b in zip(parts[I0::I2], parts[I1::I2])]


def nothing():
    pass


def attention_backward(heads, scale, between=()):
    work = iter(between)
    units = row_parts([((q, dc), (k, v)) for q, k, v, dc in heads])
    scores = [mm_nt(k, q) * scale for q, _, k, _, _ in units]
    dps = [mm_nt(v, dc) for _, dc, _, v, _ in units]
    next(work, nothing)()
    probs = softmax_parts(scores, [u[-I1] for u in units], I0)
    next(work, nothing)()
    dps = [dp.astype(BF).astype(F32) for dp in dps]
    deltas = [jnp.sum(dp * p, axis=I0, keepdims=True) for dp, p in zip(dps, probs)]
    dss = [p * (dp - delta) * scale for p, dp, delta in zip(probs, dps, deltas)]
    terms = []
    for ds in dss:
        hi = ds.astype(BF)
        rest = ds - hi.astype(F32)
        lo = rest.astype(BF)
        terms.append((hi, lo, (rest - lo.astype(F32)).astype(BF)))
    next(work, nothing)()
    dvs = [mm(p.astype(BF), u[I1]) for p, u in zip(probs, units)]
    dks = [mm(hi, u[I0]) + (mm(lo, u[I0]) + mm(tail, u[I0])) for (hi, lo, tail), u in zip(terms, units)]
    k_turned = [u[I2].T for u in units]
    dqs = [(mm(kt, hi) + (mm(kt, lo) + mm(kt, tail))).astype(BF) for (hi, lo, tail), kt in zip(terms, k_turned)]
    return [(jnp.concatenate([dqs[i].T, dqs[i + I1].T], I0), join_keys(dks[i], dks[i + I1]), join_keys(dvs[i], dvs[i + I1]))
            for i in range(I0, len(units), I2)]


def blocked(rows, stack, cols):
    total = mm(rows[:, I0:CHUNK], stack[I0, :, cols])
    for j in range(I1, stack.shape[I0]):
        total = total + mm(rows[:, j * CHUNK:(j + I1) * CHUNK], stack[j, :, cols])
    return total


def lanes(offset, size):
    return pl.ds(pl.multiple_of(offset, 128), size)


def load_resident(buf, sem, halves):
    for c in range(I6):
        for condition, ref in halves[c // I3]:
            copy = pltpu.make_async_copy(ref.at[(c % I3) * CHUNK:(c % I3 + I1) * CHUNK, :], buf.at[c], sem.at[c])
            if condition is None:
                copy.start()
            else:
                pl.when(condition)(copy.start)


def load_heads(ref, index, dst, sem):
    for r in range(I8):
        rows = pl.ds(pl.multiple_of(index * 768 + r * 96, 96), 96)
        pltpu.make_async_copy(ref.at[rows, :], dst.at[r * 128:r * 128 + 96, :], sem).start()


class Stream:
    def __init__(self, buf, sem, depth, parts, total, by_heads):
        self.buf, self.sem, self.depth, self.parts, self.total, self.by_heads = buf, sem, depth, parts, total, by_heads
        self.per_tick = sum(p[I1] for p in parts)

    def copy_in(self, ref, index, slot):
        if not self.by_heads:
            pltpu.make_async_copy(ref.at[index], self.buf.at[slot], self.sem.at[slot]).start()
            return
        load_heads(ref, index, self.buf.at[slot], self.sem.at[slot])

    def start(self, seq):
        @pl.when(seq < self.total)
        def _():
            j = seq % self.per_tick
            slot = seq % self.depth
            base = I0
            for choices, chunks in self.parts:
                for condition, ref in choices:
                    here = (j >= base) & (j < base + chunks)
                    here = here if condition is None else here & condition

                    @pl.when(here)
                    def _(ref=ref, low=base):
                        self.copy_in(ref, j - low, slot)
                base += chunks

    def prime(self):
        for seq in range(self.depth):
            self.start(jnp.int32(seq))

    def wait(self, seq):
        slot = seq % self.depth
        ref = self.parts[I0][I0][I0][I1]
        if self.by_heads:
            pltpu.make_async_copy(ref.at[I0:768, :], self.buf.at[slot, I0:768, :], self.sem.at[slot]).wait()
        else:
            pltpu.make_async_copy(ref.at[I0], self.buf.at[slot], self.sem.at[slot]).wait()
        return self.buf.at[slot]


PIECES = [(0, 0, 0), (0, 0, 1), (0, 0, 2), (1, 0, 0), (2, 1, 0), (2, 1, 1), (2, 1, 2), (2, 1, 3), (3, 0, 0), (3, 0, 1), (3, 0, 2), (3, 0, 3)]


ROUND = (10, 11)
ROUND_STEPS = (1, 3)


def piece(ref, axis, index):
    return ref.at[index * 768:(index + I1) * 768, :] if axis == I0 else ref.at[:, index * 768:(index + I1) * 768]


def weight_phase(place, is_r, own, near, far, turned, up_chunks, wn, wk, send_sem, y_send, d_send, near_sem, far_sem, load_sem, store_sem, chunk_sem,
                 round_a, round_b, ra_sem, rb_sem, x_send, xd_send, rs_send):
    wk[...] = jnp.zeros_like(wk)
    early = place.home < I2

    def piece_of(arrays, c):
        i, axis, index = PIECES[c]
        return piece(arrays[i], axis, index)

    @pl.when(place.is_l)
    def _():
        for i in range(I4):
            remote(own[i], near[i], send_sem.at[i], near_sem.at[i], place.sibling).start()

    @pl.when(is_r)
    def _():
        for k, c in enumerate(ROUND):
            @pl.when(early)
            def _(k=k, c=c):
                remote(piece_of(own, c), round_a.at[k], x_send.at[k], ra_sem.at[k], place.along_x).start()
        for c, (i, axis, index) in enumerate(PIECES):
            if c not in ROUND:
                remote(piece_of(own, c), piece_of(far, c), y_send.at[i], far_sem.at[c], place.across_other).start()
        for k, c in enumerate(ROUND):
            @pl.when(jnp.logical_not(early))
            def _(k=k, c=c):
                remote(piece_of(own, c), piece_of(far, c), x_send.at[k], far_sem.at[c], place.across_other).start()

    def load(i, refs, t, slot):
        for condition, ref in refs:
            def go(ref=ref):
                if i < I2:
                    for r in range(I2):
                        rows = pl.ds(pl.multiple_of(t * 192 + r * 96, 96), 96)
                        pltpu.make_async_copy(ref.at[rows, :], wk.at[I0, pl.ds(slot * SUB + r * 128, 96), :], load_sem.at[slot]).start()
                elif i == I2:
                    pltpu.make_async_copy(ref.at[:, lanes(t * SUB, SUB)], wn.at[slot, :, I0:SUB], load_sem.at[slot]).start()
                else:
                    rows = pl.ds(pl.multiple_of(t * SUB, SUB), SUB)
                    pltpu.make_async_copy(ref.at[rows, :], wk.at[I0, pl.ds(512 + slot * SUB, SUB), :], load_sem.at[slot]).start()
            if condition is None:
                go()
            else:
                pl.when(condition)(go)

    def loaded(i, refs, slot):
        ref = refs[I0][I1]
        if i < I2:
            pltpu.make_async_copy(ref.at[I0:192, :], wk.at[I0, I0:192, :], load_sem.at[slot]).wait()
        elif i == I2:
            pltpu.make_async_copy(ref.at[:, I0:SUB], wn.at[slot, :, I0:SUB], load_sem.at[slot]).wait()
        else:
            pltpu.make_async_copy(ref.at[I0:SUB, :], wk.at[I0, 512:768, :], load_sem.at[slot]).wait()

    def store(i, dst, t, slot):
        if i == I2:
            rows = pl.ds(pl.multiple_of(t * SUB, SUB), SUB)
            return pltpu.make_async_copy(wk.at[I1, pl.ds(slot * SUB, SUB), :], dst.at[rows, :], store_sem.at[slot])
        return pltpu.make_async_copy(wn.at[slot, :, SUB:512], dst.at[t // I4, :, lanes(t % I4 * SUB, SUB)], store_sem.at[slot])

    def keep(which, t, slot):
        return pltpu.make_async_copy(wn.at[slot, :, I0:SUB], up_chunks[which].at[t // I4, :, lanes(t % I4 * SUB, SUB)], chunk_sem.at[slot])

    def turn(i, refs, which, first, count):
        dst = turned[i][which]
        load(i, refs, first, I0)

        def step(n, c):
            slot = n % I2

            if i == I2:
                @pl.when(n > I0)
                def _():
                    keep(which, first + n - I1, I1 - slot).wait()

            @pl.when(n + I1 < count)
            def _():
                load(i, refs, first + n + I1, I1 - slot)
            loaded(i, refs, slot)
            if i == I2:
                keep(which, first + n, slot).start()

            @pl.when(n >= I2)
            def _():
                store(i, dst, first + n - I2, slot).wait()
            for b in range(I6):
                cut = slice(b * SUB, b * SUB + SUB)
                if i == I2:
                    wk[I1, pl.ds(pl.multiple_of(slot * SUB, SUB), SUB), cut] = wn[slot, cut, I0:SUB].T
                else:
                    base = I0 if i < I2 else 512
                    wn[slot, cut, SUB:512] = wk[I0, pl.ds(pl.multiple_of(base + slot * SUB, SUB), SUB), cut].T
            store(i, dst, first + n, slot).start()
            return c
        lax.fori_loop(I0, count, step, I0)
        for n in (count - I2, count - I1):
            store(i, dst, first + n, n % I2).wait()
        if i == I2:
            keep(which, first + count - I1, (count - I1) % I2).wait()

    counts = (12, I4, 12, 12)
    for i in range(I4):
        @pl.when(is_r)
        def _(i=i):
            remote(near[i], near[i], send_sem.at[i], near_sem.at[i], place.sibling).wait_recv()
        turn(i, [(place.is_l, own[i]), (is_r, near[i])], I0, I0, counts[i])
        if i < len(ROUND):
            @pl.when(place.is_l & jnp.logical_not(early))
            def _(k=i):
                remote(round_a.at[k], round_a.at[k], rs_send.at[k], ra_sem.at[k], place.sibling).wait_recv()
                remote(round_a.at[k], round_b.at[k], rs_send.at[k], rb_sem.at[k], place.across).start()
    done = [I0, I0, I0, I0]

    for c, (i, axis, index) in enumerate(PIECES):
        view = piece_of(far, c)
        for k, step in enumerate(ROUND_STEPS):
            if c == step:
                @pl.when(is_r & jnp.logical_not(early))
                def _(k=k):
                    remote(round_b.at[k], round_b.at[k], rs_send.at[k], rb_sem.at[k], place.sibling).wait_recv()
                    remote(round_b.at[k], piece_of(far, ROUND[k]), rs_send.at[k], far_sem.at[ROUND[k]], place.along_x).start()
        remote(view, view, d_send.at[i], far_sem.at[c], place.sibling).wait_recv()
        gives = is_r
        sem = d_send.at[i]
        if c in ROUND:
            gives = (early & place.is_l) | (jnp.logical_not(early) & is_r)
            sem = xd_send.at[ROUND.index(c)]

        @pl.when(gives)
        def _(c=c, view=view, sem=sem):
            remote(view, view, sem, far_sem.at[c], place.sibling).start()
        count = I4 if i < I2 else I3
        turn(i, [(None, far[i])], I1, done[i], count)
        done[i] += count

    @pl.when(place.is_l)
    def _():
        for i in range(I4):
            remote(own[i], near[i], send_sem.at[i], near_sem.at[i], place.sibling).wait_send()

    @pl.when(is_r)
    def _():
        for i in range(I4):
            part = own[i] if i < I3 else own[i].at[I0:I2 * 768, :]
            remote(part, part, y_send.at[i], far_sem.at[I0], place.across_other).wait_send()
            remote(part, part, d_send.at[i], far_sem.at[I0], place.sibling).wait_send()
        for k in range(len(ROUND)):
            remote(round_a.at[k], round_a.at[k], x_send.at[k], far_sem.at[I0], place.sibling).wait_send()

    @pl.when((early & place.is_l) | (jnp.logical_not(early) & is_r))
    def _():
        for k in range(len(ROUND)):
            remote(round_a.at[k], round_a.at[k], xd_send.at[k], far_sem.at[I0], place.sibling).wait_send()

    @pl.when(jnp.logical_not(early))
    def _():
        for k in range(len(ROUND)):
            remote(round_a.at[k], round_a.at[k], rs_send.at[k], far_sem.at[I0], place.sibling).wait_send()


def near_choices(place, own, near):
    return [(place.is_l, own), (jnp.logical_not(place.is_l), near)]


def forward_kernel(dims, x_ref, y_ref, wq, wo, wu, wd, own_gains,
                   a_s, h_s, qkv_s, u_s, g_s, oh_same, oh_other, oa_same, oa_other, og_same, og_other, loss_s, home_gains,
                   nq, no, nu, nd, fq, fo, fu, fd, tq0, to0, tu0, td0, tq1, to1, tu1, td1, uc0, uc1, round_a, round_b,
                   abuf, hbuf, obuf, nbuf, ybuf, sbuf, qkvbuf, ubuf, zbuf, ctxbuf, lossbuf, losstile, gains, wres, wores, wn,
                   send_sem, y_send, d_send, near_sem, far_sem, t_load, t_store, t_keep, ra_sem, rb_sem, x_send, xd_send, rs_send,
                   act_sem, hop_f, keep_sem, save_sem, stream_n, res_sem, out_sem, big_sem, y_sem, s_sem,
                   os_sem, oo_sem, as_sem, ao_sem, gs_sem, go_sem, bulk, gain_sem, tiny):
    micro, seq, width, heads, head_dim, ffn = dims
    place = Place()
    is_first, is_last = place.home == I0, place.home == I3
    home02 = (place.home == I0) | (place.home == I2)
    home13 = jnp.logical_not(home02)
    is_r = jnp.logical_not(place.is_l)
    takes_x = (place.home == I1) & is_r
    half = heads // I2 * HEAD_PAD
    scale = head_dim ** -0.5
    norm_factor = 1.0 / (micro * I2 * seq * width)
    own, near, far = (wq, wo, wu, wd), (nq, no, nu, nd), (fq, fo, fu, fd)
    turned = ((tq0, tq1), (to0, to1), (tu0, tu1), (td0, td1))
    entry_barrier(place)

    @pl.when(place.is_l)
    def _():
        pltpu.make_async_copy(own_gains, gains, gain_sem.at[I0]).start()
        remote(own_gains, gains, gain_sem.at[I1], gain_sem.at[I0], place.sibling).start()

    @pl.when(is_first)
    def _():
        for m in range(micro):
            pltpu.make_async_copy(x_ref.at[m, place.core], abuf.at[m], act_sem.at[m]).start()
    weight_phase(place, is_r, own, near, far, turned, (uc0, uc1), wn, wores, send_sem, y_send, d_send, near_sem, far_sem, t_load, t_store, t_keep,
                 round_a, round_b, ra_sem, rb_sem, x_send, xd_send, rs_send)
    pltpu.make_async_copy(own_gains, gains, gain_sem.at[I0]).wait()
    pltpu.make_async_copy(gains, home_gains, gain_sem.at[I0]).start()

    @pl.when(place.is_l)
    def _():
        remote(own_gains, gains, gain_sem.at[I1], gain_sem.at[I0], place.sibling).wait_send()

    def near_of(i):
        return near_choices(place, own[i], near[i])

    def saved(dst, index):
        return pltpu.make_async_copy(hbuf, dst, save_sem.at[index])

    sn = Stream(wn, stream_n, DEPTH, [([(None, tq0)], I3), ([(None, tq1)], I3), ([(None, uc0)], I3), ([(None, uc1)], I3)], micro * 12, False)
    for c, choices in enumerate((near_of(I1), [(None, fo)])):
        for condition, ref in choices:
            def go(ref=ref, c=c):
                load_heads(ref, I0, wores.at[c], out_sem.at[c])
            go() if condition is None else pl.when(condition)(go)
    sn.prime()
    load_resident(wres, res_sem, (near_of(I3), [(None, fd)]))
    lossbuf[...] = jnp.zeros_like(lossbuf)

    def qkv_out(m):
        return pltpu.make_async_copy(qkvbuf, qkv_s.at[m], big_sem.at[I0])

    def up_out(m):
        return pltpu.make_async_copy(ubuf, u_s.at[m], big_sem.at[I1])

    def act_out(m):
        return pltpu.make_async_copy(abuf.at[m], a_s.at[m], save_sem.at[I2])

    def hop_block(m, n):
        cols = lanes(n * SUB, SUB)
        return remote(obuf.at[m % I2, :, cols], abuf.at[m, :, cols], hop_f.at[m % I2], act_sem.at[m], place.chain(I1))

    def hop_forward(m):
        return remote(obuf.at[m % I2], abuf.at[m], hop_f.at[m % I2], act_sem.at[m], place.chain(I1))

    def near_hand(src, dst_far, dst_own, sem, recv_sem):
        return (lambda: remote(src, dst_far, sem, recv_sem, place.sibling)), (lambda: pltpu.make_async_copy(src, dst_own, sem))

    def hand_out(m):
        return near_hand(obuf.at[m % I2], oa_other.at[m], oa_same.at[m], keep_sem.at[m % I2], ao_sem)

    def both_kinds(condition, copies, start):
        far_copy, own_copy = copies

        @pl.when(condition & place.is_l)
        def _():
            far_copy().start() if start else far_copy().wait_send()

        @pl.when(condition & is_r)
        def _():
            own_copy().start() if start else own_copy().wait()

    def x_out(m):
        return pltpu.make_async_copy(ybuf, oa_same.at[m], y_sem), pltpu.make_async_copy(sbuf, oa_other.at[m], s_sem)

    def seed_out(m):
        return pltpu.make_async_copy(sbuf, g_s.at[m], s_sem)

    def far_mid(m, condition):
        @pl.when(condition & place.is_l)
        def _():
            remote(h_s.at[m], oh_same.at[m], bulk.at[I2], os_sem, place.across).start()

        @pl.when(condition & is_r)
        def _():
            remote(h_s.at[m], oh_other.at[m], bulk.at[I2], oo_sem, place.across_other).start()

    def send_seed(m):
        seed_out(m).wait()

        @pl.when(place.is_l & (m < EARLY_SEEDS))
        def _():
            remote(g_s.at[m], og_same.at[m], bulk.at[I1], gs_sem, place.across).start()

        @pl.when(is_r & (m < EARLY_SEEDS))
        def _():
            remote(g_s.at[m], og_other.at[m], bulk.at[I1], go_sem, place.across_other).start()

    def forward_tick(m, carry):
        act, mid, out = abuf.at[m], hbuf, obuf.at[m % I2]
        pltpu.make_async_copy(x_ref.at[m, place.core], act, act_sem.at[m]).wait()
        act_out(m).start()

        @pl.when(place.is_l)
        def _():
            pltpu.make_async_copy(act, oa_same.at[m], as_sem).start()

        @pl.when(is_last)
        def _():
            pltpu.make_async_copy(y_ref.at[m, place.core], ybuf, y_sem).start()

        @pl.when(takes_x)
        def _():
            @pl.when(m > I0)
            def _():
                for copy in x_out(m):
                    copy.wait()
            for core, buf, sem in ((place.core, ybuf, y_sem), (I1 - place.core, sbuf, s_sem)):
                pltpu.make_async_copy(x_ref.at[m, core], buf, sem).start()
        norm_rows(act, gains[I0:I1, :], nbuf, seq)

        @pl.when(m > I0)
        def _():
            qkv_out(m).wait()

        def qkv_step(j, c):
            w = sn.wait(m * 12 + j)
            for n in range(I0, CHUNK, SUB):
                qkvbuf[:, lanes(j * CHUNK + n, SUB)] = mm(nbuf[...], w[:, n:n + SUB]).astype(BF)
            sn.start(m * 12 + j + DEPTH)
            return c
        lax.fori_loop(I0, I6, qkv_step, I0)
        qkv_out(m).start()
        act_out(m).wait()

        @pl.when(is_r)
        def _():
            remote(a_s.at[m], oa_other.at[m], bulk.at[I0], ao_sem, place.sibling).start()

        def head_step(i, c):
            base = i * (I3 * half)
            views = [[qkvbuf[:, lanes(base + t * half + r * HEAD_PAD, HEAD_PAD)] for t in range(I3)] for r in range(I8)]
            for r, context in enumerate(attention_forward(views, scale)):
                ctxbuf[:, lanes(i * half + r * HEAD_PAD, HEAD_PAD)] = context
            return c
        lax.fori_loop(I0, I2, head_step, I0)

        @pl.when(m == I0)
        def _():
            for c in range(I2):
                pltpu.make_async_copy(wo, wores.at[c, I0:768, :], out_sem.at[c]).wait()
        for n in range(I0, width, SUB):
            total = mm(ctxbuf[:, I0:half], wores[I0, :, n:n + SUB]) + mm(ctxbuf[:, half:I2 * half], wores[I1, :, n:n + SUB])
            mid[:, n:n + SUB] = (act[:, n:n + SUB].astype(F32) + total).astype(BF)
        saved(h_s.at[m], I0).start()

        @pl.when(place.is_l)
        def _():
            saved(oh_same.at[m], I1).start()
        norm_rows(mid, gains[I1:I2, :], nbuf, seq)

        @pl.when(m > I0)
        def _():
            up_out(m).wait()

        def up_step(j, c):
            w = sn.wait(m * 12 + I6 + j)
            for n in range(I0, CHUNK, SUB):
                u = mm(nbuf[...], w[:, n:n + SUB]).astype(BF)
                at = lanes(j * CHUNK + n, SUB)
                ubuf[:, at] = u
                uf = u.astype(F32)
                zbuf[:, at] = (uf * gelu_gate(uf)[I0]).astype(BF)
            sn.start(m * 12 + I6 + j + DEPTH)
            return c
        lax.fori_loop(I0, I6, up_step, I0)
        up_out(m).start()

        @pl.when((m > I1) & jnp.logical_not(is_last))
        def _():
            hop_forward(m).wait_send()

        both_kinds((m > I1) & home02, hand_out(m), False)

        @pl.when(m == I0)
        def _():
            for j in range(I6):
                pltpu.make_async_copy(wd.at[I0:CHUNK, :], wres.at[j], res_sem.at[j]).wait()

        def down_step(n, c):
            cols = lanes(n * SUB, SUB)
            out[:, cols] = (mid[:, cols].astype(F32) + blocked(zbuf, wres, cols)).astype(BF)

            @pl.when((n > I0) & jnp.logical_not(is_last))
            def _():
                hop_block(m, n - I1).start()
            return c
        lax.fori_loop(I0, width // SUB, down_step, I0)

        @pl.when(jnp.logical_not(is_last))
        def _():
            hop_block(m, width // SUB - I1).start()

        both_kinds(home02, hand_out(m), True)

        @pl.when(is_last)
        def _():
            pltpu.make_async_copy(y_ref.at[m, place.core], ybuf, y_sem).wait()

            @pl.when(m > I0)
            def _():
                send_seed(m - I1)

            def seed(rows):
                error = out[rows, :].astype(F32) - ybuf[rows, :].astype(F32)
                sbuf[rows, :] = (error * norm_factor).astype(BF)
                lossbuf[...] += jnp.sum((error * error).reshape(I4, I8, width), axis=I0)
            rows_loop(seq, 32, seed)
            seed_out(m).start()

        @pl.when(takes_x)
        def _():
            for core, buf, sem in ((place.core, ybuf, y_sem), (I1 - place.core, sbuf, s_sem)):
                pltpu.make_async_copy(x_ref.at[m, core], buf, sem).wait()
            for copy in x_out(m):
                copy.start()

        saved(h_s.at[m], I0).wait()

        @pl.when(place.is_l)
        def _():
            saved(oh_same.at[m], I1).wait()

        @pl.when(is_r)
        def _():
            remote(h_s.at[m], oh_other.at[m], bulk.at[I3], oo_sem, place.sibling).start()

        far_mid(m, home13 | (m % I2 == I1))
        return carry

    @pl.when(is_first & (place.core == I0))
    def _():
        pl.delay(STAGGER_NS)
    lax.fori_loop(I0, micro, forward_tick, I0)
    for m in range(I0, micro, I2):
        far_mid(m, is_first)

    @pl.when(is_last)
    def _():
        total = lossbuf[:, I0:128]
        for n in range(128, width, 128):
            total = total + lossbuf[:, n:n + 128]
        losstile[...] = total
        pltpu.make_async_copy(losstile, loss_s, tiny).start()
    for copy in (qkv_out(micro - I1), up_out(micro - I1)):
        copy.wait()

    @pl.when(jnp.logical_not(is_last))
    def _():
        for m in (micro - I2, micro - I1):
            hop_forward(m).wait_send()
    for m in (micro - I2, micro - I1):
        both_kinds(home02, hand_out(m), False)

    @pl.when(is_last)
    def _():
        seed_out(micro - I1).wait()
        pltpu.make_async_copy(losstile, loss_s, tiny).wait()

    @pl.when(takes_x)
    def _():
        for copy in x_out(micro - I1):
            copy.wait()
    pltpu.make_async_copy(gains, home_gains, gain_sem.at[I0]).wait()
    sent, got = drain(place)

    @pl.when(place.home != I2)
    def _():
        sent(h_s, bulk.at[I2])

    @pl.when(place.home == I2)
    def _():
        sent(h_s.at[I0:micro // I2], bulk.at[I2])

    @pl.when(place.is_l | jnp.logical_not(is_last))
    def _():
        got(oh_other, oo_sem)

    @pl.when(is_r & is_last)
    def _():
        got(oh_other.at[I0:micro // I2], oo_sem)

    @pl.when(is_last)
    def _():
        sent(g_s.at[I0:EARLY_SEEDS], bulk.at[I1])

    @pl.when((place.home == I2) & is_r)
    def _():
        got(og_same.at[I0:EARLY_SEEDS], gs_sem)
        got(og_other.at[I0:EARLY_SEEDS], go_sem)

    @pl.when(is_r)
    def _():
        sent(a_s, bulk.at[I0])
        sent(h_s, bulk.at[I3])

    @pl.when(is_r & jnp.logical_not(is_last))
    def _():
        got(oh_same, os_sem)

    @pl.when(is_r & is_last)
    def _():
        got(oh_same.at[I0:micro // I2], os_sem)

    @pl.when(place.is_l)
    def _():
        got(oa_same, as_sem)

    @pl.when(place.is_l | home02)
    def _():
        got(oa_other, ao_sem)


def drain(place):
    def sent(buf, sem):
        remote(buf, buf, sem, sem, place.sibling).wait_send()

    def got(dst, sem):
        pltpu.make_async_copy(dst, dst, sem).wait()
    return sent, got


def backward_kernel(dims, a_s, h_s, qkv_s, u_s, g_s, wq, nq, fq, td0, td1, to0, to1, tu0, tu1, gains, loss_s, after, *refs):
    (dx_s, m_s, od_same, od_other, og_same, og_other, oa_same, oa_other, oh_same, oh_other, dg_same, dg_other, loss_all,
     gbuf, hbuf, obuf, qkvbuf, ubuf, habuf, zbuf, ctxbuf, dqkvbuf, acc, accg, wres, wn, wk,
     grad_sem, hop_b, back_sem, dx_sem, dx_send, save_sem, stream_n, stream_k, res_sem, load_sem,
     ds_sem, do_sem, gs_sem, go_sem, as_sem, ao_sem, os_sem, oo_sem, bulk, tiny, loss_sem, ready) = refs[I6:]
    micro, seq, width, heads, head_dim, ffn = dims
    place = Place()
    is_first, is_last = place.home == I0, place.home == I3
    home13 = (place.home == I1) | is_last
    is_r = jnp.logical_not(place.is_l)
    half = heads // I2 * HEAD_PAD
    scale = head_dim ** -0.5

    barrier = pltpu.get_barrier_semaphore()
    is_b, is_c = place.home == I1, place.home == I2
    for there in (place.sibling, place.across, place.across_other):
        pl.semaphore_signal(barrier, inc=I1, device_id=there, device_id_type=MESH)

    @pl.when(is_c)
    def _():
        pl.semaphore_signal(barrier, inc=I1, device_id=place.along_x, device_id_type=MESH)

    @pl.when(is_last)
    def _():
        for m in range(micro):
            pltpu.make_async_copy(g_s.at[m], gbuf.at[m], grad_sem.at[m]).start()
    wk[...] = jnp.zeros_like(wk)
    bn = Stream(wn, stream_n, BACK_DEPTH, [([(None, td0)], I3), ([(None, td1)], I3), ([(None, to0)], I1), ([(None, to1)], I1)], micro * I8, False)
    bk = Stream(wk, stream_k, KDEPTH, [(near_choices(place, wq, nq), I3), ([(None, fq)], I3)], micro * I6, True)
    bn.prime()
    bk.prime()
    load_resident(wres, res_sem, ([(None, tu0)], [(None, tu1)]))

    def saved(dst, index):
        return pltpu.make_async_copy(hbuf, dst, save_sem)

    def both_kinds(condition, copies, start):
        far_copy, own_copy = copies

        @pl.when(condition & place.is_l)
        def _():
            far_copy().start() if start else far_copy().wait_send()

        @pl.when(condition & is_r)
        def _():
            own_copy().start() if start else own_copy().wait()

    def near_hand(src, dst_far, dst_own, sem, recv_sem):
        return (lambda: remote(src, dst_far, sem, recv_sem, place.sibling)), (lambda: pltpu.make_async_copy(src, dst_own, sem))

    def loads(i):
        m = micro - I1 - i
        return [pltpu.make_async_copy(src.at[m], dst, load_sem.at[k])
                for k, (src, dst) in enumerate(((u_s, ubuf), (qkv_s, qkvbuf), (h_s, habuf.at[I0]), (a_s, habuf.at[I1])))]

    def load_next(i, k):
        @pl.when(i + I1 < micro)
        def _():
            loads(i + I1)[k].start()

    for copy in loads(I0):
        copy.start()
    accg[...] = jnp.zeros_like(accg)

    def norm_back(index, x, base, dst, gain_row):
        def body(rows):
            xf = x[rows, :].astype(F32)
            dy = acc[rows, :].astype(BF).astype(F32)
            inv = lax.rsqrt(jnp.mean(xf * xf, axis=-I1, keepdims=True) + NORM_EPS)
            xn = xf * inv
            accg[index] += jnp.sum((dy * xn).reshape(I4, I8, width), axis=I0)
            dyg = dy * gain_row
            dx = inv * (dyg - xn * jnp.mean(dyg * xn, axis=-I1, keepdims=True))
            dst[rows, :] = (base[rows, :].astype(F32) + dx).astype(BF)
        rows_loop(seq, 32, body)

    def hop_back(i):
        m = micro - I1 - i
        return remote(obuf.at[i % I2], gbuf.at[m], hop_b.at[i % I2], grad_sem.at[m], place.chain(-I1))

    def hand_back(i):
        m = micro - I1 - i
        return near_hand(obuf.at[i % I2], og_other.at[m], og_same.at[m], back_sem.at[i % I2], go_sem)

    def keep_dx(i):
        return pltpu.make_async_copy(obuf.at[i % I2], dx_s.at[micro - I1 - i], back_sem.at[i % I2])

    def back_ready(i):
        both_kinds((i > I1) & home13, hand_back(i), False)

        @pl.when((i > I1) & is_first)
        def _():
            keep_dx(i).wait()
            dx_to_b(i).wait_send()

        @pl.when((i > I1) & jnp.logical_not(is_first))
        def _():
            hop_back(i).wait_send()

    def pass_loss(tile):
        @pl.when(jnp.logical_not(is_first))
        def _():
            remote(tile, loss_all.at[place.core], loss_sem.at[I0], loss_sem.at[I1], place.chain(-I1)).start()
        remote(tile, loss_all.at[place.core], loss_sem.at[I2], loss_sem.at[I3], place.sibling).start()

    def dx_to_b(i):
        return remote(obuf.at[i % I2], dx_s.at[micro - I1 - i], dx_send.at[i % I2], dx_sem, place.across)

    def backward_tick(i, carry):
        m = micro - I1 - i
        slot = i % I2
        grad, dmid, prev = gbuf.at[m], hbuf, obuf.at[slot]
        u_now, qkv_now, h_now, a_now = ubuf, qkvbuf, habuf.at[I0], habuf.at[I1]

        pltpu.make_async_copy(g_s.at[m], grad, grad_sem.at[m]).wait()

        @pl.when(place.is_l)
        def _():
            pltpu.make_async_copy(grad, og_same.at[m], gs_sem).start()
        load_u, load_qkv, load_h, load_a = loads(i)
        load_u.wait()

        def mlp_step(j, c):
            w = bn.wait(i * I8 + j)
            for n in range(I0, CHUNK, SUB):
                at = lanes(j * CHUNK + n, SUB)
                dz = mm(grad[...], w[:, n:n + SUB]).astype(BF).astype(F32)
                u = u_now[:, at].astype(F32)
                gate, u2 = gelu_gate(u)
                zbuf[:, at] = (dz * gelu_slope(u * gate, gate, u2)).astype(BF)
            bn.start(i * I8 + j + BACK_DEPTH)
            return c
        lax.fori_loop(I0, I6, mlp_step, I0)

        @pl.when(i == I0)
        def _():
            for j in range(I6):
                pltpu.make_async_copy(tu0.at[I0:CHUNK, :], wres.at[j], res_sem.at[j]).wait()

        def turn_back(n, c):
            cols = lanes(n * SUB, SUB)
            acc[:, cols] = blocked(zbuf, wres, cols)
            return c
        lax.fori_loop(I0, width // SUB, turn_back, I0)
        load_next(i, I0)
        load_h.wait()
        norm_back(I1, h_now, grad, dmid, gains[I1:I2, :])
        load_next(i, I2)

        @pl.when(place.is_l)
        def _():
            saved(od_same.at[m], I0).start()

        @pl.when(is_r)
        def _():
            saved(m_s.at[m], I0).start()
        for c in range(I2):
            w = bn.wait(i * I8 + I6 + c)
            for n in range(I0, CHUNK, SUB):
                ctxbuf[:, c * CHUNK + n:c * CHUNK + n + SUB] = mm(dmid[...], w[:, n:n + SUB]).astype(BF)
            bn.start(i * I8 + I6 + c + BACK_DEPTH)
        load_qkv.wait()

        def head_step(t, c):
            base = (t // I2) * (I3 * half) + (t % I2) * (I4 * HEAD_PAD)
            at = [[lanes(base + part * half + r * HEAD_PAD, HEAD_PAD) for part in range(I3)] for r in range(I4)]
            group = [(*(qkv_now[:, p] for p in at[r]), ctxbuf[:, lanes((t * I4 + r) * HEAD_PAD, HEAD_PAD)]) for r in range(I4)]
            for r, grads in enumerate(attention_backward(group, scale)):
                for p, value in zip(at[r], grads):
                    dqkvbuf[:, p] = value
            return c
        lax.fori_loop(I0, heads // I4, head_step, I0)
        load_next(i, I1)
        acc[...] = jnp.zeros_like(acc)

        def qkv_step(j, c):
            w = bk.wait(i * I6 + j)
            for n in range(I0, width, SUB):
                acc[:, n:n + SUB] += mm(dqkvbuf[:, lanes(j * CHUNK, CHUNK)], w[:, n:n + SUB])
            bk.start(i * I6 + j + KDEPTH)
            return c
        lax.fori_loop(I0, I6, qkv_step, I0)
        load_a.wait()
        back_ready(i)
        norm_back(I0, a_now, dmid, prev, gains[I0:I1, :])
        load_next(i, I3)

        @pl.when(i == I0)
        def _():
            @pl.when(is_first | is_last)
            def _():
                pl.semaphore_wait(barrier, I3)

            @pl.when(is_c)
            def _():
                pl.semaphore_wait(ready, I1)

            @pl.when(is_last)
            def _():
                pass_loss(loss_s)

        @pl.when(jnp.logical_not(is_first))
        def _():
            hop_back(i).start()

        @pl.when(is_first)
        def _():
            keep_dx(i).start()
            dx_to_b(i).start()
        both_kinds(home13, hand_back(i), True)

        @pl.when(place.is_l)
        def _():
            saved(od_same.at[m], I0).wait()
            remote(od_same.at[m], od_same.at[m], bulk.at[I6], ds_sem, place.across).start()

        @pl.when(is_r)
        def _():
            remote(grad, og_other.at[m], bulk.at[5], go_sem, place.sibling).start()
            saved(m_s.at[m], I0).wait()
            remote(m_s.at[m], od_other.at[m], bulk.at[I6], do_sem, place.sibling).start()
            remote(m_s.at[m], od_other.at[m], bulk.at[7], do_sem, place.across_other).start()

        now = (i % I2 == I1) & (i < I2 * EARLY_G)
        far_grad(m, (place.home == I1) & now)
        far_grad(micro - I1 - i // I2, is_last & now)
        return carry

    def far_grad(m, condition):
        @pl.when(condition & place.is_l)
        def _():
            remote(gbuf.at[m], og_same.at[m], bulk.at[I4], gs_sem, place.across).start()

        @pl.when(condition & is_r)
        def _():
            remote(gbuf.at[m], og_other.at[m], bulk.at[I4], go_sem, place.across_other).start()

    @pl.when(is_b | is_c)
    def _():
        pl.semaphore_wait(barrier, 5 - place.home)

    @pl.when(is_b)
    def _():
        pl.semaphore_signal(ready, inc=I1, device_id=place.along_x, device_id_type=MESH)

    @pl.when(is_c & place.is_l)
    def _():
        for t in range(micro):
            remote(a_s.at[t], oa_same.at[t], bulk.at[I8], as_sem, place.across).start()
        for t in range(I0, micro, I2):
            remote(h_s.at[t], oh_same.at[t], bulk.at[9], os_sem, place.across).start()

    @pl.when(is_c & is_r)
    def _():
        for t in range(micro):
            remote(a_s.at[t], oa_other.at[t], bulk.at[I8], ao_sem, place.across_other).start()
        for t in range(I0, micro, I2):
            remote(h_s.at[t], oh_other.at[t], bulk.at[9], oo_sem, place.across_other).start()
    lax.fori_loop(I0, micro, backward_tick, I0)
    loss_mine = loss_all.at[place.core]

    @pl.when(is_last)
    def _():
        own_loss = pltpu.make_async_copy(loss_s, loss_mine, loss_sem.at[I1])
        own_loss.start()
        own_loss.wait()

    @pl.when(jnp.logical_not(is_last))
    def _():
        remote(loss_mine, loss_mine, loss_sem.at[I0], loss_sem.at[I1], place.sibling).wait_recv()
        pass_loss(loss_mine)

    @pl.when(place.is_l)
    def _():
        pltpu.make_async_copy(accg, dg_same, tiny.at[I0]).start()
        remote(accg, dg_same, tiny.at[I1], tiny.at[I0], place.across).start()

    @pl.when(is_r)
    def _():
        remote(accg, dg_other, tiny.at[I1], tiny.at[I4], place.sibling).start()
        remote(accg, dg_other, tiny.at[I2], tiny.at[I4], place.across_other).start()

    for i in (micro - I2, micro - I1):
        back_ready(jnp.int32(i))

    sent, got = drain(place)
    sent(m_s, bulk.at[I6])

    @pl.when(is_r)
    def _():
        sent(gbuf, bulk.at[5])
        sent(m_s, bulk.at[7])
        remote(accg, dg_other, tiny.at[I2], tiny.at[I4], place.sibling).wait_send()

    @pl.when(home13)
    def _():
        sent(gbuf.at[I0:EARLY_G], bulk.at[I4])

    @pl.when(place.home == I1)
    def _():
        got(dx_s, dx_sem)

    @pl.when(jnp.logical_not(is_first))
    def _():
        remote(loss_mine, loss_mine, loss_sem.at[I0], loss_sem.at[I1], place.sibling).wait_send()
    remote(loss_mine, loss_mine, loss_sem.at[I2], loss_sem.at[I3], place.sibling).wait_send()
    remote(loss_mine, loss_mine, loss_sem.at[I2], loss_sem.at[I3], place.sibling).wait_recv()

    @pl.when(place.home == I2)
    def _():
        sent(a_s, bulk.at[I8])
        sent(h_s.at[I0:micro // I2], bulk.at[9])

    remote(accg, dg_other, tiny.at[I1], tiny.at[I4], place.sibling).wait_send()
    got(od_other, do_sem)

    @pl.when(place.is_l | home13)
    def _():
        got(og_other, go_sem)

    @pl.when(jnp.logical_not(home13) & is_r)
    def _():
        got(og_same.at[I0:EARLY_G], gs_sem)
        got(og_other.at[I0:EARLY_G], go_sem)
    got(dg_same, tiny.at[I0])
    got(dg_other, tiny.at[I4])

    @pl.when(is_r)
    def _():
        got(od_same, ds_sem)

    @pl.when(place.is_l)
    def _():
        got(og_same, gs_sem)

    @pl.when(is_last & is_r)
    def _():
        got(oa_same, as_sem)
        got(oa_other, ao_sem)
        got(oh_same.at[I0:micro // I2], os_sem)
        got(oh_other.at[I0:micro // I2], oo_sem)


def shapes(*dims_list):
    return [jax.ShapeDtypeStruct(d, BF) for d in dims_list]


def forward_phase(dims, x, y, own, own_gains):
    micro, seq, width, heads, head_dim, ffn = dims
    half = heads // I2 * HEAD_PAD
    act = (micro, seq, width)
    raw = [w.shape for w in own]
    turned = [(I3, width, CHUNK), (I1, width, CHUNK), (ffn // I2, width), (I3, width, CHUNK)]
    out_shape = shapes(act, act, (micro, seq, I6 * half), (micro, seq, ffn), *[act] * 7)
    out_shape += [jax.ShapeDtypeStruct(s, F32) for s in ((I8, 128), own_gains.shape)]
    out_shape += shapes(*raw, *raw, *turned, *turned, turned[I0], turned[I0], *[(len(ROUND), 768, width)] * I2)
    any_spec = pl.BlockSpec(memory_space=ANY)
    vmem, dma = pltpu.VMEM, pltpu.SemaphoreType.DMA
    row = vmem((seq, width), BF)
    scratch = [
        vmem(act, BF), row, vmem((I2, seq, width), BF), row, row, row, vmem((seq, I6 * half), BF), vmem((seq, ffn), BF), vmem((seq, ffn), BF),
        vmem((seq, I2 * half), BF), vmem((I8, width), F32), vmem((I8, 128), F32), vmem((I2, width), F32),
        vmem((I6, CHUNK, width), BF), vmem((I2, CHUNK, width), BF), vmem((DEPTH, width, CHUNK), BF),
        dma((I4,)), dma((I4,)), dma((I4,)), dma((I4,)), dma((12,)), dma((I2,)), dma((I2,)), dma((I2,)), *[dma((len(ROUND),))] * 5,
        dma((micro,)), dma((I2,)), dma((I2,)), dma((I3,)), dma((DEPTH,)), dma((I6,)), dma((I2,)), dma((I2,)), dma(()), dma(()),
        dma(()), dma(()), dma(()), dma(()), dma(()), dma(()), dma((I4,)), dma((I2,)), dma(()),
    ]
    return pl.pallas_call(
        functools.partial(forward_kernel, dims),
        out_shape=tuple(out_shape),
        in_specs=[any_spec] * I6 + [pl.BlockSpec(memory_space=vmem)],
        out_specs=(any_spec,) * len(out_shape),
        scratch_shapes=scratch,
        compiler_params=pltpu.CompilerParams(collective_id=I0, has_side_effects=True, vmem_limit_bytes=VMEM_LIMIT),
        name='forward_phase',
    )(x, y, *own, own_gains)


def backward_phase(dims, saved, weights, gains, loss, after, placed):
    micro, seq, width, heads, head_dim, ffn = dims
    half = heads // I2 * HEAD_PAD
    act = (micro, seq, width)
    out_shape = shapes(*[act] * 10) + [jax.ShapeDtypeStruct((I2, I8, width), F32)] * I2 + [jax.ShapeDtypeStruct((I2, I8, 128), F32)]
    any_spec = pl.BlockSpec(memory_space=ANY)
    vmem, dma = pltpu.VMEM, pltpu.SemaphoreType.DMA
    scratch = [
        vmem(act, BF), vmem((seq, width), BF), vmem((I2, seq, width), BF), vmem((seq, I6 * half), BF), vmem((seq, ffn), BF),
        vmem((I2, seq, width), BF), vmem((seq, ffn), BF), vmem((seq, I2 * half), BF), vmem((seq, I6 * half), BF), vmem((seq, width), F32),
        vmem((I2, I8, width), F32), vmem((I6, CHUNK, width), BF), vmem((BACK_DEPTH, width, CHUNK), BF), vmem((KDEPTH, CHUNK, width), BF),
        dma((micro,)), dma((I2,)), dma((I2,)), dma(()), dma((I2,)), dma(()), dma((BACK_DEPTH,)), dma((KDEPTH,)), dma((I6,)), dma((I4,)),
        *[dma(())] * I8, dma((10,)), dma((5,)), dma((I4,)), pltpu.SemaphoreType.REGULAR,
    ]
    return pl.pallas_call(
        functools.partial(backward_kernel, dims),
        out_shape=tuple(out_shape),
        in_specs=[any_spec] * 14 + [pl.BlockSpec(memory_space=vmem)] * I2 + [any_spec] * 7,
        out_specs=(any_spec,) * len(out_shape),
        scratch_shapes=scratch,
        input_output_aliases={17 + i: I4 + i for i in range(I6)},
        compiler_params=pltpu.CompilerParams(collective_id=I1, has_side_effects=True, vmem_limit_bytes=VMEM_LIMIT),
        name='backward_phase',
    )(*saved, *weights, gains, loss, after, *placed)


def recompute_kernel(dims, early, h_same, h_other, a_same, a_other, gains, wq, wu, *refs):
    (done, u_o, qkv_o, ctx_o, n1_o, n2_o), (wqbuf, wubuf, count, sem) = refs[-10:-I4], refs[-I4:]
    micro, seq, width, heads, head_dim, ffn = dims
    place = Place()
    scale = head_dim ** -0.5
    half = heads // I2 * HEAD_PAD
    steps = I2 * micro * seq // BLOCK

    def pieces(j):
        copies = [pltpu.make_async_copy(wu.at[:, lanes(j * SUB, SUB)], wubuf.at[:, lanes(j * SUB, SUB)], sem.at[I0, j])]
        for r in range(I2):
            src = pl.ds(pl.multiple_of((I2 * j + r) * head_dim, head_dim), head_dim)
            dst = pl.ds(pl.multiple_of((I2 * j + r) * HEAD_PAD, HEAD_PAD), head_dim)
            copies.append(pltpu.make_async_copy(wq.at[src, :], wqbuf.at[dst, :], sem.at[I1 + r, j]))
        return copies

    def body(hs, ho, rs, ro, u, qkv, ctx, n1, n2):
        step = count[I0]
        count[I0] = step + I1
        for low, high, gain, dst in ((hs, ho, gains[I1:I2, :], n2), (rs, ro, gains[I0:I1, :], n1)):
            @pl.when(step < steps // I2)
            def _(low=low, gain=gain, dst=dst):
                norm_rows(low, gain, dst, BLOCK)

            @pl.when(step >= steps // I2)
            def _(high=high, gain=gain, dst=dst):
                norm_rows(high, gain, dst, BLOCK)

        @pl.when(step == I0)
        def _():
            for j in range(I3 * half // SUB):
                for copy in pieces(j):
                    copy.wait()

        def qkv_step(j, c):
            rows = pl.ds(pl.multiple_of(j * SUB, SUB), SUB)
            qkv[:, lanes(j * SUB, SUB)] = mm_nt(n1[...], wqbuf[rows, :]).astype(BF)
            u[:, lanes(j * SUB, SUB)] = mm(n2[...], wubuf[:, lanes(j * SUB, SUB)]).astype(BF)
            return c
        lax.fori_loop(I0, I3 * half // SUB, qkv_step, I0)

        def head_step(j, c):
            at = [(pl.ds(s, seq), r * HEAD_PAD) for s in range(I0, BLOCK, seq) for r in range(I4)]
            base = j * (I4 * HEAD_PAD)
            views = [[qkv[rows, lanes(base + t * half + col, HEAD_PAD)] for t in range(I3)] for rows, col in at]
            for (rows, col), context in zip(at, attention_forward(views, scale)):
                ctx[rows, lanes(base + col, HEAD_PAD)] = context
            return c
        lax.fori_loop(I0, I2, head_step, I0)

    @pl.when(place.home < I2 if early else place.home > I1)
    def _():
        pads = jnp.zeros((HEAD_PAD - head_dim, width), BF)
        for t in range(I3 * heads // I2):
            wqbuf[t * HEAD_PAD + head_dim:(t + I1) * HEAD_PAD, :] = pads
        for j in range(I3 * half // SUB):
            for copy in pieces(j):
                copy.start()
        count[I0] = I0
        low = pl.BlockSpec((BLOCK, width), lambda i: (jnp.minimum(i, steps // I2 - I1), I0))
        high = pl.BlockSpec((BLOCK, width), lambda i: (jnp.maximum(i - steps // I2, I0), I0))
        block = lambda n: pl.BlockSpec((BLOCK, n), lambda i: (i, I0))
        pltpu.emit_pipeline(body, grid=(steps,), in_specs=[low, high, low, high],
                            out_specs=[block(ffn // I2), block(I3 * half), block(half), block(width), block(width)])(
            h_same, h_other, a_same, a_other, u_o, qkv_o, ctx_o, n1_o, n2_o)


def owner_recompute(dims, early, again, h_rows, a_rows, gains, own):
    micro, seq, width, heads, head_dim, ffn = dims
    half = heads // I2 * HEAD_PAD
    tokens = I2 * micro * seq
    any_spec = pl.BlockSpec(memory_space=ANY)
    vmem = pltpu.VMEM
    earlier = () if early else tuple(again)
    return pl.pallas_call(
        functools.partial(recompute_kernel, dims, early),
        out_shape=(jax.ShapeDtypeStruct((I8, 128), F32), *shapes((tokens, ffn // I2), (tokens, I3 * half), (tokens, half), (tokens, width), (tokens, width))),
        in_specs=[any_spec] * I4 + [pl.BlockSpec(memory_space=vmem)] + [any_spec] * (I2 + len(earlier)),
        out_specs=(any_spec,) * I6,
        scratch_shapes=[vmem((I3 * half, width), BF), vmem((width, ffn // I2), BF), pltpu.SMEM((I1,), jnp.int32), pltpu.SemaphoreType.DMA((I3, ffn // I2 // SUB))],
        input_output_aliases={7 + i: I1 + i for i in range(len(earlier))},
        compiler_params=pltpu.CompilerParams(has_side_effects=True, vmem_limit_bytes=VMEM_LIMIT),
        name='owner_recompute',
    )(*h_rows, *a_rows, gains, own[I0], own[I2], *earlier)


def spread_dx(step, last, dx, d_in, og_same, og_other, bounce, here_sem, parent_sem, sib_sem, send_sems, og_sems, ready):
    place = Place()
    micro = dx.shape[I0]
    along_x = place.at(place.tp, (place.stage + I2) % I4)
    barrier = pltpu.get_barrier_semaphore()
    is_leaf = place.home > I1
    gives_g = (place.home == I1) & place.is_l
    takes_g = (place.home == I0) & jnp.logical_not(place.is_l)
    late = [micro - I1 - i for i in range(micro) if i % I2 == I0 or i > I2 * EARLY_G]

    def block(m):
        return d_in.at[m, place.core]

    def to_sibling(m, src):
        remote(src, block(m), send_sems.at[I0], sib_sem, place.sibling).start()

    def tell(there):
        pl.semaphore_signal(barrier, inc=I1, device_id=there, device_id_type=MESH)

    @pl.when(step == I0)
    def _():
        tell(place.sibling)

        @pl.when(takes_g)
        def _():
            tell(place.across)

        @pl.when(is_leaf)
        def _():
            pl.semaphore_wait(barrier, I2)
            pl.semaphore_signal(ready, inc=I1, device_id=along_x, device_id_type=MESH)

        @pl.when(jnp.logical_not(is_leaf))
        def _():
            tell(along_x)
            pl.semaphore_wait(barrier, I1 + gives_g.astype(jnp.int32))

        @pl.when(gives_g)
        def _():
            for t, og in enumerate((og_same, og_other)):
                for m in late:
                    remote(og.at[m], og.at[m], og_sems.at[t], og_sems.at[I2 + t], place.across).start()

    @pl.when((step == I3) & jnp.logical_not(is_leaf))
    def _():
        pl.semaphore_wait(ready, I1)
        for m in reversed(range(micro)):
            remote(dx.at[m], block(m), send_sems.at[I1], parent_sem.at[m], along_x).start()
            to_sibling(m, dx.at[m])
        pltpu.make_async_copy(dx, bounce, here_sem).start()

    @pl.when((step == I4) & jnp.logical_not(is_leaf))
    def _():
        pltpu.make_async_copy(dx, bounce, here_sem).wait()
        for m in range(micro):
            pltpu.make_async_copy(bounce.at[m], block(m), here_sem).start()

    for t, og in enumerate((og_same, og_other)):
        @pl.when((step == I3 * t) & takes_g)
        def _(t=t, og=og):
            part = og.at[I0:len(late)]
            remote(part, part, og_sems.at[t], og_sems.at[I2 + t], place.across).wait_recv()

    @pl.when((step == last) & is_leaf)
    def _():
        for m in reversed(range(micro)):
            remote(block(m), block(m), send_sems.at[I0], parent_sem.at[m], place.sibling).wait_recv()
            to_sibling(m, block(m))

    @pl.when(step == last)
    def _():
        remote(dx, dx, send_sems.at[I0], sib_sem, place.sibling).wait_send()

        @pl.when(jnp.logical_not(is_leaf))
        def _():
            remote(dx, dx, send_sems.at[I1], sib_sem, place.sibling).wait_send()
            pltpu.make_async_copy(dx, dx, here_sem).wait()

        @pl.when(gives_g)
        def _():
            for t, og in enumerate((og_same, og_other)):
                part = og.at[I0:len(late)]
                remote(part, part, og_sems.at[t], og_sems.at[I2 + t], place.across).wait_send()
        remote(dx, dx, send_sems.at[I0], sib_sem, place.sibling).wait_recv()


def owner_backward_kernel(dims, dx, ds, do, u, qkv, wo, wd, gs_in, go_in, dqkv, dup, z, d_in, og_same, og_other,
                          dmid, gbuf, dctx, wobuf, bounce, sem, g_sem, here_sem, parent_sem, sib_sem, send_sems, og_sems, ready):
    micro, seq, width, heads, head_dim, ffn = dims
    half = heads // I2 * HEAD_PAD
    scale = head_dim ** -0.5
    step, steps = pl.program_id(I0), pl.num_programs(I0)
    spread_dx(step, steps - I1, dx, d_in, og_same, og_other, bounce, here_sem, parent_sem, sib_sem, send_sems, og_sems, ready)

    def g_load(n, start):
        rows = BLOCK // seq
        for og, low in ((og_same, I0), (og_other, steps // I2)):
            @pl.when((n >= low) & (n < low + steps // I2))
            def _(og=og, low=low):
                copy = pltpu.make_async_copy(og.at[pl.ds((n - low) * rows, rows)], gbuf.at[n % I2], g_sem.at[n % I2])
                copy.start() if start else copy.wait()

    @pl.when(step == I0)
    def _():
        g_load(step, True)
        wobuf[...] = jnp.zeros_like(wobuf)
        load_heads(wo, I0, wobuf, sem)
        pltpu.make_async_copy(wo, wobuf.at[I0:wo.shape[I0]], sem).wait()
    g_load(step + I1, True)

    @pl.when(step < steps // I2)
    def _():
        dmid[...] = ds[...]

    @pl.when(step >= steps // I2)
    def _():
        dmid[...] = do[...]

    def ctx_step(j, c):
        rows = pl.ds(pl.multiple_of(j * SUB, SUB), SUB)
        dctx[:, lanes(j * SUB, SUB)] = mm_nt(dmid[...], wobuf[rows, :]).astype(BF)
        return c
    lax.fori_loop(I0, half // SUB, ctx_step, I0)
    g_load(step, False)
    grad = gbuf.at[step % I2]

    def mlp_block(n):
        rows = pl.ds(pl.multiple_of(n * SUB, SUB), SUB)
        cols = lanes(n * SUB, SUB)
        dz = mm_nt(grad[...].reshape(BLOCK, width), wd[rows, :]).astype(BF).astype(F32)
        up = u[:, cols].astype(F32)
        gate, up2 = gelu_gate(up)
        hidden = up * gate
        z[:, cols] = hidden.astype(BF)
        dup[:, cols] = (dz * gelu_slope(hidden, gate, up2)).astype(BF)

    def both_step(j, c):
        base = j * (I2 * HEAD_PAD)
        at = [(pl.ds(s, seq), base + r * HEAD_PAD) for s in range(I0, BLOCK, seq) for r in range(I2)]
        group = [(*(qkv[rows, lanes(t * half + col, HEAD_PAD)] for t in range(I3)), dctx[rows, lanes(col, HEAD_PAD)]) for rows, col in at]
        blocks = [functools.partial(mlp_block, j * I3 + r) for r in range(I3)]
        for (rows, col), grads in zip(at, attention_backward(group, scale, blocks)):
            for t, value in enumerate(grads):
                dqkv[rows, lanes(t * half + col, HEAD_PAD)] = value
        return c
    lax.fori_loop(I0, heads // I4, both_step, I0)


def owner_backward(dims, dx, d_rows, og, ups, qkv, own):
    micro, seq, width, heads, head_dim, ffn = dims
    half = heads // I2 * HEAD_PAD
    tokens = I2 * micro * seq
    blocks = tokens // BLOCK
    vmem, dma = pltpu.VMEM, pltpu.SemaphoreType.DMA
    any_spec = pl.BlockSpec(memory_space=ANY)
    low = pl.BlockSpec((BLOCK, width), lambda i: (jnp.minimum(i, blocks // I2 - I1), I0))
    high = pl.BlockSpec((BLOCK, width), lambda i: (jnp.maximum(i - blocks // I2, I0), I0))
    attn_block = pl.BlockSpec((BLOCK, I3 * half), lambda i: (i, I0))
    mlp_block = pl.BlockSpec((BLOCK, ffn // I2), lambda i: (i, I0))
    act = (micro, seq, width)
    return pl.pallas_call(
        functools.partial(owner_backward_kernel, dims),
        grid=(blocks,),
        out_shape=tuple(shapes((tokens, I3 * half), (tokens, ffn // I2), (tokens, ffn // I2), (micro, I2, seq, width), act, act)),
        in_specs=[any_spec, low, high, mlp_block, attn_block, any_spec, pl.BlockSpec((ffn // I2, width), lambda i: (I0, I0)), any_spec, any_spec],
        out_specs=(attn_block, mlp_block, mlp_block, any_spec, any_spec, any_spec),
        scratch_shapes=[vmem((BLOCK, width), BF), vmem((I2, BLOCK // seq, seq, width), BF), vmem((BLOCK, half), BF), vmem((half, width), BF), vmem(act, BF),
                        dma(()), dma((I2,)), dma(()), dma((micro,)), dma(()), dma((I2,)), dma((I4,)), pltpu.SemaphoreType.REGULAR],
        input_output_aliases={7: I4, I8: 5},
        compiler_params=pltpu.CompilerParams(collective_id=I2, has_side_effects=True, vmem_limit_bytes=VMEM_LIMIT),
        name='owner_backward',
    )(dx, *d_rows, ups, qkv, own[I1], own[I3], *og)


def bring(pairs, sem):
    copies = [pltpu.make_async_copy(src, dst, sem.at[i]) for i, (src, dst) in enumerate(pairs)]
    for copy in copies:
        copy.start()
    for copy in copies:
        copy.wait()


def attn_products_kernel(dq, dk, dv, ctx, n1_o, ds, do, dx_in, dwq, dwo, dx_out, n1, dmid, dqkvt, ctxt, bounce, sem, dx_sem):
    tokens, width = n1.shape
    part = tokens // I2
    head_dim = dwo.shape[I1]
    step, last = pl.program_id(I0), pl.num_programs(I0) - I1
    into, out_of = pltpu.make_async_copy(dx_in, bounce, dx_sem), pltpu.make_async_copy(bounce, dx_out, dx_sem)

    @pl.when(step == I1)
    def _():
        into.start()

    @pl.when(step == I2)
    def _():
        into.wait()
        out_of.start()

    @pl.when(step == last)
    def _():
        out_of.wait()

    @pl.when(step == I0)
    def _():
        bring([(n1_o, n1), (ds, dmid.at[pl.ds(I0, part)]), (do, dmid.at[pl.ds(part, part)])], sem)

    def turn(rows):
        for t, block in enumerate((dq, dk, dv)):
            for r in range(I2):
                at = (I2 * t + r) * head_dim
                dqkvt[at:at + head_dim, rows] = block[rows, r * HEAD_PAD:(r + I1) * HEAD_PAD].T[I0:head_dim]
        for r in range(I2):
            ctxt[r * head_dim:(r + I1) * head_dim, rows] = ctx[rows, r * HEAD_PAD:(r + I1) * HEAD_PAD].T[I0:head_dim]
    rows_loop(tokens, SUB, turn)
    for c in range(I0, width, SUB):
        cut = slice(c, c + SUB)
        dwq[:, :, :, cut] = mm(dqkvt[...], n1[:, cut]).reshape(I3, I2, head_dim, SUB)
        dwo[:, :, cut] = mm(ctxt[...], dmid[:, cut]).reshape(I2, head_dim, SUB)


def attn_products(dqkv, ctx, n1, d_rows, dx, out_dims):
    heads, head_dim, width = out_dims
    tokens = n1.shape[I0]
    vmem = pltpu.VMEM
    any_spec = pl.BlockSpec(memory_space=ANY)
    pairs = heads // I2
    cols = lambda t: pl.BlockSpec((tokens, I2 * HEAD_PAD), lambda i: (I0, t * pairs + i))
    return pl.pallas_call(
        attn_products_kernel,
        grid=(pairs,),
        out_shape=(jax.ShapeDtypeStruct((I3,) + out_dims, F32), jax.ShapeDtypeStruct(out_dims, F32), jax.ShapeDtypeStruct(dx.shape, BF)),
        in_specs=[cols(I0), cols(I1), cols(I2), cols(I0), any_spec, any_spec, any_spec, any_spec],
        out_specs=(pl.BlockSpec((I3, I2, head_dim, width), lambda i: (I0, i, I0, I0)), pl.BlockSpec((I2, head_dim, width), lambda i: (i, I0, I0)), any_spec),
        scratch_shapes=[vmem((tokens, width), BF), vmem((tokens, width), BF), vmem((I6 * head_dim, tokens), BF), vmem((I2 * head_dim, tokens), BF),
                        vmem(dx.shape, BF), pltpu.SemaphoreType.DMA((I3,)), pltpu.SemaphoreType.DMA(())],
        compiler_params=pltpu.CompilerParams(vmem_limit_bytes=VMEM_LIMIT),
        name='attn_products',
    )(dqkv, dqkv, dqkv, ctx, n1, *d_rows, dx)


def mlp_products_kernel(dup, z, n2_o, gs, go, dwu, dwd, n2t, grad, zt, stage, sem):
    width, tokens = n2t.shape
    part = tokens // I2

    @pl.when(pl.program_id(I0) == I0)
    def _():
        bring([(n2_o, stage), (gs, grad.at[pl.ds(I0, part)]), (go, grad.at[pl.ds(part, part)])], sem)

        def turn(rows):
            for c in range(I0, width, SUB):
                n2t[c:c + SUB, rows] = stage[rows, c:c + SUB].T
        rows_loop(tokens, SUB, turn)

    def turn_z(rows):
        for c in range(I0, z.shape[I1], SUB):
            zt[c:c + SUB, rows] = z[rows, c:c + SUB].T
    rows_loop(tokens, SUB, turn_z)
    for c in range(I0, width, I2 * SUB):
        dwu[c:c + I2 * SUB, :] = mm(n2t[c:c + I2 * SUB, :], dup[...])
    for c in range(I0, width, SUB):
        dwd[:, c:c + SUB] = mm(zt[...], grad[:, c:c + SUB])


def mlp_products(dup, hidden, n2, g_rows):
    tokens, width = n2.shape
    cols = dup.shape[I1]
    vmem = pltpu.VMEM
    any_spec = pl.BlockSpec(memory_space=ANY)
    block = pl.BlockSpec((tokens, SUB), lambda i: (I0, i))
    return pl.pallas_call(
        mlp_products_kernel,
        grid=(cols // SUB,),
        out_shape=(jax.ShapeDtypeStruct((width, cols), F32), jax.ShapeDtypeStruct((cols, width), F32)),
        in_specs=[block, block, any_spec, any_spec, any_spec],
        out_specs=(pl.BlockSpec((width, SUB), lambda i: (I0, i)), pl.BlockSpec((SUB, width), lambda i: (i, I0))),
        scratch_shapes=[vmem((width, tokens), BF), vmem((tokens, width), BF), vmem((SUB, tokens), BF), vmem((tokens, width), BF), pltpu.SemaphoreType.DMA((I3,))],
        compiler_params=pltpu.CompilerParams(vmem_limit_bytes=VMEM_LIMIT),
        name='mlp_products',
    )(dup, hidden, n2, *g_rows)


def solution(mesh):
    act_spec = P('rep', None, None, None)
    weight_specs = (
        P(('rep', 'stage'), None, None, 'tp', None),
        P(('rep', 'stage'), 'tp', None, None),
        P(('rep', 'stage'), None, 'tp'),
        P(('rep', 'stage'), 'tp', None),
        P(('rep', 'stage'), None),
        P(('rep', 'stage'), None),
    )

    def device_fn(inputs, targets, w_qkv, w_out, w_up, w_down, gain_attn, gain_mlp):
        micro_count, _, seq_len, width = inputs.shape
        dims = (micro_count, seq_len, width, I2 * w_out.shape[I1], w_out.shape[I2], I2 * w_up.shape[I2])
        norm_factor = 1.0 / (inputs.size)
        own = (w_qkv[I0], w_out[I0], w_up[I0], w_down[I0])
        own_gains = jnp.concatenate([gain_attn, gain_mlp]).astype(F32)
        rows_of = (own[I0].transpose(I1, I2, I3, I0).reshape(-I1, width), own[I1].reshape(-I1, width), own[I2], own[I3])

        (acts, mids, qkv, ups, seeds, oh_same, oh_other, oa_same, oa_other, og_same, og_other, loss_tile, home_gains, *weights) = forward_phase(dims, inputs, targets, rows_of, own_gains)
        (nq, no, nu, nd), (fq, fo, fu, fd) = weights[I0:I4], weights[I4:I8]
        (tq0, to0, tu0, td0), (tq1, to1, tu1, td1) = weights[I8:12], weights[12:16]

        flat = lambda *rows: [r.reshape(-I1, width) for r in rows]
        done, *again = owner_recompute(dims, True, None, flat(oh_same, oh_other), flat(oa_same, oa_other), own_gains, rows_of)
        dx, _, od_same, od_other, og_same, og_other, oa_same, oa_other, oh_same, oh_other, dg_same, dg_other, loss_all = backward_phase(
            dims, (acts, mids, qkv, ups, seeds), (rows_of[I0], nq, fq, td0, td1, to0, to1, tu0, tu1), home_gains, loss_tile, done,
            (og_same, og_other, oa_same, oa_other, oh_same, oh_other))
        _, *again = owner_recompute(dims, False, again, flat(oh_same, oh_other), flat(oa_same, oa_other), own_gains, rows_of)
        ups_own, qkv_own, ctx_own, n1, n2 = again
        d_rows = flat(od_same, od_other)
        d_qkv_rows, d_up_rows, hidden, dx_all, og_same, og_other = owner_backward(dims, dx, d_rows, (og_same, og_other), ups_own, qkv_own, rows_of)
        d_qkv, d_out, d_inputs = attn_products(d_qkv_rows, ctx_own, n1, d_rows, dx_all, w_out.shape[I1:])
        d_up, d_down = mlp_products(d_up_rows, hidden, n2, flat(og_same, og_other))
        weight_grads = (d_qkv.transpose(I3, I0, I1, I2), d_out, d_up, d_down)
        mine = jnp.sum(dg_same + dg_other, I1)
        loss = jnp.sum(loss_all) * (0.5 * norm_factor)

        return (loss.reshape(I1), d_inputs) + tuple(g[None] for g in weight_grads) + (mine[I0][None], mine[I1][None])

    return jax.shard_map(device_fn, mesh=mesh, in_specs=(act_spec, act_spec) + weight_specs, out_specs=(P('rep'), act_spec) + weight_specs, check_vma=False)
```

```python
import functools

import jax
import jax.numpy as jnp
from jax import lax
from jax.experimental import pallas as pl
from jax.experimental.pallas import tpu as pltpu
from jax.sharding import PartitionSpec as P

NORM_EPS = 1e-5
BF = jnp.bfloat16
F32 = jnp.float32
MESH = pl.DeviceIdType.MESH
ANY = pl.ANY


GELU_A = 0.7978845608028654
GELU_B = 0.044715
I0, I1, I2, I3, I4, I6, I8 = 0, 1, 2, 3, 4, 6, 8
CHUNK = 1024
BLOCK = 384
SUB = 256
DEPTH = 6
BACK_DEPTH = 5
KDEPTH = 3
EARLY_G = 3
STAGGER_NS = 6000
EARLY_SEEDS = 5
EARLY_DX = 3
HEAD_PAD = 128
VMEM_LIMIT = 67043328


def mm(a, b):
    return lax.dot_general(a, b, (((I1,), (I0,)), ((), ())), preferred_element_type=F32)


def mm_nt(a, b):
    return lax.dot_general(a, b, (((I1,), (I1,)), ((), ())), preferred_element_type=F32)


def mm_tn(a, b):
    return lax.dot_general(a, b, (((I0,), (I0,)), ((), ())), preferred_element_type=F32)


class Place:
    def __init__(self):
        self.tp = lax.axis_index('tp')
        self.stage = lax.axis_index('stage')
        self.core = self.stage % I2
        self.x_pos = self.stage // I2
        self.home = self.x_pos * (I3 - I2 * self.tp) + self.tp
        self.is_l = self.stage == self.home
        self.sib = self.stage + I1 - I2 * self.core

    def at(self, tp, stage):
        return {'tp': tp, 'stage': stage}

    @property
    def sibling(self):
        return self.at(self.tp, self.sib)

    @property
    def along_x(self):
        return self.at(self.tp, (self.stage + I2) % I4)

    @property
    def across(self):
        return self.at(I1 - self.tp, self.stage)

    @property
    def across_other(self):
        return self.at(I1 - self.tp, self.sib)

    def chain(self, delta):
        there = self.home + delta
        x_pos = there // I2
        tp = there % I2 + x_pos * (I1 - I2 * (there % I2))
        return self.at(tp, I2 * x_pos + self.core)


def entry_barrier(place):
    barrier = pltpu.get_barrier_semaphore()
    for d_tp in (I0, I1):
        for d_stage in range(I4):
            if d_tp or d_stage:
                tp = place.tp + d_tp - I2 * d_tp * place.tp
                stage = (place.stage + d_stage) % I4
                pl.semaphore_signal(barrier, inc=I1, device_id=place.at(tp, stage), device_id_type=MESH)
    pl.semaphore_wait(barrier, 7)


def remote(src, dst, send_sem, recv_sem, device_id):
    return pltpu.make_async_remote_copy(src_ref=src, dst_ref=dst, send_sem=send_sem, recv_sem=recv_sem, device_id=device_id, device_id_type=MESH)


def rows_loop(total, step, body):
    def run(i, carry):
        body(pl.ds(pl.multiple_of(i * step, step), step))
        return carry
    lax.fori_loop(I0, total // step, run, I0)


def norm_rows(src, gain_row, dst, total):
    def body(rows):
        v = src[rows, :].astype(F32)
        inv = lax.rsqrt(jnp.mean(v * v, axis=-I1, keepdims=True) + NORM_EPS)
        dst[rows, :] = (v * inv * gain_row).astype(BF)
    rows_loop(total, 32, body)


def gelu_gate(u):
    u2 = u * u
    t = jnp.tanh(u * (GELU_A + (GELU_A * GELU_B) * u2))
    return 0.5 * t + 0.5, u2


def gelu_slope(hidden, gate, u2):
    return gate + hidden * (1.0 - gate) * (2.0 * GELU_A + (6.0 * GELU_A * GELU_B) * u2)


def row_parts(heads, cut=128):
    return [(*(x[low:high] for x in queries), *(x[:high] for x in keys), low)
            for queries, keys in heads for low, high in ((I0, cut), (cut, queries[I0].shape[I0]))]


def softmax_parts(scores, starts, keys_axis):
    masked = []
    for s, start in zip(scores, starts):
        k_pos = lax.broadcasted_iota(jnp.int32, s.shape, keys_axis)
        q_pos = lax.broadcasted_iota(jnp.int32, s.shape, I1 - keys_axis) + start
        masked.append(jnp.where(k_pos <= q_pos, s, -1e30))
    tops = [jnp.max(s, axis=keys_axis, keepdims=True) for s in masked]
    powers = [jnp.exp(s - top) for s, top in zip(masked, tops)]
    scales = [1.0 / jnp.sum(e, axis=keys_axis, keepdims=True) for e in powers]
    return [e * r for e, r in zip(powers, scales)]


def join_keys(top, low, cut=128):
    return jnp.concatenate([top + low[:cut], low[cut:]], I0).astype(BF)


def attention_forward(heads, scale):
    units = row_parts([((q,), (k, v)) for q, k, v in heads])
    probs = softmax_parts([mm_nt(q, k) * scale for q, k, _, _ in units], [u[-I1] for u in units], I1)
    parts = [mm(p.astype(BF), u[I2]) for p, u in zip(probs, units)]
    return [jnp.concatenate([a, b], I0).astype(BF) for a, b in zip(parts[I0::I2], parts[I1::I2])]


def nothing():
    pass


def attention_backward(heads, scale, between=()):
    work = iter(between)
    units = row_parts([((q, dc), (k, v)) for q, k, v, dc in heads])
    scores = [mm_nt(k, q) * scale for q, _, k, _, _ in units]
    dps = [mm_nt(v, dc) for _, dc, _, v, _ in units]
    next(work, nothing)()
    probs = softmax_parts(scores, [u[-I1] for u in units], I0)
    next(work, nothing)()
    dps = [dp.astype(BF).astype(F32) for dp in dps]
    deltas = [jnp.sum(dp * p, axis=I0, keepdims=True) for dp, p in zip(dps, probs)]
    dss = [p * (dp - delta) * scale for p, dp, delta in zip(probs, dps, deltas)]
    terms = []
    for ds in dss:
        hi = ds.astype(BF)
        rest = ds - hi.astype(F32)
        lo = rest.astype(BF)
        terms.append((hi, lo, (rest - lo.astype(F32)).astype(BF)))
    next(work, nothing)()
    dvs = [mm(p.astype(BF), u[I1]) for p, u in zip(probs, units)]
    dks = [mm(hi, u[I0]) + (mm(lo, u[I0]) + mm(tail, u[I0])) for (hi, lo, tail), u in zip(terms, units)]
    k_turned = [u[I2].T for u in units]
    dqs = [(mm(kt, hi) + (mm(kt, lo) + mm(kt, tail))).astype(BF) for (hi, lo, tail), kt in zip(terms, k_turned)]
    return [(jnp.concatenate([dqs[i].T, dqs[i + I1].T], I0), join_keys(dks[i], dks[i + I1]), join_keys(dvs[i], dvs[i + I1]))
            for i in range(I0, len(units), I2)]


def blocked(rows, stack, cols):
    total = mm(rows[:, I0:CHUNK], stack[I0, :, cols])
    for j in range(I1, stack.shape[I0]):
        total = total + mm(rows[:, j * CHUNK:(j + I1) * CHUNK], stack[j, :, cols])
    return total


def lanes(offset, size):
    return pl.ds(pl.multiple_of(offset, 128), size)


def load_resident(buf, sem, halves):
    for c in range(I6):
        for condition, ref in halves[c // I3]:
            copy = pltpu.make_async_copy(ref.at[(c % I3) * CHUNK:(c % I3 + I1) * CHUNK, :], buf.at[c], sem.at[c])
            if condition is None:
                copy.start()
            else:
                pl.when(condition)(copy.start)


def load_heads(ref, index, dst, sem):
    for r in range(I8):
        rows = pl.ds(pl.multiple_of(index * 768 + r * 96, 96), 96)
        pltpu.make_async_copy(ref.at[rows, :], dst.at[r * 128:r * 128 + 96, :], sem).start()


class Stream:
    def __init__(self, buf, sem, depth, parts, total, by_heads):
        self.buf, self.sem, self.depth, self.parts, self.total, self.by_heads = buf, sem, depth, parts, total, by_heads
        self.per_tick = sum(p[I1] for p in parts)

    def copy_in(self, ref, index, slot):
        if not self.by_heads:
            pltpu.make_async_copy(ref.at[index], self.buf.at[slot], self.sem.at[slot]).start()
            return
        load_heads(ref, index, self.buf.at[slot], self.sem.at[slot])

    def start(self, seq):
        @pl.when(seq < self.total)
        def _():
            j = seq % self.per_tick
            slot = seq % self.depth
            base = I0
            for choices, chunks in self.parts:
                for condition, ref in choices:
                    here = (j >= base) & (j < base + chunks)
                    here = here if condition is None else here & condition

                    @pl.when(here)
                    def _(ref=ref, low=base):
                        self.copy_in(ref, j - low, slot)
                base += chunks

    def prime(self):
        for seq in range(self.depth):
            self.start(jnp.int32(seq))

    def wait(self, seq):
        slot = seq % self.depth
        ref = self.parts[I0][I0][I0][I1]
        if self.by_heads:
            pltpu.make_async_copy(ref.at[I0:768, :], self.buf.at[slot, I0:768, :], self.sem.at[slot]).wait()
        else:
            pltpu.make_async_copy(ref.at[I0], self.buf.at[slot], self.sem.at[slot]).wait()
        return self.buf.at[slot]


PIECES = [(0, 0, 0), (0, 0, 1), (0, 0, 2), (1, 0, 0), (2, 1, 0), (2, 1, 1), (2, 1, 2), (2, 1, 3), (3, 0, 0), (3, 0, 1), (3, 0, 2), (3, 0, 3)]


ROUND = (11,)
ROUND_STEPS = (1,)
ORDER = (0, 1, 2, 3, 4, 5, 6, 7, 11, 8, 9, 10)


def piece(ref, axis, index):
    return ref.at[index * 768:(index + I1) * 768, :] if axis == I0 else ref.at[:, index * 768:(index + I1) * 768]


def weight_phase(place, is_r, own, near, far, turned, up_chunks, wn, wk, send_sem, y_send, d_send, near_sem, far_sem, load_sem, store_sem, chunk_sem,
                 round_a, round_b, ra_sem, rb_sem, x_send, xd_send, rs_send):
    wk[...] = jnp.zeros_like(wk)
    early = place.home < I2

    def piece_of(arrays, c):
        i, axis, index = PIECES[c]
        return piece(arrays[i], axis, index)

    @pl.when(place.is_l)
    def _():
        for i in range(I4):
            remote(own[i], near[i], send_sem.at[i], near_sem.at[i], place.sibling).start()

    @pl.when(is_r)
    def _():
        for k, c in enumerate(ROUND):
            @pl.when(early)
            def _(k=k, c=c):
                remote(piece_of(own, c), round_a.at[k], x_send.at[k], ra_sem.at[k], place.along_x).start()
        for c, (i, axis, index) in enumerate(PIECES):
            if c not in ROUND:
                remote(piece_of(own, c), piece_of(far, c), y_send.at[i], far_sem.at[c], place.across_other).start()
        for k, c in enumerate(ROUND):
            @pl.when(jnp.logical_not(early))
            def _(k=k, c=c):
                remote(piece_of(own, c), piece_of(far, c), x_send.at[k], far_sem.at[c], place.across_other).start()

    def load(i, refs, t, slot):
        for condition, ref in refs:
            def go(ref=ref):
                if i < I2:
                    for r in range(I2):
                        rows = pl.ds(pl.multiple_of(t * 192 + r * 96, 96), 96)
                        pltpu.make_async_copy(ref.at[rows, :], wk.at[I0, pl.ds(slot * SUB + r * 128, 96), :], load_sem.at[slot]).start()
                elif i == I2:
                    pltpu.make_async_copy(ref.at[:, lanes(t * SUB, SUB)], wn.at[slot, :, I0:SUB], load_sem.at[slot]).start()
                else:
                    rows = pl.ds(pl.multiple_of(t * SUB, SUB), SUB)
                    pltpu.make_async_copy(ref.at[rows, :], wk.at[I0, pl.ds(512 + slot * SUB, SUB), :], load_sem.at[slot]).start()
            if condition is None:
                go()
            else:
                pl.when(condition)(go)

    def loaded(i, refs, slot):
        ref = refs[I0][I1]
        if i < I2:
            pltpu.make_async_copy(ref.at[I0:192, :], wk.at[I0, I0:192, :], load_sem.at[slot]).wait()
        elif i == I2:
            pltpu.make_async_copy(ref.at[:, I0:SUB], wn.at[slot, :, I0:SUB], load_sem.at[slot]).wait()
        else:
            pltpu.make_async_copy(ref.at[I0:SUB, :], wk.at[I0, 512:768, :], load_sem.at[slot]).wait()

    def store(i, dst, t, slot):
        if i == I2:
            rows = pl.ds(pl.multiple_of(t * SUB, SUB), SUB)
            return pltpu.make_async_copy(wk.at[I1, pl.ds(slot * SUB, SUB), :], dst.at[rows, :], store_sem.at[slot])
        return pltpu.make_async_copy(wn.at[slot, :, SUB:512], dst.at[t // I4, :, lanes(t % I4 * SUB, SUB)], store_sem.at[slot])

    def keep(which, t, slot):
        return pltpu.make_async_copy(wn.at[slot, :, I0:SUB], up_chunks[which].at[t // I4, :, lanes(t % I4 * SUB, SUB)], chunk_sem.at[slot])

    def turn(i, refs, which, first, count):
        dst = turned[i][which]
        load(i, refs, first, I0)

        def step(n, c):
            slot = n % I2

            if i == I2:
                @pl.when(n > I0)
                def _():
                    keep(which, first + n - I1, I1 - slot).wait()

            @pl.when(n + I1 < count)
            def _():
                load(i, refs, first + n + I1, I1 - slot)
            loaded(i, refs, slot)
            if i == I2:
                keep(which, first + n, slot).start()

            @pl.when(n >= I2)
            def _():
                store(i, dst, first + n - I2, slot).wait()
            for b in range(I6):
                cut = slice(b * SUB, b * SUB + SUB)
                if i == I2:
                    wk[I1, pl.ds(pl.multiple_of(slot * SUB, SUB), SUB), cut] = wn[slot, cut, I0:SUB].T
                else:
                    base = I0 if i < I2 else 512
                    wn[slot, cut, SUB:512] = wk[I0, pl.ds(pl.multiple_of(base + slot * SUB, SUB), SUB), cut].T
            store(i, dst, first + n, slot).start()
            return c
        lax.fori_loop(I0, count, step, I0)
        for n in (count - I2, count - I1):
            store(i, dst, first + n, n % I2).wait()
        if i == I2:
            keep(which, first + count - I1, (count - I1) % I2).wait()

    counts = (12, I4, 12, 12)
    for i in range(I4):
        @pl.when(is_r)
        def _(i=i):
            remote(near[i], near[i], send_sem.at[i], near_sem.at[i], place.sibling).wait_recv()
        turn(i, [(place.is_l, own[i]), (is_r, near[i])], I0, I0, counts[i])
        if i < len(ROUND):
            @pl.when(place.is_l & jnp.logical_not(early))
            def _(k=i):
                remote(round_a.at[k], round_a.at[k], rs_send.at[k], ra_sem.at[k], place.sibling).wait_recv()
                remote(round_a.at[k], round_b.at[k], rs_send.at[k], rb_sem.at[k], place.across).start()
    for c in ORDER:
        i, axis, index = PIECES[c]
        view = piece_of(far, c)
        for k, step in enumerate(ROUND_STEPS):
            if c == step:
                @pl.when(is_r & jnp.logical_not(early))
                def _(k=k):
                    remote(round_b.at[k], round_b.at[k], rs_send.at[k], rb_sem.at[k], place.sibling).wait_recv()
                    remote(round_b.at[k], piece_of(far, ROUND[k]), rs_send.at[k], far_sem.at[ROUND[k]], place.along_x).start()
        remote(view, view, d_send.at[i], far_sem.at[c], place.sibling).wait_recv()
        gives = is_r
        sem = d_send.at[i]
        if c in ROUND:
            gives = (early & place.is_l) | (jnp.logical_not(early) & is_r)
            sem = xd_send.at[ROUND.index(c)]

        @pl.when(gives)
        def _(c=c, view=view, sem=sem):
            remote(view, view, sem, far_sem.at[c], place.sibling).start()
        count = I4 if i < I2 else I3
        turn(i, [(None, far[i])], I1, index * count, count)

    @pl.when(place.is_l)
    def _():
        for i in range(I4):
            remote(own[i], near[i], send_sem.at[i], near_sem.at[i], place.sibling).wait_send()

    @pl.when(is_r)
    def _():
        for i in range(I4):
            part = own[i] if i < I3 else own[i].at[I0:(I4 - len(ROUND)) * 768, :]
            remote(part, part, y_send.at[i], far_sem.at[I0], place.across_other).wait_send()
            remote(part, part, d_send.at[i], far_sem.at[I0], place.sibling).wait_send()
        for k in range(len(ROUND)):
            remote(round_a.at[k], round_a.at[k], x_send.at[k], far_sem.at[I0], place.sibling).wait_send()

    @pl.when((early & place.is_l) | (jnp.logical_not(early) & is_r))
    def _():
        for k in range(len(ROUND)):
            remote(round_a.at[k], round_a.at[k], xd_send.at[k], far_sem.at[I0], place.sibling).wait_send()

    @pl.when(jnp.logical_not(early))
    def _():
        for k in range(len(ROUND)):
            remote(round_a.at[k], round_a.at[k], rs_send.at[k], far_sem.at[I0], place.sibling).wait_send()


def near_choices(place, own, near):
    return [(place.is_l, own), (jnp.logical_not(place.is_l), near)]


def forward_kernel(dims, x_ref, y_ref, wq, wo, wu, wd, own_gains,
                   a_s, h_s, qkv_s, u_s, g_s, oh_same, oh_other, oa_same, oa_other, og_same, og_other, loss_s, home_gains,
                   nq, no, nu, nd, fq, fo, fu, fd, tq0, to0, tu0, td0, tq1, to1, tu1, td1, uc0, uc1, round_a, round_b,
                   abuf, hbuf, obuf, nbuf, ybuf, sbuf, qkvbuf, ubuf, zbuf, ctxbuf, lossbuf, losstile, gains, wres, wores, wn,
                   send_sem, y_send, d_send, near_sem, far_sem, t_load, t_store, t_keep, ra_sem, rb_sem, x_send, xd_send, rs_send,
                   act_sem, hop_f, keep_sem, save_sem, stream_n, res_sem, out_sem, big_sem, y_sem, s_sem,
                   os_sem, oo_sem, as_sem, ao_sem, gs_sem, go_sem, bulk, gain_sem, tiny):
    micro, seq, width, heads, head_dim, ffn = dims
    place = Place()
    is_first, is_last = place.home == I0, place.home == I3
    home02 = (place.home == I0) | (place.home == I2)
    home13 = jnp.logical_not(home02)
    is_r = jnp.logical_not(place.is_l)
    takes_x = (place.home == I1) & is_r
    half = heads // I2 * HEAD_PAD
    scale = head_dim ** -0.5
    norm_factor = 1.0 / (micro * I2 * seq * width)
    own, near, far = (wq, wo, wu, wd), (nq, no, nu, nd), (fq, fo, fu, fd)
    turned = ((tq0, tq1), (to0, to1), (tu0, tu1), (td0, td1))
    entry_barrier(place)

    @pl.when(place.is_l)
    def _():
        pltpu.make_async_copy(own_gains, gains, gain_sem.at[I0]).start()
        remote(own_gains, gains, gain_sem.at[I1], gain_sem.at[I0], place.sibling).start()

    @pl.when(is_first)
    def _():
        for m in range(micro):
            pltpu.make_async_copy(x_ref.at[m, place.core], abuf.at[m], act_sem.at[m]).start()
    weight_phase(place, is_r, own, near, far, turned, (uc0, uc1), wn, wores, send_sem, y_send, d_send, near_sem, far_sem, t_load, t_store, t_keep,
                 round_a, round_b, ra_sem, rb_sem, x_send, xd_send, rs_send)
    pltpu.make_async_copy(own_gains, gains, gain_sem.at[I0]).wait()
    pltpu.make_async_copy(gains, home_gains, gain_sem.at[I0]).start()

    @pl.when(place.is_l)
    def _():
        remote(own_gains, gains, gain_sem.at[I1], gain_sem.at[I0], place.sibling).wait_send()

    def near_of(i):
        return near_choices(place, own[i], near[i])

    def saved(dst, index):
        return pltpu.make_async_copy(hbuf, dst, save_sem.at[index])

    sn = Stream(wn, stream_n, DEPTH, [([(None, tq0)], I3), ([(None, tq1)], I3), ([(None, uc0)], I3), ([(None, uc1)], I3)], micro * 12, False)
    for c, choices in enumerate((near_of(I1), [(None, fo)])):
        for condition, ref in choices:
            def go(ref=ref, c=c):
                load_heads(ref, I0, wores.at[c], out_sem.at[c])
            go() if condition is None else pl.when(condition)(go)
    sn.prime()
    load_resident(wres, res_sem, (near_of(I3), [(None, fd)]))
    lossbuf[...] = jnp.zeros_like(lossbuf)

    def qkv_out(m):
        return pltpu.make_async_copy(qkvbuf, qkv_s.at[m], big_sem.at[I0])

    def up_out(m):
        return pltpu.make_async_copy(ubuf, u_s.at[m], big_sem.at[I1])

    def act_out(m):
        return pltpu.make_async_copy(abuf.at[m], a_s.at[m], save_sem.at[I2])

    def hop_block(m, n):
        cols = lanes(n * SUB, SUB)
        return remote(obuf.at[m % I2, :, cols], abuf.at[m, :, cols], hop_f.at[m % I2], act_sem.at[m], place.chain(I1))

    def hop_forward(m):
        return remote(obuf.at[m % I2], abuf.at[m], hop_f.at[m % I2], act_sem.at[m], place.chain(I1))

    def near_hand(src, dst_far, dst_own, sem, recv_sem):
        return (lambda: remote(src, dst_far, sem, recv_sem, place.sibling)), (lambda: pltpu.make_async_copy(src, dst_own, sem))

    def hand_out(m):
        return near_hand(obuf.at[m % I2], oa_other.at[m], oa_same.at[m], keep_sem.at[m % I2], ao_sem)

    def both_kinds(condition, copies, start):
        far_copy, own_copy = copies

        @pl.when(condition & place.is_l)
        def _():
            far_copy().start() if start else far_copy().wait_send()

        @pl.when(condition & is_r)
        def _():
            own_copy().start() if start else own_copy().wait()

    def x_out(m):
        return pltpu.make_async_copy(ybuf, oa_same.at[m], y_sem), pltpu.make_async_copy(sbuf, oa_other.at[m], s_sem)

    def seed_out(m):
        return pltpu.make_async_copy(sbuf, g_s.at[m], s_sem)

    def far_mid(m, condition):
        @pl.when(condition & place.is_l)
        def _():
            remote(h_s.at[m], oh_same.at[m], bulk.at[I2], os_sem, place.across).start()

        @pl.when(condition & is_r)
        def _():
            remote(h_s.at[m], oh_other.at[m], bulk.at[I2], oo_sem, place.across_other).start()

    def send_seed(m):
        seed_out(m).wait()

        @pl.when(place.is_l & (m < EARLY_SEEDS))
        def _():
            remote(g_s.at[m], og_same.at[m], bulk.at[I1], gs_sem, place.across).start()

        @pl.when(is_r & (m < EARLY_SEEDS))
        def _():
            remote(g_s.at[m], og_other.at[m], bulk.at[I1], go_sem, place.across_other).start()

    def forward_tick(m, carry):
        act, mid, out = abuf.at[m], hbuf, obuf.at[m % I2]
        pltpu.make_async_copy(x_ref.at[m, place.core], act, act_sem.at[m]).wait()
        act_out(m).start()

        @pl.when(place.is_l)
        def _():
            pltpu.make_async_copy(act, oa_same.at[m], as_sem).start()

        @pl.when(is_last)
        def _():
            pltpu.make_async_copy(y_ref.at[m, place.core], ybuf, y_sem).start()

        @pl.when(takes_x)
        def _():
            @pl.when(m > I0)
            def _():
                for copy in x_out(m):
                    copy.wait()
            for core, buf, sem in ((place.core, ybuf, y_sem), (I1 - place.core, sbuf, s_sem)):
                pltpu.make_async_copy(x_ref.at[m, core], buf, sem).start()
        norm_rows(act, gains[I0:I1, :], nbuf, seq)

        @pl.when(m > I0)
        def _():
            qkv_out(m).wait()

        def qkv_step(j, c):
            w = sn.wait(m * 12 + j)
            for n in range(I0, CHUNK, SUB):
                qkvbuf[:, lanes(j * CHUNK + n, SUB)] = mm(nbuf[...], w[:, n:n + SUB]).astype(BF)
            sn.start(m * 12 + j + DEPTH)
            return c
        lax.fori_loop(I0, I6, qkv_step, I0)
        qkv_out(m).start()
        act_out(m).wait()

        @pl.when(is_r)
        def _():
            remote(a_s.at[m], oa_other.at[m], bulk.at[I0], ao_sem, place.sibling).start()

        def head_step(i, c):
            base = i * (I3 * half)
            views = [[qkvbuf[:, lanes(base + t * half + r * HEAD_PAD, HEAD_PAD)] for t in range(I3)] for r in range(I8)]
            for r, context in enumerate(attention_forward(views, scale)):
                ctxbuf[:, lanes(i * half + r * HEAD_PAD, HEAD_PAD)] = context
            return c
        lax.fori_loop(I0, I2, head_step, I0)

        @pl.when(m == I0)
        def _():
            for c in range(I2):
                pltpu.make_async_copy(wo, wores.at[c, I0:768, :], out_sem.at[c]).wait()
        for n in range(I0, width, SUB):
            total = mm(ctxbuf[:, I0:half], wores[I0, :, n:n + SUB]) + mm(ctxbuf[:, half:I2 * half], wores[I1, :, n:n + SUB])
            mid[:, n:n + SUB] = (act[:, n:n + SUB].astype(F32) + total).astype(BF)
        saved(h_s.at[m], I0).start()

        @pl.when(place.is_l)
        def _():
            saved(oh_same.at[m], I1).start()
        norm_rows(mid, gains[I1:I2, :], nbuf, seq)

        @pl.when(m > I0)
        def _():
            up_out(m).wait()

        def up_step(j, c):
            w = sn.wait(m * 12 + I6 + j)
            for n in range(I0, CHUNK, SUB):
                u = mm(nbuf[...], w[:, n:n + SUB]).astype(BF)
                at = lanes(j * CHUNK + n, SUB)
                ubuf[:, at] = u
                uf = u.astype(F32)
                zbuf[:, at] = (uf * gelu_gate(uf)[I0]).astype(BF)
            sn.start(m * 12 + I6 + j + DEPTH)
            return c
        lax.fori_loop(I0, I6, up_step, I0)
        up_out(m).start()

        @pl.when((m > I1) & jnp.logical_not(is_last))
        def _():
            hop_forward(m).wait_send()

        both_kinds((m > I1) & home02, hand_out(m), False)

        @pl.when(m == I0)
        def _():
            for j in range(I6):
                pltpu.make_async_copy(wd.at[I0:CHUNK, :], wres.at[j], res_sem.at[j]).wait()

        def down_step(n, c):
            cols = lanes(n * SUB, SUB)
            out[:, cols] = (mid[:, cols].astype(F32) + blocked(zbuf, wres, cols)).astype(BF)

            @pl.when((n > I0) & jnp.logical_not(is_last))
            def _():
                hop_block(m, n - I1).start()
            return c
        lax.fori_loop(I0, width // SUB, down_step, I0)

        @pl.when(jnp.logical_not(is_last))
        def _():
            hop_block(m, width // SUB - I1).start()

        both_kinds(home02, hand_out(m), True)

        @pl.when(is_last)
        def _():
            pltpu.make_async_copy(y_ref.at[m, place.core], ybuf, y_sem).wait()

            @pl.when(m > I0)
            def _():
                send_seed(m - I1)

            def seed(rows):
                error = out[rows, :].astype(F32) - ybuf[rows, :].astype(F32)
                sbuf[rows, :] = (error * norm_factor).astype(BF)
                lossbuf[...] += jnp.sum((error * error).reshape(I4, I8, width), axis=I0)
            rows_loop(seq, 32, seed)
            seed_out(m).start()

        @pl.when(takes_x)
        def _():
            for core, buf, sem in ((place.core, ybuf, y_sem), (I1 - place.core, sbuf, s_sem)):
                pltpu.make_async_copy(x_ref.at[m, core], buf, sem).wait()
            for copy in x_out(m):
                copy.start()

        saved(h_s.at[m], I0).wait()

        @pl.when(place.is_l)
        def _():
            saved(oh_same.at[m], I1).wait()

        @pl.when(is_r)
        def _():
            remote(h_s.at[m], oh_other.at[m], bulk.at[I3], oo_sem, place.sibling).start()

        far_mid(m, home13 | (m % I2 == I1))
        return carry

    @pl.when(is_first & (place.core == I0))
    def _():
        pl.delay(STAGGER_NS)
    lax.fori_loop(I0, micro, forward_tick, I0)
    for m in range(I0, micro, I2):
        far_mid(m, is_first)

    @pl.when(is_last)
    def _():
        total = lossbuf[:, I0:128]
        for n in range(128, width, 128):
            total = total + lossbuf[:, n:n + 128]
        losstile[...] = total
        pltpu.make_async_copy(losstile, loss_s, tiny).start()
    for copy in (qkv_out(micro - I1), up_out(micro - I1)):
        copy.wait()

    @pl.when(jnp.logical_not(is_last))
    def _():
        for m in (micro - I2, micro - I1):
            hop_forward(m).wait_send()
    for m in (micro - I2, micro - I1):
        both_kinds(home02, hand_out(m), False)

    @pl.when(is_last)
    def _():
        seed_out(micro - I1).wait()
        pltpu.make_async_copy(losstile, loss_s, tiny).wait()

    @pl.when(takes_x)
    def _():
        for copy in x_out(micro - I1):
            copy.wait()
    pltpu.make_async_copy(gains, home_gains, gain_sem.at[I0]).wait()
    sent, got = drain(place)

    @pl.when(place.home != I2)
    def _():
        sent(h_s, bulk.at[I2])

    @pl.when(place.home == I2)
    def _():
        sent(h_s.at[I0:micro // I2], bulk.at[I2])

    @pl.when(place.is_l | jnp.logical_not(is_last))
    def _():
        got(oh_other, oo_sem)

    @pl.when(is_r & is_last)
    def _():
        got(oh_other.at[I0:micro // I2], oo_sem)

    @pl.when(is_last)
    def _():
        sent(g_s.at[I0:EARLY_SEEDS], bulk.at[I1])

    @pl.when((place.home == I2) & is_r)
    def _():
        got(og_same.at[I0:EARLY_SEEDS], gs_sem)
        got(og_other.at[I0:EARLY_SEEDS], go_sem)

    @pl.when(is_r)
    def _():
        sent(a_s, bulk.at[I0])
        sent(h_s, bulk.at[I3])

    @pl.when(is_r & jnp.logical_not(is_last))
    def _():
        got(oh_same, os_sem)

    @pl.when(is_r & is_last)
    def _():
        got(oh_same.at[I0:micro // I2], os_sem)

    @pl.when(place.is_l)
    def _():
        got(oa_same, as_sem)

    @pl.when(place.is_l | home02)
    def _():
        got(oa_other, ao_sem)


def drain(place):
    def sent(buf, sem):
        remote(buf, buf, sem, sem, place.sibling).wait_send()

    def got(dst, sem):
        pltpu.make_async_copy(dst, dst, sem).wait()
    return sent, got


def backward_kernel(dims, a_s, h_s, qkv_s, u_s, g_s, wq, nq, fq, td0, td1, to0, to1, tu0, tu1, gains, loss_s, after, *refs):
    (dx_s, m_s, od_same, od_other, og_same, og_other, oa_same, oa_other, oh_same, oh_other, dg_same, dg_other, loss_all,
     gbuf, hbuf, obuf, qkvbuf, ubuf, habuf, zbuf, ctxbuf, dqkvbuf, acc, accg, wres, wn, wk,
     grad_sem, hop_b, back_sem, dx_sem, dx_send, save_sem, stream_n, stream_k, res_sem, load_sem,
     ds_sem, do_sem, gs_sem, go_sem, as_sem, ao_sem, os_sem, oo_sem, bulk, tiny, loss_sem, ready) = refs[I6:]
    micro, seq, width, heads, head_dim, ffn = dims
    place = Place()
    is_first, is_last = place.home == I0, place.home == I3
    home13 = (place.home == I1) | is_last
    is_r = jnp.logical_not(place.is_l)
    half = heads // I2 * HEAD_PAD
    scale = head_dim ** -0.5

    barrier = pltpu.get_barrier_semaphore()
    is_b, is_c = place.home == I1, place.home == I2
    for there in (place.sibling, place.across, place.across_other):
        pl.semaphore_signal(barrier, inc=I1, device_id=there, device_id_type=MESH)

    @pl.when(is_c)
    def _():
        pl.semaphore_signal(barrier, inc=I1, device_id=place.along_x, device_id_type=MESH)

    @pl.when(is_last)
    def _():
        for m in range(micro):
            pltpu.make_async_copy(g_s.at[m], gbuf.at[m], grad_sem.at[m]).start()
    wk[...] = jnp.zeros_like(wk)
    bn = Stream(wn, stream_n, BACK_DEPTH, [([(None, td0)], I3), ([(None, td1)], I3), ([(None, to0)], I1), ([(None, to1)], I1)], micro * I8, False)
    bk = Stream(wk, stream_k, KDEPTH, [(near_choices(place, wq, nq), I3), ([(None, fq)], I3)], micro * I6, True)
    bn.prime()
    bk.prime()
    load_resident(wres, res_sem, ([(None, tu0)], [(None, tu1)]))

    def saved(dst, index):
        return pltpu.make_async_copy(hbuf, dst, save_sem)

    def both_kinds(condition, copies, start):
        far_copy, own_copy = copies

        @pl.when(condition & place.is_l)
        def _():
            far_copy().start() if start else far_copy().wait_send()

        @pl.when(condition & is_r)
        def _():
            own_copy().start() if start else own_copy().wait()

    def near_hand(src, dst_far, dst_own, sem, recv_sem):
        return (lambda: remote(src, dst_far, sem, recv_sem, place.sibling)), (lambda: pltpu.make_async_copy(src, dst_own, sem))

    def loads(i):
        m = micro - I1 - i
        return [pltpu.make_async_copy(src.at[m], dst, load_sem.at[k])
                for k, (src, dst) in enumerate(((u_s, ubuf), (qkv_s, qkvbuf), (h_s, habuf.at[I0]), (a_s, habuf.at[I1])))]

    def load_next(i, k):
        @pl.when(i + I1 < micro)
        def _():
            loads(i + I1)[k].start()

    for copy in loads(I0):
        copy.start()
    accg[...] = jnp.zeros_like(accg)

    def norm_back(index, x, base, dst, gain_row):
        def body(rows):
            xf = x[rows, :].astype(F32)
            dy = acc[rows, :].astype(BF).astype(F32)
            inv = lax.rsqrt(jnp.mean(xf * xf, axis=-I1, keepdims=True) + NORM_EPS)
            xn = xf * inv
            accg[index] += jnp.sum((dy * xn).reshape(I4, I8, width), axis=I0)
            dyg = dy * gain_row
            dx = inv * (dyg - xn * jnp.mean(dyg * xn, axis=-I1, keepdims=True))
            dst[rows, :] = (base[rows, :].astype(F32) + dx).astype(BF)
        rows_loop(seq, 32, body)

    def hop_back(i):
        m = micro - I1 - i
        return remote(obuf.at[i % I2], gbuf.at[m], hop_b.at[i % I2], grad_sem.at[m], place.chain(-I1))

    def hand_back(i):
        m = micro - I1 - i
        return near_hand(obuf.at[i % I2], og_other.at[m], og_same.at[m], back_sem.at[i % I2], go_sem)

    def keep_dx(i):
        return pltpu.make_async_copy(obuf.at[i % I2], dx_s.at[micro - I1 - i], back_sem.at[i % I2])

    def back_ready(i):
        both_kinds((i > I1) & home13, hand_back(i), False)

        @pl.when((i > I1) & is_first)
        def _():
            keep_dx(i).wait()
            dx_to_b(i).wait_send()

        @pl.when((i > I1) & jnp.logical_not(is_first))
        def _():
            hop_back(i).wait_send()

    def pass_loss(tile):
        @pl.when(jnp.logical_not(is_first))
        def _():
            remote(tile, loss_all.at[place.core], loss_sem.at[I0], loss_sem.at[I1], place.chain(-I1)).start()
        remote(tile, loss_all.at[place.core], loss_sem.at[I2], loss_sem.at[I3], place.sibling).start()

    def dx_to_b(i):
        return remote(obuf.at[i % I2], dx_s.at[micro - I1 - i], dx_send.at[i % I2], dx_sem, place.across)

    def backward_tick(i, carry):
        m = micro - I1 - i
        slot = i % I2
        grad, dmid, prev = gbuf.at[m], hbuf, obuf.at[slot]
        u_now, qkv_now, h_now, a_now = ubuf, qkvbuf, habuf.at[I0], habuf.at[I1]

        pltpu.make_async_copy(g_s.at[m], grad, grad_sem.at[m]).wait()

        @pl.when(place.is_l)
        def _():
            pltpu.make_async_copy(grad, og_same.at[m], gs_sem).start()
        load_u, load_qkv, load_h, load_a = loads(i)
        load_u.wait()

        def mlp_step(j, c):
            w = bn.wait(i * I8 + j)
            for n in range(I0, CHUNK, SUB):
                at = lanes(j * CHUNK + n, SUB)
                dz = mm(grad[...], w[:, n:n + SUB]).astype(BF).astype(F32)
                u = u_now[:, at].astype(F32)
                gate, u2 = gelu_gate(u)
                zbuf[:, at] = (dz * gelu_slope(u * gate, gate, u2)).astype(BF)
            bn.start(i * I8 + j + BACK_DEPTH)
            return c
        lax.fori_loop(I0, I6, mlp_step, I0)

        @pl.when(i == I0)
        def _():
            for j in range(I6):
                pltpu.make_async_copy(tu0.at[I0:CHUNK, :], wres.at[j], res_sem.at[j]).wait()

        def turn_back(n, c):
            cols = lanes(n * SUB, SUB)
            acc[:, cols] = blocked(zbuf, wres, cols)
            return c
        lax.fori_loop(I0, width // SUB, turn_back, I0)
        load_next(i, I0)
        load_h.wait()
        norm_back(I1, h_now, grad, dmid, gains[I1:I2, :])
        load_next(i, I2)

        @pl.when(place.is_l)
        def _():
            saved(od_same.at[m], I0).start()

        @pl.when(is_r)
        def _():
            saved(m_s.at[m], I0).start()
        for c in range(I2):
            w = bn.wait(i * I8 + I6 + c)
            for n in range(I0, CHUNK, SUB):
                ctxbuf[:, c * CHUNK + n:c * CHUNK + n + SUB] = mm(dmid[...], w[:, n:n + SUB]).astype(BF)
            bn.start(i * I8 + I6 + c + BACK_DEPTH)
        load_qkv.wait()

        def head_step(t, c):
            base = (t // I2) * (I3 * half) + (t % I2) * (I4 * HEAD_PAD)
            at = [[lanes(base + part * half + r * HEAD_PAD, HEAD_PAD) for part in range(I3)] for r in range(I4)]
            group = [(*(qkv_now[:, p] for p in at[r]), ctxbuf[:, lanes((t * I4 + r) * HEAD_PAD, HEAD_PAD)]) for r in range(I4)]
            for r, grads in enumerate(attention_backward(group, scale)):
                for p, value in zip(at[r], grads):
                    dqkvbuf[:, p] = value
            return c
        for t in range(heads // I4):
            head_step(t, I0)
        load_next(i, I1)
        acc[...] = jnp.zeros_like(acc)

        def qkv_step(j, c):
            w = bk.wait(i * I6 + j)
            for n in range(I0, width, SUB):
                acc[:, n:n + SUB] += mm(dqkvbuf[:, lanes(j * CHUNK, CHUNK)], w[:, n:n + SUB])
            bk.start(i * I6 + j + KDEPTH)
            return c
        lax.fori_loop(I0, I6, qkv_step, I0)
        load_a.wait()
        back_ready(i)
        norm_back(I0, a_now, dmid, prev, gains[I0:I1, :])
        load_next(i, I3)

        @pl.when(i == I0)
        def _():
            @pl.when(is_first | is_last)
            def _():
                pl.semaphore_wait(barrier, I3)

            @pl.when(is_c)
            def _():
                pl.semaphore_wait(ready, I1)

            @pl.when(is_last)
            def _():
                pass_loss(loss_s)

        @pl.when(jnp.logical_not(is_first))
        def _():
            hop_back(i).start()

        @pl.when(is_first)
        def _():
            keep_dx(i).start()
            dx_to_b(i).start()
        both_kinds(home13, hand_back(i), True)

        @pl.when(place.is_l)
        def _():
            saved(od_same.at[m], I0).wait()
            remote(od_same.at[m], od_same.at[m], bulk.at[I6], ds_sem, place.across).start()

        @pl.when(is_r)
        def _():
            remote(grad, og_other.at[m], bulk.at[5], go_sem, place.sibling).start()
            saved(m_s.at[m], I0).wait()
            remote(m_s.at[m], od_other.at[m], bulk.at[I6], do_sem, place.sibling).start()
            remote(m_s.at[m], od_other.at[m], bulk.at[7], do_sem, place.across_other).start()

        now = (i % I2 == I1) & (i < I2 * EARLY_G)
        far_grad(m, (place.home == I1) & now)
        far_grad(micro - I1 - i // I2, is_last & now)
        return carry

    def far_grad(m, condition):
        @pl.when(condition & place.is_l)
        def _():
            remote(gbuf.at[m], og_same.at[m], bulk.at[I4], gs_sem, place.across).start()

        @pl.when(condition & is_r)
        def _():
            remote(gbuf.at[m], og_other.at[m], bulk.at[I4], go_sem, place.across_other).start()

    @pl.when(is_b | is_c)
    def _():
        pl.semaphore_wait(barrier, 5 - place.home)

    @pl.when(is_b)
    def _():
        pl.semaphore_signal(ready, inc=I1, device_id=place.along_x, device_id_type=MESH)

    @pl.when(is_c & place.is_l)
    def _():
        for t in range(micro):
            remote(a_s.at[t], oa_same.at[t], bulk.at[I8], as_sem, place.across).start()
        for t in range(I0, micro, I2):
            remote(h_s.at[t], oh_same.at[t], bulk.at[9], os_sem, place.across).start()

    @pl.when(is_c & is_r)
    def _():
        for t in range(micro):
            remote(a_s.at[t], oa_other.at[t], bulk.at[I8], ao_sem, place.across_other).start()
        for t in range(I0, micro, I2):
            remote(h_s.at[t], oh_other.at[t], bulk.at[9], oo_sem, place.across_other).start()
    lax.fori_loop(I0, micro, backward_tick, I0)
    loss_mine = loss_all.at[place.core]

    @pl.when(is_last)
    def _():
        own_loss = pltpu.make_async_copy(loss_s, loss_mine, loss_sem.at[I1])
        own_loss.start()
        own_loss.wait()

    @pl.when(jnp.logical_not(is_last))
    def _():
        remote(loss_mine, loss_mine, loss_sem.at[I0], loss_sem.at[I1], place.sibling).wait_recv()
        pass_loss(loss_mine)

    @pl.when(place.is_l)
    def _():
        pltpu.make_async_copy(accg, dg_same, tiny.at[I0]).start()
        remote(accg, dg_same, tiny.at[I1], tiny.at[I0], place.across).start()

    @pl.when(is_r)
    def _():
        remote(accg, dg_other, tiny.at[I1], tiny.at[I4], place.sibling).start()
        remote(accg, dg_other, tiny.at[I2], tiny.at[I4], place.across_other).start()

    for i in (micro - I2, micro - I1):
        back_ready(jnp.int32(i))

    sent, got = drain(place)
    sent(m_s, bulk.at[I6])

    @pl.when(is_r)
    def _():
        sent(gbuf, bulk.at[5])
        sent(m_s, bulk.at[7])
        remote(accg, dg_other, tiny.at[I2], tiny.at[I4], place.sibling).wait_send()

    @pl.when(home13)
    def _():
        sent(gbuf.at[I0:EARLY_G], bulk.at[I4])

    @pl.when(place.home == I1)
    def _():
        got(dx_s, dx_sem)

    @pl.when(jnp.logical_not(is_first))
    def _():
        remote(loss_mine, loss_mine, loss_sem.at[I0], loss_sem.at[I1], place.sibling).wait_send()
    remote(loss_mine, loss_mine, loss_sem.at[I2], loss_sem.at[I3], place.sibling).wait_send()
    remote(loss_mine, loss_mine, loss_sem.at[I2], loss_sem.at[I3], place.sibling).wait_recv()

    @pl.when(place.home == I2)
    def _():
        sent(a_s, bulk.at[I8])
        sent(h_s.at[I0:micro // I2], bulk.at[9])

    remote(accg, dg_other, tiny.at[I1], tiny.at[I4], place.sibling).wait_send()
    got(od_other, do_sem)

    @pl.when(place.is_l | home13)
    def _():
        got(og_other, go_sem)

    @pl.when(jnp.logical_not(home13) & is_r)
    def _():
        got(og_same.at[I0:EARLY_G], gs_sem)
        got(og_other.at[I0:EARLY_G], go_sem)
    got(dg_same, tiny.at[I0])
    got(dg_other, tiny.at[I4])

    @pl.when(is_r)
    def _():
        got(od_same, ds_sem)

    @pl.when(place.is_l)
    def _():
        got(og_same, gs_sem)

    @pl.when(is_last & is_r)
    def _():
        got(oa_same, as_sem)
        got(oa_other, ao_sem)
        got(oh_same.at[I0:micro // I2], os_sem)
        got(oh_other.at[I0:micro // I2], oo_sem)


def shapes(*dims_list):
    return [jax.ShapeDtypeStruct(d, BF) for d in dims_list]


def forward_phase(dims, x, y, own, own_gains):
    micro, seq, width, heads, head_dim, ffn = dims
    half = heads // I2 * HEAD_PAD
    act = (micro, seq, width)
    raw = [w.shape for w in own]
    turned = [(I3, width, CHUNK), (I1, width, CHUNK), (ffn // I2, width), (I3, width, CHUNK)]
    out_shape = shapes(act, act, (micro, seq, I6 * half), (micro, seq, ffn), *[act] * 7)
    out_shape += [jax.ShapeDtypeStruct(s, F32) for s in ((I8, 128), own_gains.shape)]
    out_shape += shapes(*raw, *raw, *turned, *turned, turned[I0], turned[I0], *[(len(ROUND), 768, width)] * I2)
    any_spec = pl.BlockSpec(memory_space=ANY)
    vmem, dma = pltpu.VMEM, pltpu.SemaphoreType.DMA
    row = vmem((seq, width), BF)
    scratch = [
        vmem(act, BF), row, vmem((I2, seq, width), BF), row, row, row, vmem((seq, I6 * half), BF), vmem((seq, ffn), BF), vmem((seq, ffn), BF),
        vmem((seq, I2 * half), BF), vmem((I8, width), F32), vmem((I8, 128), F32), vmem((I2, width), F32),
        vmem((I6, CHUNK, width), BF), vmem((I2, CHUNK, width), BF), vmem((DEPTH, width, CHUNK), BF),
        dma((I4,)), dma((I4,)), dma((I4,)), dma((I4,)), dma((12,)), dma((I2,)), dma((I2,)), dma((I2,)), *[dma((len(ROUND),))] * 5,
        dma((micro,)), dma((I2,)), dma((I2,)), dma((I3,)), dma((DEPTH,)), dma((I6,)), dma((I2,)), dma((I2,)), dma(()), dma(()),
        dma(()), dma(()), dma(()), dma(()), dma(()), dma(()), dma((I4,)), dma((I2,)), dma(()),
    ]
    return pl.pallas_call(
        functools.partial(forward_kernel, dims),
        out_shape=tuple(out_shape),
        in_specs=[any_spec] * I6 + [pl.BlockSpec(memory_space=vmem)],
        out_specs=(any_spec,) * len(out_shape),
        scratch_shapes=scratch,
        compiler_params=pltpu.CompilerParams(collective_id=I0, has_side_effects=True, vmem_limit_bytes=VMEM_LIMIT),
        name='forward_phase',
    )(x, y, *own, own_gains)


def backward_phase(dims, saved, weights, gains, loss, after, placed):
    micro, seq, width, heads, head_dim, ffn = dims
    half = heads // I2 * HEAD_PAD
    act = (micro, seq, width)
    out_shape = shapes(*[act] * 10) + [jax.ShapeDtypeStruct((I2, I8, width), F32)] * I2 + [jax.ShapeDtypeStruct((I2, I8, 128), F32)]
    any_spec = pl.BlockSpec(memory_space=ANY)
    vmem, dma = pltpu.VMEM, pltpu.SemaphoreType.DMA
    scratch = [
        vmem(act, BF), vmem((seq, width), BF), vmem((I2, seq, width), BF), vmem((seq, I6 * half), BF), vmem((seq, ffn), BF),
        vmem((I2, seq, width), BF), vmem((seq, ffn), BF), vmem((seq, I2 * half), BF), vmem((seq, I6 * half), BF), vmem((seq, width), F32),
        vmem((I2, I8, width), F32), vmem((I6, CHUNK, width), BF), vmem((BACK_DEPTH, width, CHUNK), BF), vmem((KDEPTH, CHUNK, width), BF),
        dma((micro,)), dma((I2,)), dma((I2,)), dma(()), dma((I2,)), dma(()), dma((BACK_DEPTH,)), dma((KDEPTH,)), dma((I6,)), dma((I4,)),
        *[dma(())] * I8, dma((10,)), dma((5,)), dma((I4,)), pltpu.SemaphoreType.REGULAR,
    ]
    return pl.pallas_call(
        functools.partial(backward_kernel, dims),
        out_shape=tuple(out_shape),
        in_specs=[any_spec] * 14 + [pl.BlockSpec(memory_space=vmem)] * I2 + [any_spec] * 7,
        out_specs=(any_spec,) * len(out_shape),
        scratch_shapes=scratch,
        input_output_aliases={17 + i: I4 + i for i in range(I6)},
        compiler_params=pltpu.CompilerParams(collective_id=I1, has_side_effects=True, vmem_limit_bytes=VMEM_LIMIT),
        name='backward_phase',
    )(*saved, *weights, gains, loss, after, *placed)


def late_rows(micro):
    return [micro - I1 - i for i in range(micro) if i % I2 == I0 or i > I2 * EARLY_G]


def hand_on(place, dx, d_in, og, sems):
    micro = dx.shape[I0]
    barrier = pltpu.get_barrier_semaphore()
    late = late_rows(micro)
    is_leaf = place.home > I1
    gives_g = (place.home == I1) & place.is_l
    takes_g = (place.home == I0) & jnp.logical_not(place.is_l)
    part, g_part = dx.at[I0:EARLY_DX], og.at[I0:len(late)]

    @pl.when(is_leaf)
    def _():
        pl.semaphore_signal(barrier, inc=I1, device_id=place.along_x, device_id_type=MESH)

    @pl.when(takes_g)
    def _():
        pl.semaphore_signal(barrier, inc=I1, device_id=place.across, device_id_type=MESH)

    @pl.when(jnp.logical_not(is_leaf))
    def _():
        pl.semaphore_wait(barrier, I1 + gives_g.astype(jnp.int32))

        @pl.when(gives_g)
        def _():
            for m in late:
                remote(og.at[m], og.at[m], sems.at[I2], sems.at[I3], place.across).start()
        for m in range(micro - EARLY_DX, micro):
            remote(dx.at[m], d_in.at[m, place.core], sems.at[I0], sems.at[I1], place.along_x).start()
        remote(part, part, sems.at[I0], sems.at[I1], place.along_x).wait_send()

        @pl.when(gives_g)
        def _():
            remote(g_part, g_part, sems.at[I2], sems.at[I3], place.across).wait_send()

    def received():
        @pl.when(is_leaf)
        def _():
            remote(part, part, sems.at[I0], sems.at[I1], place.along_x).wait_recv()

        @pl.when(takes_g)
        def _():
            remote(g_part, g_part, sems.at[I2], sems.at[I3], place.across).wait_recv()
    return received


def recompute_kernel(dims, early, h_same, h_other, a_same, a_other, gains, wq, wu, *refs):
    (wqbuf, wubuf, count, sem, sems) = refs[-5:]
    outs = refs[:-5] if early else refs[7:-5]
    (done, u_o, qkv_o, ctx_o, n1_o, n2_o) = outs[I0:I6]
    micro, seq, width, heads, head_dim, ffn = dims
    place = Place()
    scale = head_dim ** -0.5
    half = heads // I2 * HEAD_PAD
    steps = I2 * micro * seq // BLOCK

    def pieces(j):
        copies = [pltpu.make_async_copy(wu.at[:, lanes(j * SUB, SUB)], wubuf.at[:, lanes(j * SUB, SUB)], sem.at[I0, j])]
        for r in range(I2):
            src = pl.ds(pl.multiple_of((I2 * j + r) * head_dim, head_dim), head_dim)
            dst = pl.ds(pl.multiple_of((I2 * j + r) * HEAD_PAD, HEAD_PAD), head_dim)
            copies.append(pltpu.make_async_copy(wq.at[src, :], wqbuf.at[dst, :], sem.at[I1 + r, j]))
        return copies

    def body(hs, ho, rs, ro, u, qkv, ctx, n1, n2):
        step = count[I0]
        count[I0] = step + I1
        for low, high, gain, dst in ((hs, ho, gains[I1:I2, :], n2), (rs, ro, gains[I0:I1, :], n1)):
            @pl.when(step < steps // I2)
            def _(low=low, gain=gain, dst=dst):
                norm_rows(low, gain, dst, BLOCK)

            @pl.when(step >= steps // I2)
            def _(high=high, gain=gain, dst=dst):
                norm_rows(high, gain, dst, BLOCK)

        @pl.when(step == I0)
        def _():
            for j in range(I3 * half // SUB):
                for copy in pieces(j):
                    copy.wait()

        def qkv_step(j, c):
            rows = pl.ds(pl.multiple_of(j * SUB, SUB), SUB)
            qkv[:, lanes(j * SUB, SUB)] = mm_nt(n1[...], wqbuf[rows, :]).astype(BF)
            u[:, lanes(j * SUB, SUB)] = mm(n2[...], wubuf[:, lanes(j * SUB, SUB)]).astype(BF)
            return c
        lax.fori_loop(I0, I3 * half // SUB, qkv_step, I0)

        def head_step(j, c):
            at = [(pl.ds(s, seq), r * HEAD_PAD) for s in range(I0, BLOCK, seq) for r in range(I4)]
            base = j * (I4 * HEAD_PAD)
            views = [[qkv[rows, lanes(base + t * half + col, HEAD_PAD)] for t in range(I3)] for rows, col in at]
            for (rows, col), context in zip(at, attention_forward(views, scale)):
                ctx[rows, lanes(base + col, HEAD_PAD)] = context
            return c
        lax.fori_loop(I0, I2, head_step, I0)

    received = nothing if early else hand_on(place, refs[I0], outs[I6], outs[7], sems)

    @pl.when(place.home < I2 if early else place.home > I1)
    def _():
        pads = jnp.zeros((HEAD_PAD - head_dim, width), BF)
        for t in range(I3 * heads // I2):
            wqbuf[t * HEAD_PAD + head_dim:(t + I1) * HEAD_PAD, :] = pads
        for j in range(I3 * half // SUB):
            for copy in pieces(j):
                copy.start()
        count[I0] = I0
        low = pl.BlockSpec((BLOCK, width), lambda i: (jnp.minimum(i, steps // I2 - I1), I0))
        high = pl.BlockSpec((BLOCK, width), lambda i: (jnp.maximum(i - steps // I2, I0), I0))
        block = lambda n: pl.BlockSpec((BLOCK, n), lambda i: (i, I0))
        pltpu.emit_pipeline(body, grid=(steps,), in_specs=[low, high, low, high],
                            out_specs=[block(ffn // I2), block(I3 * half), block(half), block(width), block(width)])(
            h_same, h_other, a_same, a_other, u_o, qkv_o, ctx_o, n1_o, n2_o)
    received()


def owner_recompute(dims, early, again, h_rows, a_rows, gains, own):
    micro, seq, width, heads, head_dim, ffn = dims
    half = heads // I2 * HEAD_PAD
    tokens = I2 * micro * seq
    any_spec = pl.BlockSpec(memory_space=ANY)
    vmem = pltpu.VMEM
    earlier = () if early else tuple(again)
    act = (micro, seq, width)
    out_shape = [jax.ShapeDtypeStruct((I8, 128), F32), *shapes((tokens, ffn // I2), (tokens, I3 * half), (tokens, half), (tokens, width), (tokens, width))]
    if not early:
        out_shape += shapes((micro, I2, seq, width), act)
    aliases = {} if early else {I8 + i: I1 + i for i in range(5)} | {13: 7}
    comm = {} if early else dict(collective_id=I3)
    return pl.pallas_call(
        functools.partial(recompute_kernel, dims, early),
        out_shape=tuple(out_shape),
        in_specs=[any_spec] * I4 + [pl.BlockSpec(memory_space=vmem)] + [any_spec] * (I2 + len(earlier)),
        out_specs=(any_spec,) * len(out_shape),
        scratch_shapes=[vmem((I3 * half, width), BF), vmem((width, ffn // I2), BF), pltpu.SMEM((I1,), jnp.int32), pltpu.SemaphoreType.DMA((I3, ffn // I2 // SUB)), pltpu.SemaphoreType.DMA((I4,))],
        input_output_aliases=aliases,
        compiler_params=pltpu.CompilerParams(**comm, has_side_effects=True, vmem_limit_bytes=VMEM_LIMIT),
        name='owner_recompute',
    )(*h_rows, *a_rows, gains, own[I0], own[I2], *earlier)


def spread_dx(step, last, dx, d_in, og_other, bounce, here_sem, parent_sem, sib_sem, send_sems, og_sems, ready):
    place = Place()
    micro = dx.shape[I0]
    along_x = place.at(place.tp, (place.stage + I2) % I4)
    barrier = pltpu.get_barrier_semaphore()
    is_leaf = place.home > I1
    gives_g = (place.home == I1) & place.is_l
    takes_g = (place.home == I0) & jnp.logical_not(place.is_l)
    late = late_rows(micro)

    def block(m):
        return d_in.at[m, place.core]

    def to_sibling(m, src):
        remote(src, block(m), send_sems.at[I0], sib_sem, place.sibling).start()

    def tell(there):
        pl.semaphore_signal(barrier, inc=I1, device_id=there, device_id_type=MESH)

    @pl.when(step == I0)
    def _():
        tell(place.sibling)

        @pl.when(takes_g)
        def _():
            tell(place.across)

        @pl.when(is_leaf)
        def _():
            pl.semaphore_wait(barrier, I2)
            pl.semaphore_signal(ready, inc=I1, device_id=along_x, device_id_type=MESH)

        @pl.when(jnp.logical_not(is_leaf))
        def _():
            tell(along_x)
            pl.semaphore_wait(barrier, I1 + gives_g.astype(jnp.int32))

        @pl.when(gives_g)
        def _():
            for m in late:
                remote(og_other.at[m], og_other.at[m], og_sems.at[I0], og_sems.at[I1], place.across).start()

    @pl.when((step == I3) & jnp.logical_not(is_leaf))
    def _():
        pl.semaphore_wait(ready, I1)
        for m in reversed(range(micro)):
            if m < micro - EARLY_DX:
                remote(dx.at[m], block(m), send_sems.at[I1], parent_sem.at[m], along_x).start()
            to_sibling(m, dx.at[m])
        pltpu.make_async_copy(dx, bounce, here_sem).start()

    @pl.when((step == I4) & jnp.logical_not(is_leaf))
    def _():
        pltpu.make_async_copy(dx, bounce, here_sem).wait()
        for m in range(micro):
            pltpu.make_async_copy(bounce.at[m], block(m), here_sem).start()

    part = og_other.at[I0:len(late)]

    @pl.when((step == I3) & takes_g)
    def _():
        remote(part, part, og_sems.at[I0], og_sems.at[I1], place.across).wait_recv()

    @pl.when((step == last) & is_leaf)
    def _():
        for m in reversed(range(micro)):
            if m < micro - EARLY_DX:
                remote(block(m), block(m), send_sems.at[I0], parent_sem.at[m], place.sibling).wait_recv()
            to_sibling(m, block(m))

    @pl.when(step == last)
    def _():
        remote(dx, dx, send_sems.at[I0], sib_sem, place.sibling).wait_send()

        @pl.when(jnp.logical_not(is_leaf))
        def _():
            rest = dx.at[I0:micro - EARLY_DX]
            remote(rest, rest, send_sems.at[I1], sib_sem, place.sibling).wait_send()
            pltpu.make_async_copy(dx, dx, here_sem).wait()

        @pl.when(gives_g)
        def _():
            remote(part, part, og_sems.at[I0], og_sems.at[I1], place.across).wait_send()
        remote(dx, dx, send_sems.at[I0], sib_sem, place.sibling).wait_recv()


def owner_backward_kernel(dims, dx, ds, do, u, qkv, wo, wd, og_same, go_in, d_first, dqkv, dup, z, d_in, og_other,
                          dmid, gbuf, dctx, wobuf, bounce, sem, g_sem, here_sem, parent_sem, sib_sem, send_sems, og_sems, ready):
    micro, seq, width, heads, head_dim, ffn = dims
    half = heads // I2 * HEAD_PAD
    scale = head_dim ** -0.5
    step, steps = pl.program_id(I0), pl.num_programs(I0)
    spread_dx(step, steps - I1, dx, d_in, og_other, bounce, here_sem, parent_sem, sib_sem, send_sems, og_sems, ready)

    def g_load(n, start):
        rows = BLOCK // seq
        for og, low in ((og_same, I0), (og_other, steps // I2)):
            @pl.when((n >= low) & (n < low + steps // I2))
            def _(og=og, low=low):
                copy = pltpu.make_async_copy(og.at[pl.ds((n - low) * rows, rows)], gbuf.at[n % I2], g_sem.at[n % I2])
                copy.start() if start else copy.wait()

    @pl.when(step == I0)
    def _():
        g_load(step, True)
        wobuf[...] = jnp.zeros_like(wobuf)
        load_heads(wo, I0, wobuf, sem)
        pltpu.make_async_copy(wo, wobuf.at[I0:wo.shape[I0]], sem).wait()
    g_load(step + I1, True)

    @pl.when(step < steps // I2)
    def _():
        dmid[...] = ds[...]

    @pl.when(step >= steps // I2)
    def _():
        dmid[...] = do[...]

    def ctx_step(j, c):
        rows = pl.ds(pl.multiple_of(j * SUB, SUB), SUB)
        dctx[:, lanes(j * SUB, SUB)] = mm_nt(dmid[...], wobuf[rows, :]).astype(BF)
        return c
    lax.fori_loop(I0, half // SUB, ctx_step, I0)
    g_load(step, False)
    grad = gbuf.at[step % I2]

    def mlp_block(n):
        rows = pl.ds(pl.multiple_of(n * SUB, SUB), SUB)
        cols = lanes(n * SUB, SUB)
        dz = mm_nt(grad[...].reshape(BLOCK, width), wd[rows, :]).astype(BF).astype(F32)
        up = u[:, cols].astype(F32)
        gate, up2 = gelu_gate(up)
        hidden = up * gate
        z[:, cols] = hidden.astype(BF)
        dup[:, cols] = (dz * gelu_slope(hidden, gate, up2)).astype(BF)

    def both_step(j, c):
        base = j * (I2 * HEAD_PAD)
        at = [(pl.ds(s, seq), base + r * HEAD_PAD) for s in range(I0, BLOCK, seq) for r in range(I2)]
        group = [(*(qkv[rows, lanes(t * half + col, HEAD_PAD)] for t in range(I3)), dctx[rows, lanes(col, HEAD_PAD)]) for rows, col in at]
        blocks = [functools.partial(mlp_block, j * I3 + r) for r in range(I3)]
        for (rows, col), grads in zip(at, attention_backward(group, scale, blocks)):
            for t, value in enumerate(grads):
                dqkv[rows, lanes(t * half + col, HEAD_PAD)] = value
        return c
    lax.fori_loop(I0, heads // I4, both_step, I0)


def owner_backward(dims, dx, d_in, d_rows, og, ups, qkv, own):
    micro, seq, width, heads, head_dim, ffn = dims
    half = heads // I2 * HEAD_PAD
    tokens = I2 * micro * seq
    blocks = tokens // BLOCK
    vmem, dma = pltpu.VMEM, pltpu.SemaphoreType.DMA
    any_spec = pl.BlockSpec(memory_space=ANY)
    low = pl.BlockSpec((BLOCK, width), lambda i: (jnp.minimum(i, blocks // I2 - I1), I0))
    high = pl.BlockSpec((BLOCK, width), lambda i: (jnp.maximum(i - blocks // I2, I0), I0))
    attn_block = pl.BlockSpec((BLOCK, I3 * half), lambda i: (i, I0))
    mlp_block = pl.BlockSpec((BLOCK, ffn // I2), lambda i: (i, I0))
    act = (micro, seq, width)
    return pl.pallas_call(
        functools.partial(owner_backward_kernel, dims),
        grid=(blocks,),
        out_shape=tuple(shapes((tokens, I3 * half), (tokens, ffn // I2), (tokens, ffn // I2), (micro, I2, seq, width), act)),
        in_specs=[any_spec, low, high, mlp_block, attn_block, any_spec, pl.BlockSpec((ffn // I2, width), lambda i: (I0, I0)), any_spec, any_spec, any_spec],
        out_specs=(attn_block, mlp_block, mlp_block, any_spec, any_spec),
        scratch_shapes=[vmem((BLOCK, width), BF), vmem((I2, BLOCK // seq, seq, width), BF), vmem((BLOCK, half), BF), vmem((half, width), BF), vmem(act, BF),
                        dma(()), dma((I2,)), dma(()), dma((micro,)), dma(()), dma((I2,)), dma((I2,)), pltpu.SemaphoreType.REGULAR],
        input_output_aliases={I8: I4, 9: I3},
        compiler_params=pltpu.CompilerParams(collective_id=I2, has_side_effects=True, vmem_limit_bytes=VMEM_LIMIT),
        name='owner_backward',
    )(dx, *d_rows, ups, qkv, own[I1], own[I3], *og, d_in)


def bring(pairs, sem):
    copies = [pltpu.make_async_copy(src, dst, sem.at[i]) for i, (src, dst) in enumerate(pairs)]
    for copy in copies:
        copy.start()
    for copy in copies:
        copy.wait()


def attn_products_kernel(dq, dk, dv, ctx, n1_o, ds, do, dx_in, dwq, dwo, dx_out, n1, dmid, dqkvt, ctxt, bounce, sem, dx_sem):
    tokens, width = n1.shape
    part = tokens // I2
    head_dim = dwo.shape[I1]
    step, last = pl.program_id(I0), pl.num_programs(I0) - I1
    into, out_of = pltpu.make_async_copy(dx_in, bounce, dx_sem), pltpu.make_async_copy(bounce, dx_out, dx_sem)

    @pl.when(step == I1)
    def _():
        into.start()

    @pl.when(step == I2)
    def _():
        into.wait()
        out_of.start()

    @pl.when(step == last)
    def _():
        out_of.wait()

    @pl.when(step == I0)
    def _():
        bring([(n1_o, n1), (ds, dmid.at[pl.ds(I0, part)]), (do, dmid.at[pl.ds(part, part)])], sem)

    def turn(rows):
        for t, block in enumerate((dq, dk, dv)):
            for r in range(I2):
                at = (I2 * t + r) * head_dim
                dqkvt[at:at + head_dim, rows] = block[rows, r * HEAD_PAD:(r + I1) * HEAD_PAD].T[I0:head_dim]
        for r in range(I2):
            ctxt[r * head_dim:(r + I1) * head_dim, rows] = ctx[rows, r * HEAD_PAD:(r + I1) * HEAD_PAD].T[I0:head_dim]
    rows_loop(tokens, SUB, turn)
    for c in range(I0, width, SUB):
        cut = slice(c, c + SUB)
        dwq[:, :, :, cut] = mm(dqkvt[...], n1[:, cut]).reshape(I3, I2, head_dim, SUB)
        dwo[:, :, cut] = mm(ctxt[...], dmid[:, cut]).reshape(I2, head_dim, SUB)


def attn_products(dqkv, ctx, n1, d_rows, dx, out_dims):
    heads, head_dim, width = out_dims
    tokens = n1.shape[I0]
    vmem = pltpu.VMEM
    any_spec = pl.BlockSpec(memory_space=ANY)
    pairs = heads // I2
    cols = lambda t: pl.BlockSpec((tokens, I2 * HEAD_PAD), lambda i: (I0, t * pairs + i))
    return pl.pallas_call(
        attn_products_kernel,
        grid=(pairs,),
        out_shape=(jax.ShapeDtypeStruct((I3,) + out_dims, F32), jax.ShapeDtypeStruct(out_dims, F32), jax.ShapeDtypeStruct(dx.shape, BF)),
        in_specs=[cols(I0), cols(I1), cols(I2), cols(I0), any_spec, any_spec, any_spec, any_spec],
        out_specs=(pl.BlockSpec((I3, I2, head_dim, width), lambda i: (I0, i, I0, I0)), pl.BlockSpec((I2, head_dim, width), lambda i: (i, I0, I0)), any_spec),
        scratch_shapes=[vmem((tokens, width), BF), vmem((tokens, width), BF), vmem((I6 * head_dim, tokens), BF), vmem((I2 * head_dim, tokens), BF),
                        vmem(dx.shape, BF), pltpu.SemaphoreType.DMA((I3,)), pltpu.SemaphoreType.DMA(())],
        compiler_params=pltpu.CompilerParams(vmem_limit_bytes=VMEM_LIMIT),
        name='attn_products',
    )(dqkv, dqkv, dqkv, ctx, n1, *d_rows, dx)


def mlp_products_kernel(dup, z, n2_o, gs, go, dwu, dwd, n2t, grad, zt, stage, sem):
    width, tokens = n2t.shape
    part = tokens // I2

    @pl.when(pl.program_id(I0) == I0)
    def _():
        bring([(n2_o, stage), (gs, grad.at[pl.ds(I0, part)]), (go, grad.at[pl.ds(part, part)])], sem)

        def turn(rows):
            for c in range(I0, width, SUB):
                n2t[c:c + SUB, rows] = stage[rows, c:c + SUB].T
        rows_loop(tokens, SUB, turn)

    def turn_z(rows):
        for c in range(I0, z.shape[I1], SUB):
            zt[c:c + SUB, rows] = z[rows, c:c + SUB].T
    rows_loop(tokens, SUB, turn_z)
    for c in range(I0, width, I2 * SUB):
        dwu[c:c + I2 * SUB, :] = mm(n2t[c:c + I2 * SUB, :], dup[...])
    for c in range(I0, width, SUB):
        dwd[:, c:c + SUB] = mm(zt[...], grad[:, c:c + SUB])


def mlp_products(dup, hidden, n2, g_rows):
    tokens, width = n2.shape
    cols = dup.shape[I1]
    vmem = pltpu.VMEM
    any_spec = pl.BlockSpec(memory_space=ANY)
    block = pl.BlockSpec((tokens, SUB), lambda i: (I0, i))
    return pl.pallas_call(
        mlp_products_kernel,
        grid=(cols // SUB,),
        out_shape=(jax.ShapeDtypeStruct((width, cols), F32), jax.ShapeDtypeStruct((cols, width), F32)),
        in_specs=[block, block, any_spec, any_spec, any_spec],
        out_specs=(pl.BlockSpec((width, SUB), lambda i: (I0, i)), pl.BlockSpec((SUB, width), lambda i: (i, I0))),
        scratch_shapes=[vmem((width, tokens), BF), vmem((tokens, width), BF), vmem((SUB, tokens), BF), vmem((tokens, width), BF), pltpu.SemaphoreType.DMA((I3,))],
        compiler_params=pltpu.CompilerParams(vmem_limit_bytes=VMEM_LIMIT),
        name='mlp_products',
    )(dup, hidden, n2, *g_rows)


def solution(mesh):
    act_spec = P('rep', None, None, None)
    weight_specs = (
        P(('rep', 'stage'), None, None, 'tp', None),
        P(('rep', 'stage'), 'tp', None, None),
        P(('rep', 'stage'), None, 'tp'),
        P(('rep', 'stage'), 'tp', None),
        P(('rep', 'stage'), None),
        P(('rep', 'stage'), None),
    )

    def device_fn(inputs, targets, w_qkv, w_out, w_up, w_down, gain_attn, gain_mlp):
        micro_count, _, seq_len, width = inputs.shape
        dims = (micro_count, seq_len, width, I2 * w_out.shape[I1], w_out.shape[I2], I2 * w_up.shape[I2])
        norm_factor = 1.0 / (inputs.size)
        own = (w_qkv[I0], w_out[I0], w_up[I0], w_down[I0])
        own_gains = jnp.concatenate([gain_attn, gain_mlp]).astype(F32)
        rows_of = (own[I0].transpose(I1, I2, I3, I0).reshape(-I1, width), own[I1].reshape(-I1, width), own[I2], own[I3])

        (acts, mids, qkv, ups, seeds, oh_same, oh_other, oa_same, oa_other, og_same, og_other, loss_tile, home_gains, *weights) = forward_phase(dims, inputs, targets, rows_of, own_gains)
        (nq, no, nu, nd), (fq, fo, fu, fd) = weights[I0:I4], weights[I4:I8]
        (tq0, to0, tu0, td0), (tq1, to1, tu1, td1) = weights[I8:12], weights[12:16]

        flat = lambda *rows: [r.reshape(-I1, width) for r in rows]
        done, *again = owner_recompute(dims, True, None, flat(oh_same, oh_other), flat(oa_same, oa_other), own_gains, rows_of)
        dx, _, od_same, od_other, og_same, og_other, oa_same, oa_other, oh_same, oh_other, dg_same, dg_other, loss_all = backward_phase(
            dims, (acts, mids, qkv, ups, seeds), (rows_of[I0], nq, fq, td0, td1, to0, to1, tu0, tu1), home_gains, loss_tile, done,
            (og_same, og_other, oa_same, oa_other, oh_same, oh_other))
        _, *again, d_first, og_same = owner_recompute(dims, False, (dx, *again, og_same), flat(oh_same, oh_other), flat(oa_same, oa_other), own_gains, rows_of)
        ups_own, qkv_own, ctx_own, n1, n2 = again
        d_rows = flat(od_same, od_other)
        d_qkv_rows, d_up_rows, hidden, dx_all, og_other = owner_backward(dims, dx, d_first, d_rows, (og_same, og_other), ups_own, qkv_own, rows_of)
        d_qkv, d_out, d_inputs = attn_products(d_qkv_rows, ctx_own, n1, d_rows, dx_all, w_out.shape[I1:])
        d_up, d_down = mlp_products(d_up_rows, hidden, n2, flat(og_same, og_other))
        weight_grads = (d_qkv.transpose(I3, I0, I1, I2), d_out, d_up, d_down)
        mine = jnp.sum(dg_same + dg_other, I1)
        loss = jnp.sum(loss_all) * (0.5 * norm_factor)

        return (loss.reshape(I1), d_inputs) + tuple(g[None] for g in weight_grads) + (mine[I0][None], mine[I1][None])

    return jax.shard_map(device_fn, mesh=mesh, in_specs=(act_spec, act_spec) + weight_specs, out_specs=(P('rep'), act_spec) + weight_specs, check_vma=False)
```

```python
import functools

import jax
import jax.numpy as jnp
from jax import lax
from jax.experimental import pallas as pl
from jax.experimental.pallas import tpu as pltpu
from jax.sharding import PartitionSpec as P

NORM_EPS = 1e-5
BF = jnp.bfloat16
F32 = jnp.float32
MESH = pl.DeviceIdType.MESH
ANY = pl.ANY


GELU_A = 0.7978845608028654
GELU_B = 0.044715
I0, I1, I2, I3, I4, I6, I8 = 0, 1, 2, 3, 4, 6, 8
CHUNK = 1024
BLOCK = 384
SUB = 256
DEPTH = 6
BACK_DEPTH = 5
KDEPTH = 3
EARLY_G = 3
STAGGER_NS = 6000
EARLY_SEEDS = 5
EARLY_DX = 2
HEAD_PAD = 128
VMEM_LIMIT = 67043328


def mm(a, b):
    return lax.dot_general(a, b, (((I1,), (I0,)), ((), ())), preferred_element_type=F32)


def mm_nt(a, b):
    return lax.dot_general(a, b, (((I1,), (I1,)), ((), ())), preferred_element_type=F32)


def mm_tn(a, b):
    return lax.dot_general(a, b, (((I0,), (I0,)), ((), ())), preferred_element_type=F32)


class Place:
    def __init__(self):
        self.tp = lax.axis_index('tp')
        self.stage = lax.axis_index('stage')
        self.core = self.stage % I2
        self.x_pos = self.stage // I2
        self.home = self.x_pos * (I3 - I2 * self.tp) + self.tp
        self.is_l = self.stage == self.home
        self.sib = self.stage + I1 - I2 * self.core

    def at(self, tp, stage):
        return {'tp': tp, 'stage': stage}

    @property
    def sibling(self):
        return self.at(self.tp, self.sib)

    @property
    def along_x(self):
        return self.at(self.tp, (self.stage + I2) % I4)

    @property
    def across(self):
        return self.at(I1 - self.tp, self.stage)

    @property
    def across_other(self):
        return self.at(I1 - self.tp, self.sib)

    def chain(self, delta):
        there = self.home + delta
        x_pos = there // I2
        tp = there % I2 + x_pos * (I1 - I2 * (there % I2))
        return self.at(tp, I2 * x_pos + self.core)


def entry_barrier(place):
    barrier = pltpu.get_barrier_semaphore()
    for d_tp in (I0, I1):
        for d_stage in range(I4):
            if d_tp or d_stage:
                tp = place.tp + d_tp - I2 * d_tp * place.tp
                stage = (place.stage + d_stage) % I4
                pl.semaphore_signal(barrier, inc=I1, device_id=place.at(tp, stage), device_id_type=MESH)
    pl.semaphore_wait(barrier, 7)


def remote(src, dst, send_sem, recv_sem, device_id):
    return pltpu.make_async_remote_copy(src_ref=src, dst_ref=dst, send_sem=send_sem, recv_sem=recv_sem, device_id=device_id, device_id_type=MESH)


def rows_loop(total, step, body):
    def run(i, carry):
        body(pl.ds(pl.multiple_of(i * step, step), step))
        return carry
    lax.fori_loop(I0, total // step, run, I0)


def norm_rows(src, gain_row, dst, total):
    def body(rows):
        v = src[rows, :].astype(F32)
        inv = lax.rsqrt(jnp.mean(v * v, axis=-I1, keepdims=True) + NORM_EPS)
        dst[rows, :] = (v * inv * gain_row).astype(BF)
    rows_loop(total, 32, body)


def gelu_gate(u):
    u2 = u * u
    t = jnp.tanh(u * (GELU_A + (GELU_A * GELU_B) * u2))
    return 0.5 * t + 0.5, u2


def gelu_slope(hidden, gate, u2):
    return gate + hidden * (1.0 - gate) * (2.0 * GELU_A + (6.0 * GELU_A * GELU_B) * u2)


def row_parts(heads, cut=128):
    return [(*(x[low:high] for x in queries), *(x[:high] for x in keys), low)
            for queries, keys in heads for low, high in ((I0, cut), (cut, queries[I0].shape[I0]))]


def softmax_parts(scores, starts, keys_axis):
    masked = []
    for s, start in zip(scores, starts):
        k_pos = lax.broadcasted_iota(jnp.int32, s.shape, keys_axis)
        q_pos = lax.broadcasted_iota(jnp.int32, s.shape, I1 - keys_axis) + start
        masked.append(jnp.where(k_pos <= q_pos, s, -1e30))
    tops = [jnp.max(s, axis=keys_axis, keepdims=True) for s in masked]
    powers = [jnp.exp(s - top) for s, top in zip(masked, tops)]
    scales = [1.0 / jnp.sum(e, axis=keys_axis, keepdims=True) for e in powers]
    return [e * r for e, r in zip(powers, scales)]


def join_keys(top, low, cut=128):
    return jnp.concatenate([top + low[:cut], low[cut:]], I0).astype(BF)


def nothing():
    pass


def attention_forward(heads, scale, between=()):
    work = iter(between)
    units = row_parts([((q,), (k, v)) for q, k, v in heads])
    scores = [mm_nt(q, k) * scale for q, k, _, _ in units]
    next(work, nothing)()
    probs = softmax_parts(scores, [u[-I1] for u in units], I1)
    next(work, nothing)()
    parts = [mm(p.astype(BF), u[I2]) for p, u in zip(probs, units)]
    return [jnp.concatenate([a, b], I0).astype(BF) for a, b in zip(parts[I0::I2], parts[I1::I2])]


def attention_backward(heads, scale, between=()):
    work = iter(between)
    units = row_parts([((q, dc), (k, v)) for q, k, v, dc in heads])
    scores = [mm_nt(k, q) * scale for q, _, k, _, _ in units]
    dps = [mm_nt(v, dc) for _, dc, _, v, _ in units]
    next(work, nothing)()
    probs = softmax_parts(scores, [u[-I1] for u in units], I0)
    next(work, nothing)()
    dps = [dp.astype(BF).astype(F32) for dp in dps]
    deltas = [jnp.sum(dp * p, axis=I0, keepdims=True) for dp, p in zip(dps, probs)]
    dss = [p * (dp - delta) * scale for p, dp, delta in zip(probs, dps, deltas)]
    terms = []
    for ds in dss:
        hi = ds.astype(BF)
        rest = ds - hi.astype(F32)
        lo = rest.astype(BF)
        terms.append((hi, lo, (rest - lo.astype(F32)).astype(BF)))
    next(work, nothing)()
    dvs = [mm(p.astype(BF), u[I1]) for p, u in zip(probs, units)]
    dks = [mm(hi, u[I0]) + (mm(lo, u[I0]) + mm(tail, u[I0])) for (hi, lo, tail), u in zip(terms, units)]
    k_turned = [u[I2].T for u in units]
    dqs = [(mm(kt, hi) + (mm(kt, lo) + mm(kt, tail))).astype(BF) for (hi, lo, tail), kt in zip(terms, k_turned)]
    return [(jnp.concatenate([dqs[i].T, dqs[i + I1].T], I0), join_keys(dks[i], dks[i + I1]), join_keys(dvs[i], dvs[i + I1]))
            for i in range(I0, len(units), I2)]


def blocked(rows, stack, cols):
    total = mm(rows[:, I0:CHUNK], stack[I0, :, cols])
    for j in range(I1, stack.shape[I0]):
        total = total + mm(rows[:, j * CHUNK:(j + I1) * CHUNK], stack[j, :, cols])
    return total


def lanes(offset, size):
    return pl.ds(pl.multiple_of(offset, 128), size)


def load_resident(buf, sem, halves):
    for c in range(I6):
        for condition, ref in halves[c // I3]:
            copy = pltpu.make_async_copy(ref.at[(c % I3) * CHUNK:(c % I3 + I1) * CHUNK, :], buf.at[c], sem.at[c])
            if condition is None:
                copy.start()
            else:
                pl.when(condition)(copy.start)


def load_heads(ref, index, dst, sem):
    for r in range(I8):
        rows = pl.ds(pl.multiple_of(index * 768 + r * 96, 96), 96)
        pltpu.make_async_copy(ref.at[rows, :], dst.at[r * 128:r * 128 + 96, :], sem).start()


class Stream:
    def __init__(self, buf, sem, depth, parts, total, by_heads):
        self.buf, self.sem, self.depth, self.parts, self.total, self.by_heads = buf, sem, depth, parts, total, by_heads
        self.per_tick = sum(p[I1] for p in parts)

    def copy_in(self, ref, index, slot):
        if not self.by_heads:
            pltpu.make_async_copy(ref.at[index], self.buf.at[slot], self.sem.at[slot]).start()
            return
        load_heads(ref, index, self.buf.at[slot], self.sem.at[slot])

    def start(self, seq):
        @pl.when(seq < self.total)
        def _():
            j = seq % self.per_tick
            slot = seq % self.depth
            base = I0
            for choices, chunks in self.parts:
                for condition, ref in choices:
                    here = (j >= base) & (j < base + chunks)
                    here = here if condition is None else here & condition

                    @pl.when(here)
                    def _(ref=ref, low=base):
                        self.copy_in(ref, j - low, slot)
                base += chunks

    def prime(self):
        for seq in range(self.depth):
            self.start(jnp.int32(seq))

    def wait(self, seq):
        slot = seq % self.depth
        ref = self.parts[I0][I0][I0][I1]
        if self.by_heads:
            pltpu.make_async_copy(ref.at[I0:768, :], self.buf.at[slot, I0:768, :], self.sem.at[slot]).wait()
        else:
            pltpu.make_async_copy(ref.at[I0], self.buf.at[slot], self.sem.at[slot]).wait()
        return self.buf.at[slot]


PIECES = [(0, 0, 0), (0, 0, 1), (0, 0, 2), (1, 0, 0), (2, 1, 0), (2, 1, 1), (2, 1, 2), (2, 1, 3), (3, 0, 0), (3, 0, 1), (3, 0, 2), (3, 0, 3)]


ROUND = (11,)
ROUND_STEPS = (1,)
ORDER = (0, 1, 2, 3, 4, 5, 6, 7, 11, 8, 9, 10)


def piece(ref, axis, index):
    return ref.at[index * 768:(index + I1) * 768, :] if axis == I0 else ref.at[:, index * 768:(index + I1) * 768]


def weight_phase(place, is_r, own, near, far, turned, up_chunks, wn, wk, send_sem, y_send, d_send, near_sem, far_sem, load_sem, store_sem, chunk_sem,
                 round_a, round_b, ra_sem, rb_sem, x_send, xd_send, rs_send):
    wk[...] = jnp.zeros_like(wk)
    early = place.home < I2

    def piece_of(arrays, c):
        i, axis, index = PIECES[c]
        return piece(arrays[i], axis, index)

    @pl.when(place.is_l)
    def _():
        for i in range(I4):
            remote(own[i], near[i], send_sem.at[i], near_sem.at[i], place.sibling).start()

    @pl.when(is_r)
    def _():
        for k, c in enumerate(ROUND):
            @pl.when(early)
            def _(k=k, c=c):
                remote(piece_of(own, c), round_a.at[k], x_send.at[k], ra_sem.at[k], place.along_x).start()
        for c, (i, axis, index) in enumerate(PIECES):
            if c not in ROUND:
                remote(piece_of(own, c), piece_of(far, c), y_send.at[i], far_sem.at[c], place.across_other).start()
        for k, c in enumerate(ROUND):
            @pl.when(jnp.logical_not(early))
            def _(k=k, c=c):
                remote(piece_of(own, c), piece_of(far, c), x_send.at[k], far_sem.at[c], place.across_other).start()

    def load(i, refs, t, slot):
        for condition, ref in refs:
            def go(ref=ref):
                if i < I2:
                    for r in range(I2):
                        rows = pl.ds(pl.multiple_of(t * 192 + r * 96, 96), 96)
                        pltpu.make_async_copy(ref.at[rows, :], wk.at[I0, pl.ds(slot * SUB + r * 128, 96), :], load_sem.at[slot]).start()
                elif i == I2:
                    pltpu.make_async_copy(ref.at[:, lanes(t * SUB, SUB)], wn.at[slot, :, I0:SUB], load_sem.at[slot]).start()
                else:
                    rows = pl.ds(pl.multiple_of(t * SUB, SUB), SUB)
                    pltpu.make_async_copy(ref.at[rows, :], wk.at[I0, pl.ds(512 + slot * SUB, SUB), :], load_sem.at[slot]).start()
            if condition is None:
                go()
            else:
                pl.when(condition)(go)

    def loaded(i, refs, slot):
        ref = refs[I0][I1]
        if i < I2:
            pltpu.make_async_copy(ref.at[I0:192, :], wk.at[I0, I0:192, :], load_sem.at[slot]).wait()
        elif i == I2:
            pltpu.make_async_copy(ref.at[:, I0:SUB], wn.at[slot, :, I0:SUB], load_sem.at[slot]).wait()
        else:
            pltpu.make_async_copy(ref.at[I0:SUB, :], wk.at[I0, 512:768, :], load_sem.at[slot]).wait()

    def store(i, dst, t, slot):
        if i == I2:
            rows = pl.ds(pl.multiple_of(t * SUB, SUB), SUB)
            return pltpu.make_async_copy(wk.at[I1, pl.ds(slot * SUB, SUB), :], dst.at[rows, :], store_sem.at[slot])
        return pltpu.make_async_copy(wn.at[slot, :, SUB:512], dst.at[t // I4, :, lanes(t % I4 * SUB, SUB)], store_sem.at[slot])

    def keep(which, t, slot):
        return pltpu.make_async_copy(wn.at[slot, :, I0:SUB], up_chunks[which].at[t // I4, :, lanes(t % I4 * SUB, SUB)], chunk_sem.at[slot])

    def turn(i, refs, which, first, count):
        dst = turned[i][which]
        load(i, refs, first, I0)

        def step(n, c):
            slot = n % I2

            if i == I2:
                @pl.when(n > I0)
                def _():
                    keep(which, first + n - I1, I1 - slot).wait()

            @pl.when(n + I1 < count)
            def _():
                load(i, refs, first + n + I1, I1 - slot)
            loaded(i, refs, slot)
            if i == I2:
                keep(which, first + n, slot).start()

            @pl.when(n >= I2)
            def _():
                store(i, dst, first + n - I2, slot).wait()
            for b in range(I6):
                cut = slice(b * SUB, b * SUB + SUB)
                if i == I2:
                    wk[I1, pl.ds(pl.multiple_of(slot * SUB, SUB), SUB), cut] = wn[slot, cut, I0:SUB].T
                else:
                    base = I0 if i < I2 else 512
                    wn[slot, cut, SUB:512] = wk[I0, pl.ds(pl.multiple_of(base + slot * SUB, SUB), SUB), cut].T
            store(i, dst, first + n, slot).start()
            return c
        lax.fori_loop(I0, count, step, I0)
        for n in (count - I2, count - I1):
            store(i, dst, first + n, n % I2).wait()
        if i == I2:
            keep(which, first + count - I1, (count - I1) % I2).wait()

    counts = (12, I4, 12, 12)
    for i in range(I4):
        @pl.when(is_r)
        def _(i=i):
            remote(near[i], near[i], send_sem.at[i], near_sem.at[i], place.sibling).wait_recv()
        turn(i, [(place.is_l, own[i]), (is_r, near[i])], I0, I0, counts[i])
        if i < len(ROUND):
            @pl.when(place.is_l & jnp.logical_not(early))
            def _(k=i):
                remote(round_a.at[k], round_a.at[k], rs_send.at[k], ra_sem.at[k], place.sibling).wait_recv()
                remote(round_a.at[k], round_b.at[k], rs_send.at[k], rb_sem.at[k], place.across).start()
    for c in ORDER:
        i, axis, index = PIECES[c]
        view = piece_of(far, c)
        for k, step in enumerate(ROUND_STEPS):
            if c == step:
                @pl.when(is_r & jnp.logical_not(early))
                def _(k=k):
                    remote(round_b.at[k], round_b.at[k], rs_send.at[k], rb_sem.at[k], place.sibling).wait_recv()
                    remote(round_b.at[k], piece_of(far, ROUND[k]), rs_send.at[k], far_sem.at[ROUND[k]], place.along_x).start()
        remote(view, view, d_send.at[i], far_sem.at[c], place.sibling).wait_recv()
        gives = is_r
        sem = d_send.at[i]
        if c in ROUND:
            gives = (early & place.is_l) | (jnp.logical_not(early) & is_r)
            sem = xd_send.at[ROUND.index(c)]

        @pl.when(gives)
        def _(c=c, view=view, sem=sem):
            remote(view, view, sem, far_sem.at[c], place.sibling).start()
        count = I4 if i < I2 else I3
        turn(i, [(None, far[i])], I1, index * count, count)

    @pl.when(place.is_l)
    def _():
        for i in range(I4):
            remote(own[i], near[i], send_sem.at[i], near_sem.at[i], place.sibling).wait_send()

    @pl.when(is_r)
    def _():
        for i in range(I4):
            part = own[i] if i < I3 else own[i].at[I0:(I4 - len(ROUND)) * 768, :]
            remote(part, part, y_send.at[i], far_sem.at[I0], place.across_other).wait_send()
            remote(part, part, d_send.at[i], far_sem.at[I0], place.sibling).wait_send()
        for k in range(len(ROUND)):
            remote(round_a.at[k], round_a.at[k], x_send.at[k], far_sem.at[I0], place.sibling).wait_send()

    @pl.when((early & place.is_l) | (jnp.logical_not(early) & is_r))
    def _():
        for k in range(len(ROUND)):
            remote(round_a.at[k], round_a.at[k], xd_send.at[k], far_sem.at[I0], place.sibling).wait_send()

    @pl.when(jnp.logical_not(early))
    def _():
        for k in range(len(ROUND)):
            remote(round_a.at[k], round_a.at[k], rs_send.at[k], far_sem.at[I0], place.sibling).wait_send()


def near_choices(place, own, near):
    return [(place.is_l, own), (jnp.logical_not(place.is_l), near)]


def forward_kernel(dims, x_ref, y_ref, wq, wo, wu, wd, own_gains,
                   a_s, h_s, qkv_s, u_s, g_s, oh_same, oh_other, oa_same, oa_other, og_same, og_other, loss_s, home_gains,
                   nq, no, nu, nd, fq, fo, fu, fd, tq0, to0, tu0, td0, tq1, to1, tu1, td1, uc0, uc1, round_a, round_b,
                   abuf, hbuf, obuf, nbuf, ybuf, sbuf, qkvbuf, ubuf, zbuf, ctxbuf, lossbuf, losstile, gains, wres, wores, wn,
                   send_sem, y_send, d_send, near_sem, far_sem, t_load, t_store, t_keep, ra_sem, rb_sem, x_send, xd_send, rs_send,
                   act_sem, hop_f, keep_sem, save_sem, stream_n, res_sem, out_sem, big_sem, y_sem, s_sem,
                   os_sem, oo_sem, as_sem, ao_sem, gs_sem, go_sem, bulk, gain_sem, tiny):
    micro, seq, width, heads, head_dim, ffn = dims
    place = Place()
    is_first, is_last = place.home == I0, place.home == I3
    home02 = (place.home == I0) | (place.home == I2)
    home13 = jnp.logical_not(home02)
    is_r = jnp.logical_not(place.is_l)
    takes_x = (place.home == I1) & is_r
    half = heads // I2 * HEAD_PAD
    scale = head_dim ** -0.5
    norm_factor = 1.0 / (micro * I2 * seq * width)
    own, near, far = (wq, wo, wu, wd), (nq, no, nu, nd), (fq, fo, fu, fd)
    turned = ((tq0, tq1), (to0, to1), (tu0, tu1), (td0, td1))
    entry_barrier(place)

    @pl.when(place.is_l)
    def _():
        pltpu.make_async_copy(own_gains, gains, gain_sem.at[I0]).start()
        remote(own_gains, gains, gain_sem.at[I1], gain_sem.at[I0], place.sibling).start()

    @pl.when(is_first)
    def _():
        for m in range(micro):
            pltpu.make_async_copy(x_ref.at[m, place.core], abuf.at[m], act_sem.at[m]).start()
    weight_phase(place, is_r, own, near, far, turned, (uc0, uc1), wn, wores, send_sem, y_send, d_send, near_sem, far_sem, t_load, t_store, t_keep,
                 round_a, round_b, ra_sem, rb_sem, x_send, xd_send, rs_send)
    pltpu.make_async_copy(own_gains, gains, gain_sem.at[I0]).wait()
    pltpu.make_async_copy(gains, home_gains, gain_sem.at[I0]).start()

    @pl.when(place.is_l)
    def _():
        remote(own_gains, gains, gain_sem.at[I1], gain_sem.at[I0], place.sibling).wait_send()

    def near_of(i):
        return near_choices(place, own[i], near[i])

    def saved(dst, index):
        return pltpu.make_async_copy(hbuf, dst, save_sem.at[index])

    sn = Stream(wn, stream_n, DEPTH, [([(None, tq0)], I3), ([(None, tq1)], I3), ([(None, uc0)], I3), ([(None, uc1)], I3)], micro * 12, False)
    for c, choices in enumerate((near_of(I1), [(None, fo)])):
        for condition, ref in choices:
            def go(ref=ref, c=c):
                load_heads(ref, I0, wores.at[c], out_sem.at[c])
            go() if condition is None else pl.when(condition)(go)
    sn.prime()
    load_resident(wres, res_sem, (near_of(I3), [(None, fd)]))
    lossbuf[...] = jnp.zeros_like(lossbuf)

    def qkv_out(m):
        return pltpu.make_async_copy(qkvbuf, qkv_s.at[m], big_sem.at[I0])

    def up_out(m):
        return pltpu.make_async_copy(ubuf, u_s.at[m], big_sem.at[I1])

    def act_out(m):
        return pltpu.make_async_copy(abuf.at[m], a_s.at[m], save_sem.at[I2])

    def hop_block(m, n):
        cols = lanes(n * SUB, SUB)
        return remote(obuf.at[m % I2, :, cols], abuf.at[m, :, cols], hop_f.at[m % I2], act_sem.at[m], place.chain(I1))

    def hop_forward(m):
        return remote(obuf.at[m % I2], abuf.at[m], hop_f.at[m % I2], act_sem.at[m], place.chain(I1))

    def near_hand(src, dst_far, dst_own, sem, recv_sem):
        return (lambda: remote(src, dst_far, sem, recv_sem, place.sibling)), (lambda: pltpu.make_async_copy(src, dst_own, sem))

    def hand_out(m):
        return near_hand(obuf.at[m % I2], oa_other.at[m], oa_same.at[m], keep_sem.at[m % I2], ao_sem)

    def both_kinds(condition, copies, start):
        far_copy, own_copy = copies

        @pl.when(condition & place.is_l)
        def _():
            far_copy().start() if start else far_copy().wait_send()

        @pl.when(condition & is_r)
        def _():
            own_copy().start() if start else own_copy().wait()

    def x_out(m):
        return pltpu.make_async_copy(ybuf, oa_same.at[m], y_sem), pltpu.make_async_copy(sbuf, oa_other.at[m], s_sem)

    def seed_out(m):
        return pltpu.make_async_copy(sbuf, g_s.at[m], s_sem)

    def far_mid(m, condition):
        @pl.when(condition & place.is_l)
        def _():
            remote(h_s.at[m], oh_same.at[m], bulk.at[I2], os_sem, place.across).start()

        @pl.when(condition & is_r)
        def _():
            remote(h_s.at[m], oh_other.at[m], bulk.at[I2], oo_sem, place.across_other).start()

    def send_seed(m):
        seed_out(m).wait()

        @pl.when(place.is_l & (m < EARLY_SEEDS))
        def _():
            remote(g_s.at[m], og_same.at[m], bulk.at[I1], gs_sem, place.across).start()

        @pl.when(is_r & (m < EARLY_SEEDS))
        def _():
            remote(g_s.at[m], og_other.at[m], bulk.at[I1], go_sem, place.across_other).start()

    def forward_tick(m, carry):
        act, mid, out = abuf.at[m], hbuf, obuf.at[m % I2]
        pltpu.make_async_copy(x_ref.at[m, place.core], act, act_sem.at[m]).wait()
        act_out(m).start()

        @pl.when(place.is_l)
        def _():
            pltpu.make_async_copy(act, oa_same.at[m], as_sem).start()

        @pl.when(is_last)
        def _():
            pltpu.make_async_copy(y_ref.at[m, place.core], ybuf, y_sem).start()

        @pl.when(takes_x)
        def _():
            @pl.when(m > I0)
            def _():
                for copy in x_out(m):
                    copy.wait()
            for core, buf, sem in ((place.core, ybuf, y_sem), (I1 - place.core, sbuf, s_sem)):
                pltpu.make_async_copy(x_ref.at[m, core], buf, sem).start()
        norm_rows(act, gains[I0:I1, :], nbuf, seq)

        @pl.when(m > I0)
        def _():
            qkv_out(m).wait()

        def qkv_step(j, c):
            w = sn.wait(m * 12 + j)
            for n in range(I0, CHUNK, SUB):
                qkvbuf[:, lanes(j * CHUNK + n, SUB)] = mm(nbuf[...], w[:, n:n + SUB]).astype(BF)
            sn.start(m * 12 + j + DEPTH)
            return c
        lax.fori_loop(I0, I6, qkv_step, I0)
        qkv_out(m).start()
        act_out(m).wait()

        @pl.when(is_r)
        def _():
            remote(a_s.at[m], oa_other.at[m], bulk.at[I0], ao_sem, place.sibling).start()

        def head_step(i, c):
            base = i * (I3 * half)
            views = [[qkvbuf[:, lanes(base + t * half + r * HEAD_PAD, HEAD_PAD)] for t in range(I3)] for r in range(I8)]
            for r, context in enumerate(attention_forward(views, scale)):
                ctxbuf[:, lanes(i * half + r * HEAD_PAD, HEAD_PAD)] = context
            return c
        lax.fori_loop(I0, I2, head_step, I0)

        @pl.when(m == I0)
        def _():
            for c in range(I2):
                pltpu.make_async_copy(wo, wores.at[c, I0:768, :], out_sem.at[c]).wait()
        for n in range(I0, width, SUB):
            total = mm(ctxbuf[:, I0:half], wores[I0, :, n:n + SUB]) + mm(ctxbuf[:, half:I2 * half], wores[I1, :, n:n + SUB])
            mid[:, n:n + SUB] = (act[:, n:n + SUB].astype(F32) + total).astype(BF)
        saved(h_s.at[m], I0).start()

        @pl.when(place.is_l)
        def _():
            saved(oh_same.at[m], I1).start()
        norm_rows(mid, gains[I1:I2, :], nbuf, seq)

        @pl.when(m > I0)
        def _():
            up_out(m).wait()

        def up_step(j, c):
            w = sn.wait(m * 12 + I6 + j)
            for n in range(I0, CHUNK, SUB):
                u = mm(nbuf[...], w[:, n:n + SUB]).astype(BF)
                at = lanes(j * CHUNK + n, SUB)
                ubuf[:, at] = u
                uf = u.astype(F32)
                zbuf[:, at] = (uf * gelu_gate(uf)[I0]).astype(BF)
            sn.start(m * 12 + I6 + j + DEPTH)
            return c
        lax.fori_loop(I0, I6, up_step, I0)
        up_out(m).start()

        @pl.when((m > I1) & jnp.logical_not(is_last))
        def _():
            hop_forward(m).wait_send()

        both_kinds((m > I1) & home02, hand_out(m), False)

        @pl.when(m == I0)
        def _():
            for j in range(I6):
                pltpu.make_async_copy(wd.at[I0:CHUNK, :], wres.at[j], res_sem.at[j]).wait()

        def down_step(n, c):
            cols = lanes(n * SUB, SUB)
            out[:, cols] = (mid[:, cols].astype(F32) + blocked(zbuf, wres, cols)).astype(BF)

            @pl.when((n > I0) & jnp.logical_not(is_last))
            def _():
                hop_block(m, n - I1).start()
            return c
        lax.fori_loop(I0, width // SUB, down_step, I0)

        @pl.when(jnp.logical_not(is_last))
        def _():
            hop_block(m, width // SUB - I1).start()

        both_kinds(home02, hand_out(m), True)

        @pl.when(is_last)
        def _():
            pltpu.make_async_copy(y_ref.at[m, place.core], ybuf, y_sem).wait()

            @pl.when(m > I0)
            def _():
                send_seed(m - I1)

            def seed(rows):
                error = out[rows, :].astype(F32) - ybuf[rows, :].astype(F32)
                sbuf[rows, :] = (error * norm_factor).astype(BF)
                lossbuf[...] += jnp.sum((error * error).reshape(I4, I8, width), axis=I0)
            rows_loop(seq, 32, seed)
            seed_out(m).start()

        @pl.when(takes_x)
        def _():
            for core, buf, sem in ((place.core, ybuf, y_sem), (I1 - place.core, sbuf, s_sem)):
                pltpu.make_async_copy(x_ref.at[m, core], buf, sem).wait()
            for copy in x_out(m):
                copy.start()

        saved(h_s.at[m], I0).wait()

        @pl.when(place.is_l)
        def _():
            saved(oh_same.at[m], I1).wait()

        @pl.when(is_r)
        def _():
            remote(h_s.at[m], oh_other.at[m], bulk.at[I3], oo_sem, place.sibling).start()

        far_mid(m, home13 | (m % I2 == I1))
        return carry

    @pl.when(is_first & (place.core == I0))
    def _():
        pl.delay(STAGGER_NS)
    lax.fori_loop(I0, micro, forward_tick, I0)
    for m in range(I0, micro, I2):
        far_mid(m, is_first)

    @pl.when(is_last)
    def _():
        total = lossbuf[:, I0:128]
        for n in range(128, width, 128):
            total = total + lossbuf[:, n:n + 128]
        losstile[...] = total
        pltpu.make_async_copy(losstile, loss_s, tiny).start()
    for copy in (qkv_out(micro - I1), up_out(micro - I1)):
        copy.wait()

    @pl.when(jnp.logical_not(is_last))
    def _():
        for m in (micro - I2, micro - I1):
            hop_forward(m).wait_send()
    for m in (micro - I2, micro - I1):
        both_kinds(home02, hand_out(m), False)

    @pl.when(is_last)
    def _():
        seed_out(micro - I1).wait()
        pltpu.make_async_copy(losstile, loss_s, tiny).wait()

    @pl.when(takes_x)
    def _():
        for copy in x_out(micro - I1):
            copy.wait()
    pltpu.make_async_copy(gains, home_gains, gain_sem.at[I0]).wait()
    sent, got = drain(place)

    @pl.when(place.home != I2)
    def _():
        sent(h_s, bulk.at[I2])

    @pl.when(place.home == I2)
    def _():
        sent(h_s.at[I0:micro // I2], bulk.at[I2])

    @pl.when(place.is_l | jnp.logical_not(is_last))
    def _():
        got(oh_other, oo_sem)

    @pl.when(is_r & is_last)
    def _():
        got(oh_other.at[I0:micro // I2], oo_sem)

    @pl.when(is_last)
    def _():
        sent(g_s.at[I0:EARLY_SEEDS], bulk.at[I1])

    @pl.when((place.home == I2) & is_r)
    def _():
        got(og_same.at[I0:EARLY_SEEDS], gs_sem)
        got(og_other.at[I0:EARLY_SEEDS], go_sem)

    @pl.when(is_r)
    def _():
        sent(a_s, bulk.at[I0])
        sent(h_s, bulk.at[I3])

    @pl.when(is_r & jnp.logical_not(is_last))
    def _():
        got(oh_same, os_sem)

    @pl.when(is_r & is_last)
    def _():
        got(oh_same.at[I0:micro // I2], os_sem)

    @pl.when(place.is_l)
    def _():
        got(oa_same, as_sem)

    @pl.when(place.is_l | home02)
    def _():
        got(oa_other, ao_sem)


def drain(place):
    def sent(buf, sem):
        remote(buf, buf, sem, sem, place.sibling).wait_send()

    def got(dst, sem):
        pltpu.make_async_copy(dst, dst, sem).wait()
    return sent, got


def backward_kernel(dims, a_s, h_s, qkv_s, u_s, g_s, wq, nq, fq, td0, td1, to0, to1, tu0, tu1, gains, loss_s, after, *refs):
    (dx_s, m_s, od_same, od_other, og_same, og_other, oa_same, oa_other, oh_same, oh_other, dg_same, dg_other, loss_all,
     gbuf, hbuf, obuf, qkvbuf, ubuf, habuf, zbuf, ctxbuf, dqkvbuf, acc, accg, wres, wn, wk,
     grad_sem, hop_b, back_sem, dx_sem, dx_send, save_sem, stream_n, stream_k, res_sem, load_sem,
     ds_sem, do_sem, gs_sem, go_sem, as_sem, ao_sem, os_sem, oo_sem, bulk, tiny, loss_sem, ready) = refs[I6:]
    micro, seq, width, heads, head_dim, ffn = dims
    place = Place()
    is_first, is_last = place.home == I0, place.home == I3
    home13 = (place.home == I1) | is_last
    is_r = jnp.logical_not(place.is_l)
    half = heads // I2 * HEAD_PAD
    scale = head_dim ** -0.5

    barrier = pltpu.get_barrier_semaphore()
    is_b, is_c = place.home == I1, place.home == I2
    pl.semaphore_signal(barrier, inc=I1, device_id=place.sibling, device_id_type=MESH)

    @pl.when(jnp.logical_not(is_first))
    def _():
        for there in (place.across, place.across_other):
            pl.semaphore_signal(barrier, inc=I1, device_id=there, device_id_type=MESH)

    @pl.when(is_c)
    def _():
        pl.semaphore_signal(barrier, inc=I1, device_id=place.along_x, device_id_type=MESH)

    @pl.when(is_last)
    def _():
        for m in range(micro):
            pltpu.make_async_copy(g_s.at[m], gbuf.at[m], grad_sem.at[m]).start()
    wk[...] = jnp.zeros_like(wk)
    bn = Stream(wn, stream_n, BACK_DEPTH, [([(None, td0)], I3), ([(None, td1)], I3), ([(None, to0)], I1), ([(None, to1)], I1)], micro * I8, False)
    bk = Stream(wk, stream_k, KDEPTH, [(near_choices(place, wq, nq), I3), ([(None, fq)], I3)], micro * I6, True)
    bn.prime()
    bk.prime()
    load_resident(wres, res_sem, ([(None, tu0)], [(None, tu1)]))

    def saved(dst, index):
        return pltpu.make_async_copy(hbuf, dst, save_sem)

    def both_kinds(condition, copies, start):
        far_copy, own_copy = copies

        @pl.when(condition & place.is_l)
        def _():
            far_copy().start() if start else far_copy().wait_send()

        @pl.when(condition & is_r)
        def _():
            own_copy().start() if start else own_copy().wait()

    def near_hand(src, dst_far, dst_own, sem, recv_sem):
        return (lambda: remote(src, dst_far, sem, recv_sem, place.sibling)), (lambda: pltpu.make_async_copy(src, dst_own, sem))

    def loads(i):
        m = micro - I1 - i
        return [pltpu.make_async_copy(src.at[m], dst, load_sem.at[k])
                for k, (src, dst) in enumerate(((u_s, ubuf), (qkv_s, qkvbuf), (h_s, habuf.at[I0]), (a_s, habuf.at[I1])))]

    def load_next(i, k):
        @pl.when(i + I1 < micro)
        def _():
            loads(i + I1)[k].start()

    for copy in loads(I0):
        copy.start()
    accg[...] = jnp.zeros_like(accg)

    def norm_back(index, x, base, dst, gain_row):
        def body(rows):
            xf = x[rows, :].astype(F32)
            dy = acc[rows, :].astype(BF).astype(F32)
            inv = lax.rsqrt(jnp.mean(xf * xf, axis=-I1, keepdims=True) + NORM_EPS)
            xn = xf * inv
            accg[index] += jnp.sum((dy * xn).reshape(I4, I8, width), axis=I0)
            dyg = dy * gain_row
            dx = inv * (dyg - xn * jnp.mean(dyg * xn, axis=-I1, keepdims=True))
            dst[rows, :] = (base[rows, :].astype(F32) + dx).astype(BF)
        rows_loop(seq, 32, body)

    def hop_back(i):
        m = micro - I1 - i
        return remote(obuf.at[i % I2], gbuf.at[m], hop_b.at[i % I2], grad_sem.at[m], place.chain(-I1))

    def hand_back(i):
        m = micro - I1 - i
        return near_hand(obuf.at[i % I2], og_other.at[m], og_same.at[m], back_sem.at[i % I2], go_sem)

    def keep_dx(i):
        return pltpu.make_async_copy(obuf.at[i % I2], dx_s.at[micro - I1 - i], back_sem.at[i % I2])

    def back_ready(i):
        both_kinds((i > I1) & home13, hand_back(i), False)

        @pl.when((i > I1) & is_first)
        def _():
            keep_dx(i).wait()
            dx_to_b(i).wait_send()

        @pl.when((i > I1) & jnp.logical_not(is_first))
        def _():
            hop_back(i).wait_send()

    def pass_loss(tile):
        @pl.when(jnp.logical_not(is_first))
        def _():
            remote(tile, loss_all.at[place.core], loss_sem.at[I0], loss_sem.at[I1], place.chain(-I1)).start()
        remote(tile, loss_all.at[place.core], loss_sem.at[I2], loss_sem.at[I3], place.sibling).start()

    def dx_to_b(i):
        return remote(obuf.at[i % I2], dx_s.at[micro - I1 - i], dx_send.at[i % I2], dx_sem, place.across)

    def backward_tick(i, carry):
        m = micro - I1 - i
        slot = i % I2
        grad, dmid, prev = gbuf.at[m], hbuf, obuf.at[slot]
        u_now, qkv_now, h_now, a_now = ubuf, qkvbuf, habuf.at[I0], habuf.at[I1]

        pltpu.make_async_copy(g_s.at[m], grad, grad_sem.at[m]).wait()

        @pl.when(place.is_l)
        def _():
            pltpu.make_async_copy(grad, og_same.at[m], gs_sem).start()
        load_u, load_qkv, load_h, load_a = loads(i)
        load_u.wait()

        def mlp_step(j, c):
            w = bn.wait(i * I8 + j)
            for n in range(I0, CHUNK, SUB):
                at = lanes(j * CHUNK + n, SUB)
                dz = mm(grad[...], w[:, n:n + SUB]).astype(BF).astype(F32)
                u = u_now[:, at].astype(F32)
                gate, u2 = gelu_gate(u)
                zbuf[:, at] = (dz * gelu_slope(u * gate, gate, u2)).astype(BF)
            bn.start(i * I8 + j + BACK_DEPTH)
            return c
        lax.fori_loop(I0, I6, mlp_step, I0)

        @pl.when(i == I0)
        def _():
            for j in range(I6):
                pltpu.make_async_copy(tu0.at[I0:CHUNK, :], wres.at[j], res_sem.at[j]).wait()

        def turn_back(n, c):
            cols = lanes(n * SUB, SUB)
            acc[:, cols] = blocked(zbuf, wres, cols)
            return c
        lax.fori_loop(I0, width // SUB, turn_back, I0)
        load_next(i, I0)
        load_h.wait()
        norm_back(I1, h_now, grad, dmid, gains[I1:I2, :])
        load_next(i, I2)

        @pl.when(place.is_l)
        def _():
            saved(od_same.at[m], I0).start()

        @pl.when(is_r)
        def _():
            saved(m_s.at[m], I0).start()
        for c in range(I2):
            w = bn.wait(i * I8 + I6 + c)
            for n in range(I0, CHUNK, SUB):
                ctxbuf[:, c * CHUNK + n:c * CHUNK + n + SUB] = mm(dmid[...], w[:, n:n + SUB]).astype(BF)
            bn.start(i * I8 + I6 + c + BACK_DEPTH)
        load_qkv.wait()

        def head_step(t, c):
            base = (t // I2) * (I3 * half) + (t % I2) * (I4 * HEAD_PAD)
            at = [[lanes(base + part * half + r * HEAD_PAD, HEAD_PAD) for part in range(I3)] for r in range(I4)]
            group = [(*(qkv_now[:, p] for p in at[r]), ctxbuf[:, lanes((t * I4 + r) * HEAD_PAD, HEAD_PAD)]) for r in range(I4)]
            for r, grads in enumerate(attention_backward(group, scale)):
                for p, value in zip(at[r], grads):
                    dqkvbuf[:, p] = value
            return c
        lax.fori_loop(I0, I2, lambda t, c: head_step(I2 * t + I1, head_step(I2 * t, c)), I0)
        load_next(i, I1)
        acc[...] = jnp.zeros_like(acc)

        def qkv_step(j, c):
            w = bk.wait(i * I6 + j)
            for n in range(I0, width, SUB):
                acc[:, n:n + SUB] += mm(dqkvbuf[:, lanes(j * CHUNK, CHUNK)], w[:, n:n + SUB])
            bk.start(i * I6 + j + KDEPTH)
            return c
        lax.fori_loop(I0, I6, qkv_step, I0)
        load_a.wait()
        back_ready(i)
        norm_back(I0, a_now, dmid, prev, gains[I0:I1, :])
        load_next(i, I3)

        @pl.when(i == I0)
        def _():
            @pl.when(is_last)
            def _():
                pl.semaphore_wait(barrier, I3)

            @pl.when(is_c)
            def _():
                pl.semaphore_wait(ready, I1)

            @pl.when(is_b)
            def _():
                pl.semaphore_wait(ready, I2)

            @pl.when(is_last)
            def _():
                pass_loss(loss_s)

        @pl.when(jnp.logical_not(is_first))
        def _():
            hop_back(i).start()

        @pl.when(is_first)
        def _():
            keep_dx(i).start()
            dx_to_b(i).start()
        both_kinds(home13, hand_back(i), True)

        @pl.when(place.is_l)
        def _():
            saved(od_same.at[m], I0).wait()
            remote(od_same.at[m], od_same.at[m], bulk.at[I6], ds_sem, place.across).start()

        @pl.when(is_r)
        def _():
            remote(grad, og_other.at[m], bulk.at[5], go_sem, place.sibling).start()
            saved(m_s.at[m], I0).wait()
            remote(m_s.at[m], od_other.at[m], bulk.at[I6], do_sem, place.sibling).start()
            remote(m_s.at[m], od_other.at[m], bulk.at[7], do_sem, place.across_other).start()

        now = (i % I2 == I1) & (i < I2 * EARLY_G)
        far_grad(m, (place.home == I1) & now)
        far_grad(micro - I1 - i // I2, is_last & now)
        return carry

    def far_grad(m, condition):
        @pl.when(condition & place.is_l)
        def _():
            remote(gbuf.at[m], og_same.at[m], bulk.at[I4], gs_sem, place.across).start()

        @pl.when(condition & is_r)
        def _():
            remote(gbuf.at[m], og_other.at[m], bulk.at[I4], go_sem, place.across_other).start()

    @pl.when(jnp.logical_not(is_last))
    def _():
        pl.semaphore_wait(barrier, I3 - is_b.astype(jnp.int32))

    @pl.when(is_first)
    def _():
        for there in (place.across, place.across_other):
            pl.semaphore_signal(ready, inc=I1, device_id=there, device_id_type=MESH)

    @pl.when(is_b)
    def _():
        pl.semaphore_signal(ready, inc=I1, device_id=place.along_x, device_id_type=MESH)

    @pl.when(is_c & place.is_l)
    def _():
        for t in range(micro):
            remote(a_s.at[t], oa_same.at[t], bulk.at[I8], as_sem, place.across).start()
        for t in range(I0, micro, I2):
            remote(h_s.at[t], oh_same.at[t], bulk.at[9], os_sem, place.across).start()

    @pl.when(is_c & is_r)
    def _():
        for t in range(micro):
            remote(a_s.at[t], oa_other.at[t], bulk.at[I8], ao_sem, place.across_other).start()
        for t in range(I0, micro, I2):
            remote(h_s.at[t], oh_other.at[t], bulk.at[9], oo_sem, place.across_other).start()
    lax.fori_loop(I0, micro, backward_tick, I0)
    loss_mine = loss_all.at[place.core]

    @pl.when(is_last)
    def _():
        own_loss = pltpu.make_async_copy(loss_s, loss_mine, loss_sem.at[I1])
        own_loss.start()
        own_loss.wait()

    @pl.when(jnp.logical_not(is_last))
    def _():
        remote(loss_mine, loss_mine, loss_sem.at[I0], loss_sem.at[I1], place.sibling).wait_recv()
        pass_loss(loss_mine)

    @pl.when(place.is_l)
    def _():
        pltpu.make_async_copy(accg, dg_same, tiny.at[I0]).start()
        remote(accg, dg_same, tiny.at[I1], tiny.at[I0], place.across).start()

    @pl.when(is_r)
    def _():
        remote(accg, dg_other, tiny.at[I1], tiny.at[I4], place.sibling).start()
        remote(accg, dg_other, tiny.at[I2], tiny.at[I4], place.across_other).start()

    for i in (micro - I2, micro - I1):
        back_ready(jnp.int32(i))

    sent, got = drain(place)
    sent(m_s, bulk.at[I6])

    @pl.when(is_r)
    def _():
        sent(gbuf, bulk.at[5])
        sent(m_s, bulk.at[7])
        remote(accg, dg_other, tiny.at[I2], tiny.at[I4], place.sibling).wait_send()

    @pl.when(home13)
    def _():
        sent(gbuf.at[I0:EARLY_G], bulk.at[I4])

    @pl.when(place.home == I1)
    def _():
        got(dx_s, dx_sem)

    @pl.when(jnp.logical_not(is_first))
    def _():
        remote(loss_mine, loss_mine, loss_sem.at[I0], loss_sem.at[I1], place.sibling).wait_send()
    remote(loss_mine, loss_mine, loss_sem.at[I2], loss_sem.at[I3], place.sibling).wait_send()
    remote(loss_mine, loss_mine, loss_sem.at[I2], loss_sem.at[I3], place.sibling).wait_recv()

    @pl.when(place.home == I2)
    def _():
        sent(a_s, bulk.at[I8])
        sent(h_s.at[I0:micro // I2], bulk.at[9])

    remote(accg, dg_other, tiny.at[I1], tiny.at[I4], place.sibling).wait_send()
    got(od_other, do_sem)

    @pl.when(place.is_l | home13)
    def _():
        got(og_other, go_sem)

    @pl.when(jnp.logical_not(home13) & is_r)
    def _():
        got(og_same.at[I0:EARLY_G], gs_sem)
        got(og_other.at[I0:EARLY_G], go_sem)
    got(dg_same, tiny.at[I0])
    got(dg_other, tiny.at[I4])

    @pl.when(is_r)
    def _():
        got(od_same, ds_sem)

    @pl.when(place.is_l)
    def _():
        got(og_same, gs_sem)

    @pl.when(is_last & is_r)
    def _():
        got(oa_same, as_sem)
        got(oa_other, ao_sem)
        got(oh_same.at[I0:micro // I2], os_sem)
        got(oh_other.at[I0:micro // I2], oo_sem)


def shapes(*dims_list):
    return [jax.ShapeDtypeStruct(d, BF) for d in dims_list]


def forward_phase(dims, x, y, own, own_gains):
    micro, seq, width, heads, head_dim, ffn = dims
    half = heads // I2 * HEAD_PAD
    act = (micro, seq, width)
    raw = [w.shape for w in own]
    turned = [(I3, width, CHUNK), (I1, width, CHUNK), (ffn // I2, width), (I3, width, CHUNK)]
    out_shape = shapes(act, act, (micro, seq, I6 * half), (micro, seq, ffn), *[act] * 7)
    out_shape += [jax.ShapeDtypeStruct(s, F32) for s in ((I8, 128), own_gains.shape)]
    out_shape += shapes(*raw, *raw, *turned, *turned, turned[I0], turned[I0], *[(len(ROUND), 768, width)] * I2)
    any_spec = pl.BlockSpec(memory_space=ANY)
    vmem, dma = pltpu.VMEM, pltpu.SemaphoreType.DMA
    row = vmem((seq, width), BF)
    scratch = [
        vmem(act, BF), row, vmem((I2, seq, width), BF), row, row, row, vmem((seq, I6 * half), BF), vmem((seq, ffn), BF), vmem((seq, ffn), BF),
        vmem((seq, I2 * half), BF), vmem((I8, width), F32), vmem((I8, 128), F32), vmem((I2, width), F32),
        vmem((I6, CHUNK, width), BF), vmem((I2, CHUNK, width), BF), vmem((DEPTH, width, CHUNK), BF),
        dma((I4,)), dma((I4,)), dma((I4,)), dma((I4,)), dma((12,)), dma((I2,)), dma((I2,)), dma((I2,)), *[dma((len(ROUND),))] * 5,
        dma((micro,)), dma((I2,)), dma((I2,)), dma((I3,)), dma((DEPTH,)), dma((I6,)), dma((I2,)), dma((I2,)), dma(()), dma(()),
        dma(()), dma(()), dma(()), dma(()), dma(()), dma(()), dma((I4,)), dma((I2,)), dma(()),
    ]
    return pl.pallas_call(
        functools.partial(forward_kernel, dims),
        out_shape=tuple(out_shape),
        in_specs=[any_spec] * I6 + [pl.BlockSpec(memory_space=vmem)],
        out_specs=(any_spec,) * len(out_shape),
        scratch_shapes=scratch,
        compiler_params=pltpu.CompilerParams(collective_id=I0, has_side_effects=True, vmem_limit_bytes=VMEM_LIMIT),
        name='forward_phase',
    )(x, y, *own, own_gains)


def backward_phase(dims, saved, weights, gains, loss, after, placed):
    micro, seq, width, heads, head_dim, ffn = dims
    half = heads // I2 * HEAD_PAD
    act = (micro, seq, width)
    out_shape = shapes(*[act] * 10) + [jax.ShapeDtypeStruct((I2, I8, width), F32)] * I2 + [jax.ShapeDtypeStruct((I2, I8, 128), F32)]
    any_spec = pl.BlockSpec(memory_space=ANY)
    vmem, dma = pltpu.VMEM, pltpu.SemaphoreType.DMA
    scratch = [
        vmem(act, BF), vmem((seq, width), BF), vmem((I2, seq, width), BF), vmem((seq, I6 * half), BF), vmem((seq, ffn), BF),
        vmem((I2, seq, width), BF), vmem((seq, ffn), BF), vmem((seq, I2 * half), BF), vmem((seq, I6 * half), BF), vmem((seq, width), F32),
        vmem((I2, I8, width), F32), vmem((I6, CHUNK, width), BF), vmem((BACK_DEPTH, width, CHUNK), BF), vmem((KDEPTH, CHUNK, width), BF),
        dma((micro,)), dma((I2,)), dma((I2,)), dma(()), dma((I2,)), dma(()), dma((BACK_DEPTH,)), dma((KDEPTH,)), dma((I6,)), dma((I4,)),
        *[dma(())] * I8, dma((10,)), dma((5,)), dma((I4,)), pltpu.SemaphoreType.REGULAR,
    ]
    return pl.pallas_call(
        functools.partial(backward_kernel, dims),
        out_shape=tuple(out_shape),
        in_specs=[any_spec] * 14 + [pl.BlockSpec(memory_space=vmem)] * I2 + [any_spec] * 7,
        out_specs=(any_spec,) * len(out_shape),
        scratch_shapes=scratch,
        input_output_aliases={17 + i: I4 + i for i in range(I6)},
        compiler_params=pltpu.CompilerParams(collective_id=I1, has_side_effects=True, vmem_limit_bytes=VMEM_LIMIT),
        name='backward_phase',
    )(*saved, *weights, gains, loss, after, *placed)


def late_rows(micro):
    return [micro - I1 - i for i in range(micro) if i % I2 == I0 or i > I2 * EARLY_G]


def hand_on(place, dx, d_in, og, sems):
    micro = dx.shape[I0]
    barrier = pltpu.get_barrier_semaphore()
    late = late_rows(micro)
    is_leaf = place.home > I1
    gives_g = (place.home == I1) & place.is_l
    takes_g = (place.home == I0) & jnp.logical_not(place.is_l)
    part, g_part = dx.at[I0:EARLY_DX], og.at[I0:len(late)]

    @pl.when(is_leaf)
    def _():
        pl.semaphore_signal(barrier, inc=I1, device_id=place.along_x, device_id_type=MESH)

    @pl.when(takes_g)
    def _():
        pl.semaphore_signal(barrier, inc=I1, device_id=place.across, device_id_type=MESH)

    @pl.when(jnp.logical_not(is_leaf))
    def _():
        pl.semaphore_wait(barrier, I1 + gives_g.astype(jnp.int32))

        @pl.when(gives_g)
        def _():
            for m in late:
                remote(og.at[m], og.at[m], sems.at[I2], sems.at[I3], place.across).start()
        for m in range(micro - EARLY_DX, micro):
            remote(dx.at[m], d_in.at[m, place.core], sems.at[I0], sems.at[I1], place.along_x).start()
        remote(part, part, sems.at[I0], sems.at[I1], place.along_x).wait_send()

        @pl.when(gives_g)
        def _():
            remote(g_part, g_part, sems.at[I2], sems.at[I3], place.across).wait_send()

    def received():
        @pl.when(is_leaf)
        def _():
            remote(part, part, sems.at[I0], sems.at[I1], place.along_x).wait_recv()

        @pl.when(takes_g)
        def _():
            remote(g_part, g_part, sems.at[I2], sems.at[I3], place.across).wait_recv()
    return received


def recompute_kernel(dims, early, h_same, h_other, a_same, a_other, gains, wq, wu, *refs):
    (wqbuf, wubuf, count, sem, sems) = refs[-5:]
    outs = refs[:-5] if early else refs[7:-5]
    (done, u_o, qkv_o, ctx_o, n1_o, n2_o) = outs[I0:I6]
    micro, seq, width, heads, head_dim, ffn = dims
    place = Place()
    scale = head_dim ** -0.5
    half = heads // I2 * HEAD_PAD
    steps = I2 * micro * seq // BLOCK

    def pieces(j):
        copies = [pltpu.make_async_copy(wu.at[:, lanes(j * SUB, SUB)], wubuf.at[:, lanes(j * SUB, SUB)], sem.at[I0, j])]
        for r in range(I2):
            src = pl.ds(pl.multiple_of((I2 * j + r) * head_dim, head_dim), head_dim)
            dst = pl.ds(pl.multiple_of((I2 * j + r) * HEAD_PAD, HEAD_PAD), head_dim)
            copies.append(pltpu.make_async_copy(wq.at[src, :], wqbuf.at[dst, :], sem.at[I1 + r, j]))
        return copies

    def body(hs, ho, rs, ro, u, qkv, ctx, n1, n2):
        step = count[I0]
        count[I0] = step + I1
        for low, high, gain, dst in ((hs, ho, gains[I1:I2, :], n2), (rs, ro, gains[I0:I1, :], n1)):
            @pl.when(step < steps // I2)
            def _(low=low, gain=gain, dst=dst):
                norm_rows(low, gain, dst, BLOCK)

            @pl.when(step >= steps // I2)
            def _(high=high, gain=gain, dst=dst):
                norm_rows(high, gain, dst, BLOCK)

        @pl.when(step == I0)
        def _():
            for j in range(I3 * half // SUB):
                for copy in pieces(j):
                    copy.wait()

        def qkv_step(j, c):
            rows = pl.ds(pl.multiple_of(j * SUB, SUB), SUB)
            qkv[:, lanes(j * SUB, SUB)] = mm_nt(n1[...], wqbuf[rows, :]).astype(BF)
            return c
        lax.fori_loop(I0, I3 * half // SUB, qkv_step, I0)

        def head_step(j, c):
            at = [(pl.ds(s, seq), r * HEAD_PAD) for s in range(I0, BLOCK, seq) for r in range(I4)]
            base = j * (I4 * HEAD_PAD)

            def up_blocks(first):
                for n in range(I3):
                    cols = lanes((j * I6 + first + n) * SUB, SUB)
                    u[:, cols] = mm(n2[...], wubuf[:, cols]).astype(BF)
            views = [[qkv[rows, lanes(base + t * half + col, HEAD_PAD)] for t in range(I3)] for rows, col in at]
            between = [functools.partial(up_blocks, I0), functools.partial(up_blocks, I3)]
            for (rows, col), context in zip(at, attention_forward(views, scale, between)):
                ctx[rows, lanes(base + col, HEAD_PAD)] = context
            return c
        lax.fori_loop(I0, I2, head_step, I0)

    received = nothing if early else hand_on(place, refs[I0], outs[I6], outs[7], sems)

    @pl.when(place.home < I2 if early else place.home > I1)
    def _():
        pads = jnp.zeros((HEAD_PAD - head_dim, width), BF)
        for t in range(I3 * heads // I2):
            wqbuf[t * HEAD_PAD + head_dim:(t + I1) * HEAD_PAD, :] = pads
        for j in range(I3 * half // SUB):
            for copy in pieces(j):
                copy.start()
        count[I0] = I0
        low = pl.BlockSpec((BLOCK, width), lambda i: (jnp.minimum(i, steps // I2 - I1), I0))
        high = pl.BlockSpec((BLOCK, width), lambda i: (jnp.maximum(i - steps // I2, I0), I0))
        block = lambda n: pl.BlockSpec((BLOCK, n), lambda i: (i, I0))
        pltpu.emit_pipeline(body, grid=(steps,), in_specs=[low, high, low, high],
                            out_specs=[block(ffn // I2), block(I3 * half), block(half), block(width), block(width)])(
            h_same, h_other, a_same, a_other, u_o, qkv_o, ctx_o, n1_o, n2_o)
    received()


def owner_recompute(dims, early, again, h_rows, a_rows, gains, own):
    micro, seq, width, heads, head_dim, ffn = dims
    half = heads // I2 * HEAD_PAD
    tokens = I2 * micro * seq
    any_spec = pl.BlockSpec(memory_space=ANY)
    vmem = pltpu.VMEM
    earlier = () if early else tuple(again)
    act = (micro, seq, width)
    out_shape = [jax.ShapeDtypeStruct((I8, 128), F32), *shapes((tokens, ffn // I2), (tokens, I3 * half), (tokens, half), (tokens, width), (tokens, width))]
    if not early:
        out_shape += shapes((micro, I2, seq, width), act)
    aliases = {} if early else {I8 + i: I1 + i for i in range(5)} | {13: 7}
    comm = {} if early else dict(collective_id=I3)
    return pl.pallas_call(
        functools.partial(recompute_kernel, dims, early),
        out_shape=tuple(out_shape),
        in_specs=[any_spec] * I4 + [pl.BlockSpec(memory_space=vmem)] + [any_spec] * (I2 + len(earlier)),
        out_specs=(any_spec,) * len(out_shape),
        scratch_shapes=[vmem((I3 * half, width), BF), vmem((width, ffn // I2), BF), pltpu.SMEM((I1,), jnp.int32), pltpu.SemaphoreType.DMA((I3, ffn // I2 // SUB)), pltpu.SemaphoreType.DMA((I4,))],
        input_output_aliases=aliases,
        compiler_params=pltpu.CompilerParams(**comm, has_side_effects=True, vmem_limit_bytes=VMEM_LIMIT),
        name='owner_recompute',
    )(*h_rows, *a_rows, gains, own[I0], own[I2], *earlier)


def spread_dx(step, last, dx, d_in, og_other, bounce, here_sem, parent_sem, sib_sem, send_sems, og_sems, ready):
    place = Place()
    micro = dx.shape[I0]
    along_x = place.at(place.tp, (place.stage + I2) % I4)
    barrier = pltpu.get_barrier_semaphore()
    is_leaf = place.home > I1
    gives_g = (place.home == I1) & place.is_l
    takes_g = (place.home == I0) & jnp.logical_not(place.is_l)
    late = late_rows(micro)

    def block(m):
        return d_in.at[m, place.core]

    def to_sibling(m, src):
        remote(src, block(m), send_sems.at[I0], sib_sem, place.sibling).start()

    def tell(there):
        pl.semaphore_signal(barrier, inc=I1, device_id=there, device_id_type=MESH)

    @pl.when(step == I0)
    def _():
        tell(place.sibling)

        @pl.when(takes_g)
        def _():
            tell(place.across)

        @pl.when(is_leaf)
        def _():
            pl.semaphore_wait(barrier, I2)
            pl.semaphore_signal(ready, inc=I1, device_id=along_x, device_id_type=MESH)

        @pl.when(jnp.logical_not(is_leaf))
        def _():
            tell(along_x)
            pl.semaphore_wait(barrier, I1 + gives_g.astype(jnp.int32))

        @pl.when(gives_g)
        def _():
            for m in late:
                remote(og_other.at[m], og_other.at[m], og_sems.at[I0], og_sems.at[I1], place.across).start()

    @pl.when((step == I1) & jnp.logical_not(is_leaf))
    def _():
        pl.semaphore_wait(ready, I1)
        for m in reversed(range(micro)):
            if m < micro - EARLY_DX:
                remote(dx.at[m], block(m), send_sems.at[I1], parent_sem.at[m], along_x).start()
            to_sibling(m, dx.at[m])
        pltpu.make_async_copy(dx, bounce, here_sem).start()

    @pl.when((step == I2) & jnp.logical_not(is_leaf))
    def _():
        pltpu.make_async_copy(dx, bounce, here_sem).wait()
        for m in range(micro):
            pltpu.make_async_copy(bounce.at[m], block(m), here_sem).start()

    part = og_other.at[I0:len(late)]

    @pl.when((step == I3) & takes_g)
    def _():
        remote(part, part, og_sems.at[I0], og_sems.at[I1], place.across).wait_recv()

    @pl.when((step == last) & is_leaf)
    def _():
        for m in reversed(range(micro)):
            if m < micro - EARLY_DX:
                remote(block(m), block(m), send_sems.at[I0], parent_sem.at[m], place.sibling).wait_recv()
            to_sibling(m, block(m))

    @pl.when(step == last)
    def _():
        remote(dx, dx, send_sems.at[I0], sib_sem, place.sibling).wait_send()

        @pl.when(jnp.logical_not(is_leaf))
        def _():
            rest = dx.at[I0:micro - EARLY_DX]
            remote(rest, rest, send_sems.at[I1], sib_sem, place.sibling).wait_send()
            pltpu.make_async_copy(dx, dx, here_sem).wait()

        @pl.when(gives_g)
        def _():
            remote(part, part, og_sems.at[I0], og_sems.at[I1], place.across).wait_send()
        remote(dx, dx, send_sems.at[I0], sib_sem, place.sibling).wait_recv()


def owner_backward_kernel(dims, dx, ds, do, u, qkv, wo, wd, og_same, go_in, d_first, dqkv, dup, z, d_in, og_other,
                          dmid, gbuf, dctx, wobuf, bounce, sem, g_sem, here_sem, parent_sem, sib_sem, send_sems, og_sems, ready):
    micro, seq, width, heads, head_dim, ffn = dims
    half = heads // I2 * HEAD_PAD
    scale = head_dim ** -0.5
    step, steps = pl.program_id(I0), pl.num_programs(I0)
    spread_dx(step, steps - I1, dx, d_in, og_other, bounce, here_sem, parent_sem, sib_sem, send_sems, og_sems, ready)

    def g_load(n, start):
        rows = BLOCK // seq
        for og, low in ((og_same, I0), (og_other, steps // I2)):
            @pl.when((n >= low) & (n < low + steps // I2))
            def _(og=og, low=low):
                copy = pltpu.make_async_copy(og.at[pl.ds((n - low) * rows, rows)], gbuf.at[n % I2], g_sem.at[n % I2])
                copy.start() if start else copy.wait()

    @pl.when(step == I0)
    def _():
        g_load(step, True)
        wobuf[...] = jnp.zeros_like(wobuf)
        load_heads(wo, I0, wobuf, sem)
        pltpu.make_async_copy(wo, wobuf.at[I0:wo.shape[I0]], sem).wait()
    g_load(step + I1, True)

    @pl.when(step < steps // I2)
    def _():
        dmid[...] = ds[...]

    @pl.when(step >= steps // I2)
    def _():
        dmid[...] = do[...]

    def ctx_step(j, c):
        rows = pl.ds(pl.multiple_of(j * SUB, SUB), SUB)
        dctx[:, lanes(j * SUB, SUB)] = mm_nt(dmid[...], wobuf[rows, :]).astype(BF)
        return c
    lax.fori_loop(I0, half // SUB, ctx_step, I0)
    g_load(step, False)
    grad = gbuf.at[step % I2]

    def mlp_block(n):
        rows = pl.ds(pl.multiple_of(n * SUB, SUB), SUB)
        cols = lanes(n * SUB, SUB)
        dz = mm_nt(grad[...].reshape(BLOCK, width), wd[rows, :]).astype(BF).astype(F32)
        up = u[:, cols].astype(F32)
        gate, up2 = gelu_gate(up)
        hidden = up * gate
        z[:, cols] = hidden.astype(BF)
        dup[:, cols] = (dz * gelu_slope(hidden, gate, up2)).astype(BF)

    def both_step(j, c):
        base = j * (I2 * HEAD_PAD)
        at = [(pl.ds(s, seq), base + r * HEAD_PAD) for s in range(I0, BLOCK, seq) for r in range(I2)]
        group = [(*(qkv[rows, lanes(t * half + col, HEAD_PAD)] for t in range(I3)), dctx[rows, lanes(col, HEAD_PAD)]) for rows, col in at]
        blocks = [functools.partial(mlp_block, j * I3 + r) for r in range(I3)]
        for (rows, col), grads in zip(at, attention_backward(group, scale, blocks)):
            for t, value in enumerate(grads):
                dqkv[rows, lanes(t * half + col, HEAD_PAD)] = value
        return c
    lax.fori_loop(I0, heads // I4, both_step, I0)


def owner_backward(dims, dx, d_in, d_rows, og, ups, qkv, own):
    micro, seq, width, heads, head_dim, ffn = dims
    half = heads // I2 * HEAD_PAD
    tokens = I2 * micro * seq
    blocks = tokens // BLOCK
    vmem, dma = pltpu.VMEM, pltpu.SemaphoreType.DMA
    any_spec = pl.BlockSpec(memory_space=ANY)
    low = pl.BlockSpec((BLOCK, width), lambda i: (jnp.minimum(i, blocks // I2 - I1), I0))
    high = pl.BlockSpec((BLOCK, width), lambda i: (jnp.maximum(i - blocks // I2, I0), I0))
    attn_block = pl.BlockSpec((BLOCK, I3 * half), lambda i: (i, I0))
    mlp_block = pl.BlockSpec((BLOCK, ffn // I2), lambda i: (i, I0))
    act = (micro, seq, width)
    return pl.pallas_call(
        functools.partial(owner_backward_kernel, dims),
        grid=(blocks,),
        out_shape=tuple(shapes((tokens, I3 * half), (tokens, ffn // I2), (tokens, ffn // I2), (micro, I2, seq, width), act)),
        in_specs=[any_spec, low, high, mlp_block, attn_block, any_spec, pl.BlockSpec((ffn // I2, width), lambda i: (I0, I0)), any_spec, any_spec, any_spec],
        out_specs=(attn_block, mlp_block, mlp_block, any_spec, any_spec),
        scratch_shapes=[vmem((BLOCK, width), BF), vmem((I2, BLOCK // seq, seq, width), BF), vmem((BLOCK, half), BF), vmem((half, width), BF), vmem(act, BF),
                        dma(()), dma((I2,)), dma(()), dma((micro,)), dma(()), dma((I2,)), dma((I2,)), pltpu.SemaphoreType.REGULAR],
        input_output_aliases={I8: I4, 9: I3},
        compiler_params=pltpu.CompilerParams(collective_id=I2, has_side_effects=True, vmem_limit_bytes=VMEM_LIMIT),
        name='owner_backward',
    )(dx, *d_rows, ups, qkv, own[I1], own[I3], *og, d_in)


def bring(pairs, sem):
    copies = [pltpu.make_async_copy(src, dst, sem.at[i]) for i, (src, dst) in enumerate(pairs)]
    for copy in copies:
        copy.start()
    for copy in copies:
        copy.wait()


def attn_products_kernel(dq, dk, dv, ctx, n1_o, ds, do, dx_in, dwq, dwo, dx_out, n1, dmid, dqkvt, ctxt, bounce, sem, dx_sem):
    tokens, width = n1.shape
    part = tokens // I2
    head_dim = dwo.shape[I1]
    step, last = pl.program_id(I0), pl.num_programs(I0) - I1
    into, out_of = pltpu.make_async_copy(dx_in, bounce, dx_sem), pltpu.make_async_copy(bounce, dx_out, dx_sem)

    @pl.when(step == I1)
    def _():
        into.start()

    @pl.when(step == I2)
    def _():
        into.wait()
        out_of.start()

    @pl.when(step == last)
    def _():
        out_of.wait()

    @pl.when(step == I0)
    def _():
        bring([(n1_o, n1), (ds, dmid.at[pl.ds(I0, part)]), (do, dmid.at[pl.ds(part, part)])], sem)

    def turn(rows):
        for t, block in enumerate((dq, dk, dv)):
            for r in range(I2):
                at = (I2 * t + r) * head_dim
                dqkvt[at:at + head_dim, rows] = block[rows, r * HEAD_PAD:(r + I1) * HEAD_PAD].T[I0:head_dim]
        for r in range(I2):
            ctxt[r * head_dim:(r + I1) * head_dim, rows] = ctx[rows, r * HEAD_PAD:(r + I1) * HEAD_PAD].T[I0:head_dim]
    rows_loop(tokens, SUB, turn)
    for c in range(I0, width, SUB):
        cut = slice(c, c + SUB)
        dwq[:, :, :, cut] = mm(dqkvt[...], n1[:, cut]).reshape(I3, I2, head_dim, SUB)
        dwo[:, :, cut] = mm(ctxt[...], dmid[:, cut]).reshape(I2, head_dim, SUB)


def attn_products(dqkv, ctx, n1, d_rows, dx, out_dims):
    heads, head_dim, width = out_dims
    tokens = n1.shape[I0]
    vmem = pltpu.VMEM
    any_spec = pl.BlockSpec(memory_space=ANY)
    pairs = heads // I2
    cols = lambda t: pl.BlockSpec((tokens, I2 * HEAD_PAD), lambda i: (I0, t * pairs + i))
    return pl.pallas_call(
        attn_products_kernel,
        grid=(pairs,),
        out_shape=(jax.ShapeDtypeStruct((I3,) + out_dims, F32), jax.ShapeDtypeStruct(out_dims, F32), jax.ShapeDtypeStruct(dx.shape, BF)),
        in_specs=[cols(I0), cols(I1), cols(I2), cols(I0), any_spec, any_spec, any_spec, any_spec],
        out_specs=(pl.BlockSpec((I3, I2, head_dim, width), lambda i: (I0, i, I0, I0)), pl.BlockSpec((I2, head_dim, width), lambda i: (i, I0, I0)), any_spec),
        scratch_shapes=[vmem((tokens, width), BF), vmem((tokens, width), BF), vmem((I6 * head_dim, tokens), BF), vmem((I2 * head_dim, tokens), BF),
                        vmem(dx.shape, BF), pltpu.SemaphoreType.DMA((I3,)), pltpu.SemaphoreType.DMA(())],
        compiler_params=pltpu.CompilerParams(vmem_limit_bytes=VMEM_LIMIT),
        name='attn_products',
    )(dqkv, dqkv, dqkv, ctx, n1, *d_rows, dx)


def mlp_products_kernel(dup, z, n2_o, gs, go, dwu, dwd, n2t, grad, zt, stage, sem):
    width, tokens = n2t.shape
    part = tokens // I2

    @pl.when(pl.program_id(I0) == I0)
    def _():
        bring([(n2_o, stage), (gs, grad.at[pl.ds(I0, part)]), (go, grad.at[pl.ds(part, part)])], sem)

        def turn(rows):
            for c in range(I0, width, SUB):
                n2t[c:c + SUB, rows] = stage[rows, c:c + SUB].T
        rows_loop(tokens, SUB, turn)

    def turn_z(rows):
        for c in range(I0, z.shape[I1], SUB):
            zt[c:c + SUB, rows] = z[rows, c:c + SUB].T
    rows_loop(tokens, SUB, turn_z)
    for c in range(I0, width, I2 * SUB):
        dwu[c:c + I2 * SUB, :] = mm(n2t[c:c + I2 * SUB, :], dup[...])
    for c in range(I0, width, SUB):
        dwd[:, c:c + SUB] = mm(zt[...], grad[:, c:c + SUB])


def mlp_products(dup, hidden, n2, g_rows):
    tokens, width = n2.shape
    cols = dup.shape[I1]
    vmem = pltpu.VMEM
    any_spec = pl.BlockSpec(memory_space=ANY)
    block = pl.BlockSpec((tokens, SUB), lambda i: (I0, i))
    return pl.pallas_call(
        mlp_products_kernel,
        grid=(cols // SUB,),
        out_shape=(jax.ShapeDtypeStruct((width, cols), F32), jax.ShapeDtypeStruct((cols, width), F32)),
        in_specs=[block, block, any_spec, any_spec, any_spec],
        out_specs=(pl.BlockSpec((width, SUB), lambda i: (I0, i)), pl.BlockSpec((SUB, width), lambda i: (i, I0))),
        scratch_shapes=[vmem((width, tokens), BF), vmem((tokens, width), BF), vmem((SUB, tokens), BF), vmem((tokens, width), BF), pltpu.SemaphoreType.DMA((I3,))],
        compiler_params=pltpu.CompilerParams(vmem_limit_bytes=VMEM_LIMIT),
        name='mlp_products',
    )(dup, hidden, n2, *g_rows)


def solution(mesh):
    act_spec = P('rep', None, None, None)
    weight_specs = (
        P(('rep', 'stage'), None, None, 'tp', None),
        P(('rep', 'stage'), 'tp', None, None),
        P(('rep', 'stage'), None, 'tp'),
        P(('rep', 'stage'), 'tp', None),
        P(('rep', 'stage'), None),
        P(('rep', 'stage'), None),
    )

    def device_fn(inputs, targets, w_qkv, w_out, w_up, w_down, gain_attn, gain_mlp):
        micro_count, _, seq_len, width = inputs.shape
        dims = (micro_count, seq_len, width, I2 * w_out.shape[I1], w_out.shape[I2], I2 * w_up.shape[I2])
        norm_factor = 1.0 / (inputs.size)
        own = (w_qkv[I0], w_out[I0], w_up[I0], w_down[I0])
        own_gains = jnp.concatenate([gain_attn, gain_mlp]).astype(F32)
        rows_of = (own[I0].transpose(I1, I2, I3, I0).reshape(-I1, width), own[I1].reshape(-I1, width), own[I2], own[I3])

        (acts, mids, qkv, ups, seeds, oh_same, oh_other, oa_same, oa_other, og_same, og_other, loss_tile, home_gains, *weights) = forward_phase(dims, inputs, targets, rows_of, own_gains)
        (nq, no, nu, nd), (fq, fo, fu, fd) = weights[I0:I4], weights[I4:I8]
        (tq0, to0, tu0, td0), (tq1, to1, tu1, td1) = weights[I8:12], weights[12:16]

        flat = lambda *rows: [r.reshape(-I1, width) for r in rows]
        done, *again = owner_recompute(dims, True, None, flat(oh_same, oh_other), flat(oa_same, oa_other), own_gains, rows_of)
        dx, _, od_same, od_other, og_same, og_other, oa_same, oa_other, oh_same, oh_other, dg_same, dg_other, loss_all = backward_phase(
            dims, (acts, mids, qkv, ups, seeds), (rows_of[I0], nq, fq, td0, td1, to0, to1, tu0, tu1), home_gains, loss_tile, done,
            (og_same, og_other, oa_same, oa_other, oh_same, oh_other))
        _, *again, d_first, og_same = owner_recompute(dims, False, (dx, *again, og_same), flat(oh_same, oh_other), flat(oa_same, oa_other), own_gains, rows_of)
        ups_own, qkv_own, ctx_own, n1, n2 = again
        d_rows = flat(od_same, od_other)
        d_qkv_rows, d_up_rows, hidden, dx_all, og_other = owner_backward(dims, dx, d_first, d_rows, (og_same, og_other), ups_own, qkv_own, rows_of)
        d_qkv, d_out, d_inputs = attn_products(d_qkv_rows, ctx_own, n1, d_rows, dx_all, w_out.shape[I1:])
        d_up, d_down = mlp_products(d_up_rows, hidden, n2, flat(og_same, og_other))
        weight_grads = (d_qkv.transpose(I3, I0, I1, I2), d_out, d_up, d_down)
        mine = jnp.sum(dg_same + dg_other, I1)
        loss = jnp.sum(loss_all) * (0.5 * norm_factor)

        return (loss.reshape(I1), d_inputs) + tuple(g[None] for g in weight_grads) + (mine[I0][None], mine[I1][None])

    return jax.shard_map(device_fn, mesh=mesh, in_specs=(act_spec, act_spec) + weight_specs, out_specs=(P('rep'), act_spec) + weight_specs, check_vma=False)
```

```python
import functools

import jax
import jax.numpy as jnp
from jax import lax
from jax.experimental import pallas as pl
from jax.experimental.pallas import tpu as pltpu
from jax.sharding import PartitionSpec as P

NORM_EPS = 1e-5
BF = jnp.bfloat16
F32 = jnp.float32
MESH = pl.DeviceIdType.MESH
ANY = pl.ANY


GELU_A = 0.7978845608028654
GELU_B = 0.044715
I0, I1, I2, I3, I4, I6, I8 = 0, 1, 2, 3, 4, 6, 8
CHUNK = 1024
BLOCK = 384
SUB = 256
DEPTH = 6
BACK_DEPTH = 5
KDEPTH = 3
EARLY_G = 3
STAGGER_NS = 6000
EARLY_SEEDS = 5
EARLY_DX = 2
HEAD_PAD = 128
VMEM_LIMIT = 67043328


def mm(a, b):
    return lax.dot_general(a, b, (((I1,), (I0,)), ((), ())), preferred_element_type=F32)


def mm_nt(a, b):
    return lax.dot_general(a, b, (((I1,), (I1,)), ((), ())), preferred_element_type=F32)


def mm_tn(a, b):
    return lax.dot_general(a, b, (((I0,), (I0,)), ((), ())), preferred_element_type=F32)


class Place:
    def __init__(self):
        self.tp = lax.axis_index('tp')
        self.stage = lax.axis_index('stage')
        self.core = self.stage % I2
        self.x_pos = self.stage // I2
        self.home = self.x_pos * (I3 - I2 * self.tp) + self.tp
        self.is_l = self.stage == self.home
        self.sib = self.stage + I1 - I2 * self.core

    def at(self, tp, stage):
        return {'tp': tp, 'stage': stage}

    @property
    def sibling(self):
        return self.at(self.tp, self.sib)

    @property
    def along_x(self):
        return self.at(self.tp, (self.stage + I2) % I4)

    @property
    def across(self):
        return self.at(I1 - self.tp, self.stage)

    @property
    def across_other(self):
        return self.at(I1 - self.tp, self.sib)

    def chain(self, delta):
        there = self.home + delta
        x_pos = there // I2
        tp = there % I2 + x_pos * (I1 - I2 * (there % I2))
        return self.at(tp, I2 * x_pos + self.core)


def entry_barrier(place):
    barrier = pltpu.get_barrier_semaphore()
    for d_tp in (I0, I1):
        for d_stage in range(I4):
            if d_tp or d_stage:
                tp = place.tp + d_tp - I2 * d_tp * place.tp
                stage = (place.stage + d_stage) % I4
                pl.semaphore_signal(barrier, inc=I1, device_id=place.at(tp, stage), device_id_type=MESH)
    pl.semaphore_wait(barrier, 7)


def remote(src, dst, send_sem, recv_sem, device_id):
    return pltpu.make_async_remote_copy(src_ref=src, dst_ref=dst, send_sem=send_sem, recv_sem=recv_sem, device_id=device_id, device_id_type=MESH)


def rows_loop(total, step, body):
    def run(i, carry):
        body(pl.ds(pl.multiple_of(i * step, step), step))
        return carry
    lax.fori_loop(I0, total // step, run, I0)


def norm_rows(src, gain_row, dst, total):
    def body(rows):
        v = src[rows, :].astype(F32)
        inv = lax.rsqrt(jnp.mean(v * v, axis=-I1, keepdims=True) + NORM_EPS)
        dst[rows, :] = (v * inv * gain_row).astype(BF)
    rows_loop(total, 32, body)


def gelu_gate(u):
    u2 = u * u
    t = jnp.tanh(u * (GELU_A + (GELU_A * GELU_B) * u2))
    return 0.5 * t + 0.5, u2


def gelu_slope(hidden, gate, u2):
    return gate + hidden * (1.0 - gate) * (2.0 * GELU_A + (6.0 * GELU_A * GELU_B) * u2)


def row_parts(heads, cut=128):
    return [(*(x[low:high] for x in queries), *(x[:high] for x in keys), low)
            for queries, keys in heads for low, high in ((I0, cut), (cut, queries[I0].shape[I0]))]


def softmax_parts(scores, starts, keys_axis):
    masked = []
    for s, start in zip(scores, starts):
        k_pos = lax.broadcasted_iota(jnp.int32, s.shape, keys_axis)
        q_pos = lax.broadcasted_iota(jnp.int32, s.shape, I1 - keys_axis) + start
        masked.append(jnp.where(k_pos <= q_pos, s, -1e30))
    tops = [jnp.max(s, axis=keys_axis, keepdims=True) for s in masked]
    powers = [jnp.exp(s - top) for s, top in zip(masked, tops)]
    scales = [1.0 / jnp.sum(e, axis=keys_axis, keepdims=True) for e in powers]
    return [e * r for e, r in zip(powers, scales)]


def join_keys(top, low, cut=128):
    return jnp.concatenate([top + low[:cut], low[cut:]], I0).astype(BF)


def nothing():
    pass


def attention_forward(heads, scale, between=()):
    work = iter(between)
    units = row_parts([((q,), (k, v)) for q, k, v in heads])
    scores = [mm_nt(q, k) * scale for q, k, _, _ in units]
    next(work, nothing)()
    probs = softmax_parts(scores, [u[-I1] for u in units], I1)
    next(work, nothing)()
    parts = [mm(p.astype(BF), u[I2]) for p, u in zip(probs, units)]
    return [jnp.concatenate([a, b], I0).astype(BF) for a, b in zip(parts[I0::I2], parts[I1::I2])]


def attention_backward(heads, scale, between=()):
    work = iter(between)
    units = row_parts([((q, dc), (k, v)) for q, k, v, dc in heads])
    scores = [mm_nt(k, q) * scale for q, _, k, _, _ in units]
    dps = [mm_nt(v, dc) for _, dc, _, v, _ in units]
    next(work, nothing)()
    probs = softmax_parts(scores, [u[-I1] for u in units], I0)
    next(work, nothing)()
    dps = [dp.astype(BF).astype(F32) for dp in dps]
    deltas = [jnp.sum(dp * p, axis=I0, keepdims=True) for dp, p in zip(dps, probs)]
    dss = [p * (dp - delta) * scale for p, dp, delta in zip(probs, dps, deltas)]
    terms = []
    for ds in dss:
        hi = ds.astype(BF)
        rest = ds - hi.astype(F32)
        lo = rest.astype(BF)
        terms.append((hi, lo, (rest - lo.astype(F32)).astype(BF)))
    next(work, nothing)()
    dvs = [mm(p.astype(BF), u[I1]) for p, u in zip(probs, units)]
    dks = [mm(hi, u[I0]) + (mm(lo, u[I0]) + mm(tail, u[I0])) for (hi, lo, tail), u in zip(terms, units)]
    k_turned = [u[I2].T for u in units]
    dqs = [(mm(kt, hi) + (mm(kt, lo) + mm(kt, tail))).astype(BF) for (hi, lo, tail), kt in zip(terms, k_turned)]
    return [(jnp.concatenate([dqs[i].T, dqs[i + I1].T], I0), join_keys(dks[i], dks[i + I1]), join_keys(dvs[i], dvs[i + I1]))
            for i in range(I0, len(units), I2)]


def blocked(rows, stack, cols):
    total = mm(rows[:, I0:CHUNK], stack[I0, :, cols])
    for j in range(I1, stack.shape[I0]):
        total = total + mm(rows[:, j * CHUNK:(j + I1) * CHUNK], stack[j, :, cols])
    return total


def lanes(offset, size):
    return pl.ds(pl.multiple_of(offset, 128), size)


def load_resident(buf, sem, halves):
    for c in range(I6):
        for condition, ref in halves[c // I3]:
            copy = pltpu.make_async_copy(ref.at[(c % I3) * CHUNK:(c % I3 + I1) * CHUNK, :], buf.at[c], sem.at[c])
            if condition is None:
                copy.start()
            else:
                pl.when(condition)(copy.start)


def load_heads(ref, index, dst, sem):
    for r in range(I8):
        rows = pl.ds(pl.multiple_of(index * 768 + r * 96, 96), 96)
        pltpu.make_async_copy(ref.at[rows, :], dst.at[r * 128:r * 128 + 96, :], sem).start()


class Stream:
    def __init__(self, buf, sem, depth, parts, total, by_heads):
        self.buf, self.sem, self.depth, self.parts, self.total, self.by_heads = buf, sem, depth, parts, total, by_heads
        self.per_tick = sum(p[I1] for p in parts)

    def copy_in(self, ref, index, slot):
        if not self.by_heads:
            pltpu.make_async_copy(ref.at[index], self.buf.at[slot], self.sem.at[slot]).start()
            return
        load_heads(ref, index, self.buf.at[slot], self.sem.at[slot])

    def start(self, seq):
        @pl.when(seq < self.total)
        def _():
            j = seq % self.per_tick
            slot = seq % self.depth
            base = I0
            for choices, chunks in self.parts:
                for condition, ref in choices:
                    here = (j >= base) & (j < base + chunks)
                    here = here if condition is None else here & condition

                    @pl.when(here)
                    def _(ref=ref, low=base):
                        self.copy_in(ref, j - low, slot)
                base += chunks

    def prime(self):
        for seq in range(self.depth):
            self.start(jnp.int32(seq))

    def wait(self, seq):
        slot = seq % self.depth
        ref = self.parts[I0][I0][I0][I1]
        if self.by_heads:
            pltpu.make_async_copy(ref.at[I0:768, :], self.buf.at[slot, I0:768, :], self.sem.at[slot]).wait()
        else:
            pltpu.make_async_copy(ref.at[I0], self.buf.at[slot], self.sem.at[slot]).wait()
        return self.buf.at[slot]


PIECES = [(0, 0, 0), (0, 0, 1), (0, 0, 2), (1, 0, 0), (2, 1, 0), (2, 1, 1), (2, 1, 2), (2, 1, 3), (3, 0, 0), (3, 0, 1), (3, 0, 2), (3, 0, 3)]


ROUND = (11,)
ROUND_STEPS = (1,)
ORDER = (0, 1, 2, 3, 4, 5, 6, 7, 11, 8, 9, 10)


def piece(ref, axis, index):
    return ref.at[index * 768:(index + I1) * 768, :] if axis == I0 else ref.at[:, index * 768:(index + I1) * 768]


def weight_phase(place, is_r, own, near, far, turned, turned_own, up_chunks, wn, wk, send_sem, y_send, d_send, near_sem, far_sem, load_sem, store_sem, chunk_sem,
                 round_a, round_b, ra_sem, rb_sem, x_send, xd_send, rs_send):
    wk[...] = jnp.zeros_like(wk)
    early = place.home < I2

    def piece_of(arrays, c):
        i, axis, index = PIECES[c]
        return piece(arrays[i], axis, index)

    @pl.when(place.is_l)
    def _():
        for i in range(I4):
            remote(own[i], near[i], send_sem.at[i], near_sem.at[i], place.sibling).start()

    @pl.when(is_r)
    def _():
        for k, c in enumerate(ROUND):
            @pl.when(early)
            def _(k=k, c=c):
                remote(piece_of(own, c), round_a.at[k], x_send.at[k], ra_sem.at[k], place.along_x).start()
        for c, (i, axis, index) in enumerate(PIECES):
            if c not in ROUND:
                remote(piece_of(own, c), piece_of(far, c), y_send.at[i], far_sem.at[c], place.across_other).start()
        for k, c in enumerate(ROUND):
            @pl.when(jnp.logical_not(early))
            def _(k=k, c=c):
                remote(piece_of(own, c), piece_of(far, c), x_send.at[k], far_sem.at[c], place.across_other).start()

    def load(i, refs, t, slot):
        for condition, ref in refs:
            def go(ref=ref):
                if i < I2:
                    for r in range(I2):
                        rows = pl.ds(pl.multiple_of(t * 192 + r * 96, 96), 96)
                        pltpu.make_async_copy(ref.at[rows, :], wk.at[I0, pl.ds(slot * SUB + r * 128, 96), :], load_sem.at[slot]).start()
                elif i == I2:
                    pltpu.make_async_copy(ref.at[:, lanes(t * SUB, SUB)], wn.at[slot, :, I0:SUB], load_sem.at[slot]).start()
                else:
                    rows = pl.ds(pl.multiple_of(t * SUB, SUB), SUB)
                    pltpu.make_async_copy(ref.at[rows, :], wk.at[I0, pl.ds(512 + slot * SUB, SUB), :], load_sem.at[slot]).start()
            if condition is None:
                go()
            else:
                pl.when(condition)(go)

    def loaded(i, refs, slot):
        ref = refs[I0][I1]
        if i < I2:
            pltpu.make_async_copy(ref.at[I0:192, :], wk.at[I0, I0:192, :], load_sem.at[slot]).wait()
        elif i == I2:
            pltpu.make_async_copy(ref.at[:, I0:SUB], wn.at[slot, :, I0:SUB], load_sem.at[slot]).wait()
        else:
            pltpu.make_async_copy(ref.at[I0:SUB, :], wk.at[I0, 512:768, :], load_sem.at[slot]).wait()

    def store(i, dst, t, slot):
        if i == I2:
            rows = pl.ds(pl.multiple_of(t * SUB, SUB), SUB)
            return pltpu.make_async_copy(wk.at[I1, pl.ds(slot * SUB, SUB), :], dst.at[rows, :], store_sem.at[slot])
        return pltpu.make_async_copy(wn.at[slot, :, SUB:512], dst.at[t // I4, :, lanes(t % I4 * SUB, SUB)], store_sem.at[slot])

    def keep(which, t, slot):
        return pltpu.make_async_copy(wn.at[slot, :, I0:SUB], up_chunks[which].at[t // I4, :, lanes(t % I4 * SUB, SUB)], chunk_sem.at[slot])

    def turn(i, refs, which, first, count, dst=None):
        dst = turned[i][which] if dst is None else dst
        load(i, refs, first, I0)

        def step(n, c):
            slot = n % I2

            if i == I2:
                @pl.when(n > I0)
                def _():
                    keep(which, first + n - I1, I1 - slot).wait()

            @pl.when(n + I1 < count)
            def _():
                load(i, refs, first + n + I1, I1 - slot)
            loaded(i, refs, slot)
            if i == I2:
                keep(which, first + n, slot).start()

            @pl.when(n >= I2)
            def _():
                store(i, dst, first + n - I2, slot).wait()
            for b in range(I6):
                cut = slice(b * SUB, b * SUB + SUB)
                if i == I2:
                    wk[I1, pl.ds(pl.multiple_of(slot * SUB, SUB), SUB), cut] = wn[slot, cut, I0:SUB].T
                else:
                    base = I0 if i < I2 else 512
                    wn[slot, cut, SUB:512] = wk[I0, pl.ds(pl.multiple_of(base + slot * SUB, SUB), SUB), cut].T
            store(i, dst, first + n, slot).start()
            return c
        lax.fori_loop(I0, count, step, I0)
        for n in (count - I2, count - I1):
            store(i, dst, first + n, n % I2).wait()
        if i == I2:
            keep(which, first + count - I1, (count - I1) % I2).wait()

    counts = (12, I4, 12, 12)
    for i in range(I4):
        @pl.when(is_r)
        def _(i=i):
            remote(near[i], near[i], send_sem.at[i], near_sem.at[i], place.sibling).wait_recv()
        turn(i, [(place.is_l, own[i]), (is_r, near[i])], I0, I0, counts[i])
        if i < len(ROUND):
            @pl.when(place.is_l & jnp.logical_not(early))
            def _(k=i):
                remote(round_a.at[k], round_a.at[k], rs_send.at[k], ra_sem.at[k], place.sibling).wait_recv()
                remote(round_a.at[k], round_b.at[k], rs_send.at[k], rb_sem.at[k], place.across).start()

    @pl.when(is_r)
    def _():
        for i, dst in zip((I0, I3), turned_own):
            turn(i, [(None, own[i])], I0, I0, counts[i], dst)
    for c in ORDER:
        i, axis, index = PIECES[c]
        view = piece_of(far, c)
        for k, step in enumerate(ROUND_STEPS):
            if c == step:
                @pl.when(is_r & jnp.logical_not(early))
                def _(k=k):
                    remote(round_b.at[k], round_b.at[k], rs_send.at[k], rb_sem.at[k], place.sibling).wait_recv()
                    remote(round_b.at[k], piece_of(far, ROUND[k]), rs_send.at[k], far_sem.at[ROUND[k]], place.along_x).start()
        remote(view, view, d_send.at[i], far_sem.at[c], place.sibling).wait_recv()
        gives = is_r
        sem = d_send.at[i]
        if c in ROUND:
            gives = (early & place.is_l) | (jnp.logical_not(early) & is_r)
            sem = xd_send.at[ROUND.index(c)]

        @pl.when(gives)
        def _(c=c, view=view, sem=sem):
            remote(view, view, sem, far_sem.at[c], place.sibling).start()
        count = I4 if i < I2 else I3
        turn(i, [(None, far[i])], I1, index * count, count)

    @pl.when(place.is_l)
    def _():
        for i in range(I4):
            remote(own[i], near[i], send_sem.at[i], near_sem.at[i], place.sibling).wait_send()

    @pl.when(is_r)
    def _():
        for i in range(I4):
            part = own[i] if i < I3 else own[i].at[I0:(I4 - len(ROUND)) * 768, :]
            remote(part, part, y_send.at[i], far_sem.at[I0], place.across_other).wait_send()
            remote(part, part, d_send.at[i], far_sem.at[I0], place.sibling).wait_send()
        for k in range(len(ROUND)):
            remote(round_a.at[k], round_a.at[k], x_send.at[k], far_sem.at[I0], place.sibling).wait_send()

    @pl.when((early & place.is_l) | (jnp.logical_not(early) & is_r))
    def _():
        for k in range(len(ROUND)):
            remote(round_a.at[k], round_a.at[k], xd_send.at[k], far_sem.at[I0], place.sibling).wait_send()

    @pl.when(jnp.logical_not(early))
    def _():
        for k in range(len(ROUND)):
            remote(round_a.at[k], round_a.at[k], rs_send.at[k], far_sem.at[I0], place.sibling).wait_send()


def near_choices(place, own, near):
    return [(place.is_l, own), (jnp.logical_not(place.is_l), near)]


def forward_kernel(dims, x_ref, y_ref, wq, wo, wu, wd, own_gains,
                   a_s, h_s, qkv_s, u_s, g_s, oh_same, oh_other, oa_same, oa_other, og_same, og_other, loss_s, home_gains,
                   nq, no, nu, nd, fq, fo, fu, fd, tq0, to0, tu0, td0, tq1, to1, tu1, td1, uc0, uc1, tqo, tdo, round_a, round_b,
                   abuf, hbuf, obuf, nbuf, ybuf, sbuf, qkvbuf, ubuf, zbuf, ctxbuf, lossbuf, losstile, gains, wres, wores, wn,
                   send_sem, y_send, d_send, near_sem, far_sem, t_load, t_store, t_keep, ra_sem, rb_sem, x_send, xd_send, rs_send,
                   act_sem, hop_f, keep_sem, save_sem, stream_n, res_sem, out_sem, big_sem, y_sem, s_sem,
                   os_sem, oo_sem, as_sem, ao_sem, gs_sem, go_sem, bulk, gain_sem, tiny):
    micro, seq, width, heads, head_dim, ffn = dims
    place = Place()
    is_first, is_last = place.home == I0, place.home == I3
    home02 = (place.home == I0) | (place.home == I2)
    home13 = jnp.logical_not(home02)
    is_r = jnp.logical_not(place.is_l)
    takes_x = (place.home == I1) & is_r
    half = heads // I2 * HEAD_PAD
    scale = head_dim ** -0.5
    norm_factor = 1.0 / (micro * I2 * seq * width)
    own, near, far = (wq, wo, wu, wd), (nq, no, nu, nd), (fq, fo, fu, fd)
    turned = ((tq0, tq1), (to0, to1), (tu0, tu1), (td0, td1))
    entry_barrier(place)

    @pl.when(place.is_l)
    def _():
        pltpu.make_async_copy(own_gains, gains, gain_sem.at[I0]).start()
        remote(own_gains, gains, gain_sem.at[I1], gain_sem.at[I0], place.sibling).start()

    @pl.when(is_first)
    def _():
        for m in range(micro):
            pltpu.make_async_copy(x_ref.at[m, place.core], abuf.at[m], act_sem.at[m]).start()
    weight_phase(place, is_r, own, near, far, turned, (tqo, tdo), (uc0, uc1), wn, wores, send_sem, y_send, d_send, near_sem, far_sem, t_load, t_store, t_keep,
                 round_a, round_b, ra_sem, rb_sem, x_send, xd_send, rs_send)
    pltpu.make_async_copy(own_gains, gains, gain_sem.at[I0]).wait()
    pltpu.make_async_copy(gains, home_gains, gain_sem.at[I0]).start()

    @pl.when(place.is_l)
    def _():
        remote(own_gains, gains, gain_sem.at[I1], gain_sem.at[I0], place.sibling).wait_send()

    def near_of(i):
        return near_choices(place, own[i], near[i])

    def saved(dst, index):
        return pltpu.make_async_copy(hbuf, dst, save_sem.at[index])

    sn = Stream(wn, stream_n, DEPTH, [([(None, tq0)], I3), ([(None, tq1)], I3), ([(None, uc0)], I3), ([(None, uc1)], I3)], micro * 12, False)
    for c, choices in enumerate((near_of(I1), [(None, fo)])):
        for condition, ref in choices:
            def go(ref=ref, c=c):
                load_heads(ref, I0, wores.at[c], out_sem.at[c])
            go() if condition is None else pl.when(condition)(go)
    sn.prime()
    load_resident(wres, res_sem, (near_of(I3), [(None, fd)]))
    lossbuf[...] = jnp.zeros_like(lossbuf)

    def qkv_out(m):
        return pltpu.make_async_copy(qkvbuf, qkv_s.at[m], big_sem.at[I0])

    def up_out(m):
        return pltpu.make_async_copy(ubuf, u_s.at[m], big_sem.at[I1])

    def act_out(m):
        return pltpu.make_async_copy(abuf.at[m], a_s.at[m], save_sem.at[I2])

    def hop_block(m, n):
        cols = lanes(n * SUB, SUB)
        return remote(obuf.at[m % I2, :, cols], abuf.at[m, :, cols], hop_f.at[m % I2], act_sem.at[m], place.chain(I1))

    def hop_forward(m):
        return remote(obuf.at[m % I2], abuf.at[m], hop_f.at[m % I2], act_sem.at[m], place.chain(I1))

    def near_hand(src, dst_far, dst_own, sem, recv_sem):
        return (lambda: remote(src, dst_far, sem, recv_sem, place.sibling)), (lambda: pltpu.make_async_copy(src, dst_own, sem))

    def hand_out(m):
        return near_hand(obuf.at[m % I2], oa_other.at[m], oa_same.at[m], keep_sem.at[m % I2], ao_sem)

    def both_kinds(condition, copies, start):
        far_copy, own_copy = copies

        @pl.when(condition & place.is_l)
        def _():
            far_copy().start() if start else far_copy().wait_send()

        @pl.when(condition & is_r)
        def _():
            own_copy().start() if start else own_copy().wait()

    def x_out(m):
        return pltpu.make_async_copy(ybuf, oa_same.at[m], y_sem), pltpu.make_async_copy(sbuf, oa_other.at[m], s_sem)

    def seed_out(m):
        return pltpu.make_async_copy(sbuf, g_s.at[m], s_sem)

    def far_mid(m, condition):
        @pl.when(condition & place.is_l)
        def _():
            remote(h_s.at[m], oh_same.at[m], bulk.at[I2], os_sem, place.across).start()

        @pl.when(condition & is_r)
        def _():
            remote(h_s.at[m], oh_other.at[m], bulk.at[I2], oo_sem, place.across_other).start()

    def send_seed(m):
        seed_out(m).wait()

        @pl.when(place.is_l & (m < EARLY_SEEDS))
        def _():
            remote(g_s.at[m], og_same.at[m], bulk.at[I1], gs_sem, place.across).start()

        @pl.when(is_r & (m < EARLY_SEEDS))
        def _():
            remote(g_s.at[m], og_other.at[m], bulk.at[I1], go_sem, place.across_other).start()

    def forward_tick(m, carry):
        act, mid, out = abuf.at[m], hbuf, obuf.at[m % I2]
        pltpu.make_async_copy(x_ref.at[m, place.core], act, act_sem.at[m]).wait()
        act_out(m).start()

        @pl.when(place.is_l)
        def _():
            pltpu.make_async_copy(act, oa_same.at[m], as_sem).start()

        @pl.when(is_last)
        def _():
            pltpu.make_async_copy(y_ref.at[m, place.core], ybuf, y_sem).start()

        @pl.when(takes_x)
        def _():
            @pl.when(m > I0)
            def _():
                for copy in x_out(m):
                    copy.wait()
            for core, buf, sem in ((place.core, ybuf, y_sem), (I1 - place.core, sbuf, s_sem)):
                pltpu.make_async_copy(x_ref.at[m, core], buf, sem).start()
        norm_rows(act, gains[I0:I1, :], nbuf, seq)

        @pl.when(m > I0)
        def _():
            qkv_out(m).wait()

        def qkv_step(j, c):
            w = sn.wait(m * 12 + j)
            for n in range(I0, CHUNK, SUB):
                qkvbuf[:, lanes(j * CHUNK + n, SUB)] = mm(nbuf[...], w[:, n:n + SUB]).astype(BF)
            sn.start(m * 12 + j + DEPTH)
            return c
        lax.fori_loop(I0, I6, qkv_step, I0)
        qkv_out(m).start()
        act_out(m).wait()

        @pl.when(is_r)
        def _():
            remote(a_s.at[m], oa_other.at[m], bulk.at[I0], ao_sem, place.sibling).start()

        def head_step(i, c):
            base = i * (I3 * half)
            views = [[qkvbuf[:, lanes(base + t * half + r * HEAD_PAD, HEAD_PAD)] for t in range(I3)] for r in range(I8)]
            for r, context in enumerate(attention_forward(views, scale)):
                ctxbuf[:, lanes(i * half + r * HEAD_PAD, HEAD_PAD)] = context
            return c
        lax.fori_loop(I0, I2, head_step, I0)

        @pl.when(m == I0)
        def _():
            for c in range(I2):
                pltpu.make_async_copy(wo, wores.at[c, I0:768, :], out_sem.at[c]).wait()
        for n in range(I0, width, SUB):
            total = mm(ctxbuf[:, I0:half], wores[I0, :, n:n + SUB]) + mm(ctxbuf[:, half:I2 * half], wores[I1, :, n:n + SUB])
            mid[:, n:n + SUB] = (act[:, n:n + SUB].astype(F32) + total).astype(BF)
        saved(h_s.at[m], I0).start()

        @pl.when(place.is_l)
        def _():
            saved(oh_same.at[m], I1).start()
        norm_rows(mid, gains[I1:I2, :], nbuf, seq)

        @pl.when(m > I0)
        def _():
            up_out(m).wait()

        def up_step(j, c):
            w = sn.wait(m * 12 + I6 + j)
            for n in range(I0, CHUNK, SUB):
                u = mm(nbuf[...], w[:, n:n + SUB]).astype(BF)
                at = lanes(j * CHUNK + n, SUB)
                ubuf[:, at] = u
                uf = u.astype(F32)
                zbuf[:, at] = (uf * gelu_gate(uf)[I0]).astype(BF)
            sn.start(m * 12 + I6 + j + DEPTH)
            return c
        lax.fori_loop(I0, I6, up_step, I0)
        up_out(m).start()

        @pl.when((m > I1) & jnp.logical_not(is_last))
        def _():
            hop_forward(m).wait_send()

        both_kinds((m > I1) & home02, hand_out(m), False)

        @pl.when(m == I0)
        def _():
            for j in range(I6):
                pltpu.make_async_copy(wd.at[I0:CHUNK, :], wres.at[j], res_sem.at[j]).wait()

        def down_step(n, c):
            cols = lanes(n * SUB, SUB)
            out[:, cols] = (mid[:, cols].astype(F32) + blocked(zbuf, wres, cols)).astype(BF)

            @pl.when((n > I0) & jnp.logical_not(is_last))
            def _():
                hop_block(m, n - I1).start()
            return c
        lax.fori_loop(I0, width // SUB, down_step, I0)

        @pl.when(jnp.logical_not(is_last))
        def _():
            hop_block(m, width // SUB - I1).start()

        both_kinds(home02, hand_out(m), True)

        @pl.when(is_last)
        def _():
            pltpu.make_async_copy(y_ref.at[m, place.core], ybuf, y_sem).wait()

            @pl.when(m > I0)
            def _():
                send_seed(m - I1)

            def seed(rows):
                error = out[rows, :].astype(F32) - ybuf[rows, :].astype(F32)
                sbuf[rows, :] = (error * norm_factor).astype(BF)
                lossbuf[...] += jnp.sum((error * error).reshape(I4, I8, width), axis=I0)
            rows_loop(seq, 32, seed)
            seed_out(m).start()

        @pl.when(takes_x)
        def _():
            for core, buf, sem in ((place.core, ybuf, y_sem), (I1 - place.core, sbuf, s_sem)):
                pltpu.make_async_copy(x_ref.at[m, core], buf, sem).wait()
            for copy in x_out(m):
                copy.start()

        saved(h_s.at[m], I0).wait()

        @pl.when(place.is_l)
        def _():
            saved(oh_same.at[m], I1).wait()

        @pl.when(is_r)
        def _():
            remote(h_s.at[m], oh_other.at[m], bulk.at[I3], oo_sem, place.sibling).start()

        far_mid(m, home13 | (m % I2 == I1))
        return carry

    @pl.when(is_first & (place.core == I0))
    def _():
        pl.delay(STAGGER_NS)
    lax.fori_loop(I0, micro, forward_tick, I0)
    for m in range(I0, micro, I2):
        far_mid(m, is_first)

    @pl.when(is_last)
    def _():
        total = lossbuf[:, I0:128]
        for n in range(128, width, 128):
            total = total + lossbuf[:, n:n + 128]
        losstile[...] = total
        pltpu.make_async_copy(losstile, loss_s, tiny).start()
    for copy in (qkv_out(micro - I1), up_out(micro - I1)):
        copy.wait()

    @pl.when(jnp.logical_not(is_last))
    def _():
        for m in (micro - I2, micro - I1):
            hop_forward(m).wait_send()
    for m in (micro - I2, micro - I1):
        both_kinds(home02, hand_out(m), False)

    @pl.when(is_last)
    def _():
        seed_out(micro - I1).wait()
        pltpu.make_async_copy(losstile, loss_s, tiny).wait()

    @pl.when(takes_x)
    def _():
        for copy in x_out(micro - I1):
            copy.wait()
    pltpu.make_async_copy(gains, home_gains, gain_sem.at[I0]).wait()
    sent, got = drain(place)

    @pl.when(place.home != I2)
    def _():
        sent(h_s, bulk.at[I2])

    @pl.when(place.home == I2)
    def _():
        sent(h_s.at[I0:micro // I2], bulk.at[I2])

    @pl.when(place.is_l | jnp.logical_not(is_last))
    def _():
        got(oh_other, oo_sem)

    @pl.when(is_r & is_last)
    def _():
        got(oh_other.at[I0:micro // I2], oo_sem)

    @pl.when(is_last)
    def _():
        sent(g_s.at[I0:EARLY_SEEDS], bulk.at[I1])

    @pl.when((place.home == I2) & is_r)
    def _():
        got(og_same.at[I0:EARLY_SEEDS], gs_sem)
        got(og_other.at[I0:EARLY_SEEDS], go_sem)

    @pl.when(is_r)
    def _():
        sent(a_s, bulk.at[I0])
        sent(h_s, bulk.at[I3])

    @pl.when(is_r & jnp.logical_not(is_last))
    def _():
        got(oh_same, os_sem)

    @pl.when(is_r & is_last)
    def _():
        got(oh_same.at[I0:micro // I2], os_sem)

    @pl.when(place.is_l)
    def _():
        got(oa_same, as_sem)

    @pl.when(place.is_l | home02)
    def _():
        got(oa_other, ao_sem)


def drain(place):
    def sent(buf, sem):
        remote(buf, buf, sem, sem, place.sibling).wait_send()

    def got(dst, sem):
        pltpu.make_async_copy(dst, dst, sem).wait()
    return sent, got


def backward_kernel(dims, a_s, h_s, qkv_s, u_s, g_s, wq, nq, fq, td0, td1, to0, to1, tu0, tu1, gains, loss_s, after, *refs):
    (dx_s, m_s, od_same, od_other, og_same, og_other, oa_same, oa_other, oh_same, oh_other, dg_same, dg_other, loss_all,
     gbuf, hbuf, obuf, qkvbuf, ubuf, habuf, zbuf, ctxbuf, dqkvbuf, acc, accg, wres, wn, wk,
     grad_sem, hop_b, back_sem, dx_sem, dx_send, save_sem, stream_n, stream_k, res_sem, load_sem,
     ds_sem, do_sem, gs_sem, go_sem, as_sem, ao_sem, os_sem, oo_sem, bulk, tiny, loss_sem, ready) = refs[I6:]
    micro, seq, width, heads, head_dim, ffn = dims
    place = Place()
    is_first, is_last = place.home == I0, place.home == I3
    home13 = (place.home == I1) | is_last
    is_r = jnp.logical_not(place.is_l)
    half = heads // I2 * HEAD_PAD
    scale = head_dim ** -0.5

    barrier = pltpu.get_barrier_semaphore()
    is_b, is_c = place.home == I1, place.home == I2
    pl.semaphore_signal(barrier, inc=I1, device_id=place.sibling, device_id_type=MESH)

    @pl.when(jnp.logical_not(is_first))
    def _():
        for there in (place.across, place.across_other):
            pl.semaphore_signal(barrier, inc=I1, device_id=there, device_id_type=MESH)

    @pl.when(is_c)
    def _():
        pl.semaphore_signal(barrier, inc=I1, device_id=place.along_x, device_id_type=MESH)

    @pl.when(is_last)
    def _():
        for m in range(micro):
            pltpu.make_async_copy(g_s.at[m], gbuf.at[m], grad_sem.at[m]).start()
    wk[...] = jnp.zeros_like(wk)
    bn = Stream(wn, stream_n, BACK_DEPTH, [([(None, td0)], I3), ([(None, td1)], I3), ([(None, to0)], I1), ([(None, to1)], I1)], micro * I8, False)
    bk = Stream(wk, stream_k, KDEPTH, [(near_choices(place, wq, nq), I3), ([(None, fq)], I3)], micro * I6, True)
    bn.prime()
    bk.prime()
    load_resident(wres, res_sem, ([(None, tu0)], [(None, tu1)]))

    def saved(dst, index):
        return pltpu.make_async_copy(hbuf, dst, save_sem)

    def both_kinds(condition, copies, start):
        far_copy, own_copy = copies

        @pl.when(condition & place.is_l)
        def _():
            far_copy().start() if start else far_copy().wait_send()

        @pl.when(condition & is_r)
        def _():
            own_copy().start() if start else own_copy().wait()

    def near_hand(src, dst_far, dst_own, sem, recv_sem):
        return (lambda: remote(src, dst_far, sem, recv_sem, place.sibling)), (lambda: pltpu.make_async_copy(src, dst_own, sem))

    def loads(i):
        m = micro - I1 - i
        return [pltpu.make_async_copy(src.at[m], dst, load_sem.at[k])
                for k, (src, dst) in enumerate(((u_s, ubuf), (qkv_s, qkvbuf), (h_s, habuf.at[I0]), (a_s, habuf.at[I1])))]

    def load_next(i, k):
        @pl.when(i + I1 < micro)
        def _():
            loads(i + I1)[k].start()

    for copy in loads(I0):
        copy.start()
    accg[...] = jnp.zeros_like(accg)

    def norm_back(index, x, base, dst, gain_row):
        def body(rows):
            xf = x[rows, :].astype(F32)
            dy = acc[rows, :].astype(BF).astype(F32)
            inv = lax.rsqrt(jnp.mean(xf * xf, axis=-I1, keepdims=True) + NORM_EPS)
            xn = xf * inv
            accg[index] += jnp.sum((dy * xn).reshape(I4, I8, width), axis=I0)
            dyg = dy * gain_row
            dx = inv * (dyg - xn * jnp.mean(dyg * xn, axis=-I1, keepdims=True))
            dst[rows, :] = (base[rows, :].astype(F32) + dx).astype(BF)
        rows_loop(seq, 32, body)

    def hop_back(i):
        m = micro - I1 - i
        return remote(obuf.at[i % I2], gbuf.at[m], hop_b.at[i % I2], grad_sem.at[m], place.chain(-I1))

    def hand_back(i):
        m = micro - I1 - i
        return near_hand(obuf.at[i % I2], og_other.at[m], og_same.at[m], back_sem.at[i % I2], go_sem)

    def keep_dx(i):
        return pltpu.make_async_copy(obuf.at[i % I2], dx_s.at[micro - I1 - i], back_sem.at[i % I2])

    def back_ready(i):
        both_kinds((i > I1) & home13, hand_back(i), False)

        @pl.when((i > I1) & is_first)
        def _():
            keep_dx(i).wait()
            dx_to_b(i).wait_send()

        @pl.when((i > I1) & jnp.logical_not(is_first))
        def _():
            hop_back(i).wait_send()

    def pass_loss(tile):
        @pl.when(jnp.logical_not(is_first))
        def _():
            remote(tile, loss_all.at[place.core], loss_sem.at[I0], loss_sem.at[I1], place.chain(-I1)).start()
        remote(tile, loss_all.at[place.core], loss_sem.at[I2], loss_sem.at[I3], place.sibling).start()

    def dx_to_b(i):
        return remote(obuf.at[i % I2], dx_s.at[micro - I1 - i], dx_send.at[i % I2], dx_sem, place.across)

    def backward_tick(i, carry):
        m = micro - I1 - i
        slot = i % I2
        grad, dmid, prev = gbuf.at[m], hbuf, obuf.at[slot]
        u_now, qkv_now, h_now, a_now = ubuf, qkvbuf, habuf.at[I0], habuf.at[I1]

        pltpu.make_async_copy(g_s.at[m], grad, grad_sem.at[m]).wait()

        @pl.when(place.is_l)
        def _():
            pltpu.make_async_copy(grad, og_same.at[m], gs_sem).start()
        load_u, load_qkv, load_h, load_a = loads(i)
        load_u.wait()

        def mlp_step(j, c):
            w = bn.wait(i * I8 + j)
            for n in range(I0, CHUNK, SUB):
                at = lanes(j * CHUNK + n, SUB)
                dz = mm(grad[...], w[:, n:n + SUB]).astype(BF).astype(F32)
                u = u_now[:, at].astype(F32)
                gate, u2 = gelu_gate(u)
                zbuf[:, at] = (dz * gelu_slope(u * gate, gate, u2)).astype(BF)
            bn.start(i * I8 + j + BACK_DEPTH)
            return c
        lax.fori_loop(I0, I6, mlp_step, I0)

        @pl.when(i == I0)
        def _():
            for j in range(I6):
                pltpu.make_async_copy(tu0.at[I0:CHUNK, :], wres.at[j], res_sem.at[j]).wait()

        def turn_back(n, c):
            cols = lanes(n * SUB, SUB)
            acc[:, cols] = blocked(zbuf, wres, cols)
            return c
        lax.fori_loop(I0, width // SUB, turn_back, I0)
        load_next(i, I0)
        load_h.wait()
        norm_back(I1, h_now, grad, dmid, gains[I1:I2, :])
        load_next(i, I2)

        @pl.when(place.is_l)
        def _():
            saved(od_same.at[m], I0).start()

        @pl.when(is_r)
        def _():
            saved(m_s.at[m], I0).start()
        for c in range(I2):
            w = bn.wait(i * I8 + I6 + c)
            for n in range(I0, CHUNK, SUB):
                ctxbuf[:, c * CHUNK + n:c * CHUNK + n + SUB] = mm(dmid[...], w[:, n:n + SUB]).astype(BF)
            bn.start(i * I8 + I6 + c + BACK_DEPTH)
        load_qkv.wait()

        def head_step(t, c):
            base = (t // I2) * (I3 * half) + (t % I2) * (I4 * HEAD_PAD)
            at = [[lanes(base + part * half + r * HEAD_PAD, HEAD_PAD) for part in range(I3)] for r in range(I4)]
            group = [(*(qkv_now[:, p] for p in at[r]), ctxbuf[:, lanes((t * I4 + r) * HEAD_PAD, HEAD_PAD)]) for r in range(I4)]
            for r, grads in enumerate(attention_backward(group, scale)):
                for p, value in zip(at[r], grads):
                    dqkvbuf[:, p] = value
            return c
        lax.fori_loop(I0, I2, lambda t, c: head_step(I2 * t + I1, head_step(I2 * t, c)), I0)
        load_next(i, I1)
        acc[...] = jnp.zeros_like(acc)

        def qkv_step(j, c):
            w = bk.wait(i * I6 + j)
            for n in range(I0, width, SUB):
                acc[:, n:n + SUB] += mm(dqkvbuf[:, lanes(j * CHUNK, CHUNK)], w[:, n:n + SUB])
            bk.start(i * I6 + j + KDEPTH)
            return c
        lax.fori_loop(I0, I6, qkv_step, I0)
        load_a.wait()
        back_ready(i)
        norm_back(I0, a_now, dmid, prev, gains[I0:I1, :])
        load_next(i, I3)

        @pl.when(i == I0)
        def _():
            @pl.when(is_last)
            def _():
                pl.semaphore_wait(barrier, I3)

            @pl.when(is_c)
            def _():
                pl.semaphore_wait(ready, I1)

            @pl.when(is_b)
            def _():
                pl.semaphore_wait(ready, I2)

            @pl.when(is_last)
            def _():
                pass_loss(loss_s)

        @pl.when(jnp.logical_not(is_first))
        def _():
            hop_back(i).start()

        @pl.when(is_first)
        def _():
            keep_dx(i).start()
            dx_to_b(i).start()
        both_kinds(home13, hand_back(i), True)

        @pl.when(place.is_l)
        def _():
            saved(od_same.at[m], I0).wait()
            remote(od_same.at[m], od_same.at[m], bulk.at[I6], ds_sem, place.across).start()

        @pl.when(is_r)
        def _():
            remote(grad, og_other.at[m], bulk.at[5], go_sem, place.sibling).start()
            saved(m_s.at[m], I0).wait()
            remote(m_s.at[m], od_other.at[m], bulk.at[I6], do_sem, place.sibling).start()
            remote(m_s.at[m], od_other.at[m], bulk.at[7], do_sem, place.across_other).start()

        now = (i % I2 == I1) & (i < I2 * EARLY_G)
        far_grad(m, (place.home == I1) & now)
        far_grad(micro - I1 - i // I2, is_last & now)
        return carry

    def far_grad(m, condition):
        @pl.when(condition & place.is_l)
        def _():
            remote(gbuf.at[m], og_same.at[m], bulk.at[I4], gs_sem, place.across).start()

        @pl.when(condition & is_r)
        def _():
            remote(gbuf.at[m], og_other.at[m], bulk.at[I4], go_sem, place.across_other).start()

    @pl.when(jnp.logical_not(is_last))
    def _():
        pl.semaphore_wait(barrier, I3 - is_b.astype(jnp.int32))

    @pl.when(is_first)
    def _():
        for there in (place.across, place.across_other):
            pl.semaphore_signal(ready, inc=I1, device_id=there, device_id_type=MESH)

    @pl.when(is_b)
    def _():
        pl.semaphore_signal(ready, inc=I1, device_id=place.along_x, device_id_type=MESH)

    @pl.when(is_c & place.is_l)
    def _():
        for t in range(micro):
            remote(a_s.at[t], oa_same.at[t], bulk.at[I8], as_sem, place.across).start()
        for t in range(I0, micro, I2):
            remote(h_s.at[t], oh_same.at[t], bulk.at[9], os_sem, place.across).start()

    @pl.when(is_c & is_r)
    def _():
        for t in range(micro):
            remote(a_s.at[t], oa_other.at[t], bulk.at[I8], ao_sem, place.across_other).start()
        for t in range(I0, micro, I2):
            remote(h_s.at[t], oh_other.at[t], bulk.at[9], oo_sem, place.across_other).start()
    lax.fori_loop(I0, micro, backward_tick, I0)
    loss_mine = loss_all.at[place.core]

    @pl.when(is_last)
    def _():
        own_loss = pltpu.make_async_copy(loss_s, loss_mine, loss_sem.at[I1])
        own_loss.start()
        own_loss.wait()

    @pl.when(jnp.logical_not(is_last))
    def _():
        remote(loss_mine, loss_mine, loss_sem.at[I0], loss_sem.at[I1], place.sibling).wait_recv()
        pass_loss(loss_mine)

    @pl.when(place.is_l)
    def _():
        pltpu.make_async_copy(accg, dg_same, tiny.at[I0]).start()
        remote(accg, dg_same, tiny.at[I1], tiny.at[I0], place.across).start()

    @pl.when(is_r)
    def _():
        remote(accg, dg_other, tiny.at[I1], tiny.at[I4], place.sibling).start()
        remote(accg, dg_other, tiny.at[I2], tiny.at[I4], place.across_other).start()

    for i in (micro - I2, micro - I1):
        back_ready(jnp.int32(i))

    sent, got = drain(place)
    sent(m_s, bulk.at[I6])

    @pl.when(is_r)
    def _():
        sent(gbuf, bulk.at[5])
        sent(m_s, bulk.at[7])
        remote(accg, dg_other, tiny.at[I2], tiny.at[I4], place.sibling).wait_send()

    @pl.when(home13)
    def _():
        sent(gbuf.at[I0:EARLY_G], bulk.at[I4])

    @pl.when(place.home == I1)
    def _():
        got(dx_s, dx_sem)

    @pl.when(jnp.logical_not(is_first))
    def _():
        remote(loss_mine, loss_mine, loss_sem.at[I0], loss_sem.at[I1], place.sibling).wait_send()
    remote(loss_mine, loss_mine, loss_sem.at[I2], loss_sem.at[I3], place.sibling).wait_send()
    remote(loss_mine, loss_mine, loss_sem.at[I2], loss_sem.at[I3], place.sibling).wait_recv()

    @pl.when(place.home == I2)
    def _():
        sent(a_s, bulk.at[I8])
        sent(h_s.at[I0:micro // I2], bulk.at[9])

    remote(accg, dg_other, tiny.at[I1], tiny.at[I4], place.sibling).wait_send()
    got(od_other, do_sem)

    @pl.when(place.is_l | home13)
    def _():
        got(og_other, go_sem)

    @pl.when(jnp.logical_not(home13) & is_r)
    def _():
        got(og_same.at[I0:EARLY_G], gs_sem)
        got(og_other.at[I0:EARLY_G], go_sem)
    got(dg_same, tiny.at[I0])
    got(dg_other, tiny.at[I4])

    @pl.when(is_r)
    def _():
        got(od_same, ds_sem)

    @pl.when(place.is_l)
    def _():
        got(og_same, gs_sem)

    @pl.when(is_last & is_r)
    def _():
        got(oa_same, as_sem)
        got(oa_other, ao_sem)
        got(oh_same.at[I0:micro // I2], os_sem)
        got(oh_other.at[I0:micro // I2], oo_sem)


def shapes(*dims_list):
    return [jax.ShapeDtypeStruct(d, BF) for d in dims_list]


def forward_phase(dims, x, y, own, own_gains):
    micro, seq, width, heads, head_dim, ffn = dims
    half = heads // I2 * HEAD_PAD
    act = (micro, seq, width)
    raw = [w.shape for w in own]
    turned = [(I3, width, CHUNK), (I1, width, CHUNK), (ffn // I2, width), (I3, width, CHUNK)]
    out_shape = shapes(act, act, (micro, seq, I6 * half), (micro, seq, ffn), *[act] * 7)
    out_shape += [jax.ShapeDtypeStruct(s, F32) for s in ((I8, 128), own_gains.shape)]
    out_shape += shapes(*raw, *raw, *turned, *turned, *[turned[I0]] * I4, *[(len(ROUND), 768, width)] * I2)
    any_spec = pl.BlockSpec(memory_space=ANY)
    vmem, dma = pltpu.VMEM, pltpu.SemaphoreType.DMA
    row = vmem((seq, width), BF)
    scratch = [
        vmem(act, BF), row, vmem((I2, seq, width), BF), row, row, row, vmem((seq, I6 * half), BF), vmem((seq, ffn), BF), vmem((seq, ffn), BF),
        vmem((seq, I2 * half), BF), vmem((I8, width), F32), vmem((I8, 128), F32), vmem((I2, width), F32),
        vmem((I6, CHUNK, width), BF), vmem((I2, CHUNK, width), BF), vmem((DEPTH, width, CHUNK), BF),
        dma((I4,)), dma((I4,)), dma((I4,)), dma((I4,)), dma((12,)), dma((I2,)), dma((I2,)), dma((I2,)), *[dma((len(ROUND),))] * 5,
        dma((micro,)), dma((I2,)), dma((I2,)), dma((I3,)), dma((DEPTH,)), dma((I6,)), dma((I2,)), dma((I2,)), dma(()), dma(()),
        dma(()), dma(()), dma(()), dma(()), dma(()), dma(()), dma((I4,)), dma((I2,)), dma(()),
    ]
    return pl.pallas_call(
        functools.partial(forward_kernel, dims),
        out_shape=tuple(out_shape),
        in_specs=[any_spec] * I6 + [pl.BlockSpec(memory_space=vmem)],
        out_specs=(any_spec,) * len(out_shape),
        scratch_shapes=scratch,
        compiler_params=pltpu.CompilerParams(collective_id=I0, has_side_effects=True, vmem_limit_bytes=VMEM_LIMIT),
        name='forward_phase',
    )(x, y, *own, own_gains)


def backward_phase(dims, saved, weights, gains, loss, after, placed):
    micro, seq, width, heads, head_dim, ffn = dims
    half = heads // I2 * HEAD_PAD
    act = (micro, seq, width)
    out_shape = shapes(*[act] * 10) + [jax.ShapeDtypeStruct((I2, I8, width), F32)] * I2 + [jax.ShapeDtypeStruct((I2, I8, 128), F32)]
    any_spec = pl.BlockSpec(memory_space=ANY)
    vmem, dma = pltpu.VMEM, pltpu.SemaphoreType.DMA
    scratch = [
        vmem(act, BF), vmem((seq, width), BF), vmem((I2, seq, width), BF), vmem((seq, I6 * half), BF), vmem((seq, ffn), BF),
        vmem((I2, seq, width), BF), vmem((seq, ffn), BF), vmem((seq, I2 * half), BF), vmem((seq, I6 * half), BF), vmem((seq, width), F32),
        vmem((I2, I8, width), F32), vmem((I6, CHUNK, width), BF), vmem((BACK_DEPTH, width, CHUNK), BF), vmem((KDEPTH, CHUNK, width), BF),
        dma((micro,)), dma((I2,)), dma((I2,)), dma(()), dma((I2,)), dma(()), dma((BACK_DEPTH,)), dma((KDEPTH,)), dma((I6,)), dma((I4,)),
        *[dma(())] * I8, dma((10,)), dma((5,)), dma((I4,)), pltpu.SemaphoreType.REGULAR,
    ]
    return pl.pallas_call(
        functools.partial(backward_kernel, dims),
        out_shape=tuple(out_shape),
        in_specs=[any_spec] * 14 + [pl.BlockSpec(memory_space=vmem)] * I2 + [any_spec] * 7,
        out_specs=(any_spec,) * len(out_shape),
        scratch_shapes=scratch,
        input_output_aliases={17 + i: I4 + i for i in range(I6)},
        compiler_params=pltpu.CompilerParams(collective_id=I1, has_side_effects=True, vmem_limit_bytes=VMEM_LIMIT),
        name='backward_phase',
    )(*saved, *weights, gains, loss, after, *placed)


def late_rows(micro):
    return [micro - I1 - i for i in range(micro) if i % I2 == I0 or i > I2 * EARLY_G]


def hand_on(place, dx, d_in, og, sems):
    micro = dx.shape[I0]
    barrier = pltpu.get_barrier_semaphore()
    late = [m for m in late_rows(micro) if m < I4]
    is_leaf = place.home > I1
    gives_g = (place.home == I1) & place.is_l
    takes_g = (place.home == I0) & jnp.logical_not(place.is_l)
    part, g_part = dx.at[I0:EARLY_DX], og.at[I0:len(late)]

    @pl.when(is_leaf)
    def _():
        pl.semaphore_signal(barrier, inc=I1, device_id=place.along_x, device_id_type=MESH)

    @pl.when(takes_g)
    def _():
        pl.semaphore_signal(barrier, inc=I1, device_id=place.across, device_id_type=MESH)

    @pl.when(jnp.logical_not(is_leaf))
    def _():
        pl.semaphore_wait(barrier, I1 + gives_g.astype(jnp.int32))

        @pl.when(gives_g)
        def _():
            for m in late:
                remote(og.at[m], og.at[m], sems.at[I2], sems.at[I3], place.across).start()
        for m in range(micro - EARLY_DX, micro):
            remote(dx.at[m], d_in.at[m, place.core], sems.at[I0], sems.at[I1], place.along_x).start()
        remote(part, part, sems.at[I0], sems.at[I1], place.along_x).wait_send()

        @pl.when(gives_g)
        def _():
            remote(g_part, g_part, sems.at[I2], sems.at[I3], place.across).wait_send()

    def received():
        @pl.when(is_leaf)
        def _():
            remote(part, part, sems.at[I0], sems.at[I1], place.along_x).wait_recv()

        @pl.when(takes_g)
        def _():
            remote(g_part, g_part, sems.at[I2], sems.at[I3], place.across).wait_recv()
    return received


def recompute_kernel(dims, early, h_same, h_other, a_same, a_other, gains, wq_near, wq_own, wu, *refs):
    (wqbuf, wubuf, count, sem, sems) = refs[-5:]
    outs = refs[:-5] if early else refs[7:-5]
    (done, u_o, qkv_o, ctx_o, n1_o, n2_o) = outs[I0:I6]
    micro, seq, width, heads, head_dim, ffn = dims
    place = Place()
    scale = head_dim ** -0.5
    half = heads // I2 * HEAD_PAD
    steps = I2 * micro * seq // BLOCK

    def pieces(j):
        cols = lanes(j * CHUNK, CHUNK)
        up = pltpu.make_async_copy(wu.at[:, cols], wubuf.at[:, cols], sem.at[I0, j])
        return up, [pltpu.make_async_copy(wq.at[j], wqbuf.at[j], sem.at[I1, j]) for wq in (wq_near, wq_own)]

    def body(hs, ho, rs, ro, u, qkv, ctx, n1, n2):
        step = count[I0]
        count[I0] = step + I1
        for low, high, gain, dst in ((hs, ho, gains[I1:I2, :], n2), (rs, ro, gains[I0:I1, :], n1)):
            @pl.when(step < steps // I2)
            def _(low=low, gain=gain, dst=dst):
                norm_rows(low, gain, dst, BLOCK)

            @pl.when(step >= steps // I2)
            def _(high=high, gain=gain, dst=dst):
                norm_rows(high, gain, dst, BLOCK)

        @pl.when(step == I0)
        def _():
            for j in range(I3):
                up, (near, _) = pieces(j)
                up.wait()
                near.wait()

        def qkv_step(j, c):
            qkv[:, lanes(j * SUB, SUB)] = mm(n1[...], wqbuf[j // I4, :, lanes(j % I4 * SUB, SUB)]).astype(BF)
            return c
        lax.fori_loop(I0, I3 * half // SUB, qkv_step, I0)

        def head_step(j, c):
            at = [(pl.ds(s, seq), r * HEAD_PAD) for s in range(I0, BLOCK, seq) for r in range(I4)]
            base = j * (I4 * HEAD_PAD)

            def up_blocks(first):
                for n in range(I3):
                    cols = lanes((j * I6 + first + n) * SUB, SUB)
                    u[:, cols] = mm(n2[...], wubuf[:, cols]).astype(BF)
            views = [[qkv[rows, lanes(base + t * half + col, HEAD_PAD)] for t in range(I3)] for rows, col in at]
            between = [functools.partial(up_blocks, I0), functools.partial(up_blocks, I3)]
            for (rows, col), context in zip(at, attention_forward(views, scale, between)):
                ctx[rows, lanes(base + col, HEAD_PAD)] = context
            return c
        lax.fori_loop(I0, I2, head_step, I0)

    received = nothing if early else hand_on(place, refs[I0], outs[I6], outs[7], sems)

    @pl.when(place.home < I2 if early else place.home > I1)
    def _():
        for j in range(I3):
            up, (near, mine) = pieces(j)
            up.start()
            pl.when(place.is_l)(near.start)
            pl.when(jnp.logical_not(place.is_l))(mine.start)
        count[I0] = I0
        low = pl.BlockSpec((BLOCK, width), lambda i: (jnp.minimum(i, steps // I2 - I1), I0))
        high = pl.BlockSpec((BLOCK, width), lambda i: (jnp.maximum(i - steps // I2, I0), I0))
        block = lambda n: pl.BlockSpec((BLOCK, n), lambda i: (i, I0))
        pltpu.emit_pipeline(body, grid=(steps,), in_specs=[low, high, low, high],
                            out_specs=[block(ffn // I2), block(I3 * half), block(half), block(width), block(width)])(
            h_same, h_other, a_same, a_other, u_o, qkv_o, ctx_o, n1_o, n2_o)
    received()


def owner_recompute(dims, early, again, h_rows, a_rows, gains, w_qkv, w_up):
    micro, seq, width, heads, head_dim, ffn = dims
    half = heads // I2 * HEAD_PAD
    tokens = I2 * micro * seq
    any_spec = pl.BlockSpec(memory_space=ANY)
    vmem = pltpu.VMEM
    earlier = () if early else tuple(again)
    act = (micro, seq, width)
    out_shape = [jax.ShapeDtypeStruct((I8, 128), F32), *shapes((tokens, ffn // I2), (tokens, I3 * half), (tokens, half), (tokens, width), (tokens, width))]
    if not early:
        out_shape += shapes((micro, I2, seq, width), act)
    aliases = {} if early else {9 + i: I1 + i for i in range(5)} | {14: 7}
    comm = {} if early else dict(collective_id=I3)
    return pl.pallas_call(
        functools.partial(recompute_kernel, dims, early),
        out_shape=tuple(out_shape),
        in_specs=[any_spec] * I4 + [pl.BlockSpec(memory_space=vmem)] + [any_spec] * (I3 + len(earlier)),
        out_specs=(any_spec,) * len(out_shape),
        scratch_shapes=[vmem((I3, width, CHUNK), BF), vmem((width, ffn // I2), BF), pltpu.SMEM((I1,), jnp.int32), pltpu.SemaphoreType.DMA((I2, I3)), pltpu.SemaphoreType.DMA((I4,))],
        input_output_aliases=aliases,
        compiler_params=pltpu.CompilerParams(**comm, has_side_effects=True, vmem_limit_bytes=VMEM_LIMIT),
        name='owner_recompute',
    )(*h_rows, *a_rows, gains, *w_qkv, w_up, *earlier)


def spread_dx(step, last, dx, d_in, og_same, og_other, bounce, here_sem, parent_sem, sib_sem, send_sems, og_sems, ready):
    place = Place()
    micro = dx.shape[I0]
    along_x = place.at(place.tp, (place.stage + I2) % I4)
    barrier = pltpu.get_barrier_semaphore()
    is_leaf = place.home > I1
    gives_g = (place.home == I1) & place.is_l
    takes_g = (place.home == I0) & jnp.logical_not(place.is_l)
    late = late_rows(micro)
    rest_same = [m for m in late if m >= I4]

    def block(m):
        return d_in.at[m, place.core]

    def to_sibling(m, src):
        remote(src, block(m), send_sems.at[I0], sib_sem, place.sibling).start()

    def tell(there):
        pl.semaphore_signal(barrier, inc=I1, device_id=there, device_id_type=MESH)

    @pl.when(step == I0)
    def _():
        tell(place.sibling)

        @pl.when(takes_g)
        def _():
            tell(place.across)

        @pl.when(is_leaf)
        def _():
            pl.semaphore_wait(barrier, I2)
            pl.semaphore_signal(ready, inc=I1, device_id=along_x, device_id_type=MESH)

        @pl.when(jnp.logical_not(is_leaf))
        def _():
            tell(along_x)
            pl.semaphore_wait(barrier, I1 + gives_g.astype(jnp.int32))

        @pl.when(gives_g)
        def _():
            for m in rest_same:
                remote(og_same.at[m], og_same.at[m], og_sems.at[I2], og_sems.at[I3], place.across).start()
            for m in late:
                remote(og_other.at[m], og_other.at[m], og_sems.at[I0], og_sems.at[I1], place.across).start()

    @pl.when((step == I1) & jnp.logical_not(is_leaf))
    def _():
        pl.semaphore_wait(ready, I1)
        for m in reversed(range(micro)):
            if m < micro - EARLY_DX:
                remote(dx.at[m], block(m), send_sems.at[I1], parent_sem.at[m], along_x).start()
            to_sibling(m, dx.at[m])
        pltpu.make_async_copy(dx, bounce, here_sem).start()

    @pl.when((step == I2) & jnp.logical_not(is_leaf))
    def _():
        pltpu.make_async_copy(dx, bounce, here_sem).wait()
        for m in range(micro):
            pltpu.make_async_copy(bounce.at[m], block(m), here_sem).start()

    part, part_same = og_other.at[I0:len(late)], og_same.at[I0:len(rest_same)]

    @pl.when((step == I1) & takes_g)
    def _():
        remote(part_same, part_same, og_sems.at[I2], og_sems.at[I3], place.across).wait_recv()

    @pl.when((step == I3) & takes_g)
    def _():
        remote(part, part, og_sems.at[I0], og_sems.at[I1], place.across).wait_recv()

    @pl.when((step == last) & is_leaf)
    def _():
        for m in reversed(range(micro)):
            if m < micro - EARLY_DX:
                remote(block(m), block(m), send_sems.at[I0], parent_sem.at[m], place.sibling).wait_recv()
            to_sibling(m, block(m))

    @pl.when(step == last)
    def _():
        remote(dx, dx, send_sems.at[I0], sib_sem, place.sibling).wait_send()

        @pl.when(jnp.logical_not(is_leaf))
        def _():
            rest = dx.at[I0:micro - EARLY_DX]
            remote(rest, rest, send_sems.at[I1], sib_sem, place.sibling).wait_send()
            pltpu.make_async_copy(dx, dx, here_sem).wait()

        @pl.when(gives_g)
        def _():
            remote(part, part, og_sems.at[I0], og_sems.at[I1], place.across).wait_send()
            remote(part_same, part_same, og_sems.at[I2], og_sems.at[I3], place.across).wait_send()
        remote(dx, dx, send_sems.at[I0], sib_sem, place.sibling).wait_recv()


def owner_backward_kernel(dims, dx, ds, do, u, qkv, wo, wd_near, wd_own, gs_in, go_in, d_first, dqkv, dup, z, d_in, og_other, og_same,
                          dmid, gbuf, dctx, wobuf, wdbuf, bounce, sem, wd_sem, g_sem, here_sem, parent_sem, sib_sem, send_sems, og_sems, ready):
    micro, seq, width, heads, head_dim, ffn = dims
    half = heads // I2 * HEAD_PAD
    scale = head_dim ** -0.5
    step, steps = pl.program_id(I0), pl.num_programs(I0)
    spread_dx(step, steps - I1, dx, d_in, og_same, og_other, bounce, here_sem, parent_sem, sib_sem, send_sems, og_sems, ready)

    def g_load(n, start):
        rows = BLOCK // seq
        for og, low in ((og_same, I0), (og_other, steps // I2)):
            @pl.when((n >= low) & (n < low + steps // I2))
            def _(og=og, low=low):
                copy = pltpu.make_async_copy(og.at[pl.ds((n - low) * rows, rows)], gbuf.at[n % I2], g_sem.at[n % I2])
                copy.start() if start else copy.wait()

    @pl.when(step == I0)
    def _():
        g_load(step, True)
        is_l = Place().is_l
        for condition, wd in ((is_l, wd_near), (jnp.logical_not(is_l), wd_own)):
            pl.when(condition)(pltpu.make_async_copy(wd, wdbuf, wd_sem).start)
        wobuf[...] = jnp.zeros_like(wobuf)
        load_heads(wo, I0, wobuf, sem)
        pltpu.make_async_copy(wo, wobuf.at[I0:wo.shape[I0]], sem).wait()
        pltpu.make_async_copy(wd_near, wdbuf, wd_sem).wait()
    g_load(step + I1, True)

    @pl.when(step < steps // I2)
    def _():
        dmid[...] = ds[...]

    @pl.when(step >= steps // I2)
    def _():
        dmid[...] = do[...]

    def ctx_step(j, c):
        rows = pl.ds(pl.multiple_of(j * SUB, SUB), SUB)
        dctx[:, lanes(j * SUB, SUB)] = mm_nt(dmid[...], wobuf[rows, :]).astype(BF)
        return c
    lax.fori_loop(I0, half // SUB, ctx_step, I0)
    g_load(step, False)
    grad = gbuf.at[step % I2]

    def mlp_block(n):
        cols = lanes(n * SUB, SUB)
        dz = mm(grad[...].reshape(BLOCK, width), wdbuf[n // I4, :, lanes(n % I4 * SUB, SUB)]).astype(BF).astype(F32)
        up = u[:, cols].astype(F32)
        gate, up2 = gelu_gate(up)
        hidden = up * gate
        z[:, cols] = hidden.astype(BF)
        dup[:, cols] = (dz * gelu_slope(hidden, gate, up2)).astype(BF)

    def both_step(j, c):
        base = j * (I2 * HEAD_PAD)
        at = [(pl.ds(s, seq), base + r * HEAD_PAD) for s in range(I0, BLOCK, seq) for r in range(I2)]
        group = [(*(qkv[rows, lanes(t * half + col, HEAD_PAD)] for t in range(I3)), dctx[rows, lanes(col, HEAD_PAD)]) for rows, col in at]
        blocks = [functools.partial(mlp_block, j * I3 + r) for r in range(I3)]
        for (rows, col), grads in zip(at, attention_backward(group, scale, blocks)):
            for t, value in enumerate(grads):
                dqkv[rows, lanes(t * half + col, HEAD_PAD)] = value
        return c
    lax.fori_loop(I0, heads // I4, both_step, I0)


def owner_backward(dims, dx, d_in, d_rows, og, ups, qkv, w_out, w_down):
    micro, seq, width, heads, head_dim, ffn = dims
    half = heads // I2 * HEAD_PAD
    tokens = I2 * micro * seq
    blocks = tokens // BLOCK
    vmem, dma = pltpu.VMEM, pltpu.SemaphoreType.DMA
    any_spec = pl.BlockSpec(memory_space=ANY)
    low = pl.BlockSpec((BLOCK, width), lambda i: (jnp.minimum(i, blocks // I2 - I1), I0))
    high = pl.BlockSpec((BLOCK, width), lambda i: (jnp.maximum(i - blocks // I2, I0), I0))
    attn_block = pl.BlockSpec((BLOCK, I3 * half), lambda i: (i, I0))
    mlp_block = pl.BlockSpec((BLOCK, ffn // I2), lambda i: (i, I0))
    act = (micro, seq, width)
    return pl.pallas_call(
        functools.partial(owner_backward_kernel, dims),
        grid=(blocks,),
        out_shape=tuple(shapes((tokens, I3 * half), (tokens, ffn // I2), (tokens, ffn // I2), (micro, I2, seq, width), act, act)),
        in_specs=[any_spec, low, high, mlp_block, attn_block, *[any_spec] * I6],
        out_specs=(attn_block, mlp_block, mlp_block, any_spec, any_spec, any_spec),
        scratch_shapes=[vmem((BLOCK, width), BF), vmem((I2, BLOCK // seq, seq, width), BF), vmem((BLOCK, half), BF), vmem((half, width), BF), vmem((I3, width, CHUNK), BF), vmem(act, BF),
                        dma(()), dma(()), dma((I2,)), dma(()), dma((micro,)), dma(()), dma((I2,)), dma((I4,)), pltpu.SemaphoreType.REGULAR],
        input_output_aliases={I8: 5, 9: I4, 10: I3},
        compiler_params=pltpu.CompilerParams(collective_id=I2, has_side_effects=True, vmem_limit_bytes=VMEM_LIMIT),
        name='owner_backward',
    )(dx, *d_rows, ups, qkv, w_out, *w_down, *og, d_in)


def bring(pairs, sem):
    copies = [pltpu.make_async_copy(src, dst, sem.at[i]) for i, (src, dst) in enumerate(pairs)]
    for copy in copies:
        copy.start()
    for copy in copies:
        copy.wait()


def attn_products_kernel(dq, dk, dv, ctx, n1_o, ds, do, dx_in, dwq, dwo, dx_out, n1, dmid, dqkvt, ctxt, bounce, sem, dx_sem):
    tokens, width = n1.shape
    part = tokens // I2
    head_dim = dwo.shape[I1]
    step, last = pl.program_id(I0), pl.num_programs(I0) - I1
    into, out_of = pltpu.make_async_copy(dx_in, bounce, dx_sem), pltpu.make_async_copy(bounce, dx_out, dx_sem)

    @pl.when(step == I1)
    def _():
        into.start()

    @pl.when(step == I2)
    def _():
        into.wait()
        out_of.start()

    @pl.when(step == last)
    def _():
        out_of.wait()

    @pl.when(step == I0)
    def _():
        bring([(n1_o, n1), (ds, dmid.at[pl.ds(I0, part)]), (do, dmid.at[pl.ds(part, part)])], sem)

    def turn(rows):
        for t, block in enumerate((dq, dk, dv)):
            for r in range(I2):
                at = (I2 * t + r) * head_dim
                dqkvt[at:at + head_dim, rows] = block[rows, r * HEAD_PAD:(r + I1) * HEAD_PAD].T[I0:head_dim]
        for r in range(I2):
            ctxt[r * head_dim:(r + I1) * head_dim, rows] = ctx[rows, r * HEAD_PAD:(r + I1) * HEAD_PAD].T[I0:head_dim]
    rows_loop(tokens, SUB, turn)
    for c in range(I0, width, SUB):
        cut = slice(c, c + SUB)
        dwq[:, :, :, cut] = mm(dqkvt[...], n1[:, cut]).reshape(I3, I2, head_dim, SUB)
        dwo[:, :, cut] = mm(ctxt[...], dmid[:, cut]).reshape(I2, head_dim, SUB)


def attn_products(dqkv, ctx, n1, d_rows, dx, out_dims):
    heads, head_dim, width = out_dims
    tokens = n1.shape[I0]
    vmem = pltpu.VMEM
    any_spec = pl.BlockSpec(memory_space=ANY)
    pairs = heads // I2
    cols = lambda t: pl.BlockSpec((tokens, I2 * HEAD_PAD), lambda i: (I0, t * pairs + i))
    return pl.pallas_call(
        attn_products_kernel,
        grid=(pairs,),
        out_shape=(jax.ShapeDtypeStruct((I3,) + out_dims, F32), jax.ShapeDtypeStruct(out_dims, F32), jax.ShapeDtypeStruct(dx.shape, BF)),
        in_specs=[cols(I0), cols(I1), cols(I2), cols(I0), any_spec, any_spec, any_spec, any_spec],
        out_specs=(pl.BlockSpec((I3, I2, head_dim, width), lambda i: (I0, i, I0, I0)), pl.BlockSpec((I2, head_dim, width), lambda i: (i, I0, I0)), any_spec),
        scratch_shapes=[vmem((tokens, width), BF), vmem((tokens, width), BF), vmem((I6 * head_dim, tokens), BF), vmem((I2 * head_dim, tokens), BF),
                        vmem(dx.shape, BF), pltpu.SemaphoreType.DMA((I3,)), pltpu.SemaphoreType.DMA(())],
        compiler_params=pltpu.CompilerParams(vmem_limit_bytes=VMEM_LIMIT),
        name='attn_products',
    )(dqkv, dqkv, dqkv, ctx, n1, *d_rows, dx)


def mlp_products_kernel(dup, z, n2_o, gs, go, dwu, dwd, n2t, grad, zt, stage, sem):
    width, tokens = n2t.shape
    part = tokens // I2

    @pl.when(pl.program_id(I0) == I0)
    def _():
        bring([(n2_o, stage), (gs, grad.at[pl.ds(I0, part)]), (go, grad.at[pl.ds(part, part)])], sem)

        def turn(rows):
            for c in range(I0, width, SUB):
                n2t[c:c + SUB, rows] = stage[rows, c:c + SUB].T
        rows_loop(tokens, SUB, turn)

    def turn_z(rows):
        for c in range(I0, z.shape[I1], SUB):
            zt[c:c + SUB, rows] = z[rows, c:c + SUB].T
    rows_loop(tokens, SUB, turn_z)
    for c in range(I0, width, I2 * SUB):
        dwu[c:c + I2 * SUB, :] = mm(n2t[c:c + I2 * SUB, :], dup[...])
    for c in range(I0, width, SUB):
        dwd[:, c:c + SUB] = mm(zt[...], grad[:, c:c + SUB])


def mlp_products(dup, hidden, n2, g_rows):
    tokens, width = n2.shape
    cols = dup.shape[I1]
    vmem = pltpu.VMEM
    any_spec = pl.BlockSpec(memory_space=ANY)
    block = pl.BlockSpec((tokens, SUB), lambda i: (I0, i))
    return pl.pallas_call(
        mlp_products_kernel,
        grid=(cols // SUB,),
        out_shape=(jax.ShapeDtypeStruct((width, cols), F32), jax.ShapeDtypeStruct((cols, width), F32)),
        in_specs=[block, block, any_spec, any_spec, any_spec],
        out_specs=(pl.BlockSpec((width, SUB), lambda i: (I0, i)), pl.BlockSpec((SUB, width), lambda i: (i, I0))),
        scratch_shapes=[vmem((width, tokens), BF), vmem((tokens, width), BF), vmem((SUB, tokens), BF), vmem((tokens, width), BF), pltpu.SemaphoreType.DMA((I3,))],
        compiler_params=pltpu.CompilerParams(vmem_limit_bytes=VMEM_LIMIT),
        name='mlp_products',
    )(dup, hidden, n2, *g_rows)


def solution(mesh):
    act_spec = P('rep', None, None, None)
    weight_specs = (
        P(('rep', 'stage'), None, None, 'tp', None),
        P(('rep', 'stage'), 'tp', None, None),
        P(('rep', 'stage'), None, 'tp'),
        P(('rep', 'stage'), 'tp', None),
        P(('rep', 'stage'), None),
        P(('rep', 'stage'), None),
    )

    def device_fn(inputs, targets, w_qkv, w_out, w_up, w_down, gain_attn, gain_mlp):
        micro_count, _, seq_len, width = inputs.shape
        dims = (micro_count, seq_len, width, I2 * w_out.shape[I1], w_out.shape[I2], I2 * w_up.shape[I2])
        norm_factor = 1.0 / (inputs.size)
        own = (w_qkv[I0], w_out[I0], w_up[I0], w_down[I0])
        own_gains = jnp.concatenate([gain_attn, gain_mlp]).astype(F32)
        rows_of = (own[I0].transpose(I1, I2, I3, I0).reshape(-I1, width), own[I1].reshape(-I1, width), own[I2], own[I3])

        (acts, mids, qkv, ups, seeds, oh_same, oh_other, oa_same, oa_other, og_same, og_other, loss_tile, home_gains, *weights) = forward_phase(dims, inputs, targets, rows_of, own_gains)
        (nq, no, nu, nd), (fq, fo, fu, fd) = weights[I0:I4], weights[I4:I8]
        (tq0, to0, tu0, td0), (tq1, to1, tu1, td1), (tqo, tdo) = weights[I8:12], weights[12:16], weights[18:20]

        flat = lambda *rows: [r.reshape(-I1, width) for r in rows]
        done, *again = owner_recompute(dims, True, None, flat(oh_same, oh_other), flat(oa_same, oa_other), own_gains, (tq0, tqo), own[I2])
        dx, _, od_same, od_other, og_same, og_other, oa_same, oa_other, oh_same, oh_other, dg_same, dg_other, loss_all = backward_phase(
            dims, (acts, mids, qkv, ups, seeds), (rows_of[I0], nq, fq, td0, td1, to0, to1, tu0, tu1), home_gains, loss_tile, done,
            (og_same, og_other, oa_same, oa_other, oh_same, oh_other))
        _, *again, d_first, og_same = owner_recompute(dims, False, (dx, *again, og_same), flat(oh_same, oh_other), flat(oa_same, oa_other), own_gains, (tq0, tqo), own[I2])
        ups_own, qkv_own, ctx_own, n1, n2 = again
        d_rows = flat(od_same, od_other)
        d_qkv_rows, d_up_rows, hidden, dx_all, og_other, og_same = owner_backward(
            dims, dx, d_first, d_rows, (og_same, og_other), ups_own, qkv_own, rows_of[I1], (td0, tdo))
        d_qkv, d_out, d_inputs = attn_products(d_qkv_rows, ctx_own, n1, d_rows, dx_all, w_out.shape[I1:])
        d_up, d_down = mlp_products(d_up_rows, hidden, n2, flat(og_same, og_other))
        weight_grads = (d_qkv.transpose(I3, I0, I1, I2), d_out, d_up, d_down)
        mine = jnp.sum(dg_same + dg_other, I1)
        loss = jnp.sum(loss_all) * (0.5 * norm_factor)

        return (loss.reshape(I1), d_inputs) + tuple(g[None] for g in weight_grads) + (mine[I0][None], mine[I1][None])

    return jax.shard_map(device_fn, mesh=mesh, in_specs=(act_spec, act_spec) + weight_specs, out_specs=(P('rep'), act_spec) + weight_specs, check_vma=False)
```

```python
import functools

import jax
import jax.numpy as jnp
from jax import lax
from jax.experimental import pallas as pl
from jax.experimental.pallas import tpu as pltpu
from jax.sharding import PartitionSpec as P

NORM_EPS = 1e-5
BF = jnp.bfloat16
F32 = jnp.float32
MESH = pl.DeviceIdType.MESH
ANY = pl.ANY


GELU_A = 0.7978845608028654
GELU_B = 0.044715
I0, I1, I2, I3, I4, I6, I8 = 0, 1, 2, 3, 4, 6, 8
CHUNK = 1024
BLOCK = 384
SUB = 256
DEPTH = 6
BACK_DEPTH = 5
KDEPTH = 3
EARLY_G = 3
STAGGER_NS = 6000
EARLY_SEEDS = 5
EARLY_DX = 2
HEAD_PAD = 128
VMEM_LIMIT = 67043328


def mm(a, b):
    return lax.dot_general(a, b, (((I1,), (I0,)), ((), ())), preferred_element_type=F32)


def mm_nt(a, b):
    return lax.dot_general(a, b, (((I1,), (I1,)), ((), ())), preferred_element_type=F32)


def mm_tn(a, b):
    return lax.dot_general(a, b, (((I0,), (I0,)), ((), ())), preferred_element_type=F32)


class Place:
    def __init__(self):
        self.tp = lax.axis_index('tp')
        self.stage = lax.axis_index('stage')
        self.core = self.stage % I2
        self.x_pos = self.stage // I2
        self.home = self.x_pos * (I3 - I2 * self.tp) + self.tp
        self.is_l = self.stage == self.home
        self.sib = self.stage + I1 - I2 * self.core

    def at(self, tp, stage):
        return {'tp': tp, 'stage': stage}

    @property
    def sibling(self):
        return self.at(self.tp, self.sib)

    @property
    def along_x(self):
        return self.at(self.tp, (self.stage + I2) % I4)

    @property
    def across(self):
        return self.at(I1 - self.tp, self.stage)

    @property
    def across_other(self):
        return self.at(I1 - self.tp, self.sib)

    def chain(self, delta):
        there = self.home + delta
        x_pos = there // I2
        tp = there % I2 + x_pos * (I1 - I2 * (there % I2))
        return self.at(tp, I2 * x_pos + self.core)


def entry_barrier(place):
    barrier = pltpu.get_barrier_semaphore()
    for d_tp in (I0, I1):
        for d_stage in range(I4):
            if d_tp or d_stage:
                tp = place.tp + d_tp - I2 * d_tp * place.tp
                stage = (place.stage + d_stage) % I4
                pl.semaphore_signal(barrier, inc=I1, device_id=place.at(tp, stage), device_id_type=MESH)
    pl.semaphore_wait(barrier, 7)


def remote(src, dst, send_sem, recv_sem, device_id):
    return pltpu.make_async_remote_copy(src_ref=src, dst_ref=dst, send_sem=send_sem, recv_sem=recv_sem, device_id=device_id, device_id_type=MESH)


def rows_loop(total, step, body):
    def run(i, carry):
        body(pl.ds(pl.multiple_of(i * step, step), step))
        return carry
    lax.fori_loop(I0, total // step, run, I0)


def norm_rows(src, gain_row, dst, total):
    def body(rows):
        v = src[rows, :].astype(F32)
        inv = lax.rsqrt(jnp.mean(v * v, axis=-I1, keepdims=True) + NORM_EPS)
        dst[rows, :] = (v * inv * gain_row).astype(BF)
    rows_loop(total, 32, body)


def gelu_gate(u):
    u2 = u * u
    t = jnp.tanh(u * (GELU_A + (GELU_A * GELU_B) * u2))
    return 0.5 * t + 0.5, u2


def gelu_slope(hidden, gate, u2):
    return gate + hidden * (1.0 - gate) * (2.0 * GELU_A + (6.0 * GELU_A * GELU_B) * u2)


def row_parts(heads, cut=128):
    return [(*(x[low:high] for x in queries), *(x[:high] for x in keys), low)
            for queries, keys in heads for low, high in ((I0, cut), (cut, queries[I0].shape[I0]))]


def softmax_parts(scores, starts, keys_axis):
    masked = []
    for s, start in zip(scores, starts):
        k_pos = lax.broadcasted_iota(jnp.int32, s.shape, keys_axis)
        q_pos = lax.broadcasted_iota(jnp.int32, s.shape, I1 - keys_axis) + start
        masked.append(jnp.where(k_pos <= q_pos, s, -1e30))
    tops = [jnp.max(s, axis=keys_axis, keepdims=True) for s in masked]
    powers = [jnp.exp(s - top) for s, top in zip(masked, tops)]
    scales = [1.0 / jnp.sum(e, axis=keys_axis, keepdims=True) for e in powers]
    return [e * r for e, r in zip(powers, scales)]


def join_keys(top, low, cut=128):
    return jnp.concatenate([top + low[:cut], low[cut:]], I0).astype(BF)


def nothing():
    pass


def attention_forward(heads, scale, between=()):
    work = iter(between)
    units = row_parts([((q,), (k, v)) for q, k, v in heads])
    scores = [mm_nt(q, k) * scale for q, k, _, _ in units]
    next(work, nothing)()
    probs = softmax_parts(scores, [u[-I1] for u in units], I1)
    next(work, nothing)()
    parts = [mm(p.astype(BF), u[I2]) for p, u in zip(probs, units)]
    return [jnp.concatenate([a, b], I0).astype(BF) for a, b in zip(parts[I0::I2], parts[I1::I2])]


def attention_backward(heads, scale, between=()):
    work = iter(between)
    units = row_parts([((q, dc), (k, v)) for q, k, v, dc in heads])
    scores = [mm_nt(k, q) * scale for q, _, k, _, _ in units]
    dps = [mm_nt(v, dc) for _, dc, _, v, _ in units]
    next(work, nothing)()
    probs = softmax_parts(scores, [u[-I1] for u in units], I0)
    next(work, nothing)()
    dps = [dp.astype(BF).astype(F32) for dp in dps]
    deltas = [jnp.sum(dp * p, axis=I0, keepdims=True) for dp, p in zip(dps, probs)]
    dss = [p * (dp - delta) * scale for p, dp, delta in zip(probs, dps, deltas)]
    terms = []
    for ds in dss:
        hi = ds.astype(BF)
        rest = ds - hi.astype(F32)
        lo = rest.astype(BF)
        terms.append((hi, lo, (rest - lo.astype(F32)).astype(BF)))
    next(work, nothing)()
    dvs = [mm(p.astype(BF), u[I1]) for p, u in zip(probs, units)]
    dks = [mm(hi, u[I0]) + (mm(lo, u[I0]) + mm(tail, u[I0])) for (hi, lo, tail), u in zip(terms, units)]
    k_turned = [u[I2].T for u in units]
    dqs = [(mm(kt, hi) + (mm(kt, lo) + mm(kt, tail))).astype(BF) for (hi, lo, tail), kt in zip(terms, k_turned)]
    return [(jnp.concatenate([dqs[i].T, dqs[i + I1].T], I0), join_keys(dks[i], dks[i + I1]), join_keys(dvs[i], dvs[i + I1]))
            for i in range(I0, len(units), I2)]


def blocked(rows, stack, cols):
    total = mm(rows[:, I0:CHUNK], stack[I0, :, cols])
    for j in range(I1, stack.shape[I0]):
        total = total + mm(rows[:, j * CHUNK:(j + I1) * CHUNK], stack[j, :, cols])
    return total


def lanes(offset, size):
    return pl.ds(pl.multiple_of(offset, 128), size)


def load_resident(buf, sem, halves):
    for c in range(I6):
        for condition, ref in halves[c // I3]:
            copy = pltpu.make_async_copy(ref.at[(c % I3) * CHUNK:(c % I3 + I1) * CHUNK, :], buf.at[c], sem.at[c])
            if condition is None:
                copy.start()
            else:
                pl.when(condition)(copy.start)


def load_heads(ref, index, dst, sem):
    for r in range(I8):
        rows = pl.ds(pl.multiple_of(index * 768 + r * 96, 96), 96)
        pltpu.make_async_copy(ref.at[rows, :], dst.at[r * 128:r * 128 + 96, :], sem).start()


class Stream:
    def __init__(self, buf, sem, depth, parts, total, by_heads):
        self.buf, self.sem, self.depth, self.parts, self.total, self.by_heads = buf, sem, depth, parts, total, by_heads
        self.per_tick = sum(p[I1] for p in parts)

    def copy_in(self, ref, index, slot):
        if not self.by_heads:
            pltpu.make_async_copy(ref.at[index], self.buf.at[slot], self.sem.at[slot]).start()
            return
        load_heads(ref, index, self.buf.at[slot], self.sem.at[slot])

    def start(self, seq):
        @pl.when(seq < self.total)
        def _():
            j = seq % self.per_tick
            slot = seq % self.depth
            base = I0
            for choices, chunks in self.parts:
                for condition, ref in choices:
                    here = (j >= base) & (j < base + chunks)
                    here = here if condition is None else here & condition

                    @pl.when(here)
                    def _(ref=ref, low=base):
                        self.copy_in(ref, j - low, slot)
                base += chunks

    def prime(self):
        for seq in range(self.depth):
            self.start(jnp.int32(seq))

    def wait(self, seq):
        slot = seq % self.depth
        ref = self.parts[I0][I0][I0][I1]
        if self.by_heads:
            pltpu.make_async_copy(ref.at[I0:768, :], self.buf.at[slot, I0:768, :], self.sem.at[slot]).wait()
        else:
            pltpu.make_async_copy(ref.at[I0], self.buf.at[slot], self.sem.at[slot]).wait()
        return self.buf.at[slot]


PIECES = [(0, 0, 0), (0, 0, 1), (0, 0, 2), (1, 0, 0), (2, 1, 0), (2, 1, 1), (2, 1, 2), (2, 1, 3), (3, 0, 0), (3, 0, 1), (3, 0, 2), (3, 0, 3)]


ROUND = (11,)
ROUND_STEPS = (1,)
ORDER = (0, 1, 2, 3, 4, 5, 6, 7, 11, 8, 9, 10)


def piece(ref, axis, index):
    return ref.at[index * 768:(index + I1) * 768, :] if axis == I0 else ref.at[:, index * 768:(index + I1) * 768]


def weight_phase(place, is_r, own, near, far, turned, turned_own, up_chunks, wn, wk, send_sem, y_send, d_send, near_sem, far_sem, load_sem, store_sem, chunk_sem,
                 round_a, round_b, ra_sem, rb_sem, x_send, xd_send, rs_send):
    wk[...] = jnp.zeros_like(wk)
    early = place.home < I2

    def piece_of(arrays, c):
        i, axis, index = PIECES[c]
        return piece(arrays[i], axis, index)

    @pl.when(place.is_l)
    def _():
        for i in range(I4):
            remote(own[i], near[i], send_sem.at[i], near_sem.at[i], place.sibling).start()

    @pl.when(is_r)
    def _():
        for k, c in enumerate(ROUND):
            @pl.when(early)
            def _(k=k, c=c):
                remote(piece_of(own, c), round_a.at[k], x_send.at[k], ra_sem.at[k], place.along_x).start()
        for c, (i, axis, index) in enumerate(PIECES):
            if c not in ROUND:
                remote(piece_of(own, c), piece_of(far, c), y_send.at[i], far_sem.at[c], place.across_other).start()
        for k, c in enumerate(ROUND):
            @pl.when(jnp.logical_not(early))
            def _(k=k, c=c):
                remote(piece_of(own, c), piece_of(far, c), x_send.at[k], far_sem.at[c], place.across_other).start()

    def load(i, refs, t, slot):
        for condition, ref in refs:
            def go(ref=ref):
                if i < I2:
                    for r in range(I2):
                        rows = pl.ds(pl.multiple_of(t * 192 + r * 96, 96), 96)
                        pltpu.make_async_copy(ref.at[rows, :], wk.at[I0, pl.ds(slot * SUB + r * 128, 96), :], load_sem.at[slot]).start()
                elif i == I2:
                    pltpu.make_async_copy(ref.at[:, lanes(t * SUB, SUB)], wn.at[slot, :, I0:SUB], load_sem.at[slot]).start()
                else:
                    rows = pl.ds(pl.multiple_of(t * SUB, SUB), SUB)
                    pltpu.make_async_copy(ref.at[rows, :], wk.at[I0, pl.ds(512 + slot * SUB, SUB), :], load_sem.at[slot]).start()
            if condition is None:
                go()
            else:
                pl.when(condition)(go)

    def loaded(i, refs, slot):
        ref = refs[I0][I1]
        if i < I2:
            pltpu.make_async_copy(ref.at[I0:192, :], wk.at[I0, I0:192, :], load_sem.at[slot]).wait()
        elif i == I2:
            pltpu.make_async_copy(ref.at[:, I0:SUB], wn.at[slot, :, I0:SUB], load_sem.at[slot]).wait()
        else:
            pltpu.make_async_copy(ref.at[I0:SUB, :], wk.at[I0, 512:768, :], load_sem.at[slot]).wait()

    def store(i, dst, t, slot):
        if i == I2:
            rows = pl.ds(pl.multiple_of(t * SUB, SUB), SUB)
            return pltpu.make_async_copy(wk.at[I1, pl.ds(slot * SUB, SUB), :], dst.at[rows, :], store_sem.at[slot])
        return pltpu.make_async_copy(wn.at[slot, :, SUB:512], dst.at[t // I4, :, lanes(t % I4 * SUB, SUB)], store_sem.at[slot])

    def keep(which, t, slot):
        return pltpu.make_async_copy(wn.at[slot, :, I0:SUB], up_chunks[which].at[t // I4, :, lanes(t % I4 * SUB, SUB)], chunk_sem.at[slot])

    def turn(i, refs, which, first, count, dst=None):
        dst = turned[i][which] if dst is None else dst
        load(i, refs, first, I0)

        def step(n, c):
            slot = n % I2

            if i == I2:
                @pl.when(n > I0)
                def _():
                    keep(which, first + n - I1, I1 - slot).wait()

            @pl.when(n + I1 < count)
            def _():
                load(i, refs, first + n + I1, I1 - slot)
            loaded(i, refs, slot)
            if i == I2:
                keep(which, first + n, slot).start()

            @pl.when(n >= I2)
            def _():
                store(i, dst, first + n - I2, slot).wait()
            for b in range(I6):
                cut = slice(b * SUB, b * SUB + SUB)
                if i == I2:
                    wk[I1, pl.ds(pl.multiple_of(slot * SUB, SUB), SUB), cut] = wn[slot, cut, I0:SUB].T
                else:
                    base = I0 if i < I2 else 512
                    wn[slot, cut, SUB:512] = wk[I0, pl.ds(pl.multiple_of(base + slot * SUB, SUB), SUB), cut].T
            store(i, dst, first + n, slot).start()
            return c
        lax.fori_loop(I0, count, step, I0)
        for n in (count - I2, count - I1):
            store(i, dst, first + n, n % I2).wait()
        if i == I2:
            keep(which, first + count - I1, (count - I1) % I2).wait()

    counts = (12, I4, 12, 12)
    for i in range(I4):
        @pl.when(is_r)
        def _(i=i):
            remote(near[i], near[i], send_sem.at[i], near_sem.at[i], place.sibling).wait_recv()
        turn(i, [(place.is_l, own[i]), (is_r, near[i])], I0, I0, counts[i])
        if i < len(ROUND):
            @pl.when(place.is_l & jnp.logical_not(early))
            def _(k=i):
                remote(round_a.at[k], round_a.at[k], rs_send.at[k], ra_sem.at[k], place.sibling).wait_recv()
                remote(round_a.at[k], round_b.at[k], rs_send.at[k], rb_sem.at[k], place.across).start()

    @pl.when(is_r)
    def _():
        for i, dst in zip((I0, I3), turned_own):
            turn(i, [(None, own[i])], I0, I0, counts[i], dst)
    for c in ORDER:
        i, axis, index = PIECES[c]
        view = piece_of(far, c)
        for k, step in enumerate(ROUND_STEPS):
            if c == step:
                @pl.when(is_r & jnp.logical_not(early))
                def _(k=k):
                    remote(round_b.at[k], round_b.at[k], rs_send.at[k], rb_sem.at[k], place.sibling).wait_recv()
                    remote(round_b.at[k], piece_of(far, ROUND[k]), rs_send.at[k], far_sem.at[ROUND[k]], place.along_x).start()
        remote(view, view, d_send.at[i], far_sem.at[c], place.sibling).wait_recv()
        gives = is_r
        sem = d_send.at[i]
        if c in ROUND:
            gives = (early & place.is_l) | (jnp.logical_not(early) & is_r)
            sem = xd_send.at[ROUND.index(c)]

        @pl.when(gives)
        def _(c=c, view=view, sem=sem):
            remote(view, view, sem, far_sem.at[c], place.sibling).start()
        count = I4 if i < I2 else I3
        turn(i, [(None, far[i])], I1, index * count, count)

    @pl.when(place.is_l)
    def _():
        for i in range(I4):
            remote(own[i], near[i], send_sem.at[i], near_sem.at[i], place.sibling).wait_send()

    @pl.when(is_r)
    def _():
        for i in range(I4):
            part = own[i] if i < I3 else own[i].at[I0:(I4 - len(ROUND)) * 768, :]
            remote(part, part, y_send.at[i], far_sem.at[I0], place.across_other).wait_send()
            remote(part, part, d_send.at[i], far_sem.at[I0], place.sibling).wait_send()
        for k in range(len(ROUND)):
            remote(round_a.at[k], round_a.at[k], x_send.at[k], far_sem.at[I0], place.sibling).wait_send()

    @pl.when((early & place.is_l) | (jnp.logical_not(early) & is_r))
    def _():
        for k in range(len(ROUND)):
            remote(round_a.at[k], round_a.at[k], xd_send.at[k], far_sem.at[I0], place.sibling).wait_send()

    @pl.when(jnp.logical_not(early))
    def _():
        for k in range(len(ROUND)):
            remote(round_a.at[k], round_a.at[k], rs_send.at[k], far_sem.at[I0], place.sibling).wait_send()


def near_choices(place, own, near):
    return [(place.is_l, own), (jnp.logical_not(place.is_l), near)]


def forward_kernel(dims, x_ref, y_ref, wq, wo, wu, wd, own_gains,
                   a_s, h_s, qkv_s, u_s, g_s, oh_same, oh_other, oa_same, oa_other, og_same, og_other, loss_s, home_gains,
                   nq, no, nu, nd, fq, fo, fu, fd, tq0, to0, tu0, td0, tq1, to1, tu1, td1, uc0, uc1, tqo, tdo, round_a, round_b,
                   abuf, hbuf, obuf, nbuf, ybuf, sbuf, qkvbuf, ubuf, zbuf, ctxbuf, lossbuf, losstile, gains, wres, wores, wn,
                   send_sem, y_send, d_send, near_sem, far_sem, t_load, t_store, t_keep, ra_sem, rb_sem, x_send, xd_send, rs_send,
                   act_sem, hop_f, keep_sem, save_sem, stream_n, res_sem, out_sem, big_sem, y_sem, s_sem,
                   os_sem, oo_sem, as_sem, ao_sem, gs_sem, go_sem, bulk, gain_sem, tiny):
    micro, seq, width, heads, head_dim, ffn = dims
    place = Place()
    is_first, is_last = place.home == I0, place.home == I3
    home02 = (place.home == I0) | (place.home == I2)
    home13 = jnp.logical_not(home02)
    is_r = jnp.logical_not(place.is_l)
    takes_x = (place.home == I1) & is_r
    half = heads // I2 * HEAD_PAD
    scale = head_dim ** -0.5
    norm_factor = 1.0 / (micro * I2 * seq * width)
    own, near, far = (wq, wo, wu, wd), (nq, no, nu, nd), (fq, fo, fu, fd)
    turned = ((tq0, tq1), (to0, to1), (tu0, tu1), (td0, td1))
    entry_barrier(place)

    @pl.when(place.is_l)
    def _():
        pltpu.make_async_copy(own_gains, gains, gain_sem.at[I0]).start()
        remote(own_gains, gains, gain_sem.at[I1], gain_sem.at[I0], place.sibling).start()

    @pl.when(is_first)
    def _():
        for m in range(micro):
            pltpu.make_async_copy(x_ref.at[m, place.core], abuf.at[m], act_sem.at[m]).start()
    weight_phase(place, is_r, own, near, far, turned, (tqo, tdo), (uc0, uc1), wn, wores, send_sem, y_send, d_send, near_sem, far_sem, t_load, t_store, t_keep,
                 round_a, round_b, ra_sem, rb_sem, x_send, xd_send, rs_send)
    pltpu.make_async_copy(own_gains, gains, gain_sem.at[I0]).wait()
    pltpu.make_async_copy(gains, home_gains, gain_sem.at[I0]).start()

    @pl.when(place.is_l)
    def _():
        remote(own_gains, gains, gain_sem.at[I1], gain_sem.at[I0], place.sibling).wait_send()

    def near_of(i):
        return near_choices(place, own[i], near[i])

    def saved(dst, index):
        return pltpu.make_async_copy(hbuf, dst, save_sem.at[index])

    sn = Stream(wn, stream_n, DEPTH, [([(None, tq0)], I3), ([(None, tq1)], I3), ([(None, uc0)], I3), ([(None, uc1)], I3)], micro * 12, False)
    for c, choices in enumerate((near_of(I1), [(None, fo)])):
        for condition, ref in choices:
            def go(ref=ref, c=c):
                load_heads(ref, I0, wores.at[c], out_sem.at[c])
            go() if condition is None else pl.when(condition)(go)
    sn.prime()
    load_resident(wres, res_sem, (near_of(I3), [(None, fd)]))
    lossbuf[...] = jnp.zeros_like(lossbuf)

    def qkv_out(m):
        return pltpu.make_async_copy(qkvbuf, qkv_s.at[m], big_sem.at[I0])

    def up_out(m):
        return pltpu.make_async_copy(ubuf, u_s.at[m], big_sem.at[I1])

    def act_out(m):
        return pltpu.make_async_copy(abuf.at[m], a_s.at[m], save_sem.at[I2])

    def hop_block(m, n):
        cols = lanes(n * SUB, SUB)
        return remote(obuf.at[m % I2, :, cols], abuf.at[m, :, cols], hop_f.at[m % I2], act_sem.at[m], place.chain(I1))

    def hop_forward(m):
        return remote(obuf.at[m % I2], abuf.at[m], hop_f.at[m % I2], act_sem.at[m], place.chain(I1))

    def near_hand(src, dst_far, dst_own, sem, recv_sem):
        return (lambda: remote(src, dst_far, sem, recv_sem, place.sibling)), (lambda: pltpu.make_async_copy(src, dst_own, sem))

    def hand_out(m):
        return near_hand(obuf.at[m % I2], oa_other.at[m], oa_same.at[m], keep_sem.at[m % I2], ao_sem)

    def both_kinds(condition, copies, start):
        far_copy, own_copy = copies

        @pl.when(condition & place.is_l)
        def _():
            far_copy().start() if start else far_copy().wait_send()

        @pl.when(condition & is_r)
        def _():
            own_copy().start() if start else own_copy().wait()

    def x_out(m):
        return pltpu.make_async_copy(ybuf, oa_same.at[m], y_sem), pltpu.make_async_copy(sbuf, oa_other.at[m], s_sem)

    def seed_out(m):
        return pltpu.make_async_copy(sbuf, g_s.at[m], s_sem)

    def far_mid(m, condition):
        @pl.when(condition & place.is_l)
        def _():
            remote(h_s.at[m], oh_same.at[m], bulk.at[I2], os_sem, place.across).start()

        @pl.when(condition & is_r)
        def _():
            remote(h_s.at[m], oh_other.at[m], bulk.at[I2], oo_sem, place.across_other).start()

    def send_seed(m):
        seed_out(m).wait()

        @pl.when(place.is_l & (m < EARLY_SEEDS))
        def _():
            remote(g_s.at[m], og_same.at[m], bulk.at[I1], gs_sem, place.across).start()

        @pl.when(is_r & (m < EARLY_SEEDS))
        def _():
            remote(g_s.at[m], og_other.at[m], bulk.at[I1], go_sem, place.across_other).start()

    def forward_tick(m, carry):
        act, mid, out = abuf.at[m], hbuf, obuf.at[m % I2]
        pltpu.make_async_copy(x_ref.at[m, place.core], act, act_sem.at[m]).wait()
        act_out(m).start()

        @pl.when(place.is_l)
        def _():
            pltpu.make_async_copy(act, oa_same.at[m], as_sem).start()

        @pl.when(is_last)
        def _():
            pltpu.make_async_copy(y_ref.at[m, place.core], ybuf, y_sem).start()

        @pl.when(takes_x)
        def _():
            @pl.when(m > I0)
            def _():
                for copy in x_out(m):
                    copy.wait()
            for core, buf, sem in ((place.core, ybuf, y_sem), (I1 - place.core, sbuf, s_sem)):
                pltpu.make_async_copy(x_ref.at[m, core], buf, sem).start()
        norm_rows(act, gains[I0:I1, :], nbuf, seq)

        @pl.when(m > I0)
        def _():
            qkv_out(m).wait()

        def qkv_step(j, c):
            w = sn.wait(m * 12 + j)
            for n in range(I0, CHUNK, SUB):
                qkvbuf[:, lanes(j * CHUNK + n, SUB)] = mm(nbuf[...], w[:, n:n + SUB]).astype(BF)
            sn.start(m * 12 + j + DEPTH)
            return c
        lax.fori_loop(I0, I6, qkv_step, I0)
        qkv_out(m).start()
        act_out(m).wait()

        @pl.when(is_r)
        def _():
            remote(a_s.at[m], oa_other.at[m], bulk.at[I0], ao_sem, place.sibling).start()

        def head_step(i, c):
            base = i * (I3 * half)
            views = [[qkvbuf[:, lanes(base + t * half + r * HEAD_PAD, HEAD_PAD)] for t in range(I3)] for r in range(I8)]
            for r, context in enumerate(attention_forward(views, scale)):
                ctxbuf[:, lanes(i * half + r * HEAD_PAD, HEAD_PAD)] = context
            return c
        lax.fori_loop(I0, I2, head_step, I0)

        @pl.when(m == I0)
        def _():
            for c in range(I2):
                pltpu.make_async_copy(wo, wores.at[c, I0:768, :], out_sem.at[c]).wait()
        for n in range(I0, width, SUB):
            total = mm(ctxbuf[:, I0:half], wores[I0, :, n:n + SUB]) + mm(ctxbuf[:, half:I2 * half], wores[I1, :, n:n + SUB])
            mid[:, n:n + SUB] = (act[:, n:n + SUB].astype(F32) + total).astype(BF)
        saved(h_s.at[m], I0).start()

        @pl.when(place.is_l)
        def _():
            saved(oh_same.at[m], I1).start()
        norm_rows(mid, gains[I1:I2, :], nbuf, seq)

        @pl.when(m > I0)
        def _():
            up_out(m).wait()

        def up_step(j, c):
            w = sn.wait(m * 12 + I6 + j)
            for n in range(I0, CHUNK, SUB):
                u = mm(nbuf[...], w[:, n:n + SUB]).astype(BF)
                at = lanes(j * CHUNK + n, SUB)
                ubuf[:, at] = u
                uf = u.astype(F32)
                zbuf[:, at] = (uf * gelu_gate(uf)[I0]).astype(BF)
            sn.start(m * 12 + I6 + j + DEPTH)
            return c
        lax.fori_loop(I0, I6, up_step, I0)
        up_out(m).start()

        @pl.when((m > I1) & jnp.logical_not(is_last))
        def _():
            hop_forward(m).wait_send()

        both_kinds((m > I1) & home02, hand_out(m), False)

        @pl.when(m == I0)
        def _():
            for j in range(I6):
                pltpu.make_async_copy(wd.at[I0:CHUNK, :], wres.at[j], res_sem.at[j]).wait()

        def down_step(n, c):
            cols = lanes(n * SUB, SUB)
            out[:, cols] = (mid[:, cols].astype(F32) + blocked(zbuf, wres, cols)).astype(BF)

            @pl.when((n > I0) & jnp.logical_not(is_last))
            def _():
                hop_block(m, n - I1).start()
            return c
        lax.fori_loop(I0, width // SUB, down_step, I0)

        @pl.when(jnp.logical_not(is_last))
        def _():
            hop_block(m, width // SUB - I1).start()

        both_kinds(home02, hand_out(m), True)

        @pl.when(is_last)
        def _():
            pltpu.make_async_copy(y_ref.at[m, place.core], ybuf, y_sem).wait()

            @pl.when(m > I0)
            def _():
                send_seed(m - I1)

            def seed(rows):
                error = out[rows, :].astype(F32) - ybuf[rows, :].astype(F32)
                sbuf[rows, :] = (error * norm_factor).astype(BF)
                lossbuf[...] += jnp.sum((error * error).reshape(I4, I8, width), axis=I0)
            rows_loop(seq, 32, seed)
            seed_out(m).start()

        @pl.when(takes_x)
        def _():
            for core, buf, sem in ((place.core, ybuf, y_sem), (I1 - place.core, sbuf, s_sem)):
                pltpu.make_async_copy(x_ref.at[m, core], buf, sem).wait()
            for copy in x_out(m):
                copy.start()

        saved(h_s.at[m], I0).wait()

        @pl.when(place.is_l)
        def _():
            saved(oh_same.at[m], I1).wait()

        @pl.when(is_r)
        def _():
            remote(h_s.at[m], oh_other.at[m], bulk.at[I3], oo_sem, place.sibling).start()

        far_mid(m, home13 | (m % I2 == I1))
        return carry

    @pl.when(is_first & (place.core == I0))
    def _():
        pl.delay(STAGGER_NS)
    lax.fori_loop(I0, micro, forward_tick, I0)
    for m in range(I0, micro, I2):
        far_mid(m, is_first)

    @pl.when(is_last)
    def _():
        total = lossbuf[:, I0:128]
        for n in range(128, width, 128):
            total = total + lossbuf[:, n:n + 128]
        losstile[...] = total
        pltpu.make_async_copy(losstile, loss_s, tiny).start()
    for copy in (qkv_out(micro - I1), up_out(micro - I1)):
        copy.wait()

    @pl.when(jnp.logical_not(is_last))
    def _():
        for m in (micro - I2, micro - I1):
            hop_forward(m).wait_send()
    for m in (micro - I2, micro - I1):
        both_kinds(home02, hand_out(m), False)

    @pl.when(is_last)
    def _():
        seed_out(micro - I1).wait()
        pltpu.make_async_copy(losstile, loss_s, tiny).wait()

    @pl.when(takes_x)
    def _():
        for copy in x_out(micro - I1):
            copy.wait()
    pltpu.make_async_copy(gains, home_gains, gain_sem.at[I0]).wait()
    sent, got = drain(place)

    @pl.when(place.home != I2)
    def _():
        sent(h_s, bulk.at[I2])

    @pl.when(place.home == I2)
    def _():
        sent(h_s.at[I0:micro // I2], bulk.at[I2])

    @pl.when(place.is_l | jnp.logical_not(is_last))
    def _():
        got(oh_other, oo_sem)

    @pl.when(is_r & is_last)
    def _():
        got(oh_other.at[I0:micro // I2], oo_sem)

    @pl.when(is_last)
    def _():
        sent(g_s.at[I0:EARLY_SEEDS], bulk.at[I1])

    @pl.when((place.home == I2) & is_r)
    def _():
        got(og_same.at[I0:EARLY_SEEDS], gs_sem)
        got(og_other.at[I0:EARLY_SEEDS], go_sem)

    @pl.when(is_r)
    def _():
        sent(a_s, bulk.at[I0])
        sent(h_s, bulk.at[I3])

    @pl.when(is_r & jnp.logical_not(is_last))
    def _():
        got(oh_same, os_sem)

    @pl.when(is_r & is_last)
    def _():
        got(oh_same.at[I0:micro // I2], os_sem)

    @pl.when(place.is_l)
    def _():
        got(oa_same, as_sem)

    @pl.when(place.is_l | home02)
    def _():
        got(oa_other, ao_sem)


def drain(place):
    def sent(buf, sem):
        remote(buf, buf, sem, sem, place.sibling).wait_send()

    def got(dst, sem):
        pltpu.make_async_copy(dst, dst, sem).wait()
    return sent, got


def backward_kernel(dims, a_s, h_s, qkv_s, u_s, g_s, wq, nq, fq, td0, td1, to0, to1, tu0, tu1, gains, loss_s, after, *refs):
    (dx_s, m_s, od_same, od_other, og_same, og_other, oa_same, oa_other, oh_same, oh_other, dg_same, dg_other, loss_all,
     gbuf, hbuf, obuf, qkvbuf, ubuf, habuf, zbuf, ctxbuf, dqkvbuf, acc, accg, wres, wn, wk,
     grad_sem, hop_b, back_sem, dx_sem, dx_send, save_sem, stream_n, stream_k, res_sem, load_sem,
     ds_sem, do_sem, gs_sem, go_sem, as_sem, ao_sem, os_sem, oo_sem, bulk, tiny, loss_sem, ready) = refs[I6:]
    micro, seq, width, heads, head_dim, ffn = dims
    place = Place()
    is_first, is_last = place.home == I0, place.home == I3
    home13 = (place.home == I1) | is_last
    is_r = jnp.logical_not(place.is_l)
    half = heads // I2 * HEAD_PAD
    scale = head_dim ** -0.5

    barrier = pltpu.get_barrier_semaphore()
    is_b, is_c = place.home == I1, place.home == I2
    pl.semaphore_signal(barrier, inc=I1, device_id=place.sibling, device_id_type=MESH)

    @pl.when(jnp.logical_not(is_first))
    def _():
        for there in (place.across, place.across_other):
            pl.semaphore_signal(barrier, inc=I1, device_id=there, device_id_type=MESH)

    @pl.when(is_c)
    def _():
        pl.semaphore_signal(barrier, inc=I1, device_id=place.along_x, device_id_type=MESH)

    @pl.when(is_last)
    def _():
        for m in range(micro):
            pltpu.make_async_copy(g_s.at[m], gbuf.at[m], grad_sem.at[m]).start()
    wk[...] = jnp.zeros_like(wk)
    bn = Stream(wn, stream_n, BACK_DEPTH, [([(None, td0)], I3), ([(None, td1)], I3), ([(None, to0)], I1), ([(None, to1)], I1)], micro * I8, False)
    bk = Stream(wk, stream_k, KDEPTH, [(near_choices(place, wq, nq), I3), ([(None, fq)], I3)], micro * I6, True)
    bn.prime()
    bk.prime()
    load_resident(wres, res_sem, ([(None, tu0)], [(None, tu1)]))

    def saved(dst, index):
        return pltpu.make_async_copy(hbuf, dst, save_sem)

    def both_kinds(condition, copies, start):
        far_copy, own_copy = copies

        @pl.when(condition & place.is_l)
        def _():
            far_copy().start() if start else far_copy().wait_send()

        @pl.when(condition & is_r)
        def _():
            own_copy().start() if start else own_copy().wait()

    def near_hand(src, dst_far, dst_own, sem, recv_sem):
        return (lambda: remote(src, dst_far, sem, recv_sem, place.sibling)), (lambda: pltpu.make_async_copy(src, dst_own, sem))

    def loads(i):
        m = micro - I1 - i
        return [pltpu.make_async_copy(src.at[m], dst, load_sem.at[k])
                for k, (src, dst) in enumerate(((u_s, ubuf), (qkv_s, qkvbuf), (h_s, habuf.at[I0]), (a_s, habuf.at[I1])))]

    def load_next(i, k):
        @pl.when(i + I1 < micro)
        def _():
            loads(i + I1)[k].start()

    for copy in loads(I0):
        copy.start()
    accg[...] = jnp.zeros_like(accg)

    def norm_back(index, x, base, dst, gain_row):
        def body(rows):
            xf = x[rows, :].astype(F32)
            dy = acc[rows, :].astype(BF).astype(F32)
            inv = lax.rsqrt(jnp.mean(xf * xf, axis=-I1, keepdims=True) + NORM_EPS)
            xn = xf * inv
            accg[index] += jnp.sum((dy * xn).reshape(I4, I8, width), axis=I0)
            dyg = dy * gain_row
            dx = inv * (dyg - xn * jnp.mean(dyg * xn, axis=-I1, keepdims=True))
            dst[rows, :] = (base[rows, :].astype(F32) + dx).astype(BF)
        rows_loop(seq, 32, body)

    def hop_back(i):
        m = micro - I1 - i
        return remote(obuf.at[i % I2], gbuf.at[m], hop_b.at[i % I2], grad_sem.at[m], place.chain(-I1))

    def hand_back(i):
        m = micro - I1 - i
        return near_hand(obuf.at[i % I2], og_other.at[m], og_same.at[m], back_sem.at[i % I2], go_sem)

    def keep_dx(i):
        return pltpu.make_async_copy(obuf.at[i % I2], dx_s.at[micro - I1 - i], back_sem.at[i % I2])

    def back_ready(i):
        both_kinds((i > I1) & home13, hand_back(i), False)

        @pl.when((i > I1) & is_first)
        def _():
            keep_dx(i).wait()
            dx_to_b(i).wait_send()

        @pl.when((i > I1) & jnp.logical_not(is_first))
        def _():
            hop_back(i).wait_send()

    def pass_loss(tile):
        @pl.when(jnp.logical_not(is_first))
        def _():
            remote(tile, loss_all.at[place.core], loss_sem.at[I0], loss_sem.at[I1], place.chain(-I1)).start()
        remote(tile, loss_all.at[place.core], loss_sem.at[I2], loss_sem.at[I3], place.sibling).start()

    def dx_to_b(i):
        return remote(obuf.at[i % I2], dx_s.at[micro - I1 - i], dx_send.at[i % I2], dx_sem, place.across)

    def backward_tick(i, carry):
        m = micro - I1 - i
        slot = i % I2
        grad, dmid, prev = gbuf.at[m], hbuf, obuf.at[slot]
        u_now, qkv_now, h_now, a_now = ubuf, qkvbuf, habuf.at[I0], habuf.at[I1]

        pltpu.make_async_copy(g_s.at[m], grad, grad_sem.at[m]).wait()

        @pl.when(place.is_l)
        def _():
            pltpu.make_async_copy(grad, og_same.at[m], gs_sem).start()
        load_u, load_qkv, load_h, load_a = loads(i)
        load_u.wait()

        def mlp_step(j, c):
            w = bn.wait(i * I8 + j)
            for n in range(I0, CHUNK, SUB):
                at = lanes(j * CHUNK + n, SUB)
                dz = mm(grad[...], w[:, n:n + SUB]).astype(BF).astype(F32)
                u = u_now[:, at].astype(F32)
                gate, u2 = gelu_gate(u)
                zbuf[:, at] = (dz * gelu_slope(u * gate, gate, u2)).astype(BF)
            bn.start(i * I8 + j + BACK_DEPTH)
            return c
        lax.fori_loop(I0, I6, mlp_step, I0)

        @pl.when(i == I0)
        def _():
            for j in range(I6):
                pltpu.make_async_copy(tu0.at[I0:CHUNK, :], wres.at[j], res_sem.at[j]).wait()

        def turn_back(n, c):
            cols = lanes(n * SUB, SUB)
            acc[:, cols] = blocked(zbuf, wres, cols)
            return c
        lax.fori_loop(I0, width // SUB, turn_back, I0)
        load_next(i, I0)
        load_h.wait()
        norm_back(I1, h_now, grad, dmid, gains[I1:I2, :])
        load_next(i, I2)

        @pl.when(place.is_l)
        def _():
            saved(od_same.at[m], I0).start()

        @pl.when(is_r)
        def _():
            saved(m_s.at[m], I0).start()
        for c in range(I2):
            w = bn.wait(i * I8 + I6 + c)
            for n in range(I0, CHUNK, SUB):
                ctxbuf[:, c * CHUNK + n:c * CHUNK + n + SUB] = mm(dmid[...], w[:, n:n + SUB]).astype(BF)
            bn.start(i * I8 + I6 + c + BACK_DEPTH)
        load_qkv.wait()

        def head_step(t, c):
            base = (t // I2) * (I3 * half) + (t % I2) * (I4 * HEAD_PAD)
            at = [[lanes(base + part * half + r * HEAD_PAD, HEAD_PAD) for part in range(I3)] for r in range(I4)]
            group = [(*(qkv_now[:, p] for p in at[r]), ctxbuf[:, lanes((t * I4 + r) * HEAD_PAD, HEAD_PAD)]) for r in range(I4)]
            for r, grads in enumerate(attention_backward(group, scale)):
                for p, value in zip(at[r], grads):
                    dqkvbuf[:, p] = value
            return c
        lax.fori_loop(I0, I2, lambda t, c: head_step(I2 * t + I1, head_step(I2 * t, c)), I0)
        load_next(i, I1)
        acc[...] = jnp.zeros_like(acc)

        def qkv_step(j, c):
            w = bk.wait(i * I6 + j)
            for n in range(I0, width, SUB):
                acc[:, n:n + SUB] += mm(dqkvbuf[:, lanes(j * CHUNK, CHUNK)], w[:, n:n + SUB])
            bk.start(i * I6 + j + KDEPTH)
            return c
        lax.fori_loop(I0, I6, qkv_step, I0)
        load_a.wait()
        back_ready(i)
        norm_back(I0, a_now, dmid, prev, gains[I0:I1, :])
        load_next(i, I3)

        @pl.when(i == I0)
        def _():
            @pl.when(is_last)
            def _():
                pl.semaphore_wait(barrier, I3)

            @pl.when(is_c)
            def _():
                pl.semaphore_wait(ready, I1)

            @pl.when(is_b)
            def _():
                pl.semaphore_wait(ready, I2)

            @pl.when(is_last)
            def _():
                pass_loss(loss_s)

        @pl.when(jnp.logical_not(is_first))
        def _():
            hop_back(i).start()

        @pl.when(is_first)
        def _():
            keep_dx(i).start()
            dx_to_b(i).start()
        both_kinds(home13, hand_back(i), True)

        @pl.when(place.is_l)
        def _():
            saved(od_same.at[m], I0).wait()
            remote(od_same.at[m], od_same.at[m], bulk.at[I6], ds_sem, place.across).start()

        @pl.when(is_r)
        def _():
            remote(grad, og_other.at[m], bulk.at[5], go_sem, place.sibling).start()
            saved(m_s.at[m], I0).wait()
            remote(m_s.at[m], od_other.at[m], bulk.at[I6], do_sem, place.sibling).start()
            remote(m_s.at[m], od_other.at[m], bulk.at[7], do_sem, place.across_other).start()

        now = (i % I2 == I1) & (i < I2 * EARLY_G)
        far_grad(m, (place.home == I1) & now)
        far_grad(micro - I1 - i // I2, is_last & now)
        return carry

    def far_grad(m, condition):
        @pl.when(condition & place.is_l)
        def _():
            remote(gbuf.at[m], og_same.at[m], bulk.at[I4], gs_sem, place.across).start()

        @pl.when(condition & is_r)
        def _():
            remote(gbuf.at[m], og_other.at[m], bulk.at[I4], go_sem, place.across_other).start()

    @pl.when(jnp.logical_not(is_last))
    def _():
        pl.semaphore_wait(barrier, I3 - is_b.astype(jnp.int32))

    @pl.when(is_first)
    def _():
        for there in (place.across, place.across_other):
            pl.semaphore_signal(ready, inc=I1, device_id=there, device_id_type=MESH)

    @pl.when(is_b)
    def _():
        pl.semaphore_signal(ready, inc=I1, device_id=place.along_x, device_id_type=MESH)

    @pl.when(is_c & place.is_l)
    def _():
        for t in range(micro):
            remote(a_s.at[t], oa_same.at[t], bulk.at[I8], as_sem, place.across).start()
        for t in range(I0, micro, I2):
            remote(h_s.at[t], oh_same.at[t], bulk.at[9], os_sem, place.across).start()

    @pl.when(is_c & is_r)
    def _():
        for t in range(micro):
            remote(a_s.at[t], oa_other.at[t], bulk.at[I8], ao_sem, place.across_other).start()
        for t in range(I0, micro, I2):
            remote(h_s.at[t], oh_other.at[t], bulk.at[9], oo_sem, place.across_other).start()
    lax.fori_loop(I0, micro, backward_tick, I0)
    loss_mine = loss_all.at[place.core]

    @pl.when(is_last)
    def _():
        own_loss = pltpu.make_async_copy(loss_s, loss_mine, loss_sem.at[I1])
        own_loss.start()
        own_loss.wait()

    @pl.when(jnp.logical_not(is_last))
    def _():
        remote(loss_mine, loss_mine, loss_sem.at[I0], loss_sem.at[I1], place.sibling).wait_recv()
        pass_loss(loss_mine)

    @pl.when(place.is_l)
    def _():
        pltpu.make_async_copy(accg, dg_same, tiny.at[I0]).start()
        remote(accg, dg_same, tiny.at[I1], tiny.at[I0], place.across).start()

    @pl.when(is_r)
    def _():
        remote(accg, dg_other, tiny.at[I1], tiny.at[I4], place.sibling).start()
        remote(accg, dg_other, tiny.at[I2], tiny.at[I4], place.across_other).start()

    for i in (micro - I2, micro - I1):
        back_ready(jnp.int32(i))

    sent, got = drain(place)
    sent(m_s, bulk.at[I6])

    @pl.when(is_r)
    def _():
        sent(gbuf, bulk.at[5])
        sent(m_s, bulk.at[7])
        remote(accg, dg_other, tiny.at[I2], tiny.at[I4], place.sibling).wait_send()

    @pl.when(home13)
    def _():
        sent(gbuf.at[I0:EARLY_G], bulk.at[I4])

    @pl.when(place.home == I1)
    def _():
        got(dx_s, dx_sem)

    @pl.when(jnp.logical_not(is_first))
    def _():
        remote(loss_mine, loss_mine, loss_sem.at[I0], loss_sem.at[I1], place.sibling).wait_send()
    remote(loss_mine, loss_mine, loss_sem.at[I2], loss_sem.at[I3], place.sibling).wait_send()
    remote(loss_mine, loss_mine, loss_sem.at[I2], loss_sem.at[I3], place.sibling).wait_recv()

    @pl.when(place.home == I2)
    def _():
        sent(a_s, bulk.at[I8])
        sent(h_s.at[I0:micro // I2], bulk.at[9])

    remote(accg, dg_other, tiny.at[I1], tiny.at[I4], place.sibling).wait_send()
    got(od_other, do_sem)

    @pl.when(place.is_l | home13)
    def _():
        got(og_other, go_sem)

    @pl.when(jnp.logical_not(home13) & is_r)
    def _():
        got(og_same.at[I0:EARLY_G], gs_sem)
        got(og_other.at[I0:EARLY_G], go_sem)
    got(dg_same, tiny.at[I0])
    got(dg_other, tiny.at[I4])

    @pl.when(is_r)
    def _():
        got(od_same, ds_sem)

    @pl.when(place.is_l)
    def _():
        got(og_same, gs_sem)

    @pl.when(is_last & is_r)
    def _():
        got(oa_same, as_sem)
        got(oa_other, ao_sem)
        got(oh_same.at[I0:micro // I2], os_sem)
        got(oh_other.at[I0:micro // I2], oo_sem)


def shapes(*dims_list):
    return [jax.ShapeDtypeStruct(d, BF) for d in dims_list]


def forward_phase(dims, x, y, own, own_gains):
    micro, seq, width, heads, head_dim, ffn = dims
    half = heads // I2 * HEAD_PAD
    act = (micro, seq, width)
    raw = [w.shape for w in own]
    turned = [(I3, width, CHUNK), (I1, width, CHUNK), (ffn // I2, width), (I3, width, CHUNK)]
    out_shape = shapes(act, act, (micro, seq, I6 * half), (micro, seq, ffn), *[act] * 7)
    out_shape += [jax.ShapeDtypeStruct(s, F32) for s in ((I8, 128), own_gains.shape)]
    out_shape += shapes(*raw, *raw, *turned, *turned, *[turned[I0]] * I4, *[(len(ROUND), 768, width)] * I2)
    any_spec = pl.BlockSpec(memory_space=ANY)
    vmem, dma = pltpu.VMEM, pltpu.SemaphoreType.DMA
    row = vmem((seq, width), BF)
    scratch = [
        vmem(act, BF), row, vmem((I2, seq, width), BF), row, row, row, vmem((seq, I6 * half), BF), vmem((seq, ffn), BF), vmem((seq, ffn), BF),
        vmem((seq, I2 * half), BF), vmem((I8, width), F32), vmem((I8, 128), F32), vmem((I2, width), F32),
        vmem((I6, CHUNK, width), BF), vmem((I2, CHUNK, width), BF), vmem((DEPTH, width, CHUNK), BF),
        dma((I4,)), dma((I4,)), dma((I4,)), dma((I4,)), dma((12,)), dma((I2,)), dma((I2,)), dma((I2,)), *[dma((len(ROUND),))] * 5,
        dma((micro,)), dma((I2,)), dma((I2,)), dma((I3,)), dma((DEPTH,)), dma((I6,)), dma((I2,)), dma((I2,)), dma(()), dma(()),
        dma(()), dma(()), dma(()), dma(()), dma(()), dma(()), dma((I4,)), dma((I2,)), dma(()),
    ]
    return pl.pallas_call(
        functools.partial(forward_kernel, dims),
        out_shape=tuple(out_shape),
        in_specs=[any_spec] * I6 + [pl.BlockSpec(memory_space=vmem)],
        out_specs=(any_spec,) * len(out_shape),
        scratch_shapes=scratch,
        compiler_params=pltpu.CompilerParams(collective_id=I0, has_side_effects=True, vmem_limit_bytes=VMEM_LIMIT),
        name='forward_phase',
    )(x, y, *own, own_gains)


def backward_phase(dims, saved, weights, gains, loss, after, placed):
    micro, seq, width, heads, head_dim, ffn = dims
    half = heads // I2 * HEAD_PAD
    act = (micro, seq, width)
    out_shape = shapes(*[act] * 10) + [jax.ShapeDtypeStruct((I2, I8, width), F32)] * I2 + [jax.ShapeDtypeStruct((I2, I8, 128), F32)]
    any_spec = pl.BlockSpec(memory_space=ANY)
    vmem, dma = pltpu.VMEM, pltpu.SemaphoreType.DMA
    scratch = [
        vmem(act, BF), vmem((seq, width), BF), vmem((I2, seq, width), BF), vmem((seq, I6 * half), BF), vmem((seq, ffn), BF),
        vmem((I2, seq, width), BF), vmem((seq, ffn), BF), vmem((seq, I2 * half), BF), vmem((seq, I6 * half), BF), vmem((seq, width), F32),
        vmem((I2, I8, width), F32), vmem((I6, CHUNK, width), BF), vmem((BACK_DEPTH, width, CHUNK), BF), vmem((KDEPTH, CHUNK, width), BF),
        dma((micro,)), dma((I2,)), dma((I2,)), dma(()), dma((I2,)), dma(()), dma((BACK_DEPTH,)), dma((KDEPTH,)), dma((I6,)), dma((I4,)),
        *[dma(())] * I8, dma((10,)), dma((5,)), dma((I4,)), pltpu.SemaphoreType.REGULAR,
    ]
    return pl.pallas_call(
        functools.partial(backward_kernel, dims),
        out_shape=tuple(out_shape),
        in_specs=[any_spec] * 14 + [pl.BlockSpec(memory_space=vmem)] * I2 + [any_spec] * 7,
        out_specs=(any_spec,) * len(out_shape),
        scratch_shapes=scratch,
        input_output_aliases={17 + i: I4 + i for i in range(I6)},
        compiler_params=pltpu.CompilerParams(collective_id=I1, has_side_effects=True, vmem_limit_bytes=VMEM_LIMIT),
        name='backward_phase',
    )(*saved, *weights, gains, loss, after, *placed)


def late_rows(micro):
    return [micro - I1 - i for i in range(micro) if i % I2 == I0 or i > I2 * EARLY_G]


def hand_on(place, dx, d_in, og, sems):
    micro = dx.shape[I0]
    barrier = pltpu.get_barrier_semaphore()
    late = [m for m in late_rows(micro) if m < I4]
    is_leaf = place.home > I1
    gives_g = (place.home == I1) & place.is_l
    takes_g = (place.home == I0) & jnp.logical_not(place.is_l)
    part, g_part = dx.at[I0:EARLY_DX], og.at[I0:len(late)]

    @pl.when(is_leaf)
    def _():
        pl.semaphore_signal(barrier, inc=I1, device_id=place.along_x, device_id_type=MESH)

    @pl.when(takes_g)
    def _():
        pl.semaphore_signal(barrier, inc=I1, device_id=place.across, device_id_type=MESH)

    @pl.when(jnp.logical_not(is_leaf))
    def _():
        pl.semaphore_wait(barrier, I1 + gives_g.astype(jnp.int32))

        @pl.when(gives_g)
        def _():
            for m in late:
                remote(og.at[m], og.at[m], sems.at[I2], sems.at[I3], place.across).start()
        for m in range(micro - EARLY_DX, micro):
            remote(dx.at[m], d_in.at[m, place.core], sems.at[I0], sems.at[I1], place.along_x).start()
        remote(part, part, sems.at[I0], sems.at[I1], place.along_x).wait_send()

        @pl.when(gives_g)
        def _():
            remote(g_part, g_part, sems.at[I2], sems.at[I3], place.across).wait_send()

    def received():
        @pl.when(is_leaf)
        def _():
            remote(part, part, sems.at[I0], sems.at[I1], place.along_x).wait_recv()

        @pl.when(takes_g)
        def _():
            remote(g_part, g_part, sems.at[I2], sems.at[I3], place.across).wait_recv()
    return received


def recompute_kernel(dims, early, h_same, h_other, a_same, a_other, gains, wq_near, wq_own, wu, *refs):
    (wqbuf, wubuf, count, sem, sems) = refs[-5:]
    outs = refs[:-5] if early else refs[7:-5]
    (done, u_o, qkv_o, ctx_o, n1_o, n2_o) = outs[I0:I6]
    micro, seq, width, heads, head_dim, ffn = dims
    place = Place()
    scale = head_dim ** -0.5
    half = heads // I2 * HEAD_PAD
    steps = I2 * micro * seq // BLOCK

    def pieces(j):
        cols = lanes(j * CHUNK, CHUNK)
        up = pltpu.make_async_copy(wu.at[:, cols], wubuf.at[:, cols], sem.at[I0, j])
        return up, [pltpu.make_async_copy(wq.at[j], wqbuf.at[j], sem.at[I1, j]) for wq in (wq_near, wq_own)]

    def body(hs, ho, rs, ro, u, qkv, ctx, n1, n2):
        step = count[I0]
        count[I0] = step + I1
        for low, high, gain, dst in ((hs, ho, gains[I1:I2, :], n2), (rs, ro, gains[I0:I1, :], n1)):
            @pl.when(step < steps // I2)
            def _(low=low, gain=gain, dst=dst):
                norm_rows(low, gain, dst, BLOCK)

            @pl.when(step >= steps // I2)
            def _(high=high, gain=gain, dst=dst):
                norm_rows(high, gain, dst, BLOCK)

        @pl.when(step == I0)
        def _():
            for j in range(I3):
                up, (near, _) = pieces(j)
                up.wait()
                near.wait()

        def qkv_step(j, c):
            qkv[:, lanes(j * SUB, SUB)] = mm(n1[...], wqbuf[j // I4, :, lanes(j % I4 * SUB, SUB)]).astype(BF)
            return c
        lax.fori_loop(I0, I3 * half // SUB, qkv_step, I0)

        def head_step(j, c):
            at = [(pl.ds(s, seq), r * HEAD_PAD) for s in range(I0, BLOCK, seq) for r in range(I4)]
            base = j * (I4 * HEAD_PAD)

            def up_blocks(first):
                for n in range(I3):
                    cols = lanes((j * I6 + first + n) * SUB, SUB)
                    u[:, cols] = mm(n2[...], wubuf[:, cols]).astype(BF)
            views = [[qkv[rows, lanes(base + t * half + col, HEAD_PAD)] for t in range(I3)] for rows, col in at]
            between = [functools.partial(up_blocks, I0), functools.partial(up_blocks, I3)]
            for (rows, col), context in zip(at, attention_forward(views, scale, between)):
                ctx[rows, lanes(base + col, HEAD_PAD)] = context
            return c
        lax.fori_loop(I0, I2, head_step, I0)

    received = nothing if early else hand_on(place, refs[I0], outs[I6], outs[7], sems)

    @pl.when(place.home < I2 if early else place.home > I1)
    def _():
        for j in range(I3):
            up, (near, mine) = pieces(j)
            up.start()
            pl.when(place.is_l)(near.start)
            pl.when(jnp.logical_not(place.is_l))(mine.start)
        count[I0] = I0
        low = pl.BlockSpec((BLOCK, width), lambda i: (jnp.minimum(i, steps // I2 - I1), I0))
        high = pl.BlockSpec((BLOCK, width), lambda i: (jnp.maximum(i - steps // I2, I0), I0))
        block = lambda n: pl.BlockSpec((BLOCK, n), lambda i: (i, I0))
        pltpu.emit_pipeline(body, grid=(steps,), in_specs=[low, high, low, high],
                            out_specs=[block(ffn // I2), block(I3 * half), block(half), block(width), block(width)])(
            h_same, h_other, a_same, a_other, u_o, qkv_o, ctx_o, n1_o, n2_o)
    received()


def owner_recompute(dims, early, again, h_rows, a_rows, gains, w_qkv, w_up):
    micro, seq, width, heads, head_dim, ffn = dims
    half = heads // I2 * HEAD_PAD
    tokens = I2 * micro * seq
    any_spec = pl.BlockSpec(memory_space=ANY)
    vmem = pltpu.VMEM
    earlier = () if early else tuple(again)
    act = (micro, seq, width)
    out_shape = [jax.ShapeDtypeStruct((I8, 128), F32), *shapes((tokens, ffn // I2), (tokens, I3 * half), (tokens, half), (tokens, width), (tokens, width))]
    if not early:
        out_shape += shapes((micro, I2, seq, width), act)
    aliases = {} if early else {9 + i: I1 + i for i in range(5)} | {14: 7}
    comm = {} if early else dict(collective_id=I3)
    return pl.pallas_call(
        functools.partial(recompute_kernel, dims, early),
        out_shape=tuple(out_shape),
        in_specs=[any_spec] * I4 + [pl.BlockSpec(memory_space=vmem)] + [any_spec] * (I3 + len(earlier)),
        out_specs=(any_spec,) * len(out_shape),
        scratch_shapes=[vmem((I3, width, CHUNK), BF), vmem((width, ffn // I2), BF), pltpu.SMEM((I1,), jnp.int32), pltpu.SemaphoreType.DMA((I2, I3)), pltpu.SemaphoreType.DMA((I4,))],
        input_output_aliases=aliases,
        compiler_params=pltpu.CompilerParams(**comm, has_side_effects=True, vmem_limit_bytes=VMEM_LIMIT),
        name='owner_recompute',
    )(*h_rows, *a_rows, gains, *w_qkv, w_up, *earlier)


def spread_dx(step, last, dx, d_in, og_same, og_other, bounce, here_sem, parent_sem, sib_sem, send_sems, og_sems, ready):
    place = Place()
    micro = dx.shape[I0]
    along_x = place.at(place.tp, (place.stage + I2) % I4)
    barrier = pltpu.get_barrier_semaphore()
    is_leaf = place.home > I1
    gives_g = (place.home == I1) & place.is_l
    takes_g = (place.home == I0) & jnp.logical_not(place.is_l)
    late = late_rows(micro)
    rest_same = [m for m in late if m >= I4]

    def block(m):
        return d_in.at[m, place.core]

    def to_sibling(m, src):
        remote(src, block(m), send_sems.at[I0], sib_sem, place.sibling).start()

    def tell(there):
        pl.semaphore_signal(barrier, inc=I1, device_id=there, device_id_type=MESH)

    @pl.when(step == I0)
    def _():
        tell(place.sibling)

        @pl.when(takes_g)
        def _():
            tell(place.across)

        @pl.when(is_leaf)
        def _():
            pl.semaphore_wait(barrier, I2)
            pl.semaphore_signal(ready, inc=I1, device_id=along_x, device_id_type=MESH)

        @pl.when(jnp.logical_not(is_leaf))
        def _():
            tell(along_x)
            pl.semaphore_wait(barrier, I1 + gives_g.astype(jnp.int32))

        @pl.when(gives_g)
        def _():
            for m in rest_same:
                remote(og_same.at[m], og_same.at[m], og_sems.at[I2], og_sems.at[I3], place.across).start()
            for m in late:
                remote(og_other.at[m], og_other.at[m], og_sems.at[I0], og_sems.at[I1], place.across).start()

    @pl.when((step == I1) & jnp.logical_not(is_leaf))
    def _():
        pl.semaphore_wait(ready, I1)
        for m in reversed(range(micro)):
            if m < micro - EARLY_DX:
                remote(dx.at[m], block(m), send_sems.at[I1], parent_sem.at[m], along_x).start()
            to_sibling(m, dx.at[m])
        pltpu.make_async_copy(dx, bounce, here_sem).start()

    @pl.when((step == I2) & jnp.logical_not(is_leaf))
    def _():
        pltpu.make_async_copy(dx, bounce, here_sem).wait()
        for m in range(micro):
            pltpu.make_async_copy(bounce.at[m], block(m), here_sem).start()

    part, part_same = og_other.at[I0:len(late)], og_same.at[I0:len(rest_same)]

    @pl.when((step == I1) & takes_g)
    def _():
        remote(part_same, part_same, og_sems.at[I2], og_sems.at[I3], place.across).wait_recv()

    @pl.when((step == I3) & takes_g)
    def _():
        remote(part, part, og_sems.at[I0], og_sems.at[I1], place.across).wait_recv()

    first = micro - EARLY_DX
    for when, rows in ((I1, range(first, micro)), (last - I2, range(first // I2, first)), (last, range(first // I2))):
        @pl.when((step == when) & is_leaf)
        def _(rows=rows):
            for m in reversed(rows):
                if m < first:
                    remote(block(m), block(m), send_sems.at[I0], parent_sem.at[m], place.sibling).wait_recv()
                to_sibling(m, block(m))

    @pl.when(step == last)
    def _():
        remote(dx, dx, send_sems.at[I0], sib_sem, place.sibling).wait_send()

        @pl.when(jnp.logical_not(is_leaf))
        def _():
            rest = dx.at[I0:micro - EARLY_DX]
            remote(rest, rest, send_sems.at[I1], sib_sem, place.sibling).wait_send()
            pltpu.make_async_copy(dx, dx, here_sem).wait()

        @pl.when(gives_g)
        def _():
            remote(part, part, og_sems.at[I0], og_sems.at[I1], place.across).wait_send()
            remote(part_same, part_same, og_sems.at[I2], og_sems.at[I3], place.across).wait_send()
        remote(dx, dx, send_sems.at[I0], sib_sem, place.sibling).wait_recv()


def owner_backward_kernel(dims, dx, ds, do, u, qkv, wo, wd_near, wd_own, gs_in, go_in, d_first, dqkv, dup, z, d_in, og_other, og_same,
                          dmid, gbuf, dctx, wobuf, wdbuf, bounce, sem, wd_sem, g_sem, here_sem, parent_sem, sib_sem, send_sems, og_sems, ready):
    micro, seq, width, heads, head_dim, ffn = dims
    half = heads // I2 * HEAD_PAD
    scale = head_dim ** -0.5
    step, steps = pl.program_id(I0), pl.num_programs(I0)
    spread_dx(step, steps - I1, dx, d_in, og_same, og_other, bounce, here_sem, parent_sem, sib_sem, send_sems, og_sems, ready)

    def g_load(n, start):
        rows = BLOCK // seq
        for og, low in ((og_same, I0), (og_other, steps // I2)):
            @pl.when((n >= low) & (n < low + steps // I2))
            def _(og=og, low=low):
                copy = pltpu.make_async_copy(og.at[pl.ds((n - low) * rows, rows)], gbuf.at[n % I2], g_sem.at[n % I2])
                copy.start() if start else copy.wait()

    @pl.when(step == I0)
    def _():
        g_load(step, True)
        is_l = Place().is_l
        for condition, wd in ((is_l, wd_near), (jnp.logical_not(is_l), wd_own)):
            pl.when(condition)(pltpu.make_async_copy(wd, wdbuf, wd_sem).start)
        wobuf[...] = jnp.zeros_like(wobuf)
        load_heads(wo, I0, wobuf, sem)
        pltpu.make_async_copy(wo, wobuf.at[I0:wo.shape[I0]], sem).wait()
        pltpu.make_async_copy(wd_near, wdbuf, wd_sem).wait()
    g_load(step + I1, True)

    @pl.when(step < steps // I2)
    def _():
        dmid[...] = ds[...]

    @pl.when(step >= steps // I2)
    def _():
        dmid[...] = do[...]

    def ctx_step(j, c):
        rows = pl.ds(pl.multiple_of(j * SUB, SUB), SUB)
        dctx[:, lanes(j * SUB, SUB)] = mm_nt(dmid[...], wobuf[rows, :]).astype(BF)
        return c
    lax.fori_loop(I0, half // SUB, ctx_step, I0)
    g_load(step, False)
    grad = gbuf.at[step % I2]

    def mlp_block(n):
        cols = lanes(n * SUB, SUB)
        dz = mm(grad[...].reshape(BLOCK, width), wdbuf[n // I4, :, lanes(n % I4 * SUB, SUB)]).astype(BF).astype(F32)
        up = u[:, cols].astype(F32)
        gate, up2 = gelu_gate(up)
        hidden = up * gate
        z[:, cols] = hidden.astype(BF)
        dup[:, cols] = (dz * gelu_slope(hidden, gate, up2)).astype(BF)

    def both_step(j, c):
        base = j * (I2 * HEAD_PAD)
        at = [(pl.ds(s, seq), base + r * HEAD_PAD) for s in range(I0, BLOCK, seq) for r in range(I2)]
        group = [(*(qkv[rows, lanes(t * half + col, HEAD_PAD)] for t in range(I3)), dctx[rows, lanes(col, HEAD_PAD)]) for rows, col in at]
        blocks = [functools.partial(mlp_block, j * I3 + r) for r in range(I3)]
        for (rows, col), grads in zip(at, attention_backward(group, scale, blocks)):
            for t, value in enumerate(grads):
                dqkv[rows, lanes(t * half + col, HEAD_PAD)] = value
        return c
    lax.fori_loop(I0, heads // I4, both_step, I0)


def owner_backward(dims, dx, d_in, d_rows, og, ups, qkv, w_out, w_down):
    micro, seq, width, heads, head_dim, ffn = dims
    half = heads // I2 * HEAD_PAD
    tokens = I2 * micro * seq
    blocks = tokens // BLOCK
    vmem, dma = pltpu.VMEM, pltpu.SemaphoreType.DMA
    any_spec = pl.BlockSpec(memory_space=ANY)
    low = pl.BlockSpec((BLOCK, width), lambda i: (jnp.minimum(i, blocks // I2 - I1), I0))
    high = pl.BlockSpec((BLOCK, width), lambda i: (jnp.maximum(i - blocks // I2, I0), I0))
    attn_block = pl.BlockSpec((BLOCK, I3 * half), lambda i: (i, I0))
    mlp_block = pl.BlockSpec((BLOCK, ffn // I2), lambda i: (i, I0))
    act = (micro, seq, width)
    return pl.pallas_call(
        functools.partial(owner_backward_kernel, dims),
        grid=(blocks,),
        out_shape=tuple(shapes((tokens, I3 * half), (tokens, ffn // I2), (tokens, ffn // I2), (micro, I2, seq, width), act, act)),
        in_specs=[any_spec, low, high, mlp_block, attn_block, *[any_spec] * I6],
        out_specs=(attn_block, mlp_block, mlp_block, any_spec, any_spec, any_spec),
        scratch_shapes=[vmem((BLOCK, width), BF), vmem((I2, BLOCK // seq, seq, width), BF), vmem((BLOCK, half), BF), vmem((half, width), BF), vmem((I3, width, CHUNK), BF), vmem(act, BF),
                        dma(()), dma(()), dma((I2,)), dma(()), dma((micro,)), dma(()), dma((I2,)), dma((I4,)), pltpu.SemaphoreType.REGULAR],
        input_output_aliases={I8: 5, 9: I4, 10: I3},
        compiler_params=pltpu.CompilerParams(collective_id=I2, has_side_effects=True, vmem_limit_bytes=VMEM_LIMIT),
        name='owner_backward',
    )(dx, *d_rows, ups, qkv, w_out, *w_down, *og, d_in)


def bring(pairs, sem):
    copies = [pltpu.make_async_copy(src, dst, sem.at[i]) for i, (src, dst) in enumerate(pairs)]
    for copy in copies:
        copy.start()
    for copy in copies:
        copy.wait()


def attn_products_kernel(dq, dk, dv, ctx, n1_o, ds, do, dx_in, dwq, dwo, dx_out, n1, dmid, dqkvt, ctxt, bounce, sem, dx_sem):
    tokens, width = n1.shape
    part = tokens // I2
    head_dim = dwo.shape[I1]
    step, last = pl.program_id(I0), pl.num_programs(I0) - I1
    into, out_of = pltpu.make_async_copy(dx_in, bounce, dx_sem), pltpu.make_async_copy(bounce, dx_out, dx_sem)

    @pl.when(step == I1)
    def _():
        into.start()

    @pl.when(step == I2)
    def _():
        into.wait()
        out_of.start()

    @pl.when(step == last)
    def _():
        out_of.wait()

    @pl.when(step == I0)
    def _():
        bring([(n1_o, n1), (ds, dmid.at[pl.ds(I0, part)]), (do, dmid.at[pl.ds(part, part)])], sem)

    def turn(rows):
        for t, block in enumerate((dq, dk, dv)):
            for r in range(I2):
                at = (I2 * t + r) * head_dim
                dqkvt[at:at + head_dim, rows] = block[rows, r * HEAD_PAD:(r + I1) * HEAD_PAD].T[I0:head_dim]
        for r in range(I2):
            ctxt[r * head_dim:(r + I1) * head_dim, rows] = ctx[rows, r * HEAD_PAD:(r + I1) * HEAD_PAD].T[I0:head_dim]
    rows_loop(tokens, SUB, turn)
    for c in range(I0, width, SUB):
        cut = slice(c, c + SUB)
        dwq[:, :, :, cut] = mm(dqkvt[...], n1[:, cut]).reshape(I3, I2, head_dim, SUB)
        dwo[:, :, cut] = mm(ctxt[...], dmid[:, cut]).reshape(I2, head_dim, SUB)


def attn_products(dqkv, ctx, n1, d_rows, dx, out_dims):
    heads, head_dim, width = out_dims
    tokens = n1.shape[I0]
    vmem = pltpu.VMEM
    any_spec = pl.BlockSpec(memory_space=ANY)
    pairs = heads // I2
    cols = lambda t: pl.BlockSpec((tokens, I2 * HEAD_PAD), lambda i: (I0, t * pairs + i))
    return pl.pallas_call(
        attn_products_kernel,
        grid=(pairs,),
        out_shape=(jax.ShapeDtypeStruct((I3,) + out_dims, F32), jax.ShapeDtypeStruct(out_dims, F32), jax.ShapeDtypeStruct(dx.shape, BF)),
        in_specs=[cols(I0), cols(I1), cols(I2), cols(I0), any_spec, any_spec, any_spec, any_spec],
        out_specs=(pl.BlockSpec((I3, I2, head_dim, width), lambda i: (I0, i, I0, I0)), pl.BlockSpec((I2, head_dim, width), lambda i: (i, I0, I0)), any_spec),
        scratch_shapes=[vmem((tokens, width), BF), vmem((tokens, width), BF), vmem((I6 * head_dim, tokens), BF), vmem((I2 * head_dim, tokens), BF),
                        vmem(dx.shape, BF), pltpu.SemaphoreType.DMA((I3,)), pltpu.SemaphoreType.DMA(())],
        compiler_params=pltpu.CompilerParams(vmem_limit_bytes=VMEM_LIMIT),
        name='attn_products',
    )(dqkv, dqkv, dqkv, ctx, n1, *d_rows, dx)


def mlp_products_kernel(dup, z, n2_o, gs, go, dwu, dwd, n2t, grad, zt, stage, sem):
    width, tokens = n2t.shape
    part = tokens // I2

    @pl.when(pl.program_id(I0) == I0)
    def _():
        bring([(n2_o, stage), (gs, grad.at[pl.ds(I0, part)]), (go, grad.at[pl.ds(part, part)])], sem)

        def turn(rows):
            for c in range(I0, width, SUB):
                n2t[c:c + SUB, rows] = stage[rows, c:c + SUB].T
        rows_loop(tokens, SUB, turn)

    def turn_z(rows):
        for c in range(I0, z.shape[I1], SUB):
            zt[c:c + SUB, rows] = z[rows, c:c + SUB].T
    rows_loop(tokens, SUB, turn_z)
    for c in range(I0, width, I2 * SUB):
        dwu[c:c + I2 * SUB, :] = mm(n2t[c:c + I2 * SUB, :], dup[...])
    for c in range(I0, width, SUB):
        dwd[:, c:c + SUB] = mm(zt[...], grad[:, c:c + SUB])


def mlp_products(dup, hidden, n2, g_rows):
    tokens, width = n2.shape
    cols = dup.shape[I1]
    vmem = pltpu.VMEM
    any_spec = pl.BlockSpec(memory_space=ANY)
    block = pl.BlockSpec((tokens, SUB), lambda i: (I0, i))
    return pl.pallas_call(
        mlp_products_kernel,
        grid=(cols // SUB,),
        out_shape=(jax.ShapeDtypeStruct((width, cols), F32), jax.ShapeDtypeStruct((cols, width), F32)),
        in_specs=[block, block, any_spec, any_spec, any_spec],
        out_specs=(pl.BlockSpec((width, SUB), lambda i: (I0, i)), pl.BlockSpec((SUB, width), lambda i: (i, I0))),
        scratch_shapes=[vmem((width, tokens), BF), vmem((tokens, width), BF), vmem((SUB, tokens), BF), vmem((tokens, width), BF), pltpu.SemaphoreType.DMA((I3,))],
        compiler_params=pltpu.CompilerParams(vmem_limit_bytes=VMEM_LIMIT),
        name='mlp_products',
    )(dup, hidden, n2, *g_rows)


def solution(mesh):
    act_spec = P('rep', None, None, None)
    weight_specs = (
        P(('rep', 'stage'), None, None, 'tp', None),
        P(('rep', 'stage'), 'tp', None, None),
        P(('rep', 'stage'), None, 'tp'),
        P(('rep', 'stage'), 'tp', None),
        P(('rep', 'stage'), None),
        P(('rep', 'stage'), None),
    )

    def device_fn(inputs, targets, w_qkv, w_out, w_up, w_down, gain_attn, gain_mlp):
        micro_count, _, seq_len, width = inputs.shape
        dims = (micro_count, seq_len, width, I2 * w_out.shape[I1], w_out.shape[I2], I2 * w_up.shape[I2])
        norm_factor = 1.0 / (inputs.size)
        own = (w_qkv[I0], w_out[I0], w_up[I0], w_down[I0])
        own_gains = jnp.concatenate([gain_attn, gain_mlp]).astype(F32)
        rows_of = (own[I0].transpose(I1, I2, I3, I0).reshape(-I1, width), own[I1].reshape(-I1, width), own[I2], own[I3])

        (acts, mids, qkv, ups, seeds, oh_same, oh_other, oa_same, oa_other, og_same, og_other, loss_tile, home_gains, *weights) = forward_phase(dims, inputs, targets, rows_of, own_gains)
        (nq, no, nu, nd), (fq, fo, fu, fd) = weights[I0:I4], weights[I4:I8]
        (tq0, to0, tu0, td0), (tq1, to1, tu1, td1), (tqo, tdo) = weights[I8:12], weights[12:16], weights[18:20]

        flat = lambda *rows: [r.reshape(-I1, width) for r in rows]
        done, *again = owner_recompute(dims, True, None, flat(oh_same, oh_other), flat(oa_same, oa_other), own_gains, (tq0, tqo), own[I2])
        dx, _, od_same, od_other, og_same, og_other, oa_same, oa_other, oh_same, oh_other, dg_same, dg_other, loss_all = backward_phase(
            dims, (acts, mids, qkv, ups, seeds), (rows_of[I0], nq, fq, td0, td1, to0, to1, tu0, tu1), home_gains, loss_tile, done,
            (og_same, og_other, oa_same, oa_other, oh_same, oh_other))
        _, *again, d_first, og_same = owner_recompute(dims, False, (dx, *again, og_same), flat(oh_same, oh_other), flat(oa_same, oa_other), own_gains, (tq0, tqo), own[I2])
        ups_own, qkv_own, ctx_own, n1, n2 = again
        d_rows = flat(od_same, od_other)
        d_qkv_rows, d_up_rows, hidden, dx_all, og_other, og_same = owner_backward(
            dims, dx, d_first, d_rows, (og_same, og_other), ups_own, qkv_own, rows_of[I1], (td0, tdo))
        d_qkv, d_out, d_inputs = attn_products(d_qkv_rows, ctx_own, n1, d_rows, dx_all, w_out.shape[I1:])
        d_up, d_down = mlp_products(d_up_rows, hidden, n2, flat(og_same, og_other))
        weight_grads = (d_qkv.transpose(I3, I0, I1, I2), d_out, d_up, d_down)
        mine = jnp.sum(dg_same + dg_other, I1)
        loss = jnp.sum(loss_all) * (0.5 * norm_factor)

        return (loss.reshape(I1), d_inputs) + tuple(g[None] for g in weight_grads) + (mine[I0][None], mine[I1][None])

    return jax.shard_map(device_fn, mesh=mesh, in_specs=(act_spec, act_spec) + weight_specs, out_specs=(P('rep'), act_spec) + weight_specs, check_vma=False)
```
